16 devices in a mesh: sp: 16 (over z, y, x, core).
Axes of the slice: x: 2, y: 2, z: 2, core: 2. Of those that a mesh axis runs over, the one named last changes fastest.
Arguments:
- x_in: bfloat16 [2048, 2048], P('sp')
- positions: int32 [2048], P('sp')
- d_out: bfloat16 [2048, 2048], P('sp')
- norm1_gain: bfloat16 [2048], P('sp')
- norm2_gain: bfloat16 [2048], P('sp')
- w_q: bfloat16 [2048, 32, 64], P('sp')
- w_k: bfloat16 [2048, 4, 64], P('sp')
- w_v: bfloat16 [2048, 4, 64], P('sp')
- w_o: bfloat16 [32, 64, 2048], P('sp')
- w_gate: bfloat16 [2048, 5632], P('sp')
- w_up: bfloat16 [2048, 5632], P('sp')
- w_down: bfloat16 [5632, 2048], P('sp')
Outputs:
- output 1: bfloat16 [2048, 2048], P('sp')
- output 2: bfloat16 [2048, 2048], P('sp')
- output 3: float32 [2048], P('sp')
- output 4: float32 [2048], P('sp')
- output 5: float32 [2048, 32, 64], P('sp')
- output 6: float32 [2048, 4, 64], P('sp')
- output 7: float32 [2048, 4, 64], P('sp')
- output 8: float32 [32, 64, 2048], P('sp')
- output 9: float32 [2048, 5632], P('sp')
- output 10: float32 [2048, 5632], P('sp')
- output 11: float32 [5632, 2048], P('sp')
All inputs are finite; a program needn't handle non-finite values.
Results may differ from the reference program's by a relative error of at most 0.019747.
Values are sent between devices in bfloat16 or wider.
A program may use at most 1 GiB of HBM per device.

```python
import math
import jax
import jax.numpy as jnp
from jax import lax

MODEL_DIM = 2048
FFN_DIM = 5632
Q_HEADS = 32
KV_HEADS = 4
HEAD_DIM = 64
SEQ_LEN = 2048

ROPE_BASE = 10000.0
NORM_EPS = 1e-5
NEG_LARGE = -1e30
GROUP_SIZE = Q_HEADS // KV_HEADS
HALF_DIM = HEAD_DIM // 2


def setup_inputs(seed: int = 0) -> dict:
    key_list = jax.random.split(jax.random.key(seed), 12)
    qk_gain = math.log(SEQ_LEN / 4.0) ** 0.25

    def normal_draw(key_one, shape, scale_by):
        return (jax.random.normal(key_one, shape, jnp.float32) * scale_by).astype(jnp.bfloat16)

    def gain_draw(key_one):
        return (0.6 + 0.8 * jax.random.uniform(key_one, (MODEL_DIM,), jnp.float32)).astype(jnp.bfloat16)

    pos_gaps = jax.random.randint(key_list[1], (SEQ_LEN,), 1, 4, jnp.int32)
    positions = (jnp.cumsum(pos_gaps) - pos_gaps[0]).astype(jnp.int32)
    return {
        'x_in': normal_draw(key_list[0], (SEQ_LEN, MODEL_DIM), 1.0),
        'positions': positions,
        'd_out': normal_draw(key_list[2], (SEQ_LEN, MODEL_DIM), 1.0),
        'norm1_gain': gain_draw(key_list[3]),
        'norm2_gain': gain_draw(key_list[4]),
        'w_q': normal_draw(key_list[5], (MODEL_DIM, Q_HEADS, HEAD_DIM), qk_gain * MODEL_DIM ** -0.5),
        'w_k': normal_draw(key_list[6], (MODEL_DIM, KV_HEADS, HEAD_DIM), qk_gain * MODEL_DIM ** -0.5),
        'w_v': normal_draw(key_list[7], (MODEL_DIM, KV_HEADS, HEAD_DIM), MODEL_DIM ** -0.5),
        'w_o': normal_draw(key_list[8], (Q_HEADS, HEAD_DIM, MODEL_DIM), (Q_HEADS * HEAD_DIM) ** -0.5),
        'w_gate': normal_draw(key_list[9], (MODEL_DIM, FFN_DIM), MODEL_DIM ** -0.5),
        'w_up': normal_draw(key_list[10], (MODEL_DIM, FFN_DIM), MODEL_DIM ** -0.5),
        'w_down': normal_draw(key_list[11], (FFN_DIM, MODEL_DIM), FFN_DIM ** -0.5),
    }


def keep_bf16(values_in):
    return values_in.astype(jnp.bfloat16).astype(jnp.float32)


def rms_norm(hidden, gain_vec):
    inv_rms = lax.rsqrt(jnp.mean(hidden * hidden, axis=-1, keepdims=True) + NORM_EPS)
    return keep_bf16(hidden * inv_rms * gain_vec)


def apply_rope(values_in, cos_tab, sin_tab):
    first_half = values_in[..., :HALF_DIM]
    second_half = values_in[..., HALF_DIM:]
    return jnp.concatenate([first_half * cos_tab - second_half * sin_tab, second_half * cos_tab + first_half * sin_tab], axis=-1)


def head_attention(operands):
    q_head, k_head, v_head = operands
    scores = jnp.dot(q_head, k_head.T, preferred_element_type=jnp.float32) * HEAD_DIM ** -0.5
    causal = jnp.arange(SEQ_LEN)[:, None] >= jnp.arange(SEQ_LEN)[None, :]
    attn_probs = jax.nn.softmax(jnp.where(causal, scores, NEG_LARGE), axis=-1)
    return keep_bf16(jnp.dot(keep_bf16(attn_probs), v_head, preferred_element_type=jnp.float32))


def layer_forward(x_f32, cos_tab, sin_tab, gain_first, gain_second, wq_f32, wk_f32, wv_f32, wo_f32, gate_f32, up_f32, down_f32):
    normed = rms_norm(x_f32, gain_first)
    q_lin = keep_bf16(jnp.einsum('td,dhe->the', normed, wq_f32))
    k_lin = keep_bf16(jnp.einsum('td,dhe->the', normed, wk_f32))
    v_lin = keep_bf16(jnp.einsum('td,dhe->the', normed, wv_f32))
    queries = keep_bf16(apply_rope(q_lin, cos_tab, sin_tab))
    keys_rot = keep_bf16(apply_rope(k_lin, cos_tab, sin_tab))
    keys_full = jnp.repeat(keys_rot, GROUP_SIZE, axis=1)
    values_full = jnp.repeat(v_lin, GROUP_SIZE, axis=1)
    attn_heads = lax.map(jax.checkpoint(head_attention), (queries.transpose(1, 0, 2), keys_full.transpose(1, 0, 2), values_full.transpose(1, 0, 2)))
    attn_proj = jnp.einsum('hte,hed->td', attn_heads, wo_f32)
    hidden = keep_bf16(x_f32 + attn_proj)
    mlp_in = rms_norm(hidden, gain_second)
    gate_act = keep_bf16(jnp.dot(mlp_in, gate_f32, preferred_element_type=jnp.float32))
    up_act = keep_bf16(jnp.dot(mlp_in, up_f32, preferred_element_type=jnp.float32))
    glu_out = keep_bf16(jax.nn.silu(gate_act) * up_act)
    return keep_bf16(hidden + jnp.dot(glu_out, down_f32, preferred_element_type=jnp.float32))


def reference(x_in, positions, d_out, norm1_gain, norm2_gain, w_q, w_k, w_v, w_o, w_gate, w_up, w_down):
    inv_freq = 1.0 / (ROPE_BASE ** (jnp.arange(HALF_DIM, dtype=jnp.float32) * (2.0 / HEAD_DIM)))
    angles = positions.astype(jnp.float32)[:, None] * inv_freq[None, :]
    cos_tab = jnp.cos(angles)[:, None, :]
    sin_tab = jnp.sin(angles)[:, None, :]

    def forward_fn(x_f32, gain_first, gain_second, wq_f32, wk_f32, wv_f32, wo_f32, gate_f32, up_f32, down_f32):
        return layer_forward(x_f32, cos_tab, sin_tab, gain_first, gain_second, wq_f32, wk_f32, wv_f32, wo_f32, gate_f32, up_f32, down_f32)

    to_f32 = [tensor.astype(jnp.float32) for tensor in (x_in, norm1_gain, norm2_gain, w_q, w_k, w_v, w_o, w_gate, w_up, w_down)]
    y_f32, pullback = jax.vjp(forward_fn, to_f32[0], to_f32[1], to_f32[2], to_f32[3], to_f32[4], to_f32[5], to_f32[6], to_f32[7], to_f32[8], to_f32[9])
    grad_list = pullback(d_out.astype(jnp.float32))
    return (y_f32.astype(jnp.bfloat16), grad_list[0].astype(jnp.bfloat16), grad_list[1], grad_list[2], grad_list[3], grad_list[4], grad_list[5], grad_list[6], grad_list[7], grad_list[8], grad_list[9])
```

```python
import functools
import jax
import jax.numpy as jnp
from jax import lax
from jax.sharding import PartitionSpec as P

ROPE_BASE = 10000.0
NORM_EPS = 1e-5
NEG_LARGE = -1e30
F32 = jnp.float32
BF16 = jnp.bfloat16


def norm_forward(hidden, gain_vec):
    inv_rms = lax.rsqrt(jnp.mean(hidden * hidden, axis=-1, keepdims=True) + NORM_EPS)
    return hidden * inv_rms * gain_vec


def rope_tables(positions, head_dim):
    half_dim = head_dim // 2
    inv_freq = 1.0 / (ROPE_BASE ** (jnp.arange(half_dim, dtype=F32) * (2.0 / head_dim)))
    angles = positions.astype(F32)[:, None] * inv_freq[None, :]
    return jnp.cos(angles)[:, None, :], jnp.sin(angles)[:, None, :]


def rotate(values_in, cos_tab, sin_tab):
    half_dim = values_in.shape[-1] // 2
    first_half = values_in[..., :half_dim].astype(F32)
    second_half = values_in[..., half_dim:].astype(F32)
    return jnp.concatenate([first_half * cos_tab - second_half * sin_tab, second_half * cos_tab + first_half * sin_tab], axis=-1)


def gated_unit(gate_pre, up_pre):
    return jax.nn.silu(gate_pre) * up_pre


def attention_forward(queries, keys_all, values_all):
    seq_len = queries.shape[0]
    score_scale = queries.shape[-1] ** -0.5
    scores = jnp.einsum('sgd,td->gst', queries, keys_all, preferred_element_type=F32) * score_scale
    causal = jnp.arange(seq_len)[:, None] >= jnp.arange(seq_len)[None, :]
    attn_probs = jax.nn.softmax(jnp.where(causal, scores, NEG_LARGE), axis=-1)
    attn_out = jnp.einsum('gst,td->sgd', attn_probs.astype(BF16), values_all, preferred_element_type=F32)
    return attn_out.astype(BF16), attn_probs


def attention_backward(queries, keys_all, values_all, attn_probs, d_attn):
    score_scale = queries.shape[-1] ** -0.5
    probs_b16 = attn_probs.astype(BF16)
    d_probs = jnp.einsum('sgd,td->gst', d_attn, values_all, preferred_element_type=F32)
    d_probs = d_probs.astype(BF16).astype(F32)
    row_dot = jnp.sum(d_probs * attn_probs, axis=-1, keepdims=True)
    d_scores = (attn_probs * (d_probs - row_dot) * score_scale).astype(BF16)
    d_queries = jnp.einsum('gst,td->sgd', d_scores, keys_all, preferred_element_type=F32)
    d_keys = jnp.einsum('gst,sgd->td', d_scores, queries, preferred_element_type=F32)
    d_values = jnp.einsum('gst,sgd->td', probs_b16, d_attn, preferred_element_type=F32)
    return d_queries.astype(BF16), d_keys.astype(BF16), d_values.astype(BF16)


def solution(mesh):
    n_dev = mesh.shape['sp']
    gather = functools.partial(lax.all_gather, axis_name='sp', axis=0, tiled=True)
    scatter = functools.partial(lax.psum_scatter, axis_name='sp', scatter_dimension=0, tiled=True)
    swap = functools.partial(lax.all_to_all, axis_name='sp', split_axis=0, concat_axis=0, tiled=True)

    def layer_step(x_in, positions, d_out, norm1_gain, norm2_gain, w_q, w_k, w_v, w_o, w_gate, w_up, w_down):
        tokens, dim = x_in.shape
        seq_len = tokens * n_dev
        n_q, hd = w_q.shape[1], w_q.shape[2]
        n_kv = w_k.shape[1]
        hpd = n_q // n_dev
        qw, kw = hpd * hd, hd
        rows = w_q.shape[0]
        feat = w_down.shape[0]
        me = lax.axis_index('sp')

        small = jnp.stack([norm1_gain.astype(F32), norm2_gain.astype(F32), positions.astype(F32)])
        small_all = gather(small[None])
        g1 = small_all[:, 0].reshape(-1)
        g2 = small_all[:, 1].reshape(-1)
        pos_all = small_all[:, 2].reshape(-1)
        cos_tab, sin_tab = rope_tables(positions, hd)
        cos_all, sin_all = rope_tables(pos_all, hd)

        wqkv = gather(jnp.concatenate([w_q.reshape(rows, n_q * hd), w_k.reshape(rows, n_kv * hd), w_v.reshape(rows, n_kv * hd)], axis=1))
        wo_own = w_o.reshape(qw, dim)
        wo_full = gather(wo_own)

        def by_feature(w):
            return w.T.reshape(n_dev, feat, rows)
        wgu = swap(jnp.concatenate([by_feature(w_gate), by_feature(w_up)], axis=1))
        wgu = wgu.transpose(1, 0, 2).reshape(2 * feat, dim)

        x_f32 = x_in.astype(F32)
        normed_pre, norm1_pull = jax.vjp(norm_forward, x_f32, g1)
        normed = normed_pre.astype(BF16)
        qkv = jnp.dot(normed, wqkv, preferred_element_type=F32).astype(BF16)
        q_rot = rotate(qkv[:, :n_q * hd].reshape(tokens, n_q, hd), cos_tab, sin_tab).astype(BF16)
        k_rot = rotate(qkv[:, n_q * hd:(n_q + n_kv) * hd].reshape(tokens, n_kv, hd), cos_tab, sin_tab).astype(BF16)
        v_lin = qkv[:, (n_q + n_kv) * hd:].reshape(tokens, n_kv, hd)
        rep = n_dev // n_kv
        send = jnp.concatenate([
            q_rot.reshape(tokens, n_dev, qw).transpose(1, 0, 2),
            jnp.repeat(k_rot.transpose(1, 0, 2), rep, axis=0),
            jnp.repeat(v_lin.transpose(1, 0, 2), rep, axis=0)], axis=2)
        seq = swap(send).reshape(seq_len, qw + 2 * kw)
        q_seq = seq[:, :qw].reshape(seq_len, hpd, hd)
        k_seq = seq[:, qw:qw + kw]
        v_seq = seq[:, qw + kw:]
        attn_seq, attn_probs = attention_forward(q_seq, k_seq, v_seq)
        attn_seq = attn_seq.reshape(seq_len, qw)
        attn_tok = swap(attn_seq.reshape(n_dev, tokens, qw)).transpose(1, 0, 2).reshape(tokens, n_q * hd)
        attn_proj = jnp.dot(attn_tok, wo_full, preferred_element_type=F32)
        hidden = (x_f32 + attn_proj).astype(BF16)
        hidden_f32 = hidden.astype(F32)
        mlp_pre, norm2_pull = jax.vjp(norm_forward, hidden_f32, g2)
        mlp_in = mlp_pre.astype(BF16)

        m_full = gather(mlp_in)
        do_full = gather(d_out)
        u_full = gather(normed)
        gu = jnp.einsum('fd,td->ft', wgu, m_full, preferred_element_type=F32).astype(BF16)
        gate_act, up_act = gu[:feat], gu[feat:]
        glu_pre, glu_pull = jax.vjp(gated_unit, gate_act.astype(F32), up_act.astype(F32))
        glu = glu_pre.astype(BF16)
        y_part = jnp.einsum('ft,fd->td', glu, w_down, preferred_element_type=F32)
        y_out = (hidden_f32 + scatter(y_part)).astype(BF16)

        d_down = jnp.einsum('ft,td->fd', glu, do_full, preferred_element_type=F32)
        d_glu = jnp.einsum('fd,td->ft', w_down, do_full, preferred_element_type=F32).astype(BF16)
        d_gate_f, d_up_f = glu_pull(d_glu.astype(F32))
        dgu = jnp.concatenate([d_gate_f.astype(BF16), d_up_f.astype(BF16)], axis=0)
        dm_part = jnp.einsum('ft,fd->td', dgu, wgu, preferred_element_type=F32)
        d_mlp_in = scatter(dm_part).astype(BF16)
        d_hidden_norm, d_g2 = norm2_pull(d_mlp_in.astype(F32))
        d_hidden = (d_out.astype(F32) + d_hidden_norm).astype(BF16)
        dh_full = gather(d_hidden)

        dwgu = jnp.einsum('ft,td->fd', dgu, m_full, preferred_element_type=F32)
        dwgu = swap(dwgu.reshape(2 * feat, n_dev, rows).transpose(1, 0, 2))
        d_gate = dwgu[:, :feat].reshape(n_dev * feat, rows).T
        d_up = dwgu[:, feat:].reshape(n_dev * feat, rows).T

        d_wo = jnp.einsum('te,td->ed', attn_seq, dh_full, preferred_element_type=F32).reshape(w_o.shape)
        d_attn = jnp.einsum('td,ed->te', dh_full, wo_own, preferred_element_type=F32).astype(BF16)
        d_q_seq, d_k_seq, d_v_seq = attention_backward(q_seq, k_seq, v_seq, attn_probs, d_attn.reshape(seq_len, hpd, hd))
        dq_lin_seq = rotate(d_q_seq, cos_all, -sin_all).astype(BF16).reshape(seq_len, qw)
        back = swap(jnp.concatenate([dq_lin_seq, d_k_seq, d_v_seq], axis=1).reshape(n_dev, tokens, qw + 2 * kw))
        d_q_lin = back[:, :, :qw].transpose(1, 0, 2).reshape(tokens, n_q * hd)
        shares = back[:, :, qw:].reshape(n_kv, rep, tokens, 2, hd)
        dkv = jnp.sum(shares, axis=1, dtype=F32).astype(BF16)
        d_k_lin = rotate(dkv[:, :, 0].transpose(1, 0, 2), cos_tab, -sin_tab).astype(BF16).reshape(tokens, n_kv * hd)
        d_v_lin = dkv[:, :, 1].transpose(1, 0, 2).reshape(tokens, n_kv * hd)
        dkv_lin = jnp.concatenate([d_k_lin, d_v_lin], axis=1)
        dkv_full = gather(dkv_lin)
        u_own = lax.dynamic_slice_in_dim(u_full, me * rows, rows, axis=1)
        d_wkv = jnp.einsum('td,te->de', u_own, dkv_full, preferred_element_type=F32)
        d_wk = d_wkv[:, :n_kv * hd].reshape(w_k.shape)
        d_wv = d_wkv[:, n_kv * hd:].reshape(w_v.shape)
        dwq = jnp.einsum('td,te->de', u_full, dq_lin_seq, preferred_element_type=F32)
        d_normed = lax.dot_general(jnp.concatenate([d_q_lin, dkv_lin], axis=1), wqkv, (((1,), (1,)), ((), ())), preferred_element_type=F32).astype(BF16)
        d_x_norm, d_g1 = norm1_pull(d_normed.astype(F32))
        d_x = (d_hidden.astype(F32) + d_x_norm).astype(BF16)
        gains = jnp.stack([d_g1.reshape(n_dev, rows), d_g2.reshape(n_dev, rows)], axis=1)
        tail = swap(jnp.concatenate([dwq.reshape(n_dev, rows, qw), jnp.pad(gains, ((0, 0), (0, 6), (0, qw - rows)))], axis=1))
        d_wq = tail[:, :rows].transpose(1, 0, 2).reshape(w_q.shape)
        gsum = jnp.sum(tail[:, rows:, :rows], axis=0)
        return (y_out, d_x, gsum[0], gsum[1], d_wq, d_wk, d_wv, d_wo, d_gate, d_up, d_down)

    all_rows = P('sp')
    return jax.shard_map(layer_step, mesh=mesh, in_specs=(all_rows,) * 12, out_specs=(all_rows,) * 11, check_vma=False)
```

```python
import functools
import jax
import jax.numpy as jnp
from jax import lax
from jax.experimental import pallas as pl
from jax.experimental.pallas import tpu as pltpu
from jax.sharding import PartitionSpec as P

ROPE_BASE = 10000.0
NORM_EPS = 1e-5
NEG_LARGE = -1e30
F32 = jnp.float32
BF16 = jnp.bfloat16


def norm_forward(hidden, gain_vec):
    inv_rms = lax.rsqrt(jnp.mean(hidden * hidden, axis=-1, keepdims=True) + NORM_EPS)
    return hidden * inv_rms * gain_vec


def rope_tables(positions, head_dim):
    half_dim = head_dim // 2
    inv_freq = 1.0 / (ROPE_BASE ** (jnp.arange(half_dim, dtype=F32) * (2.0 / head_dim)))
    angles = positions.astype(F32)[:, None] * inv_freq[None, :]
    return jnp.cos(angles)[:, None, :], jnp.sin(angles)[:, None, :]


def rotate(values_in, cos_tab, sin_tab):
    half_dim = values_in.shape[-1] // 2
    first_half = values_in[..., :half_dim].astype(F32)
    second_half = values_in[..., half_dim:].astype(F32)
    return jnp.concatenate([first_half * cos_tab - second_half * sin_tab, second_half * cos_tab + first_half * sin_tab], axis=-1)


def gated_unit(gate_pre, up_pre):
    return jax.nn.silu(gate_pre) * up_pre


NT = (((1,), (1,)), ((), ()))
TN = (((0,), (0,)), ((), ()))
NN = (((1,), (0,)), ((), ()))


def mm(a, b, dims):
    return lax.dot_general(a, b, dims, preferred_element_type=F32)


QB = 256
KB = 256


def attn_fwd_kernel(q_ref, k_ref, v_ref, o_ref, stat_ref, s_scr):
    heads, seq, hd = q_ref.shape
    scale = hd ** -0.5
    lanes = heads * QB

    def q_block(qb, carry):
        qs = pl.ds(pl.multiple_of(qb * QB, QB), QB)
        q2 = jnp.concatenate([q_ref[h, qs, :] for h in range(heads)], axis=0)

        def scores(kb, top, diagonal):
            ks = pl.ds(pl.multiple_of(kb * KB, KB), KB)
            s = mm(k_ref[ks, :], q2, NT) * scale
            if diagonal:
                key = lax.broadcasted_iota(jnp.int32, (KB, lanes), 0)
                qry = lax.broadcasted_iota(jnp.int32, (KB, lanes), 1) % QB
                s = jnp.where(qry >= key, s, NEG_LARGE)
            s_scr[ks, :] = s
            return jnp.maximum(top, jnp.max(s, axis=0, keepdims=True))

        top = lax.fori_loop(0, qb, lambda kb, t: scores(kb, t, False), jnp.full((1, lanes), NEG_LARGE, F32))
        top = scores(qb, top, True)

        def expo(kb, tot):
            ks = pl.ds(pl.multiple_of(kb * KB, KB), KB)
            e = jnp.exp(s_scr[ks, :] - top)
            s_scr[ks, :] = e
            return tot + jnp.sum(e, axis=0, keepdims=True)

        inv = 1.0 / lax.fori_loop(0, qb + 1, expo, jnp.zeros((1, lanes), F32))

        def weigh(kb, acc):
            ks = pl.ds(pl.multiple_of(kb * KB, KB), KB)
            p = (s_scr[ks, :] * inv).astype(BF16)
            return acc + mm(v_ref[ks, :], p, TN)

        acc = lax.fori_loop(0, qb + 1, weigh, jnp.zeros((hd, lanes), F32))
        for h in range(heads):
            o_ref[h * hd:(h + 1) * hd, qs] = acc[:, h * QB:(h + 1) * QB].astype(BF16)
        stat_ref[qb, 0:1, :] = top
        stat_ref[qb, 1:2, :] = inv
        return carry

    lax.fori_loop(0, seq // QB, q_block, 0)


def attn_bwd_kernel(q_ref, k_ref, v_ref, do_ref, stat_ref, dq_ref, dk_ref, dv_ref, p_scr, dp_scr, dk_acc, dv_acc):
    heads, seq, hd = q_ref.shape
    scale = hd ** -0.5
    lanes = heads * QB
    dk_acc[...] = jnp.zeros_like(dk_acc)
    dv_acc[...] = jnp.zeros_like(dv_acc)

    def q_block(qb, carry):
        qs = pl.ds(pl.multiple_of(qb * QB, QB), QB)
        q2 = jnp.concatenate([q_ref[h, qs, :] for h in range(heads)], axis=0)
        do2 = jnp.concatenate([do_ref[h, qs, :] for h in range(heads)], axis=0)
        top = stat_ref[qb, 0:1, :]
        inv = stat_ref[qb, 1:2, :]

        def probs(kb, rd, diagonal):
            ks = pl.ds(pl.multiple_of(kb * KB, KB), KB)
            s = mm(k_ref[ks, :], q2, NT) * scale
            if diagonal:
                key = lax.broadcasted_iota(jnp.int32, (KB, lanes), 0)
                qry = lax.broadcasted_iota(jnp.int32, (KB, lanes), 1) % QB
                s = jnp.where(qry >= key, s, NEG_LARGE)
            p = jnp.exp(s - top) * inv
            dp = mm(v_ref[ks, :], do2, NT).astype(BF16)
            p_scr[ks, :] = p
            dp_scr[ks, :] = dp
            dv_acc[ks, :] += mm(p.astype(BF16), do2, NN)
            return rd + jnp.sum(dp.astype(F32) * p, axis=0, keepdims=True)

        rd = lax.fori_loop(0, qb, lambda kb, r: probs(kb, r, False), jnp.zeros((1, lanes), F32))
        rd = probs(qb, rd, True)

        def scores(kb, acc):
            ks = pl.ds(pl.multiple_of(kb * KB, KB), KB)
            ds = (p_scr[ks, :] * (dp_scr[ks, :].astype(F32) - rd) * scale).astype(BF16)
            dk_acc[ks, :] += mm(ds, q2, NN)
            return acc + mm(k_ref[ks, :], ds, TN)

        acc = lax.fori_loop(0, qb + 1, scores, jnp.zeros((hd, lanes), F32))
        for h in range(heads):
            dq_ref[h * hd:(h + 1) * hd, qs] = acc[:, h * QB:(h + 1) * QB].astype(BF16)
        return carry

    lax.fori_loop(0, seq // QB, q_block, 0)
    dk_ref[...] = dk_acc[...].astype(BF16)
    dv_ref[...] = dv_acc[...].astype(BF16)


VMEM_CAP = 60 * 1024 * 1024


def in_vmem(n):
    return [pl.BlockSpec(memory_space=pltpu.VMEM)] * n


def attention_forward(q2, k, v):
    heads, seq, hd = q2.shape
    lanes = heads * QB
    return pl.pallas_call(
        attn_fwd_kernel,
        out_shape=(jax.ShapeDtypeStruct((heads * hd, seq), BF16), jax.ShapeDtypeStruct((seq // QB, 2, lanes), F32)),
        in_specs=in_vmem(3), out_specs=tuple(in_vmem(2)),
        scratch_shapes=[pltpu.VMEM((seq, lanes), F32)],
        cost_estimate=pl.CostEstimate(flops=2 * 4 * heads * seq * seq * hd, bytes_accessed=4 * seq * hd * 8, transcendentals=0),
        compiler_params=pltpu.CompilerParams(vmem_limit_bytes=VMEM_CAP),
        name='attn_fwd',
    )(q2, k, v)


def attention_backward(q2, k, v, do2, stat):
    heads, seq, hd = q2.shape
    lanes = heads * QB
    return pl.pallas_call(
        attn_bwd_kernel,
        out_shape=(jax.ShapeDtypeStruct((heads * hd, seq), BF16), jax.ShapeDtypeStruct((seq, hd), BF16), jax.ShapeDtypeStruct((seq, hd), BF16)),
        in_specs=in_vmem(5), out_specs=tuple(in_vmem(3)),
        scratch_shapes=[pltpu.VMEM((seq, lanes), F32), pltpu.VMEM((seq, lanes), BF16), pltpu.VMEM((seq, hd), F32), pltpu.VMEM((seq, hd), F32)],
        cost_estimate=pl.CostEstimate(flops=2 * 10 * heads * seq * seq * hd, bytes_accessed=4 * seq * hd * 8, transcendentals=0),
        compiler_params=pltpu.CompilerParams(vmem_limit_bytes=VMEM_CAP),
        name='attn_bwd',
    )(q2, k, v, do2, stat)


RS_ORDERS = ((2, 4, 8), (4, 8, 2), (8, 2, 4))
RS_MASKS = (14, 6, 12, 10, 2, 4, 8, 0)
RS_FIRST = ((14, 6, 10, 2), (14, 12, 6, 4), (14, 10, 12, 8))


def first_axis(colour, mask):
    return next(i for i, a in enumerate(RS_ORDERS[colour]) if mask & a)


def rs_slots(colour):
    slots = {}
    for mask in RS_MASKS:
        for axis in RS_ORDERS[colour][:first_axis(colour, mask) if mask else 3]:
            slots[mask, axis] = len(slots)
    return slots


def flipped(index, mask):
    out = index
    for bit in (1, 2, 4, 8):
        if mask & bit:
            out = out + (1 - 2 * ((index // bit) % 2)) * bit
    return out


def enter(peers):
    barrier = pltpu.get_barrier_semaphore()
    for peer in peers:
        pl.semaphore_signal(barrier, inc=1, device_id=(peer,), device_id_type=pl.DeviceIdType.MESH)
    pl.semaphore_wait(barrier, len(peers))


def rs_kernel(cols, a_ref, w_ref, base_ref, out_ref, part, pair_in, link_in, pair_send, pair_recv, link_send, link_recv):
    tokens, dim = out_ref.shape
    me = lax.axis_index('sp')
    core = me % 2
    partner = flipped(me, 1)
    enter([partner] + [flipped(me, a) for a in (2, 4, 8)])

    def pair_copy(i):
        return pltpu.make_async_remote_copy(
            src_ref=part.at[i, 1 - core], dst_ref=pair_in.at[i], send_sem=pair_send.at[i], recv_sem=pair_recv.at[i],
            device_id=(partner,), device_id_type=pl.DeviceIdType.MESH)

    def link_copy(colour, mask):
        axis = RS_ORDERS[colour][first_axis(colour, mask)]
        slot = rs_slots(colour)[mask - axis, axis]
        lo, n = cols[colour]
        return pltpu.make_async_remote_copy(
            src_ref=part.at[RS_MASKS.index(mask), core, :, pl.ds(lo, n)], dst_ref=link_in.at[slot, :, pl.ds(lo, n)],
            send_sem=link_send.at[colour, RS_MASKS.index(mask)], recv_sem=link_recv.at[colour, slot],
            device_id=(flipped(me, axis),), device_id_type=pl.DeviceIdType.MESH)

    rows = 16

    def add(i, colour, slot):
        lo, n = cols[colour]

        def step(r, c):
            rs = pl.ds(pl.multiple_of(r * rows, rows), rows)
            part[i, core, rs, pl.ds(lo, n)] += link_in[slot, rs, pl.ds(lo, n)]
            return c
        lax.fori_loop(0, tokens // rows, step, 0)

    width = 512

    def compute(i):
        start = pl.multiple_of((flipped(me, RS_MASKS[i]) // 2) * (2 * tokens), 2 * tokens)
        a = a_ref[:, pl.ds(start, 2 * tokens)]

        def step(n, c):
            cs = pl.ds(pl.multiple_of(n * width, width), width)
            r = mm(a, w_ref[:, cs], TN)
            part[i, 0, :, cs] = r[:tokens]
            part[i, 1, :, cs] = r[tokens:]
            return c
        lax.fori_loop(0, dim // width, step, 0)
        pair_copy(i).start()

    ready = set()
    sent = [0, 0, 0]

    def finish_pair(i):
        pair_copy(i).wait_recv()

        def step(r, c):
            rs = pl.ds(pl.multiple_of(r * rows, rows), rows)
            part[i, core, rs, :] += pair_in[i, rs, :]
            return c
        lax.fori_loop(0, tokens // rows, step, 0)
        ready.add(RS_MASKS[i])
        for colour in range(3):
            todo = RS_FIRST[colour]
            while sent[colour] < 4 and todo[sent[colour]] in ready:
                link_copy(colour, todo[sent[colour]]).start()
                sent[colour] += 1

    for i in range(8):
        compute(i)
        if i:
            finish_pair(i - 1)
    finish_pair(7)

    def take(colour, mask, axis):
        link_copy(colour, mask + axis).wait_recv()
        add(RS_MASKS.index(mask), colour, rs_slots(colour)[mask, axis])

    for step in range(2):
        for colour in range(3):
            o = RS_ORDERS[colour]
            mask = (o[1] + o[2], o[1])[step]
            take(colour, mask, o[0])
            link_copy(colour, mask).start()
    for colour in range(3):
        o = RS_ORDERS[colour]
        take(colour, o[2], o[0])
        take(colour, o[2], o[1])
        link_copy(colour, o[2]).start()
    for colour in range(3):
        o = RS_ORDERS[colour]
        for axis in o:
            take(colour, 0, axis)
    out_ref[...] = (base_ref[...].astype(F32) + part[7, core]).astype(out_ref.dtype)
    for i in range(8):
        pair_copy(i).wait_send()
    for colour in range(3):
        for mask in RS_MASKS[:7]:
            link_copy(colour, mask).wait_send()


def product_scatter(a, w, base, ident):
    feat, seq = a.shape
    tokens, dim = base.shape
    unit = 128
    n = dim // unit
    wide = (n + 2) // 3
    cols = ((0, wide * unit), (wide * unit, (n - wide) // 2 * unit), ((wide + (n - wide) // 2) * unit, (n - wide - (n - wide) // 2) * unit))
    return pl.pallas_call(
        functools.partial(rs_kernel, cols),
        out_shape=jax.ShapeDtypeStruct((tokens, dim), BF16),
        in_specs=in_vmem(3), out_specs=in_vmem(1)[0],
        scratch_shapes=[
            pltpu.VMEM((8, 2, tokens, dim), F32), pltpu.VMEM((8, tokens, dim), F32), pltpu.VMEM((7, tokens, dim), F32),
            pltpu.SemaphoreType.DMA((8,)), pltpu.SemaphoreType.DMA((8,)), pltpu.SemaphoreType.DMA((3, 8)), pltpu.SemaphoreType.DMA((3, 7))],
        cost_estimate=pl.CostEstimate(flops=2 * seq * feat * dim, bytes_accessed=2 * (a.size + w.size), transcendentals=0),
        compiler_params=pltpu.CompilerParams(collective_id=ident, has_side_effects=True, vmem_limit_bytes=VMEM_CAP),
        name=f'product_scatter_{ident}',
    )(a, w, base)


def solution(mesh):
    n_dev = mesh.shape['sp']
    gather = functools.partial(lax.all_gather, axis_name='sp', axis=0, tiled=True)
    swap = functools.partial(lax.all_to_all, axis_name='sp', split_axis=0, concat_axis=0, tiled=True)

    def layer_step(x_in, positions, d_out, norm1_gain, norm2_gain, w_q, w_k, w_v, w_o, w_gate, w_up, w_down):
        tokens, dim = x_in.shape
        seq_len = tokens * n_dev
        n_q, hd = w_q.shape[1], w_q.shape[2]
        n_kv = w_k.shape[1]
        hpd = n_q // n_dev
        qw, kw = hpd * hd, hd
        rows = w_q.shape[0]
        feat = w_down.shape[0]
        me = lax.axis_index('sp')

        small = jnp.stack([norm1_gain.astype(F32), norm2_gain.astype(F32), positions.astype(F32)])
        small_all = gather(small[None])
        g1 = small_all[:, 0].reshape(-1)
        g2 = small_all[:, 1].reshape(-1)
        pos_all = small_all[:, 2].reshape(-1)
        cos_tab, sin_tab = rope_tables(positions, hd)
        cos_all, sin_all = rope_tables(pos_all, hd)

        wqkv = gather(jnp.concatenate([w_q.reshape(rows, n_q * hd), w_k.reshape(rows, n_kv * hd), w_v.reshape(rows, n_kv * hd)], axis=1))
        wo_own = w_o.reshape(qw, dim)
        wo_full = gather(wo_own)

        def by_feature(w):
            return w.T.reshape(n_dev, feat, rows)
        wgu = swap(jnp.concatenate([by_feature(w_gate), by_feature(w_up)], axis=1))
        wgu = wgu.transpose(1, 0, 2).reshape(2 * feat, dim)

        x_f32 = x_in.astype(F32)
        normed_pre, norm1_pull = jax.vjp(norm_forward, x_f32, g1)
        normed = normed_pre.astype(BF16)
        qkv = jnp.dot(normed, wqkv, preferred_element_type=F32).astype(BF16)
        q_rot = rotate(qkv[:, :n_q * hd].reshape(tokens, n_q, hd), cos_tab, sin_tab).astype(BF16)
        k_rot = rotate(qkv[:, n_q * hd:(n_q + n_kv) * hd].reshape(tokens, n_kv, hd), cos_tab, sin_tab).astype(BF16)
        v_lin = qkv[:, (n_q + n_kv) * hd:].reshape(tokens, n_kv, hd)
        rep = n_dev // n_kv
        send = jnp.concatenate([
            q_rot.reshape(tokens, n_dev, qw).transpose(1, 0, 2),
            jnp.repeat(k_rot.transpose(1, 0, 2), rep, axis=0),
            jnp.repeat(v_lin.transpose(1, 0, 2), rep, axis=0)], axis=2)
        seq = swap(send).reshape(seq_len, qw + 2 * kw)
        q_seq = seq[:, :qw].reshape(seq_len, hpd, hd).transpose(1, 0, 2)
        k_seq = seq[:, qw:qw + kw]
        v_seq = seq[:, qw + kw:]
        attn_t, stat = attention_forward(q_seq, k_seq, v_seq)
        attn_tok = swap(attn_t.reshape(qw, n_dev, tokens).transpose(1, 2, 0)).transpose(1, 0, 2).reshape(tokens, n_q * hd)
        attn_proj = jnp.dot(attn_tok, wo_full, preferred_element_type=F32)
        hidden = (x_f32 + attn_proj).astype(BF16)
        hidden_f32 = hidden.astype(F32)
        mlp_pre, norm2_pull = jax.vjp(norm_forward, hidden_f32, g2)
        mlp_in = mlp_pre.astype(BF16)

        m_full = gather(mlp_in)
        do_full = gather(d_out)
        u_full = gather(normed)
        gu = jnp.einsum('fd,td->ft', wgu, m_full, preferred_element_type=F32).astype(BF16)
        gate_act, up_act = gu[:feat], gu[feat:]
        glu_pre, glu_pull = jax.vjp(gated_unit, gate_act.astype(F32), up_act.astype(F32))
        glu = glu_pre.astype(BF16)
        y_out = product_scatter(glu, w_down, hidden, 0)

        d_down = jnp.einsum('ft,td->fd', glu, do_full, preferred_element_type=F32)
        d_glu = jnp.einsum('fd,td->ft', w_down, do_full, preferred_element_type=F32).astype(BF16)
        d_gate_f, d_up_f = glu_pull(d_glu.astype(F32))
        dgu = jnp.concatenate([d_gate_f.astype(BF16), d_up_f.astype(BF16)], axis=0)
        d_mlp_in = product_scatter(dgu, wgu, jnp.zeros_like(hidden), 1)
        d_hidden_norm, d_g2 = norm2_pull(d_mlp_in.astype(F32))
        d_hidden = (d_out.astype(F32) + d_hidden_norm).astype(BF16)
        dh_full = gather(d_hidden)

        dwgu = jnp.einsum('ft,td->fd', dgu, m_full, preferred_element_type=F32)
        dwgu = swap(dwgu.reshape(2 * feat, n_dev, rows).transpose(1, 0, 2))
        d_gate = dwgu[:, :feat].reshape(n_dev * feat, rows).T
        d_up = dwgu[:, feat:].reshape(n_dev * feat, rows).T

        d_wo = jnp.einsum('et,td->ed', attn_t, dh_full, preferred_element_type=F32).reshape(w_o.shape)
        d_attn = jnp.einsum('td,ed->te', dh_full, wo_own, preferred_element_type=F32).astype(BF16)
        d_q_t, d_k_seq, d_v_seq = attention_backward(q_seq, k_seq, v_seq, d_attn.reshape(seq_len, hpd, hd).transpose(1, 0, 2), stat)
        d_q_seq = d_q_t.reshape(hpd, hd, seq_len).transpose(2, 0, 1)
        dq_lin_seq = rotate(d_q_seq, cos_all, -sin_all).astype(BF16).reshape(seq_len, qw)
        back = swap(jnp.concatenate([dq_lin_seq, d_k_seq, d_v_seq], axis=1).reshape(n_dev, tokens, qw + 2 * kw))
        d_q_lin = back[:, :, :qw].transpose(1, 0, 2).reshape(tokens, n_q * hd)
        shares = back[:, :, qw:].reshape(n_kv, rep, tokens, 2, hd)
        dkv = jnp.sum(shares, axis=1, dtype=F32).astype(BF16)
        d_k_lin = rotate(dkv[:, :, 0].transpose(1, 0, 2), cos_tab, -sin_tab).astype(BF16).reshape(tokens, n_kv * hd)
        d_v_lin = dkv[:, :, 1].transpose(1, 0, 2).reshape(tokens, n_kv * hd)
        dkv_lin = jnp.concatenate([d_k_lin, d_v_lin], axis=1)
        dkv_full = gather(dkv_lin)
        u_own = lax.dynamic_slice_in_dim(u_full, me * rows, rows, axis=1)
        d_wkv = jnp.einsum('td,te->de', u_own, dkv_full, preferred_element_type=F32)
        d_wk = d_wkv[:, :n_kv * hd].reshape(w_k.shape)
        d_wv = d_wkv[:, n_kv * hd:].reshape(w_v.shape)
        dwq = jnp.einsum('td,te->de', u_full, dq_lin_seq, preferred_element_type=F32)
        d_normed = lax.dot_general(jnp.concatenate([d_q_lin, dkv_lin], axis=1), wqkv, (((1,), (1,)), ((), ())), preferred_element_type=F32).astype(BF16)
        d_x_norm, d_g1 = norm1_pull(d_normed.astype(F32))
        d_x = (d_hidden.astype(F32) + d_x_norm).astype(BF16)
        gains = jnp.stack([d_g1.reshape(n_dev, rows), d_g2.reshape(n_dev, rows)], axis=1)
        tail = swap(jnp.concatenate([dwq.reshape(n_dev, rows, qw), jnp.pad(gains, ((0, 0), (0, 6), (0, qw - rows)))], axis=1))
        d_wq = tail[:, :rows].transpose(1, 0, 2).reshape(w_q.shape)
        gsum = jnp.sum(tail[:, rows:, :rows], axis=0)
        return (y_out, d_x, gsum[0], gsum[1], d_wq, d_wk, d_wv, d_wo, d_gate, d_up, d_down)

    all_rows = P('sp')
    return jax.shard_map(layer_step, mesh=mesh, in_specs=(all_rows,) * 12, out_specs=(all_rows,) * 11, check_vma=False)
```

```python
import functools
import jax
import jax.numpy as jnp
from jax import lax
from jax.experimental import pallas as pl
from jax.experimental.pallas import tpu as pltpu
from jax.sharding import PartitionSpec as P

ROPE_BASE = 10000.0
NORM_EPS = 1e-5
NEG_LARGE = -1e30
F32 = jnp.float32
BF16 = jnp.bfloat16
N_DEV, N_CHIP, LANE, WIDE, CHUNK = 16, 8, 128, 256, 512


def norm_forward(hidden, gain_vec):
    inv_rms = lax.rsqrt(jnp.mean(hidden * hidden, axis=-1, keepdims=True) + NORM_EPS)
    return hidden * inv_rms * gain_vec


def rope_tables(positions, head_dim):
    half_dim = head_dim // 2
    inv_freq = 1.0 / (ROPE_BASE ** (jnp.arange(half_dim, dtype=F32) * (2.0 / head_dim)))
    angles = positions.astype(F32)[:, None] * inv_freq[None, :]
    return jnp.cos(angles)[:, None, :], jnp.sin(angles)[:, None, :]


def gated_unit(gate_pre, up_pre):
    return jax.nn.silu(gate_pre) * up_pre


NT = (((1,), (1,)), ((), ()))
TN = (((0,), (0,)), ((), ()))
NN = (((1,), (0,)), ((), ()))


def mm(a, b, dims):
    return lax.dot_general(a, b, dims, preferred_element_type=F32)


VMEM_CAP = 60 * 1024 * 1024


def in_vmem(n):
    return [pl.BlockSpec(memory_space=pltpu.VMEM)] * n


def comm_params(ident):
    return pltpu.CompilerParams(collective_id=ident, has_side_effects=True, vmem_limit_bytes=VMEM_CAP)


RS_ORDERS = ((2, 4, 8), (4, 8, 2), (8, 2, 4))
RS_MASKS = (14, 6, 12, 10, 2, 4, 8, 0)
RS_FIRST = ((14, 6, 10, 2), (14, 12, 6, 4), (14, 10, 12, 8))


def first_axis(colour, mask):
    return next(i for i, a in enumerate(RS_ORDERS[colour]) if mask & a)


def rs_slots(colour):
    slots = {}
    for mask in RS_MASKS:
        for axis in RS_ORDERS[colour][:first_axis(colour, mask) if mask else 3]:
            slots[mask, axis] = len(slots)
    return slots


def flipped(index, mask):
    out = index
    for bit in (1, 2, 4, N_CHIP):
        if mask & bit:
            out = out + (1 - 2 * ((index // bit) % 2)) * bit
    return out


def enter(peers):
    barrier = pltpu.get_barrier_semaphore()
    for peer in peers:
        pl.semaphore_signal(barrier, inc=1, device_id=(peer,), device_id_type=pl.DeviceIdType.MESH)
    pl.semaphore_wait(barrier, len(peers))


def rs_kernel(cols, a_ref, w_ref, base_ref, out_ref, part, pair_in, link_in, pair_send, pair_recv, link_send, link_recv):
    tokens, dim = out_ref.shape
    me = lax.axis_index('sp')
    core = me % 2
    partner = flipped(me, 1)
    enter([partner] + [flipped(me, a) for a in (2, 4, N_CHIP)])

    def pair_copy(i):
        return pltpu.make_async_remote_copy(
            src_ref=part.at[i, 1 - core], dst_ref=pair_in.at[i], send_sem=pair_send.at[i], recv_sem=pair_recv.at[i],
            device_id=(partner,), device_id_type=pl.DeviceIdType.MESH)

    def link_copy(colour, mask):
        axis = RS_ORDERS[colour][first_axis(colour, mask)]
        slot = rs_slots(colour)[mask - axis, axis]
        lo, n = cols[colour]
        return pltpu.make_async_remote_copy(
            src_ref=part.at[RS_MASKS.index(mask), core, :, pl.ds(lo, n)], dst_ref=link_in.at[slot, :, pl.ds(lo, n)],
            send_sem=link_send.at[colour, RS_MASKS.index(mask)], recv_sem=link_recv.at[colour, slot],
            device_id=(flipped(me, axis),), device_id_type=pl.DeviceIdType.MESH)

    rows = N_DEV

    def add(i, colour, slot):
        lo, n = cols[colour]

        def step(r, c):
            rs = pl.ds(pl.multiple_of(r * rows, rows), rows)
            part[i, core, rs, pl.ds(lo, n)] += link_in[slot, rs, pl.ds(lo, n)]
            return c
        lax.fori_loop(0, tokens // rows, step, 0)

    width = CHUNK

    def compute(i):
        start = pl.multiple_of((flipped(me, RS_MASKS[i]) // 2) * (2 * tokens), 2 * tokens)
        a = a_ref[:, pl.ds(start, 2 * tokens)]

        def step(n, c):
            cs = pl.ds(pl.multiple_of(n * width, width), width)
            r = mm(a, w_ref[:, cs], TN)
            part[i, 0, :, cs] = r[:tokens]
            part[i, 1, :, cs] = r[tokens:]
            return c
        lax.fori_loop(0, dim // width, step, 0)
        pair_copy(i).start()

    ready = set()
    sent = [0, 0, 0]

    def finish_pair(i):
        pair_copy(i).wait_recv()

        def step(r, c):
            rs = pl.ds(pl.multiple_of(r * rows, rows), rows)
            part[i, core, rs, :] += pair_in[i, rs, :]
            return c
        lax.fori_loop(0, tokens // rows, step, 0)
        ready.add(RS_MASKS[i])
        for colour in range(3):
            todo = RS_FIRST[colour]
            while sent[colour] < 4 and todo[sent[colour]] in ready:
                link_copy(colour, todo[sent[colour]]).start()
                sent[colour] += 1

    for i in range(N_CHIP):
        compute(i)
        if i:
            finish_pair(i - 1)
    finish_pair(7)

    def take(colour, mask, axis):
        link_copy(colour, mask + axis).wait_recv()
        add(RS_MASKS.index(mask), colour, rs_slots(colour)[mask, axis])

    for step in range(2):
        for colour in range(3):
            o = RS_ORDERS[colour]
            mask = (o[1] + o[2], o[1])[step]
            take(colour, mask, o[0])
            link_copy(colour, mask).start()
    for colour in range(3):
        o = RS_ORDERS[colour]
        take(colour, o[2], o[0])
        take(colour, o[2], o[1])
        link_copy(colour, o[2]).start()
    for colour in range(3):
        o = RS_ORDERS[colour]
        for axis in o:
            take(colour, 0, axis)
    out_ref[...] = (base_ref[...].astype(F32) + part[7, core]).astype(out_ref.dtype)
    for i in range(N_CHIP):
        pair_copy(i).wait_send()
    for colour in range(3):
        for mask in RS_MASKS[:7]:
            link_copy(colour, mask).wait_send()


def product_scatter(a, w, base, ident):
    feat, seq = a.shape
    tokens, dim = base.shape
    cols = thirds(dim, LANE)
    return pl.pallas_call(
        functools.partial(rs_kernel, cols),
        out_shape=jax.ShapeDtypeStruct((tokens, dim), BF16),
        in_specs=in_vmem(3), out_specs=in_vmem(1)[0],
        scratch_shapes=[
            pltpu.VMEM((N_CHIP, 2, tokens, dim), F32), pltpu.VMEM((N_CHIP, tokens, dim), F32), pltpu.VMEM((7, tokens, dim), F32),
            pltpu.SemaphoreType.DMA((N_CHIP,)), pltpu.SemaphoreType.DMA((N_CHIP,)), pltpu.SemaphoreType.DMA((3, N_CHIP)), pltpu.SemaphoreType.DMA((3, 7))],
        cost_estimate=pl.CostEstimate(flops=2 * seq * feat * dim, bytes_accessed=2 * (a.size + w.size), transcendentals=0),
        compiler_params=comm_params(ident),
        name=f'product_scatter_{ident}',
    )(a, w, base)


GATHER_ROUNDS = ((0,), (1,), (2,), (0, 1), (0, 2), (1, 2), (0, 1, 2))
TURNS = ((0,), (), (), (2,), (4,), (8,), (6, 10, 12, 14))


class Gather:
    def __init__(self, own, block, cut, sems, me):
        self.own, self.block, self.cut, self.me = own, block, cut, me
        self.send, self.recv, self.pair_send, self.pair_recv = sems

    def source(self, mask):
        return self.own if mask == 0 else self.block(flipped(self.me, mask))

    def unit(self, colour, mask, axis):
        return pltpu.make_async_remote_copy(
            src_ref=self.cut(self.source(mask), colour), dst_ref=self.cut(self.block(flipped(self.me, mask)), colour),
            send_sem=self.send.at[colour, mask // 2, RS_ORDERS[colour].index(axis)], recv_sem=self.recv.at[colour, (mask + axis) // 2],
            device_id=(flipped(self.me, axis),), device_id_type=MESH)

    def arrival(self, colour, mask):
        view = self.cut(self.block(flipped(self.me, mask)), colour)
        return pltpu.make_async_remote_copy(
            src_ref=view, dst_ref=view, send_sem=self.send.at[colour, 0, 0], recv_sem=self.recv.at[colour, mask // 2],
            device_id=(self.me,), device_id_type=MESH)

    def pair(self, mask):
        return pltpu.make_async_remote_copy(
            src_ref=self.source(mask), dst_ref=self.block(flipped(self.me, mask)),
            send_sem=self.pair_send.at[mask // 2], recv_sem=self.pair_recv.at[mask // 2],
            device_id=(flipped(self.me, 1),), device_id_type=MESH)

    def wait_pair(self, mask):
        view = self.block(flipped(self.me, mask + 1))
        pltpu.make_async_remote_copy(
            src_ref=view, dst_ref=view, send_sem=self.pair_send.at[mask // 2], recv_sem=self.pair_recv.at[mask // 2],
            device_id=(self.me,), device_id_type=MESH).wait_recv()

    def start(self):
        for pos in range(3):
            for colour in range(3):
                self.unit(colour, 0, RS_ORDERS[colour][pos]).start()
        self.pair(0).start()

    def round(self, r):
        for colour in range(3):
            order = RS_ORDERS[colour]
            mask = sum(order[p] for p in GATHER_ROUNDS[r])
            self.arrival(colour, mask).wait_recv()
            for axis in order[GATHER_ROUNDS[r][-1] + 1:]:
                self.unit(colour, mask, axis).start()
        for mask in {2: (2, 4, N_CHIP), 5: (6, 10, 12), 6: (14,)}.get(r, ()):
            self.pair(mask).start()

    def finish(self):
        for colour in range(3):
            order = RS_ORDERS[colour]
            for pos in range(3):
                self.unit(colour, 0, order[pos]).wait_send()
            for picks in GATHER_ROUNDS:
                for axis in order[picks[-1] + 1:]:
                    self.unit(colour, sum(order[p] for p in picks), axis).wait_send()
        for mask in CHIP_MASKS:
            self.pair(mask).wait_send()


CHIP_MASKS = (0, 2, 4, 8, 6, 10, 12, 14)
MESH = pl.DeviceIdType.MESH


def gather_sems():
    return [pltpu.SemaphoreType.DMA((3, N_CHIP, 3)), pltpu.SemaphoreType.DMA((3, N_CHIP)), pltpu.SemaphoreType.DMA((N_CHIP,)), pltpu.SemaphoreType.DMA((N_CHIP,))]


def thirds(total, unit):
    n = total // unit
    first = (n + 2) // 3
    second = (n - first + 1) // 2
    sizes = (first * unit, second * unit, (n - first - second) * unit)
    return ((0, sizes[0]), (sizes[0], sizes[1]), (sizes[0] + sizes[1], sizes[2]))


def lane_block(index, width=LANE):
    return pl.ds(pl.multiple_of(index * width, width), width)


class Swap:
    def __init__(self, src, dst, send, recv, me):
        self.src, self.dst, self.send, self.recv, self.me = src, dst, send, recv, me

    def copy(self, mask):
        peer = flipped(self.me, mask)
        return pltpu.make_async_remote_copy(
            src_ref=self.src(peer), dst_ref=self.dst(self.me), send_sem=self.send.at[mask], recv_sem=self.recv.at[mask],
            device_id=(peer,), device_id_type=MESH)

    def start(self):
        for mask in range(1, N_DEV):
            self.copy(mask).start()

    def wait_recv(self):
        for mask in range(1, N_DEV):
            view = self.dst(flipped(self.me, mask))
            pltpu.make_async_remote_copy(
                src_ref=view, dst_ref=view, send_sem=self.send.at[mask], recv_sem=self.recv.at[mask],
                device_id=(self.me,), device_id_type=MESH).wait_recv()

    def wait_send(self):
        for mask in range(1, N_DEV):
            self.copy(mask).wait_send()


def swap_sems():
    return [pltpu.SemaphoreType.DMA((N_DEV,)), pltpu.SemaphoreType.DMA((N_DEV,))]


def qkv_kernel(groups, hd, x_ref, small_ref, w_ref, cos_ref, sin_ref, qkv_ref, ucol_ref, small_all, w_out,
               full, acc, rot, u_scr, g_scr, *sems):
    me = lax.axis_index('sp')
    tokens, dim = x_ref.shape
    cols = w_ref.shape[0]
    n_dev = N_DEV
    qw = tokens
    q_all = n_dev * qw
    gsems, osem, rest = sems[:4], sems[4], sems[5:]
    enter([flipped(me, m) for m in range(1, N_DEV)])
    smalls = Swap(lambda peer: small_ref, lambda o: small_all.at[o], rest[0], rest[1], me)
    smalls.start()
    parts = thirds(cols, N_DEV)

    def block(o):
        return full.at[o // 2, :, lane_block(o % 2)]

    g = Gather(w_ref, block, lambda view, c: view.at[pl.ds(parts[c][0], parts[c][1]), :], gsems, me)
    g.start()

    def own_block(i, c):
        rs = pl.ds(pl.multiple_of(i * WIDE, WIDE), WIDE)
        full[me // 2, rs, lane_block(me % 2)] = w_ref[rs, :]
        return c
    lax.fori_loop(0, cols // WIDE, own_block, 0)
    acc[...] = jnp.zeros_like(acc)
    small_all[me] = small_ref[...]
    smalls.wait_recv()
    for o in range(n_dev):
        g_scr[0:1, o * LANE:(o + 1) * LANE] = small_all[o, 0:1, :]

    def norm(i, c):
        rs = pl.ds(pl.multiple_of(i * N_DEV, N_DEV), N_DEV)
        xf = x_ref[rs, :].astype(F32)
        inv = lax.rsqrt(jnp.mean(xf * xf, axis=-1, keepdims=True) + NORM_EPS)
        u_scr[rs, :] = (xf * inv * g_scr[0:1, :]).astype(BF16)
        return c
    lax.fori_loop(0, tokens // N_DEV, norm, 0)
    ucols = Swap(lambda peer: u_scr.at[:, lane_block(peer)], lambda o: ucol_ref.at[pl.ds(pl.multiple_of(o * tokens, tokens), tokens), :], rest[2], rest[3], me)

    def use(mask):
        g.wait_pair(mask)
        chip = flipped(me, mask) // 2
        pltpu.make_async_copy(full.at[chip], w_out.at[chip], osem.at[mask // 2]).start()
        u = u_scr[:, lane_block(chip, WIDE)]

        def step(i, c):
            rs = pl.ds(pl.multiple_of(i * CHUNK, CHUNK), CHUNK)
            acc[rs, :] += mm(full[chip, rs, :], u, NT)
            return c
        lax.fori_loop(0, cols // CHUNK, step, 0)

    for r in range(7):
        g.round(r)
        if r == 0:
            ucols.start()
        for mask in TURNS[r]:
            use(mask)

    half = hd // 2
    cos, sin = cos_ref[...], sin_ref[...]

    def turn(h, c):
        first = pl.ds(pl.multiple_of(h * hd, hd), half)
        second = pl.ds(pl.multiple_of(h * hd + half, half), half)
        p = acc[first, :].astype(BF16).astype(F32)
        q = acc[second, :].astype(BF16).astype(F32)
        rot[first, :] = (p * cos - q * sin).astype(BF16)
        rot[second, :] = (q * cos + p * sin).astype(BF16)
        return c
    lax.fori_loop(0, q_all // hd, turn, 0)
    for k in range(groups):
        turn(q_all // hd + 2 * k, 0)
        vs = pl.ds(q_all + (2 * k + 1) * hd, hd)
        rot[vs, :] = acc[vs, :].astype(BF16)
    per = n_dev // groups
    tok = lambda o: lane_block(o, tokens)
    qs = Swap(lambda peer: rot.at[pl.ds(pl.multiple_of(peer * qw, qw), qw), :], lambda o: qkv_ref.at[pl.ds(0, qw), tok(o)], rest[4], rest[5], me)
    kvs = Swap(lambda peer: rot.at[pl.ds(pl.multiple_of(q_all + (peer // per) * 2 * hd, 2 * hd), 2 * hd), :], lambda o: qkv_ref.at[pl.ds(qw, 2 * hd), tok(o)], rest[6], rest[7], me)
    qs.start()
    kvs.start()
    qkv_ref[0:qw, tok(me)] = rot[pl.ds(pl.multiple_of(me * qw, qw), qw), :]
    qkv_ref[qw:qw + 2 * hd, tok(me)] = rot[pl.ds(pl.multiple_of(q_all + (me // per) * 2 * hd, 2 * hd), 2 * hd), :]
    ucol_ref[pl.ds(pl.multiple_of(me * tokens, tokens), tokens), :] = u_scr[:, lane_block(me)]
    for swap in (ucols, qs, kvs):
        swap.wait_recv()
    for mask in CHIP_MASKS:
        chip = flipped(me, mask) // 2
        pltpu.make_async_copy(full.at[chip], w_out.at[chip], osem.at[mask // 2]).wait()
    g.finish()
    for swap in (smalls, ucols, qs, kvs):
        swap.wait_send()


def project_qkv(x, small, w, cos, sin, groups, hd):
    tokens, dim = x.shape
    cols = w.shape[0]
    seq = N_DEV * tokens
    return pl.pallas_call(
        functools.partial(qkv_kernel, groups, hd),
        out_shape=(jax.ShapeDtypeStruct((tokens + 2 * hd, seq), BF16), jax.ShapeDtypeStruct((seq, LANE), BF16),
                   jax.ShapeDtypeStruct((N_DEV,) + small.shape, F32), jax.ShapeDtypeStruct((N_CHIP, cols, WIDE), BF16)),
        in_specs=in_vmem(5), out_specs=tuple(in_vmem(3)) + (pl.BlockSpec(memory_space=pl.ANY),),
        scratch_shapes=[pltpu.VMEM((N_CHIP, cols, WIDE), BF16), pltpu.VMEM((cols, tokens), F32), pltpu.VMEM((cols, tokens), BF16),
                        pltpu.VMEM((tokens, dim), BF16), pltpu.VMEM((N_CHIP, dim), F32)]
        + gather_sems() + [pltpu.SemaphoreType.DMA((N_CHIP,))] + 4 * swap_sems(),
        cost_estimate=pl.CostEstimate(flops=2 * tokens * dim * cols, bytes_accessed=4 * N_DEV * w.size, transcendentals=0),
        compiler_params=comm_params(2),
        name='project_qkv',
    )(x, small, w, cos, sin)


def token_gather(full, own_ref, gsems, me):
    tokens = own_ref.shape[0]
    parts = thirds(own_ref.shape[1], LANE)

    def block(o):
        return full.at[o // 2, pl.ds(pl.multiple_of((o % 2) * tokens, tokens), tokens), :]

    g = Gather(own_ref, block, lambda view, c: view.at[:, pl.ds(parts[c][0], parts[c][1])], gsems, me)
    enter([flipped(me, m) for m in (1, 2, 4, N_CHIP)])
    g.start()
    for i in range(0, tokens, 32):
        full[me // 2, pl.ds(pl.multiple_of((me % 2) * tokens + i, 32), 32), :] = own_ref[i:i + 32, :]
    return g


def gate_up_kernel(m_ref, w_ref, gu_ref, m_out, full, *sems):
    me = lax.axis_index('sp')
    gsems, osem = sems[:4], sems[4]
    g = token_gather(full, m_ref, gsems, me)

    def use(mask):
        g.wait_pair(mask)
        chip = flipped(me, mask) // 2
        pltpu.make_async_copy(full.at[chip], m_out.at[chip], osem.at[mask // 2]).start()
        gu_ref[:, lane_block(chip, WIDE)] = mm(w_ref[...], full[chip], NT).astype(BF16)

    for r in range(7):
        g.round(r)
        for mask in TURNS[r]:
            use(mask)
    for mask in CHIP_MASKS:
        chip = flipped(me, mask) // 2
        pltpu.make_async_copy(full.at[chip], m_out.at[chip], osem.at[mask // 2]).wait()
    g.finish()


def gather_gate_up(m, w):
    tokens, dim = m.shape
    feat = w.shape[0]
    return pl.pallas_call(
        gate_up_kernel,
        out_shape=(jax.ShapeDtypeStruct((feat, N_DEV * tokens), BF16), jax.ShapeDtypeStruct((N_CHIP, 2 * tokens, dim), BF16)),
        in_specs=in_vmem(2), out_specs=(in_vmem(1)[0], pl.BlockSpec(memory_space=pl.ANY)),
        scratch_shapes=[pltpu.VMEM((N_CHIP, 2 * tokens, dim), BF16)] + gather_sems() + [pltpu.SemaphoreType.DMA((N_CHIP,))],
        cost_estimate=pl.CostEstimate(flops=2 * feat * N_DEV * tokens * dim, bytes_accessed=4 * N_DEV * m.size, transcendentals=0),
        compiler_params=comm_params(3),
        name='gather_gate_up',
    )(m, w)


def d_attn_kernel(dh_ref, wo_ref, o_ref, do_ref, dwo_ref, full, *sems):
    me = lax.axis_index('sp')
    g = token_gather(full, dh_ref, sems, me)
    dwo_ref[...] = jnp.zeros_like(dwo_ref)
    dim = wo_ref.shape[1]

    def use(mask):
        g.wait_pair(mask)
        chip = flipped(me, mask) // 2
        do_ref[:, lane_block(chip, WIDE)] = mm(wo_ref[...], full[chip], NT).astype(BF16)
        o = o_ref[:, lane_block(chip, WIDE)]

        def step(n, c):
            cs = lane_block(n, CHUNK)
            dwo_ref[:, cs] += mm(o, full[chip, :, cs], NN)
            return c
        lax.fori_loop(0, dim // CHUNK, step, 0)

    for r in range(7):
        g.round(r)
        for mask in TURNS[r]:
            use(mask)
    g.finish()


def gather_d_attn(dh, wo, o):
    tokens, dim = dh.shape
    return pl.pallas_call(
        d_attn_kernel,
        out_shape=(jax.ShapeDtypeStruct(o.shape, BF16), jax.ShapeDtypeStruct(wo.shape, F32)),
        in_specs=in_vmem(3), out_specs=tuple(in_vmem(2)),
        scratch_shapes=[pltpu.VMEM((N_CHIP, 2 * tokens, dim), BF16)] + gather_sems(),
        cost_estimate=pl.CostEstimate(flops=4 * wo.shape[0] * N_DEV * tokens * dim, bytes_accessed=4 * N_DEV * dh.size, transcendentals=0),
        compiler_params=comm_params(4),
        name='gather_d_attn',
    )(dh, wo, o)


QB = WIDE
KB = WIDE


def key_rows(dst, src, lo, hd):
    def step(i, c):
        ks = lane_block(i, KB)
        dst[ks, :] = src[lo:lo + hd, ks].T
        return c
    lax.fori_loop(0, src.shape[1] // KB, step, 0)


def score_block(k, q2, scale, diagonal):
    s = mm(k, q2, NN) * scale
    if diagonal:
        key = lax.broadcasted_iota(jnp.int32, s.shape, 0)
        qry = lax.broadcasted_iota(jnp.int32, s.shape, 1) % QB
        s = jnp.where(qry >= key, s, NEG_LARGE)
    return s


def attn_fwd_kernel(hd, qkv_ref, wg_ref, wu_ref, ot_ref, o_ref, stat_ref, w_ref, s_scr, k_scr, *sems):
    heads = qkv_ref.shape[0] // hd - 2
    seq = qkv_ref.shape[1]
    scale = hd ** -0.5
    lanes = heads * QB
    me = lax.axis_index('sp')
    qw = heads * hd
    feat = wg_ref.shape[0] // N_DEV
    enter([flipped(me, m) for m in range(1, N_DEV)])
    rows = lambda peer: pl.ds(pl.multiple_of(peer * feat, 32), feat)
    gates = Swap(lambda peer: wg_ref.at[rows(peer), :], lambda o: w_ref.at[pl.ds(0, feat), lane_block(o)], sems[0], sems[1], me)
    ups = Swap(lambda peer: wu_ref.at[rows(peer), :], lambda o: w_ref.at[pl.ds(feat, feat), lane_block(o)], sems[2], sems[3], me)
    osend, orecv = sems[4], sems[5]
    gates.start()
    ups.start()
    w_ref[0:feat, lane_block(me)] = wg_ref[rows(me), :]
    w_ref[feat:2 * feat, lane_block(me)] = wu_ref[rows(me), :]
    key_rows(k_scr, qkv_ref, qw, hd)
    own = pl.ds(pl.multiple_of(me * qw, qw), qw)

    def o_copy(peer, origin):
        return pltpu.make_async_remote_copy(
            src_ref=o_ref.at[:, lane_block(peer)], dst_ref=ot_ref.at[pl.ds(pl.multiple_of(origin * qw, qw), qw), :],
            send_sem=osend.at[peer], recv_sem=orecv.at[origin], device_id=(peer,), device_id_type=MESH)

    def q_block(qb, carry):
        qs = lane_block(qb, QB)
        q2 = jnp.concatenate([qkv_ref[h * hd:(h + 1) * hd, qs] for h in range(heads)], axis=1)

        def scores(kb, top, diagonal):
            ks = lane_block(kb, KB)
            s = score_block(k_scr[ks, :], q2, scale, diagonal)
            s_scr[ks, :] = s
            return jnp.maximum(top, jnp.max(s, axis=0, keepdims=True))

        top = lax.fori_loop(0, qb, lambda kb, t: scores(kb, t, False), jnp.full((1, lanes), NEG_LARGE, F32))
        top = scores(qb, top, True)

        def expo(kb, tot):
            ks = lane_block(kb, KB)
            e = jnp.exp(s_scr[ks, :] - top)
            s_scr[ks, :] = e
            return tot + jnp.sum(e, axis=0, keepdims=True)

        inv = 1.0 / lax.fori_loop(0, qb + 1, expo, jnp.zeros((1, lanes), F32))

        def weigh(kb, acc):
            ks = lane_block(kb, KB)
            p = (s_scr[ks, :] * inv).astype(BF16)
            return acc + mm(qkv_ref[qw + hd:qw + 2 * hd, ks], p, NN)

        acc = lax.fori_loop(0, qb + 1, weigh, jnp.zeros((hd, lanes), F32))
        for h in range(heads):
            o_ref[h * hd:(h + 1) * hd, qs] = acc[:, h * QB:(h + 1) * QB].astype(BF16)
        stat_ref[qb, 0:1, :] = top
        stat_ref[qb, 1:2, :] = inv
        for core in range(2):
            peer = 2 * qb + core

            @pl.when(peer != me)
            def _():
                o_copy(peer, me).start()
        return carry

    lax.fori_loop(0, seq // QB, q_block, 0)
    ot_ref[own, :] = o_ref[:, lane_block(me)]
    for mask in range(1, N_DEV):
        o_copy(me, flipped(me, mask)).wait_recv()
    gates.wait_recv()
    ups.wait_recv()
    for mask in range(1, N_DEV):
        o_copy(flipped(me, mask), me).wait_send()
    gates.wait_send()
    ups.wait_send()


def attention_forward(qkv, wg, wu, hd):
    rows, seq = qkv.shape
    qw = rows - 2 * hd
    lanes = qw // hd * QB
    feat = wg.shape[0] // N_DEV
    return pl.pallas_call(
        functools.partial(attn_fwd_kernel, hd),
        out_shape=(jax.ShapeDtypeStruct((N_DEV * qw, seq // N_DEV), BF16), jax.ShapeDtypeStruct((qw, seq), BF16),
                   jax.ShapeDtypeStruct((seq // QB, 2, lanes), F32), jax.ShapeDtypeStruct((2 * feat, N_DEV * wg.shape[1]), BF16)),
        in_specs=in_vmem(3), out_specs=tuple(in_vmem(4)),
        scratch_shapes=[pltpu.VMEM((seq, lanes), F32), pltpu.VMEM((seq, hd), BF16)] + 3 * swap_sems(),
        cost_estimate=pl.CostEstimate(flops=2 * 4 * qw * seq * seq, bytes_accessed=4 * wg.size, transcendentals=0),
        compiler_params=comm_params(5),
        name='attn_fwd',
    )(qkv, wg, wu)


def attn_bwd_kernel(hd, qkv_ref, do_ref, stat_ref, cos_ref, sin_ref, dq_ref, dk_ref, dv_ref, p_scr, dp_scr, k_scr, v_scr, dk_acc, dv_acc):
    heads = qkv_ref.shape[0] // hd - 2
    seq = qkv_ref.shape[1]
    scale = hd ** -0.5
    lanes = heads * QB
    qw = heads * hd
    half = hd // 2
    dk_acc[...] = jnp.zeros_like(dk_acc)
    dv_acc[...] = jnp.zeros_like(dv_acc)
    key_rows(k_scr, qkv_ref, qw, hd)
    key_rows(v_scr, qkv_ref, qw + hd, hd)

    def q_block(qb, carry):
        qs = lane_block(qb, QB)
        q2 = jnp.concatenate([qkv_ref[h * hd:(h + 1) * hd, qs] for h in range(heads)], axis=1)
        do2 = jnp.concatenate([do_ref[h * hd:(h + 1) * hd, qs] for h in range(heads)], axis=1)
        top = stat_ref[qb, 0:1, :]
        inv = stat_ref[qb, 1:2, :]

        def probs(kb, rd, diagonal):
            ks = lane_block(kb, KB)
            s = score_block(k_scr[ks, :], q2, scale, diagonal)
            p = jnp.exp(s - top) * inv
            dp = mm(v_scr[ks, :], do2, NN).astype(BF16)
            p_scr[ks, :] = p
            dp_scr[ks, :] = dp
            dv_acc[ks, :] += mm(p.astype(BF16), do2, NT)
            return rd + jnp.sum(dp.astype(F32) * p, axis=0, keepdims=True)

        rd = lax.fori_loop(0, qb, lambda kb, r: probs(kb, r, False), jnp.zeros((1, lanes), F32))
        rd = probs(qb, rd, True)

        def d_scores(kb, acc):
            ks = lane_block(kb, KB)
            ds = (p_scr[ks, :] * (dp_scr[ks, :].astype(F32) - rd) * scale).astype(BF16)
            dk_acc[ks, :] += mm(ds, q2, NT)
            return acc + mm(qkv_ref[qw:qw + hd, ks], ds, NN)

        acc = lax.fori_loop(0, qb + 1, d_scores, jnp.zeros((hd, lanes), F32))
        cos, sin = cos_ref[:, qs], sin_ref[:, qs]
        for h in range(heads):
            dq = acc[:, h * QB:(h + 1) * QB].astype(BF16).astype(F32)
            p, q = dq[:half], dq[half:]
            dq_ref[h * hd:h * hd + half, qs] = (p * cos + q * sin).astype(BF16)
            dq_ref[h * hd + half:(h + 1) * hd, qs] = (q * cos - p * sin).astype(BF16)
        return carry

    lax.fori_loop(0, seq // QB, q_block, 0)
    dk_ref[...] = dk_acc[...].astype(BF16)
    dv_ref[...] = dv_acc[...].astype(BF16)


def attention_backward(qkv, do, stat, cos, sin, hd):
    rows, seq = qkv.shape
    qw = rows - 2 * hd
    lanes = qw // hd * QB
    return pl.pallas_call(
        functools.partial(attn_bwd_kernel, hd),
        out_shape=(jax.ShapeDtypeStruct((qw, seq), BF16), jax.ShapeDtypeStruct((seq, hd), BF16), jax.ShapeDtypeStruct((seq, hd), BF16)),
        in_specs=in_vmem(5), out_specs=tuple(in_vmem(3)),
        scratch_shapes=[pltpu.VMEM((seq, lanes), F32), pltpu.VMEM((seq, lanes), BF16), pltpu.VMEM((seq, hd), BF16), pltpu.VMEM((seq, hd), BF16),
                        pltpu.VMEM((seq, hd), F32), pltpu.VMEM((seq, hd), F32)],
        cost_estimate=pl.CostEstimate(flops=2 * 10 * qw * seq * seq, bytes_accessed=4 * seq * hd * N_CHIP, transcendentals=0),
        compiler_params=pltpu.CompilerParams(vmem_limit_bytes=VMEM_CAP),
        name='attn_bwd',
    )(qkv, do, stat, cos, sin)


def solution(mesh):
    n_dev = mesh.shape['sp']
    gather = functools.partial(lax.all_gather, axis_name='sp', axis=0, tiled=True)
    swap = functools.partial(lax.all_to_all, axis_name='sp', split_axis=0, concat_axis=0, tiled=True)

    def layer_step(x_in, positions, d_out, norm1_gain, norm2_gain, w_q, w_k, w_v, w_o, w_gate, w_up, w_down):
        tokens, dim = x_in.shape
        seq_len = tokens * n_dev
        n_q, hd = w_q.shape[1], w_q.shape[2]
        n_kv = w_k.shape[1]
        qw = n_q // n_dev * hd
        rows = w_q.shape[0]
        feat = w_down.shape[0]
        me = lax.axis_index('sp')

        small = jnp.stack([norm1_gain.astype(F32), norm2_gain.astype(F32), positions.astype(F32)] + [jnp.zeros((rows,), F32)] * 5)
        cos_tab, sin_tab = rope_tables(positions, hd)
        wq_t = w_q.transpose(1, 2, 0).reshape(n_q * hd, rows)
        wkv_t = jnp.stack([w_k.transpose(1, 2, 0), w_v.transpose(1, 2, 0)], axis=1).reshape(2 * n_kv * hd, rows)
        wo_own = w_o.reshape(qw, dim)
        wo_full = gather(wo_own)
        do_full = gather(d_out)

        qkv, u_col, small_all, wqkv = project_qkv(x_in, small, jnp.concatenate([wq_t, wkv_t], axis=0), cos_tab[:, 0].T, sin_tab[:, 0].T, n_kv, hd)
        g1 = small_all[:, 0].reshape(-1)
        g2 = small_all[:, 1].reshape(-1)
        cos_all, sin_all = rope_tables(small_all[:, 2].reshape(-1), hd)

        attn_tok, attn_t, stat, wgu = attention_forward(qkv, w_gate.T, w_up.T, hd)
        x_f32 = x_in.astype(F32)
        attn_proj = jnp.einsum('et,ed->td', attn_tok, wo_full, preferred_element_type=F32)
        hidden = (x_f32 + attn_proj).astype(BF16)
        hidden_f32 = hidden.astype(F32)
        mlp_pre, norm2_pull = jax.vjp(norm_forward, hidden_f32, g2)
        mlp_in = mlp_pre.astype(BF16)

        gu, m_full = gather_gate_up(mlp_in, wgu)
        m_full = m_full.reshape(seq_len, dim)
        gate_act, up_act = gu[:feat], gu[feat:]
        glu_pre, glu_pull = jax.vjp(gated_unit, gate_act.astype(F32), up_act.astype(F32))
        glu = glu_pre.astype(BF16)
        y_out = product_scatter(glu, w_down, hidden, 0)

        d_down = jnp.einsum('ft,td->fd', glu, do_full, preferred_element_type=F32)
        d_glu = jnp.einsum('fd,td->ft', w_down, do_full, preferred_element_type=F32).astype(BF16)
        d_gate_f, d_up_f = glu_pull(d_glu.astype(F32))
        dgu = jnp.concatenate([d_gate_f.astype(BF16), d_up_f.astype(BF16)], axis=0)
        d_mlp_in = product_scatter(dgu, wgu, jnp.zeros_like(hidden), 1)
        d_hidden_norm, d_g2 = norm2_pull(d_mlp_in.astype(F32))
        d_hidden = (d_out.astype(F32) + d_hidden_norm).astype(BF16)

        dwgu = jnp.einsum('ft,td->fd', dgu, m_full, preferred_element_type=F32)
        dwgu = swap(dwgu.reshape(2 * feat, n_dev, rows).transpose(1, 0, 2))
        d_gate = dwgu[:, :feat].reshape(n_dev * feat, rows).T
        d_up = dwgu[:, feat:].reshape(n_dev * feat, rows).T

        d_attn, d_wo = gather_d_attn(d_hidden, wo_own, attn_t)
        dq_t, d_k_seq, d_v_seq = attention_backward(qkv, d_attn, stat, cos_all[:, 0].T, sin_all[:, 0].T, hd)
        dq_full = gather(dq_t)
        shares = swap(jnp.concatenate([d_k_seq, d_v_seq], axis=1).reshape(n_dev, tokens, 2 * hd))
        dkv = jnp.sum(shares.reshape(n_kv, n_dev // n_kv, tokens, 2 * hd), axis=1, dtype=F32).astype(BF16).astype(F32)
        first, second = dkv[:, :, :hd // 2], dkv[:, :, hd // 2:hd]
        cos_k, sin_k = cos_tab[None], sin_tab[None]
        cos_k, sin_k = cos_k[:, :, 0], sin_k[:, :, 0]
        dkv = jnp.concatenate([first * cos_k + second * sin_k, second * cos_k - first * sin_k, dkv[:, :, hd:]], axis=2).astype(BF16)
        dkv = dkv.transpose(1, 0, 2).reshape(tokens, 2 * n_kv * hd)
        dkv_full = gather(dkv)
        dwkv = jnp.einsum('te,td->ed', dkv_full, u_col, preferred_element_type=F32).reshape(n_kv, 2, hd, rows)
        d_wk = dwkv[:, 0].transpose(2, 0, 1)
        d_wv = dwkv[:, 1].transpose(2, 0, 1)
        d_wq = jnp.einsum('et,td->ed', dq_full, u_col, preferred_element_type=F32).reshape(n_q, hd, rows).transpose(2, 0, 1)
        dq_own = lax.dynamic_slice_in_dim(dq_full, me * tokens, tokens, axis=1)
        dqkv = jnp.concatenate([dq_own, dkv.T], axis=0)
        d_normed = jnp.einsum('et,ced->tcd', dqkv, wqkv, preferred_element_type=F32).reshape(tokens, dim).astype(BF16)
        norm1_pull = jax.vjp(norm_forward, x_f32, g1)[1]
        d_x_norm, d_g1 = norm1_pull(d_normed.astype(F32))
        d_x = (d_hidden.astype(F32) + d_x_norm).astype(BF16)
        gains = jnp.stack([d_g1.reshape(n_dev, rows), d_g2.reshape(n_dev, rows)] + [jnp.zeros((n_dev, rows), F32)] * 6, axis=1)
        gsum = jnp.sum(swap(gains), axis=0)
        return (y_out, d_x, gsum[0], gsum[1], d_wq, d_wk, d_wv, d_wo.reshape(w_o.shape), d_gate, d_up, d_down)

    all_rows = P('sp')
    return jax.shard_map(layer_step, mesh=mesh, in_specs=(all_rows,) * 12, out_specs=(all_rows,) * 11, check_vma=False)
```

```python
import functools
import jax
import jax.numpy as jnp
from jax import lax
from jax.experimental import pallas as pl
from jax.experimental.pallas import tpu as pltpu
from jax.sharding import PartitionSpec as P

ROPE_BASE = 10000.0
NORM_EPS = 1e-5
NEG_LARGE = -1e30
F32 = jnp.float32
BF16 = jnp.bfloat16
N_DEV, N_CHIP, LANE, WIDE, CHUNK, STRIP = 16, 8, 128, 256, 512, 16
NT = (((1,), (1,)), ((), ()))
TN = (((0,), (0,)), ((), ()))
NN = (((1,), (0,)), ((), ()))
MESH = pl.DeviceIdType.MESH
VMEM_CAP = 62 * 1024 * 1024

CORE, X, Y, Z = 1, 2, 4, 8
XYZ = X + Y + Z
ORDERS = ((X, Y, Z), (Y, Z, X), (Z, X, Y))
CHIP_MASKS = (0, X, Y, Z, X + Y, X + Z, Y + Z, XYZ)
NEAR = (CORE, X, Y, Z)
OTHERS = range(1, N_DEV)
COLOURS = range(len(ORDERS))


def mm(a, b, dims):
    return lax.dot_general(a, b, dims, preferred_element_type=F32)


def seg(index, width=LANE):
    return pl.ds(pl.multiple_of(index * width, width), width)


def loop(count, body):
    lax.fori_loop(0, count, lambda i, c: (body(i), c)[1], 0)


def flipped(index, mask):
    out = index
    for bit in NEAR:
        if mask & bit:
            out = out + (1 - 2 * ((index // bit) % 2)) * bit
    return out


def thirds(total, unit):
    n = total // unit
    first = (n + 2) // 3
    second = (n - first + 1) // 2
    sizes = (first * unit, second * unit, (n - first - second) * unit)
    return ((0, sizes[0]), (sizes[0], sizes[1]), (sizes[0] + sizes[1], sizes[2]))


def enter(me, masks):
    barrier = pltpu.get_barrier_semaphore()
    for mask in masks:
        pl.semaphore_signal(barrier, inc=1, device_id=(flipped(me, mask),), device_id_type=MESH)
    pl.semaphore_wait(barrier, len(masks))


def remote(src, dst, send, recv, peer):
    return pltpu.make_async_remote_copy(src_ref=src, dst_ref=dst, send_sem=send, recv_sem=recv, device_id=(peer,), device_id_type=MESH)


def dma(*shape):
    return pltpu.SemaphoreType.DMA(shape)


class Swap:
    sems = (dma(N_DEV), dma(N_DEV))

    def __init__(self, src, dst, sems, me):
        self.src, self.dst, (self.send, self.recv), self.me = src, dst, sems, me

    def copy(self, mask):
        peer = flipped(self.me, mask)
        return remote(self.src(peer), self.dst(self.me), self.send.at[mask], self.recv.at[mask], peer)

    def start(self, masks=OTHERS):
        for mask in masks:
            self.copy(mask).start()

    def wait_recv(self):
        for mask in OTHERS:
            view = self.dst(flipped(self.me, mask))
            remote(view, view, self.send.at[mask], self.recv.at[mask], self.me).wait_recv()

    def wait_send(self):
        for mask in OTHERS:
            self.copy(mask).wait_send()


class Gather:
    ROUNDS = ((0,), (1,), (2,), (0, 1), (0, 2), (1, 2), (0, 1, 2))
    READY = ((0,), (), (), (X,), (Y,), (Z, X + Y), (X + Z, Y + Z, XYZ))
    sems = (dma(3, N_CHIP, 3), dma(3, N_CHIP), dma(N_CHIP), dma(N_CHIP))

    def __init__(self, own, block, cut, sems, me):
        self.own, self.block, self.cut, self.me = own, block, cut, me
        self.send, self.recv, self.pair_send, self.pair_recv = sems

    def source(self, mask):
        return self.block(flipped(self.me, mask)) if mask else self.own

    def unit(self, colour, mask, axis):
        return remote(self.cut(self.source(mask), colour), self.cut(self.block(flipped(self.me, mask)), colour),
                      self.send.at[colour, mask // 2, ORDERS[colour].index(axis)], self.recv.at[colour, (mask + axis) // 2],
                      flipped(self.me, axis))

    def pair(self, mask):
        return remote(self.source(mask), self.block(flipped(self.me, mask)), self.pair_send.at[mask // 2],
                      self.pair_recv.at[mask // 2], flipped(self.me, CORE))

    def wait_pair(self, mask):
        view = self.block(flipped(self.me, mask + CORE))
        remote(view, view, self.pair_send.at[mask // 2], self.pair_recv.at[mask // 2], self.me).wait_recv()

    def onward(self, colour):
        order = ORDERS[colour]
        for picks in self.ROUNDS:
            for axis in order[picks[-1] + 1:]:
                yield picks, sum(order[p] for p in picks), axis

    def start(self):
        for pos in COLOURS:
            for colour in COLOURS:
                self.unit(colour, 0, ORDERS[colour][pos]).start()
        self.pair(0).start()

    def round(self, r):
        for colour in COLOURS:
            mask = sum(ORDERS[colour][p] for p in self.ROUNDS[r])
            view = self.cut(self.block(flipped(self.me, mask)), colour)
            remote(view, view, self.send.at[colour, 0, 0], self.recv.at[colour, mask // 2], self.me).wait_recv()
            for picks, at, axis in self.onward(colour):
                if picks == self.ROUNDS[r]:
                    self.unit(colour, at, axis).start()
        for mask in {2: (X, Y, Z), 5: (X + Y, X + Z, Y + Z), 6: (XYZ,)}.get(r, ()):
            self.pair(mask).start()

    def run(self, use):
        self.start()
        for r in range(len(self.ROUNDS)):
            self.round(r)
            for mask in self.READY[r]:
                use(mask)

    def finish(self):
        for colour in COLOURS:
            for axis in ORDERS[colour]:
                self.unit(colour, 0, axis).wait_send()
            for _, at, axis in self.onward(colour):
                self.unit(colour, at, axis).wait_send()
        for mask in CHIP_MASKS:
            self.pair(mask).wait_send()


def row_gather(own, full, sems, me):
    width = own.shape[1]
    parts = thirds(width, LANE)

    def block(o):
        return full.at[o // 2, seg(o % 2), :]

    return Gather(own, block, lambda view, c: view.at[:, pl.ds(*parts[c])], sems, me)


def keep_own(own, full, me):
    def step(i):
        full[me // 2, pl.ds(pl.multiple_of((me % 2) * LANE + i * STRIP, STRIP), STRIP), :] = own[seg(i, STRIP), :]
    loop(LANE // STRIP, step)


class Scatter:
    ORDER = (XYZ, X + Y, Y + Z, X + Z, X, Y, Z, 0)
    sems = (dma(N_CHIP), dma(N_CHIP), dma(3, N_CHIP), dma(3, N_CHIP))

    @staticmethod
    def scratch(tokens, dim):
        return [pltpu.VMEM((N_CHIP, 2, tokens, dim), F32), pltpu.VMEM((N_CHIP, tokens, dim), F32), pltpu.VMEM((N_CHIP - 1, tokens, dim), F32)]

    def __init__(self, part, pair_in, link_in, sems, me):
        self.part, self.pair_in, self.link_in, self.me = part, pair_in, link_in, me
        self.pair_send, self.pair_recv, self.link_send, self.link_recv = sems
        self.core = me % 2
        self.tokens, self.dim = part.shape[2:]
        self.cols = thirds(self.dim, LANE)
        self.ready, self.sent = set(), [0] * len(ORDERS)

    @staticmethod
    def first(colour, mask):
        return next((i for i, a in enumerate(ORDERS[colour]) if mask & a), 3)

    def slot(self, colour, mask, axis):
        slots = [(m, a) for m in self.ORDER for a in ORDERS[colour][:self.first(colour, m)]]
        return slots.index((mask, axis))

    def pair(self, i):
        return remote(self.part.at[i, 1 - self.core], self.pair_in.at[i], self.pair_send.at[i], self.pair_recv.at[i], flipped(self.me, CORE))

    def link(self, colour, mask):
        axis = ORDERS[colour][self.first(colour, mask)]
        slot = self.slot(colour, mask - axis, axis)
        cs = pl.ds(*self.cols[colour])
        i = self.ORDER.index(mask)
        return remote(self.part.at[i, self.core, :, cs], self.link_in.at[slot, :, cs], self.link_send.at[colour, i],
                      self.link_recv.at[colour, slot], flipped(self.me, axis))

    def add(self, mask, ref, cs):
        i = self.ORDER.index(mask)

        def step(r):
            rs = seg(r, STRIP)
            self.part[i, self.core, rs, cs] += ref[rs, cs]
        loop(self.tokens // STRIP, step)

    def finish_pair(self, i):
        self.pair(i).wait_recv()
        self.add(self.ORDER[i], self.pair_in.at[i], pl.ds(0, self.dim))
        self.ready.add(self.ORDER[i])
        for colour in COLOURS:
            a, b, c = ORDERS[colour]
            todo = (XYZ, a + b, a + c, a)
            while self.sent[colour] < len(todo) and todo[self.sent[colour]] in self.ready:
                self.link(colour, todo[self.sent[colour]]).start()
                self.sent[colour] += 1

    def take(self, colour, mask, axis):
        self.link(colour, mask + axis).wait_recv()
        self.add(mask, self.link_in.at[self.slot(colour, mask, axis)], pl.ds(*self.cols[colour]))

    def run(self, product):
        for i, mask in enumerate(self.ORDER):
            product(i, flipped(self.me, mask) // 2)
            self.pair(i).start()
            if i:
                self.finish_pair(i - 1)
        self.finish_pair(N_CHIP - 1)
        for step in range(2):
            for colour in COLOURS:
                a, b, c = ORDERS[colour]
                mask = (b + c, b)[step]
                self.take(colour, mask, a)
                self.link(colour, mask).start()
        for colour in COLOURS:
            a, b, c = ORDERS[colour]
            self.take(colour, c, a)
            self.take(colour, c, b)
            self.link(colour, c).start()
        for colour in COLOURS:
            for axis in ORDERS[colour]:
                self.take(colour, 0, axis)
        return self.part.at[N_CHIP - 1, self.core]

    def finish(self):
        for i in range(N_CHIP):
            self.pair(i).wait_send()
        for colour in COLOURS:
            for mask in self.ORDER[:-1]:
                self.link(colour, mask).wait_send()


def block_product(part, a_ref, w_ref):
    tokens = part.shape[2]

    def product(i, chip):
        a = a_ref[:, seg(chip, 2 * tokens)]

        def step(n):
            cs = seg(n, CHUNK)
            r = mm(a, w_ref[:, cs], TN)
            part[i, 0, :, cs] = r[:tokens]
            part[i, 1, :, cs] = r[tokens:]
        loop(part.shape[3] // CHUNK, step)
    return product


def on_chip(n):
    return [pl.BlockSpec(memory_space=pltpu.VMEM)] * n


IN_HBM = pl.BlockSpec(memory_space=pl.ANY)


def call(kernel, ident, args, outs, scratch, flops, far_in=(), far_out=()):
    specs = [IN_HBM if i in far_in else on_chip(1)[0] for i in range(len(args))]
    out_specs = [IN_HBM if i in far_out else on_chip(1)[0] for i in range(len(outs))]
    return pl.pallas_call(
        kernel,
        out_shape=[jax.ShapeDtypeStruct(shape, dtype) for shape, dtype in outs],
        in_specs=specs, out_specs=out_specs, scratch_shapes=scratch,
        cost_estimate=pl.CostEstimate(flops=flops, bytes_accessed=flops // CHUNK, transcendentals=0),
        compiler_params=pltpu.CompilerParams(collective_id=ident, has_side_effects=True, vmem_limit_bytes=VMEM_CAP),
        name=kernel.func.__name__ if isinstance(kernel, functools.partial) else kernel.__name__,
    )(*args)


def gain_row(dst, small_all, which):
    for o in range(N_DEV):
        dst[:1, o * LANE:(o + 1) * LANE] = small_all[o, which:which + 1, :]


def norm_rows(src, gain, dst):
    def step(i):
        rs = seg(i, STRIP)
        t = src[rs, :].astype(F32)
        dst[rs, :] = (t * lax.rsqrt(jnp.mean(t * t, axis=-1, keepdims=True) + NORM_EPS) * gain[:1, :]).astype(BF16)
    loop(src.shape[0] // STRIP, step)


def norm_back(dy, src, gain, skip, dst, dgain):
    def step(i):
        rs = seg(i, STRIP)
        d = dy[rs, :].astype(BF16).astype(F32)
        t = src[rs, :].astype(F32)
        inv = lax.rsqrt(jnp.mean(t * t, axis=-1, keepdims=True) + NORM_EPS)
        gd = gain[:1, :] * d
        pull = jnp.mean(gd * t, axis=-1, keepdims=True)
        dst[rs, :] = (skip[rs, :].astype(F32) + (inv * gd - t * (inv * inv * inv * pull))).astype(BF16)
        g = d * (t * inv)
        dgain[...] += g[:N_CHIP] + g[N_CHIP:]
    dgain[...] = jnp.zeros_like(dgain)
    loop(src.shape[0] // STRIP, step)


def project_qkv(groups, hd, x_ref, small_ref, w_ref, cos_ref, sin_ref, qkv_ref, ucol_ref, small_all, w_out,
                full, acc, rot, u_scr, g_scr, osem, *sems):
    me = lax.axis_index('sp')
    tokens, dim = x_ref.shape
    cols = w_ref.shape[0]
    qw = tokens
    q_all = N_DEV * qw
    gsems, ssems, usems, qsems, ksems = sems[:4], sems[4:6], sems[6:8], sems[8:10], sems[10:]
    enter(me, OTHERS)
    smalls = Swap(lambda peer: small_ref, lambda o: small_all.at[o], ssems, me)
    smalls.start()
    parts = thirds(cols, STRIP)
    g = Gather(w_ref, lambda o: full.at[o // 2, :, seg(o % 2)], lambda view, c: view.at[pl.ds(*parts[c]), :], gsems, me)
    g.start()

    def own_block(i):
        full[me // 2, seg(i, WIDE), seg(me % 2)] = w_ref[seg(i, WIDE), :]
    loop(cols // WIDE, own_block)
    acc[...] = jnp.zeros_like(acc)
    small_all[me] = small_ref[...]
    smalls.wait_recv()
    gain_row(g_scr, small_all, 0)
    norm_rows(x_ref, g_scr, u_scr)
    ucols = Swap(lambda peer: u_scr.at[:, seg(peer)], lambda o: ucol_ref.at[seg(o, tokens), :], usems, me)

    def keep(mask):
        chip = flipped(me, mask) // 2
        return pltpu.make_async_copy(full.at[chip], w_out.at[chip], osem.at[mask // 2])

    def use(mask):
        g.wait_pair(mask)
        keep(mask).start()
        chip = flipped(me, mask) // 2
        u = u_scr[:, seg(chip, WIDE)]

        def step(i):
            rs = seg(i, CHUNK)
            acc[rs, :] += mm(full[chip, rs, :], u, NT)
        loop(cols // CHUNK, step)

    for r in range(len(g.ROUNDS)):
        g.round(r)
        if r == 0:
            ucols.start()
        for mask in g.READY[r]:
            use(mask)

    half = hd // 2
    cos, sin = cos_ref[...], sin_ref[...]

    def turn(h):
        first = seg(2 * h, half)
        second = seg(2 * h + 1, half)
        p = acc[first, :].astype(BF16).astype(F32)
        q = acc[second, :].astype(BF16).astype(F32)
        rot[first, :] = (p * cos - q * sin).astype(BF16)
        rot[second, :] = (q * cos + p * sin).astype(BF16)
    loop(q_all // hd, turn)
    for k in range(groups):
        turn(q_all // hd + 2 * k)
        vs = seg(q_all // hd + 2 * k + 1, hd)
        rot[vs, :] = acc[vs, :].astype(BF16)
    per = N_DEV // groups
    q_rows = lambda peer: seg(peer, qw)
    kv_rows = lambda peer: seg(q_all // (2 * hd) + peer // per, 2 * hd)
    qs = Swap(lambda peer: rot.at[q_rows(peer), :], lambda o: qkv_ref.at[:qw, seg(o, tokens)], qsems, me)
    kvs = Swap(lambda peer: rot.at[kv_rows(peer), :], lambda o: qkv_ref.at[qw:, seg(o, tokens)], ksems, me)
    qs.start()
    kvs.start()
    qkv_ref[:qw, seg(me, tokens)] = rot[q_rows(me), :]
    qkv_ref[qw:, seg(me, tokens)] = rot[kv_rows(me), :]
    ucol_ref[seg(me, tokens), :] = u_scr[:, seg(me)]
    for swap in (ucols, qs, kvs):
        swap.wait_recv()
    for mask in CHIP_MASKS:
        keep(mask).wait()
    g.finish()
    for swap in (smalls, ucols, qs, kvs):
        swap.wait_send()


QB = 256
KB = 256


def key_rows(dst, src, lo, hd):
    def step(i):
        dst[seg(i, KB), :] = src[lo:lo + hd, seg(i, KB)].T
    loop(src.shape[1] // KB, step)


def score_block(k, q2, scale, diagonal):
    s = mm(k, q2, NN) * scale
    if diagonal:
        key = lax.broadcasted_iota(jnp.int32, s.shape, 0)
        qry = lax.broadcasted_iota(jnp.int32, s.shape, 1) % QB
        s = jnp.where(qry >= key, s, NEG_LARGE)
    return s


def side_by_side(ref, heads, hd, qs):
    return jnp.concatenate([ref[h * hd:(h + 1) * hd, qs] for h in range(heads)], axis=1)


def attn_fwd(hd, qkv_ref, wg_ref, wu_ref, ot_ref, o_ref, stat_ref, w_ref, s_scr, k_scr, *sems):
    heads = qkv_ref.shape[0] // hd - 2
    seq = qkv_ref.shape[1]
    scale = hd ** -0.5
    lanes = heads * QB
    me = lax.axis_index('sp')
    qw = heads * hd
    feat = wg_ref.shape[0] // N_DEV
    enter(me, OTHERS)
    gates = Swap(lambda peer: wg_ref.at[seg(peer, feat), :], lambda o: w_ref.at[:feat, seg(o)], sems[:2], me)
    ups = Swap(lambda peer: wu_ref.at[seg(peer, feat), :], lambda o: w_ref.at[feat:, seg(o)], sems[2:4], me)
    osend, orecv = sems[4:]
    gates.start()
    ups.start()
    w_ref[:feat, seg(me)] = wg_ref[seg(me, feat), :]
    w_ref[feat:, seg(me)] = wu_ref[seg(me, feat), :]
    key_rows(k_scr, qkv_ref, qw, hd)

    def o_copy(peer, origin):
        return remote(o_ref.at[:, seg(peer)], ot_ref.at[seg(origin, qw), :], osend.at[peer], orecv.at[origin], peer)

    def q_block(qb):
        qs = seg(qb, QB)
        q2 = side_by_side(qkv_ref, heads, hd, qs)

        def scores(kb, top, diagonal):
            s = score_block(k_scr[seg(kb, KB), :], q2, scale, diagonal)
            s_scr[seg(kb, KB), :] = s
            return jnp.maximum(top, jnp.max(s, axis=0, keepdims=True))

        top = lax.fori_loop(0, qb, lambda kb, t: scores(kb, t, False), jnp.full((1, lanes), NEG_LARGE, F32))
        top = scores(qb, top, True)

        def expo(kb, tot):
            e = jnp.exp(s_scr[seg(kb, KB), :] - top)
            s_scr[seg(kb, KB), :] = e
            return tot + jnp.sum(e, axis=0, keepdims=True)

        inv = 1.0 / lax.fori_loop(0, qb + 1, expo, jnp.zeros((1, lanes), F32))

        def weigh(kb, acc):
            p = (s_scr[seg(kb, KB), :] * inv).astype(BF16)
            return acc + mm(qkv_ref[qw + hd:, seg(kb, KB)], p, NN)

        acc = lax.fori_loop(0, qb + 1, weigh, jnp.zeros((hd, lanes), F32))
        for h in range(heads):
            o_ref[h * hd:(h + 1) * hd, qs] = acc[:, h * QB:(h + 1) * QB].astype(BF16)
        stat_ref[qb, :1, :] = top
        stat_ref[qb, 1:, :] = inv
        for core in range(2):
            peer = 2 * qb + core

            @pl.when(peer != me)
            def _():
                o_copy(peer, me).start()

    loop(seq // QB, q_block)
    ot_ref[seg(me, qw), :] = o_ref[:, seg(me)]
    for mask in OTHERS:
        o_copy(me, flipped(me, mask)).wait_recv()
    gates.wait_recv()
    ups.wait_recv()
    for mask in OTHERS:
        o_copy(flipped(me, mask), me).wait_send()
    gates.wait_send()
    ups.wait_send()


def mlp_local(ot_ref, wo_ref, x_ref, small_all, dout_ref, wgu_ref, down_ref, h_ref, m_out, glu_ref, dgu_ref, ddown_ref,
              full_w, full_d, full_m, acc, m_scr, g_scr, osem, *sems):
    me = lax.axis_index('sp')
    feat, dim = down_ref.shape
    enter(me, NEAR)
    gw = row_gather(wo_ref, full_w, sems[:4], me)
    gd = row_gather(dout_ref, full_d, sems[4:8], me)
    gm = row_gather(m_scr, full_m, sems[8:], me)

    def project(mask):
        gw.wait_pair(mask)
        chip = flipped(me, mask) // 2
        o = ot_ref[seg(chip, WIDE), :]

        def step(n):
            acc[:, seg(n, CHUNK)] += mm(o, full_w[chip, :, seg(n, CHUNK)], TN)
        loop(dim // CHUNK, step)

    gw.start()
    keep_own(wo_ref, full_w, me)
    keep_own(dout_ref, full_d, me)
    gain_row(g_scr, small_all, 1)
    acc[...] = jnp.zeros_like(acc)
    ddown_ref[...] = jnp.zeros_like(ddown_ref)
    for r in range(len(gw.ROUNDS)):
        gw.round(r)
        if r == 3:
            gd.start()
        for mask in gw.READY[r]:
            project(mask)

    def residual(i):
        rs = seg(i, STRIP)
        h_ref[rs, :] = (x_ref[rs, :].astype(F32) + acc[rs, :]).astype(BF16)
    loop(x_ref.shape[0] // STRIP, residual)
    norm_rows(h_ref, g_scr, m_scr)
    gm.start()
    keep_own(m_scr, full_m, me)

    def keep(mask):
        chip = flipped(me, mask) // 2
        return pltpu.make_async_copy(full_m.at[chip], m_out.at[chip], osem.at[mask // 2])

    def use(mask):
        gd.wait_pair(mask)
        gm.wait_pair(mask)
        keep(mask).start()
        chip = flipped(me, mask) // 2
        ts = seg(chip, WIDE)
        gu = mm(wgu_ref[...], full_m[chip], NT).astype(BF16).astype(F32)
        gate, up = gu[:feat], gu[feat:]
        d_glu = mm(down_ref[...], full_d[chip], NT).astype(BF16).astype(F32)
        sig = jax.nn.sigmoid(gate)
        act = gate * sig
        glu = (act * up).astype(BF16)
        glu_ref[:, ts] = glu
        dgu_ref[:feat, ts] = (d_glu * up * (sig * (1.0 + gate * (1.0 - sig)))).astype(BF16)
        dgu_ref[feat:, ts] = (d_glu * act).astype(BF16)

        def step(n):
            ddown_ref[:, seg(n, CHUNK)] += mm(glu, full_d[chip, :, seg(n, CHUNK)], NN)
        loop(dim // CHUNK, step)

    for r in range(len(gm.ROUNDS)):
        gd.round(r)
        gm.round(r)
        for mask in gm.READY[r]:
            use(mask)
    for mask in CHIP_MASKS:
        keep(mask).wait()
    for g in (gw, gd, gm):
        g.finish()


def scatter_y(a_ref, w_ref, h_ref, y_ref, *scr):
    me = lax.axis_index('sp')
    enter(me, NEAR)
    s = Scatter(*scr[:3], scr[3:], me)
    total = s.run(block_product(s.part, a_ref, w_ref))
    y_ref[...] = (h_ref[...].astype(F32) + total[...]).astype(BF16)
    s.finish()


def mlp_back(dgu_ref, wgu_ref, h_ref, small_all, dout_ref, wo_ref, o_ref, dh_ref, do_ref, dwo_ref, dg_ref,
             full, g_scr, *scr):
    me = lax.axis_index('sp')
    dim = wo_ref.shape[1]
    enter(me, NEAR)
    s = Scatter(*scr[:3], scr[3:7], me)
    g = row_gather(dh_ref, full, scr[7:], me)
    gain_row(g_scr, small_all, 1)
    dwo_ref[...] = jnp.zeros_like(dwo_ref)
    total = s.run(block_product(s.part, dgu_ref, wgu_ref))
    norm_back(total, h_ref, g_scr, dout_ref, dh_ref, dg_ref)

    def use(mask):
        g.wait_pair(mask)
        chip = flipped(me, mask) // 2
        do_ref[:, seg(chip, WIDE)] = mm(wo_ref[...], full[chip], NT).astype(BF16)
        o = o_ref[:, seg(chip, WIDE)]

        def step(n):
            dwo_ref[:, seg(n, CHUNK)] += mm(o, full[chip, :, seg(n, CHUNK)], NN)
        loop(dim // CHUNK, step)

    g.start()
    keep_own(dh_ref, full, me)
    for r in range(len(g.ROUNDS)):
        g.round(r)
        for mask in g.READY[r]:
            use(mask)
    s.finish()
    g.finish()


def attn_bwd(hd, qkv_ref, do_ref, stat_ref, cos_ref, sin_ref, dgu_ref, m_ref, dq_ref, dkv_ref, dg_ref, du_ref,
             p_scr, dp_scr, k_scr, v_scr, dk_acc, dv_acc, stage, *sems):
    heads = qkv_ref.shape[0] // hd - 2
    seq = qkv_ref.shape[1]
    scale = hd ** -0.5
    lanes = heads * QB
    qw = heads * hd
    half = hd // 2
    me = lax.axis_index('sp')
    feat = dgu_ref.shape[0] // 2
    enter(me, OTHERS)

    def piece(lo):
        return lambda peer: stage.at[peer // 2, lo:lo + feat, seg(peer % 2)]
    gates = Swap(piece(0), lambda o: dg_ref.at[seg(o, feat), :], sems[:2], me)
    ups = Swap(piece(feat), lambda o: du_ref.at[seg(o, feat), :], sems[2:], me)
    for mask in (XYZ, X + Y, X + Z, Y + Z, X, Y, Z, 0):
        chip = flipped(me, mask) // 2
        cols = m_ref[:, :, seg(chip, WIDE)].reshape(seq, WIDE)
        stage[chip] = mm(dgu_ref[...], cols, NN)
        for swap in (gates, ups):
            swap.start([m for m in (mask, mask + CORE) if m])
    dg_ref[seg(me, feat), :] = stage[me // 2, :feat, seg(me % 2)]
    du_ref[seg(me, feat), :] = stage[me // 2, feat:, seg(me % 2)]

    dk_acc[...] = jnp.zeros_like(dk_acc)
    dv_acc[...] = jnp.zeros_like(dv_acc)
    key_rows(k_scr, qkv_ref, qw, hd)
    key_rows(v_scr, qkv_ref, qw + hd, hd)

    def q_block(qb):
        qs = seg(qb, QB)
        q2 = side_by_side(qkv_ref, heads, hd, qs)
        do2 = side_by_side(do_ref, heads, hd, qs)
        top = stat_ref[qb, :1, :]
        inv = stat_ref[qb, 1:, :]

        def probs(kb, rd, diagonal):
            ks = seg(kb, KB)
            s = score_block(k_scr[ks, :], q2, scale, diagonal)
            p = jnp.exp(s - top) * inv
            dp = mm(v_scr[ks, :], do2, NN).astype(BF16)
            p_scr[ks, :] = p
            dp_scr[ks, :] = dp
            dv_acc[ks, :] += mm(p.astype(BF16), do2, NT)
            return rd + jnp.sum(dp.astype(F32) * p, axis=0, keepdims=True)

        rd = lax.fori_loop(0, qb, lambda kb, r: probs(kb, r, False), jnp.zeros((1, lanes), F32))
        rd = probs(qb, rd, True)

        def d_scores(kb, acc):
            ks = seg(kb, KB)
            ds = (p_scr[ks, :] * (dp_scr[ks, :].astype(F32) - rd) * scale).astype(BF16)
            dk_acc[ks, :] += mm(ds, q2, NT)
            return acc + mm(qkv_ref[qw:qw + hd, ks], ds, NN)

        acc = lax.fori_loop(0, qb + 1, d_scores, jnp.zeros((hd, lanes), F32))
        cos, sin = cos_ref[:, qs], sin_ref[:, qs]
        for h in range(heads):
            dq = acc[:, h * QB:(h + 1) * QB].astype(BF16).astype(F32)
            p, q = dq[:half], dq[half:]
            dq_ref[h * hd:h * hd + half, qs] = (p * cos + q * sin).astype(BF16)
            dq_ref[h * hd + half:(h + 1) * hd, qs] = (q * cos - p * sin).astype(BF16)

    loop(seq // QB, q_block)

    def share(i):
        rs = seg(i, WIDE)
        dkv_ref[rs, :] = jnp.concatenate([dk_acc[rs, :], dv_acc[rs, :]], axis=1).astype(BF16)
    loop(seq // WIDE, share)
    for swap in (gates, ups):
        swap.wait_recv()
    for swap in (gates, ups):
        swap.wait_send()


def tail(groups, hd, dq_ref, dkv_ref, ucol_ref, cos_ref, sin_ref, w_hbm, x_ref, small_all, dh_ref, dg2_ref,
         dwq_ref, dwkv_ref, dx_ref, gain_ref, full, w_scr, shares, dkv_own, full_kv, dqkv, dn, g_scr, dg1, gains, gains_in, wsem, *sems):
    me = lax.axis_index('sp')
    seq, tokens = ucol_ref.shape
    half = hd // 2
    per = N_DEV // groups
    q_all = dwq_ref.shape[0]
    enter(me, OTHERS)
    load = pltpu.make_async_copy(w_hbm, w_scr, wsem)
    load.start()
    sh = Swap(lambda peer: dkv_ref.at[seg(peer, tokens), :], lambda o: shares.at[o], sems[:2], me)
    gq = row_gather(dq_ref, full, sems[2:6], me)
    parts = thirds(dkv_own.shape[0], STRIP)
    gk = Gather(dkv_own, lambda o: full_kv.at[:, seg(o, tokens)], lambda view, c: view.at[pl.ds(*parts[c]), :], sems[6:10], me)
    gs = Swap(lambda peer: gains.at[:, seg(peer)], lambda o: gains_in.at[o], sems[10:], me)
    sh.start()
    gq.start()
    keep_own(dq_ref, full, me)
    gain_row(g_scr, small_all, 0)
    shares[me] = dkv_ref[seg(me, tokens), :]
    sh.wait_recv()
    cos, sin = cos_ref[...], sin_ref[...]
    for k in range(groups):
        both = sum(shares[per * k + i].astype(F32) for i in range(per)).astype(BF16).astype(F32).T
        p, q = both[:half], both[half:hd]
        lo = 2 * hd * k
        dkv_own[lo:lo + half, :] = (p * cos + q * sin).astype(BF16)
        dkv_own[lo + half:lo + hd, :] = (q * cos - p * sin).astype(BF16)
        dkv_own[lo + hd:lo + 2 * hd, :] = both[hd:].astype(BF16)
    gk.start()
    full_kv[:, seg(me, tokens)] = dkv_own[...]
    dqkv[q_all:, :] = dkv_own[...]

    def use(mask):
        gq.wait_pair(mask)
        chip = flipped(me, mask) // 2
        dwq_ref[seg(chip, WIDE), :] = mm(full[chip], ucol_ref[...], NN)
        dqkv[seg(chip, WIDE), :] = full[chip, :, seg(me, tokens)]

    for r in range(len(gq.ROUNDS)):
        gq.round(r)
        gk.round(r)
        for mask in gq.READY[r]:
            use(mask)
    load.wait()

    def normed(i):
        dn[:, seg(i, WIDE)] = mm(dqkv[...], w_scr[i], TN)
    loop(N_CHIP, normed)
    norm_back(dn, x_ref, g_scr, dh_ref, dx_ref, dg1)
    gains[...] = jnp.concatenate([jnp.sum(dg1[...], axis=0, keepdims=True), jnp.sum(dg2_ref[...], axis=0, keepdims=True),
                                  jnp.zeros((N_CHIP - 2, dg1.shape[1]), F32)], axis=0)
    gs.start()
    gains_in[me] = gains[:, seg(me)]
    for mask in CHIP_MASKS:
        gk.wait_pair(mask)
    dwkv_ref[...] = mm(full_kv[...], ucol_ref[...], NN)
    gs.wait_recv()
    gain_ref[...] = sum(gains_in[o] for o in range(N_DEV))
    for c in (sh, gs):
        c.wait_send()
    for g in (gq, gk):
        g.finish()


def rope_tables(positions, head_dim):
    half_dim = head_dim // 2
    inv_freq = 1.0 / (ROPE_BASE ** (jnp.arange(half_dim, dtype=F32) * (2.0 / head_dim)))
    angles = positions.astype(F32)[None, :] * inv_freq[:, None]
    return jnp.cos(angles), jnp.sin(angles)


def solution(mesh):
    assert mesh.shape['sp'] == N_DEV

    def layer_step(x_in, positions, d_out, norm1_gain, norm2_gain, w_q, w_k, w_v, w_o, w_gate, w_up, w_down):
        tokens, dim = x_in.shape
        seq = tokens * N_DEV
        n_q, hd = w_q.shape[1:]
        n_kv = w_k.shape[1]
        qw = n_q // N_DEV * hd
        rows = w_q.shape[0]
        feat = w_down.shape[0]
        cols = (n_q + 2 * n_kv) * hd
        lanes = qw // hd * QB
        vm = pltpu.VMEM
        full = vm((N_CHIP, WIDE, dim), BF16)
        gain_scr = vm((N_CHIP, dim), F32)
        small_shape = ((N_DEV, N_CHIP, rows), F32)

        small = jnp.stack([norm1_gain.astype(F32), norm2_gain.astype(F32), positions.astype(F32)])
        small = jnp.pad(small, ((0, N_CHIP - small.shape[0]), (0, 0)))
        cos_own, sin_own = rope_tables(positions, hd)
        wq_t = w_q.transpose(1, 2, 0).reshape(n_q * hd, rows)
        wkv_t = jnp.stack([w_k.transpose(1, 2, 0), w_v.transpose(1, 2, 0)], axis=1).reshape(2 * n_kv * hd, rows)
        wo_own = w_o.reshape(qw, dim)

        qkv, u_col, small_all, wqkv = call(
            functools.partial(project_qkv, n_kv, hd), 0, (x_in, small, jnp.concatenate([wq_t, wkv_t], axis=0), cos_own, sin_own),
            (((qw + 2 * hd, seq), BF16), ((seq, rows), BF16), small_shape, ((N_CHIP, cols, WIDE), BF16)),
            [vm((N_CHIP, cols, WIDE), BF16), vm((cols, tokens), F32), vm((cols, tokens), BF16), vm((tokens, dim), BF16), gain_scr, dma(N_CHIP),
             *Gather.sems, *(4 * Swap.sems)], 2 * tokens * dim * cols, far_out=(3,))
        attn_tok, attn_t, stat, wgu = call(
            functools.partial(attn_fwd, hd), 1, (qkv, w_gate.T, w_up.T),
            (((n_q * hd, tokens), BF16), ((qw, seq), BF16), ((seq // QB, 2, lanes), F32), ((2 * feat, dim), BF16)),
            [vm((seq, lanes), F32), vm((seq, hd), BF16), *(3 * Swap.sems)], 4 * qw * seq * seq)
        hidden, m_full, glu, dgu, d_down = call(
            mlp_local, 2, (attn_tok, wo_own, x_in, small_all, d_out, wgu, w_down),
            (((tokens, dim), BF16), ((N_CHIP, WIDE, dim), BF16), ((feat, seq), BF16), ((2 * feat, seq), BF16), ((feat, dim), F32)),
            [full, full, full, vm((tokens, dim), F32), vm((tokens, dim), BF16), gain_scr, dma(N_CHIP), *(3 * Gather.sems)],
            8 * feat * seq * dim, far_out=(1,))
        d_hidden, d_attn, d_wo, d_g2 = call(
            mlp_back, 3, (dgu, wgu, hidden, small_all, d_out, wo_own, attn_t),
            (((tokens, dim), BF16), ((qw, seq), BF16), ((qw, dim), F32), ((N_CHIP, dim), F32)),
            [full, gain_scr, *Scatter.scratch(tokens, dim), *Scatter.sems, *Gather.sems], 4 * feat * seq * dim)
        cos_all, sin_all = rope_tables(small_all[:, 2].reshape(-1), hd)
        dq_t, dkv, d_gate_t, d_up_t = call(
            functools.partial(attn_bwd, hd), 4, (qkv, d_attn, stat, cos_all, sin_all, dgu, m_full),
            (((qw, seq), BF16), ((seq, 2 * hd), BF16), ((feat * N_DEV, rows), F32), ((feat * N_DEV, rows), F32)),
            [vm((seq, lanes), F32), vm((seq, lanes), BF16), vm((seq, hd), BF16), vm((seq, hd), BF16), vm((seq, hd), F32), vm((seq, hd), F32),
             vm((N_CHIP, 2 * feat, WIDE), F32), *(2 * Swap.sems)], 10 * qw * seq * seq)
        d_wq, d_wkv, d_x, gains = call(
            functools.partial(tail, n_kv, hd), 5, (dq_t, dkv, u_col, cos_own, sin_own, wqkv, x_in, small_all, d_hidden, d_g2),
            (((n_q * hd, rows), F32), ((2 * n_kv * hd, rows), F32), ((tokens, dim), BF16), ((N_CHIP, rows), F32)),
            [full, vm((N_CHIP, cols, WIDE), BF16), vm((N_DEV, tokens, 2 * hd), BF16), vm((2 * n_kv * hd, tokens), BF16), vm((2 * n_kv * hd, seq), BF16),
             vm((cols, tokens), BF16), vm((tokens, dim), F32), gain_scr, gain_scr, gain_scr, vm((N_DEV, N_CHIP, rows), F32), dma(),
             *Swap.sems, *(2 * Gather.sems), *Swap.sems], 4 * tokens * dim * cols, far_in=(5,))
        y_out, = call(scatter_y, 6, (glu, w_down, hidden), (((tokens, dim), BF16),),
                      [*Scatter.scratch(tokens, dim), *Scatter.sems], 2 * feat * seq * dim)

        d_wkv = d_wkv.reshape(n_kv, 2, hd, rows).transpose(3, 0, 2, 1)
        return (y_out, d_x, gains[0], gains[1], d_wq.reshape(n_q, hd, rows).transpose(2, 0, 1), d_wkv[..., 0], d_wkv[..., 1],
                d_wo.reshape(w_o.shape), d_gate_t.T, d_up_t.T, d_down)

    all_rows = P('sp')
    return jax.shard_map(layer_step, mesh=mesh, in_specs=(all_rows,) * 12, out_specs=(all_rows,) * 11, check_vma=False)
```

```python
import functools
import jax
import jax.numpy as jnp
from jax import lax
from jax.experimental import pallas as pl
from jax.experimental.pallas import tpu as pltpu
from jax.sharding import PartitionSpec as P

ROPE_BASE = 10000.0
NORM_EPS = 1e-5
NEG_LARGE = -1e30
F32 = jnp.float32
BF16 = jnp.bfloat16
N_DEV, N_CHIP, LANE, WIDE, CHUNK, STRIP = 16, 8, 128, 256, 512, 16
NT = (((1,), (1,)), ((), ()))
TN = (((0,), (0,)), ((), ()))
NN = (((1,), (0,)), ((), ()))
MESH = pl.DeviceIdType.MESH
VMEM_CAP = 62 * 1024 * 1024

CORE, X, Y, Z = 1, 2, 4, 8
XYZ = X + Y + Z
ORDERS = ((X, Y, Z), (Y, Z, X), (Z, X, Y))
CHIP_MASKS = (0, X, Y, Z, X + Y, X + Z, Y + Z, XYZ)
NEAR = (CORE, X, Y, Z)
OTHERS = range(1, N_DEV)
SETS = tuple(tuple(m + c for m in masks for c in (0, CORE)) for masks in ((XYZ,), (X, Y + Z), (Y, X + Z), (Z, X + Y)))
COLOURS = range(len(ORDERS))


def mm(a, b, dims):
    return lax.dot_general(a, b, dims, preferred_element_type=F32)


def seg(index, width=LANE):
    return pl.ds(pl.multiple_of(index * width, width), width)


def loop(count, body):
    lax.fori_loop(0, count, lambda i, c: (body(i), c)[1], 0)


def flipped(index, mask):
    out = index
    for bit in NEAR:
        if mask & bit:
            out = out + (1 - 2 * ((index // bit) % 2)) * bit
    return out


def other_chip(chip, k):
    return sum(((chip // b + k // b) % 2) * b for b in (1, 2, 4))


def thirds(total, unit):
    n = total // unit
    first = (n + 2) // 3
    second = (n - first + 1) // 2
    sizes = (first * unit, second * unit, (n - first - second) * unit)
    return ((0, sizes[0]), (sizes[0], sizes[1]), (sizes[0] + sizes[1], sizes[2]))


def enter(me, masks):
    barrier = pltpu.get_barrier_semaphore()
    for mask in masks:
        pl.semaphore_signal(barrier, inc=1, device_id=(flipped(me, mask),), device_id_type=MESH)
    pl.semaphore_wait(barrier, len(masks))


def remote(src, dst, send, recv, peer):
    return pltpu.make_async_remote_copy(src_ref=src, dst_ref=dst, send_sem=send, recv_sem=recv, device_id=(peer,), device_id_type=MESH)


def dma(*shape):
    return pltpu.SemaphoreType.DMA(shape)


class Swap:
    sems = (dma(N_DEV), dma(N_DEV))

    def __init__(self, src, dst, sems, me):
        self.src, self.dst, (self.send, self.recv), self.me = src, dst, sems, me

    def copy(self, mask):
        peer = flipped(self.me, mask)
        return remote(self.src(peer), self.dst(self.me), self.send.at[mask], self.recv.at[mask], peer)

    def start(self, masks=OTHERS):
        for mask in masks:
            self.copy(mask).start()

    def advance(self, n):
        if n:
            for mask in SETS[n - 1]:
                self.copy(mask).wait_send()
        self.start(SETS[n])

    def wait_recv(self):
        for mask in OTHERS:
            view = self.dst(flipped(self.me, mask))
            remote(view, view, self.send.at[mask], self.recv.at[mask], self.me).wait_recv()

    def wait_send(self, masks=OTHERS):
        for mask in masks:
            self.copy(mask).wait_send()


class Gather:
    ROUNDS = ((0,), (1,), (2,), (0, 1), (0, 2), (1, 2), (0, 1, 2))
    READY = ((0,), (), (), (X,), (Y,), (Z, X + Y), (X + Z, Y + Z, XYZ))
    sems = (dma(3, N_CHIP, 3), dma(3, N_CHIP), dma(N_CHIP), dma(N_CHIP))

    def __init__(self, own, block, cut, sems, me):
        self.own, self.block, self.cut, self.me = own, block, cut, me
        self.send, self.recv, self.pair_send, self.pair_recv = sems

    def source(self, mask):
        return self.block(flipped(self.me, mask)) if mask else self.own

    def unit(self, colour, mask, axis):
        return remote(self.cut(self.source(mask), colour), self.cut(self.block(flipped(self.me, mask)), colour),
                      self.send.at[colour, mask // 2, ORDERS[colour].index(axis)], self.recv.at[colour, (mask + axis) // 2],
                      flipped(self.me, axis))

    def pair(self, mask):
        return remote(self.source(mask), self.block(flipped(self.me, mask)), self.pair_send.at[mask // 2],
                      self.pair_recv.at[mask // 2], flipped(self.me, CORE))

    def wait_pair(self, mask):
        view = self.block(flipped(self.me, mask + CORE))
        remote(view, view, self.pair_send.at[mask // 2], self.pair_recv.at[mask // 2], self.me).wait_recv()

    def onward(self, colour):
        order = ORDERS[colour]
        for picks in self.ROUNDS:
            for axis in order[picks[-1] + 1:]:
                yield picks, sum(order[p] for p in picks), axis

    def start(self):
        for pos in COLOURS:
            for colour in COLOURS:
                self.unit(colour, 0, ORDERS[colour][pos]).start()
        self.pair(0).start()

    def round(self, r):
        for colour in COLOURS:
            mask = sum(ORDERS[colour][p] for p in self.ROUNDS[r])
            view = self.cut(self.block(flipped(self.me, mask)), colour)
            remote(view, view, self.send.at[colour, 0, 0], self.recv.at[colour, mask // 2], self.me).wait_recv()
            for picks, at, axis in self.onward(colour):
                if picks == self.ROUNDS[r]:
                    self.unit(colour, at, axis).start()
        for mask in {2: (X, Y, Z), 5: (X + Y, X + Z, Y + Z), 6: (XYZ,)}.get(r, ()):
            self.pair(mask).start()

    def run(self, use):
        self.start()
        for r in range(len(self.ROUNDS)):
            self.round(r)
            for mask in self.READY[r]:
                use(mask)

    def finish(self):
        for colour in COLOURS:
            for axis in ORDERS[colour]:
                self.unit(colour, 0, axis).wait_send()
            for _, at, axis in self.onward(colour):
                self.unit(colour, at, axis).wait_send()
        for mask in CHIP_MASKS:
            self.pair(mask).wait_send()


def row_gather(own, full, sems, me):
    width = own.shape[1]
    parts = thirds(width, LANE)

    def block(o):
        return full.at[o // 2, seg(o % 2), :]

    return Gather(own, block, lambda view, c: view.at[:, pl.ds(*parts[c])], sems, me)


def keep_own(own, full, me):
    def step(i):
        full[me // 2, pl.ds(pl.multiple_of((me % 2) * LANE + i * STRIP, STRIP), STRIP), :] = own[seg(i, STRIP), :]
    loop(LANE // STRIP, step)


class Scatter:
    ORDER = (XYZ, X + Y, Y + Z, X + Z, X, Y, Z, 0)
    sems = (dma(N_CHIP), dma(N_CHIP), dma(3, N_CHIP), dma(3, N_CHIP))

    @staticmethod
    def scratch(tokens, dim):
        return [pltpu.VMEM((N_CHIP, 2, tokens, dim), F32), pltpu.VMEM((N_CHIP, tokens, dim), F32), pltpu.VMEM((N_CHIP - 1, tokens, dim), F32)]

    def __init__(self, part, pair_in, link_in, sems, me):
        self.part, self.pair_in, self.link_in, self.me = part, pair_in, link_in, me
        self.pair_send, self.pair_recv, self.link_send, self.link_recv = sems
        self.core = me % 2
        self.tokens, self.dim = part.shape[2:]
        self.cols = thirds(self.dim, LANE)
        self.ready, self.sent = set(), [0] * len(ORDERS)

    @staticmethod
    def first(colour, mask):
        return next((i for i, a in enumerate(ORDERS[colour]) if mask & a), 3)

    def slot(self, colour, mask, axis):
        slots = [(m, a) for m in self.ORDER for a in ORDERS[colour][:self.first(colour, m)]]
        return slots.index((mask, axis))

    def pair(self, i):
        return remote(self.part.at[i, 1 - self.core], self.pair_in.at[i], self.pair_send.at[i], self.pair_recv.at[i], flipped(self.me, CORE))

    def link(self, colour, mask):
        axis = ORDERS[colour][self.first(colour, mask)]
        slot = self.slot(colour, mask - axis, axis)
        cs = pl.ds(*self.cols[colour])
        i = self.ORDER.index(mask)
        return remote(self.part.at[i, self.core, :, cs], self.link_in.at[slot, :, cs], self.link_send.at[colour, i],
                      self.link_recv.at[colour, slot], flipped(self.me, axis))

    def add(self, mask, ref, cs):
        i = self.ORDER.index(mask)

        def step(r):
            rs = seg(r, STRIP)
            self.part[i, self.core, rs, cs] += ref[rs, cs]
        loop(self.tokens // STRIP, step)

    def finish_pair(self, i):
        self.pair(i).wait_recv()
        self.add(self.ORDER[i], self.pair_in.at[i], pl.ds(0, self.dim))
        self.ready.add(self.ORDER[i])
        for colour in COLOURS:
            a, b, c = ORDERS[colour]
            todo = (XYZ, a + b, a + c, a)
            while self.sent[colour] < len(todo) and todo[self.sent[colour]] in self.ready:
                self.link(colour, todo[self.sent[colour]]).start()
                self.sent[colour] += 1

    def take(self, colour, mask, axis):
        self.link(colour, mask + axis).wait_recv()
        self.add(mask, self.link_in.at[self.slot(colour, mask, axis)], pl.ds(*self.cols[colour]))

    def run(self, product):
        for i, mask in enumerate(self.ORDER):
            product(i, flipped(self.me, mask) // 2)
            self.pair(i).start()
            if i:
                self.finish_pair(i - 1)
        self.finish_pair(N_CHIP - 1)
        for step in range(2):
            for colour in COLOURS:
                a, b, c = ORDERS[colour]
                mask = (b + c, b)[step]
                self.take(colour, mask, a)
                self.link(colour, mask).start()
        for colour in COLOURS:
            a, b, c = ORDERS[colour]
            self.take(colour, c, a)
            self.take(colour, c, b)
            self.link(colour, c).start()
        for colour in COLOURS:
            for axis in ORDERS[colour]:
                self.take(colour, 0, axis)
        return self.part.at[N_CHIP - 1, self.core]

    def finish(self):
        for i in range(N_CHIP):
            self.pair(i).wait_send()
        for colour in COLOURS:
            for mask in self.ORDER[:-1]:
                self.link(colour, mask).wait_send()


def block_product(part, a_ref, w_ref):
    tokens = part.shape[2]

    def product(i, chip):
        a = a_ref[:, seg(chip, 2 * tokens)]

        def step(n):
            cs = seg(n, CHUNK)
            r = mm(a, w_ref[:, cs], TN)
            part[i, 0, :, cs] = r[:tokens]
            part[i, 1, :, cs] = r[tokens:]
        loop(part.shape[3] // CHUNK, step)
    return product


def on_chip(n):
    return [pl.BlockSpec(memory_space=pltpu.VMEM)] * n


IN_HBM = pl.BlockSpec(memory_space=pl.ANY)


def call(kernel, ident, args, outs, scratch, flops, far_in=(), far_out=()):
    specs = [IN_HBM if i in far_in else on_chip(1)[0] for i in range(len(args))]
    out_specs = [IN_HBM if i in far_out else on_chip(1)[0] for i in range(len(outs))]
    return pl.pallas_call(
        kernel,
        out_shape=[jax.ShapeDtypeStruct(shape, dtype) for shape, dtype in outs],
        in_specs=specs, out_specs=out_specs, scratch_shapes=scratch,
        cost_estimate=pl.CostEstimate(flops=flops, bytes_accessed=flops // CHUNK, transcendentals=0),
        compiler_params=pltpu.CompilerParams(collective_id=ident, has_side_effects=True, vmem_limit_bytes=VMEM_CAP),
        name=kernel.func.__name__ if isinstance(kernel, functools.partial) else kernel.__name__,
    )(*args)


def gain_row(dst, small_all, which):
    for o in range(N_DEV):
        dst[:1, o * LANE:(o + 1) * LANE] = small_all[o, which:which + 1, :]


def norm_rows(src, gain, dst):
    def step(i):
        rs = seg(i, STRIP)
        t = src[rs, :].astype(F32)
        dst[rs, :] = (t * lax.rsqrt(jnp.mean(t * t, axis=-1, keepdims=True) + NORM_EPS) * gain[:1, :]).astype(BF16)
    loop(src.shape[0] // STRIP, step)


def norm_back(dy, src, gain, skip, dst, dgain):
    def step(i):
        rs = seg(i, STRIP)
        d = dy[rs, :].astype(BF16).astype(F32)
        t = src[rs, :].astype(F32)
        inv = lax.rsqrt(jnp.mean(t * t, axis=-1, keepdims=True) + NORM_EPS)
        gd = gain[:1, :] * d
        pull = jnp.mean(gd * t, axis=-1, keepdims=True)
        dst[rs, :] = (skip[rs, :].astype(F32) + (inv * gd - t * (inv * inv * inv * pull))).astype(BF16)
        g = d * (t * inv)
        dgain[...] += g[:N_CHIP] + g[N_CHIP:]
    dgain[...] = jnp.zeros_like(dgain)
    loop(src.shape[0] // STRIP, step)


QB = 256
KB = 256


def key_rows(dst, src, lo, hd):
    def step(i):
        dst[seg(i, KB), :] = src[lo:lo + hd, seg(i, KB)].T
    loop(src.shape[1] // KB, step)


def score_block(k, q2, scale, diagonal):
    s = mm(k, q2, NN) * scale
    if diagonal:
        key = lax.broadcasted_iota(jnp.int32, s.shape, 0)
        qry = lax.broadcasted_iota(jnp.int32, s.shape, 1) % QB
        s = jnp.where(qry >= key, s, NEG_LARGE)
    return s


def side_by_side(ref, heads, hd, qs):
    return jnp.concatenate([ref[h * hd:(h + 1) * hd, qs] for h in range(heads)], axis=1)


def head(groups, hd, x_ref, small_ref, w_ref, cos_ref, sin_ref, wg_ref, wu_ref, qkv_ref, ucol_ref, small_all, w_out, ot_ref, o_ref, stat_ref, wgu_ref,
         full, acc, rot, u_scr, g_scr, wg_t, wu_t, s_scr, k_scr, osem, *sems):
    me = lax.axis_index('sp')
    tokens, dim = x_ref.shape
    cols = w_ref.shape[0]
    qw = tokens
    q_all = N_DEV * qw
    gsems, ssems, usems, qsems, ksems, gate_sems, up_sems, (osend, orecv) = sems[:4], *(sems[i:i + 2] for i in range(4, len(sems), 2))
    feat = wg_ref.shape[1] // N_DEV
    enter(me, OTHERS)
    smalls = Swap(lambda peer: small_ref, lambda o: small_all.at[o], ssems, me)
    smalls.start()
    parts = thirds(cols, STRIP)
    g = Gather(w_ref, lambda o: full.at[o // 2, :, seg(o % 2)], lambda view, c: view.at[pl.ds(*parts[c]), :], gsems, me)
    g.start()

    def own_block(i):
        full[me // 2, seg(i, WIDE), seg(me % 2)] = w_ref[seg(i, WIDE), :]
    loop(cols // WIDE, own_block)
    acc[...] = jnp.zeros_like(acc)
    small_all[me] = small_ref[...]
    smalls.wait_recv()
    gain_row(g_scr, small_all, 0)
    norm_rows(x_ref, g_scr, u_scr)
    gates = Swap(lambda peer: wg_t.at[seg(peer, feat), :], lambda o: wgu_ref.at[:feat, seg(o)], gate_sems, me)
    ups = Swap(lambda peer: wu_t.at[seg(peer, feat), :], lambda o: wgu_ref.at[feat:, seg(o)], up_sems, me)
    turns = wg_ref.shape[1] // LANE // 4

    def transpose(i):
        wg_t[seg(i), :] = wg_ref[:, seg(i)].T
        wu_t[seg(i), :] = wu_ref[:, seg(i)].T

    ucols = Swap(lambda peer: u_scr.at[:, seg(peer)], lambda o: ucol_ref.at[seg(o, tokens), :], usems, me)

    def keep(mask):
        chip = flipped(me, mask) // 2
        return pltpu.make_async_copy(full.at[chip], w_out.at[chip], osem.at[mask // 2])

    def use(mask):
        g.wait_pair(mask)
        keep(mask).start()
        chip = flipped(me, mask) // 2
        u = u_scr[:, seg(chip, WIDE)]

        def step(i):
            rs = seg(i, CHUNK)
            acc[rs, :] += mm(full[chip, rs, :], u, NT)
        loop(cols // CHUNK, step)

    for r in range(len(g.ROUNDS)):
        g.round(r)
        if r < 4:
            loop(turns, lambda i: transpose(turns * r + i))
        if r == 5:
            gates.advance(0)
            ups.advance(0)
        for mask in g.READY[r]:
            use(mask)

    half = hd // 2
    cos, sin = cos_ref[...], sin_ref[...]

    def turn(h):
        first = seg(2 * h, half)
        second = seg(2 * h + 1, half)
        p = acc[first, :].astype(BF16).astype(F32)
        q = acc[second, :].astype(BF16).astype(F32)
        rot[first, :] = (p * cos - q * sin).astype(BF16)
        rot[second, :] = (q * cos + p * sin).astype(BF16)
    loop(q_all // hd, turn)
    for k in range(groups):
        turn(q_all // hd + 2 * k)
        vs = seg(q_all // hd + 2 * k + 1, hd)
        rot[vs, :] = acc[vs, :].astype(BF16)
    per = N_DEV // groups
    q_rows = lambda peer: seg(peer, qw)
    kv_rows = lambda peer: seg(q_all // (2 * hd) + peer // per, 2 * hd)
    qs = Swap(lambda peer: rot.at[q_rows(peer), :], lambda o: qkv_ref.at[:qw, seg(o, tokens)], qsems, me)
    kvs = Swap(lambda peer: rot.at[kv_rows(peer), :], lambda o: qkv_ref.at[qw:, seg(o, tokens)], ksems, me)
    qs.start()
    kvs.start()
    qkv_ref[:qw, seg(me, tokens)] = rot[q_rows(me), :]
    qkv_ref[qw:, seg(me, tokens)] = rot[kv_rows(me), :]
    ucol_ref[seg(me, tokens), :] = u_scr[:, seg(me)]
    wgu_ref[:feat, seg(me)] = wg_t[seg(me, feat), :]
    wgu_ref[feat:, seg(me)] = wu_t[seg(me, feat), :]
    gates.start((CORE,))
    ups.start((CORE,))
    for swap in (qs, kvs):
        swap.wait_recv()
    gates.advance(1)
    ups.advance(1)
    heads = qkv_ref.shape[0] // hd - 2
    seq = qkv_ref.shape[1]
    scale = hd ** -0.5
    lanes = heads * QB
    key_rows(k_scr, qkv_ref, qw, hd)

    def o_copy(peer, origin):
        return remote(o_ref.at[:, seg(peer)], ot_ref.at[seg(origin, qw), :], osend.at[peer], orecv.at[origin], peer)

    def q_block(i):
        qb = other_chip(me // 2, N_CHIP - 1 - i)
        for at, n in ((3, 2), (6, 3)):
            @pl.when(i == at)
            def _():
                gates.advance(n)
                ups.advance(n)
        qs = seg(qb, QB)
        q2 = side_by_side(qkv_ref, heads, hd, qs)

        def scores(kb, top, diagonal):
            s = score_block(k_scr[seg(kb, KB), :], q2, scale, diagonal)
            s_scr[seg(kb, KB), :] = s
            return jnp.maximum(top, jnp.max(s, axis=0, keepdims=True))

        top = lax.fori_loop(0, qb, lambda kb, t: scores(kb, t, False), jnp.full((1, lanes), NEG_LARGE, F32))
        top = scores(qb, top, True)

        def expo(kb, tot):
            e = jnp.exp(s_scr[seg(kb, KB), :] - top)
            s_scr[seg(kb, KB), :] = e
            return tot + jnp.sum(e, axis=0, keepdims=True)

        inv = 1.0 / lax.fori_loop(0, qb + 1, expo, jnp.zeros((1, lanes), F32))

        def weigh(kb, acc):
            p = (s_scr[seg(kb, KB), :] * inv).astype(BF16)
            return acc + mm(qkv_ref[qw + hd:, seg(kb, KB)], p, NN)

        acc = lax.fori_loop(0, qb + 1, weigh, jnp.zeros((hd, lanes), F32))
        for h in range(heads):
            o_ref[h * hd:(h + 1) * hd, qs] = acc[:, h * QB:(h + 1) * QB].astype(BF16)
        stat_ref[qb, :1, :] = top
        stat_ref[qb, 1:, :] = inv
        for core in range(2):
            peer = 2 * qb + core

            @pl.when(peer != me)
            def _():
                o_copy(peer, me).start()

    loop(seq // QB, q_block)
    ot_ref[seg(me, qw), :] = o_ref[:, seg(me)]
    for mask in OTHERS:
        o_copy(me, flipped(me, mask)).wait_recv()
    ucols.start()
    for swap in (gates, ups, ucols):
        swap.wait_recv()
    for mask in CHIP_MASKS:
        keep(mask).wait()
    for mask in OTHERS:
        o_copy(flipped(me, mask), me).wait_send()
    for swap in (gates, ups):
        swap.wait_send((CORE,) + SETS[3])
    g.finish()
    for swap in (smalls, ucols, qs, kvs):
        swap.wait_send()


def mlp_local(ot_ref, wo_ref, x_ref, small_all, dout_ref, wgu_ref, down_ref, h_ref, m_out, glu_ref, dgu_ref, ddown_ref,
              full_w, full_d, full_m, acc, m_scr, g_scr, osem, *sems):
    me = lax.axis_index('sp')
    feat, dim = down_ref.shape
    enter(me, NEAR)
    gw = row_gather(wo_ref, full_w, sems[:4], me)
    gd = row_gather(dout_ref, full_d, sems[4:8], me)
    gm = row_gather(m_scr, full_m, sems[8:], me)

    def project(mask):
        gw.wait_pair(mask)
        chip = flipped(me, mask) // 2
        o = ot_ref[seg(chip, WIDE), :]

        def step(n):
            acc[:, seg(n, CHUNK)] += mm(o, full_w[chip, :, seg(n, CHUNK)], TN)
        loop(dim // CHUNK, step)

    gw.start()
    keep_own(wo_ref, full_w, me)
    keep_own(dout_ref, full_d, me)
    gain_row(g_scr, small_all, 1)
    acc[...] = jnp.zeros_like(acc)
    ddown_ref[...] = jnp.zeros_like(ddown_ref)
    for r in range(len(gw.ROUNDS)):
        gw.round(r)
        if r == 3:
            gd.start()
        for mask in gw.READY[r]:
            project(mask)

    def residual(i):
        rs = seg(i, STRIP)
        h_ref[rs, :] = (x_ref[rs, :].astype(F32) + acc[rs, :]).astype(BF16)
    loop(x_ref.shape[0] // STRIP, residual)
    norm_rows(h_ref, g_scr, m_scr)
    gm.start()
    keep_own(m_scr, full_m, me)

    def keep(mask):
        chip = flipped(me, mask) // 2
        return pltpu.make_async_copy(full_m.at[chip], m_out.at[chip], osem.at[mask // 2])

    def use(mask):
        gd.wait_pair(mask)
        gm.wait_pair(mask)
        keep(mask).start()
        chip = flipped(me, mask) // 2
        ts = seg(chip, WIDE)
        gu = mm(wgu_ref[...], full_m[chip], NT).astype(BF16).astype(F32)
        gate, up = gu[:feat], gu[feat:]
        d_glu = mm(down_ref[...], full_d[chip], NT).astype(BF16).astype(F32)
        sig = jax.nn.sigmoid(gate)
        act = gate * sig
        glu = (act * up).astype(BF16)
        glu_ref[:, ts] = glu
        dgu_ref[:feat, ts] = (d_glu * up * (sig * (1.0 + gate * (1.0 - sig)))).astype(BF16)
        dgu_ref[feat:, ts] = (d_glu * act).astype(BF16)

        def step(n):
            ddown_ref[:, seg(n, CHUNK)] += mm(glu, full_d[chip, :, seg(n, CHUNK)], NN)
        loop(dim // CHUNK, step)

    for r in range(len(gm.ROUNDS)):
        gd.round(r)
        gm.round(r)
        for mask in gm.READY[r]:
            use(mask)
    for mask in CHIP_MASKS:
        keep(mask).wait()
    for g in (gw, gd, gm):
        g.finish()


def scatter_y(a_ref, w_ref, h_ref, y_ref, *scr):
    me = lax.axis_index('sp')
    enter(me, NEAR)
    s = Scatter(*scr[:3], scr[3:], me)
    total = s.run(block_product(s.part, a_ref, w_ref))
    y_ref[...] = (h_ref[...].astype(F32) + total[...]).astype(BF16)
    s.finish()


def mlp_back(dgu_ref, wgu_ref, h_ref, small_all, dout_ref, wo_ref, o_ref, dh_ref, do_ref, dwo_ref, dg_ref,
             full, g_scr, *scr):
    me = lax.axis_index('sp')
    dim = wo_ref.shape[1]
    enter(me, NEAR)
    s = Scatter(*scr[:3], scr[3:7], me)
    g = row_gather(dh_ref, full, scr[7:], me)
    gain_row(g_scr, small_all, 1)
    dwo_ref[...] = jnp.zeros_like(dwo_ref)
    total = s.run(block_product(s.part, dgu_ref, wgu_ref))
    norm_back(total, h_ref, g_scr, dout_ref, dh_ref, dg_ref)

    def use(mask):
        g.wait_pair(mask)
        chip = flipped(me, mask) // 2
        do_ref[:, seg(chip, WIDE)] = mm(wo_ref[...], full[chip], NT).astype(BF16)
        o = o_ref[:, seg(chip, WIDE)]

        def step(n):
            dwo_ref[:, seg(n, CHUNK)] += mm(o, full[chip, :, seg(n, CHUNK)], NN)
        loop(dim // CHUNK, step)

    g.start()
    keep_own(dh_ref, full, me)
    for r in range(len(g.ROUNDS)):
        g.round(r)
        for mask in g.READY[r]:
            use(mask)
    s.finish()
    g.finish()


def back(groups, hd, qkv_ref, do_ref, stat_ref, cos_all, sin_all, dgu_ref, m_ref, ucol_ref, cos_ref, sin_ref, w_hbm, x_ref, small_all, dh_ref, dg2_ref,
         dg_hbm, du_hbm, dwq_ref, dwkv_ref, dx_ref, gain_ref,
         p_scr, dp_scr, k_scr, v_scr, dk_acc, dv_acc, stage, dq_scr, dkv_scr,
         full, w_scr, shares, dkv_own, full_kv, dqkv, dn, g_scr, dg1, gains, gains_in, wsem, lsem, *sems):
    heads = qkv_ref.shape[0] // hd - 2
    seq = qkv_ref.shape[1]
    scale = hd ** -0.5
    lanes = heads * QB
    qw = heads * hd
    half = hd // 2
    me = lax.axis_index('sp')
    feat = dgu_ref.shape[0] // 2
    enter(me, OTHERS)
    load = pltpu.make_async_copy(w_hbm, w_scr, wsem)
    load.start()
    gain_row(g_scr, small_all, 0)

    def piece(lo):
        return lambda peer: stage.at[peer // 2, lo:lo + feat, seg(peer % 2)]
    gates = Swap(piece(0), lambda o: dg_hbm.at[seg(o, feat), :], sems[:2], me)
    ups = Swap(piece(feat), lambda o: du_hbm.at[seg(o, feat), :], sems[2:4], me)
    own = [pltpu.make_async_copy(swap.src(me), swap.dst(me), lsem.at[i]) for i, swap in enumerate((gates, ups))]

    def make(mask):
        chip = flipped(me, mask) // 2
        cols = m_ref[:, :, seg(chip, WIDE)].reshape(seq, WIDE)
        stage[chip] = mm(dgu_ref[...], cols, NN)

    def advance(n):
        gates.advance(n)
        ups.advance(n)

    make(XYZ)
    make(X)
    advance(0)
    for mask in (Y + Z, Y, X + Z, Z, X + Y, 0):
        make(mask)
    gates.start((CORE,))
    ups.start((CORE,))
    for copy in own:
        copy.start()

    dk_acc[...] = jnp.zeros_like(dk_acc)
    dv_acc[...] = jnp.zeros_like(dv_acc)
    key_rows(k_scr, qkv_ref, qw, hd)
    key_rows(v_scr, qkv_ref, qw + hd, hd)

    def q_block(qb):
        for at, n in ((4, 1), (7, 2)):
            @pl.when(qb == at)
            def _():
                advance(n)
        qs = seg(qb, QB)
        q2 = side_by_side(qkv_ref, heads, hd, qs)
        do2 = side_by_side(do_ref, heads, hd, qs)
        top = stat_ref[qb, :1, :]
        inv = stat_ref[qb, 1:, :]

        def probs(kb, rd, diagonal):
            ks = seg(kb, KB)
            s = score_block(k_scr[ks, :], q2, scale, diagonal)
            p = jnp.exp(s - top) * inv
            dp = mm(v_scr[ks, :], do2, NN).astype(BF16)
            p_scr[ks, :] = p
            dp_scr[ks, :] = dp
            dv_acc[ks, :] += mm(p.astype(BF16), do2, NT)
            return rd + jnp.sum(dp.astype(F32) * p, axis=0, keepdims=True)

        rd = lax.fori_loop(0, qb, lambda kb, r: probs(kb, r, False), jnp.zeros((1, lanes), F32))
        rd = probs(qb, rd, True)

        def d_scores(kb, acc):
            ks = seg(kb, KB)
            ds = (p_scr[ks, :] * (dp_scr[ks, :].astype(F32) - rd) * scale).astype(BF16)
            dk_acc[ks, :] += mm(ds, q2, NT)
            return acc + mm(qkv_ref[qw:qw + hd, ks], ds, NN)

        acc = lax.fori_loop(0, qb + 1, d_scores, jnp.zeros((hd, lanes), F32))
        cos, sin = cos_all[:, qs], sin_all[:, qs]
        for h in range(heads):
            dq = acc[:, h * QB:(h + 1) * QB].astype(BF16).astype(F32)
            p, q = dq[:half], dq[half:]
            dq_scr[h * hd:h * hd + half, qs] = (p * cos + q * sin).astype(BF16)
            dq_scr[h * hd + half:(h + 1) * hd, qs] = (q * cos - p * sin).astype(BF16)

    loop(seq // QB, q_block)

    def share(i):
        rs = seg(i, WIDE)
        dkv_scr[rs, :] = jnp.concatenate([dk_acc[rs, :], dv_acc[rs, :]], axis=1).astype(BF16)
    loop(seq // WIDE, share)
    tokens = ucol_ref.shape[1]
    per = N_DEV // groups
    q_all = dwq_ref.shape[0]
    sh = Swap(lambda peer: dkv_scr.at[seg(peer, tokens), :], lambda o: shares.at[o], sems[4:6], me)
    gq = row_gather(dq_scr, full, sems[6:10], me)
    parts = thirds(dkv_own.shape[0], STRIP)
    gk = Gather(dkv_own, lambda o: full_kv.at[:, seg(o, tokens)], lambda view, c: view.at[pl.ds(*parts[c]), :], sems[10:14], me)
    gs = Swap(lambda peer: gains.at[:, seg(peer)], lambda o: gains_in.at[o], sems[14:], me)
    sh.start()
    gq.start()
    keep_own(dq_scr, full, me)
    shares[me] = dkv_scr[seg(me, tokens), :]
    sh.wait_recv()
    cos, sin = cos_ref[...], sin_ref[...]
    for k in range(groups):
        both = sum(shares[per * k + i].astype(F32) for i in range(per)).astype(BF16).astype(F32).T
        p, q = both[:half], both[half:hd]
        lo = 2 * hd * k
        dkv_own[lo:lo + half, :] = (p * cos + q * sin).astype(BF16)
        dkv_own[lo + half:lo + hd, :] = (q * cos - p * sin).astype(BF16)
        dkv_own[lo + hd:lo + 2 * hd, :] = both[hd:].astype(BF16)
    gk.start()
    full_kv[:, seg(me, tokens)] = dkv_own[...]
    dqkv[q_all:, :] = dkv_own[...]

    def use(mask):
        gq.wait_pair(mask)
        chip = flipped(me, mask) // 2
        dwq_ref[seg(chip, WIDE), :] = mm(full[chip], ucol_ref[...], NN)
        dqkv[seg(chip, WIDE), :] = full[chip, :, seg(me, tokens)]

    for r in range(len(gq.ROUNDS)):
        gq.round(r)
        gk.round(r)
        if r == 3:
            advance(3)
        for mask in gq.READY[r]:
            use(mask)
    load.wait()

    def normed(i):
        dn[:, seg(i, WIDE)] = mm(dqkv[...], w_scr[i], TN)
    loop(N_CHIP, normed)
    norm_back(dn, x_ref, g_scr, dh_ref, dx_ref, dg1)
    gains[...] = jnp.concatenate([jnp.sum(dg1[...], axis=0, keepdims=True), jnp.sum(dg2_ref[...], axis=0, keepdims=True),
                                  jnp.zeros((N_CHIP - 2, dg1.shape[1]), F32)], axis=0)
    gs.start()
    gains_in[me] = gains[:, seg(me)]
    for mask in CHIP_MASKS:
        gk.wait_pair(mask)
    dwkv_ref[...] = mm(full_kv[...], ucol_ref[...], NN)
    gs.wait_recv()
    gain_ref[...] = sum(gains_in[o] for o in range(N_DEV))
    for swap in (gates, ups):
        swap.wait_recv()
        swap.wait_send((CORE,) + SETS[3])
    for copy in own:
        copy.wait()
    for c in (sh, gs):
        c.wait_send()
    for g in (gq, gk):
        g.finish()


def rope_tables(positions, head_dim):
    half_dim = head_dim // 2
    inv_freq = 1.0 / (ROPE_BASE ** (jnp.arange(half_dim, dtype=F32) * (2.0 / head_dim)))
    angles = positions.astype(F32)[None, :] * inv_freq[:, None]
    return jnp.cos(angles), jnp.sin(angles)


def solution(mesh):
    assert mesh.shape['sp'] == N_DEV

    def layer_step(x_in, positions, d_out, norm1_gain, norm2_gain, w_q, w_k, w_v, w_o, w_gate, w_up, w_down):
        tokens, dim = x_in.shape
        seq = tokens * N_DEV
        n_q, hd = w_q.shape[1:]
        n_kv = w_k.shape[1]
        qw = n_q // N_DEV * hd
        rows = w_q.shape[0]
        feat = w_down.shape[0]
        cols = (n_q + 2 * n_kv) * hd
        lanes = qw // hd * QB
        vm = pltpu.VMEM
        full = vm((N_CHIP, WIDE, dim), BF16)
        gain_scr = vm((N_CHIP, dim), F32)
        small_shape = ((N_DEV, N_CHIP, rows), F32)

        small = jnp.stack([norm1_gain.astype(F32), norm2_gain.astype(F32), positions.astype(F32)])
        small = jnp.pad(small, ((0, N_CHIP - small.shape[0]), (0, 0)))
        cos_own, sin_own = rope_tables(positions, hd)
        wq_t = w_q.transpose(1, 2, 0).reshape(n_q * hd, rows)
        wkv_t = jnp.stack([w_k.transpose(1, 2, 0), w_v.transpose(1, 2, 0)], axis=1).reshape(2 * n_kv * hd, rows)
        wo_own = w_o.reshape(qw, dim)

        qkv, u_col, small_all, wqkv, attn_tok, attn_t, stat, wgu = call(
            functools.partial(head, n_kv, hd), 0,
            (x_in, small, jnp.concatenate([wq_t, wkv_t], axis=0), cos_own, sin_own, w_gate, w_up),
            (((qw + 2 * hd, seq), BF16), ((seq, rows), BF16), small_shape, ((N_CHIP, cols, WIDE), BF16),
             ((n_q * hd, tokens), BF16), ((qw, seq), BF16), ((seq // QB, 2, lanes), F32), ((2 * feat, dim), BF16)),
            [vm((N_CHIP, cols, WIDE), BF16), vm((cols, tokens), F32), vm((cols, tokens), BF16), vm((tokens, dim), BF16), gain_scr,
             vm((feat * N_DEV, rows), BF16), vm((feat * N_DEV, rows), BF16), vm((seq, lanes), F32), vm((seq, hd), BF16), dma(N_CHIP),
             *Gather.sems, *(7 * Swap.sems)], 4 * qw * seq * seq, far_out=(3,))
        hidden, m_full, glu, dgu, d_down = call(
            mlp_local, 2, (attn_tok, wo_own, x_in, small_all, d_out, wgu, w_down),
            (((tokens, dim), BF16), ((N_CHIP, WIDE, dim), BF16), ((feat, seq), BF16), ((2 * feat, seq), BF16), ((feat, dim), F32)),
            [full, full, full, vm((tokens, dim), F32), vm((tokens, dim), BF16), gain_scr, dma(N_CHIP), *(3 * Gather.sems)],
            8 * feat * seq * dim, far_out=(1,))
        d_hidden, d_attn, d_wo, d_g2 = call(
            mlp_back, 3, (dgu, wgu, hidden, small_all, d_out, wo_own, attn_t),
            (((tokens, dim), BF16), ((qw, seq), BF16), ((qw, dim), F32), ((N_CHIP, dim), F32)),
            [full, gain_scr, *Scatter.scratch(tokens, dim), *Scatter.sems, *Gather.sems], 4 * feat * seq * dim)
        cos_all, sin_all = rope_tables(small_all[:, 2].reshape(-1), hd)
        d_gate_t, d_up_t, d_wq, d_wkv, d_x, gains = call(
            functools.partial(back, n_kv, hd), 4,
            (qkv, d_attn, stat, cos_all, sin_all, dgu, m_full, u_col, cos_own, sin_own, wqkv, x_in, small_all, d_hidden, d_g2),
            (((feat * N_DEV, rows), F32), ((feat * N_DEV, rows), F32),
             ((n_q * hd, rows), F32), ((2 * n_kv * hd, rows), F32), ((tokens, dim), BF16), ((N_CHIP, rows), F32)),
            [vm((seq, lanes), F32), vm((seq, lanes), BF16), vm((seq, hd), BF16), vm((seq, hd), BF16), vm((seq, hd), F32), vm((seq, hd), F32),
             vm((N_CHIP, 2 * feat, WIDE), F32), vm((qw, seq), BF16), vm((seq, 2 * hd), BF16),
             full, vm((N_CHIP, cols, WIDE), BF16), vm((N_DEV, tokens, 2 * hd), BF16), vm((2 * n_kv * hd, tokens), BF16), vm((2 * n_kv * hd, seq), BF16),
             vm((cols, tokens), BF16), vm((tokens, dim), F32), gain_scr, gain_scr, gain_scr, vm((N_DEV, N_CHIP, rows), F32), dma(), dma(2),
             *(3 * Swap.sems), *(2 * Gather.sems), *Swap.sems], 10 * qw * seq * seq, far_in=(10,), far_out=(0, 1))
        y_out, = call(scatter_y, 5, (glu, w_down, hidden), (((tokens, dim), BF16),),
                      [*Scatter.scratch(tokens, dim), *Scatter.sems], 2 * feat * seq * dim)

        d_wkv = d_wkv.reshape(n_kv, 2, hd, rows).transpose(3, 0, 2, 1)
        return (y_out, d_x, gains[0], gains[1], d_wq.reshape(n_q, hd, rows).transpose(2, 0, 1), d_wkv[..., 0], d_wkv[..., 1],
                d_wo.reshape(w_o.shape), d_gate_t.T, d_up_t.T, d_down)

    all_rows = P('sp')
    return jax.shard_map(layer_step, mesh=mesh, in_specs=(all_rows,) * 12, out_specs=(all_rows,) * 11, check_vma=False)
```

```python
import functools
import jax
import jax.numpy as jnp
from jax import lax
from jax.experimental import pallas as pl
from jax.experimental.pallas import tpu as pltpu
from jax.sharding import PartitionSpec as P

ROPE_BASE = 10000.0
NORM_EPS = 1e-5
NEG_LARGE = -1e30
F32 = jnp.float32
BF16 = jnp.bfloat16
N_DEV, N_CHIP, LANE, WIDE, CHUNK, STRIP = 16, 8, 128, 256, 512, 16
NT = (((1,), (1,)), ((), ()))
TN = (((0,), (0,)), ((), ()))
NN = (((1,), (0,)), ((), ()))
MESH = pl.DeviceIdType.MESH
VMEM_CAP = 62 * 1024 * 1024

CORE, X, Y, Z = 1, 2, 4, 8
XYZ = X + Y + Z
ORDERS = ((X, Y, Z), (Y, Z, X), (Z, X, Y))
CHIP_MASKS = (0, X, Y, Z, X + Y, X + Z, Y + Z, XYZ)
NEAR = (CORE, X, Y, Z)
OTHERS = range(1, N_DEV)
SETS = tuple(tuple(m + c for m in masks for c in (0, CORE)) for masks in ((XYZ,), (X, Y + Z), (Y, X + Z), (Z, X + Y)))
COLOURS = range(len(ORDERS))


def mm(a, b, dims):
    return lax.dot_general(a, b, dims, preferred_element_type=F32)


def seg(index, width=LANE):
    return pl.ds(pl.multiple_of(index * width, width), width)


def loop(count, body):
    lax.fori_loop(0, count, lambda i, c: (body(i), c)[1], 0)


def flipped(index, mask):
    out = index
    for bit in NEAR:
        if mask & bit:
            out = out + (1 - 2 * ((index // bit) % 2)) * bit
    return out


def thirds(total, unit):
    n = total // unit
    first = (n + 2) // 3
    second = (n - first + 1) // 2
    sizes = (first * unit, second * unit, (n - first - second) * unit)
    return ((0, sizes[0]), (sizes[0], sizes[1]), (sizes[0] + sizes[1], sizes[2]))


def pieces(rows, cols, unit):
    share = cols // LANE // 3 * LANE
    strips = thirds(rows, unit)
    rest = cols - 3 * share
    return [[(pl.ds(0, rows), pl.ds(c * share, share)), (pl.ds(*strips[c]), pl.ds(3 * share, rest))] for c in COLOURS]


def enter(me, masks):
    barrier = pltpu.get_barrier_semaphore()
    for mask in masks:
        pl.semaphore_signal(barrier, inc=1, device_id=(flipped(me, mask),), device_id_type=MESH)
    pl.semaphore_wait(barrier, len(masks))


def remote(src, dst, send, recv, peer):
    return pltpu.make_async_remote_copy(src_ref=src, dst_ref=dst, send_sem=send, recv_sem=recv, device_id=(peer,), device_id_type=MESH)


def dma(*shape):
    return pltpu.SemaphoreType.DMA(shape)


class Swap:
    sems = (dma(N_DEV), dma(N_DEV))

    def __init__(self, src, dst, sems, me):
        self.src, self.dst, (self.send, self.recv), self.me = src, dst, sems, me

    def copy(self, mask):
        peer = flipped(self.me, mask)
        return remote(self.src(peer), self.dst(self.me), self.send.at[mask], self.recv.at[mask], peer)

    def start(self, masks=OTHERS):
        for mask in masks:
            self.copy(mask).start()

    def advance(self, n):
        if n:
            for mask in SETS[n - 1]:
                self.copy(mask).wait_send()
        self.start(SETS[n])

    def wait_recv(self):
        for mask in OTHERS:
            view = self.dst(flipped(self.me, mask))
            remote(view, view, self.send.at[mask], self.recv.at[mask], self.me).wait_recv()

    def wait_send(self, masks=OTHERS):
        for mask in masks:
            self.copy(mask).wait_send()


class Gather:
    ROUNDS = ((0,), (1,), (2,), (0, 1), (0, 2), (1, 2), (0, 1, 2))
    READY = ((0,), (), (), (X, Y), (Z,), (X + Y, X + Z), (Y + Z, XYZ))
    sems = (dma(3, N_CHIP, 3, 2), dma(3, N_CHIP, 2), dma(N_CHIP), dma(N_CHIP))

    def __init__(self, own, block, cut, sems, me):
        self.own, self.block, self.cut, self.me = own, block, cut, me
        self.send, self.recv, self.pair_send, self.pair_recv = sems

    def source(self, mask):
        return self.block(flipped(self.me, mask)) if mask else self.own

    def unit(self, colour, mask, axis):
        ends = zip(self.cut(self.source(mask), colour), self.cut(self.block(flipped(self.me, mask)), colour))
        return [remote(src, dst, self.send.at[colour, mask // 2, ORDERS[colour].index(axis), i], self.recv.at[colour, (mask + axis) // 2, i],
                       flipped(self.me, axis)) for i, (src, dst) in enumerate(ends)]

    def start_unit(self, colour, mask, axis):
        for copy in self.unit(colour, mask, axis):
            copy.start()

    def pair(self, mask):
        return remote(self.source(mask), self.block(flipped(self.me, mask)), self.pair_send.at[mask // 2],
                      self.pair_recv.at[mask // 2], flipped(self.me, CORE))

    def wait_pair(self, mask):
        view = self.block(flipped(self.me, mask + CORE))
        remote(view, view, self.pair_send.at[mask // 2], self.pair_recv.at[mask // 2], self.me).wait_recv()

    def onward(self, colour):
        order = ORDERS[colour]
        for picks in self.ROUNDS:
            for axis in order[picks[-1] + 1:]:
                yield picks, sum(order[p] for p in picks), axis

    def start(self):
        for pos in COLOURS:
            for colour in COLOURS:
                self.start_unit(colour, 0, ORDERS[colour][pos])
        self.pair(0).start()

    def round(self, r):
        for colour in COLOURS:
            mask = sum(ORDERS[colour][p] for p in self.ROUNDS[r])
            for i, view in enumerate(self.cut(self.block(flipped(self.me, mask)), colour)):
                remote(view, view, self.send.at[colour, 0, 0, i], self.recv.at[colour, mask // 2, i], self.me).wait_recv()
            for picks, at, axis in self.onward(colour):
                if picks == self.ROUNDS[r]:
                    self.start_unit(colour, at, axis)
        for mask in {2: (X, Y, Z), 5: (X + Y, X + Z, Y + Z), 6: (XYZ,)}.get(r, ()):
            self.pair(mask).start()

    def finish(self):
        for colour in COLOURS:
            for at, axis in [(0, axis) for axis in ORDERS[colour]] + [step[1:] for step in self.onward(colour)]:
                for copy in self.unit(colour, at, axis):
                    copy.wait_send()
        for mask in CHIP_MASKS:
            self.pair(mask).wait_send()


def row_gather(own, full, sems, me, extra=None):
    rows, width = own.shape
    parts = pieces(rows, width, STRIP)
    if extra is not None:
        share = width // LANE // 3 * LANE
        more = width - 3 * share
        parts = [[(pl.ds(0, rows), pl.ds(c * share + more * (c > extra), share + more * (c == extra)))] for c in COLOURS]

    def block(o):
        return full.at[o // 2, seg(o % 2), :]

    return Gather(own, block, lambda view, c: [view.at[rs, cs] for rs, cs in parts[c]], sems, me)


def keep_own(own, full, me):
    def step(i):
        full[me // 2, pl.ds(pl.multiple_of((me % 2) * LANE + i * STRIP, STRIP), STRIP), :] = own[seg(i, STRIP), :]
    loop(LANE // STRIP, step)


class Scatter:
    ORDER = (XYZ, X + Y, Y + Z, X + Z, X, Y, Z, 0)
    sems = (dma(N_CHIP), dma(N_CHIP), dma(3, N_CHIP, 2), dma(3, N_CHIP, 2))

    @staticmethod
    def scratch(tokens, dim):
        return [pltpu.VMEM((N_CHIP, 2, tokens, dim), F32), pltpu.VMEM((N_CHIP, tokens, dim), F32), pltpu.VMEM((N_CHIP - 1, tokens, dim), F32)]

    def __init__(self, part, pair_in, link_in, sems, me):
        self.part, self.pair_in, self.link_in, self.me = part, pair_in, link_in, me
        self.pair_send, self.pair_recv, self.link_send, self.link_recv = sems
        self.core = me % 2
        self.tokens, self.dim = part.shape[2:]
        self.pieces = pieces(self.tokens, self.dim, STRIP // 2)
        self.ready, self.sent = set(), [0] * len(ORDERS)

    @staticmethod
    def first(colour, mask):
        return next((i for i, a in enumerate(ORDERS[colour]) if mask & a), 3)

    def slot(self, colour, mask, axis):
        slots = [(m, a) for m in self.ORDER for a in ORDERS[colour][:self.first(colour, m)]]
        return slots.index((mask, axis))

    def pair(self, i):
        return remote(self.part.at[i, 1 - self.core], self.pair_in.at[i], self.pair_send.at[i], self.pair_recv.at[i], flipped(self.me, CORE))

    def link(self, colour, mask):
        axis = ORDERS[colour][self.first(colour, mask)]
        slot = self.slot(colour, mask - axis, axis)
        i = self.ORDER.index(mask)
        return [remote(self.part.at[i, self.core, rs, cs], self.link_in.at[slot, rs, cs], self.link_send.at[colour, i, k],
                       self.link_recv.at[colour, slot, k], flipped(self.me, axis)) for k, (rs, cs) in enumerate(self.pieces[colour])]

    def start_link(self, colour, mask):
        for copy in self.link(colour, mask):
            copy.start()

    def add(self, mask, ref, cs):
        i = self.ORDER.index(mask)

        def step(r):
            rs = seg(r, STRIP)
            self.part[i, self.core, rs, cs] += ref[rs, cs]
        loop(self.tokens // STRIP, step)

    def finish_pair(self, i):
        self.pair(i).wait_recv()
        self.add(self.ORDER[i], self.pair_in.at[i], pl.ds(0, self.dim))
        self.ready.add(self.ORDER[i])
        for colour in COLOURS:
            a, b, c = ORDERS[colour]
            todo = (XYZ, a + b, a + c, a)
            while self.sent[colour] < len(todo) and todo[self.sent[colour]] in self.ready:
                self.start_link(colour, todo[self.sent[colour]])
                self.sent[colour] += 1

    def take(self, colour, mask, axis):
        for copy in self.link(colour, mask + axis):
            copy.wait_recv()
        ref = self.link_in.at[self.slot(colour, mask, axis)]
        (_, wide), (rs, cs) = self.pieces[colour]
        self.add(mask, ref, wide)
        self.part[self.ORDER.index(mask), self.core, rs, cs] += ref[rs, cs]

    def run(self, product, between=lambda i: None):
        for i, mask in enumerate(self.ORDER):
            product(i, flipped(self.me, mask) // 2)
            self.pair(i).start()
            if i:
                self.finish_pair(i - 1)
            between(i)
        self.finish_pair(N_CHIP - 1)
        for step in range(2):
            for colour in COLOURS:
                a, b, c = ORDERS[colour]
                mask = (b + c, b)[step]
                self.take(colour, mask, a)
                self.start_link(colour, mask)
        for colour in COLOURS:
            a, b, c = ORDERS[colour]
            self.take(colour, c, a)
            self.take(colour, c, b)
            self.start_link(colour, c)
        for colour in COLOURS:
            for axis in ORDERS[colour]:
                self.take(colour, 0, axis)
        return self.part.at[N_CHIP - 1, self.core]

    def finish(self):
        for i in range(N_CHIP):
            self.pair(i).wait_send()
        for colour in COLOURS:
            for mask in self.ORDER[:-1]:
                for copy in self.link(colour, mask):
                    copy.wait_send()


def block_product(part, a_ref, w_ref, a_t):
    tokens = part.shape[2]

    def product(i, chip):
        a_t[...] = a_ref[:, seg(chip, 2 * tokens)].T

        def step(n):
            cs = seg(n, CHUNK)
            r = mm(a_t[...], w_ref[:, cs], NN)
            part[i, 0, :, cs] = r[:tokens]
            part[i, 1, :, cs] = r[tokens:]
        loop(part.shape[3] // CHUNK, step)
    return product


def on_chip(n):
    return [pl.BlockSpec(memory_space=pltpu.VMEM)] * n


IN_HBM = pl.BlockSpec(memory_space=pl.ANY)


def call(kernel, ident, args, outs, scratch, flops, far_in=(), far_out=()):
    specs = [IN_HBM if i in far_in else on_chip(1)[0] for i in range(args)]
    out_specs = [IN_HBM if i in far_out else on_chip(1)[0] for i in range(len(outs))]
    return pl.pallas_call(
        kernel,
        out_shape=[jax.ShapeDtypeStruct(shape, dtype) for shape, dtype in outs],
        in_specs=specs, out_specs=out_specs, scratch_shapes=scratch,
        cost_estimate=pl.CostEstimate(flops=flops, bytes_accessed=flops // CHUNK, transcendentals=0),
        compiler_params=pltpu.CompilerParams(collective_id=ident, has_side_effects=True, vmem_limit_bytes=VMEM_CAP),
        name=kernel.func.__name__ if isinstance(kernel, functools.partial) else kernel.__name__,
    )


def gain_row(dst, small_all, which):
    for o in range(N_DEV):
        dst[:1, o * LANE:(o + 1) * LANE] = small_all[o, which:which + 1, :]


def norm_rows(src, gain, dst):
    def step(i):
        rs = seg(i, STRIP)
        t = src[rs, :].astype(F32)
        dst[rs, :] = (t * lax.rsqrt(jnp.mean(t * t, axis=-1, keepdims=True) + NORM_EPS) * gain[:1, :]).astype(BF16)
    loop(src.shape[0] // STRIP, step)


def norm_back(dy, src, gain, skip, dst, dgain):
    def step(i):
        rs = seg(i, STRIP)
        d = dy[rs, :].astype(BF16).astype(F32)
        t = src[rs, :].astype(F32)
        inv = lax.rsqrt(jnp.mean(t * t, axis=-1, keepdims=True) + NORM_EPS)
        gd = gain[:1, :] * d
        pull = jnp.mean(gd * t, axis=-1, keepdims=True)
        dst[rs, :] = (skip[rs, :].astype(F32) + (inv * gd - t * (inv * inv * inv * pull))).astype(BF16)
        g = d * (t * inv)
        dgain[...] += g[:N_CHIP] + g[N_CHIP:]
    dgain[...] = jnp.zeros_like(dgain)
    loop(src.shape[0] // STRIP, step)


QB = 256
KB = 256


def key_rows(dst, src, lo, hd):
    def step(i):
        dst[seg(i, KB), :] = src[lo:lo + hd, seg(i, KB)].T
    loop(src.shape[1] // KB, step)


def score_block(k, q2, scale, diagonal):
    s = mm(k, q2, NN) * scale
    if diagonal:
        key = lax.broadcasted_iota(jnp.int32, s.shape, 0)
        qry = lax.broadcasted_iota(jnp.int32, s.shape, 1) % QB
        s = jnp.where(qry >= key, s, NEG_LARGE)
    return s


def side_by_side(ref, heads, hd, qs):
    return jnp.concatenate([ref[h * hd:(h + 1) * hd, qs] for h in range(heads)], axis=1)


def head(groups, hd, x_ref, g1_ref, g2_ref, pos_ref, wq_ref, wk_ref, wv_ref, cos_ref, sin_ref, wg_ref, wu_ref, qkv_ref, ucol_ref, small_all, w_out, ot_ref, o_ref, stat_ref, wgu_ref,
         small_ref, w_ref, full, acc, rot, u_scr, g_scr, wg_t, wu_t, s_scr, k_scr, osem, *sems):
    me = lax.axis_index('sp')
    tokens, dim = x_ref.shape
    cols = w_ref.shape[0]
    small_ref[...] = jnp.concatenate([r[...].astype(F32) for r in (g1_ref, g2_ref, pos_ref)] + [jnp.zeros((N_CHIP - 3, LANE), F32)], axis=0)
    w_ref[:wq_ref.shape[0], :] = wq_ref[...]
    for k in range(groups):
        for i, ref in enumerate((wk_ref, wv_ref)):
            w_ref[pl.ds(wq_ref.shape[0] + (2 * k + i) * hd, hd), :] = ref[k * hd:(k + 1) * hd, :]
    qw = tokens
    q_all = N_DEV * qw
    gsems, ssems, usems, qsems, ksems, gate_sems, up_sems, (osend, orecv) = sems[:4], *(sems[i:i + 2] for i in range(4, len(sems), 2))
    feat = wg_ref.shape[1] // N_DEV
    enter(me, OTHERS)
    smalls = Swap(lambda peer: small_ref, lambda o: small_all.at[o], ssems, me)
    smalls.start()
    parts = thirds(cols, STRIP)
    g = Gather(w_ref, lambda o: full.at[o // 2, :, seg(o % 2)], lambda view, c: [view.at[pl.ds(*parts[c]), :]], gsems, me)
    g.start()

    def own_block(i):
        full[me // 2, seg(i, WIDE), seg(me % 2)] = w_ref[seg(i, WIDE), :]
    loop(cols // WIDE, own_block)
    acc[...] = jnp.zeros_like(acc)
    small_all[me] = small_ref[...]
    smalls.wait_recv()
    gain_row(g_scr, small_all, 0)
    norm_rows(x_ref, g_scr, u_scr)
    gates = Swap(lambda peer: wg_t.at[seg(peer, feat), :], lambda o: wgu_ref.at[:feat, seg(o)], gate_sems, me)
    ups = Swap(lambda peer: wu_t.at[seg(peer, feat), :], lambda o: wgu_ref.at[feat:, seg(o)], up_sems, me)
    turns = wg_ref.shape[1] // LANE // 4

    def transpose(i):
        wg_t[seg(i), :] = wg_ref[:, seg(i)].T
        wu_t[seg(i), :] = wu_ref[:, seg(i)].T

    ucols = Swap(lambda peer: u_scr.at[:, seg(peer)], lambda o: ucol_ref.at[seg(o, tokens), :], usems, me)

    def keep(mask):
        chip = flipped(me, mask) // 2
        return pltpu.make_async_copy(full.at[chip], w_out.at[chip], osem.at[mask // 2])

    def use(mask):
        g.wait_pair(mask)
        keep(mask).start()
        chip = flipped(me, mask) // 2
        u = u_scr[:, seg(chip, WIDE)]

        def step(i):
            rs = seg(i, cols // 2)
            acc[rs, :] += mm(full[chip, rs, :], u, NT)
        loop(2, step)

    for r in range(len(g.ROUNDS)):
        g.round(r)
        if r < 4:
            loop(turns, lambda i: transpose(turns * r + i))
        if r == 3:
            ucols.start()
        for mask in g.READY[r]:
            use(mask)

    half = hd // 2
    cos, sin = cos_ref[...], sin_ref[...]

    def turn(h):
        first = seg(2 * h, half)
        second = seg(2 * h + 1, half)
        p = acc[first, :].astype(BF16).astype(F32)
        q = acc[second, :].astype(BF16).astype(F32)
        rot[first, :] = (p * cos - q * sin).astype(BF16)
        rot[second, :] = (q * cos + p * sin).astype(BF16)
    loop(q_all // hd, turn)
    for k in range(groups):
        turn(q_all // hd + 2 * k)
        vs = seg(q_all // hd + 2 * k + 1, hd)
        rot[vs, :] = acc[vs, :].astype(BF16)
    per = N_DEV // groups
    q_rows = lambda peer: seg(peer, qw)
    kv_rows = lambda peer: seg(q_all // (2 * hd) + peer // per, 2 * hd)
    qs = Swap(lambda peer: rot.at[q_rows(peer), :], lambda o: qkv_ref.at[:qw, seg(o, tokens)], qsems, me)
    kvs = Swap(lambda peer: rot.at[kv_rows(peer), :], lambda o: qkv_ref.at[qw:, seg(o, tokens)], ksems, me)
    qs.start()
    kvs.start()
    gates.advance(0)
    ups.advance(0)
    qkv_ref[:qw, seg(me, tokens)] = rot[q_rows(me), :]
    qkv_ref[qw:, seg(me, tokens)] = rot[kv_rows(me), :]
    ucol_ref[seg(me, tokens), :] = u_scr[:, seg(me)]
    wgu_ref[:feat, seg(me)] = wg_t[seg(me, feat), :]
    wgu_ref[feat:, seg(me)] = wu_t[seg(me, feat), :]
    gates.start((CORE,))
    ups.start((CORE,))
    for swap in (qs, kvs):
        swap.wait_recv()
    heads = qkv_ref.shape[0] // hd - 2
    seq = qkv_ref.shape[1]
    scale = hd ** -0.5
    lanes = heads * QB
    key_rows(k_scr, qkv_ref, qw, hd)

    def o_copy(peer, origin):
        return remote(o_ref.at[:, seg(peer)], ot_ref.at[seg(origin, qw), :], osend.at[peer], orecv.at[origin], peer)

    def q_block(qb):
        for at, n in ((5, 1), (7, 2)):
            @pl.when(qb == at)
            def _():
                gates.advance(n)
                ups.advance(n)
        qs = seg(qb, QB)
        q2 = side_by_side(qkv_ref, heads, hd, qs)

        def scores(kb, top, diagonal):
            s = score_block(k_scr[seg(kb, KB), :], q2, scale, diagonal)
            s_scr[seg(kb, KB), :] = s
            return jnp.maximum(top, jnp.max(s, axis=0, keepdims=True))

        top = lax.fori_loop(0, qb, lambda kb, t: scores(kb, t, False), jnp.full((1, lanes), NEG_LARGE, F32))
        top = scores(qb, top, True)

        def expo(kb, tot):
            e = jnp.exp(s_scr[seg(kb, KB), :] - top)
            s_scr[seg(kb, KB), :] = e
            return tot + jnp.sum(e, axis=0, keepdims=True)

        inv = 1.0 / lax.fori_loop(0, qb + 1, expo, jnp.zeros((1, lanes), F32))

        def weigh(kb, acc):
            p = (s_scr[seg(kb, KB), :] * inv).astype(BF16)
            return acc + mm(qkv_ref[qw + hd:, seg(kb, KB)], p, NN)

        acc = lax.fori_loop(0, qb + 1, weigh, jnp.zeros((hd, lanes), F32))
        for h in range(heads):
            o_ref[h * hd:(h + 1) * hd, qs] = acc[:, h * QB:(h + 1) * QB].astype(BF16)
        stat_ref[qb, :1, :] = top
        stat_ref[qb, 1:, :] = inv
        for core in range(2):
            peer = 2 * qb + core

            @pl.when(peer != me)
            def _():
                o_copy(peer, me).start()

    loop(seq // QB, q_block)
    gates.advance(3)
    ups.advance(3)
    ot_ref[seg(me, qw), :] = o_ref[:, seg(me)]
    for mask in OTHERS:
        o_copy(me, flipped(me, mask)).wait_recv()
    for swap in (gates, ups, ucols):
        swap.wait_recv()
    for mask in CHIP_MASKS:
        keep(mask).wait()
    for mask in OTHERS:
        o_copy(flipped(me, mask), me).wait_send()
    for swap in (gates, ups):
        swap.wait_send((CORE,) + SETS[3])
    g.finish()
    for swap in (smalls, ucols, qs, kvs):
        swap.wait_send()


def mlp_local(ot_ref, wo_ref, x_ref, small_all, dout_ref, wgu_ref, down_ref, h_ref, m_out, glu_ref, dgu_ref, ddown_ref,
              full_w, full_d, full_m, acc, m_scr, o_scr, g_scr, osem, *sems):
    me = lax.axis_index('sp')
    feat, dim = down_ref.shape
    enter(me, NEAR)
    gw = row_gather(wo_ref, full_w, sems[:4], me, 0)
    gd = row_gather(dout_ref, full_d, sems[4:8], me, 1)
    gm = row_gather(m_scr, full_m, sems[8:], me, 2)

    def project(mask):
        gw.wait_pair(mask)
        chip = flipped(me, mask) // 2
        o = o_scr[:, seg(chip, WIDE)]

        def step(n):
            acc[:, seg(n, CHUNK)] += mm(o, full_w[chip, :, seg(n, CHUNK)], NN)
        loop(dim // CHUNK, step)

    gw.start()
    keep_own(wo_ref, full_w, me)
    keep_own(dout_ref, full_d, me)

    def turn(i):
        o_scr[:, seg(i)] = ot_ref[seg(i), :].T
    loop(ot_ref.shape[0] // LANE, turn)
    gain_row(g_scr, small_all, 1)
    acc[...] = jnp.zeros_like(acc)
    ddown_ref[...] = jnp.zeros_like(ddown_ref)
    for r in range(len(gw.ROUNDS)):
        gw.round(r)
        if r == 3:
            gd.start()
        for mask in gw.READY[r]:
            project(mask)

    def residual(i):
        rs = seg(i, STRIP)
        h_ref[rs, :] = (x_ref[rs, :].astype(F32) + acc[rs, :]).astype(BF16)
    loop(x_ref.shape[0] // STRIP, residual)
    norm_rows(h_ref, g_scr, m_scr)
    gm.start()
    keep_own(m_scr, full_m, me)

    def keep(mask):
        chip = flipped(me, mask) // 2
        return pltpu.make_async_copy(full_m.at[chip], m_out.at[chip], osem.at[mask // 2])

    def use(mask):
        gd.wait_pair(mask)
        gm.wait_pair(mask)
        keep(mask).start()
        chip = flipped(me, mask) // 2
        ts = seg(chip, WIDE)
        gu = mm(wgu_ref[...], full_m[chip], NT).astype(BF16).astype(F32)
        gate, up = gu[:feat], gu[feat:]
        d_glu = mm(down_ref[...], full_d[chip], NT).astype(BF16).astype(F32)
        sig = jax.nn.sigmoid(gate)
        act = gate * sig
        glu = (act * up).astype(BF16)
        glu_ref[:, ts] = glu
        dgu_ref[:feat, ts] = (d_glu * up * (sig * (1.0 + gate * (1.0 - sig)))).astype(BF16)
        dgu_ref[feat:, ts] = (d_glu * act).astype(BF16)

        def step(n):
            ddown_ref[:, seg(n, CHUNK)] += mm(glu, full_d[chip, :, seg(n, CHUNK)], NN)
        loop(dim // CHUNK, step)

    for r in range(len(gm.ROUNDS)):
        gd.round(r)
        gm.round(r)
        for mask in gm.READY[r]:
            use(mask)
    for mask in CHIP_MASKS:
        keep(mask).wait()
    for g in (gw, gd, gm):
        g.finish()


def mlp_back(dgu_ref, wgu_ref, h_ref, small_all, dout_ref, wo_ref, o_ref, glu_ref, down_ref, y_ref, dh_ref, do_ref, dwo_ref, dg_ref,
             full, g_scr, dgu_t, glu_t, free, *scr):
    me = lax.axis_index('sp')
    dim = wo_ref.shape[1]
    enter(me, NEAR)
    s = Scatter(*scr[:3], scr[3:7], me)
    g = row_gather(dh_ref, full, scr[7:], me)
    gain_row(g_scr, small_all, 1)
    dwo_ref[...] = jnp.zeros_like(dwo_ref)
    total = s.run(block_product(s.part, dgu_ref, wgu_ref, dgu_t))
    for mask in NEAR:
        pl.semaphore_signal(free, inc=1, device_id=(flipped(me, mask),), device_id_type=MESH)
    norm_back(total, h_ref, g_scr, dout_ref, dh_ref, dg_ref)
    g.start()
    keep_own(dh_ref, full, me)
    s.finish()
    pl.semaphore_wait(free, len(NEAR))

    def use(mask):
        g.wait_pair(mask)
        chip = flipped(me, mask) // 2
        do_ref[:, seg(chip, WIDE)] = mm(wo_ref[...], full[chip], NT).astype(BF16)
        o = o_ref[:, seg(chip, WIDE)]

        def step(n):
            dwo_ref[:, seg(n, CHUNK)] += mm(o, full[chip, :, seg(n, CHUNK)], NN)
        loop(dim // CHUNK, step)

    def between(i):
        if i < len(g.ROUNDS):
            g.round(i)
            for mask in g.READY[i]:
                use(mask)

    s = Scatter(*scr[:3], scr[3:7], me)
    total = s.run(block_product(s.part, glu_ref, down_ref, glu_t), between)
    y_ref[...] = (h_ref[...].astype(F32) + total[...]).astype(BF16)
    s.finish()
    g.finish()


def back(groups, hd, qkv_ref, do_ref, stat_ref, cos_all, sin_all, dgu_ref, m_hbm, ucol_ref, cos_ref, sin_ref, w_hbm, x_ref, small_all, dh_ref, dg2_ref,
         dg_hbm, du_hbm, dwq_ref, dwkv_ref, dx_ref, gain_ref,
         p_scr, dp_scr, k_scr, v_scr, dk_acc, dv_acc, stage, dq_scr, dkv_scr, m_scr,
         full, w_scr, shares, dkv_own, full_kv, dqkv, dn, g_scr, dg1, gains, gains_in, wsem, lsem, msem, *sems):
    heads = qkv_ref.shape[0] // hd - 2
    seq = qkv_ref.shape[1]
    scale = hd ** -0.5
    lanes = heads * QB
    qw = heads * hd
    half = hd // 2
    me = lax.axis_index('sp')
    feat = dgu_ref.shape[0] // 2
    first = (XYZ, X, Y + Z, Y, X + Z, Z, X + Y, 0)

    def fetch(mask):
        cols = seg(flipped(me, mask) // 2, WIDE)
        return pltpu.make_async_copy(m_hbm.at[:, :, cols], m_scr.at[:, :, cols], msem.at[mask // 2])
    for mask in first:
        fetch(mask).start()
    load = pltpu.make_async_copy(w_hbm, w_scr, wsem)
    load.start()
    enter(me, OTHERS)
    gain_row(g_scr, small_all, 0)

    def piece(lo):
        return lambda peer: stage.at[peer // 2, lo:lo + feat, seg(peer % 2)]
    gates = Swap(piece(0), lambda o: dg_hbm.at[seg(o, feat), :], sems[:2], me)
    ups = Swap(piece(feat), lambda o: du_hbm.at[seg(o, feat), :], sems[2:4], me)
    own = [pltpu.make_async_copy(swap.src(me), swap.dst(me), lsem.at[i]) for i, swap in enumerate((gates, ups))]

    def make(mask):
        chip = flipped(me, mask) // 2
        fetch(mask).wait()
        cols = m_scr[:, :, seg(chip, WIDE)].reshape(seq, WIDE)
        stage[chip] = mm(dgu_ref[...], cols, NN)

    def advance(n):
        gates.advance(n)
        ups.advance(n)

    for i, mask in enumerate(first):
        make(mask)
        if i == 1:
            advance(0)
    gates.start((CORE,))
    ups.start((CORE,))
    for copy in own:
        copy.start()

    dk_acc[...] = jnp.zeros_like(dk_acc)
    dv_acc[...] = jnp.zeros_like(dv_acc)
    key_rows(k_scr, qkv_ref, qw, hd)
    key_rows(v_scr, qkv_ref, qw + hd, hd)

    def q_block(qb):
        for at, n in ((4, 1), (7, 2)):
            @pl.when(qb == at)
            def _():
                advance(n)
        qs = seg(qb, QB)
        q2 = side_by_side(qkv_ref, heads, hd, qs)
        do2 = side_by_side(do_ref, heads, hd, qs)
        top = stat_ref[qb, :1, :]
        inv = stat_ref[qb, 1:, :]

        def probs(kb, rd, diagonal):
            ks = seg(kb, KB)
            s = score_block(k_scr[ks, :], q2, scale, diagonal)
            p = jnp.exp(s - top) * inv
            dp = mm(v_scr[ks, :], do2, NN).astype(BF16)
            p_scr[ks, :] = p
            dp_scr[ks, :] = dp
            dv_acc[ks, :] += mm(p.astype(BF16), do2, NT)
            return rd + jnp.sum(dp.astype(F32) * p, axis=0, keepdims=True)

        rd = lax.fori_loop(0, qb, lambda kb, r: probs(kb, r, False), jnp.zeros((1, lanes), F32))
        rd = probs(qb, rd, True)

        def d_scores(kb, acc):
            ks = seg(kb, KB)
            ds = (p_scr[ks, :] * (dp_scr[ks, :].astype(F32) - rd) * scale).astype(BF16)
            dk_acc[ks, :] += mm(ds, q2, NT)
            return acc + mm(qkv_ref[qw:qw + hd, ks], ds, NN)

        acc = lax.fori_loop(0, qb + 1, d_scores, jnp.zeros((hd, lanes), F32))
        cos, sin = cos_all[:, qs], sin_all[:, qs]
        for h in range(heads):
            dq = acc[:, h * QB:(h + 1) * QB].astype(BF16).astype(F32)
            p, q = dq[:half], dq[half:]
            dq_scr[h * hd:h * hd + half, qs] = (p * cos + q * sin).astype(BF16)
            dq_scr[h * hd + half:(h + 1) * hd, qs] = (q * cos - p * sin).astype(BF16)

    loop(seq // QB, q_block)

    def share(i):
        rs = seg(i, WIDE)
        dkv_scr[rs, :] = jnp.concatenate([dk_acc[rs, :], dv_acc[rs, :]], axis=1).astype(BF16)
    loop(seq // WIDE, share)
    tokens = ucol_ref.shape[1]
    per = N_DEV // groups
    q_all = dwq_ref.shape[0]
    sh = Swap(lambda peer: dkv_scr.at[seg(peer, tokens), :], lambda o: shares.at[o], sems[4:6], me)
    gq = row_gather(dq_scr, full, sems[6:10], me)
    parts = thirds(dkv_own.shape[0], STRIP)
    gk = Gather(dkv_own, lambda o: full_kv.at[:, seg(o, tokens)], lambda view, c: [view.at[pl.ds(*parts[c]), :]], sems[10:14], me)
    gs = Swap(lambda peer: gains.at[:, seg(peer)], lambda o: gains_in.at[o], sems[14:], me)
    sh.start()
    gq.start()
    keep_own(dq_scr, full, me)
    shares[me] = dkv_scr[seg(me, tokens), :]
    sh.wait_recv()
    cos, sin = cos_ref[...], sin_ref[...]
    for k in range(groups):
        both = sum(shares[per * k + i].astype(F32) for i in range(per)).astype(BF16).astype(F32).T
        p, q = both[:half], both[half:hd]
        lo = 2 * hd * k
        dkv_own[lo:lo + half, :] = (p * cos + q * sin).astype(BF16)
        dkv_own[lo + half:lo + hd, :] = (q * cos - p * sin).astype(BF16)
        dkv_own[lo + hd:lo + 2 * hd, :] = both[hd:].astype(BF16)
    gk.start()
    full_kv[:, seg(me, tokens)] = dkv_own[...]
    for k in range(groups):
        dqkv[:, q_all + 2 * hd * k:q_all + 2 * hd * (k + 1)] = dkv_own[2 * hd * k:2 * hd * (k + 1), :].T

    def use(mask):
        gq.wait_pair(mask)
        chip = flipped(me, mask) // 2
        dwq_ref[seg(chip, WIDE), :] = mm(full[chip], ucol_ref[...], NN)
        dqkv[:, seg(chip, WIDE)] = full[chip, :, seg(me, tokens)].T

    for r in range(len(gq.ROUNDS)):
        gq.round(r)
        gk.round(r)
        if r == 3:
            advance(3)
        for mask in gq.READY[r]:
            use(mask)
    load.wait()

    def normed(i):
        dn[:, seg(i, WIDE)] = mm(dqkv[...], w_scr[i], NN)
    loop(N_CHIP, normed)
    norm_back(dn, x_ref, g_scr, dh_ref, dx_ref, dg1)
    gains[...] = jnp.concatenate([jnp.sum(dg1[...], axis=0, keepdims=True), jnp.sum(dg2_ref[...], axis=0, keepdims=True),
                                  jnp.zeros((N_CHIP - 2, dg1.shape[1]), F32)], axis=0)
    gs.start()
    gains_in[me] = gains[:, seg(me)]
    for mask in CHIP_MASKS:
        gk.wait_pair(mask)
    dwkv_ref[...] = mm(full_kv[...], ucol_ref[...], NN)
    gs.wait_recv()
    gain_ref[...] = sum(gains_in[o] for o in range(N_DEV))
    for swap in (gates, ups):
        swap.wait_recv()
        swap.wait_send((CORE,) + SETS[3])
    for copy in own:
        copy.wait()
    for c in (sh, gs):
        c.wait_send()
    for g in (gq, gk):
        g.finish()


def finish(dg_hbm, du_hbm, dkv_hbm, *refs):
    n = (len(refs) - 11) // 3
    srcs, (gate, up, dk, dv), dsts = refs[:n], refs[n:n + 4], refs[n + 4:2 * n + 4]
    (g_in, g_out, kv_in), holds, sems = refs[2 * n + 4:2 * n + 7], refs[2 * n + 7:3 * n + 7], refs[3 * n + 7:]
    t_in, t_out, p_in, p_out = sems
    step = LANE * 11
    cols = g_in.shape[1]
    hd = dk.shape[0] // (kv_in.shape[0] // LANE)
    starts = [(w, i) for i in range(cols // step) for w in range(2)]

    def fetch(w, i):
        rs = pl.ds(i * step, step)
        return pltpu.make_async_copy((dg_hbm, du_hbm)[w].at[rs, :], g_in.at[w, rs, :], t_in.at[w, i])

    def put(w, i):
        cs = pl.ds(i * step, step)
        return pltpu.make_async_copy(g_out.at[w, :, cs], (gate, up)[w].at[:, cs], t_out.at[w, i])
    moves = [(pltpu.make_async_copy(a, h, p_in.at[k]), pltpu.make_async_copy(h, b, p_out.at[k])) for k, (a, h, b) in enumerate(zip(srcs, holds, dsts))]
    kv = pltpu.make_async_copy(dkv_hbm, kv_in, p_in.at[n])
    for w, i in starts:
        fetch(w, i).start()
    kv.start()
    for load, _ in moves:
        load.start()
    for w, i in starts:
        fetch(w, i).wait()

        def turn(j):
            at = seg(i * (step // LANE) + j)
            g_out[w, :, at] = g_in[w, at, :].T
        loop(step // LANE, turn)
        put(w, i).start()
    kv.wait()
    for k in range(dk.shape[0] // hd):
        for i, ref in enumerate((dk, dv)):
            ref[k * hd:(k + 1) * hd, :] = kv_in[(2 * k + i) * hd:(2 * k + i + 1) * hd, :]
    for load, store in moves:
        load.wait()
        store.start()
    for w, i in starts:
        put(w, i).wait()
    for _, store in moves:
        store.wait()


def rope_tables(positions, head_dim):
    half_dim = head_dim // 2
    inv_freq = 1.0 / (ROPE_BASE ** (jnp.arange(half_dim, dtype=F32) * (2.0 / head_dim)))
    angles = positions.astype(F32)[None, :] * inv_freq[:, None]
    return jnp.cos(angles), jnp.sin(angles)


def solution(mesh):
    assert mesh.shape['sp'] == N_DEV

    def layer_step(x_in, positions, d_out, norm1_gain, norm2_gain, w_q, w_k, w_v, w_o, w_gate, w_up, w_down):
        tokens, dim = x_in.shape
        seq = tokens * N_DEV
        n_q, hd = w_q.shape[1:]
        n_kv = w_k.shape[1]
        qw = n_q // N_DEV * hd
        rows = w_q.shape[0]
        feat = w_down.shape[0]
        cols = (n_q + 2 * n_kv) * hd
        lanes = qw // hd * QB
        vm = pltpu.VMEM
        full = vm((N_CHIP, WIDE, dim), BF16)
        gain_scr = vm((N_CHIP, dim), F32)
        small_shape = ((N_DEV, N_CHIP, rows), F32)

        cos_own, sin_own = rope_tables(positions, hd)
        row = lambda v: v.reshape(1, rows)
        by_head = lambda w: w.transpose(1, 2, 0).reshape(-1, rows)
        wo_own = w_o.reshape(qw, dim)

        args = (x_in, row(norm1_gain), row(norm2_gain), row(positions), by_head(w_q), by_head(w_k), by_head(w_v), cos_own, sin_own, w_gate, w_up)
        qkv, u_col, small_all, wqkv, attn_tok, attn_t, stat, wgu = call(
            functools.partial(head, n_kv, hd), 0, len(args),
            (((qw + 2 * hd, seq), BF16), ((seq, rows), BF16), small_shape, ((N_CHIP, cols, WIDE), BF16),
             ((n_q * hd, tokens), BF16), ((qw, seq), BF16), ((seq // QB, 2, lanes), F32), ((2 * feat, dim), BF16)),
            [vm((N_CHIP, rows), F32), vm((cols, rows), BF16), vm((N_CHIP, cols, WIDE), BF16), vm((cols, tokens), F32), vm((cols, tokens), BF16), vm((tokens, dim), BF16), gain_scr,
             vm((feat * N_DEV, rows), BF16), vm((feat * N_DEV, rows), BF16), vm((seq, lanes), F32), vm((seq, hd), BF16), dma(N_CHIP),
             *Gather.sems, *(7 * Swap.sems)], 4 * qw * seq * seq, far_out=(3,))(*args)
        args = (attn_tok, wo_own, x_in, small_all, d_out, wgu, w_down)
        hidden, m_full, glu, dgu, d_down = call(
            mlp_local, 2, len(args),
            (((tokens, dim), BF16), ((N_CHIP, WIDE, dim), BF16), ((feat, seq), BF16), ((2 * feat, seq), BF16), ((feat, dim), F32)),
            [full, full, full, vm((tokens, dim), F32), vm((tokens, dim), BF16), vm((tokens, n_q * hd), BF16), gain_scr, dma(N_CHIP), *(3 * Gather.sems)],
            8 * feat * seq * dim, far_out=(1,))(*args)
        args = (dgu, wgu, hidden, small_all, d_out, wo_own, attn_t, glu, w_down)
        y_out, d_hidden, d_attn, d_wo, d_g2 = call(
            mlp_back, 3, len(args),
            (((tokens, dim), BF16), ((tokens, dim), BF16), ((qw, seq), BF16), ((qw, dim), F32), ((N_CHIP, dim), F32)),
            [full, gain_scr, vm((WIDE, 2 * feat), BF16), vm((WIDE, feat), BF16), pltpu.SemaphoreType.REGULAR,
             *Scatter.scratch(tokens, dim), *Scatter.sems, *Gather.sems], 4 * feat * seq * dim)(*args)
        cos_all, sin_all = rope_tables(small_all[:, 2].reshape(-1), hd)
        args = (qkv, d_attn, stat, cos_all, sin_all, dgu, m_full, u_col, cos_own, sin_own, wqkv, x_in, small_all, d_hidden, d_g2)
        d_gate_t, d_up_t, d_wq, d_wkv, d_x, gains = call(
            functools.partial(back, n_kv, hd), 4, len(args),
            (((feat * N_DEV, rows), F32), ((feat * N_DEV, rows), F32),
             ((n_q * hd, rows), F32), ((2 * n_kv * hd, rows), F32), ((tokens, dim), BF16), ((N_CHIP, rows), F32)),
            [vm((seq, lanes), F32), vm((seq, lanes), BF16), vm((seq, hd), BF16), vm((seq, hd), BF16), vm((seq, hd), F32), vm((seq, hd), F32),
             vm((N_CHIP, 2 * feat, WIDE), F32), vm((qw, seq), BF16), vm((seq, 2 * hd), BF16), full,
             full, vm((N_CHIP, cols, WIDE), BF16), vm((N_DEV, tokens, 2 * hd), BF16), vm((2 * n_kv * hd, tokens), BF16), vm((2 * n_kv * hd, seq), BF16),
             vm((tokens, cols), BF16), vm((tokens, dim), F32), gain_scr, gain_scr, gain_scr, vm((N_DEV, N_CHIP, rows), F32), dma(), dma(2), dma(N_CHIP),
             *(3 * Swap.sems), *(2 * Gather.sems), *Swap.sems], 10 * qw * seq * seq, far_in=(6, 10), far_out=(0, 1))(*args)
        moved = (d_wq, d_wo, d_down, d_x, y_out, gains)
        half_kv = jax.ShapeDtypeStruct((n_kv * hd, rows), F32)
        wide = jax.ShapeDtypeStruct((rows, feat * N_DEV), F32)
        d_gate, d_up, d_wk, d_wv, d_wq, d_wo, d_down, d_x, y_out, gains = pl.pallas_call(
            finish,
            out_shape=[wide, wide, half_kv, half_kv] + [jax.ShapeDtypeStruct(v.shape, v.dtype) for v in moved],
            in_specs=[IN_HBM] * (3 + len(moved)), out_specs=[IN_HBM] * 2 + on_chip(2) + [IN_HBM] * len(moved),
            scratch_shapes=[vm((2, feat * N_DEV, rows), F32), vm((2, rows, feat * N_DEV), F32), vm(d_wkv.shape, F32)]
            + [vm(v.shape, v.dtype) for v in moved] + [dma(2, 4), dma(2, 4), dma(len(moved) + 1), dma(len(moved))],
            compiler_params=pltpu.CompilerParams(vmem_limit_bytes=VMEM_CAP), name='finish',
        )(d_gate_t, d_up_t, d_wkv, *moved)
        by_row = lambda g, heads: g.reshape(heads, hd, rows).transpose(2, 0, 1)
        return (y_out, d_x, gains[0], gains[1], by_row(d_wq, n_q), by_row(d_wk, n_kv), by_row(d_wv, n_kv),
                d_wo.reshape(w_o.shape), d_gate, d_up, d_down)

    all_rows = P('sp')
    return jax.shard_map(layer_step, mesh=mesh, in_specs=(all_rows,) * 12, out_specs=(all_rows,) * 11, check_vma=False)
```

```python
import functools
import jax
import jax.numpy as jnp
from jax import lax
from jax.experimental import pallas as pl
from jax.experimental.pallas import tpu as pltpu
from jax.sharding import PartitionSpec as P

ROPE_BASE = 10000.0
NORM_EPS = 1e-5
NEG_LARGE = -1e30
F32 = jnp.float32
BF16 = jnp.bfloat16
N_DEV, N_CHIP, LANE, WIDE, CHUNK, STRIP = 16, 8, 128, 256, 512, 16
NT = (((1,), (1,)), ((), ()))
TN = (((0,), (0,)), ((), ()))
NN = (((1,), (0,)), ((), ()))
MESH = pl.DeviceIdType.MESH
VMEM_CAP = 62 * 1024 * 1024

CORE, X, Y, Z = 1, 2, 4, 8
XYZ = X + Y + Z
ORDERS = ((X, Y, Z), (Y, Z, X), (Z, X, Y))
CHIP_MASKS = (0, X, Y, Z, X + Y, X + Z, Y + Z, XYZ)
NEAR = (CORE, X, Y, Z)
OTHERS = range(1, N_DEV)
SETS = tuple(tuple(m + c for m in masks for c in (0, CORE)) for masks in ((XYZ,), (X, Y + Z), (Y, X + Z), (Z, X + Y)))
COLOURS = range(len(ORDERS))


def mm(a, b, dims):
    return lax.dot_general(a, b, dims, preferred_element_type=F32)


def seg(index, width=LANE):
    return pl.ds(pl.multiple_of(index * width, width), width)


def loop(count, body):
    lax.fori_loop(0, count, lambda i, c: (body(i), c)[1], 0)


def flipped(index, mask):
    out = index
    for bit in NEAR:
        if mask & bit:
            out = out + (1 - 2 * ((index // bit) % 2)) * bit
    return out


def thirds(total, unit):
    n = total // unit
    first = (n + 2) // 3
    second = (n - first + 1) // 2
    sizes = (first * unit, second * unit, (n - first - second) * unit)
    return ((0, sizes[0]), (sizes[0], sizes[1]), (sizes[0] + sizes[1], sizes[2]))


def pieces(rows, cols, unit):
    share = cols // LANE // 3 * LANE
    strips = thirds(rows, unit)
    rest = cols - 3 * share
    return [[(pl.ds(0, rows), pl.ds(c * share, share)), (pl.ds(*strips[c]), pl.ds(3 * share, rest))] for c in COLOURS]


def enter(me, masks):
    barrier = pltpu.get_barrier_semaphore()
    for mask in masks:
        pl.semaphore_signal(barrier, inc=1, device_id=(flipped(me, mask),), device_id_type=MESH)
    pl.semaphore_wait(barrier, len(masks))


def remote(src, dst, send, recv, peer):
    return pltpu.make_async_remote_copy(src_ref=src, dst_ref=dst, send_sem=send, recv_sem=recv, device_id=(peer,), device_id_type=MESH)


def dma(*shape):
    return pltpu.SemaphoreType.DMA(shape)


class Swap:
    sems = (dma(N_DEV), dma(N_DEV))

    def __init__(self, src, dst, sems, me):
        self.src, self.dst, (self.send, self.recv), self.me = src, dst, sems, me

    def copy(self, mask):
        peer = flipped(self.me, mask)
        return remote(self.src(peer), self.dst(self.me), self.send.at[mask], self.recv.at[mask], peer)

    def start(self, masks=OTHERS):
        for mask in masks:
            self.copy(mask).start()

    def advance(self, n):
        if n:
            for mask in SETS[n - 1]:
                self.copy(mask).wait_send()
        self.start(SETS[n])

    def wait_recv(self):
        for mask in OTHERS:
            view = self.dst(flipped(self.me, mask))
            remote(view, view, self.send.at[mask], self.recv.at[mask], self.me).wait_recv()

    def wait_send(self, masks=OTHERS):
        for mask in masks:
            self.copy(mask).wait_send()


class Gather:
    ROUNDS = ((0,), (1,), (2,), (0, 1), (0, 2), (1, 2), (0, 1, 2))
    READY = ((0,), (), (), (X, Y), (Z,), (X + Y, X + Z), (Y + Z, XYZ))
    sems = (dma(3, N_CHIP, 3, 2), dma(3, N_CHIP, 2), dma(N_CHIP), dma(N_CHIP))

    def __init__(self, own, block, cut, sems, me):
        self.own, self.block, self.cut, self.me = own, block, cut, me
        self.send, self.recv, self.pair_send, self.pair_recv = sems

    def source(self, mask):
        return self.block(flipped(self.me, mask)) if mask else self.own

    def unit(self, colour, mask, axis):
        ends = zip(self.cut(self.source(mask), colour), self.cut(self.block(flipped(self.me, mask)), colour))
        return [remote(src, dst, self.send.at[colour, mask // 2, ORDERS[colour].index(axis), i], self.recv.at[colour, (mask + axis) // 2, i],
                       flipped(self.me, axis)) for i, (src, dst) in enumerate(ends)]

    def start_unit(self, colour, mask, axis):
        for copy in self.unit(colour, mask, axis):
            copy.start()

    def pair(self, mask):
        return remote(self.source(mask), self.block(flipped(self.me, mask)), self.pair_send.at[mask // 2],
                      self.pair_recv.at[mask // 2], flipped(self.me, CORE))

    def wait_pair(self, mask):
        view = self.block(flipped(self.me, mask + CORE))
        remote(view, view, self.pair_send.at[mask // 2], self.pair_recv.at[mask // 2], self.me).wait_recv()

    def onward(self, colour):
        order = ORDERS[colour]
        for picks in self.ROUNDS:
            for axis in order[picks[-1] + 1:]:
                yield picks, sum(order[p] for p in picks), axis

    def start(self):
        for pos in COLOURS:
            for colour in COLOURS:
                self.start_unit(colour, 0, ORDERS[colour][pos])
        self.pair(0).start()

    def round(self, r):
        for colour in COLOURS:
            mask = sum(ORDERS[colour][p] for p in self.ROUNDS[r])
            for i, view in enumerate(self.cut(self.block(flipped(self.me, mask)), colour)):
                remote(view, view, self.send.at[colour, 0, 0, i], self.recv.at[colour, mask // 2, i], self.me).wait_recv()
            for picks, at, axis in self.onward(colour):
                if picks == self.ROUNDS[r]:
                    self.start_unit(colour, at, axis)
        for mask in {2: (X, Y, Z), 5: (X + Y, X + Z, Y + Z), 6: (XYZ,)}.get(r, ()):
            self.pair(mask).start()

    def finish(self):
        for colour in COLOURS:
            for at, axis in [(0, axis) for axis in ORDERS[colour]] + [step[1:] for step in self.onward(colour)]:
                for copy in self.unit(colour, at, axis):
                    copy.wait_send()
        for mask in CHIP_MASKS:
            self.pair(mask).wait_send()


def row_gather(own, full, sems, me, extra=None):
    rows, width = own.shape
    parts = pieces(rows, width, STRIP)
    if extra is not None:
        share = width // LANE // 3 * LANE
        more = width - 3 * share
        parts = [[(pl.ds(0, rows), pl.ds(c * share + more * (c > extra), share + more * (c == extra)))] for c in COLOURS]

    def block(o):
        return full.at[o // 2, seg(o % 2), :]

    return Gather(own, block, lambda view, c: [view.at[rs, cs] for rs, cs in parts[c]], sems, me)


def keep_own(own, full, me):
    def step(i):
        full[me // 2, pl.ds(pl.multiple_of((me % 2) * LANE + i * STRIP, STRIP), STRIP), :] = own[seg(i, STRIP), :]
    loop(LANE // STRIP, step)


class Scatter:
    ORDER = (XYZ, X + Y, Y + Z, X + Z, X, Y, Z, 0)
    sems = (dma(N_CHIP), dma(N_CHIP), dma(3, N_CHIP, 2), dma(3, N_CHIP, 2))

    @staticmethod
    def scratch(tokens, dim):
        return [pltpu.VMEM((N_CHIP, 2, tokens, dim), F32), pltpu.VMEM((N_CHIP, tokens, dim), F32), pltpu.VMEM((N_CHIP - 1, tokens, dim), F32)]

    def __init__(self, part, pair_in, link_in, sems, me):
        self.part, self.pair_in, self.link_in, self.me = part, pair_in, link_in, me
        self.pair_send, self.pair_recv, self.link_send, self.link_recv = sems
        self.core = me % 2
        self.tokens, self.dim = part.shape[2:]
        self.pieces = pieces(self.tokens, self.dim, STRIP // 2)
        self.ready, self.sent = set(), [0] * len(ORDERS)

    @staticmethod
    def first(colour, mask):
        return next((i for i, a in enumerate(ORDERS[colour]) if mask & a), 3)

    def slot(self, colour, mask, axis):
        slots = [(m, a) for m in self.ORDER for a in ORDERS[colour][:self.first(colour, m)]]
        return slots.index((mask, axis))

    def pair(self, i):
        return remote(self.part.at[i, 1 - self.core], self.pair_in.at[i], self.pair_send.at[i], self.pair_recv.at[i], flipped(self.me, CORE))

    def link(self, colour, mask):
        axis = ORDERS[colour][self.first(colour, mask)]
        slot = self.slot(colour, mask - axis, axis)
        i = self.ORDER.index(mask)
        return [remote(self.part.at[i, self.core, rs, cs], self.link_in.at[slot, rs, cs], self.link_send.at[colour, i, k],
                       self.link_recv.at[colour, slot, k], flipped(self.me, axis)) for k, (rs, cs) in enumerate(self.pieces[colour])]

    def start_link(self, colour, mask):
        for copy in self.link(colour, mask):
            copy.start()

    def add(self, mask, ref, cs):
        i = self.ORDER.index(mask)

        def step(r):
            rs = seg(r, STRIP)
            self.part[i, self.core, rs, cs] += ref[rs, cs]
        loop(self.tokens // STRIP, step)

    def finish_pair(self, i):
        self.pair(i).wait_recv()
        self.add(self.ORDER[i], self.pair_in.at[i], pl.ds(0, self.dim))
        self.ready.add(self.ORDER[i])
        for colour in COLOURS:
            a, b, c = ORDERS[colour]
            todo = (XYZ, a + b, a + c, a)
            while self.sent[colour] < len(todo) and todo[self.sent[colour]] in self.ready:
                self.start_link(colour, todo[self.sent[colour]])
                self.sent[colour] += 1

    def take(self, colour, mask, axis):
        for copy in self.link(colour, mask + axis):
            copy.wait_recv()
        ref = self.link_in.at[self.slot(colour, mask, axis)]
        (_, wide), (rs, cs) = self.pieces[colour]
        self.add(mask, ref, wide)
        self.part[self.ORDER.index(mask), self.core, rs, cs] += ref[rs, cs]

    def run(self, product, between=lambda i: None):
        for i, mask in enumerate(self.ORDER):
            product(i, flipped(self.me, mask) // 2)
            self.pair(i).start()
            if i:
                self.finish_pair(i - 1)
            between(i)
        self.finish_pair(N_CHIP - 1)
        for step in range(2):
            for colour in COLOURS:
                a, b, c = ORDERS[colour]
                mask = (b + c, b)[step]
                self.take(colour, mask, a)
                self.start_link(colour, mask)
        for colour in COLOURS:
            a, b, c = ORDERS[colour]
            self.take(colour, c, a)
            self.take(colour, c, b)
            self.start_link(colour, c)
        for colour in COLOURS:
            for axis in ORDERS[colour]:
                self.take(colour, 0, axis)
        return self.part.at[N_CHIP - 1, self.core]

    def finish(self):
        for i in range(N_CHIP):
            self.pair(i).wait_send()
        for colour in COLOURS:
            for mask in self.ORDER[:-1]:
                for copy in self.link(colour, mask):
                    copy.wait_send()


def block_product(part, a_ref, w_ref, a_t):
    tokens = part.shape[2]

    def product(i, chip):
        a_t[...] = a_ref[:, seg(chip, 2 * tokens)].T

        def step(n):
            cs = seg(n, CHUNK)
            r = mm(a_t[...], w_ref[:, cs], NN)
            part[i, 0, :, cs] = r[:tokens]
            part[i, 1, :, cs] = r[tokens:]
        loop(part.shape[3] // CHUNK, step)
    return product


def on_chip(n):
    return [pl.BlockSpec(memory_space=pltpu.VMEM)] * n


IN_HBM = pl.BlockSpec(memory_space=pl.ANY)


def call(kernel, ident, args, outs, scratch, flops, far_in=(), far_out=()):
    specs = [IN_HBM if i in far_in else on_chip(1)[0] for i in range(args)]
    out_specs = [IN_HBM if i in far_out else on_chip(1)[0] for i in range(len(outs))]
    return pl.pallas_call(
        kernel,
        out_shape=[jax.ShapeDtypeStruct(shape, dtype) for shape, dtype in outs],
        in_specs=specs, out_specs=out_specs, scratch_shapes=scratch,
        cost_estimate=pl.CostEstimate(flops=flops, bytes_accessed=flops // CHUNK, transcendentals=0),
        compiler_params=pltpu.CompilerParams(collective_id=ident, has_side_effects=True, vmem_limit_bytes=VMEM_CAP),
        name=kernel.func.__name__ if isinstance(kernel, functools.partial) else kernel.__name__,
    )


def fetch_all(sem, *pairs):
    copies = [pltpu.make_async_copy(src, dst, sem.at[i]) for i, (src, dst) in enumerate(pairs)]
    for copy in copies:
        copy.start()
    return copies


def gain_row(dst, small_all, which):
    for o in range(N_DEV):
        dst[:1, o * LANE:(o + 1) * LANE] = small_all[o, which:which + 1, :]


def norm_rows(src, gain, dst):
    def step(i):
        rs = seg(i, STRIP)
        t = src[rs, :].astype(F32)
        dst[rs, :] = (t * lax.rsqrt(jnp.mean(t * t, axis=-1, keepdims=True) + NORM_EPS) * gain[:1, :]).astype(BF16)
    loop(src.shape[0] // STRIP, step)


def norm_back(dy, src, gain, skip, dst, dgain):
    def step(i):
        rs = seg(i, STRIP)
        d = dy[rs, :].astype(BF16).astype(F32)
        t = src[rs, :].astype(F32)
        inv = lax.rsqrt(jnp.mean(t * t, axis=-1, keepdims=True) + NORM_EPS)
        gd = gain[:1, :] * d
        pull = jnp.mean(gd * t, axis=-1, keepdims=True)
        dst[rs, :] = (skip[rs, :].astype(F32) + (inv * gd - t * (inv * inv * inv * pull))).astype(BF16)
        g = d * (t * inv)
        dgain[...] += g[:N_CHIP] + g[N_CHIP:]
    dgain[...] = jnp.zeros_like(dgain)
    loop(src.shape[0] // STRIP, step)


QB = 256
KB = 256


def key_rows(dst, src, lo, hd):
    def step(i):
        dst[seg(i, KB), :] = src[lo:lo + hd, seg(i, KB)].T
    loop(src.shape[1] // KB, step)


def score_block(k, q2, scale, diagonal):
    s = mm(k, q2, NN) * scale
    if diagonal:
        key = lax.broadcasted_iota(jnp.int32, s.shape, 0)
        qry = lax.broadcasted_iota(jnp.int32, s.shape, 1) % QB
        s = jnp.where(qry >= key, s, NEG_LARGE)
    return s


def side_by_side(ref, heads, hd, qs):
    return jnp.concatenate([ref[h * hd:(h + 1) * hd, qs] for h in range(heads)], axis=1)


def head(groups, hd, x_ref, g1_ref, g2_ref, pos_ref, wq_ref, wk_ref, wv_ref, cos_ref, sin_ref, wg_ref, wu_ref, qkv_ref, ucol_ref, small_all, w_out, ot_ref, o_ref, stat_ref, wgu_ref,
         small_ref, w_ref, full, acc, rot, u_scr, g_scr, wg_t, wu_t, s_scr, k_scr, osem, *sems):
    me = lax.axis_index('sp')
    tokens, dim = x_ref.shape
    cols = w_ref.shape[0]
    small_ref[...] = jnp.concatenate([r[...].astype(F32) for r in (g1_ref, g2_ref, pos_ref)] + [jnp.zeros((N_CHIP - 3, LANE), F32)], axis=0)
    w_ref[:wq_ref.shape[0], :] = wq_ref[...]
    for k in range(groups):
        for i, ref in enumerate((wk_ref, wv_ref)):
            w_ref[pl.ds(wq_ref.shape[0] + (2 * k + i) * hd, hd), :] = ref[k * hd:(k + 1) * hd, :]
    qw = tokens
    q_all = N_DEV * qw
    gsems, ssems, usems, qsems, ksems, gate_sems, up_sems, osems = sems[:4], *(sems[i:i + 2] for i in range(4, len(sems), 2))
    feat = wg_ref.shape[1] // N_DEV
    enter(me, OTHERS)
    smalls = Swap(lambda peer: small_ref, lambda o: small_all.at[o], ssems, me)
    smalls.start()
    parts = thirds(cols, STRIP)
    g = Gather(w_ref, lambda o: full.at[o // 2, :, seg(o % 2)], lambda view, c: [view.at[pl.ds(*parts[c]), :]], gsems, me)
    g.start()

    def own_block(i):
        full[me // 2, seg(i, WIDE), seg(me % 2)] = w_ref[seg(i, WIDE), :]
    loop(cols // WIDE, own_block)
    acc[...] = jnp.zeros_like(acc)
    small_all[me] = small_ref[...]
    smalls.wait_recv()
    gain_row(g_scr, small_all, 0)
    norm_rows(x_ref, g_scr, u_scr)
    gates = Swap(lambda peer: wg_t.at[seg(peer, feat), :], lambda o: wgu_ref.at[:feat, seg(o)], gate_sems, me)
    ups = Swap(lambda peer: wu_t.at[seg(peer, feat), :], lambda o: wgu_ref.at[feat:, seg(o)], up_sems, me)
    turns = wg_ref.shape[1] // LANE // 4

    def transpose(i):
        wg_t[seg(i), :] = wg_ref[:, seg(i)].T
        wu_t[seg(i), :] = wu_ref[:, seg(i)].T

    ucols = Swap(lambda peer: u_scr.at[:, seg(peer)], lambda o: ucol_ref.at[seg(o, tokens), :], usems, me)

    def keep(mask):
        chip = flipped(me, mask) // 2
        return pltpu.make_async_copy(full.at[chip], w_out.at[chip], osem.at[mask // 2])

    def use(mask):
        g.wait_pair(mask)
        keep(mask).start()
        chip = flipped(me, mask) // 2
        u = u_scr[:, seg(chip, WIDE)]

        def step(i):
            rs = seg(i, cols // 2)
            acc[rs, :] += mm(full[chip, rs, :], u, NT)
        loop(2, step)

    for r in range(len(g.ROUNDS)):
        g.round(r)
        if r < 4:
            loop(turns, lambda i: transpose(turns * r + i))
        if r == 3:
            ucols.start()
        for mask in g.READY[r]:
            use(mask)

    half = hd // 2
    cos, sin = cos_ref[...], sin_ref[...]

    def turn(h):
        first = seg(2 * h, half)
        second = seg(2 * h + 1, half)
        p = acc[first, :].astype(BF16).astype(F32)
        q = acc[second, :].astype(BF16).astype(F32)
        rot[first, :] = (p * cos - q * sin).astype(BF16)
        rot[second, :] = (q * cos + p * sin).astype(BF16)
    loop(q_all // hd, turn)
    for k in range(groups):
        turn(q_all // hd + 2 * k)
        vs = seg(q_all // hd + 2 * k + 1, hd)
        rot[vs, :] = acc[vs, :].astype(BF16)
    per = N_DEV // groups
    q_rows = lambda peer: seg(peer, qw)
    kv_rows = lambda peer: seg(q_all // (2 * hd) + peer // per, 2 * hd)
    qs = Swap(lambda peer: rot.at[q_rows(peer), :], lambda o: qkv_ref.at[:qw, seg(o, tokens)], qsems, me)
    kvs = Swap(lambda peer: rot.at[kv_rows(peer), :], lambda o: qkv_ref.at[qw:, seg(o, tokens)], ksems, me)
    qs.start()
    kvs.start()
    gates.advance(0)
    ups.advance(0)
    qkv_ref[:qw, seg(me, tokens)] = rot[q_rows(me), :]
    qkv_ref[qw:, seg(me, tokens)] = rot[kv_rows(me), :]
    ucol_ref[seg(me, tokens), :] = u_scr[:, seg(me)]
    wgu_ref[:feat, seg(me)] = wg_t[seg(me, feat), :]
    wgu_ref[feat:, seg(me)] = wu_t[seg(me, feat), :]
    gates.start((CORE,))
    ups.start((CORE,))
    for swap in (qs, kvs):
        swap.wait_recv()
    heads = qkv_ref.shape[0] // hd - 2
    seq = qkv_ref.shape[1]
    scale = hd ** -0.5
    lanes = heads * QB
    key_rows(k_scr, qkv_ref, qw, hd)

    outs = Swap(lambda peer: o_ref.at[:, seg(peer)], lambda o: ot_ref.at[seg(o, qw), :], osems, me)

    def q_block(qb):
        for at, n in ((5, 1), (7, 2)):
            @pl.when(qb == at)
            def _():
                gates.advance(n)
                ups.advance(n)
        qs = seg(qb, QB)
        q2 = side_by_side(qkv_ref, heads, hd, qs)

        def scores(kb, top, diagonal):
            s = score_block(k_scr[seg(kb, KB), :], q2, scale, diagonal)
            s_scr[seg(kb, KB), :] = s
            return jnp.maximum(top, jnp.max(s, axis=0, keepdims=True))

        top = lax.fori_loop(0, qb, lambda kb, t: scores(kb, t, False), jnp.full((1, lanes), NEG_LARGE, F32))
        top = scores(qb, top, True)

        def expo(kb, tot):
            e = jnp.exp(s_scr[seg(kb, KB), :] - top)
            s_scr[seg(kb, KB), :] = e
            return tot + jnp.sum(e, axis=0, keepdims=True)

        inv = 1.0 / lax.fori_loop(0, qb + 1, expo, jnp.zeros((1, lanes), F32))

        def weigh(kb, acc):
            p = (s_scr[seg(kb, KB), :] * inv).astype(BF16)
            return acc + mm(qkv_ref[qw + hd:, seg(kb, KB)], p, NN)

        acc = lax.fori_loop(0, qb + 1, weigh, jnp.zeros((hd, lanes), F32))
        for h in range(heads):
            o_ref[h * hd:(h + 1) * hd, qs] = acc[:, h * QB:(h + 1) * QB].astype(BF16)
        stat_ref[qb, :1, :] = top
        stat_ref[qb, 1:, :] = inv
    loop(seq // QB, q_block)
    outs.start()
    gates.advance(3)
    ups.advance(3)
    ot_ref[seg(me, qw), :] = o_ref[:, seg(me)]
    for swap in (outs, gates, ups, ucols):
        swap.wait_recv()
    for mask in CHIP_MASKS:
        keep(mask).wait()
    outs.wait_send()
    for swap in (gates, ups):
        swap.wait_send((CORE,) + SETS[3])
    g.finish()
    for swap in (smalls, ucols, qs, kvs):
        swap.wait_send()


def mlp_local(ot_ref, wo_ref, x_ref, small_all, dout_ref, wgu_hbm, down_hbm, h_ref, m_out, glu_out, dgu_out, ddown_ref,
              wgu_ref, down_ref, glu_ref, dgu_ref, isem, full_w, full_d, full_m, acc, m_scr, o_scr, g_scr, osem, *sems):
    me = lax.axis_index('sp')
    feat, dim = down_ref.shape
    loads = fetch_all(isem, (wgu_hbm, wgu_ref), (down_hbm, down_ref))
    enter(me, NEAR)
    gw = row_gather(wo_ref, full_w, sems[:4], me, 0)
    gd = row_gather(dout_ref, full_d, sems[4:8], me, 1)
    gm = row_gather(m_scr, full_m, sems[8:], me, 2)

    def project(mask):
        gw.wait_pair(mask)
        chip = flipped(me, mask) // 2
        o = o_scr[:, seg(chip, WIDE)]

        def step(n):
            acc[:, seg(n, CHUNK)] += mm(o, full_w[chip, :, seg(n, CHUNK)], NN)
        loop(dim // CHUNK, step)

    gw.start()
    keep_own(wo_ref, full_w, me)
    keep_own(dout_ref, full_d, me)

    def turn(i):
        o_scr[:, seg(i)] = ot_ref[seg(i), :].T
    loop(ot_ref.shape[0] // LANE, turn)
    gain_row(g_scr, small_all, 1)
    acc[...] = jnp.zeros_like(acc)
    ddown_ref[...] = jnp.zeros_like(ddown_ref)
    for r in range(len(gw.ROUNDS)):
        gw.round(r)
        if r == 3:
            gd.start()
        for mask in gw.READY[r]:
            project(mask)

    def residual(i):
        rs = seg(i, STRIP)
        h_ref[rs, :] = (x_ref[rs, :].astype(F32) + acc[rs, :]).astype(BF16)
    loop(x_ref.shape[0] // STRIP, residual)
    norm_rows(h_ref, g_scr, m_scr)
    gm.start()
    keep_own(m_scr, full_m, me)

    def keep(mask):
        chip = flipped(me, mask) // 2
        ts = seg(chip, WIDE)
        ends = ((full_m.at[chip], m_out.at[chip]), (glu_ref.at[:, ts], glu_out.at[:, ts]), (dgu_ref.at[:, ts], dgu_out.at[:, ts]))
        return [pltpu.make_async_copy(src, dst, osem.at[mask // 2, i]) for i, (src, dst) in enumerate(ends)]

    for load in loads:
        load.wait()

    def use(mask):
        gd.wait_pair(mask)
        gm.wait_pair(mask)
        chip = flipped(me, mask) // 2
        ts = seg(chip, WIDE)
        gu = mm(wgu_ref[...], full_m[chip], NT).astype(BF16).astype(F32)
        gate, up = gu[:feat], gu[feat:]
        d_glu = mm(down_ref[...], full_d[chip], NT).astype(BF16).astype(F32)
        sig = jax.nn.sigmoid(gate)
        act = gate * sig
        glu = (act * up).astype(BF16)
        glu_ref[:, ts] = glu
        dgu_ref[:feat, ts] = (d_glu * up * (sig * (1.0 + gate * (1.0 - sig)))).astype(BF16)
        dgu_ref[feat:, ts] = (d_glu * act).astype(BF16)

        def step(n):
            ddown_ref[:, seg(n, CHUNK)] += mm(glu, full_d[chip, :, seg(n, CHUNK)], NN)
        loop(dim // CHUNK, step)
        for copy in keep(mask):
            copy.start()

    for r in range(len(gm.ROUNDS)):
        gd.round(r)
        gm.round(r)
        for mask in gm.READY[r]:
            use(mask)
    for mask in CHIP_MASKS:
        for copy in keep(mask):
            copy.wait()
    for g in (gw, gd, gm):
        g.finish()


def mlp_back(dgu_hbm, wgu_hbm, h_ref, small_all, dout_ref, wo_ref, o_ref, glu_hbm, down_hbm, y_ref, dh_ref, do_ref, dwo_ref, dg_ref,
             dgu_ref, wgu_ref, glu_ref, down_ref, isem, full, g_scr, dgu_t, glu_t, free, *scr):
    me = lax.axis_index('sp')
    dim = wo_ref.shape[1]
    loads = fetch_all(isem, (dgu_hbm, dgu_ref), (wgu_hbm, wgu_ref), (glu_hbm, glu_ref), (down_hbm, down_ref))
    enter(me, NEAR)
    s = Scatter(*scr[:3], scr[3:7], me)
    g = row_gather(dh_ref, full, scr[7:], me)
    gain_row(g_scr, small_all, 1)
    dwo_ref[...] = jnp.zeros_like(dwo_ref)
    for load in loads:
        load.wait()
    total = s.run(block_product(s.part, dgu_ref, wgu_ref, dgu_t))
    for mask in NEAR:
        pl.semaphore_signal(free, inc=1, device_id=(flipped(me, mask),), device_id_type=MESH)
    norm_back(total, h_ref, g_scr, dout_ref, dh_ref, dg_ref)
    g.start()
    keep_own(dh_ref, full, me)
    s.finish()
    pl.semaphore_wait(free, len(NEAR))

    def use(mask):
        g.wait_pair(mask)
        chip = flipped(me, mask) // 2
        do_ref[:, seg(chip, WIDE)] = mm(wo_ref[...], full[chip], NT).astype(BF16)
        o = o_ref[:, seg(chip, WIDE)]

        def step(n):
            dwo_ref[:, seg(n, CHUNK)] += mm(o, full[chip, :, seg(n, CHUNK)], NN)
        loop(dim // CHUNK, step)

    def between(i):
        if i < len(g.ROUNDS):
            g.round(i)
            for mask in g.READY[i]:
                use(mask)

    s = Scatter(*scr[:3], scr[3:7], me)
    total = s.run(block_product(s.part, glu_ref, down_ref, glu_t), between)
    y_ref[...] = (h_ref[...].astype(F32) + total[...]).astype(BF16)
    s.finish()
    g.finish()


def back(groups, hd, qkv_ref, do_ref, stat_ref, cos_all, sin_all, dgu_ref, m_hbm, ucol_ref, cos_ref, sin_ref, w_hbm, x_ref, small_all, dh_ref, dg2_ref,
         dg_hbm, du_hbm, dwq_ref, dwkv_ref, dx_ref, gain_ref,
         p_scr, dp_scr, k_scr, v_scr, dk_acc, dv_acc, stage, dq_scr, dkv_scr, m_scr,
         full, w_scr, shares, dkv_own, full_kv, dqkv, dn, g_scr, dg1, gains, gains_in, wsem, lsem, msem, *sems):
    heads = qkv_ref.shape[0] // hd - 2
    seq = qkv_ref.shape[1]
    scale = hd ** -0.5
    lanes = heads * QB
    qw = heads * hd
    half = hd // 2
    me = lax.axis_index('sp')
    feat = dgu_ref.shape[0] // 2
    first = (XYZ, X, Y + Z, Y, X + Z, Z, X + Y, 0)

    def fetch(mask):
        cols = seg(flipped(me, mask) // 2, WIDE)
        return pltpu.make_async_copy(m_hbm.at[:, :, cols], m_scr.at[:, :, cols], msem.at[mask // 2])
    for mask in first:
        fetch(mask).start()
    load = pltpu.make_async_copy(w_hbm, w_scr, wsem)
    load.start()
    enter(me, OTHERS)
    gain_row(g_scr, small_all, 0)

    def piece(lo):
        return lambda peer: stage.at[peer // 2, lo:lo + feat, seg(peer % 2)]
    gates = Swap(piece(0), lambda o: dg_hbm.at[seg(o, feat), :], sems[:2], me)
    ups = Swap(piece(feat), lambda o: du_hbm.at[seg(o, feat), :], sems[2:4], me)
    own = [pltpu.make_async_copy(swap.src(me), swap.dst(me), lsem.at[i]) for i, swap in enumerate((gates, ups))]

    def make(mask):
        chip = flipped(me, mask) // 2
        fetch(mask).wait()
        cols = m_scr[:, :, seg(chip, WIDE)].reshape(seq, WIDE)
        stage[chip] = mm(dgu_ref[...], cols, NN)

    def advance(n):
        gates.advance(n)
        ups.advance(n)

    for i, mask in enumerate(first):
        make(mask)
        if i == 0:
            advance(0)
    gates.start((CORE,))
    ups.start((CORE,))
    for copy in own:
        copy.start()

    dk_acc[...] = jnp.zeros_like(dk_acc)
    dv_acc[...] = jnp.zeros_like(dv_acc)
    key_rows(k_scr, qkv_ref, qw, hd)
    key_rows(v_scr, qkv_ref, qw + hd, hd)

    def q_block(qb):
        for at, n in ((4, 1), (7, 2)):
            @pl.when(qb == at)
            def _():
                advance(n)
        qs = seg(qb, QB)
        q2 = side_by_side(qkv_ref, heads, hd, qs)
        do2 = side_by_side(do_ref, heads, hd, qs)
        top = stat_ref[qb, :1, :]
        inv = stat_ref[qb, 1:, :]

        def probs(kb, rd, diagonal):
            ks = seg(kb, KB)
            s = score_block(k_scr[ks, :], q2, scale, diagonal)
            p = jnp.exp(s - top) * inv
            dp = mm(v_scr[ks, :], do2, NN).astype(BF16)
            p_scr[ks, :] = p
            dp_scr[ks, :] = dp
            dv_acc[ks, :] += mm(p.astype(BF16), do2, NT)
            return rd + jnp.sum(dp.astype(F32) * p, axis=0, keepdims=True)

        rd = lax.fori_loop(0, qb, lambda kb, r: probs(kb, r, False), jnp.zeros((1, lanes), F32))
        rd = probs(qb, rd, True)

        def d_scores(kb, acc):
            ks = seg(kb, KB)
            ds = (p_scr[ks, :] * (dp_scr[ks, :].astype(F32) - rd) * scale).astype(BF16)
            dk_acc[ks, :] += mm(ds, q2, NT)
            return acc + mm(qkv_ref[qw:qw + hd, ks], ds, NN)

        acc = lax.fori_loop(0, qb + 1, d_scores, jnp.zeros((hd, lanes), F32))
        cos, sin = cos_all[:, qs], sin_all[:, qs]
        for h in range(heads):
            dq = acc[:, h * QB:(h + 1) * QB].astype(BF16).astype(F32)
            p, q = dq[:half], dq[half:]
            dq_scr[h * hd:h * hd + half, qs] = (p * cos + q * sin).astype(BF16)
            dq_scr[h * hd + half:(h + 1) * hd, qs] = (q * cos - p * sin).astype(BF16)

    loop(seq // QB, q_block)

    def share(i):
        rs = seg(i, WIDE)
        dkv_scr[rs, :] = jnp.concatenate([dk_acc[rs, :], dv_acc[rs, :]], axis=1).astype(BF16)
    loop(seq // WIDE, share)
    tokens = ucol_ref.shape[1]
    per = N_DEV // groups
    q_all = dwq_ref.shape[0]
    sh = Swap(lambda peer: dkv_scr.at[seg(peer, tokens), :], lambda o: shares.at[o], sems[4:6], me)
    gq = row_gather(dq_scr, full, sems[6:10], me)
    parts = thirds(dkv_own.shape[0], STRIP)
    gk = Gather(dkv_own, lambda o: full_kv.at[:, seg(o, tokens)], lambda view, c: [view.at[pl.ds(*parts[c]), :]], sems[10:14], me)
    gs = Swap(lambda peer: gains.at[:, seg(peer)], lambda o: gains_in.at[o], sems[14:], me)
    sh.start()
    gq.start()
    keep_own(dq_scr, full, me)
    shares[me] = dkv_scr[seg(me, tokens), :]
    sh.wait_recv()
    cos, sin = cos_ref[...], sin_ref[...]
    for k in range(groups):
        both = sum(shares[per * k + i].astype(F32) for i in range(per)).astype(BF16).astype(F32).T
        p, q = both[:half], both[half:hd]
        lo = 2 * hd * k
        dkv_own[lo:lo + half, :] = (p * cos + q * sin).astype(BF16)
        dkv_own[lo + half:lo + hd, :] = (q * cos - p * sin).astype(BF16)
        dkv_own[lo + hd:lo + 2 * hd, :] = both[hd:].astype(BF16)
    gk.start()
    full_kv[:, seg(me, tokens)] = dkv_own[...]
    for k in range(groups):
        dqkv[:, q_all + 2 * hd * k:q_all + 2 * hd * (k + 1)] = dkv_own[2 * hd * k:2 * hd * (k + 1), :].T

    def use(mask):
        gq.wait_pair(mask)
        chip = flipped(me, mask) // 2
        dwq_ref[seg(chip, WIDE), :] = mm(full[chip], ucol_ref[...], NN)
        dqkv[:, seg(chip, WIDE)] = full[chip, :, seg(me, tokens)].T

    for r in range(len(gq.ROUNDS)):
        gq.round(r)
        gk.round(r)
        if r == 3:
            advance(3)
        for mask in gq.READY[r]:
            use(mask)
    load.wait()

    def normed(i):
        dn[:, seg(i, WIDE)] = mm(dqkv[...], w_scr[i], NN)
    loop(N_CHIP, normed)
    norm_back(dn, x_ref, g_scr, dh_ref, dx_ref, dg1)
    gains[...] = jnp.concatenate([jnp.sum(dg1[...], axis=0, keepdims=True), jnp.sum(dg2_ref[...], axis=0, keepdims=True),
                                  jnp.zeros((N_CHIP - 2, dg1.shape[1]), F32)], axis=0)
    gs.start()
    gains_in[me] = gains[:, seg(me)]
    for mask in CHIP_MASKS:
        gk.wait_pair(mask)
    dwkv_ref[...] = mm(full_kv[...], ucol_ref[...], NN)
    gs.wait_recv()
    gain_ref[...] = sum(gains_in[o] for o in range(N_DEV))
    for swap in (gates, ups):
        swap.wait_recv()
        swap.wait_send((CORE,) + SETS[3])
    for copy in own:
        copy.wait()
    for c in (sh, gs):
        c.wait_send()
    for g in (gq, gk):
        g.finish()


def finish(dg_hbm, du_hbm, dkv_hbm, *refs):
    n = (len(refs) - 11) // 3
    srcs, (gate, up, dk, dv), dsts = refs[:n], refs[n:n + 4], refs[n + 4:2 * n + 4]
    (g_in, g_out, kv_in), holds, sems = refs[2 * n + 4:2 * n + 7], refs[2 * n + 7:3 * n + 7], refs[3 * n + 7:]
    t_in, t_out, p_in, p_out = sems
    step = LANE * 11
    cols = g_in.shape[1]
    hd = dk.shape[0] // (kv_in.shape[0] // LANE)
    starts = [(w, i) for i in range(cols // step) for w in range(2)]

    def fetch(w, i):
        rs = pl.ds(i * step, step)
        return pltpu.make_async_copy((dg_hbm, du_hbm)[w].at[rs, :], g_in.at[w, rs, :], t_in.at[w, i])

    def put(w, i):
        cs = pl.ds(i * step, step)
        return pltpu.make_async_copy(g_out.at[w, :, cs], (gate, up)[w].at[:, cs], t_out.at[w, i])
    moves = [(pltpu.make_async_copy(a, h, p_in.at[k]), pltpu.make_async_copy(h, b, p_out.at[k])) for k, (a, h, b) in enumerate(zip(srcs, holds, dsts))]
    kv = pltpu.make_async_copy(dkv_hbm, kv_in, p_in.at[n])
    for w, i in starts:
        fetch(w, i).start()
    kv.start()
    for load, _ in moves:
        load.start()
    for w, i in starts:
        fetch(w, i).wait()

        at = pl.ds(i * step, step)
        g_out[w, :, at] = g_in[w, at, :].T
        put(w, i).start()
    kv.wait()
    for k in range(dk.shape[0] // hd):
        for i, ref in enumerate((dk, dv)):
            ref[k * hd:(k + 1) * hd, :] = kv_in[(2 * k + i) * hd:(2 * k + i + 1) * hd, :]
    for load, store in moves:
        load.wait()
        store.start()
    for w, i in starts:
        put(w, i).wait()
    for _, store in moves:
        store.wait()


def rope_tables(positions, head_dim):
    half_dim = head_dim // 2
    inv_freq = 1.0 / (ROPE_BASE ** (jnp.arange(half_dim, dtype=F32) * (2.0 / head_dim)))
    angles = positions.astype(F32)[None, :] * inv_freq[:, None]
    return jnp.cos(angles), jnp.sin(angles)


def solution(mesh):
    assert mesh.shape['sp'] == N_DEV

    def layer_step(x_in, positions, d_out, norm1_gain, norm2_gain, w_q, w_k, w_v, w_o, w_gate, w_up, w_down):
        tokens, dim = x_in.shape
        seq = tokens * N_DEV
        n_q, hd = w_q.shape[1:]
        n_kv = w_k.shape[1]
        qw = n_q // N_DEV * hd
        rows = w_q.shape[0]
        feat = w_down.shape[0]
        cols = (n_q + 2 * n_kv) * hd
        lanes = qw // hd * QB
        vm = pltpu.VMEM
        full = vm((N_CHIP, WIDE, dim), BF16)
        gain_scr = vm((N_CHIP, dim), F32)
        small_shape = ((N_DEV, N_CHIP, rows), F32)

        cos_own, sin_own = rope_tables(positions, hd)
        row = lambda v: v.reshape(1, rows)
        by_head = lambda w: w.transpose(1, 2, 0).reshape(-1, rows)
        wo_own = w_o.reshape(qw, dim)

        args = (x_in, row(norm1_gain), row(norm2_gain), row(positions), by_head(w_q), by_head(w_k), by_head(w_v), cos_own, sin_own, w_gate, w_up)
        qkv, u_col, small_all, wqkv, attn_tok, attn_t, stat, wgu = call(
            functools.partial(head, n_kv, hd), 0, len(args),
            (((qw + 2 * hd, seq), BF16), ((seq, rows), BF16), small_shape, ((N_CHIP, cols, WIDE), BF16),
             ((n_q * hd, tokens), BF16), ((qw, seq), BF16), ((seq // QB, 2, lanes), F32), ((2 * feat, dim), BF16)),
            [vm((N_CHIP, rows), F32), vm((cols, rows), BF16), vm((N_CHIP, cols, WIDE), BF16), vm((cols, tokens), F32), vm((cols, tokens), BF16), vm((tokens, dim), BF16), gain_scr,
             vm((feat * N_DEV, rows), BF16), vm((feat * N_DEV, rows), BF16), vm((seq, lanes), F32), vm((seq, hd), BF16), dma(N_CHIP),
             *Gather.sems, *(7 * Swap.sems)], 4 * qw * seq * seq, far_out=(3,))(*args)
        args = (attn_tok, wo_own, x_in, small_all, d_out, wgu, w_down)
        hidden, m_full, glu, dgu, d_down = call(
            mlp_local, 2, len(args),
            (((tokens, dim), BF16), ((N_CHIP, WIDE, dim), BF16), ((feat, seq), BF16), ((2 * feat, seq), BF16), ((feat, dim), F32)),
            [vm((2 * feat, dim), BF16), vm((feat, dim), BF16), vm((feat, seq), BF16), vm((2 * feat, seq), BF16), dma(2),
             full, full, full, vm((tokens, dim), F32), vm((tokens, dim), BF16), vm((tokens, n_q * hd), BF16), gain_scr, dma(N_CHIP, 3), *(3 * Gather.sems)],
            8 * feat * seq * dim, far_in=(5, 6), far_out=(1, 2, 3))(*args)
        args = (dgu, wgu, hidden, small_all, d_out, wo_own, attn_t, glu, w_down)
        y_out, d_hidden, d_attn, d_wo, d_g2 = call(
            mlp_back, 3, len(args),
            (((tokens, dim), BF16), ((tokens, dim), BF16), ((qw, seq), BF16), ((qw, dim), F32), ((N_CHIP, dim), F32)),
            [vm((2 * feat, seq), BF16), vm((2 * feat, dim), BF16), vm((feat, seq), BF16), vm((feat, dim), BF16), dma(4),
             full, gain_scr, vm((WIDE, 2 * feat), BF16), vm((WIDE, feat), BF16), pltpu.SemaphoreType.REGULAR,
             *Scatter.scratch(tokens, dim), *Scatter.sems, *Gather.sems], 4 * feat * seq * dim, far_in=(0, 1, 7, 8))(*args)
        cos_all, sin_all = rope_tables(small_all[:, 2].reshape(-1), hd)
        args = (qkv, d_attn, stat, cos_all, sin_all, dgu, m_full, u_col, cos_own, sin_own, wqkv, x_in, small_all, d_hidden, d_g2)
        d_gate_t, d_up_t, d_wq, d_wkv, d_x, gains = call(
            functools.partial(back, n_kv, hd), 4, len(args),
            (((feat * N_DEV, rows), F32), ((feat * N_DEV, rows), F32),
             ((n_q * hd, rows), F32), ((2 * n_kv * hd, rows), F32), ((tokens, dim), BF16), ((N_CHIP, rows), F32)),
            [vm((seq, lanes), F32), vm((seq, lanes), BF16), vm((seq, hd), BF16), vm((seq, hd), BF16), vm((seq, hd), F32), vm((seq, hd), F32),
             vm((N_CHIP, 2 * feat, WIDE), F32), vm((qw, seq), BF16), vm((seq, 2 * hd), BF16), full,
             full, vm((N_CHIP, cols, WIDE), BF16), vm((N_DEV, tokens, 2 * hd), BF16), vm((2 * n_kv * hd, tokens), BF16), vm((2 * n_kv * hd, seq), BF16),
             vm((tokens, cols), BF16), vm((tokens, dim), F32), gain_scr, gain_scr, gain_scr, vm((N_DEV, N_CHIP, rows), F32), dma(), dma(2), dma(N_CHIP),
             *(3 * Swap.sems), *(2 * Gather.sems), *Swap.sems], 10 * qw * seq * seq, far_in=(6, 10), far_out=(0, 1))(*args)
        moved = (d_wq, d_wo, d_down, d_x, y_out, gains)
        half_kv = jax.ShapeDtypeStruct((n_kv * hd, rows), F32)
        wide = jax.ShapeDtypeStruct((rows, feat * N_DEV), F32)
        d_gate, d_up, d_wk, d_wv, d_wq, d_wo, d_down, d_x, y_out, gains = pl.pallas_call(
            finish,
            out_shape=[wide, wide, half_kv, half_kv] + [jax.ShapeDtypeStruct(v.shape, v.dtype) for v in moved],
            in_specs=[IN_HBM] * (3 + len(moved)), out_specs=[IN_HBM] * 2 + on_chip(2) + [IN_HBM] * len(moved),
            scratch_shapes=[vm((2, feat * N_DEV, rows), F32), vm((2, rows, feat * N_DEV), F32), vm(d_wkv.shape, F32)]
            + [vm(v.shape, v.dtype) for v in moved] + [dma(2, 4), dma(2, 4), dma(len(moved) + 1), dma(len(moved))],
            compiler_params=pltpu.CompilerParams(vmem_limit_bytes=VMEM_CAP), name='finish',
        )(d_gate_t, d_up_t, d_wkv, *moved)
        by_row = lambda g, heads: g.reshape(heads, hd, rows).transpose(2, 0, 1)
        return (y_out, d_x, gains[0], gains[1], by_row(d_wq, n_q), by_row(d_wk, n_kv), by_row(d_wv, n_kv),
                d_wo.reshape(w_o.shape), d_gate, d_up, d_down)

    all_rows = P('sp')
    return jax.shard_map(layer_step, mesh=mesh, in_specs=(all_rows,) * 12, out_specs=(all_rows,) * 11, check_vma=False)
```

```python
import functools
import jax
import jax.numpy as jnp
from jax import lax
from jax.experimental import pallas as pl
from jax.experimental.pallas import tpu as pltpu
from jax.sharding import PartitionSpec as P

ROPE_BASE = 10000.0
NORM_EPS = 1e-5
NEG_LARGE = -1e30
F32 = jnp.float32
BF16 = jnp.bfloat16
N_DEV, N_CHIP, LANE, WIDE, CHUNK, STRIP = 16, 8, 128, 256, 512, 16
NT = (((1,), (1,)), ((), ()))
TN = (((0,), (0,)), ((), ()))
NN = (((1,), (0,)), ((), ()))
MESH = pl.DeviceIdType.MESH
VMEM_CAP = 62 * 1024 * 1024

CORE, X, Y, Z = 1, 2, 4, 8
XYZ = X + Y + Z
ORDERS = ((X, Y, Z), (Y, Z, X), (Z, X, Y))
CHIP_MASKS = (0, X, Y, Z, X + Y, X + Z, Y + Z, XYZ)
NEAR = (CORE, X, Y, Z)
OTHERS = range(1, N_DEV)
SETS = tuple(tuple(m + c for m in masks for c in (0, CORE)) for masks in ((XYZ,), (X, Y + Z), (Y, X + Z), (Z, X + Y)))
COLOURS = range(len(ORDERS))


def mm(a, b, dims):
    return lax.dot_general(a, b, dims, preferred_element_type=F32)


def seg(index, width=LANE):
    return pl.ds(pl.multiple_of(index * width, width), width)


def loop(count, body):
    lax.fori_loop(0, count, lambda i, c: (body(i), c)[1], 0)


def differing(index, mask):
    return sum(((index // bit + mask // bit) % 2) * bit for bit in NEAR)


def flipped(index, mask):
    out = index
    for bit in NEAR:
        if mask & bit:
            out = out + (1 - 2 * ((index // bit) % 2)) * bit
    return out


def thirds(total, unit):
    n = total // unit
    first = (n + 2) // 3
    second = (n - first + 1) // 2
    sizes = (first * unit, second * unit, (n - first - second) * unit)
    return ((0, sizes[0]), (sizes[0], sizes[1]), (sizes[0] + sizes[1], sizes[2]))


def pieces(rows, cols, unit):
    share = cols // LANE // 3 * LANE
    strips = thirds(rows, unit)
    rest = cols - 3 * share
    return [[(pl.ds(0, rows), pl.ds(c * share, share)), (pl.ds(*strips[c]), pl.ds(3 * share, rest))] for c in COLOURS]


def enter(me, masks):
    barrier = pltpu.get_barrier_semaphore()
    for mask in masks:
        pl.semaphore_signal(barrier, inc=1, device_id=(flipped(me, mask),), device_id_type=MESH)
    pl.semaphore_wait(barrier, len(masks))


def remote(src, dst, send, recv, peer):
    return pltpu.make_async_remote_copy(src_ref=src, dst_ref=dst, send_sem=send, recv_sem=recv, device_id=(peer,), device_id_type=MESH)


def dma(*shape):
    return pltpu.SemaphoreType.DMA(shape)


class Swap:
    sems = (dma(N_DEV), dma(N_DEV))

    def __init__(self, src, dst, sems, me):
        self.src, self.dst, (self.send, self.recv), self.me = src, dst, sems, me

    def copy(self, mask):
        peer = differing(self.me, mask)
        return remote(self.src(peer), self.dst(self.me), self.send.at[mask], self.recv.at[mask], peer)

    def arrival(self, mask):
        view = self.dst(differing(self.me, mask))
        return remote(view, view, self.send.at[mask], self.recv.at[mask], self.me)

    def each(self, masks, act):
        if masks is None:
            loop(N_DEV - 1, lambda i: act(i + 1))
        else:
            for mask in masks:
                act(mask)

    def start(self, masks=None):
        self.each(masks, lambda mask: self.copy(mask).start())

    def advance(self, n):
        if n:
            self.wait_send(SETS[n - 1])
        self.start(SETS[n])

    def wait_recv(self, masks=None):
        self.each(masks, lambda mask: self.arrival(mask).wait_recv())

    def wait_send(self, masks=None):
        self.each(masks, lambda mask: self.copy(mask).wait_send())


class Gather:
    ROUNDS = ((0,), (1,), (2,), (0, 1), (0, 2), (1, 2), (0, 1, 2))
    READY = ((0,), (), (), (X, Y), (Z,), (X + Y, X + Z), (Y + Z, XYZ))
    sems = (dma(3, N_CHIP, 3, 2), dma(3, N_CHIP, 2), dma(N_CHIP), dma(N_CHIP))

    def __init__(self, own, block, cut, sems, me):
        self.own, self.block, self.cut, self.me = own, block, cut, me
        self.send, self.recv, self.pair_send, self.pair_recv = sems

    def source(self, mask):
        return self.block(flipped(self.me, mask)) if mask else self.own

    def unit(self, colour, mask, axis):
        ends = zip(self.cut(self.source(mask), colour), self.cut(self.block(flipped(self.me, mask)), colour))
        return [remote(src, dst, self.send.at[colour, mask // 2, ORDERS[colour].index(axis), i], self.recv.at[colour, (mask + axis) // 2, i],
                       flipped(self.me, axis)) for i, (src, dst) in enumerate(ends)]

    def start_unit(self, colour, mask, axis):
        for copy in self.unit(colour, mask, axis):
            copy.start()

    def pair(self, mask):
        return remote(self.source(mask), self.block(flipped(self.me, mask)), self.pair_send.at[mask // 2],
                      self.pair_recv.at[mask // 2], flipped(self.me, CORE))

    def wait_pair(self, mask):
        view = self.block(flipped(self.me, mask + CORE))
        remote(view, view, self.pair_send.at[mask // 2], self.pair_recv.at[mask // 2], self.me).wait_recv()

    def onward(self, colour):
        order = ORDERS[colour]
        for picks in self.ROUNDS:
            for axis in order[picks[-1] + 1:]:
                yield picks, sum(order[p] for p in picks), axis

    def start(self):
        for pos in COLOURS:
            for colour in COLOURS:
                self.start_unit(colour, 0, ORDERS[colour][pos])
        self.pair(0).start()

    def round(self, r):
        for colour in COLOURS:
            mask = sum(ORDERS[colour][p] for p in self.ROUNDS[r])
            for i, view in enumerate(self.cut(self.block(flipped(self.me, mask)), colour)):
                remote(view, view, self.send.at[colour, 0, 0, i], self.recv.at[colour, mask // 2, i], self.me).wait_recv()
            for picks, at, axis in self.onward(colour):
                if picks == self.ROUNDS[r]:
                    self.start_unit(colour, at, axis)
        for mask in {2: (X, Y, Z), 5: (X + Y, X + Z, Y + Z), 6: (XYZ,)}.get(r, ()):
            self.pair(mask).start()

    def finish(self):
        for colour in COLOURS:
            for at, axis in [(0, axis) for axis in ORDERS[colour]] + [step[1:] for step in self.onward(colour)]:
                for copy in self.unit(colour, at, axis):
                    copy.wait_send()
        for mask in CHIP_MASKS:
            self.pair(mask).wait_send()


def row_gather(own, full, sems, me, extra=None):
    rows, width = own.shape
    parts = pieces(rows, width, STRIP)
    if extra is not None:
        share = width // LANE // 3 * LANE
        more = width - 3 * share
        parts = [[(pl.ds(0, rows), pl.ds(c * share + more * (c > extra), share + more * (c == extra)))] for c in COLOURS]

    def block(o):
        return full.at[o // 2, seg(o % 2), :]

    return Gather(own, block, lambda view, c: [view.at[rs, cs] for rs, cs in parts[c]], sems, me)


def keep_own(own, full, me):
    def step(i):
        full[me // 2, pl.ds(pl.multiple_of((me % 2) * LANE + i * STRIP, STRIP), STRIP), :] = own[seg(i, STRIP), :]
    loop(LANE // STRIP, step)


class Scatter:
    ORDER = (XYZ, X + Y, Y + Z, X + Z, X, Y, Z, 0)
    sems = (dma(N_CHIP), dma(N_CHIP), dma(3, N_CHIP, 2), dma(3, N_CHIP, 2))

    @staticmethod
    def scratch(tokens, dim):
        return [pltpu.VMEM((N_CHIP, 2, tokens, dim), F32), pltpu.VMEM((N_CHIP, tokens, dim), F32), pltpu.VMEM((N_CHIP - 1, tokens, dim), F32)]

    def __init__(self, part, pair_in, link_in, sems, me):
        self.part, self.pair_in, self.link_in, self.me = part, pair_in, link_in, me
        self.pair_send, self.pair_recv, self.link_send, self.link_recv = sems
        self.core = me % 2
        self.tokens, self.dim = part.shape[2:]
        self.pieces = pieces(self.tokens, self.dim, STRIP // 2)
        self.ready, self.sent = set(), [0] * len(ORDERS)

    @staticmethod
    def first(colour, mask):
        return next((i for i, a in enumerate(ORDERS[colour]) if mask & a), 3)

    def slot(self, colour, mask, axis):
        slots = [(m, a) for m in self.ORDER for a in ORDERS[colour][:self.first(colour, m)]]
        return slots.index((mask, axis))

    def pair(self, i):
        return remote(self.part.at[i, 1 - self.core], self.pair_in.at[i], self.pair_send.at[i], self.pair_recv.at[i], flipped(self.me, CORE))

    def link(self, colour, mask):
        axis = ORDERS[colour][self.first(colour, mask)]
        slot = self.slot(colour, mask - axis, axis)
        i = self.ORDER.index(mask)
        return [remote(self.part.at[i, self.core, rs, cs], self.link_in.at[slot, rs, cs], self.link_send.at[colour, i, k],
                       self.link_recv.at[colour, slot, k], flipped(self.me, axis)) for k, (rs, cs) in enumerate(self.pieces[colour])]

    def start_link(self, colour, mask):
        for copy in self.link(colour, mask):
            copy.start()

    def add(self, mask, ref, cs):
        i = self.ORDER.index(mask)

        def step(r):
            rs = seg(r, STRIP)
            self.part[i, self.core, rs, cs] += ref[rs, cs]
        loop(self.tokens // STRIP, step)

    def finish_pair(self, i):
        self.pair(i).wait_recv()
        self.add(self.ORDER[i], self.pair_in.at[i], pl.ds(0, self.dim))
        self.ready.add(self.ORDER[i])
        for colour in COLOURS:
            a, b, c = ORDERS[colour]
            todo = (XYZ, a + b, a + c, a)
            while self.sent[colour] < len(todo) and todo[self.sent[colour]] in self.ready:
                self.start_link(colour, todo[self.sent[colour]])
                self.sent[colour] += 1

    def take(self, colour, mask, axis):
        for copy in self.link(colour, mask + axis):
            copy.wait_recv()
        ref = self.link_in.at[self.slot(colour, mask, axis)]
        (_, wide), (rs, cs) = self.pieces[colour]
        self.add(mask, ref, wide)
        self.part[self.ORDER.index(mask), self.core, rs, cs] += ref[rs, cs]

    def run(self, product, between=lambda i: None):
        for i, mask in enumerate(self.ORDER):
            product(i, flipped(self.me, mask) // 2)
            self.pair(i).start()
            if i:
                self.finish_pair(i - 1)
            between(i)
        self.finish_pair(N_CHIP - 1)
        for step in range(2):
            for colour in COLOURS:
                a, b, c = ORDERS[colour]
                mask = (b + c, b)[step]
                self.take(colour, mask, a)
                self.start_link(colour, mask)
        for colour in COLOURS:
            a, b, c = ORDERS[colour]
            self.take(colour, c, a)
            self.take(colour, c, b)
            self.start_link(colour, c)
        for colour in COLOURS:
            for axis in ORDERS[colour]:
                self.take(colour, 0, axis)
        return self.part.at[N_CHIP - 1, self.core]

    def finish(self):
        for i in range(N_CHIP):
            self.pair(i).wait_send()
        for colour in COLOURS:
            for mask in self.ORDER[:-1]:
                for copy in self.link(colour, mask):
                    copy.wait_send()


def block_product(part, a_ref, w_ref, a_t):
    tokens = part.shape[2]

    def product(i, chip):
        a_t[...] = a_ref[:, seg(chip, 2 * tokens)].T

        def step(n):
            cs = seg(n, CHUNK)
            r = mm(a_t[...], w_ref[:, cs], NN)
            part[i, 0, :, cs] = r[:tokens]
            part[i, 1, :, cs] = r[tokens:]
        loop(part.shape[3] // CHUNK, step)
    return product


def on_chip(n):
    return [pl.BlockSpec(memory_space=pltpu.VMEM)] * n


IN_HBM = pl.BlockSpec(memory_space=pl.ANY)


def call(kernel, ident, args, outs, scratch, flops, far_in=(), far_out=(), aliases={}):
    specs = [IN_HBM if i in far_in else on_chip(1)[0] for i in range(args)]
    out_specs = [IN_HBM if i in far_out else on_chip(1)[0] for i in range(len(outs))]
    return pl.pallas_call(
        kernel,
        out_shape=[jax.ShapeDtypeStruct(shape, dtype) for shape, dtype in outs],
        in_specs=specs, out_specs=out_specs, scratch_shapes=scratch, input_output_aliases=aliases,
        cost_estimate=pl.CostEstimate(flops=flops, bytes_accessed=flops // CHUNK, transcendentals=0),
        compiler_params=pltpu.CompilerParams(collective_id=ident, has_side_effects=True, vmem_limit_bytes=VMEM_CAP),
        name=kernel.func.__name__ if isinstance(kernel, functools.partial) else kernel.__name__,
    )


def fetch_all(sem, *pairs):
    copies = [pltpu.make_async_copy(src, dst, sem.at[i]) for i, (src, dst) in enumerate(pairs)]
    for copy in copies:
        copy.start()
    return copies


def gain_row(dst, small_all, which):
    for o in range(N_DEV):
        dst[:1, o * LANE:(o + 1) * LANE] = small_all[o, which:which + 1, :]


def norm_rows(src, gain, dst):
    def step(i):
        rs = seg(i, STRIP)
        t = src[rs, :].astype(F32)
        dst[rs, :] = (t * lax.rsqrt(jnp.mean(t * t, axis=-1, keepdims=True) + NORM_EPS) * gain[:1, :]).astype(BF16)
    loop(src.shape[0] // STRIP, step)


def norm_back(dy, src, gain, skip, dst, dgain):
    def step(i):
        rs = seg(i, STRIP)
        d = dy[rs, :].astype(BF16).astype(F32)
        t = src[rs, :].astype(F32)
        inv = lax.rsqrt(jnp.mean(t * t, axis=-1, keepdims=True) + NORM_EPS)
        gd = gain[:1, :] * d
        pull = jnp.mean(gd * t, axis=-1, keepdims=True)
        dst[rs, :] = (skip[rs, :].astype(F32) + (inv * gd - t * (inv * inv * inv * pull))).astype(BF16)
        g = d * (t * inv)
        dgain[...] += g[:N_CHIP] + g[N_CHIP:]
    dgain[...] = jnp.zeros_like(dgain)
    loop(src.shape[0] // STRIP, step)


QB = 256
KB = 256


def key_rows(dst, src, lo, hd):
    def step(i):
        dst[seg(i, KB), :] = src[lo:lo + hd, seg(i, KB)].T
    loop(src.shape[1] // KB, step)


def score_block(k, q2, scale, diagonal):
    s = mm(k, q2, NN) * scale
    if diagonal:
        key = lax.broadcasted_iota(jnp.int32, s.shape, 0)
        qry = lax.broadcasted_iota(jnp.int32, s.shape, 1) % QB
        s = jnp.where(qry >= key, s, NEG_LARGE)
    return s


def side_by_side(ref, heads, hd, qs):
    return jnp.concatenate([ref[h * hd:(h + 1) * hd, qs] for h in range(heads)], axis=1)


def head(groups, hd, x_ref, g1_ref, g2_ref, pos_ref, wq_ref, wk_ref, wv_ref, cos_ref, sin_ref, wg_ref, wu_ref, wo_ref, qkv_ref, ucol_ref, small_all, w_out, o_ref, stat_ref, wgu_ref, h_ref, m_ref,
         full_w, acc_o, o_tok, o_send, small_ref, w_ref, full, acc, rot, u_scr, g_scr, wg_t, wu_t, s_scr, k_scr, osem, *sems):
    me = lax.axis_index('sp')
    tokens, dim = x_ref.shape
    cols = w_ref.shape[0]
    small_ref[...] = jnp.concatenate([r[...].astype(F32) for r in (g1_ref, g2_ref, pos_ref)] + [jnp.zeros((N_CHIP - 3, LANE), F32)], axis=0)
    w_ref[:wq_ref.shape[0], :] = wq_ref[...]
    for k in range(groups):
        for i, ref in enumerate((wk_ref, wv_ref)):
            w_ref[pl.ds(wq_ref.shape[0] + (2 * k + i) * hd, hd), :] = ref[k * hd:(k + 1) * hd, :]
    qw = tokens
    q_all = N_DEV * qw
    gsems, ssems, usems, qsems, ksems, gate_sems, up_sems, osems = sems[:4], *(sems[i:i + 2] for i in range(4, len(sems) - 4, 2))
    gw = row_gather(wo_ref, full_w, sems[-4:], me, 1)
    feat = wg_ref.shape[1] // N_DEV
    enter(me, OTHERS)
    smalls = Swap(lambda peer: small_ref, lambda o: small_all.at[o], ssems, me)
    smalls.start()
    parts = thirds(cols, STRIP)
    g = Gather(w_ref, lambda o: full.at[o // 2, :, seg(o % 2)], lambda view, c: [view.at[pl.ds(*parts[c]), :]], gsems, me)
    g.start()
    gates = Swap(lambda peer: wg_t.at[seg(peer, feat), :], lambda o: wgu_ref.at[:feat, seg(o)], gate_sems, me)
    ups = Swap(lambda peer: wu_t.at[seg(peer, feat), :], lambda o: wgu_ref.at[feat:, seg(o)], up_sems, me)

    def advance(n):
        gates.advance(n)
        ups.advance(n)

    def transpose(i):
        wg_t[seg(i, CHUNK), :] = wg_ref[:, seg(i, CHUNK)].T
        wu_t[seg(i, CHUNK), :] = wu_ref[:, seg(i, CHUNK)].T
    loop(wg_ref.shape[1] // CHUNK, transpose)
    advance(0)

    def own_block(i):
        full[me // 2, seg(i, WIDE), seg(me % 2)] = w_ref[seg(i, WIDE), :]
    loop(cols // WIDE, own_block)
    acc[...] = jnp.zeros_like(acc)
    small_all[me] = small_ref[...]
    smalls.wait_recv()
    gain_row(g_scr, small_all, 0)
    norm_rows(x_ref, g_scr, u_scr)
    ucols = Swap(lambda peer: u_scr.at[:, seg(peer)], lambda o: ucol_ref.at[seg(o, tokens), :], usems, me)

    def keep(mask):
        chip = flipped(me, mask) // 2
        return pltpu.make_async_copy(full.at[chip], w_out.at[chip], osem.at[mask // 2])

    def use(mask):
        g.wait_pair(mask)
        keep(mask).start()
        chip = flipped(me, mask) // 2
        u = u_scr[:, seg(chip, WIDE)]

        def step(i):
            rs = seg(i, cols // 2)
            acc[rs, :] += mm(full[chip, rs, :], u, NT)
        loop(2, step)

    for r in range(len(g.ROUNDS)):
        g.round(r)
        if r in (1, 3, 5):
            advance((r + 1) // 2)
        for mask in g.READY[r]:
            use(mask)

    half = hd // 2
    cos, sin = cos_ref[...], sin_ref[...]

    def turn(h):
        first = seg(2 * h, half)
        second = seg(2 * h + 1, half)
        p = acc[first, :].astype(BF16).astype(F32)
        q = acc[second, :].astype(BF16).astype(F32)
        rot[first, :] = (p * cos - q * sin).astype(BF16)
        rot[second, :] = (q * cos + p * sin).astype(BF16)
    loop(q_all // hd, turn)
    for k in range(groups):
        turn(q_all // hd + 2 * k)
        vs = seg(q_all // hd + 2 * k + 1, hd)
        rot[vs, :] = acc[vs, :].astype(BF16)
    per = N_DEV // groups
    q_rows = lambda peer: seg(peer, qw)
    kv_rows = lambda peer: seg(q_all // (2 * hd) + peer // per, 2 * hd)
    qs = Swap(lambda peer: rot.at[q_rows(peer), :], lambda o: qkv_ref.at[:qw, seg(o, tokens)], qsems, me)
    kvs = Swap(lambda peer: rot.at[kv_rows(peer), :], lambda o: qkv_ref.at[qw:, seg(o, tokens)], ksems, me)
    qs.start()
    kvs.start()
    ucols.start()
    gw.start()
    keep_own(wo_ref, full_w, me)
    gain_row(g_scr, small_all, 1)
    qkv_ref[:qw, seg(me, tokens)] = rot[q_rows(me), :]
    qkv_ref[qw:, seg(me, tokens)] = rot[kv_rows(me), :]
    ucol_ref[seg(me, tokens), :] = u_scr[:, seg(me)]
    wgu_ref[:feat, seg(me)] = wg_t[seg(me, feat), :]
    wgu_ref[feat:, seg(me)] = wu_t[seg(me, feat), :]
    gates.start((CORE,))
    ups.start((CORE,))
    for swap in (qs, kvs):
        swap.wait_recv()
    heads = qkv_ref.shape[0] // hd - 2
    seq = qkv_ref.shape[1]
    scale = hd ** -0.5
    lanes = heads * QB
    key_rows(k_scr, qkv_ref, qw, hd)

    outs = Swap(lambda peer: o_send.at[seg(peer), :], lambda o: o_tok.at[:, seg(o)], osems, me)

    def q_block(qb):
        for at, r in ((2, 0), (4, 1), (5, 2), (6, 3), (7, 4)):
            @pl.when(qb == at)
            def _():
                gw.round(r)
        qs = seg(qb, QB)
        q2 = side_by_side(qkv_ref, heads, hd, qs)

        def scores(kb, top, diagonal):
            s = score_block(k_scr[seg(kb, KB), :], q2, scale, diagonal)
            s_scr[seg(kb, KB), :] = s
            return jnp.maximum(top, jnp.max(s, axis=0, keepdims=True))

        top = lax.fori_loop(0, qb, lambda kb, t: scores(kb, t, False), jnp.full((1, lanes), NEG_LARGE, F32))
        top = scores(qb, top, True)

        def expo(kb, tot):
            e = jnp.exp(s_scr[seg(kb, KB), :] - top)
            s_scr[seg(kb, KB), :] = e
            return tot + jnp.sum(e, axis=0, keepdims=True)

        inv = 1.0 / lax.fori_loop(0, qb + 1, expo, jnp.zeros((1, lanes), F32))

        def weigh(kb, acc):
            p = (s_scr[seg(kb, KB), :] * inv).astype(BF16)
            return acc + mm(qkv_ref[qw + hd:, seg(kb, KB)], p, NN)

        acc = lax.fori_loop(0, qb + 1, weigh, jnp.zeros((hd, lanes), F32))
        for h in range(heads):
            o_ref[h * hd:(h + 1) * hd, qs] = acc[:, h * QB:(h + 1) * QB].astype(BF16)
        stat_ref[qb, :1, :] = top
        stat_ref[qb, 1:, :] = inv
        o_send[qs, :] = o_ref[:, qs].T

    loop(seq // QB, q_block)
    outs.start()
    o_tok[:, seg(me)] = o_send[seg(me), :]
    for r in (5, 6):
        gw.round(r)
    outs.wait_recv()
    for mask in CHIP_MASKS:
        gw.wait_pair(mask)

    def project(n):
        cs = seg(n, CHUNK)
        acc_o[:, cs] = mm(o_tok[...], full_w[:, :, cs].reshape(dim, CHUNK), NN)
    loop(dim // CHUNK, project)

    def residual(i):
        rs = seg(i, STRIP)
        h_ref[rs, :] = (x_ref[rs, :].astype(F32) + acc_o[rs, :]).astype(BF16)
    loop(tokens // STRIP, residual)
    norm_rows(h_ref, g_scr, m_ref)
    for swap in (gates, ups, ucols):
        swap.wait_recv()
    for mask in CHIP_MASKS:
        keep(mask).wait()
    outs.wait_send()
    for swap in (gates, ups):
        swap.wait_send((CORE,) + SETS[3])
    g.finish()
    gw.finish()
    for swap in (smalls, ucols, qs, kvs):
        swap.wait_send()


def mlp_local(m_ref, dout_ref, wgu_hbm, down_hbm, m_out, glu_out, dgu_out, ddown_ref,
              wgu_ref, down_ref, glu_ref, dgu_ref, isem, full_d, full_m, osem, *sems):
    me = lax.axis_index('sp')
    feat, dim = down_ref.shape
    loads = fetch_all(isem, (wgu_hbm, wgu_ref), (down_hbm, down_ref))
    enter(me, NEAR)
    gd = row_gather(dout_ref, full_d, sems[:4], me, 0)
    gm = row_gather(m_ref, full_m, sems[4:], me, 2)
    gm.start()
    gd.start()
    keep_own(m_ref, full_m, me)
    keep_own(dout_ref, full_d, me)
    ddown_ref[...] = jnp.zeros_like(ddown_ref)

    def keep(mask):
        chip = flipped(me, mask) // 2
        ts = seg(chip, WIDE)
        ends = ((full_m.at[chip], m_out.at[chip]), (glu_ref.at[:, ts], glu_out.at[:, ts]), (dgu_ref.at[:, ts], dgu_out.at[:, ts]))
        return [pltpu.make_async_copy(src, dst, osem.at[mask // 2, i]) for i, (src, dst) in enumerate(ends)]

    for load in loads:
        load.wait()

    def use(mask):
        gd.wait_pair(mask)
        gm.wait_pair(mask)
        chip = flipped(me, mask) // 2
        ts = seg(chip, WIDE)
        gu = mm(wgu_ref[...], full_m[chip], NT).astype(BF16).astype(F32)
        gate, up = gu[:feat], gu[feat:]
        d_glu = mm(down_ref[...], full_d[chip], NT).astype(BF16).astype(F32)
        sig = jax.nn.sigmoid(gate)
        act = gate * sig
        glu = (act * up).astype(BF16)
        glu_ref[:, ts] = glu
        dgu_ref[:feat, ts] = (d_glu * up * (sig * (1.0 + gate * (1.0 - sig)))).astype(BF16)
        dgu_ref[feat:, ts] = (d_glu * act).astype(BF16)

        def step(n):
            ddown_ref[:, seg(n, CHUNK)] += mm(glu, full_d[chip, :, seg(n, CHUNK)], NN)
        loop(dim // CHUNK, step)
        for copy in keep(mask):
            copy.start()

    for r in range(len(gm.ROUNDS)):
        gm.round(r)
        gd.round(r)
        for mask in gm.READY[r]:
            use(mask)
    for mask in CHIP_MASKS:
        for copy in keep(mask):
            copy.wait()
    for g in (gd, gm):
        g.finish()


def dw_swaps(stage, gate_hbm, up_hbm, sems, me):
    feat = gate_hbm.shape[0] // N_DEV
    return [Swap(lambda peer, lo=lo: stage(peer).at[lo:lo + feat, seg(peer % 2)], lambda o, dst=dst: dst.at[seg(o, feat), :], sems[i:i + 2], me)
            for lo, dst, i in ((0, gate_hbm, 0), (feat, up_hbm, 2))]


def mlp_back(dgu_hbm, wgu_hbm, h_ref, small_all, dout_ref, wo_ref, o_ref, glu_hbm, down_hbm, m_hbm,
             y_ref, dh_ref, do_ref, dwo_ref, dg_ref, gate_hbm, up_hbm, m_cols, stage, dgu_ref, wgu_ref, glu_ref, down_ref, isem, full, g_scr, dgu_t, glu_t, free, *scr):
    me = lax.axis_index('sp')
    dim = wo_ref.shape[1]
    far = seg(flipped(me, XYZ) // 2, WIDE)
    loads = fetch_all(isem, (dgu_hbm, dgu_ref), (m_hbm.at[:, :, far], m_cols), (wgu_hbm, wgu_ref), (glu_hbm, glu_ref), (down_hbm, down_ref))
    enter(me, NEAR + SETS[0])
    s = Scatter(*scr[:3], scr[3:7], me)
    g = row_gather(dh_ref, full, scr[7:11], me)
    gates, ups = dw_swaps(lambda peer: stage, gate_hbm, up_hbm, scr[11:], me)
    gain_row(g_scr, small_all, 1)
    dwo_ref[...] = jnp.zeros_like(dwo_ref)
    for load in loads[:2]:
        load.wait()
    stage[...] = mm(dgu_ref[...], m_cols[...].reshape(dgu_ref.shape[1], WIDE), NN)
    for swap in (gates, ups):
        swap.start(SETS[0])
    for load in loads[2:]:
        load.wait()
    total = s.run(block_product(s.part, dgu_ref, wgu_ref, dgu_t))
    for mask in NEAR:
        pl.semaphore_signal(free, inc=1, device_id=(flipped(me, mask),), device_id_type=MESH)
    norm_back(total, h_ref, g_scr, dout_ref, dh_ref, dg_ref)
    g.start()
    keep_own(dh_ref, full, me)
    s.finish()
    pl.semaphore_wait(free, len(NEAR))

    def use(mask):
        g.wait_pair(mask)
        chip = flipped(me, mask) // 2
        do_ref[:, seg(chip, WIDE)] = mm(wo_ref[...], full[chip], NT).astype(BF16)
        o = o_ref[:, seg(chip, WIDE)]

        def step(n):
            dwo_ref[:, seg(n, CHUNK)] += mm(o, full[chip, :, seg(n, CHUNK)], NN)
        loop(dim // CHUNK, step)

    def between(i):
        if i < len(g.ROUNDS):
            g.round(i)
            for mask in g.READY[i]:
                use(mask)

    s = Scatter(*scr[:3], scr[3:7], me)
    total = s.run(block_product(s.part, glu_ref, down_ref, glu_t), between)
    y_ref[...] = (h_ref[...].astype(F32) + total[...]).astype(BF16)
    s.finish()
    g.finish()
    for swap in (gates, ups):
        swap.wait_recv(SETS[0])
        swap.wait_send(SETS[0])


def back(groups, hd, qkv_ref, do_ref, stat_ref, cos_all, sin_all, dgu_ref, m_hbm, ucol_ref, cos_ref, sin_ref, w_hbm, x_ref, small_all, dh_ref, dg2_ref, dg_in, du_in,
         dg_hbm, du_hbm, dwq_ref, dwkv_ref, dx_ref, gain_ref,
         p_scr, dp_scr, k_scr, v_scr, dk_acc, dv_acc, stage, dq_scr, dkv_scr, m_scr,
         full, w_scr, shares, dkv_own, full_kv, dqkv, dn, g_scr, dg1, gains, gains_in, wsem, lsem, msem, *sems):
    heads = qkv_ref.shape[0] // hd - 2
    seq = qkv_ref.shape[1]
    scale = hd ** -0.5
    lanes = heads * QB
    qw = heads * hd
    half = hd // 2
    me = lax.axis_index('sp')
    feat = dgu_ref.shape[0] // 2
    first = (X, Y + Z, Y, X + Z, Z, X + Y, 0)

    def fetch(mask):
        cols = seg(flipped(me, mask) // 2, WIDE)
        return pltpu.make_async_copy(m_hbm.at[:, :, cols], m_scr.at[:, :, cols], msem.at[mask // 2])
    for mask in first:
        fetch(mask).start()
    load = pltpu.make_async_copy(w_hbm, w_scr, wsem)
    load.start()
    enter(me, OTHERS)
    gain_row(g_scr, small_all, 0)

    gates, ups = dw_swaps(lambda peer: stage.at[peer // 2], dg_hbm, du_hbm, sems[:4], me)
    own = [pltpu.make_async_copy(swap.src(me), swap.dst(me), lsem.at[i]) for i, swap in enumerate((gates, ups))]

    def make(mask):
        chip = flipped(me, mask) // 2
        fetch(mask).wait()
        cols = m_scr[:, :, seg(chip, WIDE)].reshape(seq, WIDE)
        stage[chip] = mm(dgu_ref[...], cols, NN)

    def advance(n):
        for swap in (gates, ups):
            if n > 1:
                swap.wait_send(SETS[n - 1])
            swap.start(SETS[n])

    for i, mask in enumerate(first):
        make(mask)
        if i == 1:
            advance(1)
    gates.start((CORE,))
    ups.start((CORE,))
    for copy in own:
        copy.start()

    dk_acc[...] = jnp.zeros_like(dk_acc)
    dv_acc[...] = jnp.zeros_like(dv_acc)
    key_rows(k_scr, qkv_ref, qw, hd)
    key_rows(v_scr, qkv_ref, qw + hd, hd)

    def q_block(qb):
        @pl.when(qb == 5)
        def _():
            advance(2)
        qs = seg(qb, QB)
        q2 = side_by_side(qkv_ref, heads, hd, qs)
        do2 = side_by_side(do_ref, heads, hd, qs)
        top = stat_ref[qb, :1, :]
        inv = stat_ref[qb, 1:, :]

        def probs(kb, rd, diagonal):
            ks = seg(kb, KB)
            s = score_block(k_scr[ks, :], q2, scale, diagonal)
            p = jnp.exp(s - top) * inv
            dp = mm(v_scr[ks, :], do2, NN).astype(BF16)
            p_scr[ks, :] = p
            dp_scr[ks, :] = dp
            dv_acc[ks, :] += mm(p.astype(BF16), do2, NT)
            return rd + jnp.sum(dp.astype(F32) * p, axis=0, keepdims=True)

        rd = lax.fori_loop(0, qb, lambda kb, r: probs(kb, r, False), jnp.zeros((1, lanes), F32))
        rd = probs(qb, rd, True)

        def d_scores(kb, acc):
            ks = seg(kb, KB)
            ds = (p_scr[ks, :] * (dp_scr[ks, :].astype(F32) - rd) * scale).astype(BF16)
            dk_acc[ks, :] += mm(ds, q2, NT)
            return acc + mm(qkv_ref[qw:qw + hd, ks], ds, NN)

        acc = lax.fori_loop(0, qb + 1, d_scores, jnp.zeros((hd, lanes), F32))
        cos, sin = cos_all[:, qs], sin_all[:, qs]
        for h in range(heads):
            dq = acc[:, h * QB:(h + 1) * QB].astype(BF16).astype(F32)
            p, q = dq[:half], dq[half:]
            dq_scr[h * hd:h * hd + half, qs] = (p * cos + q * sin).astype(BF16)
            dq_scr[h * hd + half:(h + 1) * hd, qs] = (q * cos - p * sin).astype(BF16)

    loop(seq // QB, q_block)

    def share(i):
        rs = seg(i, WIDE)
        dkv_scr[rs, :] = jnp.concatenate([dk_acc[rs, :], dv_acc[rs, :]], axis=1).astype(BF16)
    loop(seq // WIDE, share)
    tokens = ucol_ref.shape[1]
    per = N_DEV // groups
    q_all = dwq_ref.shape[0]
    sh = Swap(lambda peer: dkv_scr.at[seg(peer, tokens), :], lambda o: shares.at[o], sems[4:6], me)
    gq = row_gather(dq_scr, full, sems[6:10], me)
    parts = thirds(dkv_own.shape[0], STRIP)
    gk = Gather(dkv_own, lambda o: full_kv.at[:, seg(o, tokens)], lambda view, c: [view.at[pl.ds(*parts[c]), :]], sems[10:14], me)
    gs = Swap(lambda peer: gains.at[:, seg(peer)], lambda o: gains_in.at[o], sems[14:], me)
    sh.start()
    gq.start()
    keep_own(dq_scr, full, me)
    shares[me] = dkv_scr[seg(me, tokens), :]
    sh.wait_recv()
    cos, sin = cos_ref[...], sin_ref[...]
    for k in range(groups):
        both = sum(shares[per * k + i].astype(F32) for i in range(per)).astype(BF16).astype(F32).T
        p, q = both[:half], both[half:hd]
        lo = 2 * hd * k
        dkv_own[lo:lo + half, :] = (p * cos + q * sin).astype(BF16)
        dkv_own[lo + half:lo + hd, :] = (q * cos - p * sin).astype(BF16)
        dkv_own[lo + hd:lo + 2 * hd, :] = both[hd:].astype(BF16)
    gk.start()
    full_kv[:, seg(me, tokens)] = dkv_own[...]
    for k in range(groups):
        dqkv[:, q_all + 2 * hd * k:q_all + 2 * hd * (k + 1)] = dkv_own[2 * hd * k:2 * hd * (k + 1), :].T

    def use(mask):
        gq.wait_pair(mask)
        chip = flipped(me, mask) // 2
        dwq_ref[seg(chip, WIDE), :] = mm(full[chip], ucol_ref[...], NN)
        dqkv[:, seg(chip, WIDE)] = full[chip, :, seg(me, tokens)].T

    for r in range(len(gq.ROUNDS)):
        gq.round(r)
        gk.round(r)
        if r == 3:
            advance(3)
        for mask in gq.READY[r]:
            use(mask)
    load.wait()

    def normed(i):
        dn[:, seg(i, WIDE)] = mm(dqkv[...], w_scr[i], NN)
    loop(N_CHIP, normed)
    norm_back(dn, x_ref, g_scr, dh_ref, dx_ref, dg1)
    gains[...] = jnp.concatenate([jnp.sum(dg1[...], axis=0, keepdims=True), jnp.sum(dg2_ref[...], axis=0, keepdims=True),
                                  jnp.zeros((N_CHIP - 2, dg1.shape[1]), F32)], axis=0)
    gs.start()
    gains_in[me] = gains[:, seg(me)]
    for mask in CHIP_MASKS:
        gk.wait_pair(mask)
    dwkv_ref[...] = mm(full_kv[...], ucol_ref[...], NN)
    gs.wait_recv()
    gain_ref[...] = sum(gains_in[o] for o in range(N_DEV))
    for swap in (gates, ups):
        swap.wait_recv((CORE,) + SETS[1] + SETS[2] + SETS[3])
        swap.wait_send((CORE,) + SETS[3])
    for copy in own:
        copy.wait()
    for c in (sh, gs):
        c.wait_send()
    for g in (gq, gk):
        g.finish()


def finish(dg_hbm, du_hbm, dkv_hbm, *refs):
    n = (len(refs) - 11) // 3
    srcs, (gate, up, dk, dv), dsts = refs[:n], refs[n:n + 4], refs[n + 4:2 * n + 4]
    (g_in, g_out, kv_in), holds, sems = refs[2 * n + 4:2 * n + 7], refs[2 * n + 7:3 * n + 7], refs[3 * n + 7:]
    t_in, t_out, p_in, p_out = sems
    step = LANE * 11
    cols = g_in.shape[1]
    hd = dk.shape[0] // (kv_in.shape[0] // LANE)
    starts = [(w, i) for i in range(cols // step) for w in range(2)]

    def fetch(w, i):
        rs = pl.ds(i * step, step)
        return pltpu.make_async_copy((dg_hbm, du_hbm)[w].at[rs, :], g_in.at[w, rs, :], t_in.at[w, i])

    def put(w, i):
        cs = pl.ds(i * step, step)
        return pltpu.make_async_copy(g_out.at[w, :, cs], (gate, up)[w].at[:, cs], t_out.at[w, i])
    moves = [(pltpu.make_async_copy(a, h, p_in.at[k]), pltpu.make_async_copy(h, b, p_out.at[k])) for k, (a, h, b) in enumerate(zip(srcs, holds, dsts))]
    kv = pltpu.make_async_copy(dkv_hbm, kv_in, p_in.at[n])
    for w, i in starts:
        fetch(w, i).start()
    kv.start()
    for load, _ in moves:
        load.start()
    for w, i in starts:
        fetch(w, i).wait()

        at = pl.ds(i * step, step)
        g_out[w, :, at] = g_in[w, at, :].T
        put(w, i).start()
    kv.wait()
    for k in range(dk.shape[0] // hd):
        for i, ref in enumerate((dk, dv)):
            ref[k * hd:(k + 1) * hd, :] = kv_in[(2 * k + i) * hd:(2 * k + i + 1) * hd, :]
    for load, store in moves:
        load.wait()
        store.start()
    for w, i in starts:
        put(w, i).wait()
    for _, store in moves:
        store.wait()


def rope_tables(positions, head_dim):
    half_dim = head_dim // 2
    inv_freq = 1.0 / (ROPE_BASE ** (jnp.arange(half_dim, dtype=F32) * (2.0 / head_dim)))
    angles = positions.astype(F32)[None, :] * inv_freq[:, None]
    return jnp.cos(angles), jnp.sin(angles)


def solution(mesh):
    assert mesh.shape['sp'] == N_DEV

    def layer_step(x_in, positions, d_out, norm1_gain, norm2_gain, w_q, w_k, w_v, w_o, w_gate, w_up, w_down):
        tokens, dim = x_in.shape
        seq = tokens * N_DEV
        n_q, hd = w_q.shape[1:]
        n_kv = w_k.shape[1]
        qw = n_q // N_DEV * hd
        rows = w_q.shape[0]
        feat = w_down.shape[0]
        cols = (n_q + 2 * n_kv) * hd
        lanes = qw // hd * QB
        vm = pltpu.VMEM
        full = vm((N_CHIP, WIDE, dim), BF16)
        gain_scr = vm((N_CHIP, dim), F32)
        tok_shapes = 2 * (((tokens, dim), BF16),)
        dw_shapes = 2 * (((feat * N_DEV, rows), F32),)

        cos_own, sin_own = rope_tables(positions, hd)
        row = lambda v: v.reshape(1, rows)
        by_head = lambda w: w.transpose(1, 2, 0).reshape(-1, rows)
        wo_own = w_o.reshape(qw, dim)

        args = (x_in, row(norm1_gain), row(norm2_gain), row(positions), by_head(w_q), by_head(w_k), by_head(w_v), cos_own, sin_own, w_gate, w_up, wo_own)
        qkv, u_col, small_all, wqkv, attn_t, stat, wgu, hidden, mlp_in = call(
            functools.partial(head, n_kv, hd), 0, len(args),
            (((qw + 2 * hd, seq), BF16), ((seq, rows), BF16), ((N_DEV, N_CHIP, rows), F32), ((N_CHIP, cols, WIDE), BF16),
             ((qw, seq), BF16), ((seq // QB, 2, lanes), F32), ((2 * feat, dim), BF16), *tok_shapes),
            [full, vm((tokens, dim), F32), vm((tokens, dim), BF16), vm((seq, qw), BF16),
             vm((N_CHIP, rows), F32), vm((cols, rows), BF16), vm((N_CHIP, cols, WIDE), BF16), vm((cols, tokens), F32), vm((cols, tokens), BF16), vm((tokens, dim), BF16), gain_scr,
             vm((feat * N_DEV, rows), BF16), vm((feat * N_DEV, rows), BF16), vm((seq, lanes), F32), vm((seq, hd), BF16), dma(N_CHIP),
             *Gather.sems, *(7 * Swap.sems), *Gather.sems], 4 * qw * seq * seq, far_out=(3,))(*args)
        args = (mlp_in, d_out, wgu, w_down)
        m_full, glu, dgu, d_down = call(
            mlp_local, 1, len(args),
            (((N_CHIP, WIDE, dim), BF16), ((feat, seq), BF16), ((2 * feat, seq), BF16), ((feat, dim), F32)),
            [vm((2 * feat, dim), BF16), vm((feat, dim), BF16), vm((feat, seq), BF16), vm((2 * feat, seq), BF16), dma(2),
             full, full, dma(N_CHIP, 3), *(2 * Gather.sems)],
            8 * feat * seq * dim, far_in=(2, 3), far_out=(0, 1, 2))(*args)
        args = (dgu, wgu, hidden, small_all, d_out, wo_own, attn_t, glu, w_down, m_full)
        y_out, d_hidden, d_attn, d_wo, d_g2, d_gate_t, d_up_t = call(
            mlp_back, 2, len(args),
            (*tok_shapes, ((qw, seq), BF16), ((qw, dim), F32), ((N_CHIP, dim), F32), *dw_shapes),
            [vm((N_CHIP, WIDE, WIDE), BF16), vm((2 * feat, WIDE), F32),
             vm((2 * feat, seq), BF16), vm((2 * feat, dim), BF16), vm((feat, seq), BF16), vm((feat, dim), BF16), dma(5),
             full, gain_scr, vm((WIDE, 2 * feat), BF16), vm((WIDE, feat), BF16), pltpu.SemaphoreType.REGULAR,
             *Scatter.scratch(tokens, dim), *Scatter.sems, *Gather.sems, *(2 * Swap.sems)], 4 * feat * seq * dim,
            far_in=(0, 1, 7, 8, 9), far_out=(5, 6))(*args)
        cos_all, sin_all = rope_tables(small_all[:, 2].reshape(-1), hd)
        args = (qkv, d_attn, stat, cos_all, sin_all, dgu, m_full, u_col, cos_own, sin_own, wqkv, x_in, small_all, d_hidden, d_g2, d_gate_t, d_up_t)
        d_gate_t, d_up_t, d_wq, d_wkv, d_x, gains = call(
            functools.partial(back, n_kv, hd), 3, len(args),
            (*dw_shapes, ((n_q * hd, rows), F32), ((2 * n_kv * hd, rows), F32), tok_shapes[0], ((N_CHIP, rows), F32)),
            [vm((seq, lanes), F32), vm((seq, lanes), BF16), vm((seq, hd), BF16), vm((seq, hd), BF16), vm((seq, hd), F32), vm((seq, hd), F32),
             vm((N_CHIP, 2 * feat, WIDE), F32), vm((qw, seq), BF16), vm((seq, 2 * hd), BF16), full,
             full, vm((N_CHIP, cols, WIDE), BF16), vm((N_DEV, tokens, 2 * hd), BF16), vm((2 * n_kv * hd, tokens), BF16), vm((2 * n_kv * hd, seq), BF16),
             vm((tokens, cols), BF16), vm((tokens, dim), F32), gain_scr, gain_scr, gain_scr, vm((N_DEV, N_CHIP, rows), F32), dma(), dma(2), dma(N_CHIP),
             *(3 * Swap.sems), *(2 * Gather.sems), *Swap.sems], 10 * qw * seq * seq, far_in=(6, 10, 15, 16), far_out=(0, 1), aliases={15: 0, 16: 1})(*args)
        moved = (d_wq, d_wo, d_down, d_x, y_out, gains)
        half_kv = jax.ShapeDtypeStruct((n_kv * hd, rows), F32)
        wide = jax.ShapeDtypeStruct((rows, feat * N_DEV), F32)
        d_gate, d_up, d_wk, d_wv, d_wq, d_wo, d_down, d_x, y_out, gains = pl.pallas_call(
            finish,
            out_shape=[wide, wide, half_kv, half_kv] + [jax.ShapeDtypeStruct(v.shape, v.dtype) for v in moved],
            in_specs=[IN_HBM] * (3 + len(moved)), out_specs=[IN_HBM] * 2 + on_chip(2) + [IN_HBM] * len(moved),
            scratch_shapes=[vm((2, feat * N_DEV, rows), F32), vm((2, rows, feat * N_DEV), F32), vm(d_wkv.shape, F32)]
            + [vm(v.shape, v.dtype) for v in moved] + [dma(2, 4), dma(2, 4), dma(len(moved) + 1), dma(len(moved))],
            compiler_params=pltpu.CompilerParams(vmem_limit_bytes=VMEM_CAP), name='finish',
        )(d_gate_t, d_up_t, d_wkv, *moved)
        by_row = lambda g, heads: g.reshape(heads, hd, rows).transpose(2, 0, 1)
        return (y_out, d_x, gains[0], gains[1], by_row(d_wq, n_q), by_row(d_wk, n_kv), by_row(d_wv, n_kv),
                d_wo.reshape(w_o.shape), d_gate, d_up, d_down)

    all_rows = P('sp')
    return jax.shard_map(layer_step, mesh=mesh, in_specs=(all_rows,) * 12, out_specs=(all_rows,) * 11, check_vma=False)
```

```python
import functools
import jax
import jax.numpy as jnp
from jax import lax
from jax.experimental import pallas as pl
from jax.experimental.pallas import tpu as pltpu
from jax.sharding import PartitionSpec as P

ROPE_BASE = 10000.0
NORM_EPS = 1e-5
NEG_LARGE = -1e30
F32 = jnp.float32
BF16 = jnp.bfloat16
N_DEV, N_CHIP, LANE, WIDE, CHUNK, STRIP = 16, 8, 128, 256, 512, 16
NT = (((1,), (1,)), ((), ()))
TN = (((0,), (0,)), ((), ()))
NN = (((1,), (0,)), ((), ()))
MESH = pl.DeviceIdType.MESH
VMEM_CAP = 62 * 1024 * 1024

CORE, X, Y, Z = 1, 2, 4, 8
XYZ = X + Y + Z
ORDERS = ((X, Y, Z), (Y, Z, X), (Z, X, Y))
CHIP_MASKS = (0, X, Y, Z, X + Y, X + Z, Y + Z, XYZ)
NEAR = (CORE, X, Y, Z)
OTHERS = range(1, N_DEV)
SETS = tuple(tuple(m + c for m in masks for c in (0, CORE)) for masks in ((XYZ,), (X, Y + Z), (Y, X + Z), (Z, X + Y)))
N_COL = len(ORDERS)
COLOURS = range(N_COL)


def mm(a, b, dims):
    return lax.dot_general(a, b, dims, preferred_element_type=F32)


def seg(index, width=LANE):
    return pl.ds(pl.multiple_of(index * width, width), width)


def loop(count, body):
    lax.fori_loop(0, count, lambda i, c: (body(i), c)[1], 0)


def differing(index, mask):
    return sum(((index // bit + mask // bit) % 2) * bit for bit in NEAR)


def flipped(index, mask):
    out = index
    for bit in NEAR:
        if mask & bit:
            out = out + (1 - 2 * ((index // bit) % 2)) * bit
    return out


def thirds(total, unit):
    n = total // unit
    first = (n + 2) // 3
    second = (n - first + 1) // 2
    sizes = (first * unit, second * unit, (n - first - second) * unit)
    return ((0, sizes[0]), (sizes[0], sizes[1]), (sizes[0] + sizes[1], sizes[2]))


def pieces(rows, cols, unit):
    share = cols // LANE // N_COL * LANE
    strips = thirds(rows, unit)
    rest = cols - N_COL * share
    return [[(pl.ds(0, rows), pl.ds(c * share, share)), (pl.ds(*strips[c]), pl.ds(N_COL * share, rest))] for c in COLOURS]


def enter(me, masks):
    barrier = pltpu.get_barrier_semaphore()
    for mask in masks:
        pl.semaphore_signal(barrier, inc=1, device_id=(flipped(me, mask),), device_id_type=MESH)
    pl.semaphore_wait(barrier, len(masks))


def remote(src, dst, send, recv, peer):
    return pltpu.make_async_remote_copy(src_ref=src, dst_ref=dst, send_sem=send, recv_sem=recv, device_id=(peer,), device_id_type=MESH)


def dma(*shape):
    return pltpu.SemaphoreType.DMA(shape)


class Swap:
    sems = (dma(N_DEV), dma(N_DEV))

    def __init__(self, src, dst, sems, me):
        self.src, self.dst, (self.send, self.recv), self.me = src, dst, sems, me

    def copy(self, mask):
        peer = differing(self.me, mask)
        return remote(self.src(peer), self.dst(self.me), self.send.at[mask], self.recv.at[mask], peer)

    def arrival(self, mask):
        view = self.dst(differing(self.me, mask))
        return remote(view, view, self.send.at[mask], self.recv.at[mask], self.me)

    def each(self, masks, act):
        if masks is None:
            loop(N_DEV - 1, lambda i: act(i + 1))
        else:
            for mask in masks:
                act(mask)

    def start(self, masks=None):
        self.each(masks, lambda mask: self.copy(mask).start())

    def advance(self, n):
        if n:
            self.wait_send(SETS[n - 1])
        self.start(SETS[n])

    def wait_recv(self, masks=None):
        self.each(masks, lambda mask: self.arrival(mask).wait_recv())

    def wait_send(self, masks=None):
        self.each(masks, lambda mask: self.copy(mask).wait_send())


class Gather:
    ROUNDS = ((0,), (1,), (2,), (0, 1), (0, 2), (1, 2), (0, 1, 2))
    READY = ((0,), (), (), (X, Y), (Z,), (X + Y, X + Z), (Y + Z, XYZ))
    sems = (dma(N_COL, N_CHIP, 3, 2), dma(N_COL, N_CHIP, 2), dma(N_CHIP), dma(N_CHIP))

    def __init__(self, own, block, cut, sems, me):
        self.own, self.block, self.cut, self.me = own, block, cut, me
        self.send, self.recv, self.pair_send, self.pair_recv = sems

    def source(self, mask):
        return self.block(flipped(self.me, mask)) if mask else self.own

    def unit(self, colour, mask, axis):
        ends = zip(self.cut(self.source(mask), colour), self.cut(self.block(flipped(self.me, mask)), colour))
        return [remote(src, dst, self.send.at[colour, mask // 2, ORDERS[colour].index(axis), i], self.recv.at[colour, (mask + axis) // 2, i],
                       flipped(self.me, axis)) for i, (src, dst) in enumerate(ends)]

    def start_unit(self, colour, mask, axis):
        for copy in self.unit(colour, mask, axis):
            copy.start()

    def pair(self, mask):
        return remote(self.source(mask), self.block(flipped(self.me, mask)), self.pair_send.at[mask // 2],
                      self.pair_recv.at[mask // 2], flipped(self.me, CORE))

    def wait_pair(self, mask):
        view = self.block(flipped(self.me, mask + CORE))
        remote(view, view, self.pair_send.at[mask // 2], self.pair_recv.at[mask // 2], self.me).wait_recv()

    def onward(self, colour):
        order = ORDERS[colour]
        for picks in self.ROUNDS:
            for axis in order[picks[-1] + 1:]:
                yield picks, sum(order[p] for p in picks), axis

    def start(self, colours=COLOURS):
        for pos in COLOURS:
            for colour in colours:
                self.start_unit(colour, 0, ORDERS[colour][pos])
        if 2 in colours:
            self.pair(0).start()

    def round(self, r, colours=COLOURS):
        for colour in colours:
            mask = sum(ORDERS[colour][p] for p in self.ROUNDS[r])
            for i, view in enumerate(self.cut(self.block(flipped(self.me, mask)), colour)):
                remote(view, view, self.send.at[colour, 0, 0, i], self.recv.at[colour, mask // 2, i], self.me).wait_recv()
            for picks, at, axis in self.onward(colour):
                if picks == self.ROUNDS[r]:
                    self.start_unit(colour, at, axis)
        if 2 in colours:
            for mask in {2: (X, Y, Z), 5: (X + Y, X + Z, Y + Z), 6: (XYZ,)}.get(r, ()):
                self.pair(mask).start()

    def finish(self):
        for colour in COLOURS:
            for at, axis in [(0, axis) for axis in ORDERS[colour]] + [step[1:] for step in self.onward(colour)]:
                for copy in self.unit(colour, at, axis):
                    copy.wait_send()
        for mask in CHIP_MASKS:
            self.pair(mask).wait_send()


def row_gather(own, full, sems, me, extra=None):
    rows, width = own.shape
    parts = pieces(rows, width, STRIP)
    if extra is not None:
        share = width // LANE // N_COL * LANE
        more = width - N_COL * share
        parts = [[(pl.ds(0, rows), pl.ds(c * share + more * (c > extra), share + more * (c == extra)))] for c in COLOURS]

    def block(o):
        return full.at[o // 2, seg(o % 2), :]

    return Gather(own, block, lambda view, c: [view.at[rs, cs] for rs, cs in parts[c]], sems, me)


def keep_own(own, full, me):
    def step(i):
        full[me // 2, pl.ds(pl.multiple_of((me % 2) * LANE + i * STRIP, STRIP), STRIP), :] = own[seg(i, STRIP), :]
    loop(LANE // STRIP, step)


class Scatter:
    ORDER = (XYZ, X + Y, Y + Z, X + Z, X, Y, Z, 0)
    sems = (dma(N_CHIP), dma(N_CHIP), dma(N_COL, N_CHIP, 2), dma(N_COL, N_CHIP, 2))

    @staticmethod
    def scratch(tokens, dim):
        return [pltpu.VMEM((N_CHIP, 2, tokens, dim), F32), pltpu.VMEM((N_CHIP, tokens, dim), F32), pltpu.VMEM((N_CHIP - 1, tokens, dim), F32)]

    def __init__(self, part, pair_in, link_in, sems, me):
        self.part, self.pair_in, self.link_in, self.me = part, pair_in, link_in, me
        self.pair_send, self.pair_recv, self.link_send, self.link_recv = sems
        self.core = me % 2
        self.tokens, self.dim = part.shape[2:]
        self.pieces = pieces(self.tokens, self.dim, STRIP // 2)
        self.ready, self.sent = set(), [0] * N_COL

    @staticmethod
    def first(colour, mask):
        return next((i for i, a in enumerate(ORDERS[colour]) if mask & a), 3)

    def slot(self, colour, mask, axis):
        slots = [(m, a) for m in self.ORDER for a in ORDERS[colour][:self.first(colour, m)]]
        return slots.index((mask, axis))

    def pair(self, i):
        return remote(self.part.at[i, 1 - self.core], self.pair_in.at[i], self.pair_send.at[i], self.pair_recv.at[i], flipped(self.me, CORE))

    def link(self, colour, mask):
        axis = ORDERS[colour][self.first(colour, mask)]
        slot = self.slot(colour, mask - axis, axis)
        i = self.ORDER.index(mask)
        return [remote(self.part.at[i, self.core, rs, cs], self.link_in.at[slot, rs, cs], self.link_send.at[colour, i, k],
                       self.link_recv.at[colour, slot, k], flipped(self.me, axis)) for k, (rs, cs) in enumerate(self.pieces[colour])]

    def start_link(self, colour, mask):
        for copy in self.link(colour, mask):
            copy.start()

    def add(self, mask, ref, cs):
        i = self.ORDER.index(mask)

        def step(r):
            rs = seg(r, STRIP)
            self.part[i, self.core, rs, cs] += ref[rs, cs]
        loop(self.tokens // STRIP, step)

    def finish_pair(self, i):
        self.pair(i).wait_recv()
        self.add(self.ORDER[i], self.pair_in.at[i], pl.ds(0, self.dim))
        self.ready.add(self.ORDER[i])
        for colour in COLOURS:
            a, b, c = ORDERS[colour]
            todo = (XYZ, a + b, a + c, a)
            while self.sent[colour] < len(todo) and todo[self.sent[colour]] in self.ready:
                self.start_link(colour, todo[self.sent[colour]])
                self.sent[colour] += 1

    def take(self, colour, mask, axis):
        for copy in self.link(colour, mask + axis):
            copy.wait_recv()
        ref = self.link_in.at[self.slot(colour, mask, axis)]
        (_, wide), (rs, cs) = self.pieces[colour]
        self.add(mask, ref, wide)
        self.part[self.ORDER.index(mask), self.core, rs, cs] += ref[rs, cs]

    def run(self, product, between=lambda i: None):
        for i, mask in enumerate(self.ORDER):
            product(i, flipped(self.me, mask) // 2)
            self.pair(i).start()
            if i:
                self.finish_pair(i - 1)
            between(i)
        self.finish_pair(N_CHIP - 1)
        for step in range(2):
            for colour in COLOURS:
                a, b, c = ORDERS[colour]
                mask = (b + c, b)[step]
                self.take(colour, mask, a)
                self.start_link(colour, mask)
        for colour in COLOURS:
            a, b, c = ORDERS[colour]
            self.take(colour, c, a)
            self.take(colour, c, b)
            self.start_link(colour, c)
        for colour in COLOURS:
            for axis in ORDERS[colour]:
                self.take(colour, 0, axis)
        return self.part.at[N_CHIP - 1, self.core]

    def finish(self):
        for i in range(N_CHIP):
            self.pair(i).wait_send()
        for colour in COLOURS:
            for mask in self.ORDER[:-1]:
                for copy in self.link(colour, mask):
                    copy.wait_send()


def block_product(part, a_ref, w_ref, a_t):
    tokens = part.shape[2]

    def product(i, chip):
        a_t[...] = a_ref[:, seg(chip, 2 * tokens)].T

        def step(n):
            cs = seg(n, CHUNK)
            r = mm(a_t[...], w_ref[:, cs], NN)
            part[i, 0, :, cs] = r[:tokens]
            part[i, 1, :, cs] = r[tokens:]
        loop(part.shape[3] // CHUNK, step)
    return product


def on_chip(n):
    return [pl.BlockSpec(memory_space=pltpu.VMEM)] * n


IN_HBM = pl.BlockSpec(memory_space=pl.ANY)


def call(kernel, ident, args, outs, scratch, flops, far_in=(), far_out=(), aliases={}):
    specs = [IN_HBM if i in far_in else on_chip(1)[0] for i in range(args)]
    out_specs = [IN_HBM if i in far_out else on_chip(1)[0] for i in range(len(outs))]
    return pl.pallas_call(
        kernel,
        out_shape=[jax.ShapeDtypeStruct(shape, dtype) for shape, dtype in outs],
        in_specs=specs, out_specs=out_specs, scratch_shapes=scratch, input_output_aliases=aliases,
        cost_estimate=pl.CostEstimate(flops=flops, bytes_accessed=flops // CHUNK, transcendentals=0),
        compiler_params=pltpu.CompilerParams(collective_id=ident, has_side_effects=True, vmem_limit_bytes=VMEM_CAP),
        name=kernel.func.__name__ if isinstance(kernel, functools.partial) else kernel.__name__,
    )


def fetch_all(sem, *pairs):
    copies = [pltpu.make_async_copy(src, dst, sem.at[i]) for i, (src, dst) in enumerate(pairs)]
    for copy in copies:
        copy.start()
    return copies


def gain_row(dst, small_all, which):
    for o in range(N_DEV):
        dst[:1, o * LANE:(o + 1) * LANE] = small_all[o, which:which + 1, :]


def norm_rows(src, gain, dst):
    def step(i):
        rs = seg(i, STRIP)
        t = src[rs, :].astype(F32)
        dst[rs, :] = (t * lax.rsqrt(jnp.mean(t * t, axis=-1, keepdims=True) + NORM_EPS) * gain[:1, :]).astype(BF16)
    loop(src.shape[0] // STRIP, step)


def norm_back(dy, src, gain, skip, dst, dgain):
    def step(i):
        rs = seg(i, STRIP)
        d = dy[rs, :].astype(BF16).astype(F32)
        t = src[rs, :].astype(F32)
        inv = lax.rsqrt(jnp.mean(t * t, axis=-1, keepdims=True) + NORM_EPS)
        gd = gain[:1, :] * d
        pull = jnp.mean(gd * t, axis=-1, keepdims=True)
        dst[rs, :] = (skip[rs, :].astype(F32) + (inv * gd - t * (inv * inv * inv * pull))).astype(BF16)
        g = d * (t * inv)
        dgain[...] += g[:N_CHIP] + g[N_CHIP:]
    dgain[...] = jnp.zeros_like(dgain)
    loop(src.shape[0] // STRIP, step)


QB = 256
KB = 256


def key_rows(dst, src, lo, hd):
    def step(i):
        dst[seg(i, KB), :] = src[lo:lo + hd, seg(i, KB)].T
    loop(src.shape[1] // KB, step)


def score_block(k, q2, scale, diagonal):
    s = mm(k, q2, NN) * scale
    if diagonal:
        key = lax.broadcasted_iota(jnp.int32, s.shape, 0)
        qry = lax.broadcasted_iota(jnp.int32, s.shape, 1) % QB
        s = jnp.where(qry >= key, s, NEG_LARGE)
    return s


def side_by_side(ref, heads, hd, qs):
    return jnp.concatenate([ref[h * hd:(h + 1) * hd, qs] for h in range(heads)], axis=1)


def head(groups, hd, x_ref, g1_ref, g2_ref, pos_ref, wq_ref, wk_ref, wv_ref, cos_ref, sin_ref, wg_ref, wu_ref, wo_ref, qkv_ref, u_scr, small_all, w_out, o_ref, stat_ref, wgu_ref, h_ref, m_ref,
         full_w, acc_o, o_tok, o_send, small_ref, w_ref, full, acc, rot, g_scr, wg_t, wu_t, s_scr, k_scr, osem, *sems):
    me = lax.axis_index('sp')
    tokens, dim = x_ref.shape
    cols = w_ref.shape[0]
    small_ref[...] = jnp.concatenate([r[...].astype(F32) for r in (g1_ref, g2_ref, pos_ref)] + [jnp.zeros((N_CHIP - 3, LANE), F32)], axis=0)
    w_ref[:wq_ref.shape[0], :] = wq_ref[...]
    for k in range(groups):
        for i, ref in enumerate((wk_ref, wv_ref)):
            w_ref[pl.ds(wq_ref.shape[0] + (2 * k + i) * hd, hd), :] = ref[k * hd:(k + 1) * hd, :]
    qw = tokens
    q_all = N_DEV * qw
    gsems, ssems, qsems, ksems, gate_sems, up_sems, osems = sems[:4], *(sems[i:i + 2] for i in range(4, len(sems) - 4, 2))
    gw = row_gather(wo_ref, full_w, sems[-4:], me, 1)
    feat = wg_ref.shape[1] // N_DEV
    enter(me, OTHERS)
    smalls = Swap(lambda peer: small_ref, lambda o: small_all.at[o], ssems, me)
    smalls.start()
    parts = thirds(cols, STRIP)
    g = Gather(w_ref, lambda o: full.at[o // 2, :, seg(o % 2)], lambda view, c: [view.at[pl.ds(*parts[c]), :]], gsems, me)
    g.start()
    gates = Swap(lambda peer: wg_t.at[seg(peer, feat), :], lambda o: wgu_ref.at[:feat, seg(o)], gate_sems, me)
    ups = Swap(lambda peer: wu_t.at[seg(peer, feat), :], lambda o: wgu_ref.at[feat:, seg(o)], up_sems, me)

    def advance(n):
        gates.advance(n)
        ups.advance(n)

    def transpose(i):
        wg_t[seg(i, CHUNK), :] = wg_ref[:, seg(i, CHUNK)].T
        wu_t[seg(i, CHUNK), :] = wu_ref[:, seg(i, CHUNK)].T
    loop(wg_ref.shape[1] // CHUNK, transpose)
    advance(0)

    def own_block(i):
        full[me // 2, seg(i, WIDE), seg(me % 2)] = w_ref[seg(i, WIDE), :]
    loop(cols // WIDE, own_block)
    acc[...] = jnp.zeros_like(acc)
    small_all[me] = small_ref[...]
    smalls.wait_recv()
    gain_row(g_scr, small_all, 0)
    norm_rows(x_ref, g_scr, u_scr)

    def keep(mask):
        chip = flipped(me, mask) // 2
        return pltpu.make_async_copy(full.at[chip], w_out.at[chip], osem.at[mask // 2])

    def use(mask):
        g.wait_pair(mask)
        keep(mask).start()
        chip = flipped(me, mask) // 2
        u = u_scr[:, seg(chip, WIDE)]

        def step(i):
            rs = seg(i, cols // 2)
            acc[rs, :] += mm(full[chip, rs, :], u, NT)
        loop(2, step)

    for r in range(len(g.ROUNDS)):
        g.round(r)
        if r in (2, 4):
            advance(r // 2)
        for mask in g.READY[r]:
            use(mask)

    half = hd // 2
    cos, sin = cos_ref[...], sin_ref[...]

    def turn(h):
        first = seg(2 * h, half)
        second = seg(2 * h + 1, half)
        p = acc[first, :].astype(BF16).astype(F32)
        q = acc[second, :].astype(BF16).astype(F32)
        rot[first, :] = (p * cos - q * sin).astype(BF16)
        rot[second, :] = (q * cos + p * sin).astype(BF16)
    loop(q_all // hd, turn)
    for k in range(groups):
        turn(q_all // hd + 2 * k)
        vs = seg(q_all // hd + 2 * k + 1, hd)
        rot[vs, :] = acc[vs, :].astype(BF16)
    per = N_DEV // groups
    q_rows = lambda peer: seg(peer, qw)
    kv_rows = lambda peer: seg(q_all // (2 * hd) + peer // per, 2 * hd)
    qs = Swap(lambda peer: rot.at[q_rows(peer), :], lambda o: qkv_ref.at[:qw, seg(o, tokens)], qsems, me)
    kvs = Swap(lambda peer: rot.at[kv_rows(peer), :], lambda o: qkv_ref.at[qw:, seg(o, tokens)], ksems, me)
    qs.start()
    kvs.start()
    gw.start()
    keep_own(wo_ref, full_w, me)
    gain_row(g_scr, small_all, 1)
    qkv_ref[:qw, seg(me, tokens)] = rot[q_rows(me), :]
    qkv_ref[qw:, seg(me, tokens)] = rot[kv_rows(me), :]
    wgu_ref[:feat, seg(me)] = wg_t[seg(me, feat), :]
    wgu_ref[feat:, seg(me)] = wu_t[seg(me, feat), :]
    gates.start((CORE,))
    ups.start((CORE,))
    for swap in (qs, kvs):
        swap.wait_recv()
    heads = qkv_ref.shape[0] // hd - 2
    seq = qkv_ref.shape[1]
    scale = hd ** -0.5
    lanes = heads * QB
    key_rows(k_scr, qkv_ref, qw, hd)

    outs = Swap(lambda peer: o_send.at[seg(peer), :], lambda o: o_tok.at[:, seg(o)], osems, me)

    def q_block(qb):
        for at, r in ((2, 0), (4, 1), (5, 2), (6, 3), (7, 4)):
            @pl.when(qb == at)
            def _():
                gw.round(r)
        qs = seg(qb, QB)
        q2 = side_by_side(qkv_ref, heads, hd, qs)

        def scores(kb, top, diagonal):
            s = score_block(k_scr[seg(kb, KB), :], q2, scale, diagonal)
            s_scr[seg(kb, KB), :] = s
            return jnp.maximum(top, jnp.max(s, axis=0, keepdims=True))

        top = lax.fori_loop(0, qb, lambda kb, t: scores(kb, t, False), jnp.full((1, lanes), NEG_LARGE, F32))
        top = scores(qb, top, True)

        def expo(kb, tot):
            e = jnp.exp(s_scr[seg(kb, KB), :] - top)
            s_scr[seg(kb, KB), :] = e
            return tot + jnp.sum(e, axis=0, keepdims=True)

        inv = 1.0 / lax.fori_loop(0, qb + 1, expo, jnp.zeros((1, lanes), F32))

        def weigh(kb, acc):
            p = (s_scr[seg(kb, KB), :] * inv).astype(BF16)
            return acc + mm(qkv_ref[qw + hd:, seg(kb, KB)], p, NN)

        acc = lax.fori_loop(0, qb + 1, weigh, jnp.zeros((hd, lanes), F32))
        for h in range(heads):
            o_ref[h * hd:(h + 1) * hd, qs] = acc[:, h * QB:(h + 1) * QB].astype(BF16)
        stat_ref[qb, :1, :] = top
        stat_ref[qb, 1:, :] = inv
        o_send[qs, :] = o_ref[:, qs].T

    loop(seq // QB, q_block)
    outs.start()
    advance(3)
    o_tok[:, seg(me)] = o_send[seg(me), :]
    for r in (5, 6):
        gw.round(r)
    outs.wait_recv()
    for mask in CHIP_MASKS:
        gw.wait_pair(mask)

    def project(n):
        cs = seg(n, CHUNK)
        acc_o[:, cs] = mm(o_tok[...], full_w[:, :, cs].reshape(dim, CHUNK), NN)
    loop(dim // CHUNK, project)

    def residual(i):
        rs = seg(i, STRIP)
        h_ref[rs, :] = (x_ref[rs, :].astype(F32) + acc_o[rs, :]).astype(BF16)
    loop(tokens // STRIP, residual)
    norm_rows(h_ref, g_scr, m_ref)
    for swap in (gates, ups):
        swap.wait_recv()
    for mask in CHIP_MASKS:
        keep(mask).wait()
    outs.wait_send()
    for swap in (gates, ups):
        swap.wait_send((CORE,) + SETS[3])
    g.finish()
    gw.finish()
    for swap in (smalls, qs, kvs):
        swap.wait_send()


def mlp_local(m_ref, dout_ref, wgu_hbm, down_hbm, u_ref, ucol_ref, m_out, glu_out, dgu_out, ddown_ref,
              wgu_ref, down_ref, glu_ref, dgu_ref, isem, full_d, full_m, osem, *sems):
    me = lax.axis_index('sp')
    feat, dim = down_ref.shape
    loads = fetch_all(isem, (wgu_hbm, wgu_ref), (down_hbm, down_ref))
    enter(me, OTHERS)
    gd = row_gather(dout_ref, full_d, sems[:4], me, 0)
    gm = row_gather(m_ref, full_m, sems[4:8], me, 2)
    ucols = Swap(lambda peer: u_ref.at[:, seg(peer)], lambda o: ucol_ref.at[seg(o), :], sems[8:], me)
    ucol_ref[seg(me), :] = u_ref[:, seg(me)]
    gm.start()
    gd.start()
    keep_own(m_ref, full_m, me)
    keep_own(dout_ref, full_d, me)
    ddown_ref[...] = jnp.zeros_like(ddown_ref)

    def keep(mask):
        chip = flipped(me, mask) // 2
        ts = seg(chip, WIDE)
        ends = ((full_m.at[chip], m_out.at[chip]), (glu_ref.at[:, ts], glu_out.at[:, ts]), (dgu_ref.at[:, ts], dgu_out.at[:, ts]))
        return [pltpu.make_async_copy(src, dst, osem.at[mask // 2, i]) for i, (src, dst) in enumerate(ends)]

    for load in loads:
        load.wait()

    def use(mask):
        gd.wait_pair(mask)
        gm.wait_pair(mask)
        chip = flipped(me, mask) // 2
        ts = seg(chip, WIDE)
        gu = mm(wgu_ref[...], full_m[chip], NT).astype(BF16).astype(F32)
        gate, up = gu[:feat], gu[feat:]
        d_glu = mm(down_ref[...], full_d[chip], NT).astype(BF16).astype(F32)
        sig = jax.nn.sigmoid(gate)
        act = gate * sig
        glu = (act * up).astype(BF16)
        glu_ref[:, ts] = glu
        dgu_ref[:feat, ts] = (d_glu * up * (sig * (1.0 + gate * (1.0 - sig)))).astype(BF16)
        dgu_ref[feat:, ts] = (d_glu * act).astype(BF16)

        def step(n):
            ddown_ref[:, seg(n, CHUNK)] += mm(glu, full_d[chip, :, seg(n, CHUNK)], NN)
        loop(dim // CHUNK, step)
        for copy in keep(mask):
            copy.start()

    for r in range(len(gm.ROUNDS)):
        gm.round(r)
        gd.round(r)
        if r == 3:
            ucols.start()
        for mask in gm.READY[r]:
            use(mask)
    for mask in CHIP_MASKS:
        for copy in keep(mask):
            copy.wait()
    ucols.wait_recv()
    ucols.wait_send()
    for g in (gd, gm):
        g.finish()


def dw_swaps(stage, gate_hbm, up_hbm, sems, me):
    feat = gate_hbm.shape[0] // N_DEV
    return [Swap(lambda peer, lo=lo: stage(peer).at[lo:lo + feat, seg(peer % 2)], lambda o, dst=dst: dst.at[seg(o, feat), :], sems[i:i + 2], me)
            for lo, dst, i in ((0, gate_hbm, 0), (feat, up_hbm, 2))]


def mlp_back(dgu_hbm, wgu_hbm, h_ref, small_all, dout_ref, wo_ref, o_ref, glu_hbm, down_hbm, m_hbm,
             y_ref, dh_ref, do_ref, dwo_ref, dg_ref, gate_hbm, up_hbm, m_cols, stage, dgu_ref, wgu_ref, glu_ref, down_ref, isem, full, g_scr, dgu_t, glu_t, free, *scr):
    me = lax.axis_index('sp')
    dim = wo_ref.shape[1]
    far = seg(flipped(me, XYZ) // 2, WIDE)
    loads = fetch_all(isem, (dgu_hbm, dgu_ref), (m_hbm.at[:, :, far], m_cols), (wgu_hbm, wgu_ref), (glu_hbm, glu_ref), (down_hbm, down_ref))
    enter(me, NEAR + SETS[0])
    s = Scatter(*scr[:3], scr[3:7], me)
    g = row_gather(dh_ref, full, scr[7:11], me)
    gates, ups = dw_swaps(lambda peer: stage, gate_hbm, up_hbm, scr[11:], me)
    gain_row(g_scr, small_all, 1)
    dwo_ref[...] = jnp.zeros_like(dwo_ref)
    for load in loads[:2]:
        load.wait()
    stage[...] = mm(dgu_ref[...], m_cols[...].reshape(dgu_ref.shape[1], WIDE), NN)
    for swap in (gates, ups):
        swap.start(SETS[0])
    for load in loads[2:]:
        load.wait()
    total = s.run(block_product(s.part, dgu_ref, wgu_ref, dgu_t))
    for mask in NEAR:
        pl.semaphore_signal(free, inc=1, device_id=(flipped(me, mask),), device_id_type=MESH)
    norm_back(total, h_ref, g_scr, dout_ref, dh_ref, dg_ref)
    g.start()
    keep_own(dh_ref, full, me)
    s.finish()
    pl.semaphore_wait(free, len(NEAR))

    def use(mask):
        g.wait_pair(mask)
        chip = flipped(me, mask) // 2
        do_ref[:, seg(chip, WIDE)] = mm(wo_ref[...], full[chip], NT).astype(BF16)
        o = o_ref[:, seg(chip, WIDE)]

        def step(n):
            dwo_ref[:, seg(n, CHUNK)] += mm(o, full[chip, :, seg(n, CHUNK)], NN)
        loop(dim // CHUNK, step)

    def between(i):
        if i < len(g.ROUNDS):
            g.round(i)
            for mask in g.READY[i]:
                use(mask)

    s = Scatter(*scr[:3], scr[3:7], me)
    total = s.run(block_product(s.part, glu_ref, down_ref, glu_t), between)
    y_ref[...] = (h_ref[...].astype(F32) + total[...]).astype(BF16)
    s.finish()
    g.finish()
    for swap in (gates, ups):
        swap.wait_recv(SETS[0])
        swap.wait_send(SETS[0])


def back(groups, hd, qkv_ref, do_ref, stat_ref, cos_all, sin_all, dgu_ref, m_hbm, ucol_ref, cos_ref, sin_ref, w_hbm, x_ref, small_all, dh_ref, dg2_ref, dg_in, du_in,
         dg_hbm, du_hbm, dwq_ref, dwkv_ref, dx_ref, gain_ref,
         p_scr, dp_scr, k_scr, v_scr, dk_acc, dv_acc, stage, dq_scr, dkv_scr, m_scr,
         full, w_scr, shares, dkv_own, full_kv, dqkv, dn, g_scr, dg1, gains, gains_in, wsem, lsem, msem, *sems):
    heads = qkv_ref.shape[0] // hd - 2
    seq = qkv_ref.shape[1]
    scale = hd ** -0.5
    lanes = heads * QB
    qw = heads * hd
    half = hd // 2
    me = lax.axis_index('sp')
    feat = dgu_ref.shape[0] // 2
    first = (X, Y + Z, Y, X + Z, Z, X + Y, 0)

    def fetch(mask):
        cols = seg(flipped(me, mask) // 2, WIDE)
        return pltpu.make_async_copy(m_hbm.at[:, :, cols], m_scr.at[:, :, cols], msem.at[mask // 2])
    for mask in first:
        fetch(mask).start()
    load = pltpu.make_async_copy(w_hbm, w_scr, wsem)
    load.start()
    enter(me, OTHERS)
    gain_row(g_scr, small_all, 0)

    gates, ups = dw_swaps(lambda peer: stage.at[peer // 2], dg_hbm, du_hbm, sems[:4], me)
    gq = row_gather(dq_scr, full, sems[6:10], me, 0)
    own = [pltpu.make_async_copy(swap.src(me), swap.dst(me), lsem.at[i]) for i, swap in enumerate((gates, ups))]

    def make(mask):
        chip = flipped(me, mask) // 2
        fetch(mask).wait()
        cols = m_scr[:, :, seg(chip, WIDE)].reshape(seq, WIDE)
        stage[chip] = mm(dgu_ref[...], cols, NN)

    def advance(n):
        for swap in (gates, ups):
            if n > 1:
                swap.wait_send(SETS[n - 1])
            swap.start(SETS[n])

    for i, mask in enumerate(first):
        make(mask)
        if i == 1:
            advance(1)
    gates.start((CORE,))
    ups.start((CORE,))
    for copy in own:
        copy.start()

    dk_acc[...] = jnp.zeros_like(dk_acc)
    dv_acc[...] = jnp.zeros_like(dv_acc)
    key_rows(k_scr, qkv_ref, qw, hd)
    key_rows(v_scr, qkv_ref, qw + hd, hd)

    def q_block(qb):
        for at, act in ((3, lambda: gq.start((0,))), (4, lambda: advance(2)), (5, lambda: gq.round(0, (0,))), (6, lambda: (gq.start((1,)), gq.round(1, (0,)))),
                        (7, lambda: gq.round(2, (0,)))):
            pl.when(qb == at)(lambda act=act: (act(), None)[1])
        qs = seg(qb, QB)
        q2 = side_by_side(qkv_ref, heads, hd, qs)
        do2 = side_by_side(do_ref, heads, hd, qs)
        top = stat_ref[qb, :1, :]
        inv = stat_ref[qb, 1:, :]

        def probs(kb, rd, diagonal):
            ks = seg(kb, KB)
            s = score_block(k_scr[ks, :], q2, scale, diagonal)
            p = jnp.exp(s - top) * inv
            dp = mm(v_scr[ks, :], do2, NN).astype(BF16)
            p_scr[ks, :] = p
            dp_scr[ks, :] = dp
            dv_acc[ks, :] += mm(p.astype(BF16), do2, NT)
            return rd + jnp.sum(dp.astype(F32) * p, axis=0, keepdims=True)

        rd = lax.fori_loop(0, qb, lambda kb, r: probs(kb, r, False), jnp.zeros((1, lanes), F32))
        rd = probs(qb, rd, True)

        def d_scores(kb, acc):
            ks = seg(kb, KB)
            ds = (p_scr[ks, :] * (dp_scr[ks, :].astype(F32) - rd) * scale).astype(BF16)
            dk_acc[ks, :] += mm(ds, q2, NT)
            return acc + mm(qkv_ref[qw:qw + hd, ks], ds, NN)

        acc = lax.fori_loop(0, qb + 1, d_scores, jnp.zeros((hd, lanes), F32))
        cos, sin = cos_all[:, qs], sin_all[:, qs]
        for h in range(heads):
            dq = acc[:, h * QB:(h + 1) * QB].astype(BF16).astype(F32)
            p, q = dq[:half], dq[half:]
            dq_scr[h * hd:h * hd + half, qs] = (p * cos + q * sin).astype(BF16)
            dq_scr[h * hd + half:(h + 1) * hd, qs] = (q * cos - p * sin).astype(BF16)

    loop(seq // QB, q_block)

    def share(i):
        rs = seg(i, WIDE)
        dkv_scr[rs, :] = jnp.concatenate([dk_acc[rs, :], dv_acc[rs, :]], axis=1).astype(BF16)
    loop(seq // WIDE, share)
    tokens = ucol_ref.shape[1]
    per = N_DEV // groups
    q_all = dwq_ref.shape[0]
    sh = Swap(lambda peer: dkv_scr.at[seg(peer, tokens), :], lambda o: shares.at[o], sems[4:6], me)
    parts = thirds(dkv_own.shape[0], STRIP)
    gk = Gather(dkv_own, lambda o: full_kv.at[:, seg(o, tokens)], lambda view, c: [view.at[pl.ds(*parts[c]), :]], sems[10:14], me)
    gs = Swap(lambda peer: gains.at[:, seg(peer)], lambda o: gains_in.at[o], sems[14:], me)
    sh.start()
    gq.start((2,))
    keep_own(dq_scr, full, me)
    shares[me] = dkv_scr[seg(me, tokens), :]
    sh.wait_recv()
    cos, sin = cos_ref[...], sin_ref[...]
    for k in range(groups):
        both = sum(shares[per * k + i].astype(F32) for i in range(per)).astype(BF16).astype(F32).T
        p, q = both[:half], both[half:hd]
        lo = 2 * hd * k
        dkv_own[lo:lo + half, :] = (p * cos + q * sin).astype(BF16)
        dkv_own[lo + half:lo + hd, :] = (q * cos - p * sin).astype(BF16)
        dkv_own[lo + hd:lo + 2 * hd, :] = both[hd:].astype(BF16)
    gk.start()
    full_kv[:, seg(me, tokens)] = dkv_own[...]
    for k in range(groups):
        dqkv[:, q_all + 2 * hd * k:q_all + 2 * hd * (k + 1)] = dkv_own[2 * hd * k:2 * hd * (k + 1), :].T

    def use(mask):
        gq.wait_pair(mask)
        chip = flipped(me, mask) // 2
        dwq_ref[seg(chip, WIDE), :] = mm(full[chip], ucol_ref[...], NN)
        dqkv[:, seg(chip, WIDE)] = full[chip, :, seg(me, tokens)].T

    for r in range(3, len(gq.ROUNDS)):
        gq.round(r, (0,))
    for r in range(len(gq.ROUNDS)):
        gq.round(r, (1, 2))
        gk.round(r)
        if r == 3:
            advance(3)
        for mask in gq.READY[r]:
            use(mask)
    load.wait()

    def normed(i):
        dn[:, seg(i, WIDE)] = mm(dqkv[...], w_scr[i], NN)
    loop(N_CHIP, normed)
    norm_back(dn, x_ref, g_scr, dh_ref, dx_ref, dg1)
    gains[...] = jnp.concatenate([jnp.sum(dg1[...], axis=0, keepdims=True), jnp.sum(dg2_ref[...], axis=0, keepdims=True),
                                  jnp.zeros((N_CHIP - 2, dg1.shape[1]), F32)], axis=0)
    gs.start()
    gains_in[me] = gains[:, seg(me)]
    for mask in CHIP_MASKS:
        gk.wait_pair(mask)
    dwkv_ref[...] = mm(full_kv[...], ucol_ref[...], NN)
    gs.wait_recv()
    gain_ref[...] = sum(gains_in[o] for o in range(N_DEV))
    for swap in (gates, ups):
        swap.wait_recv((CORE,) + SETS[1] + SETS[2] + SETS[3])
        swap.wait_send((CORE,) + SETS[3])
    for copy in own:
        copy.wait()
    for c in (sh, gs):
        c.wait_send()
    for g in (gq, gk):
        g.finish()


def finish(dg_hbm, du_hbm, dkv_hbm, *refs):
    n = (len(refs) - 11) // 3
    srcs, (gate, up, dk, dv), dsts = refs[:n], refs[n:n + 4], refs[n + 4:2 * n + 4]
    (g_in, g_out, kv_in), holds, sems = refs[2 * n + 4:2 * n + 7], refs[2 * n + 7:3 * n + 7], refs[3 * n + 7:]
    t_in, t_out, p_in, p_out = sems
    step = LANE * 11
    cols = g_in.shape[1]
    hd = dk.shape[0] // (kv_in.shape[0] // LANE)
    starts = [(w, i) for i in range(cols // step) for w in range(2)]

    def fetch(w, i):
        rs = pl.ds(i * step, step)
        return pltpu.make_async_copy((dg_hbm, du_hbm)[w].at[rs, :], g_in.at[w, rs, :], t_in.at[w, i])

    def put(w, i):
        cs = pl.ds(i * step, step)
        return pltpu.make_async_copy(g_out.at[w, :, cs], (gate, up)[w].at[:, cs], t_out.at[w, i])
    moves = [(pltpu.make_async_copy(a, h, p_in.at[k]), pltpu.make_async_copy(h, b, p_out.at[k])) for k, (a, h, b) in enumerate(zip(srcs, holds, dsts))]
    kv = pltpu.make_async_copy(dkv_hbm, kv_in, p_in.at[n])
    for w, i in starts:
        fetch(w, i).start()
    kv.start()
    for load, _ in moves:
        load.start()
    for w, i in starts:
        fetch(w, i).wait()

        at = pl.ds(i * step, step)
        g_out[w, :, at] = g_in[w, at, :].T
        put(w, i).start()
    kv.wait()
    for k in range(dk.shape[0] // hd):
        for i, ref in enumerate((dk, dv)):
            ref[k * hd:(k + 1) * hd, :] = kv_in[(2 * k + i) * hd:(2 * k + i + 1) * hd, :]
    for load, store in moves:
        load.wait()
        store.start()
    for w, i in starts:
        put(w, i).wait()
    for _, store in moves:
        store.wait()


def rope_tables(positions, head_dim):
    half_dim = head_dim // 2
    inv_freq = 1.0 / (ROPE_BASE ** (jnp.arange(half_dim, dtype=F32) * (2.0 / head_dim)))
    angles = positions.astype(F32)[None, :] * inv_freq[:, None]
    return jnp.cos(angles), jnp.sin(angles)


def solution(mesh):
    assert mesh.shape['sp'] == N_DEV

    def layer_step(x_in, positions, d_out, norm1_gain, norm2_gain, w_q, w_k, w_v, w_o, w_gate, w_up, w_down):
        tokens, dim = x_in.shape
        seq = tokens * N_DEV
        n_q, hd = w_q.shape[1:]
        n_kv = w_k.shape[1]
        qw = n_q // N_DEV * hd
        rows = w_q.shape[0]
        feat = w_down.shape[0]
        cols = (n_q + 2 * n_kv) * hd
        lanes = qw // hd * QB
        vm = pltpu.VMEM
        full = vm((N_CHIP, WIDE, dim), BF16)
        gain_scr = vm((N_CHIP, dim), F32)
        tok_shapes = 2 * (((tokens, dim), BF16),)
        dw_shapes = 2 * (((feat * N_DEV, rows), F32),)

        cos_own, sin_own = rope_tables(positions, hd)
        row = lambda v: v.reshape(1, rows)
        by_head = lambda w: w.transpose(1, 2, 0).reshape(-1, rows)
        wo_own = w_o.reshape(qw, dim)

        args = (x_in, row(norm1_gain), row(norm2_gain), row(positions), by_head(w_q), by_head(w_k), by_head(w_v), cos_own, sin_own, w_gate, w_up, wo_own)
        qkv, u, small_all, wqkv, attn_t, stat, wgu, hidden, mlp_in = call(
            functools.partial(head, n_kv, hd), 0, len(args),
            (((qw + 2 * hd, seq), BF16), tok_shapes[0], ((N_DEV, N_CHIP, rows), F32), ((N_CHIP, cols, WIDE), BF16),
             ((qw, seq), BF16), ((seq // QB, 2, lanes), F32), ((2 * feat, dim), BF16), *tok_shapes),
            [full, vm((tokens, dim), F32), vm((tokens, dim), BF16), vm((seq, qw), BF16),
             vm((N_CHIP, rows), F32), vm((cols, rows), BF16), vm((N_CHIP, cols, WIDE), BF16), vm((cols, tokens), F32), vm((cols, tokens), BF16), gain_scr,
             vm((feat * N_DEV, rows), BF16), vm((feat * N_DEV, rows), BF16), vm((seq, lanes), F32), vm((seq, hd), BF16), dma(N_CHIP),
             *Gather.sems, *(6 * Swap.sems), *Gather.sems], 4 * qw * seq * seq, far_out=(3,))(*args)
        args = (mlp_in, d_out, wgu, w_down, u)
        u_col, m_full, glu, dgu, d_down = call(
            mlp_local, 1, len(args),
            (((seq, rows), BF16), ((N_CHIP, WIDE, dim), BF16), ((feat, seq), BF16), ((2 * feat, seq), BF16), ((feat, dim), F32)),
            [vm((2 * feat, dim), BF16), vm((feat, dim), BF16), vm((feat, seq), BF16), vm((2 * feat, seq), BF16), dma(2),
             full, full, dma(N_CHIP, 3), *(2 * Gather.sems), *Swap.sems],
            8 * feat * seq * dim, far_in=(2, 3), far_out=(1, 2, 3))(*args)
        args = (dgu, wgu, hidden, small_all, d_out, wo_own, attn_t, glu, w_down, m_full)
        y_out, d_hidden, d_attn, d_wo, d_g2, d_gate_t, d_up_t = call(
            mlp_back, 2, len(args),
            (*tok_shapes, ((qw, seq), BF16), ((qw, dim), F32), ((N_CHIP, dim), F32), *dw_shapes),
            [vm((N_CHIP, WIDE, WIDE), BF16), vm((2 * feat, WIDE), F32),
             vm((2 * feat, seq), BF16), vm((2 * feat, dim), BF16), vm((feat, seq), BF16), vm((feat, dim), BF16), dma(5),
             full, gain_scr, vm((WIDE, 2 * feat), BF16), vm((WIDE, feat), BF16), pltpu.SemaphoreType.REGULAR,
             *Scatter.scratch(tokens, dim), *Scatter.sems, *Gather.sems, *(2 * Swap.sems)], 4 * feat * seq * dim,
            far_in=(0, 1, 7, 8, 9), far_out=(5, 6))(*args)
        cos_all, sin_all = rope_tables(small_all[:, 2].reshape(-1), hd)
        args = (qkv, d_attn, stat, cos_all, sin_all, dgu, m_full, u_col, cos_own, sin_own, wqkv, x_in, small_all, d_hidden, d_g2, d_gate_t, d_up_t)
        d_gate_t, d_up_t, d_wq, d_wkv, d_x, gains = call(
            functools.partial(back, n_kv, hd), 3, len(args),
            (*dw_shapes, ((n_q * hd, rows), F32), ((2 * n_kv * hd, rows), F32), tok_shapes[0], ((N_CHIP, rows), F32)),
            [vm((seq, lanes), F32), vm((seq, lanes), BF16), vm((seq, hd), BF16), vm((seq, hd), BF16), vm((seq, hd), F32), vm((seq, hd), F32),
             vm((N_CHIP, 2 * feat, WIDE), F32), vm((qw, seq), BF16), vm((seq, 2 * hd), BF16), full,
             full, vm((N_CHIP, cols, WIDE), BF16), vm((N_DEV, tokens, 2 * hd), BF16), vm((2 * n_kv * hd, tokens), BF16), vm((2 * n_kv * hd, seq), BF16),
             vm((tokens, cols), BF16), vm((tokens, dim), F32), gain_scr, gain_scr, gain_scr, vm((N_DEV, N_CHIP, rows), F32), dma(), dma(2), dma(N_CHIP),
             *(3 * Swap.sems), *(2 * Gather.sems), *Swap.sems], 10 * qw * seq * seq, far_in=(6, 10, 15, 16), far_out=(0, 1), aliases={15: 0, 16: 1})(*args)
        moved = (d_wq, d_wo, d_down, d_x, y_out, gains)
        half_kv = jax.ShapeDtypeStruct((n_kv * hd, rows), F32)
        wide = jax.ShapeDtypeStruct((rows, feat * N_DEV), F32)
        d_gate, d_up, d_wk, d_wv, d_wq, d_wo, d_down, d_x, y_out, gains = pl.pallas_call(
            finish,
            out_shape=[wide, wide, half_kv, half_kv] + [jax.ShapeDtypeStruct(v.shape, v.dtype) for v in moved],
            in_specs=[IN_HBM] * (3 + len(moved)), out_specs=[IN_HBM] * 2 + on_chip(2) + [IN_HBM] * len(moved),
            scratch_shapes=[vm((2, feat * N_DEV, rows), F32), vm((2, rows, feat * N_DEV), F32), vm(d_wkv.shape, F32)]
            + [vm(v.shape, v.dtype) for v in moved] + [dma(2, 4), dma(2, 4), dma(len(moved) + 1), dma(len(moved))],
            compiler_params=pltpu.CompilerParams(vmem_limit_bytes=VMEM_CAP), name='finish',
        )(d_gate_t, d_up_t, d_wkv, *moved)
        by_row = lambda g, heads: g.reshape(heads, hd, rows).transpose(2, 0, 1)
        return (y_out, d_x, gains[0], gains[1], by_row(d_wq, n_q), by_row(d_wk, n_kv), by_row(d_wv, n_kv),
                d_wo.reshape(w_o.shape), d_gate, d_up, d_down)

    all_rows = P('sp')
    return jax.shard_map(layer_step, mesh=mesh, in_specs=(all_rows,) * 12, out_specs=(all_rows,) * 11, check_vma=False)
```

```python
import functools
import jax
import jax.numpy as jnp
from jax import lax
from jax.experimental import pallas as pl
from jax.experimental.pallas import tpu as pltpu
from jax.sharding import PartitionSpec as P

ROPE_BASE = 10000.0
NORM_EPS = 1e-5
NEG_LARGE = -1e30
F32 = jnp.float32
BF16 = jnp.bfloat16
N_DEV, N_CHIP, LANE, WIDE, CHUNK, STRIP = 16, 8, 128, 256, 512, 16
NT = (((1,), (1,)), ((), ()))
TN = (((0,), (0,)), ((), ()))
NN = (((1,), (0,)), ((), ()))
MESH = pl.DeviceIdType.MESH
VMEM_CAP = 62 * 1024 * 1024

CORE, X, Y, Z = 1, 2, 4, 8
XYZ = X + Y + Z
ORDERS = ((X, Y, Z), (Y, Z, X), (Z, X, Y))
CHIP_MASKS = (0, X, Y, Z, X + Y, X + Z, Y + Z, XYZ)
NEAR = (CORE, X, Y, Z)
OTHERS = range(1, N_DEV)
SETS = tuple(tuple(m + c for m in masks for c in (0, CORE)) for masks in ((XYZ,), (X, Y + Z), (Y, X + Z), (Z, X + Y)))
N_COL = len(ORDERS)
COLOURS = range(N_COL)


def mm(a, b, dims):
    return lax.dot_general(a, b, dims, preferred_element_type=F32)


def seg(index, width=LANE):
    return pl.ds(pl.multiple_of(index * width, width), width)


def loop(count, body):
    lax.fori_loop(0, count, lambda i, c: (body(i), c)[1], 0)


def differing(index, mask):
    return sum(((index // bit + mask // bit) % 2) * bit for bit in NEAR)


def flipped(index, mask):
    out = index
    for bit in NEAR:
        if mask & bit:
            out = out + (1 - 2 * ((index // bit) % 2)) * bit
    return out


def thirds(total, unit):
    n = total // unit
    first = (n + 2) // 3
    second = (n - first + 1) // 2
    sizes = (first * unit, second * unit, (n - first - second) * unit)
    return ((0, sizes[0]), (sizes[0], sizes[1]), (sizes[0] + sizes[1], sizes[2]))


def pieces(rows, cols, unit):
    share = cols // LANE // N_COL * LANE
    strips = thirds(rows, unit)
    rest = cols - N_COL * share
    return [[(pl.ds(0, rows), pl.ds(c * share, share)), (pl.ds(*strips[c]), pl.ds(N_COL * share, rest))] for c in COLOURS]


def enter(me, masks):
    barrier = pltpu.get_barrier_semaphore()
    for mask in masks:
        pl.semaphore_signal(barrier, inc=1, device_id=(flipped(me, mask),), device_id_type=MESH)
    pl.semaphore_wait(barrier, len(masks))


def remote(src, dst, send, recv, peer):
    return pltpu.make_async_remote_copy(src_ref=src, dst_ref=dst, send_sem=send, recv_sem=recv, device_id=(peer,), device_id_type=MESH)


def dma(*shape):
    return pltpu.SemaphoreType.DMA(shape)


class Swap:
    sems = (dma(N_DEV), dma(N_DEV))

    def __init__(self, src, dst, sems, me):
        self.src, self.dst, (self.send, self.recv), self.me = src, dst, sems, me

    def copy(self, mask):
        peer = differing(self.me, mask)
        return remote(self.src(peer), self.dst(self.me), self.send.at[mask], self.recv.at[mask], peer)

    def arrival(self, mask):
        view = self.dst(differing(self.me, mask))
        return remote(view, view, self.send.at[mask], self.recv.at[mask], self.me)

    def each(self, masks, act):
        if masks is None:
            loop(N_DEV - 1, lambda i: act(i + 1))
        else:
            for mask in masks:
                act(mask)

    def start(self, masks=None):
        self.each(masks, lambda mask: self.copy(mask).start())

    def advance(self, n):
        if n:
            self.wait_send(SETS[n - 1])
        self.start(SETS[n])

    def wait_recv(self, masks=None):
        self.each(masks, lambda mask: self.arrival(mask).wait_recv())

    def wait_send(self, masks=None):
        self.each(masks, lambda mask: self.copy(mask).wait_send())


class Gather:
    ROUNDS = ((0,), (1,), (2,), (0, 1), (0, 2), (1, 2), (0, 1, 2))
    READY = ((0,), (), (), (X, Y), (Z,), (X + Y, X + Z), (Y + Z, XYZ))
    sems = (dma(N_COL, N_CHIP, 2), dma(N_COL, N_CHIP, 2), dma(N_CHIP), dma(N_CHIP))

    def __init__(self, own, block, cut, sems, me):
        self.own, self.block, self.cut, self.me = own, block, cut, me
        self.send, self.recv, self.pair_send, self.pair_recv = sems

    def source(self, mask):
        return self.block(flipped(self.me, mask)) if mask else self.own

    def unit(self, colour, mask, axis):
        ends = zip(self.cut(self.source(mask), colour), self.cut(self.block(flipped(self.me, mask)), colour))
        j = self.sends(colour).index((mask, axis))
        return [remote(src, dst, self.send.at[colour, j, i], self.recv.at[colour, (mask + axis) // 2, i],
                       flipped(self.me, axis)) for i, (src, dst) in enumerate(ends)]

    def sends(self, colour):
        return [(0, axis) for axis in ORDERS[colour]] + [step[1:] for step in self.onward(colour)]

    def start_unit(self, colour, mask, axis):
        for copy in self.unit(colour, mask, axis):
            copy.start()

    def pair(self, mask):
        return remote(self.source(mask), self.block(flipped(self.me, mask)), self.pair_send.at[mask // 2],
                      self.pair_recv.at[mask // 2], flipped(self.me, CORE))

    def wait_pair(self, mask):
        view = self.block(flipped(self.me, mask + CORE))
        remote(view, view, self.pair_send.at[mask // 2], self.pair_recv.at[mask // 2], self.me).wait_recv()

    def onward(self, colour):
        order = ORDERS[colour]
        for picks in self.ROUNDS:
            for axis in order[picks[-1] + 1:]:
                yield picks, sum(order[p] for p in picks), axis

    def start(self):
        for pos in COLOURS:
            for colour in COLOURS:
                self.start_unit(colour, 0, ORDERS[colour][pos])
        self.pair(0).start()

    def round(self, r):
        for colour in COLOURS:
            mask = sum(ORDERS[colour][p] for p in self.ROUNDS[r])
            for i, view in enumerate(self.cut(self.block(flipped(self.me, mask)), colour)):
                remote(view, view, self.send.at[colour, 0, i], self.recv.at[colour, mask // 2, i], self.me).wait_recv()
            for picks, at, axis in self.onward(colour):
                if picks == self.ROUNDS[r]:
                    self.start_unit(colour, at, axis)
        for mask in {2: (X, Y, Z), 5: (X + Y, X + Z, Y + Z), 6: (XYZ,)}.get(r, ()):
            self.pair(mask).start()

    def finish(self):
        for colour in COLOURS:
            for i, view in enumerate(self.cut(self.own, colour)):
                loop(len(self.sends(colour)), lambda j: remote(view, view, self.send.at[colour, j, i], self.recv.at[colour, j, i], self.me).wait_send())
        loop(N_CHIP, lambda j: remote(self.own, self.own, self.pair_send.at[j], self.pair_recv.at[j], self.me).wait_send())


def row_gather(own, full, sems, me, extra=None):
    rows, width = own.shape
    parts = pieces(rows, width, STRIP)
    if extra is not None:
        share = width // LANE // N_COL * LANE
        more = width - N_COL * share
        parts = [[(pl.ds(0, rows), pl.ds(c * share + more * (c > extra), share + more * (c == extra)))] for c in COLOURS]

    def block(o):
        return full.at[o // 2, seg(o % 2), :]

    return Gather(own, block, lambda view, c: [view.at[rs, cs] for rs, cs in parts[c]], sems, me)


def keep_own(own, full, me):
    def step(i):
        full[me // 2, pl.ds(pl.multiple_of((me % 2) * LANE + i * STRIP, STRIP), STRIP), :] = own[seg(i, STRIP), :]
    loop(LANE // STRIP, step)


class Scatter:
    ORDER = (XYZ, X + Y, Y + Z, X + Z, X, Y, Z, 0)
    sems = (dma(N_CHIP), dma(N_CHIP), dma(N_COL, N_CHIP, 2), dma(N_COL, N_CHIP, 2))

    @staticmethod
    def scratch(tokens, dim):
        return [pltpu.VMEM((n, tokens, dim), F32) for n in (N_CHIP, 2, N_CHIP, N_CHIP - 1)]

    def __init__(self, part, other, pair_in, link_in, sems, me):
        self.part, self.other, self.pair_in, self.link_in, self.me = part, other, pair_in, link_in, me
        self.pair_send, self.pair_recv, self.link_send, self.link_recv = sems
        self.tokens, self.dim = part.shape[1:]
        self.pieces = pieces(self.tokens, self.dim, STRIP // 2)
        self.ready, self.sent = set(), [0] * N_COL

    @staticmethod
    def first(colour, mask):
        return next((i for i, a in enumerate(ORDERS[colour]) if mask & a), 3)

    def slot(self, colour, mask, axis):
        slots = [(m, a) for m in self.ORDER for a in ORDERS[colour][:self.first(colour, m)]]
        return slots.index((mask, axis))

    def pair(self, i):
        return remote(self.other.at[i % 2], self.pair_in.at[i], self.pair_send.at[i], self.pair_recv.at[i], flipped(self.me, CORE))

    def link(self, colour, mask):
        axis = ORDERS[colour][self.first(colour, mask)]
        slot = self.slot(colour, mask - axis, axis)
        i = self.ORDER.index(mask)
        return [remote(self.part.at[i, rs, cs], self.link_in.at[slot, rs, cs], self.link_send.at[colour, i, k],
                       self.link_recv.at[colour, slot, k], flipped(self.me, axis)) for k, (rs, cs) in enumerate(self.pieces[colour])]

    def start_link(self, colour, mask):
        for copy in self.link(colour, mask):
            copy.start()

    def add(self, mask, ref, cs):
        i = self.ORDER.index(mask)

        def step(r):
            rs = seg(r, STRIP)
            self.part[i, rs, cs] += ref[rs, cs]
        loop(self.tokens // STRIP, step)

    def finish_pair(self, i):
        self.pair(i).wait_recv()
        self.add(self.ORDER[i], self.pair_in.at[i], pl.ds(0, self.dim))
        self.ready.add(self.ORDER[i])
        for colour in COLOURS:
            a, b, c = ORDERS[colour]
            todo = (XYZ, a + b, a + c, a)
            while self.sent[colour] < len(todo) and todo[self.sent[colour]] in self.ready:
                self.start_link(colour, todo[self.sent[colour]])
                self.sent[colour] += 1

    def take(self, colour, mask, axis):
        for copy in self.link(colour, mask + axis):
            copy.wait_recv()
        ref = self.link_in.at[self.slot(colour, mask, axis)]
        (_, wide), (rs, cs) = self.pieces[colour]
        self.add(mask, ref, wide)
        self.part[self.ORDER.index(mask), rs, cs] += ref[rs, cs]

    def run(self, product, between=lambda i: None):
        for i, mask in enumerate(self.ORDER):
            if i > 1:
                self.pair(i - 2).wait_send()
            product(i, flipped(self.me, mask) // 2)
            self.pair(i).start()
            if i:
                self.finish_pair(i - 1)
            between(i)
        self.finish_pair(N_CHIP - 1)
        for step in range(2):
            for colour in COLOURS:
                a, b, c = ORDERS[colour]
                mask = (b + c, b)[step]
                self.take(colour, mask, a)
                self.start_link(colour, mask)
        for colour in COLOURS:
            a, b, c = ORDERS[colour]
            self.take(colour, c, a)
            self.take(colour, c, b)
            self.start_link(colour, c)
        for colour in COLOURS:
            for axis in ORDERS[colour]:
                self.take(colour, 0, axis)
        return self.part.at[N_CHIP - 1]

    def finish(self):
        for i in (N_CHIP - 2, N_CHIP - 1):
            self.pair(i).wait_send()
        for colour in COLOURS:
            for k, (rs, cs) in enumerate(self.pieces[colour]):
                view = self.part.at[0, rs, cs]
                loop(N_CHIP - 1, lambda i: remote(view, view, self.link_send.at[colour, i, k], self.link_recv.at[colour, i, k], self.me).wait_send())


def block_product(s, a_ref, w_ref, a_t):
    core = s.me % 2

    def product(i, chip):
        a_t[...] = a_ref[:, seg(chip, WIDE)].T

        def step(n):
            cs = seg(n, CHUNK)
            s.other[i % 2, :, cs] = mm(a_t[seg(1 - core), :], w_ref[:, cs], NN)
            s.part[i, :, cs] = mm(a_t[seg(core), :], w_ref[:, cs], NN)
        loop(s.dim // CHUNK, step)
    return product


def on_chip(n):
    return [pl.BlockSpec(memory_space=pltpu.VMEM)] * n


IN_HBM = pl.BlockSpec(memory_space=pl.ANY)


def call(kernel, ident, args, outs, scratch, flops, far_in=(), far_out=(), aliases={}):
    specs = [IN_HBM if i in far_in else on_chip(1)[0] for i in range(args)]
    out_specs = [IN_HBM if i in far_out else on_chip(1)[0] for i in range(len(outs))]
    return pl.pallas_call(
        kernel,
        out_shape=[jax.ShapeDtypeStruct(shape, dtype) for shape, dtype in outs],
        in_specs=specs, out_specs=out_specs, scratch_shapes=scratch, input_output_aliases=aliases,
        cost_estimate=pl.CostEstimate(flops=flops, bytes_accessed=flops // CHUNK, transcendentals=0),
        compiler_params=pltpu.CompilerParams(collective_id=ident, has_side_effects=True, vmem_limit_bytes=VMEM_CAP),
        name=kernel.func.__name__ if isinstance(kernel, functools.partial) else kernel.__name__,
    )


def fetch_all(sem, *pairs):
    copies = [pltpu.make_async_copy(src, dst, sem.at[i]) for i, (src, dst) in enumerate(pairs)]
    for copy in copies:
        copy.start()
    return copies


def gain_row(dst, small_all, which):
    for o in range(N_DEV):
        dst[:1, o * LANE:(o + 1) * LANE] = small_all[o, which:which + 1, :]


def norm_rows(src, gain, dst):
    def step(i):
        rs = seg(i, STRIP)
        t = src[rs, :].astype(F32)
        dst[rs, :] = (t * lax.rsqrt(jnp.mean(t * t, axis=-1, keepdims=True) + NORM_EPS) * gain[:1, :]).astype(BF16)
    loop(src.shape[0] // STRIP, step)


def norm_back(dy, src, gain, skip, dst, dgain):
    def step(i):
        rs = seg(i, STRIP)
        d = dy[rs, :].astype(BF16).astype(F32)
        t = src[rs, :].astype(F32)
        inv = lax.rsqrt(jnp.mean(t * t, axis=-1, keepdims=True) + NORM_EPS)
        gd = gain[:1, :] * d
        pull = jnp.mean(gd * t, axis=-1, keepdims=True)
        dst[rs, :] = (skip[rs, :].astype(F32) + (inv * gd - t * (inv * inv * inv * pull))).astype(BF16)
        g = d * (t * inv)
        dgain[...] += g[:N_CHIP] + g[N_CHIP:]
    dgain[...] = jnp.zeros_like(dgain)
    loop(src.shape[0] // STRIP, step)


QB = 256
KB = 256


def key_rows(dst, src, lo, hd):
    def step(i):
        dst[seg(i, KB), :] = src[lo:lo + hd, seg(i, KB)].T
    loop(src.shape[1] // KB, step)


def score_block(k, q2, scale, diagonal):
    s = mm(k, q2, NN) * scale
    if diagonal:
        key = lax.broadcasted_iota(jnp.int32, s.shape, 0)
        qry = lax.broadcasted_iota(jnp.int32, s.shape, 1) % QB
        s = jnp.where(qry >= key, s, NEG_LARGE)
    return s


def side_by_side(ref, heads, hd, qs):
    return jnp.concatenate([ref[h * hd:(h + 1) * hd, qs] for h in range(heads)], axis=1)


def head(groups, hd, x_ref, g1_ref, g2_ref, pos_ref, wq_ref, wk_ref, wv_ref, cos_ref, sin_ref, wg_ref, wu_ref, wo_ref, qkv_ref, u_scr, small_all, w_out, o_ref, stat_ref, wgu_ref, h_ref, m_ref,
         full_w, acc_o, o_tok, o_send, small_ref, w_ref, full, acc, rot, g_scr, wg_t, wu_t, s_scr, k_scr, osem, *sems):
    me = lax.axis_index('sp')
    tokens, dim = x_ref.shape
    cols = w_ref.shape[0]
    small_ref[...] = jnp.concatenate([r[...].astype(F32) for r in (g1_ref, g2_ref, pos_ref)] + [jnp.zeros((N_CHIP - 3, LANE), F32)], axis=0)
    w_ref[:wq_ref.shape[0], :] = wq_ref[...]
    for k in range(groups):
        for i, ref in enumerate((wk_ref, wv_ref)):
            w_ref[pl.ds(wq_ref.shape[0] + (2 * k + i) * hd, hd), :] = ref[k * hd:(k + 1) * hd, :]
    qw = tokens
    q_all = N_DEV * qw
    gsems, ssems, qsems, ksems, gate_sems, up_sems, osems = sems[:4], *(sems[i:i + 2] for i in range(4, len(sems) - 4, 2))
    gw = row_gather(wo_ref, full_w, sems[-4:], me, 1)
    feat = wg_ref.shape[1] // N_DEV
    enter(me, OTHERS)
    smalls = Swap(lambda peer: small_ref, lambda o: small_all.at[o], ssems, me)
    smalls.start()
    parts = thirds(cols, STRIP)
    g = Gather(w_ref, lambda o: full.at[o // 2, :, seg(o % 2)], lambda view, c: [view.at[pl.ds(*parts[c]), :]], gsems, me)
    g.start()
    gates = Swap(lambda peer: wg_t.at[seg(peer, feat), :], lambda o: wgu_ref.at[:feat, seg(o)], gate_sems, me)
    ups = Swap(lambda peer: wu_t.at[seg(peer, feat), :], lambda o: wgu_ref.at[feat:, seg(o)], up_sems, me)

    def advance(n):
        gates.advance(n)
        ups.advance(n)

    def transpose(i):
        wg_t[seg(i, CHUNK), :] = wg_ref[:, seg(i, CHUNK)].T
        wu_t[seg(i, CHUNK), :] = wu_ref[:, seg(i, CHUNK)].T
    loop(wg_ref.shape[1] // CHUNK, transpose)
    advance(0)

    def own_block(i):
        full[me // 2, seg(i, WIDE), seg(me % 2)] = w_ref[seg(i, WIDE), :]
    loop(cols // WIDE, own_block)
    acc[...] = jnp.zeros_like(acc)
    small_all[me] = small_ref[...]
    smalls.wait_recv()
    gain_row(g_scr, small_all, 0)
    norm_rows(x_ref, g_scr, u_scr)

    def keep(mask):
        chip = flipped(me, mask) // 2
        return pltpu.make_async_copy(full.at[chip], w_out.at[chip], osem.at[mask // 2])

    def use(mask):
        g.wait_pair(mask)
        keep(mask).start()
        chip = flipped(me, mask) // 2
        u = u_scr[:, seg(chip, WIDE)]

        def step(i):
            rs = seg(i, cols // 2)
            acc[rs, :] += mm(full[chip, rs, :], u, NT)
        loop(2, step)

    for r in range(len(g.ROUNDS)):
        g.round(r)
        if r in (2, 4):
            advance(r // 2)
        for mask in g.READY[r]:
            use(mask)

    half = hd // 2
    cos, sin = cos_ref[...], sin_ref[...]

    def turn(h):
        first = seg(2 * h, half)
        second = seg(2 * h + 1, half)
        p = acc[first, :].astype(BF16).astype(F32)
        q = acc[second, :].astype(BF16).astype(F32)
        rot[first, :] = (p * cos - q * sin).astype(BF16)
        rot[second, :] = (q * cos + p * sin).astype(BF16)
    loop(q_all // hd, turn)
    for k in range(groups):
        turn(q_all // hd + 2 * k)
        vs = seg(q_all // hd + 2 * k + 1, hd)
        rot[vs, :] = acc[vs, :].astype(BF16)
    per = N_DEV // groups
    q_rows = lambda peer: seg(peer, qw)
    kv_rows = lambda peer: seg(q_all // (2 * hd) + peer // per, 2 * hd)
    qs = Swap(lambda peer: rot.at[q_rows(peer), :], lambda o: qkv_ref.at[:qw, seg(o, tokens)], qsems, me)
    kvs = Swap(lambda peer: rot.at[kv_rows(peer), :], lambda o: qkv_ref.at[qw:, seg(o, tokens)], ksems, me)
    qs.start()
    kvs.start()
    gw.start()
    keep_own(wo_ref, full_w, me)
    gain_row(g_scr, small_all, 1)
    qkv_ref[:qw, seg(me, tokens)] = rot[q_rows(me), :]
    qkv_ref[qw:, seg(me, tokens)] = rot[kv_rows(me), :]
    wgu_ref[:feat, seg(me)] = wg_t[seg(me, feat), :]
    wgu_ref[feat:, seg(me)] = wu_t[seg(me, feat), :]
    gates.start((CORE,))
    ups.start((CORE,))
    for swap in (qs, kvs):
        swap.wait_recv()
    heads = qkv_ref.shape[0] // hd - 2
    seq = qkv_ref.shape[1]
    scale = hd ** -0.5
    lanes = heads * QB
    key_rows(k_scr, qkv_ref, qw, hd)

    outs = Swap(lambda peer: o_send.at[seg(peer), :], lambda o: o_tok.at[:, seg(o)], osems, me)

    def q_block(qb):
        for at, r in ((2, 0), (4, 1), (5, 2), (6, 3), (7, 4)):
            @pl.when(qb == at)
            def _():
                gw.round(r)
        qs = seg(qb, QB)
        q2 = side_by_side(qkv_ref, heads, hd, qs)

        def scores(kb, top, diagonal):
            s = score_block(k_scr[seg(kb, KB), :], q2, scale, diagonal)
            s_scr[seg(kb, KB), :] = s
            return jnp.maximum(top, jnp.max(s, axis=0, keepdims=True))

        top = lax.fori_loop(0, qb, lambda kb, t: scores(kb, t, False), jnp.full((1, lanes), NEG_LARGE, F32))
        top = scores(qb, top, True)

        def expo(kb, tot):
            e = jnp.exp(s_scr[seg(kb, KB), :] - top)
            s_scr[seg(kb, KB), :] = e
            return tot + jnp.sum(e, axis=0, keepdims=True)

        inv = 1.0 / lax.fori_loop(0, qb + 1, expo, jnp.zeros((1, lanes), F32))

        def weigh(kb, acc):
            p = (s_scr[seg(kb, KB), :] * inv).astype(BF16)
            return acc + mm(qkv_ref[qw + hd:, seg(kb, KB)], p, NN)

        acc = lax.fori_loop(0, qb + 1, weigh, jnp.zeros((hd, lanes), F32))
        for h in range(heads):
            o_ref[h * hd:(h + 1) * hd, qs] = acc[:, h * QB:(h + 1) * QB].astype(BF16)
        stat_ref[qb, :1, :] = top
        stat_ref[qb, 1:, :] = inv
        o_send[qs, :] = o_ref[:, qs].T

    loop(seq // QB, q_block)
    outs.start()
    advance(3)
    o_tok[:, seg(me)] = o_send[seg(me), :]
    for r in (5, 6):
        gw.round(r)
    outs.wait_recv()
    for mask in CHIP_MASKS:
        gw.wait_pair(mask)

    def project(n):
        cs = seg(n, CHUNK)
        acc_o[:, cs] = mm(o_tok[...], full_w[:, :, cs].reshape(dim, CHUNK), NN)
    loop(dim // CHUNK, project)

    def residual(i):
        rs = seg(i, STRIP)
        h_ref[rs, :] = (x_ref[rs, :].astype(F32) + acc_o[rs, :]).astype(BF16)
    loop(tokens // STRIP, residual)
    norm_rows(h_ref, g_scr, m_ref)
    for swap in (gates, ups):
        swap.wait_recv()
    for mask in CHIP_MASKS:
        keep(mask).wait()
    outs.wait_send()
    for swap in (gates, ups):
        swap.wait_send((CORE,) + SETS[3])
    g.finish()
    gw.finish()
    for swap in (smalls, qs, kvs):
        swap.wait_send()


def dw_swaps(stage, gate_hbm, up_hbm, sems, me):
    feat = gate_hbm.shape[0] // N_DEV
    return [Swap(lambda peer, lo=lo: stage(peer).at[lo:lo + feat, seg(peer % 2)], lambda o, dst=dst: dst.at[seg(o, feat), :], sems[i:i + 2], me)
            for lo, dst, i in ((0, gate_hbm, 0), (feat, up_hbm, 2))]


def mlp(m_ref, dout_ref, wgu_hbm, down_hbm, u_ref, h_ref, small_all, wo_ref, o_ref,
        ucol_ref, m_out, dgu_out, ddown_ref, y_ref, dh_ref, do_ref, dwo_ref, dg_ref, gate_hbm, up_hbm,
        wgu_ref, down_ref, glu_ref, dgu_ref, isem, full_d, full_m, osem, stage, g_scr, dgu_t, glu_t, free, *scr):
    me = lax.axis_index('sp')
    feat, dim = down_ref.shape
    loads = fetch_all(isem, (wgu_hbm, wgu_ref), (down_hbm, down_ref))
    enter(me, OTHERS)
    sems = scr[4:]
    gd = row_gather(dout_ref, full_d, sems[:4], me, 0)
    gm = row_gather(m_ref, full_m, sems[4:8], me, 2)
    g = row_gather(dh_ref, full_d, sems[8:12], me, 1)
    ucols = Swap(lambda peer: u_ref.at[:, seg(peer)], lambda o: ucol_ref.at[seg(o), :], sems[12:14], me)
    gates, ups = dw_swaps(lambda peer: stage, gate_hbm, up_hbm, sems[14:18], me)
    gm.start()
    gd.start()
    ucol_ref[seg(me), :] = u_ref[:, seg(me)]
    keep_own(m_ref, full_m, me)
    keep_own(dout_ref, full_d, me)
    gain_row(g_scr, small_all, 1)
    dwo_ref[...] = jnp.zeros_like(dwo_ref)
    ddown_ref[...] = jnp.zeros_like(ddown_ref)

    def keep(mask):
        chip = flipped(me, mask) // 2
        ts = seg(chip, WIDE)
        ends = ((full_m.at[chip], m_out.at[chip]), (dgu_ref.at[:, ts], dgu_out.at[:, ts]))
        return [pltpu.make_async_copy(src, dst, osem.at[mask // 2, i]) for i, (src, dst) in enumerate(ends)]

    for load in loads:
        load.wait()

    def use(mask):
        gd.wait_pair(mask)
        gm.wait_pair(mask)
        chip = flipped(me, mask) // 2
        ts = seg(chip, WIDE)
        gu = mm(wgu_ref[...], full_m[chip], NT).astype(BF16).astype(F32)
        gate, up = gu[:feat], gu[feat:]
        d_glu = mm(down_ref[...], full_d[chip], NT).astype(BF16).astype(F32)
        sig = jax.nn.sigmoid(gate)
        act = gate * sig
        glu = (act * up).astype(BF16)
        glu_ref[:, ts] = glu
        dgu_ref[:feat, ts] = (d_glu * up * (sig * (1.0 + gate * (1.0 - sig)))).astype(BF16)
        dgu_ref[feat:, ts] = (d_glu * act).astype(BF16)

        def step(n):
            ddown_ref[:, seg(n, CHUNK)] += mm(glu, full_d[chip, :, seg(n, CHUNK)], NN)
        loop(dim // CHUNK, step)
        for copy in keep(mask):
            copy.start()

    for r in range(len(gm.ROUNDS)):
        gm.round(r)
        gd.round(r)
        if r == 3:
            ucols.start()
        for mask in gm.READY[r]:
            use(mask)
    far = seg(flipped(me, XYZ) // 2, WIDE)
    stage[...] = mm(dgu_ref[...], full_m[:, :, far].reshape(dgu_ref.shape[1], WIDE), NN)
    for swap in (gates, ups):
        swap.start(SETS[0])
    for gather in (gd, gm):
        gather.finish()
    s = Scatter(*scr[:4], sems[18:], me)
    total = s.run(block_product(s, dgu_ref, wgu_ref, dgu_t))
    for mask in NEAR:
        pl.semaphore_signal(free, inc=1, device_id=(flipped(me, mask),), device_id_type=MESH)
    norm_back(total, h_ref, g_scr, dout_ref, dh_ref, dg_ref)
    g.start()
    keep_own(dh_ref, full_d, me)
    s.finish()
    pl.semaphore_wait(free, len(NEAR))

    def use_dh(mask):
        g.wait_pair(mask)
        chip = flipped(me, mask) // 2
        do_ref[:, seg(chip, WIDE)] = mm(wo_ref[...], full_d[chip], NT).astype(BF16)
        o = o_ref[:, seg(chip, WIDE)]

        def step(n):
            dwo_ref[:, seg(n, CHUNK)] += mm(o, full_d[chip, :, seg(n, CHUNK)], NN)
        loop(dim // CHUNK, step)

    def between(i):
        if i < len(g.ROUNDS):
            g.round(i)
            for mask in g.READY[i]:
                use_dh(mask)

    s = Scatter(*scr[:4], sems[18:], me)
    total = s.run(block_product(s, glu_ref, down_ref, glu_t), between)
    y_ref[...] = (h_ref[...].astype(F32) + total[...]).astype(BF16)
    s.finish()
    g.finish()
    for swap in (gates, ups):
        swap.wait_recv(SETS[0])
        swap.wait_send(SETS[0])
    ucols.wait_recv()
    ucols.wait_send()
    for mask in CHIP_MASKS:
        for copy in keep(mask):
            copy.wait()


def back(groups, hd, qkv_ref, do_ref, stat_ref, cos_all, sin_all, dgu_ref, m_hbm, ucol_ref, cos_ref, sin_ref, w_hbm, x_ref, small_all, dh_ref, dg2_ref, dg_in, du_in,
         dg_hbm, du_hbm, dwq_ref, dwkv_ref, dx_ref, gain_ref,
         p_scr, dp_scr, k_scr, v_scr, dk_acc, dv_acc, stage, dq_scr, dkv_scr, m_scr,
         full, w_scr, shares, dkv_own, full_kv, dqkv, dn, g_scr, dg1, gains, gains_in, wsem, lsem, msem, *sems):
    heads = qkv_ref.shape[0] // hd - 2
    seq = qkv_ref.shape[1]
    scale = hd ** -0.5
    lanes = heads * QB
    qw = heads * hd
    half = hd // 2
    me = lax.axis_index('sp')
    feat = dgu_ref.shape[0] // 2
    first = (X, Y + Z, Y, X + Z, Z, X + Y, 0)

    def fetch(mask):
        cols = seg(flipped(me, mask) // 2, WIDE)
        return pltpu.make_async_copy(m_hbm.at[:, :, cols], m_scr.at[:, :, cols], msem.at[mask // 2])
    for mask in first:
        fetch(mask).start()
    load = pltpu.make_async_copy(w_hbm, w_scr, wsem)
    load.start()
    enter(me, OTHERS)
    gain_row(g_scr, small_all, 0)

    gates, ups = dw_swaps(lambda peer: stage.at[peer // 2], dg_hbm, du_hbm, sems[:4], me)
    gq = row_gather(dq_scr, full, sems[6:10], me)
    own = [pltpu.make_async_copy(swap.src(me), swap.dst(me), lsem.at[i]) for i, swap in enumerate((gates, ups))]

    def make(mask):
        chip = flipped(me, mask) // 2
        fetch(mask).wait()
        cols = m_scr[:, :, seg(chip, WIDE)].reshape(seq, WIDE)
        stage[chip] = mm(dgu_ref[...], cols, NN)

    def advance(n):
        for swap in (gates, ups):
            if n > 1:
                swap.wait_send(SETS[n - 1])
            swap.start(SETS[n])

    for i, mask in enumerate(first):
        make(mask)
        if i == 1:
            advance(1)
    gates.start((CORE,))
    ups.start((CORE,))
    for copy in own:
        copy.start()

    dk_acc[...] = jnp.zeros_like(dk_acc)
    dv_acc[...] = jnp.zeros_like(dv_acc)
    key_rows(k_scr, qkv_ref, qw, hd)
    key_rows(v_scr, qkv_ref, qw + hd, hd)

    def q_block(qb):
        @pl.when(qb == 4)
        def _():
            advance(2)
        qs = seg(qb, QB)
        q2 = side_by_side(qkv_ref, heads, hd, qs)
        do2 = side_by_side(do_ref, heads, hd, qs)
        top = stat_ref[qb, :1, :]
        inv = stat_ref[qb, 1:, :]

        def probs(kb, rd, diagonal):
            ks = seg(kb, KB)
            s = score_block(k_scr[ks, :], q2, scale, diagonal)
            p = jnp.exp(s - top) * inv
            dp = mm(v_scr[ks, :], do2, NN).astype(BF16)
            p_scr[ks, :] = p
            dp_scr[ks, :] = dp
            dv_acc[ks, :] += mm(p.astype(BF16), do2, NT)
            return rd + jnp.sum(dp.astype(F32) * p, axis=0, keepdims=True)

        rd = lax.fori_loop(0, qb, lambda kb, r: probs(kb, r, False), jnp.zeros((1, lanes), F32))
        rd = probs(qb, rd, True)

        def d_scores(kb, acc):
            ks = seg(kb, KB)
            ds = (p_scr[ks, :] * (dp_scr[ks, :].astype(F32) - rd) * scale).astype(BF16)
            dk_acc[ks, :] += mm(ds, q2, NT)
            return acc + mm(qkv_ref[qw:qw + hd, ks], ds, NN)

        acc = lax.fori_loop(0, qb + 1, d_scores, jnp.zeros((hd, lanes), F32))
        cos, sin = cos_all[:, qs], sin_all[:, qs]
        for h in range(heads):
            dq = acc[:, h * QB:(h + 1) * QB].astype(BF16).astype(F32)
            p, q = dq[:half], dq[half:]
            dq_scr[h * hd:h * hd + half, qs] = (p * cos + q * sin).astype(BF16)
            dq_scr[h * hd + half:(h + 1) * hd, qs] = (q * cos - p * sin).astype(BF16)

    loop(seq // QB, q_block)

    def share(i):
        rs = seg(i, WIDE)
        dkv_scr[rs, :] = jnp.concatenate([dk_acc[rs, :], dv_acc[rs, :]], axis=1).astype(BF16)
    loop(seq // WIDE, share)
    tokens = ucol_ref.shape[1]
    per = N_DEV // groups
    q_all = dwq_ref.shape[0]
    sh = Swap(lambda peer: dkv_scr.at[seg(peer, tokens), :], lambda o: shares.at[o], sems[4:6], me)
    parts = thirds(dkv_own.shape[0], STRIP)
    gk = Gather(dkv_own, lambda o: full_kv.at[:, seg(o, tokens)], lambda view, c: [view.at[pl.ds(*parts[c]), :]], sems[10:14], me)
    gs = Swap(lambda peer: gains.at[:, seg(peer)], lambda o: gains_in.at[o], sems[14:], me)
    sh.start()
    gq.start()
    keep_own(dq_scr, full, me)
    shares[me] = dkv_scr[seg(me, tokens), :]
    sh.wait_recv()
    cos, sin = cos_ref[...], sin_ref[...]
    for k in range(groups):
        both = sum(shares[per * k + i].astype(F32) for i in range(per)).astype(BF16).astype(F32).T
        p, q = both[:half], both[half:hd]
        lo = 2 * hd * k
        dkv_own[lo:lo + half, :] = (p * cos + q * sin).astype(BF16)
        dkv_own[lo + half:lo + hd, :] = (q * cos - p * sin).astype(BF16)
        dkv_own[lo + hd:lo + 2 * hd, :] = both[hd:].astype(BF16)
    gk.start()
    full_kv[:, seg(me, tokens)] = dkv_own[...]
    for k in range(groups):
        dqkv[:, q_all + 2 * hd * k:q_all + 2 * hd * (k + 1)] = dkv_own[2 * hd * k:2 * hd * (k + 1), :].T

    def use(mask):
        gq.wait_pair(mask)
        chip = flipped(me, mask) // 2
        dwq_ref[seg(chip, WIDE), :] = mm(full[chip], ucol_ref[...], NN)
        dqkv[:, seg(chip, WIDE)] = full[chip, :, seg(me, tokens)].T

    for r in range(len(gq.ROUNDS)):
        gq.round(r)
        gk.round(r)
        if r == 3:
            advance(3)
        for mask in gq.READY[r]:
            use(mask)
    load.wait()

    def normed(i):
        dn[:, seg(i, WIDE)] = mm(dqkv[...], w_scr[i], NN)
    loop(N_CHIP, normed)
    norm_back(dn, x_ref, g_scr, dh_ref, dx_ref, dg1)
    gains[...] = jnp.concatenate([jnp.sum(dg1[...], axis=0, keepdims=True), jnp.sum(dg2_ref[...], axis=0, keepdims=True),
                                  jnp.zeros((N_CHIP - 2, dg1.shape[1]), F32)], axis=0)
    gs.start()
    gains_in[me] = gains[:, seg(me)]
    for mask in CHIP_MASKS:
        gk.wait_pair(mask)
    dwkv_ref[...] = mm(full_kv[...], ucol_ref[...], NN)
    gs.wait_recv()
    gain_ref[...] = sum(gains_in[o] for o in range(N_DEV))
    for swap in (gates, ups):
        swap.wait_recv((CORE,) + SETS[1] + SETS[2] + SETS[3])
        swap.wait_send((CORE,) + SETS[3])
    for copy in own:
        copy.wait()
    for c in (sh, gs):
        c.wait_send()
    for g in (gq, gk):
        g.finish()


def finish(dg_hbm, du_hbm, dkv_hbm, *refs):
    n = (len(refs) - 11) // 3
    srcs, (gate, up, dk, dv), dsts = refs[:n], refs[n:n + 4], refs[n + 4:2 * n + 4]
    (g_in, g_out, kv_in), holds, sems = refs[2 * n + 4:2 * n + 7], refs[2 * n + 7:3 * n + 7], refs[3 * n + 7:]
    t_in, t_out, p_in, p_out = sems
    step = LANE * 11
    cols = g_in.shape[1]
    hd = dk.shape[0] // (kv_in.shape[0] // LANE)
    starts = [(w, i) for i in range(cols // step) for w in range(2)]

    def fetch(w, i):
        rs = pl.ds(i * step, step)
        return pltpu.make_async_copy((dg_hbm, du_hbm)[w].at[rs, :], g_in.at[w, rs, :], t_in.at[w, i])

    def put(w, i):
        cs = pl.ds(i * step, step)
        return pltpu.make_async_copy(g_out.at[w, :, cs], (gate, up)[w].at[:, cs], t_out.at[w, i])
    moves = [(pltpu.make_async_copy(a, h, p_in.at[k]), pltpu.make_async_copy(h, b, p_out.at[k])) for k, (a, h, b) in enumerate(zip(srcs, holds, dsts))]
    kv = pltpu.make_async_copy(dkv_hbm, kv_in, p_in.at[n])
    for w, i in starts:
        fetch(w, i).start()
    kv.start()
    for load, _ in moves:
        load.start()
    for w, i in starts:
        fetch(w, i).wait()

        at = pl.ds(i * step, step)
        g_out[w, :, at] = g_in[w, at, :].T
        put(w, i).start()
    kv.wait()
    for k in range(dk.shape[0] // hd):
        for i, ref in enumerate((dk, dv)):
            ref[k * hd:(k + 1) * hd, :] = kv_in[(2 * k + i) * hd:(2 * k + i + 1) * hd, :]
    for load, store in moves:
        load.wait()
        store.start()
    for w, i in starts:
        put(w, i).wait()
    for _, store in moves:
        store.wait()


def rope_tables(positions, head_dim):
    half_dim = head_dim // 2
    inv_freq = 1.0 / (ROPE_BASE ** (jnp.arange(half_dim, dtype=F32) * (2.0 / head_dim)))
    angles = positions.astype(F32)[None, :] * inv_freq[:, None]
    return jnp.cos(angles), jnp.sin(angles)


def solution(mesh):
    assert mesh.shape['sp'] == N_DEV

    def layer_step(x_in, positions, d_out, norm1_gain, norm2_gain, w_q, w_k, w_v, w_o, w_gate, w_up, w_down):
        tokens, dim = x_in.shape
        seq = tokens * N_DEV
        n_q, hd = w_q.shape[1:]
        n_kv = w_k.shape[1]
        qw = n_q // N_DEV * hd
        rows = w_q.shape[0]
        feat = w_down.shape[0]
        cols = (n_q + 2 * n_kv) * hd
        lanes = qw // hd * QB
        vm = pltpu.VMEM
        full = vm((N_CHIP, WIDE, dim), BF16)
        gain_scr = vm((N_CHIP, dim), F32)
        tok_shapes = 2 * (((tokens, dim), BF16),)
        dw_shapes = 2 * (((feat * N_DEV, rows), F32),)

        cos_own, sin_own = rope_tables(positions, hd)
        row = lambda v: v.reshape(1, rows)
        by_head = lambda w: w.transpose(1, 2, 0).reshape(-1, rows)
        wo_own = w_o.reshape(qw, dim)

        args = (x_in, row(norm1_gain), row(norm2_gain), row(positions), by_head(w_q), by_head(w_k), by_head(w_v), cos_own, sin_own, w_gate, w_up, wo_own)
        qkv, u, small_all, wqkv, attn_t, stat, wgu, hidden, mlp_in = call(
            functools.partial(head, n_kv, hd), 0, len(args),
            (((qw + 2 * hd, seq), BF16), tok_shapes[0], ((N_DEV, N_CHIP, rows), F32), ((N_CHIP, cols, WIDE), BF16),
             ((qw, seq), BF16), ((seq // QB, 2, lanes), F32), ((2 * feat, dim), BF16), *tok_shapes),
            [full, vm((tokens, dim), F32), vm((tokens, dim), BF16), vm((seq, qw), BF16),
             vm((N_CHIP, rows), F32), vm((cols, rows), BF16), vm((N_CHIP, cols, WIDE), BF16), vm((cols, tokens), F32), vm((cols, tokens), BF16), gain_scr,
             vm((feat * N_DEV, rows), BF16), vm((feat * N_DEV, rows), BF16), vm((seq, lanes), F32), vm((seq, hd), BF16), dma(N_CHIP),
             *Gather.sems, *(6 * Swap.sems), *Gather.sems], 4 * qw * seq * seq, far_out=(3,))(*args)
        args = (mlp_in, d_out, wgu, w_down, u, hidden, small_all, wo_own, attn_t)
        u_col, m_full, dgu, d_down, y_out, d_hidden, d_attn, d_wo, d_g2, d_gate_t, d_up_t = call(
            mlp, 1, len(args),
            (((seq, rows), BF16), ((N_CHIP, WIDE, dim), BF16), ((2 * feat, seq), BF16), ((feat, dim), F32),
             *tok_shapes, ((qw, seq), BF16), ((qw, dim), F32), ((N_CHIP, dim), F32), *dw_shapes),
            [vm((2 * feat, dim), BF16), vm((feat, dim), BF16), vm((feat, seq), BF16), vm((2 * feat, seq), BF16), dma(2),
             full, full, dma(N_CHIP, 2), vm((2 * feat, WIDE), F32), gain_scr, vm((WIDE, 2 * feat), BF16), vm((WIDE, feat), BF16), pltpu.SemaphoreType.REGULAR,
             *Scatter.scratch(tokens, dim), *(3 * Gather.sems), *(3 * Swap.sems), *Scatter.sems], 12 * feat * seq * dim,
            far_in=(2, 3), far_out=(1, 2, 9, 10))(*args)
        cos_all, sin_all = rope_tables(small_all[:, 2].reshape(-1), hd)
        args = (qkv, d_attn, stat, cos_all, sin_all, dgu, m_full, u_col, cos_own, sin_own, wqkv, x_in, small_all, d_hidden, d_g2, d_gate_t, d_up_t)
        d_gate_t, d_up_t, d_wq, d_wkv, d_x, gains = call(
            functools.partial(back, n_kv, hd), 3, len(args),
            (*dw_shapes, ((n_q * hd, rows), F32), ((2 * n_kv * hd, rows), F32), tok_shapes[0], ((N_CHIP, rows), F32)),
            [vm((seq, lanes), F32), vm((seq, lanes), BF16), vm((seq, hd), BF16), vm((seq, hd), BF16), vm((seq, hd), F32), vm((seq, hd), F32),
             vm((N_CHIP, 2 * feat, WIDE), F32), vm((qw, seq), BF16), vm((seq, 2 * hd), BF16), full,
             full, vm((N_CHIP, cols, WIDE), BF16), vm((N_DEV, tokens, 2 * hd), BF16), vm((2 * n_kv * hd, tokens), BF16), vm((2 * n_kv * hd, seq), BF16),
             vm((tokens, cols), BF16), vm((tokens, dim), F32), gain_scr, gain_scr, gain_scr, vm((N_DEV, N_CHIP, rows), F32), dma(), dma(2), dma(N_CHIP),
             *(3 * Swap.sems), *(2 * Gather.sems), *Swap.sems], 10 * qw * seq * seq, far_in=(6, 10, 15, 16), far_out=(0, 1), aliases={15: 0, 16: 1})(*args)
        moved = (d_wq, d_wo, d_down, d_x, y_out, gains)
        half_kv = jax.ShapeDtypeStruct((n_kv * hd, rows), F32)
        wide = jax.ShapeDtypeStruct((rows, feat * N_DEV), F32)
        d_gate, d_up, d_wk, d_wv, d_wq, d_wo, d_down, d_x, y_out, gains = pl.pallas_call(
            finish,
            out_shape=[wide, wide, half_kv, half_kv] + [jax.ShapeDtypeStruct(v.shape, v.dtype) for v in moved],
            in_specs=[IN_HBM] * (3 + len(moved)), out_specs=[IN_HBM] * 2 + on_chip(2) + [IN_HBM] * len(moved),
            scratch_shapes=[vm((2, feat * N_DEV, rows), F32), vm((2, rows, feat * N_DEV), F32), vm(d_wkv.shape, F32)]
            + [vm(v.shape, v.dtype) for v in moved] + [dma(2, 4), dma(2, 4), dma(len(moved) + 1), dma(len(moved))],
            compiler_params=pltpu.CompilerParams(vmem_limit_bytes=VMEM_CAP), name='finish',
        )(d_gate_t, d_up_t, d_wkv, *moved)
        by_row = lambda g, heads: g.reshape(heads, hd, rows).transpose(2, 0, 1)
        return (y_out, d_x, gains[0], gains[1], by_row(d_wq, n_q), by_row(d_wk, n_kv), by_row(d_wv, n_kv),
                d_wo.reshape(w_o.shape), d_gate, d_up, d_down)

    all_rows = P('sp')
    return jax.shard_map(layer_step, mesh=mesh, in_specs=(all_rows,) * 12, out_specs=(all_rows,) * 11, check_vma=False)
```

```python
import functools
import jax
import jax.numpy as jnp
from jax import lax
from jax.experimental import pallas as pl
from jax.experimental.pallas import tpu as pltpu
from jax.sharding import PartitionSpec as P

ROPE_BASE = 10000.0
NORM_EPS = 1e-5
NEG_LARGE = -1e30
F32 = jnp.float32
BF16 = jnp.bfloat16
N_DEV, N_CHIP, LANE, WIDE, CHUNK, STRIP = 16, 8, 128, 256, 512, 16
NT = (((1,), (1,)), ((), ()))
TN = (((0,), (0,)), ((), ()))
NN = (((1,), (0,)), ((), ()))
MESH = pl.DeviceIdType.MESH
VMEM_CAP = 62 * 1024 * 1024

CORE, X, Y, Z = 1, 2, 4, 8
XYZ = X + Y + Z
ORDERS = ((X, Y, Z), (Y, Z, X), (Z, X, Y))
CHIP_MASKS = (0, X, Y, Z, X + Y, X + Z, Y + Z, XYZ)
NEAR = (CORE, X, Y, Z)
OTHERS = range(1, N_DEV)
SETS = tuple(tuple(m + c for m in masks for c in (0, CORE)) for masks in ((XYZ,), (X, Y + Z), (Y, X + Z), (Z, X + Y)))
N_COL = len(ORDERS)
COLOURS = range(N_COL)


def mm(a, b, dims):
    return lax.dot_general(a, b, dims, preferred_element_type=F32)


def seg(index, width=LANE):
    return pl.ds(pl.multiple_of(index * width, width), width)


def loop(count, body):
    lax.fori_loop(0, count, lambda i, c: (body(i), c)[1], 0)


def differing(index, mask):
    return sum(((index // bit + mask // bit) % 2) * bit for bit in NEAR)


def flipped(index, mask):
    out = index
    for bit in NEAR:
        if mask & bit:
            out = out + (1 - 2 * ((index // bit) % 2)) * bit
    return out


def thirds(total, unit):
    n = total // unit
    first = (n + 2) // 3
    second = (n - first + 1) // 2
    sizes = (first * unit, second * unit, (n - first - second) * unit)
    return ((0, sizes[0]), (sizes[0], sizes[1]), (sizes[0] + sizes[1], sizes[2]))


def pieces(rows, cols, unit):
    share = cols // LANE // N_COL * LANE
    strips = thirds(rows, unit)
    rest = cols - N_COL * share
    return [[(pl.ds(0, rows), pl.ds(c * share, share)), (pl.ds(*strips[c]), pl.ds(N_COL * share, rest))] for c in COLOURS]


def enter(me, masks):
    barrier = pltpu.get_barrier_semaphore()
    for mask in masks:
        pl.semaphore_signal(barrier, inc=1, device_id=(flipped(me, mask),), device_id_type=MESH)
    pl.semaphore_wait(barrier, len(masks))


def remote(src, dst, send, recv, peer):
    return pltpu.make_async_remote_copy(src_ref=src, dst_ref=dst, send_sem=send, recv_sem=recv, device_id=(peer,), device_id_type=MESH)


def dma(*shape):
    return pltpu.SemaphoreType.DMA(shape)


class Swap:
    sems = (dma(N_DEV), dma(N_DEV))

    def __init__(self, src, dst, sems, me):
        self.src, self.dst, (self.send, self.recv), self.me = src, dst, sems, me

    def copy(self, mask):
        peer = differing(self.me, mask)
        return remote(self.src(peer), self.dst(self.me), self.send.at[mask], self.recv.at[mask], peer)

    def arrival(self, mask):
        view = self.dst(differing(self.me, mask))
        return remote(view, view, self.send.at[mask], self.recv.at[mask], self.me)

    def each(self, masks, act):
        if masks is None:
            loop(N_DEV - 1, lambda i: act(i + 1))
        else:
            for mask in masks:
                act(mask)

    def start(self, masks=None):
        self.each(masks, lambda mask: self.copy(mask).start())

    def advance(self, n):
        if n:
            self.wait_send(SETS[n - 1])
        self.start(SETS[n])

    def wait_recv(self, masks=None):
        self.each(masks, lambda mask: self.arrival(mask).wait_recv())

    def wait_send(self, masks=None):
        self.each(masks, lambda mask: self.copy(mask).wait_send())


class Gather:
    ROUNDS = ((0,), (1,), (2,), (0, 1), (0, 2), (1, 2), (0, 1, 2))
    READY = ((0,), (), (), (X, Y), (Z,), (X + Y, X + Z), (Y + Z, XYZ))
    sems = (dma(N_COL, N_CHIP, 2), dma(N_COL, N_CHIP, 2), dma(N_CHIP), dma(N_CHIP))

    def __init__(self, own, block, cut, sems, me):
        self.own, self.block, self.cut, self.me = own, block, cut, me
        self.send, self.recv, self.pair_send, self.pair_recv = sems

    def source(self, mask):
        return self.block(flipped(self.me, mask)) if mask else self.own

    def unit(self, colour, mask, axis):
        ends = zip(self.cut(self.source(mask), colour), self.cut(self.block(flipped(self.me, mask)), colour))
        j = self.sends(colour).index((mask, axis))
        return [remote(src, dst, self.send.at[colour, j, i], self.recv.at[colour, (mask + axis) // 2, i],
                       flipped(self.me, axis)) for i, (src, dst) in enumerate(ends)]

    def sends(self, colour):
        return [(0, axis) for axis in ORDERS[colour]] + [step[1:] for step in self.onward(colour)]

    def start_unit(self, colour, mask, axis):
        for copy in self.unit(colour, mask, axis):
            copy.start()

    def pair(self, mask):
        return remote(self.source(mask), self.block(flipped(self.me, mask)), self.pair_send.at[mask // 2],
                      self.pair_recv.at[mask // 2], flipped(self.me, CORE))

    def wait_pair(self, mask):
        view = self.block(flipped(self.me, mask + CORE))
        remote(view, view, self.pair_send.at[mask // 2], self.pair_recv.at[mask // 2], self.me).wait_recv()

    def onward(self, colour):
        order = ORDERS[colour]
        for picks in self.ROUNDS:
            for axis in order[picks[-1] + 1:]:
                yield picks, sum(order[p] for p in picks), axis

    def start(self):
        for pos in COLOURS:
            for colour in COLOURS:
                self.start_unit(colour, 0, ORDERS[colour][pos])
        self.pair(0).start()

    def round(self, r):
        for colour in COLOURS:
            mask = sum(ORDERS[colour][p] for p in self.ROUNDS[r])
            for i, view in enumerate(self.cut(self.block(flipped(self.me, mask)), colour)):
                remote(view, view, self.send.at[colour, 0, i], self.recv.at[colour, mask // 2, i], self.me).wait_recv()
            for picks, at, axis in self.onward(colour):
                if picks == self.ROUNDS[r]:
                    self.start_unit(colour, at, axis)
        for mask in {2: (X, Y, Z), 5: (X + Y, X + Z, Y + Z), 6: (XYZ,)}.get(r, ()):
            self.pair(mask).start()

    def finish(self):
        for colour in COLOURS:
            for i, view in enumerate(self.cut(self.own, colour)):
                loop(len(self.sends(colour)), lambda j: remote(view, view, self.send.at[colour, j, i], self.recv.at[colour, j, i], self.me).wait_send())
        loop(N_CHIP, lambda j: remote(self.own, self.own, self.pair_send.at[j], self.pair_recv.at[j], self.me).wait_send())


def row_gather(own, full, sems, me, extra=None):
    rows, width = own.shape
    parts = pieces(rows, width, STRIP)
    if extra is not None:
        share = width // LANE // N_COL * LANE
        more = width - N_COL * share
        parts = [[(pl.ds(0, rows), pl.ds(c * share + more * (c > extra), share + more * (c == extra)))] for c in COLOURS]

    def block(o):
        return full.at[o // 2, seg(o % 2), :]

    return Gather(own, block, lambda view, c: [view.at[rs, cs] for rs, cs in parts[c]], sems, me)


def keep_own(own, full, me):
    def step(i):
        full[me // 2, pl.ds(pl.multiple_of((me % 2) * LANE + i * STRIP, STRIP), STRIP), :] = own[seg(i, STRIP), :]
    loop(LANE // STRIP, step)


class Scatter:
    ORDER = (XYZ, X + Y, Y + Z, X + Z, X, Y, Z, 0)
    sems = (dma(N_CHIP), dma(N_CHIP), dma(N_COL, N_CHIP, 2), dma(N_COL, N_CHIP, 2))

    @staticmethod
    def scratch(tokens, dim):
        return [pltpu.VMEM((n, tokens, dim), F32) for n in (N_CHIP, 2, N_CHIP, N_CHIP - 1)]

    def __init__(self, part, other, pair_in, link_in, sems, me):
        self.part, self.other, self.pair_in, self.link_in, self.me = part, other, pair_in, link_in, me
        self.pair_send, self.pair_recv, self.link_send, self.link_recv = sems
        self.tokens, self.dim = part.shape[1:]
        self.pieces = pieces(self.tokens, self.dim, STRIP // 2)
        self.ready, self.sent = set(), [0] * N_COL

    @staticmethod
    def first(colour, mask):
        return next((i for i, a in enumerate(ORDERS[colour]) if mask & a), 3)

    def slot(self, colour, mask, axis):
        slots = [(m, a) for m in self.ORDER for a in ORDERS[colour][:self.first(colour, m)]]
        return slots.index((mask, axis))

    def pair(self, i):
        return remote(self.other.at[i % 2], self.pair_in.at[i], self.pair_send.at[i], self.pair_recv.at[i], flipped(self.me, CORE))

    def link(self, colour, mask):
        axis = ORDERS[colour][self.first(colour, mask)]
        slot = self.slot(colour, mask - axis, axis)
        i = self.ORDER.index(mask)
        return [remote(self.part.at[i, rs, cs], self.link_in.at[slot, rs, cs], self.link_send.at[colour, i, k],
                       self.link_recv.at[colour, slot, k], flipped(self.me, axis)) for k, (rs, cs) in enumerate(self.pieces[colour])]

    def start_link(self, colour, mask):
        for copy in self.link(colour, mask):
            copy.start()

    def add(self, mask, ref, cs):
        i = self.ORDER.index(mask)

        def step(r):
            rs = seg(r, STRIP)
            self.part[i, rs, cs] += ref[rs, cs]
        loop(self.tokens // STRIP, step)

    def finish_pair(self, i):
        self.pair(i).wait_recv()
        self.add(self.ORDER[i], self.pair_in.at[i], pl.ds(0, self.dim))
        self.ready.add(self.ORDER[i])
        for colour in COLOURS:
            a, b, c = ORDERS[colour]
            todo = (XYZ, a + b, a + c, a)
            while self.sent[colour] < len(todo) and todo[self.sent[colour]] in self.ready:
                self.start_link(colour, todo[self.sent[colour]])
                self.sent[colour] += 1

    def take(self, colour, mask, axis):
        for copy in self.link(colour, mask + axis):
            copy.wait_recv()
        ref = self.link_in.at[self.slot(colour, mask, axis)]
        (_, wide), (rs, cs) = self.pieces[colour]
        self.add(mask, ref, wide)
        self.part[self.ORDER.index(mask), rs, cs] += ref[rs, cs]

    def run(self, product, between=lambda i: None):
        for i, mask in enumerate(self.ORDER):
            if i > 1:
                self.pair(i - 2).wait_send()
            product(i, flipped(self.me, mask) // 2)
            self.pair(i).start()
            if i:
                self.finish_pair(i - 1)
            between(i)
        self.finish_pair(N_CHIP - 1)
        for step in range(2):
            for colour in COLOURS:
                a, b, c = ORDERS[colour]
                mask = (b + c, b)[step]
                self.take(colour, mask, a)
                self.start_link(colour, mask)
        for colour in COLOURS:
            a, b, c = ORDERS[colour]
            self.take(colour, c, a)
            self.take(colour, c, b)
            self.start_link(colour, c)
        for colour in COLOURS:
            for axis in ORDERS[colour]:
                self.take(colour, 0, axis)
        return self.part.at[N_CHIP - 1]

    def finish(self):
        for i in (N_CHIP - 2, N_CHIP - 1):
            self.pair(i).wait_send()
        for colour in COLOURS:
            for k, (rs, cs) in enumerate(self.pieces[colour]):
                view = self.part.at[0, rs, cs]
                loop(N_CHIP - 1, lambda i: remote(view, view, self.link_send.at[colour, i, k], self.link_recv.at[colour, i, k], self.me).wait_send())


def block_product(s, a_ref, w_ref, a_t):
    core = s.me % 2

    def product(i, chip):
        a_t[...] = a_ref[:, seg(chip, WIDE)].T

        def step(n):
            cs = seg(n, CHUNK)
            s.other[i % 2, :, cs] = mm(a_t[seg(1 - core), :], w_ref[:, cs], NN)
            s.part[i, :, cs] = mm(a_t[seg(core), :], w_ref[:, cs], NN)
        loop(s.dim // CHUNK, step)
    return product


def on_chip(n):
    return [pl.BlockSpec(memory_space=pltpu.VMEM)] * n


IN_HBM = pl.BlockSpec(memory_space=pl.ANY)


def call(kernel, ident, args, outs, scratch, flops, far_in=(), far_out=(), aliases={}):
    specs = [IN_HBM if i in far_in else on_chip(1)[0] for i in range(args)]
    out_specs = [IN_HBM if i in far_out else on_chip(1)[0] for i in range(len(outs))]
    return pl.pallas_call(
        kernel,
        out_shape=[jax.ShapeDtypeStruct(shape, dtype) for shape, dtype in outs],
        in_specs=specs, out_specs=out_specs, scratch_shapes=scratch, input_output_aliases=aliases,
        cost_estimate=pl.CostEstimate(flops=flops, bytes_accessed=flops // CHUNK, transcendentals=0),
        compiler_params=pltpu.CompilerParams(collective_id=ident, has_side_effects=True, vmem_limit_bytes=VMEM_CAP),
        name=kernel.func.__name__ if isinstance(kernel, functools.partial) else kernel.__name__,
    )


def fetch_all(sem, *pairs):
    copies = [pltpu.make_async_copy(src, dst, sem.at[i]) for i, (src, dst) in enumerate(pairs)]
    for copy in copies:
        copy.start()
    return copies


def gain_row(dst, small_all, which):
    for o in range(N_DEV):
        dst[:1, o * LANE:(o + 1) * LANE] = small_all[o, which:which + 1, :]


def norm_rows(src, gain, dst):
    def step(i):
        rs = seg(i, STRIP)
        t = src[rs, :].astype(F32)
        dst[rs, :] = (t * lax.rsqrt(jnp.mean(t * t, axis=-1, keepdims=True) + NORM_EPS) * gain[:1, :]).astype(BF16)
    loop(src.shape[0] // STRIP, step)


def norm_back(dy, src, gain, skip, dst, dgain):
    def step(i):
        rs = seg(i, STRIP)
        d = dy[rs, :].astype(BF16).astype(F32)
        t = src[rs, :].astype(F32)
        inv = lax.rsqrt(jnp.mean(t * t, axis=-1, keepdims=True) + NORM_EPS)
        gd = gain[:1, :] * d
        pull = jnp.mean(gd * t, axis=-1, keepdims=True)
        dst[rs, :] = (skip[rs, :].astype(F32) + (inv * gd - t * (inv * inv * inv * pull))).astype(BF16)
        g = d * (t * inv)
        dgain[...] += g[:N_CHIP] + g[N_CHIP:]
    dgain[...] = jnp.zeros_like(dgain)
    loop(src.shape[0] // STRIP, step)


QB = 256
KB = 256


def key_rows(dst, src, lo, hd):
    def step(i):
        dst[seg(i, KB), :] = src[lo:lo + hd, seg(i, KB)].T
    loop(src.shape[1] // KB, step)


def score_block(k, q2, scale, diagonal):
    s = mm(k, q2, NN) * scale
    if diagonal:
        key = lax.broadcasted_iota(jnp.int32, s.shape, 0)
        qry = lax.broadcasted_iota(jnp.int32, s.shape, 1) % QB
        s = jnp.where(qry >= key, s, NEG_LARGE)
    return s


def side_by_side(ref, heads, hd, qs):
    return jnp.concatenate([ref[h * hd:(h + 1) * hd, qs] for h in range(heads)], axis=1)


def head(groups, hd, x_ref, g1_ref, g2_ref, pos_ref, wq_ref, wk_ref, wv_ref, freq_ref, wg_ref, wu_ref, wo_ref, qkv_ref, u_scr, small_all, w_out, o_ref, stat_ref, wgu_ref, h_ref, m_ref, cos_ref, sin_ref,
         full_w, acc_o, o_tok, o_send, small_ref, w_ref, full, acc, rot, g_scr, wg_t, wu_t, s_scr, k_scr, osem, *sems):
    me = lax.axis_index('sp')
    tokens, dim = x_ref.shape
    cols = w_ref.shape[0]
    small_ref[...] = jnp.concatenate([r[...].astype(F32) for r in (g1_ref, g2_ref, pos_ref)] + [jnp.zeros((N_CHIP - 3, LANE), F32)], axis=0)
    w_ref[:wq_ref.shape[0], :] = wq_ref[...]
    for k in range(groups):
        for i, ref in enumerate((wk_ref, wv_ref)):
            w_ref[pl.ds(wq_ref.shape[0] + (2 * k + i) * hd, hd), :] = ref[k * hd:(k + 1) * hd, :]
    qw = tokens
    q_all = N_DEV * qw
    gsems, ssems, qsems, ksems, gate_sems, up_sems, osems = sems[:4], *(sems[i:i + 2] for i in range(4, len(sems) - 4, 2))
    gw = row_gather(wo_ref, full_w, sems[-4:], me, 1)
    feat = wg_ref.shape[1] // N_DEV
    enter(me, OTHERS)
    smalls = Swap(lambda peer: small_ref, lambda o: small_all.at[o], ssems, me)
    smalls.start()
    parts = thirds(cols, STRIP)
    g = Gather(w_ref, lambda o: full.at[o // 2, :, seg(o % 2)], lambda view, c: [view.at[pl.ds(*parts[c]), :]], gsems, me)
    g.start()
    gates = Swap(lambda peer: wg_t.at[seg(peer, feat), :], lambda o: wgu_ref.at[:feat, seg(o)], gate_sems, me)
    ups = Swap(lambda peer: wu_t.at[seg(peer, feat), :], lambda o: wgu_ref.at[feat:, seg(o)], up_sems, me)

    def advance(n):
        gates.advance(n)
        ups.advance(n)

    def transpose(i):
        wg_t[seg(i, CHUNK), :] = wg_ref[:, seg(i, CHUNK)].T
        wu_t[seg(i, CHUNK), :] = wu_ref[:, seg(i, CHUNK)].T
    loop(wg_ref.shape[1] // CHUNK, transpose)
    advance(0)

    def own_block(i):
        full[me // 2, seg(i, WIDE), seg(me % 2)] = w_ref[seg(i, WIDE), :]
    loop(cols // WIDE, own_block)
    acc[...] = jnp.zeros_like(acc)
    small_all[me] = small_ref[...]
    smalls.wait_recv()
    gain_row(g_scr, small_all, 0)
    norm_rows(x_ref, g_scr, u_scr)

    def keep(mask):
        chip = flipped(me, mask) // 2
        return pltpu.make_async_copy(full.at[chip], w_out.at[chip], osem.at[mask // 2])

    def use(mask):
        g.wait_pair(mask)
        keep(mask).start()
        chip = flipped(me, mask) // 2
        u = u_scr[:, seg(chip, WIDE)]

        def step(i):
            rs = seg(i, cols // 2)
            acc[rs, :] += mm(full[chip, rs, :], u, NT)
        loop(2, step)

    def tables(o):
        angles = freq_ref[...] * small_all[o, 2:3, :]
        cos_ref[:, seg(o)] = jnp.cos(angles)
        sin_ref[:, seg(o)] = jnp.sin(angles)

    for r in range(len(g.ROUNDS)):
        g.round(r)
        if r in (2, 4):
            advance(r // 2)
        if r == 1:
            loop(N_DEV, tables)
        for mask in g.READY[r]:
            use(mask)

    half = hd // 2
    cos, sin = cos_ref[:, seg(me)], sin_ref[:, seg(me)]

    def turn(h):
        first = seg(2 * h, half)
        second = seg(2 * h + 1, half)
        p = acc[first, :].astype(BF16).astype(F32)
        q = acc[second, :].astype(BF16).astype(F32)
        rot[first, :] = (p * cos - q * sin).astype(BF16)
        rot[second, :] = (q * cos + p * sin).astype(BF16)
    loop(q_all // hd, turn)
    for k in range(groups):
        turn(q_all // hd + 2 * k)
        vs = seg(q_all // hd + 2 * k + 1, hd)
        rot[vs, :] = acc[vs, :].astype(BF16)
    per = N_DEV // groups
    q_rows = lambda peer: seg(peer, qw)
    kv_rows = lambda peer: seg(q_all // (2 * hd) + peer // per, 2 * hd)
    qs = Swap(lambda peer: rot.at[q_rows(peer), :], lambda o: qkv_ref.at[:qw, seg(o, tokens)], qsems, me)
    kvs = Swap(lambda peer: rot.at[kv_rows(peer), :], lambda o: qkv_ref.at[qw:, seg(o, tokens)], ksems, me)
    qs.start()
    kvs.start()
    gw.start()
    keep_own(wo_ref, full_w, me)
    gain_row(g_scr, small_all, 1)
    qkv_ref[:qw, seg(me, tokens)] = rot[q_rows(me), :]
    qkv_ref[qw:, seg(me, tokens)] = rot[kv_rows(me), :]
    wgu_ref[:feat, seg(me)] = wg_t[seg(me, feat), :]
    wgu_ref[feat:, seg(me)] = wu_t[seg(me, feat), :]
    gates.start((CORE,))
    ups.start((CORE,))
    for swap in (qs, kvs):
        swap.wait_recv()
    heads = qkv_ref.shape[0] // hd - 2
    seq = qkv_ref.shape[1]
    scale = hd ** -0.5
    lanes = heads * QB
    key_rows(k_scr, qkv_ref, qw, hd)

    outs = Swap(lambda peer: o_send.at[seg(peer), :], lambda o: o_tok.at[:, seg(o)], osems, me)

    def q_block(qb):
        for at, r in ((2, 0), (4, 1), (5, 2), (6, 3), (7, 4)):
            @pl.when(qb == at)
            def _():
                gw.round(r)
        qs = seg(qb, QB)
        q2 = side_by_side(qkv_ref, heads, hd, qs)

        def scores(kb, top, diagonal):
            s = score_block(k_scr[seg(kb, KB), :], q2, scale, diagonal)
            s_scr[seg(kb, KB), :] = s
            return jnp.maximum(top, jnp.max(s, axis=0, keepdims=True))

        top = lax.fori_loop(0, qb, lambda kb, t: scores(kb, t, False), jnp.full((1, lanes), NEG_LARGE, F32))
        top = scores(qb, top, True)

        def expo(kb, tot):
            e = jnp.exp(s_scr[seg(kb, KB), :] - top)
            s_scr[seg(kb, KB), :] = e
            return tot + jnp.sum(e, axis=0, keepdims=True)

        inv = 1.0 / lax.fori_loop(0, qb + 1, expo, jnp.zeros((1, lanes), F32))

        def weigh(kb, acc):
            p = (s_scr[seg(kb, KB), :] * inv).astype(BF16)
            return acc + mm(qkv_ref[qw + hd:, seg(kb, KB)], p, NN)

        acc = lax.fori_loop(0, qb + 1, weigh, jnp.zeros((hd, lanes), F32))
        for h in range(heads):
            o_ref[h * hd:(h + 1) * hd, qs] = acc[:, h * QB:(h + 1) * QB].astype(BF16)
        stat_ref[qb, :1, :] = top
        stat_ref[qb, 1:, :] = inv
        o_send[qs, :] = o_ref[:, qs].T

    loop(seq // QB, q_block)
    outs.start()
    advance(3)
    o_tok[:, seg(me)] = o_send[seg(me), :]
    for r in (5, 6):
        gw.round(r)
    outs.wait_recv()
    for mask in CHIP_MASKS:
        gw.wait_pair(mask)

    def project(n):
        cs = seg(n, CHUNK)
        acc_o[:, cs] = mm(o_tok[...], full_w[:, :, cs].reshape(dim, CHUNK), NN)
    loop(dim // CHUNK, project)

    def residual(i):
        rs = seg(i, STRIP)
        h_ref[rs, :] = (x_ref[rs, :].astype(F32) + acc_o[rs, :]).astype(BF16)
    loop(tokens // STRIP, residual)
    norm_rows(h_ref, g_scr, m_ref)
    for swap in (gates, ups):
        swap.wait_recv()
    for mask in CHIP_MASKS:
        keep(mask).wait()
    outs.wait_send()
    for swap in (gates, ups):
        swap.wait_send((CORE,) + SETS[3])
    g.finish()
    gw.finish()
    for swap in (smalls, qs, kvs):
        swap.wait_send()


def dw_swaps(stage, gate_hbm, up_hbm, sems, me):
    feat = gate_hbm.shape[0] // N_DEV
    return [Swap(lambda peer, lo=lo: stage(peer).at[lo:lo + feat, seg(peer % 2)], lambda o, dst=dst: dst.at[seg(o, feat), :], sems[i:i + 2], me)
            for lo, dst, i in ((0, gate_hbm, 0), (feat, up_hbm, 2))]


def mlp(m_ref, dout_ref, wgu_hbm, down_hbm, u_ref, h_ref, small_all, wo_ref, o_ref,
        ucol_ref, m_out, dgu_out, ddown_out, y_ref, dh_ref, do_ref, dwo_ref, dg_ref, gate_hbm, up_hbm,
        wgu_ref, down_ref, glu_ref, dgu_ref, ddown_ref, isem, dsem, full_d, full_m, osem, stage, g_scr, dgu_t, glu_t, free, *scr):
    me = lax.axis_index('sp')
    feat, dim = down_ref.shape
    loads = fetch_all(isem, (wgu_hbm, wgu_ref), (down_hbm, down_ref))
    enter(me, OTHERS)
    sems = scr[4:]
    gd = row_gather(dout_ref, full_d, sems[:4], me, 0)
    gm = row_gather(m_ref, full_m, sems[4:8], me, 2)
    g = row_gather(dh_ref, full_d, sems[8:12], me, 1)
    ucols = Swap(lambda peer: u_ref.at[:, seg(peer)], lambda o: ucol_ref.at[seg(o), :], sems[12:14], me)
    gates, ups = dw_swaps(lambda peer: stage, gate_hbm, up_hbm, sems[14:18], me)
    gm.start()
    gd.start()
    ucol_ref[seg(me), :] = u_ref[:, seg(me)]
    keep_own(m_ref, full_m, me)
    keep_own(dout_ref, full_d, me)
    gain_row(g_scr, small_all, 1)
    dwo_ref[...] = jnp.zeros_like(dwo_ref)
    ddown_ref[...] = jnp.zeros_like(ddown_ref)

    def keep(mask):
        chip = flipped(me, mask) // 2
        ts = seg(chip, WIDE)
        ends = ((full_m.at[chip], m_out.at[chip]), (dgu_ref.at[:, ts], dgu_out.at[:, ts]))
        return [pltpu.make_async_copy(src, dst, osem.at[mask // 2, i]) for i, (src, dst) in enumerate(ends)]

    for load in loads:
        load.wait()

    def use(mask):
        gd.wait_pair(mask)
        gm.wait_pair(mask)
        chip = flipped(me, mask) // 2
        ts = seg(chip, WIDE)
        gu = mm(wgu_ref[...], full_m[chip], NT).astype(BF16).astype(F32)
        gate, up = gu[:feat], gu[feat:]
        d_glu = mm(down_ref[...], full_d[chip], NT).astype(BF16).astype(F32)
        sig = jax.nn.sigmoid(gate)
        act = gate * sig
        glu = (act * up).astype(BF16)
        glu_ref[:, ts] = glu
        dgu_ref[:feat, ts] = (d_glu * up * (sig * (1.0 + gate * (1.0 - sig)))).astype(BF16)
        dgu_ref[feat:, ts] = (d_glu * act).astype(BF16)

        def step(n):
            ddown_ref[:, seg(n, CHUNK)] += mm(glu, full_d[chip, :, seg(n, CHUNK)], NN)
        loop(dim // CHUNK, step)
        for copy in keep(mask):
            copy.start()

    for r in range(len(gm.ROUNDS)):
        gm.round(r)
        gd.round(r)
        if r == 3:
            ucols.start()
        for mask in gm.READY[r]:
            use(mask)
    far = seg(flipped(me, XYZ) // 2, WIDE)
    stage[...] = mm(dgu_ref[...], full_m[:, :, far].reshape(dgu_ref.shape[1], WIDE), NN)
    for swap in (gates, ups):
        swap.start(SETS[0])
    for gather in (gd, gm):
        gather.finish()
    leave = pltpu.make_async_copy(ddown_ref, ddown_out, dsem)
    leave.start()
    s = Scatter(*scr[:4], sems[18:], me)
    total = s.run(block_product(s, dgu_ref, wgu_ref, dgu_t))
    for mask in NEAR:
        pl.semaphore_signal(free, inc=1, device_id=(flipped(me, mask),), device_id_type=MESH)
    norm_back(total, h_ref, g_scr, dout_ref, dh_ref, dg_ref)
    g.start()
    keep_own(dh_ref, full_d, me)
    s.finish()
    pl.semaphore_wait(free, len(NEAR))

    def use_dh(mask):
        g.wait_pair(mask)
        chip = flipped(me, mask) // 2
        do_ref[:, seg(chip, WIDE)] = mm(wo_ref[...], full_d[chip], NT).astype(BF16)
        o = o_ref[:, seg(chip, WIDE)]

        def step(n):
            dwo_ref[:, seg(n, CHUNK)] += mm(o, full_d[chip, :, seg(n, CHUNK)], NN)
        loop(dim // CHUNK, step)

    def between(i):
        if i < len(g.ROUNDS):
            g.round(i)
            for mask in g.READY[i]:
                use_dh(mask)

    s = Scatter(*scr[:4], sems[18:], me)
    total = s.run(block_product(s, glu_ref, down_ref, glu_t), between)
    y_ref[...] = (h_ref[...].astype(F32) + total[...]).astype(BF16)
    s.finish()
    g.finish()
    for swap in (gates, ups):
        swap.wait_recv(SETS[0])
        swap.wait_send(SETS[0])
    ucols.wait_recv()
    ucols.wait_send()
    leave.wait()
    for mask in CHIP_MASKS:
        for copy in keep(mask):
            copy.wait()


def back(groups, hd, qkv_ref, do_ref, stat_ref, cos_all, sin_all, dgu_ref, m_hbm, ucol_ref, w_hbm, x_ref, small_all, dh_ref, dg2_ref, dg_in, du_in,
         dg_hbm, du_hbm, dwq_ref, dwkv_ref, dx_ref, gain_ref,
         p_scr, dp_scr, k_scr, v_scr, dk_acc, dv_acc, stage, dq_scr, dkv_scr, m_scr,
         full, w_scr, shares, dkv_own, full_kv, dqkv, dn, g_scr, dg1, gains, gains_in, wsem, lsem, msem, *sems):
    heads = qkv_ref.shape[0] // hd - 2
    seq = qkv_ref.shape[1]
    scale = hd ** -0.5
    lanes = heads * QB
    qw = heads * hd
    half = hd // 2
    me = lax.axis_index('sp')
    feat = dgu_ref.shape[0] // 2
    first = (X, Y + Z, Y, X + Z, Z, X + Y, 0)

    def fetch(mask):
        cols = seg(flipped(me, mask) // 2, WIDE)
        return pltpu.make_async_copy(m_hbm.at[:, :, cols], m_scr.at[:, :, cols], msem.at[mask // 2])
    for mask in first:
        fetch(mask).start()
    load = pltpu.make_async_copy(w_hbm, w_scr, wsem)
    load.start()
    enter(me, OTHERS)
    gain_row(g_scr, small_all, 0)

    gates, ups = dw_swaps(lambda peer: stage.at[peer // 2], dg_hbm, du_hbm, sems[:4], me)
    gq = row_gather(dq_scr, full, sems[6:10], me)
    own = [pltpu.make_async_copy(swap.src(me), swap.dst(me), lsem.at[i]) for i, swap in enumerate((gates, ups))]

    def make(mask):
        chip = flipped(me, mask) // 2
        fetch(mask).wait()
        cols = m_scr[:, :, seg(chip, WIDE)].reshape(seq, WIDE)
        stage[chip] = mm(dgu_ref[...], cols, NN)

    def advance(n):
        for swap in (gates, ups):
            if n > 1:
                swap.wait_send(SETS[n - 1])
            swap.start(SETS[n])

    for mask in first[:2]:
        make(mask)
        for swap in (gates, ups):
            swap.start((mask, mask + CORE))
    for mask in first[2:4]:
        make(mask)

    dk_acc[...] = jnp.zeros_like(dk_acc)
    dv_acc[...] = jnp.zeros_like(dv_acc)
    key_rows(k_scr, qkv_ref, qw, hd)
    key_rows(v_scr, qkv_ref, qw + hd, hd)

    def q_block(qb):
        @pl.when(qb == 4)
        def _():
            advance(2)
        qs = seg(qb, QB)
        q2 = side_by_side(qkv_ref, heads, hd, qs)
        do2 = side_by_side(do_ref, heads, hd, qs)
        top = stat_ref[qb, :1, :]
        inv = stat_ref[qb, 1:, :]

        def probs(kb, rd, diagonal):
            ks = seg(kb, KB)
            s = score_block(k_scr[ks, :], q2, scale, diagonal)
            p = jnp.exp(s - top) * inv
            dp = mm(v_scr[ks, :], do2, NN).astype(BF16)
            p_scr[ks, :] = p
            dp_scr[ks, :] = dp
            dv_acc[ks, :] += mm(p.astype(BF16), do2, NT)
            return rd + jnp.sum(dp.astype(F32) * p, axis=0, keepdims=True)

        rd = lax.fori_loop(0, qb, lambda kb, r: probs(kb, r, False), jnp.zeros((1, lanes), F32))
        rd = probs(qb, rd, True)

        def d_scores(kb, acc):
            ks = seg(kb, KB)
            ds = (p_scr[ks, :] * (dp_scr[ks, :].astype(F32) - rd) * scale).astype(BF16)
            dk_acc[ks, :] += mm(ds, q2, NT)
            return acc + mm(qkv_ref[qw:qw + hd, ks], ds, NN)

        acc = lax.fori_loop(0, qb + 1, d_scores, jnp.zeros((hd, lanes), F32))
        cos, sin = cos_all[:, qs], sin_all[:, qs]
        for h in range(heads):
            dq = acc[:, h * QB:(h + 1) * QB].astype(BF16).astype(F32)
            p, q = dq[:half], dq[half:]
            dq_scr[h * hd:h * hd + half, qs] = (p * cos + q * sin).astype(BF16)
            dq_scr[h * hd + half:(h + 1) * hd, qs] = (q * cos - p * sin).astype(BF16)

    loop(seq // QB, q_block)

    def share(i):
        rs = seg(i, WIDE)
        dkv_scr[rs, :] = jnp.concatenate([dk_acc[rs, :], dv_acc[rs, :]], axis=1).astype(BF16)
    loop(seq // WIDE, share)
    tokens = ucol_ref.shape[1]
    per = N_DEV // groups
    q_all = dwq_ref.shape[0]
    sh = Swap(lambda peer: dkv_scr.at[seg(peer, tokens), :], lambda o: shares.at[o], sems[4:6], me)
    parts = thirds(dkv_own.shape[0], STRIP)
    gk = Gather(dkv_own, lambda o: full_kv.at[:, seg(o, tokens)], lambda view, c: [view.at[pl.ds(*parts[c]), :]], sems[10:14], me)
    gs = Swap(lambda peer: gains.at[:, seg(peer)], lambda o: gains_in.at[o], sems[14:], me)
    sh.start()
    gq.start()
    for mask in first[4:]:
        make(mask)
    for swap in (gates, ups):
        swap.start((CORE,))
    for copy in own:
        copy.start()
    keep_own(dq_scr, full, me)
    shares[me] = dkv_scr[seg(me, tokens), :]
    sh.wait_recv()
    cos, sin = cos_all[:, seg(me)], sin_all[:, seg(me)]
    for k in range(groups):
        both = sum(shares[per * k + i].astype(F32) for i in range(per)).astype(BF16).astype(F32).T
        p, q = both[:half], both[half:hd]
        lo = 2 * hd * k
        dkv_own[lo:lo + half, :] = (p * cos + q * sin).astype(BF16)
        dkv_own[lo + half:lo + hd, :] = (q * cos - p * sin).astype(BF16)
        dkv_own[lo + hd:lo + 2 * hd, :] = both[hd:].astype(BF16)
    gk.start()
    full_kv[:, seg(me, tokens)] = dkv_own[...]
    for k in range(groups):
        dqkv[:, q_all + 2 * hd * k:q_all + 2 * hd * (k + 1)] = dkv_own[2 * hd * k:2 * hd * (k + 1), :].T

    def use(mask):
        gq.wait_pair(mask)
        chip = flipped(me, mask) // 2
        dwq_ref[seg(chip, WIDE), :] = mm(full[chip], ucol_ref[...], NN)
        dqkv[:, seg(chip, WIDE)] = full[chip, :, seg(me, tokens)].T

    for r in range(len(gq.ROUNDS)):
        gq.round(r)
        gk.round(r)
        if r == 3:
            advance(3)
        for mask in gq.READY[r]:
            use(mask)
    load.wait()

    def normed(i):
        dn[:, seg(i, WIDE)] = mm(dqkv[...], w_scr[i], NN)
    loop(N_CHIP, normed)
    norm_back(dn, x_ref, g_scr, dh_ref, dx_ref, dg1)
    gains[...] = jnp.concatenate([jnp.sum(dg1[...], axis=0, keepdims=True), jnp.sum(dg2_ref[...], axis=0, keepdims=True),
                                  jnp.zeros((N_CHIP - 2, dg1.shape[1]), F32)], axis=0)
    gs.start()
    gains_in[me] = gains[:, seg(me)]
    for mask in CHIP_MASKS:
        gk.wait_pair(mask)
    dwkv_ref[...] = mm(full_kv[...], ucol_ref[...], NN)
    gs.wait_recv()
    gain_ref[...] = sum(gains_in[o] for o in range(N_DEV))
    for swap in (gates, ups):
        swap.wait_recv((CORE,) + SETS[1] + SETS[2] + SETS[3])
        swap.wait_send((CORE,) + SETS[3])
    for copy in own:
        copy.wait()
    for c in (sh, gs):
        c.wait_send()
    for g in (gq, gk):
        g.finish()


def finish(dg_hbm, du_hbm, dkv_hbm, *refs):
    n = (len(refs) - 11) // 3
    srcs, (gate, up, dk, dv), dsts = refs[:n], refs[n:n + 4], refs[n + 4:2 * n + 4]
    (g_in, g_out, kv_in), holds, sems = refs[2 * n + 4:2 * n + 7], refs[2 * n + 7:3 * n + 7], refs[3 * n + 7:]
    t_in, t_out, p_in, p_out = sems
    step = LANE * 11
    cols = g_in.shape[1]
    hd = dk.shape[0] // (kv_in.shape[0] // LANE)
    starts = [(w, i) for i in range(cols // step) for w in range(2)]

    def fetch(w, i):
        rs = pl.ds(i * step, step)
        return pltpu.make_async_copy((dg_hbm, du_hbm)[w].at[rs, :], g_in.at[w, rs, :], t_in.at[w, i])

    def put(w, i):
        cs = pl.ds(i * step, step)
        return pltpu.make_async_copy(g_out.at[w, :, cs], (gate, up)[w].at[:, cs], t_out.at[w, i])
    moves = [(pltpu.make_async_copy(a, h, p_in.at[k]), pltpu.make_async_copy(h, b, p_out.at[k])) for k, (a, h, b) in enumerate(zip(srcs, holds, dsts))]
    kv = pltpu.make_async_copy(dkv_hbm, kv_in, p_in.at[n])
    for w, i in starts:
        fetch(w, i).start()
    kv.start()
    for k, (w, i) in enumerate(starts):
        fetch(w, i).wait()
        if k < len(moves):
            moves[k][0].start()

        at = pl.ds(i * step, step)
        g_out[w, :, at] = g_in[w, at, :].T
        put(w, i).start()
    kv.wait()
    for k in range(dk.shape[0] // hd):
        for i, ref in enumerate((dk, dv)):
            ref[k * hd:(k + 1) * hd, :] = kv_in[(2 * k + i) * hd:(2 * k + i + 1) * hd, :]
    for load, store in moves:
        load.wait()
        store.start()
    for w, i in starts:
        put(w, i).wait()
    for _, store in moves:
        store.wait()


def solution(mesh):
    assert mesh.shape['sp'] == N_DEV

    def layer_step(x_in, positions, d_out, norm1_gain, norm2_gain, w_q, w_k, w_v, w_o, w_gate, w_up, w_down):
        tokens, dim = x_in.shape
        seq = tokens * N_DEV
        n_q, hd = w_q.shape[1:]
        n_kv = w_k.shape[1]
        qw = n_q // N_DEV * hd
        rows = w_q.shape[0]
        feat = w_down.shape[0]
        cols = (n_q + 2 * n_kv) * hd
        lanes = qw // hd * QB
        vm = pltpu.VMEM
        full = vm((N_CHIP, WIDE, dim), BF16)
        gain_scr = vm((N_CHIP, dim), F32)
        tok_shapes = 2 * (((tokens, dim), BF16),)
        dw_shapes = 2 * (((feat * N_DEV, rows), F32),)

        inv_freq = 1.0 / (ROPE_BASE ** (jnp.arange(hd // 2, dtype=F32) * (2.0 / hd)))
        freq = jnp.broadcast_to(inv_freq[:, None], (hd // 2, rows))
        row = lambda v: v.reshape(1, rows)
        by_head = lambda w: w.transpose(1, 2, 0).reshape(-1, rows)
        wo_own = w_o.reshape(qw, dim)

        args = (x_in, row(norm1_gain), row(norm2_gain), row(positions), by_head(w_q), by_head(w_k), by_head(w_v), freq, w_gate, w_up, wo_own)
        qkv, u, small_all, wqkv, attn_t, stat, wgu, hidden, mlp_in, cos_all, sin_all = call(
            functools.partial(head, n_kv, hd), 0, len(args),
            (((qw + 2 * hd, seq), BF16), tok_shapes[0], ((N_DEV, N_CHIP, rows), F32), ((N_CHIP, cols, WIDE), BF16),
             ((qw, seq), BF16), ((seq // QB, 2, lanes), F32), ((2 * feat, dim), BF16), *tok_shapes, *(2 * (((hd // 2, seq), F32),))),
            [full, vm((tokens, dim), F32), vm((tokens, dim), BF16), vm((seq, qw), BF16),
             vm((N_CHIP, rows), F32), vm((cols, rows), BF16), vm((N_CHIP, cols, WIDE), BF16), vm((cols, tokens), F32), vm((cols, tokens), BF16), gain_scr,
             vm((feat * N_DEV, rows), BF16), vm((feat * N_DEV, rows), BF16), vm((seq, lanes), F32), vm((seq, hd), BF16), dma(N_CHIP),
             *Gather.sems, *(6 * Swap.sems), *Gather.sems], 4 * qw * seq * seq, far_out=(3,))(*args)
        args = (mlp_in, d_out, wgu, w_down, u, hidden, small_all, wo_own, attn_t)
        u_col, m_full, dgu, d_down, y_out, d_hidden, d_attn, d_wo, d_g2, d_gate_t, d_up_t = call(
            mlp, 1, len(args),
            (((seq, rows), BF16), ((N_CHIP, WIDE, dim), BF16), ((2 * feat, seq), BF16), ((feat, dim), F32),
             *tok_shapes, ((qw, seq), BF16), ((qw, dim), F32), ((N_CHIP, dim), F32), *dw_shapes),
            [vm((2 * feat, dim), BF16), vm((feat, dim), BF16), vm((feat, seq), BF16), vm((2 * feat, seq), BF16), vm((feat, dim), F32), dma(2), dma(),
             full, full, dma(N_CHIP, 2), vm((2 * feat, WIDE), F32), gain_scr, vm((WIDE, 2 * feat), BF16), vm((WIDE, feat), BF16), pltpu.SemaphoreType.REGULAR,
             *Scatter.scratch(tokens, dim), *(3 * Gather.sems), *(3 * Swap.sems), *Scatter.sems], 12 * feat * seq * dim,
            far_in=(2, 3), far_out=(1, 2, 3, 9, 10))(*args)
        args = (qkv, d_attn, stat, cos_all, sin_all, dgu, m_full, u_col, wqkv, x_in, small_all, d_hidden, d_g2, d_gate_t, d_up_t)
        d_gate_t, d_up_t, d_wq, d_wkv, d_x, gains = call(
            functools.partial(back, n_kv, hd), 3, len(args),
            (*dw_shapes, ((n_q * hd, rows), F32), ((2 * n_kv * hd, rows), F32), tok_shapes[0], ((N_CHIP, rows), F32)),
            [vm((seq, lanes), F32), vm((seq, lanes), BF16), vm((seq, hd), BF16), vm((seq, hd), BF16), vm((seq, hd), F32), vm((seq, hd), F32),
             vm((N_CHIP, 2 * feat, WIDE), F32), vm((qw, seq), BF16), vm((seq, 2 * hd), BF16), full,
             full, vm((N_CHIP, cols, WIDE), BF16), vm((N_DEV, tokens, 2 * hd), BF16), vm((2 * n_kv * hd, tokens), BF16), vm((2 * n_kv * hd, seq), BF16),
             vm((tokens, cols), BF16), vm((tokens, dim), F32), gain_scr, gain_scr, gain_scr, vm((N_DEV, N_CHIP, rows), F32), dma(), dma(2), dma(N_CHIP),
             *(3 * Swap.sems), *(2 * Gather.sems), *Swap.sems], 10 * qw * seq * seq, far_in=(6, 8, 13, 14), far_out=(0, 1), aliases={13: 0, 14: 1})(*args)
        moved = (d_wq, d_wo, d_down, d_x, y_out, gains)
        half_kv = jax.ShapeDtypeStruct((n_kv * hd, rows), F32)
        wide = jax.ShapeDtypeStruct((rows, feat * N_DEV), F32)
        d_gate, d_up, d_wk, d_wv, d_wq, d_wo, d_down, d_x, y_out, gains = pl.pallas_call(
            finish,
            out_shape=[wide, wide, half_kv, half_kv] + [jax.ShapeDtypeStruct(v.shape, v.dtype) for v in moved],
            in_specs=[IN_HBM] * (3 + len(moved)), out_specs=[IN_HBM] * 2 + on_chip(2) + [IN_HBM] * len(moved),
            scratch_shapes=[vm((2, feat * N_DEV, rows), F32), vm((2, rows, feat * N_DEV), F32), vm(d_wkv.shape, F32)]
            + [vm(v.shape, v.dtype) for v in moved] + [dma(2, 4), dma(2, 4), dma(len(moved) + 1), dma(len(moved))],
            compiler_params=pltpu.CompilerParams(vmem_limit_bytes=VMEM_CAP), name='finish',
        )(d_gate_t, d_up_t, d_wkv, *moved)
        by_row = lambda g, heads: g.reshape(heads, hd, rows).transpose(2, 0, 1)
        return (y_out, d_x, gains[0], gains[1], by_row(d_wq, n_q), by_row(d_wk, n_kv), by_row(d_wv, n_kv),
                d_wo.reshape(w_o.shape), d_gate, d_up, d_down)

    all_rows = P('sp')
    return jax.shard_map(layer_step, mesh=mesh, in_specs=(all_rows,) * 12, out_specs=(all_rows,) * 11, check_vma=False)
```

```python
import functools
import jax
import jax.numpy as jnp
from jax import lax
from jax.experimental import pallas as pl
from jax.experimental.pallas import tpu as pltpu
from jax.sharding import PartitionSpec as P

ROPE_BASE = 10000.0
NORM_EPS = 1e-5
NEG_LARGE = -1e30
F32 = jnp.float32
BF16 = jnp.bfloat16
N_DEV, N_CHIP, LANE, WIDE, CHUNK, STRIP = 16, 8, 128, 256, 512, 16
NT = (((1,), (1,)), ((), ()))
TN = (((0,), (0,)), ((), ()))
NN = (((1,), (0,)), ((), ()))
MESH = pl.DeviceIdType.MESH
VMEM_CAP = 67043328

CORE, X, Y, Z = 1, 2, 4, 8
XYZ = X + Y + Z
ORDERS = ((X, Y, Z), (Y, Z, X), (Z, X, Y))
CHIP_MASKS = (0, X, Y, Z, X + Y, X + Z, Y + Z, XYZ)
NEAR = (CORE, X, Y, Z)
OTHERS = range(1, N_DEV)
SETS = tuple(tuple(m + c for m in masks for c in (0, CORE)) for masks in ((XYZ,), (X, Y + Z), (Y, X + Z), (Z, X + Y)))
N_COL = len(ORDERS)
COLOURS = range(N_COL)


def mm(a, b, dims):
    return lax.dot_general(a, b, dims, preferred_element_type=F32)


def seg(index, width=LANE):
    return pl.ds(pl.multiple_of(index * width, width), width)


def loop(count, body):
    lax.fori_loop(0, count, lambda i, c: (body(i), c)[1], 0)


def differing(index, mask):
    return sum(((index // bit + mask // bit) % 2) * bit for bit in NEAR)


def flipped(index, mask):
    out = index
    for bit in NEAR:
        if mask & bit:
            out = out + (1 - 2 * ((index // bit) % 2)) * bit
    return out


def thirds(total, unit):
    n = total // unit
    first = (n + 2) // 3
    second = (n - first + 1) // 2
    sizes = (first * unit, second * unit, (n - first - second) * unit)
    return ((0, sizes[0]), (sizes[0], sizes[1]), (sizes[0] + sizes[1], sizes[2]))


def pieces(rows, cols, unit):
    share = cols // LANE // N_COL * LANE
    strips = thirds(rows, unit)
    rest = cols - N_COL * share
    return [[(pl.ds(0, rows), pl.ds(c * share, share)), (pl.ds(*strips[c]), pl.ds(N_COL * share, rest))] for c in COLOURS]


def enter(me, masks):
    barrier = pltpu.get_barrier_semaphore()
    for mask in masks:
        pl.semaphore_signal(barrier, inc=1, device_id=(flipped(me, mask),), device_id_type=MESH)
    pl.semaphore_wait(barrier, len(masks))


def remote(src, dst, send, recv, peer):
    return pltpu.make_async_remote_copy(src_ref=src, dst_ref=dst, send_sem=send, recv_sem=recv, device_id=(peer,), device_id_type=MESH)


def dma(*shape):
    return pltpu.SemaphoreType.DMA(shape)


class Swap:
    sems = (dma(N_DEV), dma(N_DEV))

    def __init__(self, src, dst, sems, me):
        self.src, self.dst, (self.send, self.recv), self.me = src, dst, sems, me

    def copy(self, mask):
        peer = differing(self.me, mask)
        return remote(self.src(peer), self.dst(self.me), self.send.at[mask], self.recv.at[mask], peer)

    def arrival(self, mask):
        view = self.dst(differing(self.me, mask))
        return remote(view, view, self.send.at[mask], self.recv.at[mask], self.me)

    def each(self, masks, act):
        if masks is None:
            loop(N_DEV - 1, lambda i: act(i + 1))
        else:
            for mask in masks:
                act(mask)

    def start(self, masks=None):
        self.each(masks, lambda mask: self.copy(mask).start())

    def advance(self, n):
        if n:
            self.wait_send(SETS[n - 1])
        self.start(SETS[n])

    def wait_recv(self, masks=None):
        self.each(masks, lambda mask: self.arrival(mask).wait_recv())

    def wait_send(self, masks=None):
        self.each(masks, lambda mask: self.copy(mask).wait_send())


class Gather:
    ROUNDS = ((0,), (1,), (2,), (0, 1), (0, 2), (1, 2), (0, 1, 2))
    READY = ((0,), (), (), (X, Y), (Z,), (X + Y, X + Z), (Y + Z, XYZ))
    sems = (dma(N_COL, N_CHIP, 2), dma(N_COL, N_CHIP, 2), dma(N_CHIP), dma(N_CHIP))

    def __init__(self, own, block, cut, sems, me):
        self.own, self.block, self.cut, self.me = own, block, cut, me
        self.send, self.recv, self.pair_send, self.pair_recv = sems

    def source(self, mask):
        return self.block(flipped(self.me, mask)) if mask else self.own

    def unit(self, colour, mask, axis):
        ends = zip(self.cut(self.source(mask), colour), self.cut(self.block(flipped(self.me, mask)), colour))
        j = self.sends(colour).index((mask, axis))
        return [remote(src, dst, self.send.at[colour, j, i], self.recv.at[colour, (mask + axis) // 2, i],
                       flipped(self.me, axis)) for i, (src, dst) in enumerate(ends)]

    def sends(self, colour):
        return [(0, axis) for axis in ORDERS[colour]] + [step[1:] for step in self.onward(colour)]

    def start_unit(self, colour, mask, axis):
        for copy in self.unit(colour, mask, axis):
            copy.start()

    def pair(self, mask):
        return remote(self.source(mask), self.block(flipped(self.me, mask)), self.pair_send.at[mask // 2],
                      self.pair_recv.at[mask // 2], flipped(self.me, CORE))

    def wait_pair(self, mask):
        view = self.block(flipped(self.me, mask + CORE))
        remote(view, view, self.pair_send.at[mask // 2], self.pair_recv.at[mask // 2], self.me).wait_recv()

    def onward(self, colour):
        order = ORDERS[colour]
        for picks in self.ROUNDS:
            for axis in order[picks[-1] + 1:]:
                yield picks, sum(order[p] for p in picks), axis

    def start(self):
        for pos in COLOURS:
            for colour in COLOURS:
                self.start_unit(colour, 0, ORDERS[colour][pos])
        self.pair(0).start()

    def round(self, r):
        for colour in COLOURS:
            mask = sum(ORDERS[colour][p] for p in self.ROUNDS[r])
            for i, view in enumerate(self.cut(self.block(flipped(self.me, mask)), colour)):
                remote(view, view, self.send.at[colour, 0, i], self.recv.at[colour, mask // 2, i], self.me).wait_recv()
            for picks, at, axis in self.onward(colour):
                if picks == self.ROUNDS[r]:
                    self.start_unit(colour, at, axis)
        for mask in {2: (X, Y, Z), 5: (X + Y, X + Z, Y + Z), 6: (XYZ,)}.get(r, ()):
            self.pair(mask).start()

    def finish(self):
        for colour in COLOURS:
            for i, view in enumerate(self.cut(self.own, colour)):
                loop(len(self.sends(colour)), lambda j: remote(view, view, self.send.at[colour, j, i], self.recv.at[colour, j, i], self.me).wait_send())
        loop(N_CHIP, lambda j: remote(self.own, self.own, self.pair_send.at[j], self.pair_recv.at[j], self.me).wait_send())


def row_gather(own, full, sems, me, extra=None):
    rows, width = own.shape
    parts = pieces(rows, width, STRIP)
    if extra is not None:
        share = width // LANE // N_COL * LANE
        more = width - N_COL * share
        parts = [[(pl.ds(0, rows), pl.ds(c * share + more * (c > extra), share + more * (c == extra)))] for c in COLOURS]

    def block(o):
        return full.at[o // 2, seg(o % 2), :]

    return Gather(own, block, lambda view, c: [view.at[rs, cs] for rs, cs in parts[c]], sems, me)


def keep_own(own, full, me):
    def step(i):
        full[me // 2, pl.ds(pl.multiple_of((me % 2) * LANE + i * STRIP, STRIP), STRIP), :] = own[seg(i, STRIP), :]
    loop(LANE // STRIP, step)


class Scatter:
    ORDER = (XYZ, X + Y, Y + Z, X + Z, X, Y, Z, 0)
    sems = (dma(N_CHIP), dma(N_CHIP), dma(N_COL, N_CHIP, 2), dma(N_COL, N_CHIP, 2))

    @staticmethod
    def scratch(tokens, dim):
        return [pltpu.VMEM((n, tokens, dim), F32) for n in (N_CHIP, 2, N_CHIP, N_CHIP - 1)]

    def __init__(self, part, other, pair_in, link_in, sems, me):
        self.part, self.other, self.pair_in, self.link_in, self.me = part, other, pair_in, link_in, me
        self.pair_send, self.pair_recv, self.link_send, self.link_recv = sems
        self.tokens, self.dim = part.shape[1:]
        self.pieces = pieces(self.tokens, self.dim, STRIP // 2)
        self.ready, self.sent = set(), [0] * N_COL

    @staticmethod
    def first(colour, mask):
        return next((i for i, a in enumerate(ORDERS[colour]) if mask & a), 3)

    def slot(self, colour, mask, axis):
        slots = [(m, a) for m in self.ORDER for a in ORDERS[colour][:self.first(colour, m)]]
        return slots.index((mask, axis))

    def pair(self, i):
        return remote(self.other.at[i % 2], self.pair_in.at[i], self.pair_send.at[i], self.pair_recv.at[i], flipped(self.me, CORE))

    def link(self, colour, mask):
        axis = ORDERS[colour][self.first(colour, mask)]
        slot = self.slot(colour, mask - axis, axis)
        i = self.ORDER.index(mask)
        return [remote(self.part.at[i, rs, cs], self.link_in.at[slot, rs, cs], self.link_send.at[colour, i, k],
                       self.link_recv.at[colour, slot, k], flipped(self.me, axis)) for k, (rs, cs) in enumerate(self.pieces[colour])]

    def start_link(self, colour, mask):
        for copy in self.link(colour, mask):
            copy.start()

    def add(self, mask, ref, cs):
        i = self.ORDER.index(mask)

        def step(r):
            rs = seg(r, STRIP)
            self.part[i, rs, cs] += ref[rs, cs]
        loop(self.tokens // STRIP, step)

    def finish_pair(self, i):
        self.pair(i).wait_recv()
        self.add(self.ORDER[i], self.pair_in.at[i], pl.ds(0, self.dim))
        self.ready.add(self.ORDER[i])
        for colour in COLOURS:
            a, b, c = ORDERS[colour]
            todo = (XYZ, a + b, a + c, a)
            while self.sent[colour] < len(todo) and todo[self.sent[colour]] in self.ready:
                self.start_link(colour, todo[self.sent[colour]])
                self.sent[colour] += 1

    def take(self, colour, mask, axis):
        for copy in self.link(colour, mask + axis):
            copy.wait_recv()
        ref = self.link_in.at[self.slot(colour, mask, axis)]
        (_, wide), (rs, cs) = self.pieces[colour]
        self.add(mask, ref, wide)
        self.part[self.ORDER.index(mask), rs, cs] += ref[rs, cs]

    def run(self, product, between=lambda i: None, before_last=lambda: None):
        for i, mask in enumerate(self.ORDER):
            if i > 1:
                self.pair(i - 2).wait_send()
            product(i, flipped(self.me, mask) // 2)
            self.pair(i).start()
            if i:
                self.finish_pair(i - 1)
            between(i)
        self.finish_pair(N_CHIP - 1)
        for step in range(2):
            for colour in COLOURS:
                a, b, c = ORDERS[colour]
                mask = (b + c, b)[step]
                self.take(colour, mask, a)
                self.start_link(colour, mask)
        before_last()
        for colour in COLOURS:
            a, b, c = ORDERS[colour]
            self.take(colour, c, a)
            self.take(colour, c, b)
            self.start_link(colour, c)
        for colour in COLOURS:
            for axis in ORDERS[colour]:
                self.take(colour, 0, axis)
        return self.part.at[N_CHIP - 1]

    def finish(self):
        for i in (N_CHIP - 2, N_CHIP - 1):
            self.pair(i).wait_send()
        for colour in COLOURS:
            for k, (rs, cs) in enumerate(self.pieces[colour]):
                view = self.part.at[0, rs, cs]
                loop(N_CHIP - 1, lambda i: remote(view, view, self.link_send.at[colour, i, k], self.link_recv.at[colour, i, k], self.me).wait_send())


def block_product(s, a_ref, w_ref, a_t):
    core = s.me % 2

    def product(i, chip):
        a_t[...] = a_ref[:, seg(chip, WIDE)].T

        def step(n):
            cs = seg(n, CHUNK)
            s.other[i % 2, :, cs] = mm(a_t[seg(1 - core), :], w_ref[:, cs], NN)
            s.part[i, :, cs] = mm(a_t[seg(core), :], w_ref[:, cs], NN)
        loop(s.dim // CHUNK, step)
    return product


def on_chip(n):
    return [pl.BlockSpec(memory_space=pltpu.VMEM)] * n


IN_HBM = pl.BlockSpec(memory_space=pl.ANY)


def call(kernel, ident, args, outs, scratch, flops, far_in=(), far_out=(), aliases={}):
    specs = [IN_HBM if i in far_in else on_chip(1)[0] for i in range(args)]
    out_specs = [IN_HBM if i in far_out else on_chip(1)[0] for i in range(len(outs))]
    return pl.pallas_call(
        kernel,
        out_shape=[jax.ShapeDtypeStruct(shape, dtype) for shape, dtype in outs],
        in_specs=specs, out_specs=out_specs, scratch_shapes=scratch, input_output_aliases=aliases,
        cost_estimate=pl.CostEstimate(flops=flops, bytes_accessed=flops // CHUNK, transcendentals=0),
        compiler_params=pltpu.CompilerParams(collective_id=ident, has_side_effects=True, vmem_limit_bytes=VMEM_CAP),
        name=kernel.func.__name__ if isinstance(kernel, functools.partial) else kernel.__name__,
    )


def fetch_all(sem, *pairs):
    copies = [pltpu.make_async_copy(src, dst, sem.at[i]) for i, (src, dst) in enumerate(pairs)]
    for copy in copies:
        copy.start()
    return copies


def gain_row(dst, small_all, which):
    for o in range(N_DEV):
        dst[:1, o * LANE:(o + 1) * LANE] = small_all[o, which:which + 1, :]


def norm_rows(src, gain, dst):
    def step(i):
        rs = seg(i, STRIP)
        t = src[rs, :].astype(F32)
        dst[rs, :] = (t * lax.rsqrt(jnp.mean(t * t, axis=-1, keepdims=True) + NORM_EPS) * gain[:1, :]).astype(BF16)
    loop(src.shape[0] // STRIP, step)


def norm_back(dy, src, gain, skip, dst, dgain):
    def step(i):
        rs = seg(i, STRIP)
        d = dy[rs, :].astype(BF16).astype(F32)
        t = src[rs, :].astype(F32)
        inv = lax.rsqrt(jnp.mean(t * t, axis=-1, keepdims=True) + NORM_EPS)
        gd = gain[:1, :] * d
        pull = jnp.mean(gd * t, axis=-1, keepdims=True)
        dst[rs, :] = (skip[rs, :].astype(F32) + (inv * gd - t * (inv * inv * inv * pull))).astype(BF16)
        g = d * (t * inv)
        dgain[...] += g[:N_CHIP] + g[N_CHIP:]
    dgain[...] = jnp.zeros_like(dgain)
    loop(src.shape[0] // STRIP, step)


QB = 256
KB = 256


def key_rows(dst, src, lo, hd):
    def step(i):
        dst[seg(i, KB), :] = src[lo:lo + hd, seg(i, KB)].T
    loop(src.shape[1] // KB, step)


def score_block(k, q2, scale, diagonal):
    s = mm(k, q2, NN) * scale
    if diagonal:
        key = lax.broadcasted_iota(jnp.int32, s.shape, 0)
        qry = lax.broadcasted_iota(jnp.int32, s.shape, 1) % QB
        s = jnp.where(qry >= key, s, NEG_LARGE)
    return s


def side_by_side(ref, heads, hd, qs):
    return jnp.concatenate([ref[h * hd:(h + 1) * hd, qs] for h in range(heads)], axis=1)


def head(groups, hd, x_ref, g1_ref, g2_ref, pos_ref, wq_ref, wk_ref, wv_ref, freq_ref, wg_ref, wu_ref, wo_ref, qkv_ref, u_scr, small_all, w_out, o_ref, stat_ref, wgu_ref, h_ref, m_ref, cos_ref, sin_ref,
         full_w, acc_o, o_tok, o_send, small_ref, w_ref, full, acc, rot, g_scr, wg_t, wu_t, s_scr, k_scr, osem, *sems):
    me = lax.axis_index('sp')
    tokens, dim = x_ref.shape
    cols = w_ref.shape[0]
    small_ref[...] = jnp.concatenate([r[...].astype(F32) for r in (g1_ref, g2_ref, pos_ref)] + [jnp.zeros((N_CHIP - 3, LANE), F32)], axis=0)
    w_ref[:wq_ref.shape[0], :] = wq_ref[...]
    for k in range(groups):
        for i, ref in enumerate((wk_ref, wv_ref)):
            w_ref[pl.ds(wq_ref.shape[0] + (2 * k + i) * hd, hd), :] = ref[k * hd:(k + 1) * hd, :]
    qw = tokens
    q_all = N_DEV * qw
    gsems, ssems, qsems, ksems, gate_sems, up_sems, osems = sems[:4], *(sems[i:i + 2] for i in range(4, len(sems) - 4, 2))
    gw = row_gather(wo_ref, full_w, sems[-4:], me, 1)
    feat = wg_ref.shape[1] // N_DEV
    enter(me, OTHERS)
    smalls = Swap(lambda peer: small_ref, lambda o: small_all.at[o], ssems, me)
    smalls.start()
    parts = thirds(cols, STRIP)
    g = Gather(w_ref, lambda o: full.at[o // 2, :, seg(o % 2)], lambda view, c: [view.at[pl.ds(*parts[c]), :]], gsems, me)
    g.start()
    gates = Swap(lambda peer: wg_t.at[seg(peer, feat), :], lambda o: wgu_ref.at[:feat, seg(o)], gate_sems, me)
    ups = Swap(lambda peer: wu_t.at[seg(peer, feat), :], lambda o: wgu_ref.at[feat:, seg(o)], up_sems, me)

    def advance(n):
        gates.advance(n)
        ups.advance(n)

    def transpose(i):
        wg_t[seg(i, CHUNK), :] = wg_ref[:, seg(i, CHUNK)].T
        wu_t[seg(i, CHUNK), :] = wu_ref[:, seg(i, CHUNK)].T
    loop(wg_ref.shape[1] // CHUNK, transpose)
    advance(0)

    def own_block(i):
        full[me // 2, seg(i, WIDE), seg(me % 2)] = w_ref[seg(i, WIDE), :]
    loop(cols // WIDE, own_block)
    acc[...] = jnp.zeros_like(acc)
    small_all[me] = small_ref[...]
    smalls.wait_recv()
    gain_row(g_scr, small_all, 0)
    norm_rows(x_ref, g_scr, u_scr)

    def keep(mask):
        chip = flipped(me, mask) // 2
        return pltpu.make_async_copy(full.at[chip], w_out.at[chip], osem.at[mask // 2])

    def use(mask):
        g.wait_pair(mask)
        keep(mask).start()
        chip = flipped(me, mask) // 2
        u = u_scr[:, seg(chip, WIDE)]

        def step(i):
            rs = seg(i, cols // 2)
            acc[rs, :] += mm(full[chip, rs, :], u, NT)
        loop(2, step)

    def tables(o):
        angles = freq_ref[...] * small_all[o, 2:3, :]
        cos_ref[:, seg(o)] = jnp.cos(angles)
        sin_ref[:, seg(o)] = jnp.sin(angles)

    for r in range(len(g.ROUNDS)):
        g.round(r)
        if r in (2, 4):
            advance(r // 2)
        if r == 1:
            loop(N_DEV, tables)
        for mask in g.READY[r]:
            use(mask)

    half = hd // 2
    cos, sin = cos_ref[:, seg(me)], sin_ref[:, seg(me)]

    def turn(h):
        first = seg(2 * h, half)
        second = seg(2 * h + 1, half)
        p = acc[first, :].astype(BF16).astype(F32)
        q = acc[second, :].astype(BF16).astype(F32)
        rot[first, :] = (p * cos - q * sin).astype(BF16)
        rot[second, :] = (q * cos + p * sin).astype(BF16)
    loop(q_all // hd, turn)
    for k in range(groups):
        turn(q_all // hd + 2 * k)
        vs = seg(q_all // hd + 2 * k + 1, hd)
        rot[vs, :] = acc[vs, :].astype(BF16)
    per = N_DEV // groups
    q_rows = lambda peer: seg(peer, qw)
    kv_rows = lambda peer: seg(q_all // (2 * hd) + peer // per, 2 * hd)
    qs = Swap(lambda peer: rot.at[q_rows(peer), :], lambda o: qkv_ref.at[:qw, seg(o, tokens)], qsems, me)
    kvs = Swap(lambda peer: rot.at[kv_rows(peer), :], lambda o: qkv_ref.at[qw:, seg(o, tokens)], ksems, me)
    qs.start()
    kvs.start()
    gw.start()
    keep_own(wo_ref, full_w, me)
    gain_row(g_scr, small_all, 1)
    qkv_ref[:qw, seg(me, tokens)] = rot[q_rows(me), :]
    qkv_ref[qw:, seg(me, tokens)] = rot[kv_rows(me), :]
    wgu_ref[:feat, seg(me)] = wg_t[seg(me, feat), :]
    wgu_ref[feat:, seg(me)] = wu_t[seg(me, feat), :]
    gates.start((CORE,))
    ups.start((CORE,))
    for swap in (qs, kvs):
        swap.wait_recv()
    heads = qkv_ref.shape[0] // hd - 2
    seq = qkv_ref.shape[1]
    scale = hd ** -0.5
    lanes = heads * QB
    key_rows(k_scr, qkv_ref, qw, hd)

    outs = Swap(lambda peer: o_send.at[seg(peer), :], lambda o: o_tok.at[:, seg(o)], osems, me)

    def q_block(qb):
        for at, r in ((2, 0), (4, 1), (5, 2), (6, 3), (7, 4)):
            @pl.when(qb == at)
            def _():
                gw.round(r)
        qs = seg(qb, QB)
        q2 = side_by_side(qkv_ref, heads, hd, qs)

        def scores(kb, top, diagonal):
            s = score_block(k_scr[seg(kb, KB), :], q2, scale, diagonal)
            s_scr[seg(kb, KB), :] = s
            return jnp.maximum(top, jnp.max(s, axis=0, keepdims=True))

        top = lax.fori_loop(0, qb, lambda kb, t: scores(kb, t, False), jnp.full((1, lanes), NEG_LARGE, F32))
        top = scores(qb, top, True)

        def expo(kb, tot):
            e = jnp.exp(s_scr[seg(kb, KB), :] - top)
            s_scr[seg(kb, KB), :] = e
            return tot + jnp.sum(e, axis=0, keepdims=True)

        inv = 1.0 / lax.fori_loop(0, qb + 1, expo, jnp.zeros((1, lanes), F32))

        def weigh(kb, acc):
            p = (s_scr[seg(kb, KB), :] * inv).astype(BF16)
            return acc + mm(qkv_ref[qw + hd:, seg(kb, KB)], p, NN)

        acc = lax.fori_loop(0, qb + 1, weigh, jnp.zeros((hd, lanes), F32))
        for h in range(heads):
            o_ref[h * hd:(h + 1) * hd, qs] = acc[:, h * QB:(h + 1) * QB].astype(BF16)
        stat_ref[qb, :1, :] = top
        stat_ref[qb, 1:, :] = inv
        o_send[qs, :] = o_ref[:, qs].T

    loop(seq // QB, q_block)
    outs.start()
    advance(3)
    o_tok[:, seg(me)] = o_send[seg(me), :]
    for r in (5, 6):
        gw.round(r)
    outs.wait_recv()
    for mask in CHIP_MASKS:
        gw.wait_pair(mask)

    def project(n):
        cs = seg(n, CHUNK)
        acc_o[:, cs] = mm(o_tok[...], full_w[:, :, cs].reshape(dim, CHUNK), NN)
    loop(dim // CHUNK, project)

    def residual(i):
        rs = seg(i, STRIP)
        h_ref[rs, :] = (x_ref[rs, :].astype(F32) + acc_o[rs, :]).astype(BF16)
    loop(tokens // STRIP, residual)
    norm_rows(h_ref, g_scr, m_ref)
    for swap in (gates, ups):
        swap.wait_recv()
    for mask in CHIP_MASKS:
        keep(mask).wait()
    outs.wait_send()
    for swap in (gates, ups):
        swap.wait_send((CORE,) + SETS[3])
    g.finish()
    gw.finish()
    for swap in (smalls, qs, kvs):
        swap.wait_send()


def dw_swap(stage, dw_hbm, sems, me):
    return Swap(lambda peer: stage(peer).at[:, seg(peer % 2)], lambda o: dw_hbm.at[o], sems, me)


def mlp(m_ref, dout_ref, wgu_hbm, down_hbm, u_ref, h_ref, small_all, wo_ref, o_ref,
        ucol_ref, m_out, dgu_out, ddown_out, y_ref, dh_ref, do_ref, dwo_ref, dg_ref, dw_hbm,
        wgu_ref, down_ref, glu_ref, dgu_ref, ddown_ref, isem, dsem, full_d, full_m, osem, stage, g_scr, dgu_t, glu_t, free, *scr):
    me = lax.axis_index('sp')
    feat, dim = down_ref.shape
    loads = fetch_all(isem, (wgu_hbm, wgu_ref), (down_hbm, down_ref))
    enter(me, OTHERS)
    sems = scr[4:]
    gd = row_gather(dout_ref, full_d, sems[:4], me, 0)
    gm = row_gather(m_ref, full_m, sems[4:8], me, 2)
    g = row_gather(dh_ref, full_d, sems[8:12], me, 1)
    ucols = Swap(lambda peer: u_ref.at[:, seg(peer)], lambda o: ucol_ref.at[seg(o), :], sems[12:14], me)
    def dw_part(slot, mask):
        cols = full_m[:, :, seg(flipped(me, mask) // 2, WIDE)].reshape(dgu_ref.shape[1], WIDE)
        stage[slot] = mm(dgu_ref[...], cols, NN)
        swap = dw_swap(lambda peer: stage.at[slot], dw_hbm, sems[14:16], me)
        loop(2, lambda core: swap.copy(mask + core).start())

    gm.start()
    gd.start()
    ucol_ref[seg(me), :] = u_ref[:, seg(me)]
    keep_own(m_ref, full_m, me)
    keep_own(dout_ref, full_d, me)
    gain_row(g_scr, small_all, 1)
    dwo_ref[...] = jnp.zeros_like(dwo_ref)
    ddown_ref[...] = jnp.zeros_like(ddown_ref)

    def keep(mask):
        chip = flipped(me, mask) // 2
        ts = seg(chip, WIDE)
        ends = ((full_m.at[chip], m_out.at[chip]), (dgu_ref.at[:, ts], dgu_out.at[:, ts]))
        return [pltpu.make_async_copy(src, dst, osem.at[mask // 2, i]) for i, (src, dst) in enumerate(ends)]

    for load in loads:
        load.wait()

    def use(mask):
        gd.wait_pair(mask)
        gm.wait_pair(mask)
        chip = flipped(me, mask) // 2
        ts = seg(chip, WIDE)
        gu = mm(wgu_ref[...], full_m[chip], NT).astype(BF16).astype(F32)
        gate, up = gu[:feat], gu[feat:]
        d_glu = mm(down_ref[...], full_d[chip], NT).astype(BF16).astype(F32)
        sig = jax.nn.sigmoid(gate)
        act = gate * sig
        glu = (act * up).astype(BF16)
        glu_ref[:, ts] = glu
        dgu_ref[:feat, ts] = (d_glu * up * (sig * (1.0 + gate * (1.0 - sig)))).astype(BF16)
        dgu_ref[feat:, ts] = (d_glu * act).astype(BF16)

        def step(n):
            ddown_ref[:, seg(n, CHUNK)] += mm(glu, full_d[chip, :, seg(n, CHUNK)], NN)
        loop(dim // CHUNK, step)
        for copy in keep(mask):
            copy.start()

    for r in range(len(gm.ROUNDS)):
        gm.round(r)
        gd.round(r)
        if r == 3:
            ucols.start()
        for mask in gm.READY[r]:
            use(mask)
    dw_part(0, XYZ)
    for gather in (gd, gm):
        gather.finish()
    leave = pltpu.make_async_copy(ddown_ref, ddown_out, dsem)
    leave.start()
    s = Scatter(*scr[:4], sems[16:], me)
    total = s.run(block_product(s, dgu_ref, wgu_ref, dgu_t))
    for mask in NEAR:
        pl.semaphore_signal(free, inc=1, device_id=(flipped(me, mask),), device_id_type=MESH)
    norm_back(total, h_ref, g_scr, dout_ref, dh_ref, dg_ref)
    g.start()
    keep_own(dh_ref, full_d, me)
    s.finish()
    pl.semaphore_wait(free, len(NEAR))

    def use_dh(mask):
        g.wait_pair(mask)
        chip = flipped(me, mask) // 2
        do_ref[:, seg(chip, WIDE)] = mm(wo_ref[...], full_d[chip], NT).astype(BF16)
        o = o_ref[:, seg(chip, WIDE)]

        def step(n):
            dwo_ref[:, seg(n, CHUNK)] += mm(o, full_d[chip, :, seg(n, CHUNK)], NN)
        loop(dim // CHUNK, step)

    def between(i):
        if i < len(g.ROUNDS):
            g.round(i)
            for mask in g.READY[i]:
                use_dh(mask)

    s = Scatter(*scr[:4], sems[16:], me)
    total = s.run(block_product(s, glu_ref, down_ref, glu_t), between, lambda: (dw_part(1, X), dw_part(2, Y + Z)))
    y_ref[...] = (h_ref[...].astype(F32) + total[...]).astype(BF16)
    s.finish()
    g.finish()
    swap = dw_swap(lambda peer: stage.at[0], dw_hbm, sems[14:16], me)
    for mask in (XYZ, X, Y + Z):
        loop(2, lambda core: (swap.arrival(mask + core).wait_recv(), swap.copy(mask + core).wait_send()))
    ucols.wait_recv()
    ucols.wait_send()
    leave.wait()
    loop(N_CHIP, lambda j: [pltpu.make_async_copy(src, dst, osem.at[j, i]).wait() for i, (src, dst) in enumerate(
        ((full_m.at[0], m_out.at[0]), (dgu_ref.at[:, seg(0, WIDE)], dgu_out.at[:, seg(0, WIDE)])))])


def back(groups, hd, qkv_ref, do_ref, stat_ref, cos_all, sin_all, dgu_ref, m_hbm, ucol_ref, w_hbm, x_ref, small_all, dh_ref, dg2_ref, dw_in,
         dw_hbm, dwq_ref, dwkv_ref, dx_ref, gain_ref,
         p_scr, dp_scr, k_scr, v_scr, dk_acc, dv_acc, stage, dq_scr, dkv_scr, m_scr,
         full, w_scr, shares, dkv_own, full_kv, dqkv, dn, g_scr, dg1, gains, gains_in, wsem, lsem, msem, *sems):
    heads = qkv_ref.shape[0] // hd - 2
    seq = qkv_ref.shape[1]
    scale = hd ** -0.5
    lanes = heads * QB
    qw = heads * hd
    half = hd // 2
    me = lax.axis_index('sp')
    feat = dgu_ref.shape[0] // 2
    first = (Y, X + Z, Z, X + Y, 0)

    def fetch(mask):
        cols = seg(flipped(me, mask) // 2, WIDE)
        return pltpu.make_async_copy(m_hbm.at[:, :, cols], m_scr.at[:, :, cols], msem.at[mask // 2])
    for mask in first:
        fetch(mask).start()
    load = pltpu.make_async_copy(w_hbm, w_scr, wsem)
    load.start()
    enter(me, OTHERS)
    gain_row(g_scr, small_all, 0)

    dws = dw_swap(lambda peer: stage.at[peer // 2], dw_hbm, sems[:2], me)
    gq = row_gather(dq_scr, full, sems[4:8], me)
    own = pltpu.make_async_copy(dws.src(me), dws.dst(me), lsem)

    def make(mask):
        chip = flipped(me, mask) // 2
        fetch(mask).wait()
        cols = m_scr[:, :, seg(chip, WIDE)].reshape(seq, WIDE)
        stage[chip] = mm(dgu_ref[...], cols, NN)

    def advance(n):
        if n > 2:
            dws.wait_send(SETS[n - 1])
        dws.start(SETS[n])

    for i, mask in enumerate(first):
        make(mask)
        if i == 1:
            advance(2)
    dws.start((CORE,))
    own.start()

    dk_acc[...] = jnp.zeros_like(dk_acc)
    dv_acc[...] = jnp.zeros_like(dv_acc)
    key_rows(k_scr, qkv_ref, qw, hd)
    key_rows(v_scr, qkv_ref, qw + hd, hd)

    def q_block(qb):
        @pl.when(qb == 5)
        def _():
            advance(3)
        qs = seg(qb, QB)
        q2 = side_by_side(qkv_ref, heads, hd, qs)
        do2 = side_by_side(do_ref, heads, hd, qs)
        top = stat_ref[qb, :1, :]
        inv = stat_ref[qb, 1:, :]

        def probs(kb, rd, diagonal):
            ks = seg(kb, KB)
            s = score_block(k_scr[ks, :], q2, scale, diagonal)
            p = jnp.exp(s - top) * inv
            dp = mm(v_scr[ks, :], do2, NN).astype(BF16)
            p_scr[ks, :] = p
            dp_scr[ks, :] = dp
            dv_acc[ks, :] += mm(p.astype(BF16), do2, NT)
            return rd + jnp.sum(dp.astype(F32) * p, axis=0, keepdims=True)

        rd = lax.fori_loop(0, qb, lambda kb, r: probs(kb, r, False), jnp.zeros((1, lanes), F32))
        rd = probs(qb, rd, True)

        def d_scores(kb, acc):
            ks = seg(kb, KB)
            ds = (p_scr[ks, :] * (dp_scr[ks, :].astype(F32) - rd) * scale).astype(BF16)
            dk_acc[ks, :] += mm(ds, q2, NT)
            return acc + mm(qkv_ref[qw:qw + hd, ks], ds, NN)

        acc = lax.fori_loop(0, qb + 1, d_scores, jnp.zeros((hd, lanes), F32))
        cos, sin = cos_all[:, qs], sin_all[:, qs]
        for h in range(heads):
            dq = acc[:, h * QB:(h + 1) * QB].astype(BF16).astype(F32)
            p, q = dq[:half], dq[half:]
            dq_scr[h * hd:h * hd + half, qs] = (p * cos + q * sin).astype(BF16)
            dq_scr[h * hd + half:(h + 1) * hd, qs] = (q * cos - p * sin).astype(BF16)

    loop(seq // QB, q_block)

    def share(i):
        rs = seg(i, WIDE)
        dkv_scr[rs, :] = jnp.concatenate([dk_acc[rs, :], dv_acc[rs, :]], axis=1).astype(BF16)
    loop(seq // WIDE, share)
    tokens = ucol_ref.shape[1]
    per = N_DEV // groups
    q_all = dwq_ref.shape[0]
    sh = Swap(lambda peer: dkv_scr.at[seg(peer, tokens), :], lambda o: shares.at[o], sems[2:4], me)
    parts = thirds(dkv_own.shape[0], STRIP)
    gk = Gather(dkv_own, lambda o: full_kv.at[:, seg(o, tokens)], lambda view, c: [view.at[pl.ds(*parts[c]), :]], sems[8:12], me)
    gs = Swap(lambda peer: gains.at[:, seg(peer)], lambda o: gains_in.at[o], sems[12:], me)
    sh.start()
    gq.start()
    keep_own(dq_scr, full, me)
    shares[me] = dkv_scr[seg(me, tokens), :]
    sh.wait_recv()
    cos, sin = cos_all[:, seg(me)], sin_all[:, seg(me)]
    for k in range(groups):
        both = sum(shares[per * k + i].astype(F32) for i in range(per)).astype(BF16).astype(F32).T
        p, q = both[:half], both[half:hd]
        lo = 2 * hd * k
        dkv_own[lo:lo + half, :] = (p * cos + q * sin).astype(BF16)
        dkv_own[lo + half:lo + hd, :] = (q * cos - p * sin).astype(BF16)
        dkv_own[lo + hd:lo + 2 * hd, :] = both[hd:].astype(BF16)
    gk.start()
    full_kv[:, seg(me, tokens)] = dkv_own[...]
    for k in range(groups):
        dqkv[:, q_all + 2 * hd * k:q_all + 2 * hd * (k + 1)] = dkv_own[2 * hd * k:2 * hd * (k + 1), :].T

    def use(mask):
        gq.wait_pair(mask)
        chip = flipped(me, mask) // 2
        dwq_ref[seg(chip, WIDE), :] = mm(full[chip], ucol_ref[...], NN)
        dqkv[:, seg(chip, WIDE)] = full[chip, :, seg(me, tokens)].T

    for r in range(len(gq.ROUNDS)):
        gq.round(r)
        gk.round(r)
        for mask in gq.READY[r]:
            use(mask)
    load.wait()

    def normed(i):
        dn[:, seg(i, WIDE)] = mm(dqkv[...], w_scr[i], NN)
    loop(N_CHIP, normed)
    norm_back(dn, x_ref, g_scr, dh_ref, dx_ref, dg1)
    gains[...] = jnp.concatenate([jnp.sum(dg1[...], axis=0, keepdims=True), jnp.sum(dg2_ref[...], axis=0, keepdims=True),
                                  jnp.zeros((N_CHIP - 2, dg1.shape[1]), F32)], axis=0)
    gs.start()
    gains_in[me] = gains[:, seg(me)]
    for mask in CHIP_MASKS:
        gk.wait_pair(mask)
    dwkv_ref[...] = mm(full_kv[...], ucol_ref[...], NN)
    gs.wait_recv()
    gain_ref[...] = sum(gains_in[o] for o in range(N_DEV))
    dws.wait_recv((CORE,) + SETS[2] + SETS[3])
    dws.wait_send((CORE,) + SETS[3])
    own.wait()
    for c in (sh, gs):
        c.wait_send()
    for g in (gq, gk):
        g.finish()


def finish(dw_hbm, dkv_hbm, *refs):
    n = (len(refs) - 11) // 3
    srcs, (gate, up, dk, dv), dsts = refs[:n], refs[n:n + 4], refs[n + 4:2 * n + 4]
    (g_in, g_out, kv_in), holds, sems = refs[2 * n + 4:2 * n + 7], refs[2 * n + 7:3 * n + 7], refs[3 * n + 7:]
    t_in, t_out, p_in, p_out = sems
    feat = g_in.shape[2]
    four = N_DEV // 4
    step = four * feat
    hd = dk.shape[0] // (kv_in.shape[0] // LANE)
    starts = [(w, i) for i in range(4) for w in range(2)]

    def fetch(w, i):
        at = pl.ds(i * four, four)
        return pltpu.make_async_copy(dw_hbm.at[at, pl.ds(w * feat, feat), :], g_in.at[w, at], t_in.at[w, i])

    def put(w, i):
        cs = pl.ds(i * step, step)
        return pltpu.make_async_copy(g_out.at[w, :, cs], (gate, up)[w].at[:, cs], t_out.at[w, i])
    moves = [(pltpu.make_async_copy(a, h, p_in.at[k]), pltpu.make_async_copy(h, b, p_out.at[k])) for k, (a, h, b) in enumerate(zip(srcs, holds, dsts))]
    kv = pltpu.make_async_copy(dkv_hbm, kv_in, p_in.at[n])
    for w, i in starts:
        fetch(w, i).start()
    kv.start()
    for k, (w, i) in enumerate(starts):
        fetch(w, i).wait()
        if k < len(moves):
            moves[k][0].start()

        g_out[w, :, pl.ds(i * step, step)] = g_in[w, pl.ds(i * four, four)].reshape(step, LANE).T
        put(w, i).start()
    kv.wait()
    for k in range(dk.shape[0] // hd):
        for i, ref in enumerate((dk, dv)):
            ref[k * hd:(k + 1) * hd, :] = kv_in[(2 * k + i) * hd:(2 * k + i + 1) * hd, :]
    for load, store in moves:
        load.wait()
        store.start()
    for w, i in starts:
        put(w, i).wait()
    for _, store in moves:
        store.wait()


def solution(mesh):
    assert mesh.shape['sp'] == N_DEV

    def layer_step(x_in, positions, d_out, norm1_gain, norm2_gain, w_q, w_k, w_v, w_o, w_gate, w_up, w_down):
        tokens, dim = x_in.shape
        seq = tokens * N_DEV
        n_q, hd = w_q.shape[1:]
        n_kv = w_k.shape[1]
        qw = n_q // N_DEV * hd
        rows = w_q.shape[0]
        feat = w_down.shape[0]
        cols = (n_q + 2 * n_kv) * hd
        lanes = qw // hd * QB
        vm = pltpu.VMEM
        full = vm((N_CHIP, WIDE, dim), BF16)
        gain_scr = vm((N_CHIP, dim), F32)
        tok_shapes = 2 * (((tokens, dim), BF16),)
        dw_shape = ((N_DEV, 2 * feat, rows), F32)

        inv_freq = 1.0 / (ROPE_BASE ** (jnp.arange(hd // 2, dtype=F32) * (2.0 / hd)))
        freq = jnp.broadcast_to(inv_freq[:, None], (hd // 2, rows))
        row = lambda v: v.reshape(1, rows)
        by_head = lambda w: w.transpose(1, 2, 0).reshape(-1, rows)
        wo_own = w_o.reshape(qw, dim)

        args = (x_in, row(norm1_gain), row(norm2_gain), row(positions), by_head(w_q), by_head(w_k), by_head(w_v), freq, w_gate, w_up, wo_own)
        qkv, u, small_all, wqkv, attn_t, stat, wgu, hidden, mlp_in, cos_all, sin_all = call(
            functools.partial(head, n_kv, hd), 0, len(args),
            (((qw + 2 * hd, seq), BF16), tok_shapes[0], ((N_DEV, N_CHIP, rows), F32), ((N_CHIP, cols, WIDE), BF16),
             ((qw, seq), BF16), ((seq // QB, 2, lanes), F32), ((2 * feat, dim), BF16), *tok_shapes, *(2 * (((hd // 2, seq), F32),))),
            [full, vm((tokens, dim), F32), vm((tokens, dim), BF16), vm((seq, qw), BF16),
             vm((N_CHIP, rows), F32), vm((cols, rows), BF16), vm((N_CHIP, cols, WIDE), BF16), vm((cols, tokens), F32), vm((cols, tokens), BF16), gain_scr,
             vm((feat * N_DEV, rows), BF16), vm((feat * N_DEV, rows), BF16), vm((seq, lanes), F32), vm((seq, hd), BF16), dma(N_CHIP),
             *Gather.sems, *(6 * Swap.sems), *Gather.sems], 4 * qw * seq * seq, far_out=(3,))(*args)
        args = (mlp_in, d_out, wgu, w_down, u, hidden, small_all, wo_own, attn_t)
        u_col, m_full, dgu, d_down, y_out, d_hidden, d_attn, d_wo, d_g2, d_gu = call(
            mlp, 1, len(args),
            (((seq, rows), BF16), ((N_CHIP, WIDE, dim), BF16), ((2 * feat, seq), BF16), ((feat, dim), F32),
             *tok_shapes, ((qw, seq), BF16), ((qw, dim), F32), ((N_CHIP, dim), F32), dw_shape),
            [vm((2 * feat, dim), BF16), vm((feat, dim), BF16), vm((feat, seq), BF16), vm((2 * feat, seq), BF16), vm((feat, dim), F32), dma(2), dma(),
             full, full, dma(N_CHIP, 2), vm((3, 2 * feat, WIDE), F32), gain_scr, vm((WIDE, 2 * feat), BF16), vm((WIDE, feat), BF16), pltpu.SemaphoreType.REGULAR,
             *Scatter.scratch(tokens, dim), *(3 * Gather.sems), *(2 * Swap.sems), *Scatter.sems], 12 * feat * seq * dim,
            far_in=(2, 3), far_out=(1, 2, 3, 9))(*args)
        args = (qkv, d_attn, stat, cos_all, sin_all, dgu, m_full, u_col, wqkv, x_in, small_all, d_hidden, d_g2, d_gu)
        d_gu, d_wq, d_wkv, d_x, gains = call(
            functools.partial(back, n_kv, hd), 3, len(args),
            (dw_shape, ((n_q * hd, rows), F32), ((2 * n_kv * hd, rows), F32), tok_shapes[0], ((N_CHIP, rows), F32)),
            [vm((seq, lanes), F32), vm((seq, lanes), BF16), vm((seq, hd), BF16), vm((seq, hd), BF16), vm((seq, hd), F32), vm((seq, hd), F32),
             vm((N_CHIP, 2 * feat, WIDE), F32), vm((qw, seq), BF16), vm((seq, 2 * hd), BF16), full,
             full, vm((N_CHIP, cols, WIDE), BF16), vm((N_DEV, tokens, 2 * hd), BF16), vm((2 * n_kv * hd, tokens), BF16), vm((2 * n_kv * hd, seq), BF16),
             vm((tokens, cols), BF16), vm((tokens, dim), F32), gain_scr, gain_scr, gain_scr, vm((N_DEV, N_CHIP, rows), F32), dma(), dma(), dma(N_CHIP),
             *(2 * Swap.sems), *(2 * Gather.sems), *Swap.sems], 10 * qw * seq * seq, far_in=(6, 8, 13), far_out=(0,), aliases={13: 0})(*args)
        moved = (d_wq, d_wo, d_down, d_x, y_out, gains)
        half_kv = jax.ShapeDtypeStruct((n_kv * hd, rows), F32)
        wide = jax.ShapeDtypeStruct((rows, feat * N_DEV), F32)
        d_gate, d_up, d_wk, d_wv, d_wq, d_wo, d_down, d_x, y_out, gains = pl.pallas_call(
            finish,
            out_shape=[wide, wide, half_kv, half_kv] + [jax.ShapeDtypeStruct(v.shape, v.dtype) for v in moved],
            in_specs=[IN_HBM] * (2 + len(moved)), out_specs=[IN_HBM] * 2 + on_chip(2) + [IN_HBM] * len(moved),
            scratch_shapes=[vm((2, N_DEV, feat, rows), F32), vm((2, rows, feat * N_DEV), F32), vm(d_wkv.shape, F32)]
            + [vm(v.shape, v.dtype) for v in moved] + [dma(2, 4), dma(2, 4), dma(len(moved) + 1), dma(len(moved))],
            compiler_params=pltpu.CompilerParams(vmem_limit_bytes=VMEM_CAP), name='finish',
        )(d_gu, d_wkv, *moved)
        by_row = lambda g, heads: g.reshape(heads, hd, rows).transpose(2, 0, 1)
        return (y_out, d_x, gains[0], gains[1], by_row(d_wq, n_q), by_row(d_wk, n_kv), by_row(d_wv, n_kv),
                d_wo.reshape(w_o.shape), d_gate, d_up, d_down)

    all_rows = P('sp')
    return jax.shard_map(layer_step, mesh=mesh, in_specs=(all_rows,) * 12, out_specs=(all_rows,) * 11, check_vma=False)
```

```python
import functools
import jax
import jax.numpy as jnp
from jax import lax
from jax.experimental import pallas as pl
from jax.experimental.pallas import tpu as pltpu
from jax.sharding import PartitionSpec as P

ROPE_BASE = 10000.0
NORM_EPS = 1e-5
NEG_LARGE = -1e30
F32 = jnp.float32
BF16 = jnp.bfloat16
N_DEV, N_CHIP, LANE, WIDE, CHUNK, STRIP = 16, 8, 128, 256, 512, 16
NT = (((1,), (1,)), ((), ()))
TN = (((0,), (0,)), ((), ()))
NN = (((1,), (0,)), ((), ()))
MESH = pl.DeviceIdType.MESH
VMEM_CAP = 67043328

CORE, X, Y, Z = 1, 2, 4, 8
XYZ = X + Y + Z
ORDERS = ((X, Y, Z), (Y, Z, X), (Z, X, Y))
CHIP_MASKS = (0, X, Y, Z, X + Y, X + Z, Y + Z, XYZ)
NEAR = (CORE, X, Y, Z)
OTHERS = range(1, N_DEV)
SETS = tuple(tuple(m + c for m in masks for c in (0, CORE)) for masks in ((XYZ,), (X, Y + Z), (Y, X + Z), (Z, X + Y)))
N_COL = len(ORDERS)
COLOURS = range(N_COL)


def mm(a, b, dims):
    return lax.dot_general(a, b, dims, preferred_element_type=F32)


def seg(index, width=LANE):
    return pl.ds(pl.multiple_of(index * width, width), width)


def loop(count, body):
    lax.fori_loop(0, count, lambda i, c: (body(i), c)[1], 0)


def differing(index, mask):
    return sum(((index // bit + mask // bit) % 2) * bit for bit in NEAR)


def flipped(index, mask):
    out = index
    for bit in NEAR:
        if mask & bit:
            out = out + (1 - 2 * ((index // bit) % 2)) * bit
    return out


def thirds(total, unit):
    n = total // unit
    first = (n + 2) // 3
    second = (n - first + 1) // 2
    sizes = (first * unit, second * unit, (n - first - second) * unit)
    return ((0, sizes[0]), (sizes[0], sizes[1]), (sizes[0] + sizes[1], sizes[2]))


def pieces(rows, cols, unit):
    share = cols // LANE // N_COL * LANE
    strips = thirds(rows, unit)
    rest = cols - N_COL * share
    return [[(pl.ds(0, rows), pl.ds(c * share, share)), (pl.ds(*strips[c]), pl.ds(N_COL * share, rest))] for c in COLOURS]


def enter(me, masks):
    barrier = pltpu.get_barrier_semaphore()
    for mask in masks:
        pl.semaphore_signal(barrier, inc=1, device_id=(flipped(me, mask),), device_id_type=MESH)
    pl.semaphore_wait(barrier, len(masks))


def remote(src, dst, send, recv, peer):
    return pltpu.make_async_remote_copy(src_ref=src, dst_ref=dst, send_sem=send, recv_sem=recv, device_id=(peer,), device_id_type=MESH)


def dma(*shape):
    return pltpu.SemaphoreType.DMA(shape)


class Swap:
    sems = (dma(N_DEV), dma(N_DEV))

    def __init__(self, src, dst, sems, me):
        self.src, self.dst, (self.send, self.recv), self.me = src, dst, sems, me

    def copy(self, mask):
        peer = differing(self.me, mask)
        return remote(self.src(peer), self.dst(self.me), self.send.at[mask], self.recv.at[mask], peer)

    def arrival(self, mask):
        view = self.dst(differing(self.me, mask))
        return remote(view, view, self.send.at[mask], self.recv.at[mask], self.me)

    def each(self, masks, act):
        if masks is None:
            loop(N_DEV - 1, lambda i: act(i + 1))
        else:
            for mask in masks:
                act(mask)

    def start(self, masks=None):
        self.each(masks, lambda mask: self.copy(mask).start())

    def advance(self, n):
        if n:
            self.wait_send(SETS[n - 1])
        self.start(SETS[n])

    def wait_recv(self, masks=None):
        self.each(masks, lambda mask: self.arrival(mask).wait_recv())

    def wait_send(self, masks=None):
        self.each(masks, lambda mask: self.copy(mask).wait_send())


class Gather:
    ROUNDS = ((0,), (1,), (2,), (0, 1), (0, 2), (1, 2), (0, 1, 2))
    READY = ((0,), (), (), (X, Y), (Z,), (X + Y, X + Z), (Y + Z, XYZ))
    sems = (dma(N_COL, N_CHIP, 2), dma(N_COL, N_CHIP, 2), dma(N_CHIP), dma(N_CHIP))

    def __init__(self, own, block, cut, sems, me):
        self.own, self.block, self.cut, self.me = own, block, cut, me
        self.send, self.recv, self.pair_send, self.pair_recv = sems

    def source(self, mask):
        return self.block(flipped(self.me, mask)) if mask else self.own

    def unit(self, colour, mask, axis):
        ends = zip(self.cut(self.source(mask), colour), self.cut(self.block(flipped(self.me, mask)), colour))
        j = self.sends(colour).index((mask, axis))
        return [remote(src, dst, self.send.at[colour, j, i], self.recv.at[colour, (mask + axis) // 2, i],
                       flipped(self.me, axis)) for i, (src, dst) in enumerate(ends)]

    def sends(self, colour):
        return [(0, axis) for axis in ORDERS[colour]] + [step[1:] for step in self.onward(colour)]

    def start_unit(self, colour, mask, axis):
        for copy in self.unit(colour, mask, axis):
            copy.start()

    def pair(self, mask):
        return remote(self.source(mask), self.block(flipped(self.me, mask)), self.pair_send.at[mask // 2],
                      self.pair_recv.at[mask // 2], flipped(self.me, CORE))

    def wait_pair(self, mask):
        view = self.block(flipped(self.me, mask + CORE))
        remote(view, view, self.pair_send.at[mask // 2], self.pair_recv.at[mask // 2], self.me).wait_recv()

    def onward(self, colour):
        order = ORDERS[colour]
        for picks in self.ROUNDS:
            for axis in order[picks[-1] + 1:]:
                yield picks, sum(order[p] for p in picks), axis

    def start(self):
        for pos in COLOURS:
            for colour in COLOURS:
                self.start_unit(colour, 0, ORDERS[colour][pos])
        self.pair(0).start()

    def round(self, r):
        for colour in COLOURS:
            mask = sum(ORDERS[colour][p] for p in self.ROUNDS[r])
            for i, view in enumerate(self.cut(self.block(flipped(self.me, mask)), colour)):
                remote(view, view, self.send.at[colour, 0, i], self.recv.at[colour, mask // 2, i], self.me).wait_recv()
            for picks, at, axis in self.onward(colour):
                if picks == self.ROUNDS[r]:
                    self.start_unit(colour, at, axis)
        for mask in {2: (X, Y, Z), 5: (X + Y, X + Z, Y + Z), 6: (XYZ,)}.get(r, ()):
            self.pair(mask).start()

    def finish(self):
        for colour in COLOURS:
            for i, view in enumerate(self.cut(self.own, colour)):
                loop(len(self.sends(colour)), lambda j: remote(view, view, self.send.at[colour, j, i], self.recv.at[colour, j, i], self.me).wait_send())
        loop(N_CHIP, lambda j: remote(self.own, self.own, self.pair_send.at[j], self.pair_recv.at[j], self.me).wait_send())


def row_gather(own, full, sems, me, extra=None):
    rows, width = own.shape
    parts = pieces(rows, width, STRIP)
    if extra is not None:
        share = width // LANE // N_COL * LANE
        more = width - N_COL * share
        parts = [[(pl.ds(0, rows), pl.ds(c * share + more * (c > extra), share + more * (c == extra)))] for c in COLOURS]

    def block(o):
        return full.at[o // 2, seg(o % 2), :]

    return Gather(own, block, lambda view, c: [view.at[rs, cs] for rs, cs in parts[c]], sems, me)


def keep_own(own, full, me):
    def step(i):
        full[me // 2, pl.ds(pl.multiple_of((me % 2) * LANE + i * STRIP, STRIP), STRIP), :] = own[seg(i, STRIP), :]
    loop(LANE // STRIP, step)


class Scatter:
    ORDER = (XYZ, X + Y, Y + Z, X + Z, X, Y, Z, 0)
    sems = (dma(N_CHIP), dma(N_CHIP), dma(N_COL, N_CHIP, 2), dma(N_COL, N_CHIP, 2))

    @staticmethod
    def scratch(tokens, dim):
        return [pltpu.VMEM((n, tokens, dim), F32) for n in (N_CHIP, 2, N_CHIP, N_CHIP - 1)]

    def __init__(self, part, other, pair_in, link_in, sems, me):
        self.part, self.other, self.pair_in, self.link_in, self.me = part, other, pair_in, link_in, me
        self.pair_send, self.pair_recv, self.link_send, self.link_recv = sems
        self.tokens, self.dim = part.shape[1:]
        self.pieces = pieces(self.tokens, self.dim, STRIP // 2)
        self.ready, self.sent = set(), [0] * N_COL

    @staticmethod
    def first(colour, mask):
        return next((i for i, a in enumerate(ORDERS[colour]) if mask & a), 3)

    def slot(self, colour, mask, axis):
        slots = [(m, a) for m in self.ORDER for a in ORDERS[colour][:self.first(colour, m)]]
        return slots.index((mask, axis))

    def pair(self, i):
        return remote(self.other.at[i % 2], self.pair_in.at[i], self.pair_send.at[i], self.pair_recv.at[i], flipped(self.me, CORE))

    def link(self, colour, mask):
        axis = ORDERS[colour][self.first(colour, mask)]
        slot = self.slot(colour, mask - axis, axis)
        i = self.ORDER.index(mask)
        return [remote(self.part.at[i, rs, cs], self.link_in.at[slot, rs, cs], self.link_send.at[colour, i, k],
                       self.link_recv.at[colour, slot, k], flipped(self.me, axis)) for k, (rs, cs) in enumerate(self.pieces[colour])]

    def start_link(self, colour, mask):
        for copy in self.link(colour, mask):
            copy.start()

    def add(self, mask, ref, cs):
        i = self.ORDER.index(mask)

        def step(r):
            rs = seg(r, STRIP)
            self.part[i, rs, cs] += ref[rs, cs]
        loop(self.tokens // STRIP, step)

    def finish_pair(self, i):
        self.pair(i).wait_recv()
        self.add(self.ORDER[i], self.pair_in.at[i], pl.ds(0, self.dim))
        self.ready.add(self.ORDER[i])
        for colour in COLOURS:
            a, b, c = ORDERS[colour]
            todo = (XYZ, a + b, a + c, a)
            while self.sent[colour] < len(todo) and todo[self.sent[colour]] in self.ready:
                self.start_link(colour, todo[self.sent[colour]])
                self.sent[colour] += 1

    def take(self, colour, mask, axis):
        for copy in self.link(colour, mask + axis):
            copy.wait_recv()
        ref = self.link_in.at[self.slot(colour, mask, axis)]
        (_, wide), (rs, cs) = self.pieces[colour]
        self.add(mask, ref, wide)
        self.part[self.ORDER.index(mask), rs, cs] += ref[rs, cs]

    def run(self, product, between=lambda i: None):
        for i, mask in enumerate(self.ORDER):
            if i > 1:
                self.pair(i - 2).wait_send()
            product(i, flipped(self.me, mask) // 2)
            self.pair(i).start()
            if i:
                self.finish_pair(i - 1)
            between(i)
        self.finish_pair(N_CHIP - 1)
        for step in range(2):
            for colour in COLOURS:
                a, b, c = ORDERS[colour]
                mask = (b + c, b)[step]
                self.take(colour, mask, a)
                self.start_link(colour, mask)
        for colour in COLOURS:
            a, b, c = ORDERS[colour]
            self.take(colour, c, a)
            self.take(colour, c, b)
            self.start_link(colour, c)
        for colour in COLOURS:
            for axis in ORDERS[colour]:
                self.take(colour, 0, axis)
        return self.part.at[N_CHIP - 1]

    def finish(self):
        for i in (N_CHIP - 2, N_CHIP - 1):
            self.pair(i).wait_send()
        for colour in COLOURS:
            for k, (rs, cs) in enumerate(self.pieces[colour]):
                view = self.part.at[0, rs, cs]
                loop(N_CHIP - 1, lambda i: remote(view, view, self.link_send.at[colour, i, k], self.link_recv.at[colour, i, k], self.me).wait_send())


def block_product(s, a_ref, w_ref, a_t):
    core = s.me % 2

    def product(i, chip):
        a_t[...] = a_ref[:, seg(chip, WIDE)].T

        def step(n):
            cs = seg(n, CHUNK)
            s.other[i % 2, :, cs] = mm(a_t[seg(1 - core), :], w_ref[:, cs], NN)
            s.part[i, :, cs] = mm(a_t[seg(core), :], w_ref[:, cs], NN)
        loop(s.dim // CHUNK, step)
    return product


def on_chip(n):
    return [pl.BlockSpec(memory_space=pltpu.VMEM)] * n


IN_HBM = pl.BlockSpec(memory_space=pl.ANY)


def call(kernel, ident, args, outs, scratch, flops, far_in=(), far_out=(), aliases={}):
    specs = [IN_HBM if i in far_in else on_chip(1)[0] for i in range(args)]
    out_specs = [IN_HBM if i in far_out else on_chip(1)[0] for i in range(len(outs))]
    return pl.pallas_call(
        kernel,
        out_shape=[jax.ShapeDtypeStruct(shape, dtype) for shape, dtype in outs],
        in_specs=specs, out_specs=out_specs, scratch_shapes=scratch, input_output_aliases=aliases,
        cost_estimate=pl.CostEstimate(flops=flops, bytes_accessed=flops // CHUNK, transcendentals=0),
        compiler_params=pltpu.CompilerParams(collective_id=ident, has_side_effects=True, vmem_limit_bytes=VMEM_CAP),
        name=kernel.func.__name__ if isinstance(kernel, functools.partial) else kernel.__name__,
    )


def fetch_all(sem, *pairs):
    copies = [pltpu.make_async_copy(src, dst, sem.at[i]) for i, (src, dst) in enumerate(pairs)]
    for copy in copies:
        copy.start()
    return copies


def gain_row(dst, small_all, which):
    for o in range(N_DEV):
        dst[:1, o * LANE:(o + 1) * LANE] = small_all[o, which:which + 1, :]


def norm_rows(src, gain, dst):
    def step(i):
        rs = seg(i, STRIP)
        t = src[rs, :].astype(F32)
        dst[rs, :] = (t * lax.rsqrt(jnp.mean(t * t, axis=-1, keepdims=True) + NORM_EPS) * gain[:1, :]).astype(BF16)
    loop(src.shape[0] // STRIP, step)


def norm_back(dy, src, gain, skip, dst, dgain):
    def step(i):
        rs = seg(i, STRIP)
        d = dy[rs, :].astype(BF16).astype(F32)
        t = src[rs, :].astype(F32)
        inv = lax.rsqrt(jnp.mean(t * t, axis=-1, keepdims=True) + NORM_EPS)
        gd = gain[:1, :] * d
        pull = jnp.mean(gd * t, axis=-1, keepdims=True)
        dst[rs, :] = (skip[rs, :].astype(F32) + (inv * gd - t * (inv * inv * inv * pull))).astype(BF16)
        g = d * (t * inv)
        dgain[...] += g[:N_CHIP] + g[N_CHIP:]
    dgain[...] = jnp.zeros_like(dgain)
    loop(src.shape[0] // STRIP, step)


QB = 256
KB = 256


def key_rows(dst, src, lo, hd):
    def step(i):
        dst[seg(i, KB), :] = src[lo:lo + hd, seg(i, KB)].T
    loop(src.shape[1] // KB, step)


def score_block(k, q2, scale, diagonal):
    s = mm(k, q2, NN) * scale
    if diagonal:
        key = lax.broadcasted_iota(jnp.int32, s.shape, 0)
        qry = lax.broadcasted_iota(jnp.int32, s.shape, 1) % QB
        s = jnp.where(qry >= key, s, NEG_LARGE)
    return s


def side_by_side(ref, heads, hd, qs):
    return jnp.concatenate([ref[h * hd:(h + 1) * hd, qs] for h in range(heads)], axis=1)


def head(groups, hd, x_ref, g1_ref, g2_ref, pos_ref, wq_ref, wk_ref, wv_ref, freq_ref, wg_ref, wu_ref, wo_ref, qkv_ref, u_scr, small_all, w_out, o_ref, stat_ref, wgu_ref, h_ref, m_ref, cos_ref, sin_ref,
         full_w, acc_o, o_tok, o_send, small_ref, w_ref, full, acc, rot, g_scr, wg_t, wu_t, s_scr, k_scr, osem, *sems):
    me = lax.axis_index('sp')
    tokens, dim = x_ref.shape
    cols = w_ref.shape[0]
    small_ref[...] = jnp.concatenate([r[...].astype(F32) for r in (g1_ref, g2_ref, pos_ref)] + [jnp.zeros((N_CHIP - 3, LANE), F32)], axis=0)
    w_ref[:wq_ref.shape[0], :] = wq_ref[...]
    for k in range(groups):
        for i, ref in enumerate((wk_ref, wv_ref)):
            w_ref[pl.ds(wq_ref.shape[0] + (2 * k + i) * hd, hd), :] = ref[k * hd:(k + 1) * hd, :]
    qw = tokens
    q_all = N_DEV * qw
    gsems, ssems, qsems, ksems, gate_sems, up_sems, osems = sems[:4], *(sems[i:i + 2] for i in range(4, len(sems) - 4, 2))
    gw = row_gather(wo_ref, full_w, sems[-4:], me, 1)
    feat = wg_ref.shape[1] // N_DEV
    enter(me, OTHERS)
    smalls = Swap(lambda peer: small_ref, lambda o: small_all.at[o], ssems, me)
    smalls.start()
    parts = thirds(cols, STRIP)
    g = Gather(w_ref, lambda o: full.at[o // 2, :, seg(o % 2)], lambda view, c: [view.at[pl.ds(*parts[c]), :]], gsems, me)
    g.start()
    gates = Swap(lambda peer: wg_t.at[seg(peer, feat), :], lambda o: wgu_ref.at[:feat, seg(o)], gate_sems, me)
    ups = Swap(lambda peer: wu_t.at[seg(peer, feat), :], lambda o: wgu_ref.at[feat:, seg(o)], up_sems, me)

    def advance(n):
        gates.advance(n)
        ups.advance(n)

    def transpose(i):
        wg_t[seg(i, CHUNK), :] = wg_ref[:, seg(i, CHUNK)].T
        wu_t[seg(i, CHUNK), :] = wu_ref[:, seg(i, CHUNK)].T
    loop(wg_ref.shape[1] // CHUNK, transpose)
    advance(0)

    def own_block(i):
        full[me // 2, seg(i, WIDE), seg(me % 2)] = w_ref[seg(i, WIDE), :]
    loop(cols // WIDE, own_block)
    acc[...] = jnp.zeros_like(acc)
    small_all[me] = small_ref[...]
    smalls.wait_recv()
    gain_row(g_scr, small_all, 0)
    norm_rows(x_ref, g_scr, u_scr)

    def keep(mask):
        chip = flipped(me, mask) // 2
        return pltpu.make_async_copy(full.at[chip], w_out.at[chip], osem.at[mask // 2])

    def use(mask):
        g.wait_pair(mask)
        keep(mask).start()
        chip = flipped(me, mask) // 2
        u = u_scr[:, seg(chip, WIDE)]

        def step(i):
            rs = seg(i, cols // 2)
            acc[rs, :] += mm(full[chip, rs, :], u, NT)
        loop(2, step)

    def tables(o):
        angles = freq_ref[...] * small_all[o, 2:3, :]
        cos_ref[:, seg(o)] = jnp.cos(angles)
        sin_ref[:, seg(o)] = jnp.sin(angles)

    for r in range(len(g.ROUNDS)):
        g.round(r)
        if r in (2, 4):
            advance(r // 2)
        if r == 1:
            loop(N_DEV, tables)
        for mask in g.READY[r]:
            use(mask)

    half = hd // 2
    cos, sin = cos_ref[:, seg(me)], sin_ref[:, seg(me)]

    def turn(h):
        first = seg(2 * h, half)
        second = seg(2 * h + 1, half)
        p = acc[first, :].astype(BF16).astype(F32)
        q = acc[second, :].astype(BF16).astype(F32)
        rot[first, :] = (p * cos - q * sin).astype(BF16)
        rot[second, :] = (q * cos + p * sin).astype(BF16)
    loop(q_all // hd, turn)
    for k in range(groups):
        turn(q_all // hd + 2 * k)
        vs = seg(q_all // hd + 2 * k + 1, hd)
        rot[vs, :] = acc[vs, :].astype(BF16)
    per = N_DEV // groups
    q_rows = lambda peer: seg(peer, qw)
    kv_rows = lambda peer: seg(q_all // (2 * hd) + peer // per, 2 * hd)
    qs = Swap(lambda peer: rot.at[q_rows(peer), :], lambda o: qkv_ref.at[:qw, seg(o, tokens)], qsems, me)
    kvs = Swap(lambda peer: rot.at[kv_rows(peer), :], lambda o: qkv_ref.at[qw:, seg(o, tokens)], ksems, me)
    qs.start()
    kvs.start()
    gw.start()
    keep_own(wo_ref, full_w, me)
    gain_row(g_scr, small_all, 1)
    qkv_ref[:qw, seg(me, tokens)] = rot[q_rows(me), :]
    qkv_ref[qw:, seg(me, tokens)] = rot[kv_rows(me), :]
    wgu_ref[:feat, seg(me)] = wg_t[seg(me, feat), :]
    wgu_ref[feat:, seg(me)] = wu_t[seg(me, feat), :]
    gates.start((CORE,))
    ups.start((CORE,))
    for swap in (qs, kvs):
        swap.wait_recv()
    heads = qkv_ref.shape[0] // hd - 2
    seq = qkv_ref.shape[1]
    scale = hd ** -0.5
    lanes = heads * QB
    key_rows(k_scr, qkv_ref, qw, hd)

    outs = Swap(lambda peer: o_send.at[seg(peer), :], lambda o: o_tok.at[:, seg(o)], osems, me)

    def q_block(qb):
        for at, r in ((2, 0), (4, 1), (5, 2), (6, 3), (7, 4)):
            @pl.when(qb == at)
            def _():
                gw.round(r)
        qs = seg(qb, QB)
        q2 = side_by_side(qkv_ref, heads, hd, qs)

        def scores(kb, top, diagonal):
            s = score_block(k_scr[seg(kb, KB), :], q2, scale, diagonal)
            s_scr[seg(kb, KB), :] = s
            return jnp.maximum(top, jnp.max(s, axis=0, keepdims=True))

        top = lax.fori_loop(0, qb, lambda kb, t: scores(kb, t, False), jnp.full((1, lanes), NEG_LARGE, F32))
        top = scores(qb, top, True)

        def expo(kb, tot):
            e = jnp.exp(s_scr[seg(kb, KB), :] - top)
            s_scr[seg(kb, KB), :] = e
            return tot + jnp.sum(e, axis=0, keepdims=True)

        inv = 1.0 / lax.fori_loop(0, qb + 1, expo, jnp.zeros((1, lanes), F32))

        def weigh(kb, acc):
            p = (s_scr[seg(kb, KB), :] * inv).astype(BF16)
            return acc + mm(qkv_ref[qw + hd:, seg(kb, KB)], p, NN)

        acc = lax.fori_loop(0, qb + 1, weigh, jnp.zeros((hd, lanes), F32))
        for h in range(heads):
            o_ref[h * hd:(h + 1) * hd, qs] = acc[:, h * QB:(h + 1) * QB].astype(BF16)
        stat_ref[qb, :1, :] = top
        stat_ref[qb, 1:, :] = inv
        o_send[qs, :] = o_ref[:, qs].T

    loop(seq // QB, q_block)
    outs.start()
    advance(3)
    o_tok[:, seg(me)] = o_send[seg(me), :]
    for r in (5, 6):
        gw.round(r)
    outs.wait_recv()
    for mask in CHIP_MASKS:
        gw.wait_pair(mask)

    def project(n):
        cs = seg(n, CHUNK)
        acc_o[:, cs] = mm(o_tok[...], full_w[:, :, cs].reshape(dim, CHUNK), NN)
    loop(dim // CHUNK, project)

    def residual(i):
        rs = seg(i, STRIP)
        h_ref[rs, :] = (x_ref[rs, :].astype(F32) + acc_o[rs, :]).astype(BF16)
    loop(tokens // STRIP, residual)
    norm_rows(h_ref, g_scr, m_ref)
    for swap in (gates, ups):
        swap.wait_recv()
    for mask in CHIP_MASKS:
        keep(mask).wait()
    outs.wait_send()
    for swap in (gates, ups):
        swap.wait_send((CORE,) + SETS[3])
    g.finish()
    gw.finish()
    for swap in (smalls, qs, kvs):
        swap.wait_send()


def dw_swap(stage, dw_hbm, sems, me):
    return Swap(lambda peer: stage(peer).at[:, seg(peer % 2)], lambda o: dw_hbm.at[o], sems, me)


def mlp(m_ref, dout_ref, wgu_hbm, down_hbm, u_ref, h_ref, small_all, wo_ref, o_ref,
        ucol_ref, m_out, dgu_out, ddown_out, y_ref, dh_ref, do_ref, dwo_ref, dg_ref, dw_hbm,
        wgu_ref, down_ref, glu_ref, dgu_ref, ddown_ref, isem, dsem, full_d, full_m, osem, stage, g_scr, dgu_t, glu_t, free, *scr):
    me = lax.axis_index('sp')
    feat, dim = down_ref.shape
    loads = fetch_all(isem, (wgu_hbm, wgu_ref), (down_hbm, down_ref))
    enter(me, OTHERS)
    sems = scr[4:]
    gd = row_gather(dout_ref, full_d, sems[:4], me, 0)
    gm = row_gather(m_ref, full_m, sems[4:8], me, 2)
    g = row_gather(dh_ref, full_d, sems[8:12], me, 1)
    ucols = Swap(lambda peer: u_ref.at[:, seg(peer)], lambda o: ucol_ref.at[seg(o), :], sems[12:14], me)
    def dw_part(mask):
        cols = full_m[:, :, seg(flipped(me, mask) // 2, WIDE)].reshape(dgu_ref.shape[1], WIDE)
        stage[...] = mm(dgu_ref[...], cols, NN)
        swap = dw_swap(lambda peer: stage, dw_hbm, sems[14:16], me)
        loop(2, lambda core: swap.copy(mask + core).start())

    gm.start()
    gd.start()
    ucol_ref[seg(me), :] = u_ref[:, seg(me)]
    keep_own(m_ref, full_m, me)
    keep_own(dout_ref, full_d, me)
    gain_row(g_scr, small_all, 1)
    dwo_ref[...] = jnp.zeros_like(dwo_ref)
    ddown_ref[...] = jnp.zeros_like(ddown_ref)

    def keep(mask):
        chip = flipped(me, mask) // 2
        ts = seg(chip, WIDE)
        ends = ((full_m.at[chip], m_out.at[chip]), (dgu_ref.at[:, ts], dgu_out.at[:, ts]))
        return [pltpu.make_async_copy(src, dst, osem.at[mask // 2, i]) for i, (src, dst) in enumerate(ends)]

    for load in loads:
        load.wait()

    def use(mask):
        gd.wait_pair(mask)
        gm.wait_pair(mask)
        chip = flipped(me, mask) // 2
        ts = seg(chip, WIDE)
        gu = mm(wgu_ref[...], full_m[chip], NT).astype(BF16).astype(F32)
        gate, up = gu[:feat], gu[feat:]
        d_glu = mm(down_ref[...], full_d[chip], NT).astype(BF16).astype(F32)
        sig = jax.nn.sigmoid(gate)
        act = gate * sig
        glu = (act * up).astype(BF16)
        glu_ref[:, ts] = glu
        dgu_ref[:feat, ts] = (d_glu * up * (sig * (1.0 + gate * (1.0 - sig)))).astype(BF16)
        dgu_ref[feat:, ts] = (d_glu * act).astype(BF16)

        def step(n):
            ddown_ref[:, seg(n, CHUNK)] += mm(glu, full_d[chip, :, seg(n, CHUNK)], NN)
        loop(dim // CHUNK, step)
        for copy in keep(mask):
            copy.start()

    for r in range(len(gm.ROUNDS)):
        gm.round(r)
        gd.round(r)
        if r == 3:
            ucols.start()
        for mask in gm.READY[r]:
            use(mask)
    dw_part(XYZ)
    for gather in (gd, gm):
        gather.finish()
    leave = pltpu.make_async_copy(ddown_ref, ddown_out, dsem)
    leave.start()
    s = Scatter(*scr[:4], sems[16:], me)
    total = s.run(block_product(s, dgu_ref, wgu_ref, dgu_t))
    for mask in NEAR:
        pl.semaphore_signal(free, inc=1, device_id=(flipped(me, mask),), device_id_type=MESH)
    norm_back(total, h_ref, g_scr, dout_ref, dh_ref, dg_ref)
    g.start()
    keep_own(dh_ref, full_d, me)
    s.finish()
    pl.semaphore_wait(free, len(NEAR))

    def use_dh(mask):
        g.wait_pair(mask)
        chip = flipped(me, mask) // 2
        do_ref[:, seg(chip, WIDE)] = mm(wo_ref[...], full_d[chip], NT).astype(BF16)
        o = o_ref[:, seg(chip, WIDE)]

        def step(n):
            dwo_ref[:, seg(n, CHUNK)] += mm(o, full_d[chip, :, seg(n, CHUNK)], NN)
        loop(dim // CHUNK, step)

    def between(i):
        if i < len(g.ROUNDS):
            g.round(i)
            for mask in g.READY[i]:
                use_dh(mask)

    s = Scatter(*scr[:4], sems[16:], me)
    total = s.run(block_product(s, glu_ref, down_ref, glu_t), between)
    y_ref[...] = (h_ref[...].astype(F32) + total[...]).astype(BF16)
    s.finish()
    g.finish()
    swap = dw_swap(lambda peer: stage, dw_hbm, sems[14:16], me)
    loop(2, lambda core: (swap.arrival(XYZ + core).wait_recv(), swap.copy(XYZ + core).wait_send()))
    ucols.wait_recv()
    ucols.wait_send()
    leave.wait()
    loop(N_CHIP, lambda j: [pltpu.make_async_copy(src, dst, osem.at[j, i]).wait() for i, (src, dst) in enumerate(
        ((full_m.at[0], m_out.at[0]), (dgu_ref.at[:, seg(0, WIDE)], dgu_out.at[:, seg(0, WIDE)])))])


def back(groups, hd, qkv_ref, do_ref, stat_ref, cos_all, sin_all, dgu_ref, m_hbm, ucol_ref, w_hbm, x_ref, small_all, dh_ref, dg2_ref, dw_in,
         dw_hbm, dwq_ref, dwkv_ref, dx_ref, gain_ref,
         p_scr, dp_scr, k_scr, v_scr, dk_acc, dv_acc, stage, dq_scr, dkv_scr, m_scr,
         full, w_scr, shares, dkv_own, full_kv, dqkv, dn, g_scr, dg1, gains, gains_in, wsem, lsem, msem, *sems):
    heads = qkv_ref.shape[0] // hd - 2
    seq = qkv_ref.shape[1]
    scale = hd ** -0.5
    lanes = heads * QB
    qw = heads * hd
    half = hd // 2
    me = lax.axis_index('sp')
    feat = dgu_ref.shape[0] // 2
    first = (X, Y + Z, Y, X + Z, Z, X + Y, 0)

    def fetch(mask):
        cols = seg(flipped(me, mask) // 2, WIDE)
        return pltpu.make_async_copy(m_hbm.at[:, :, cols], m_scr.at[:, :, cols], msem.at[mask // 2])
    for mask in first:
        fetch(mask).start()
    load = pltpu.make_async_copy(w_hbm, w_scr, wsem)
    load.start()
    enter(me, OTHERS)
    gain_row(g_scr, small_all, 0)

    dws = dw_swap(lambda peer: stage.at[peer // 2], dw_hbm, sems[:2], me)
    gq = row_gather(dq_scr, full, sems[4:8], me)
    own = pltpu.make_async_copy(dws.src(me), dws.dst(me), lsem)

    def make(mask):
        chip = flipped(me, mask) // 2
        fetch(mask).wait()
        cols = m_scr[:, :, seg(chip, WIDE)].reshape(seq, WIDE)
        stage[chip] = mm(dgu_ref[...], cols, NN)

    def advance(n):
        if n > 1:
            dws.wait_send(SETS[n - 1])
        dws.start(SETS[n])

    for i, mask in enumerate(first[:4]):
        make(mask)
        if i == 1:
            advance(1)

    dk_acc[...] = jnp.zeros_like(dk_acc)
    dv_acc[...] = jnp.zeros_like(dv_acc)
    key_rows(k_scr, qkv_ref, qw, hd)
    key_rows(v_scr, qkv_ref, qw + hd, hd)

    def q_block(qb):
        @pl.when(qb == 5)
        def _():
            advance(2)
        qs = seg(qb, QB)
        q2 = side_by_side(qkv_ref, heads, hd, qs)
        do2 = side_by_side(do_ref, heads, hd, qs)
        top = stat_ref[qb, :1, :]
        inv = stat_ref[qb, 1:, :]

        def probs(kb, rd, diagonal):
            ks = seg(kb, KB)
            s = score_block(k_scr[ks, :], q2, scale, diagonal)
            p = jnp.exp(s - top) * inv
            dp = mm(v_scr[ks, :], do2, NN).astype(BF16)
            p_scr[ks, :] = p
            dp_scr[ks, :] = dp
            dv_acc[ks, :] += mm(p.astype(BF16), do2, NT)
            return rd + jnp.sum(dp.astype(F32) * p, axis=0, keepdims=True)

        rd = lax.fori_loop(0, qb, lambda kb, r: probs(kb, r, False), jnp.zeros((1, lanes), F32))
        rd = probs(qb, rd, True)

        def d_scores(kb, acc):
            ks = seg(kb, KB)
            ds = (p_scr[ks, :] * (dp_scr[ks, :].astype(F32) - rd) * scale).astype(BF16)
            dk_acc[ks, :] += mm(ds, q2, NT)
            return acc + mm(qkv_ref[qw:qw + hd, ks], ds, NN)

        acc = lax.fori_loop(0, qb + 1, d_scores, jnp.zeros((hd, lanes), F32))
        cos, sin = cos_all[:, qs], sin_all[:, qs]
        for h in range(heads):
            dq = acc[:, h * QB:(h + 1) * QB].astype(BF16).astype(F32)
            p, q = dq[:half], dq[half:]
            dq_scr[h * hd:h * hd + half, qs] = (p * cos + q * sin).astype(BF16)
            dq_scr[h * hd + half:(h + 1) * hd, qs] = (q * cos - p * sin).astype(BF16)

    loop(seq // QB, q_block)

    def share(i):
        rs = seg(i, WIDE)
        dkv_scr[rs, :] = jnp.concatenate([dk_acc[rs, :], dv_acc[rs, :]], axis=1).astype(BF16)
    loop(seq // WIDE, share)
    tokens = ucol_ref.shape[1]
    per = N_DEV // groups
    q_all = dwq_ref.shape[0]
    sh = Swap(lambda peer: dkv_scr.at[seg(peer, tokens), :], lambda o: shares.at[o], sems[2:4], me)
    parts = thirds(dkv_own.shape[0], STRIP)
    gk = Gather(dkv_own, lambda o: full_kv.at[:, seg(o, tokens)], lambda view, c: [view.at[pl.ds(*parts[c]), :]], sems[8:12], me)
    gs = Swap(lambda peer: gains.at[:, seg(peer)], lambda o: gains_in.at[o], sems[12:], me)
    sh.start()
    gq.start()
    for mask in first[4:]:
        make(mask)
    dws.start((CORE,))
    own.start()
    keep_own(dq_scr, full, me)
    shares[me] = dkv_scr[seg(me, tokens), :]
    sh.wait_recv()
    cos, sin = cos_all[:, seg(me)], sin_all[:, seg(me)]
    for k in range(groups):
        both = sum(shares[per * k + i].astype(F32) for i in range(per)).astype(BF16).astype(F32).T
        p, q = both[:half], both[half:hd]
        lo = 2 * hd * k
        dkv_own[lo:lo + half, :] = (p * cos + q * sin).astype(BF16)
        dkv_own[lo + half:lo + hd, :] = (q * cos - p * sin).astype(BF16)
        dkv_own[lo + hd:lo + 2 * hd, :] = both[hd:].astype(BF16)
    gk.start()
    full_kv[:, seg(me, tokens)] = dkv_own[...]
    for k in range(groups):
        dqkv[:, q_all + 2 * hd * k:q_all + 2 * hd * (k + 1)] = dkv_own[2 * hd * k:2 * hd * (k + 1), :].T

    def spread(cols):
        part = dqkv[:, cols]

        def step(i):
            dn[:, seg(i, WIDE)] += mm(part, w_scr[i, cols, :], NN)
        loop(N_CHIP, step)

    def use(mask):
        gq.wait_pair(mask)
        chip = flipped(me, mask) // 2
        dwq_ref[seg(chip, WIDE), :] = mm(full[chip], ucol_ref[...], NN)
        dqkv[:, seg(chip, WIDE)] = full[chip, :, seg(me, tokens)].T
        spread(seg(chip, WIDE))

    load.wait()
    dn[...] = jnp.zeros_like(dn)
    spread(pl.ds(q_all, dqkv.shape[1] - q_all))
    for r in range(len(gq.ROUNDS)):
        gq.round(r)
        if r == 3:
            advance(3)
            for i in range(4):
                gk.round(i)
        if r > 3:
            gk.round(r)
        for mask in gq.READY[r]:
            use(mask)
    norm_back(dn, x_ref, g_scr, dh_ref, dx_ref, dg1)
    gains[...] = jnp.concatenate([jnp.sum(dg1[...], axis=0, keepdims=True), jnp.sum(dg2_ref[...], axis=0, keepdims=True),
                                  jnp.zeros((N_CHIP - 2, dg1.shape[1]), F32)], axis=0)
    gs.start()
    gains_in[me] = gains[:, seg(me)]
    for mask in CHIP_MASKS:
        gk.wait_pair(mask)
    dwkv_ref[...] = mm(full_kv[...], ucol_ref[...], NN)
    gs.wait_recv()
    gain_ref[...] = sum(gains_in[o] for o in range(N_DEV))
    dws.wait_recv((CORE,) + SETS[1] + SETS[2] + SETS[3])
    dws.wait_send((CORE,) + SETS[3])
    own.wait()
    for c in (sh, gs):
        c.wait_send()
    for g in (gq, gk):
        g.finish()


def finish(dw_hbm, dkv_hbm, *refs):
    n = (len(refs) - 11) // 3
    srcs, (gate, up, dk, dv), dsts = refs[:n], refs[n:n + 4], refs[n + 4:2 * n + 4]
    (g_in, g_out, kv_in), holds, sems = refs[2 * n + 4:2 * n + 7], refs[2 * n + 7:3 * n + 7], refs[3 * n + 7:]
    t_in, t_out, p_in, p_out = sems
    feat = g_in.shape[2]
    four = N_DEV // 4
    step = four * feat
    hd = dk.shape[0] // (kv_in.shape[0] // LANE)
    starts = [(w, i) for i in range(4) for w in range(2)]

    def fetch(w, i):
        at = pl.ds(i * four, four)
        return pltpu.make_async_copy(dw_hbm.at[at, pl.ds(w * feat, feat), :], g_in.at[w, at], t_in.at[w, i])

    def put(w, i):
        cs = pl.ds(i * step, step)
        return pltpu.make_async_copy(g_out.at[w, :, cs], (gate, up)[w].at[:, cs], t_out.at[w, i])
    moves = [(pltpu.make_async_copy(a, h, p_in.at[k]), pltpu.make_async_copy(h, b, p_out.at[k])) for k, (a, h, b) in enumerate(zip(srcs, holds, dsts))]
    kv = pltpu.make_async_copy(dkv_hbm, kv_in, p_in.at[n])
    for w, i in starts:
        fetch(w, i).start()
    kv.start()
    for k, (w, i) in enumerate(starts):
        fetch(w, i).wait()
        if k < len(moves):
            moves[k][0].start()

        g_out[w, :, pl.ds(i * step, step)] = g_in[w, pl.ds(i * four, four)].reshape(step, LANE).T
        put(w, i).start()
    kv.wait()
    for k in range(dk.shape[0] // hd):
        for i, ref in enumerate((dk, dv)):
            ref[k * hd:(k + 1) * hd, :] = kv_in[(2 * k + i) * hd:(2 * k + i + 1) * hd, :]
    for load, store in moves:
        load.wait()
        store.start()
    for w, i in starts:
        put(w, i).wait()
    for _, store in moves:
        store.wait()


def solution(mesh):
    assert mesh.shape['sp'] == N_DEV

    def layer_step(x_in, positions, d_out, norm1_gain, norm2_gain, w_q, w_k, w_v, w_o, w_gate, w_up, w_down):
        tokens, dim = x_in.shape
        seq = tokens * N_DEV
        n_q, hd = w_q.shape[1:]
        n_kv = w_k.shape[1]
        qw = n_q // N_DEV * hd
        rows = w_q.shape[0]
        feat = w_down.shape[0]
        cols = (n_q + 2 * n_kv) * hd
        lanes = qw // hd * QB
        vm = pltpu.VMEM
        full = vm((N_CHIP, WIDE, dim), BF16)
        gain_scr = vm((N_CHIP, dim), F32)
        tok_shapes = 2 * (((tokens, dim), BF16),)
        dw_shape = ((N_DEV, 2 * feat, rows), F32)

        inv_freq = 1.0 / (ROPE_BASE ** (jnp.arange(hd // 2, dtype=F32) * (2.0 / hd)))
        freq = jnp.broadcast_to(inv_freq[:, None], (hd // 2, rows))
        row = lambda v: v.reshape(1, rows)
        by_head = lambda w: w.transpose(1, 2, 0).reshape(-1, rows)
        wo_own = w_o.reshape(qw, dim)

        args = (x_in, row(norm1_gain), row(norm2_gain), row(positions), by_head(w_q), by_head(w_k), by_head(w_v), freq, w_gate, w_up, wo_own)
        qkv, u, small_all, wqkv, attn_t, stat, wgu, hidden, mlp_in, cos_all, sin_all = call(
            functools.partial(head, n_kv, hd), 0, len(args),
            (((qw + 2 * hd, seq), BF16), tok_shapes[0], ((N_DEV, N_CHIP, rows), F32), ((N_CHIP, cols, WIDE), BF16),
             ((qw, seq), BF16), ((seq // QB, 2, lanes), F32), ((2 * feat, dim), BF16), *tok_shapes, *(2 * (((hd // 2, seq), F32),))),
            [full, vm((tokens, dim), F32), vm((tokens, dim), BF16), vm((seq, qw), BF16),
             vm((N_CHIP, rows), F32), vm((cols, rows), BF16), vm((N_CHIP, cols, WIDE), BF16), vm((cols, tokens), F32), vm((cols, tokens), BF16), gain_scr,
             vm((feat * N_DEV, rows), BF16), vm((feat * N_DEV, rows), BF16), vm((seq, lanes), F32), vm((seq, hd), BF16), dma(N_CHIP),
             *Gather.sems, *(6 * Swap.sems), *Gather.sems], 4 * qw * seq * seq, far_out=(3,))(*args)
        args = (mlp_in, d_out, wgu, w_down, u, hidden, small_all, wo_own, attn_t)
        u_col, m_full, dgu, d_down, y_out, d_hidden, d_attn, d_wo, d_g2, d_gu = call(
            mlp, 1, len(args),
            (((seq, rows), BF16), ((N_CHIP, WIDE, dim), BF16), ((2 * feat, seq), BF16), ((feat, dim), F32),
             *tok_shapes, ((qw, seq), BF16), ((qw, dim), F32), ((N_CHIP, dim), F32), dw_shape),
            [vm((2 * feat, dim), BF16), vm((feat, dim), BF16), vm((feat, seq), BF16), vm((2 * feat, seq), BF16), vm((feat, dim), F32), dma(2), dma(),
             full, full, dma(N_CHIP, 2), vm((2 * feat, WIDE), F32), gain_scr, vm((WIDE, 2 * feat), BF16), vm((WIDE, feat), BF16), pltpu.SemaphoreType.REGULAR,
             *Scatter.scratch(tokens, dim), *(3 * Gather.sems), *(2 * Swap.sems), *Scatter.sems], 12 * feat * seq * dim,
            far_in=(2, 3), far_out=(1, 2, 3, 9))(*args)
        args = (qkv, d_attn, stat, cos_all, sin_all, dgu, m_full, u_col, wqkv, x_in, small_all, d_hidden, d_g2, d_gu)
        d_gu, d_wq, d_wkv, d_x, gains = call(
            functools.partial(back, n_kv, hd), 3, len(args),
            (dw_shape, ((n_q * hd, rows), F32), ((2 * n_kv * hd, rows), F32), tok_shapes[0], ((N_CHIP, rows), F32)),
            [vm((seq, lanes), F32), vm((seq, lanes), BF16), vm((seq, hd), BF16), vm((seq, hd), BF16), vm((seq, hd), F32), vm((seq, hd), F32),
             vm((N_CHIP, 2 * feat, WIDE), F32), vm((qw, seq), BF16), vm((seq, 2 * hd), BF16), full,
             full, vm((N_CHIP, cols, WIDE), BF16), vm((N_DEV, tokens, 2 * hd), BF16), vm((2 * n_kv * hd, tokens), BF16), vm((2 * n_kv * hd, seq), BF16),
             vm((tokens, cols), BF16), vm((tokens, dim), F32), gain_scr, gain_scr, gain_scr, vm((N_DEV, N_CHIP, rows), F32), dma(), dma(), dma(N_CHIP),
             *(2 * Swap.sems), *(2 * Gather.sems), *Swap.sems], 10 * qw * seq * seq, far_in=(6, 8, 13), far_out=(0,), aliases={13: 0})(*args)
        moved = (d_wq, d_wo, d_down, d_x, y_out, gains)
        half_kv = jax.ShapeDtypeStruct((n_kv * hd, rows), F32)
        wide = jax.ShapeDtypeStruct((rows, feat * N_DEV), F32)
        d_gate, d_up, d_wk, d_wv, d_wq, d_wo, d_down, d_x, y_out, gains = pl.pallas_call(
            finish,
            out_shape=[wide, wide, half_kv, half_kv] + [jax.ShapeDtypeStruct(v.shape, v.dtype) for v in moved],
            in_specs=[IN_HBM] * (2 + len(moved)), out_specs=[IN_HBM] * 2 + on_chip(2) + [IN_HBM] * len(moved),
            scratch_shapes=[vm((2, N_DEV, feat, rows), F32), vm((2, rows, feat * N_DEV), F32), vm(d_wkv.shape, F32)]
            + [vm(v.shape, v.dtype) for v in moved] + [dma(2, 4), dma(2, 4), dma(len(moved) + 1), dma(len(moved))],
            compiler_params=pltpu.CompilerParams(vmem_limit_bytes=VMEM_CAP), name='finish',
        )(d_gu, d_wkv, *moved)
        by_row = lambda g, heads: g.reshape(heads, hd, rows).transpose(2, 0, 1)
        return (y_out, d_x, gains[0], gains[1], by_row(d_wq, n_q), by_row(d_wk, n_kv), by_row(d_wv, n_kv),
                d_wo.reshape(w_o.shape), d_gate, d_up, d_down)

    all_rows = P('sp')
    return jax.shard_map(layer_step, mesh=mesh, in_specs=(all_rows,) * 12, out_specs=(all_rows,) * 11, check_vma=False)
```

```python
import functools
import jax
import jax.numpy as jnp
from jax import lax
from jax.experimental import pallas as pl
from jax.experimental.pallas import tpu as pltpu
from jax.sharding import PartitionSpec as P

ROPE_BASE = 10000.0
NORM_EPS = 1e-5
NEG_LARGE = -1e30
F32 = jnp.float32
BF16 = jnp.bfloat16
N_DEV, N_CHIP, LANE, WIDE, CHUNK, STRIP = 16, 8, 128, 256, 512, 16
NT = (((1,), (1,)), ((), ()))
TN = (((0,), (0,)), ((), ()))
NN = (((1,), (0,)), ((), ()))
MESH = pl.DeviceIdType.MESH
VMEM_CAP = 62 * 1024 * 1024

CORE, X, Y, Z = 1, 2, 4, 8
XYZ = X + Y + Z
ORDERS = ((X, Y, Z), (Y, Z, X), (Z, X, Y))
CHIP_MASKS = (0, X, Y, Z, X + Y, X + Z, Y + Z, XYZ)
NEAR = (CORE, X, Y, Z)
OTHERS = range(1, N_DEV)
SETS = tuple(tuple(m + c for m in masks for c in (0, CORE)) for masks in ((XYZ,), (X, Y + Z), (Y, X + Z), (Z, X + Y)))
N_COL = len(ORDERS)
COLOURS = range(N_COL)


def mm(a, b, dims):
    return lax.dot_general(a, b, dims, preferred_element_type=F32)


def seg(index, width=LANE):
    return pl.ds(pl.multiple_of(index * width, width), width)


def loop(count, body):
    lax.fori_loop(0, count, lambda i, c: (body(i), c)[1], 0)


def differing(index, mask):
    return sum(((index // bit + mask // bit) % 2) * bit for bit in NEAR)


def flipped(index, mask):
    out = index
    for bit in NEAR:
        if mask & bit:
            out = out + (1 - 2 * ((index // bit) % 2)) * bit
    return out


def thirds(total, unit):
    n = total // unit
    first = (n + 2) // 3
    second = (n - first + 1) // 2
    sizes = (first * unit, second * unit, (n - first - second) * unit)
    return ((0, sizes[0]), (sizes[0], sizes[1]), (sizes[0] + sizes[1], sizes[2]))


def pieces(rows, cols, unit):
    share = cols // LANE // N_COL * LANE
    strips = thirds(rows, unit)
    rest = cols - N_COL * share
    return [[(pl.ds(0, rows), pl.ds(c * share, share)), (pl.ds(*strips[c]), pl.ds(N_COL * share, rest))] for c in COLOURS]


def enter(me, masks):
    barrier = pltpu.get_barrier_semaphore()
    for mask in masks:
        pl.semaphore_signal(barrier, inc=1, device_id=(flipped(me, mask),), device_id_type=MESH)
    pl.semaphore_wait(barrier, len(masks))


def remote(src, dst, send, recv, peer):
    return pltpu.make_async_remote_copy(src_ref=src, dst_ref=dst, send_sem=send, recv_sem=recv, device_id=(peer,), device_id_type=MESH)


def dma(*shape):
    return pltpu.SemaphoreType.DMA(shape)


class Swap:
    sems = (dma(N_DEV), dma(N_DEV))

    def __init__(self, src, dst, sems, me):
        self.src, self.dst, (self.send, self.recv), self.me = src, dst, sems, me

    def copy(self, mask):
        peer = differing(self.me, mask)
        return remote(self.src(peer), self.dst(self.me), self.send.at[mask], self.recv.at[mask], peer)

    def arrival(self, mask):
        view = self.dst(differing(self.me, mask))
        return remote(view, view, self.send.at[mask], self.recv.at[mask], self.me)

    def each(self, masks, act):
        if masks is None:
            loop(N_DEV - 1, lambda i: act(i + 1))
        else:
            for mask in masks:
                act(mask)

    def start(self, masks=None):
        self.each(masks, lambda mask: self.copy(mask).start())

    def advance(self, n):
        if n:
            self.wait_send(SETS[n - 1])
        self.start(SETS[n])

    def wait_recv(self, masks=None):
        self.each(masks, lambda mask: self.arrival(mask).wait_recv())

    def wait_send(self, masks=None):
        self.each(masks, lambda mask: self.copy(mask).wait_send())


class Gather:
    ROUNDS = ((0,), (1,), (2,), (0, 1), (0, 2), (1, 2), (0, 1, 2))
    READY = ((0,), (), (), (X, Y), (Z,), (X + Y, X + Z), (Y + Z, XYZ))
    sems = (dma(N_COL, N_CHIP, 2), dma(N_COL, N_CHIP, 2), dma(N_CHIP), dma(N_CHIP))

    def __init__(self, own, block, cut, sems, me):
        self.own, self.block, self.cut, self.me = own, block, cut, me
        self.send, self.recv, self.pair_send, self.pair_recv = sems

    def source(self, mask):
        return self.block(flipped(self.me, mask)) if mask else self.own

    def unit(self, colour, mask, axis):
        ends = zip(self.cut(self.source(mask), colour), self.cut(self.block(flipped(self.me, mask)), colour))
        j = self.sends(colour).index((mask, axis))
        return [remote(src, dst, self.send.at[colour, j, i], self.recv.at[colour, (mask + axis) // 2, i],
                       flipped(self.me, axis)) for i, (src, dst) in enumerate(ends)]

    def sends(self, colour):
        return [(0, axis) for axis in ORDERS[colour]] + [step[1:] for step in self.onward(colour)]

    def start_unit(self, colour, mask, axis):
        for copy in self.unit(colour, mask, axis):
            copy.start()

    def pair(self, mask):
        return remote(self.source(mask), self.block(flipped(self.me, mask)), self.pair_send.at[mask // 2],
                      self.pair_recv.at[mask // 2], flipped(self.me, CORE))

    def wait_pair(self, mask):
        view = self.block(flipped(self.me, mask + CORE))
        remote(view, view, self.pair_send.at[mask // 2], self.pair_recv.at[mask // 2], self.me).wait_recv()

    def onward(self, colour):
        order = ORDERS[colour]
        for picks in self.ROUNDS:
            for axis in order[picks[-1] + 1:]:
                yield picks, sum(order[p] for p in picks), axis

    def start(self):
        for pos in COLOURS:
            for colour in COLOURS:
                self.start_unit(colour, 0, ORDERS[colour][pos])
        self.pair(0).start()

    def round(self, r):
        for colour in COLOURS:
            mask = sum(ORDERS[colour][p] for p in self.ROUNDS[r])
            for i, view in enumerate(self.cut(self.block(flipped(self.me, mask)), colour)):
                remote(view, view, self.send.at[colour, 0, i], self.recv.at[colour, mask // 2, i], self.me).wait_recv()
            for picks, at, axis in self.onward(colour):
                if picks == self.ROUNDS[r]:
                    self.start_unit(colour, at, axis)
        for mask in {2: (X, Y, Z), 5: (X + Y, X + Z, Y + Z), 6: (XYZ,)}.get(r, ()):
            self.pair(mask).start()

    def finish(self):
        for colour in COLOURS:
            for i, view in enumerate(self.cut(self.own, colour)):
                loop(len(self.sends(colour)), lambda j: remote(view, view, self.send.at[colour, j, i], self.recv.at[colour, j, i], self.me).wait_send())
        loop(N_CHIP, lambda j: remote(self.own, self.own, self.pair_send.at[j], self.pair_recv.at[j], self.me).wait_send())


def row_gather(own, full, sems, me, extra=None):
    rows, width = own.shape
    parts = pieces(rows, width, STRIP)
    if extra is not None:
        share = width // LANE // N_COL * LANE
        more = width - N_COL * share
        parts = [[(pl.ds(0, rows), pl.ds(c * share + more * (c > extra), share + more * (c == extra)))] for c in COLOURS]

    def block(o):
        return full.at[o // 2, seg(o % 2), :]

    return Gather(own, block, lambda view, c: [view.at[rs, cs] for rs, cs in parts[c]], sems, me)


def keep_own(own, full, me):
    def step(i):
        full[me // 2, pl.ds(pl.multiple_of((me % 2) * LANE + i * STRIP, STRIP), STRIP), :] = own[seg(i, STRIP), :]
    loop(LANE // STRIP, step)


class Scatter:
    ORDER = (XYZ, X + Y, Y + Z, X + Z, X, Y, Z, 0)
    sems = (dma(N_CHIP), dma(N_CHIP), dma(N_COL, N_CHIP, 2), dma(N_COL, N_CHIP, 2))

    @staticmethod
    def scratch(tokens, dim):
        return [pltpu.VMEM((n, tokens, dim), F32) for n in (N_CHIP, 2, N_CHIP, N_CHIP - 1)]

    def __init__(self, part, other, pair_in, link_in, sems, me):
        self.part, self.other, self.pair_in, self.link_in, self.me = part, other, pair_in, link_in, me
        self.pair_send, self.pair_recv, self.link_send, self.link_recv = sems
        self.tokens, self.dim = part.shape[1:]
        self.pieces = pieces(self.tokens, self.dim, STRIP // 2)
        self.ready, self.sent = set(), [0] * N_COL

    @staticmethod
    def first(colour, mask):
        return next((i for i, a in enumerate(ORDERS[colour]) if mask & a), 3)

    def slot(self, colour, mask, axis):
        slots = [(m, a) for m in self.ORDER for a in ORDERS[colour][:self.first(colour, m)]]
        return slots.index((mask, axis))

    def pair(self, i):
        return remote(self.other.at[i % 2], self.pair_in.at[i], self.pair_send.at[i], self.pair_recv.at[i], flipped(self.me, CORE))

    def link(self, colour, mask):
        axis = ORDERS[colour][self.first(colour, mask)]
        slot = self.slot(colour, mask - axis, axis)
        i = self.ORDER.index(mask)
        return [remote(self.part.at[i, rs, cs], self.link_in.at[slot, rs, cs], self.link_send.at[colour, i, k],
                       self.link_recv.at[colour, slot, k], flipped(self.me, axis)) for k, (rs, cs) in enumerate(self.pieces[colour])]

    def start_link(self, colour, mask):
        for copy in self.link(colour, mask):
            copy.start()

    def add(self, mask, ref, cs):
        i = self.ORDER.index(mask)

        def step(r):
            rs = seg(r, STRIP)
            self.part[i, rs, cs] += ref[rs, cs]
        loop(self.tokens // STRIP, step)

    def finish_pair(self, i):
        self.pair(i).wait_recv()
        self.add(self.ORDER[i], self.pair_in.at[i], pl.ds(0, self.dim))
        self.ready.add(self.ORDER[i])
        for colour in COLOURS:
            a, b, c = ORDERS[colour]
            todo = (XYZ, a + b, a + c, a)
            while self.sent[colour] < len(todo) and todo[self.sent[colour]] in self.ready:
                self.start_link(colour, todo[self.sent[colour]])
                self.sent[colour] += 1

    def take(self, colour, mask, axis):
        for copy in self.link(colour, mask + axis):
            copy.wait_recv()
        ref = self.link_in.at[self.slot(colour, mask, axis)]
        (_, wide), (rs, cs) = self.pieces[colour]
        self.add(mask, ref, wide)
        self.part[self.ORDER.index(mask), rs, cs] += ref[rs, cs]

    def run(self, product, between=lambda i: None):
        for i, mask in enumerate(self.ORDER):
            if i > 1:
                self.pair(i - 2).wait_send()
            product(i, flipped(self.me, mask) // 2)
            self.pair(i).start()
            if i:
                self.finish_pair(i - 1)
            between(i)
        self.finish_pair(N_CHIP - 1)
        for step in range(2):
            between(N_CHIP + step)
            for colour in COLOURS:
                a, b, c = ORDERS[colour]
                mask = (b + c, b)[step]
                self.take(colour, mask, a)
                self.start_link(colour, mask)
        between(N_CHIP + 2)
        for colour in COLOURS:
            a, b, c = ORDERS[colour]
            self.take(colour, c, a)
            self.take(colour, c, b)
            self.start_link(colour, c)
        between(N_CHIP + 3)
        for colour in COLOURS:
            for axis in ORDERS[colour]:
                self.take(colour, 0, axis)
        return self.part.at[N_CHIP - 1]

    def finish(self):
        for i in (N_CHIP - 2, N_CHIP - 1):
            self.pair(i).wait_send()
        for colour in COLOURS:
            for k, (rs, cs) in enumerate(self.pieces[colour]):
                view = self.part.at[0, rs, cs]
                loop(N_CHIP - 1, lambda i: remote(view, view, self.link_send.at[colour, i, k], self.link_recv.at[colour, i, k], self.me).wait_send())


def block_product(s, a_ref, w_ref, a_t):
    core = s.me % 2

    def product(i, chip):
        a_t[...] = a_ref[:, seg(chip, WIDE)].T

        def step(n):
            cs = seg(n, CHUNK)
            s.other[i % 2, :, cs] = mm(a_t[seg(1 - core), :], w_ref[:, cs], NN)
            s.part[i, :, cs] = mm(a_t[seg(core), :], w_ref[:, cs], NN)
        loop(s.dim // CHUNK, step)
    return product


def on_chip(n):
    return [pl.BlockSpec(memory_space=pltpu.VMEM)] * n


IN_HBM = pl.BlockSpec(memory_space=pl.ANY)


def call(kernel, ident, args, outs, scratch, flops, far_in=(), far_out=(), aliases={}):
    specs = [IN_HBM if i in far_in else on_chip(1)[0] for i in range(args)]
    out_specs = [IN_HBM if i in far_out else on_chip(1)[0] for i in range(len(outs))]
    return pl.pallas_call(
        kernel,
        out_shape=[jax.ShapeDtypeStruct(shape, dtype) for shape, dtype in outs],
        in_specs=specs, out_specs=out_specs, scratch_shapes=scratch, input_output_aliases=aliases,
        cost_estimate=pl.CostEstimate(flops=flops, bytes_accessed=flops // CHUNK, transcendentals=0),
        compiler_params=pltpu.CompilerParams(collective_id=ident, has_side_effects=True, vmem_limit_bytes=VMEM_CAP),
        name=kernel.func.__name__ if isinstance(kernel, functools.partial) else kernel.__name__,
    )


def fetch_all(sem, *pairs):
    copies = [pltpu.make_async_copy(src, dst, sem.at[i]) for i, (src, dst) in enumerate(pairs)]
    for copy in copies:
        copy.start()
    return copies


def gain_row(dst, small_all, which):
    for o in range(N_DEV):
        dst[:1, o * LANE:(o + 1) * LANE] = small_all[o, which:which + 1, :]


def norm_rows(src, gain, dst):
    def step(i):
        rs = seg(i, STRIP)
        t = src[rs, :].astype(F32)
        dst[rs, :] = (t * lax.rsqrt(jnp.mean(t * t, axis=-1, keepdims=True) + NORM_EPS) * gain[:1, :]).astype(BF16)
    loop(src.shape[0] // STRIP, step)


def norm_back(dy, src, gain, skip, dst, dgain):
    def step(i):
        rs = seg(i, STRIP)
        d = dy[rs, :].astype(BF16).astype(F32)
        t = src[rs, :].astype(F32)
        inv = lax.rsqrt(jnp.mean(t * t, axis=-1, keepdims=True) + NORM_EPS)
        gd = gain[:1, :] * d
        pull = jnp.mean(gd * t, axis=-1, keepdims=True)
        dst[rs, :] = (skip[rs, :].astype(F32) + (inv * gd - t * (inv * inv * inv * pull))).astype(BF16)
        g = d * (t * inv)
        dgain[...] += g[:N_CHIP] + g[N_CHIP:]
    dgain[...] = jnp.zeros_like(dgain)
    loop(src.shape[0] // STRIP, step)


QB = 256
KB = 256


def key_rows(dst, src, lo, hd):
    def step(i):
        dst[seg(i, KB), :] = src[lo:lo + hd, seg(i, KB)].T
    loop(src.shape[1] // KB, step)


def score_block(k, q2, scale, diagonal):
    s = mm(k, q2, NN) * scale
    if diagonal:
        key = lax.broadcasted_iota(jnp.int32, s.shape, 0)
        qry = lax.broadcasted_iota(jnp.int32, s.shape, 1) % QB
        s = jnp.where(qry >= key, s, NEG_LARGE)
    return s


def side_by_side(ref, heads, hd, qs):
    return jnp.concatenate([ref[h * hd:(h + 1) * hd, qs] for h in range(heads)], axis=1)


def head(groups, hd, x_ref, g1_ref, g2_ref, pos_ref, wq_ref, wk_ref, wv_ref, freq_ref, wg_ref, wu_ref, wo_ref, qkv_ref, u_scr, small_all, w_out, o_ref, stat_ref, wgu_ref, h_ref, m_ref, cos_ref, sin_ref,
         full_w, acc_o, o_tok, o_send, small_ref, w_ref, full, acc, rot, g_scr, wg_t, wu_t, s_scr, k_scr, osem, *sems):
    me = lax.axis_index('sp')
    tokens, dim = x_ref.shape
    cols = w_ref.shape[0]
    small_ref[...] = jnp.concatenate([r[...].astype(F32) for r in (g1_ref, g2_ref, pos_ref)] + [jnp.zeros((N_CHIP - 3, LANE), F32)], axis=0)
    w_ref[:wq_ref.shape[0], :] = wq_ref[...]
    for k in range(groups):
        for i, ref in enumerate((wk_ref, wv_ref)):
            w_ref[pl.ds(wq_ref.shape[0] + (2 * k + i) * hd, hd), :] = ref[k * hd:(k + 1) * hd, :]
    qw = tokens
    q_all = N_DEV * qw
    gsems, ssems, qsems, ksems, gate_sems, up_sems, osems = sems[:4], *(sems[i:i + 2] for i in range(4, len(sems) - 4, 2))
    gw = row_gather(wo_ref, full_w, sems[-4:], me, 1)
    feat = wg_ref.shape[1] // N_DEV
    enter(me, OTHERS)
    smalls = Swap(lambda peer: small_ref, lambda o: small_all.at[o], ssems, me)
    smalls.start()
    parts = thirds(cols, STRIP)
    g = Gather(w_ref, lambda o: full.at[o // 2, :, seg(o % 2)], lambda view, c: [view.at[pl.ds(*parts[c]), :]], gsems, me)
    g.start()
    gates = Swap(lambda peer: wg_t.at[seg(peer, feat), :], lambda o: wgu_ref.at[:feat, seg(o)], gate_sems, me)
    ups = Swap(lambda peer: wu_t.at[seg(peer, feat), :], lambda o: wgu_ref.at[feat:, seg(o)], up_sems, me)

    def advance(n):
        gates.advance(n)
        ups.advance(n)

    def transpose(i):
        wg_t[seg(i, CHUNK), :] = wg_ref[:, seg(i, CHUNK)].T
        wu_t[seg(i, CHUNK), :] = wu_ref[:, seg(i, CHUNK)].T
    loop(wg_ref.shape[1] // CHUNK, transpose)
    advance(0)

    def own_block(i):
        full[me // 2, seg(i, WIDE), seg(me % 2)] = w_ref[seg(i, WIDE), :]
    loop(cols // WIDE, own_block)
    acc[...] = jnp.zeros_like(acc)
    small_all[me] = small_ref[...]
    smalls.wait_recv()
    gain_row(g_scr, small_all, 0)
    norm_rows(x_ref, g_scr, u_scr)

    def keep(mask):
        chip = flipped(me, mask) // 2
        return pltpu.make_async_copy(full.at[chip], w_out.at[chip], osem.at[mask // 2])

    def use(mask):
        g.wait_pair(mask)
        keep(mask).start()
        chip = flipped(me, mask) // 2
        u = u_scr[:, seg(chip, WIDE)]

        def step(i):
            rs = seg(i, cols // 2)
            acc[rs, :] += mm(full[chip, rs, :], u, NT)
        loop(2, step)

    def tables(o):
        angles = freq_ref[...] * small_all[o, 2:3, :]
        cos_ref[:, seg(o)] = jnp.cos(angles)
        sin_ref[:, seg(o)] = jnp.sin(angles)

    for r in range(len(g.ROUNDS)):
        g.round(r)
        if r in (2, 4):
            advance(r // 2)
        if r == 1:
            loop(N_DEV, tables)
        for mask in g.READY[r]:
            use(mask)

    half = hd // 2
    cos, sin = cos_ref[:, seg(me)], sin_ref[:, seg(me)]

    def turn(h):
        first = seg(2 * h, half)
        second = seg(2 * h + 1, half)
        p = acc[first, :].astype(BF16).astype(F32)
        q = acc[second, :].astype(BF16).astype(F32)
        rot[first, :] = (p * cos - q * sin).astype(BF16)
        rot[second, :] = (q * cos + p * sin).astype(BF16)
    loop(q_all // hd, turn)
    for k in range(groups):
        turn(q_all // hd + 2 * k)
        vs = seg(q_all // hd + 2 * k + 1, hd)
        rot[vs, :] = acc[vs, :].astype(BF16)
    per = N_DEV // groups
    q_rows = lambda peer: seg(peer, qw)
    kv_rows = lambda peer: seg(q_all // (2 * hd) + peer // per, 2 * hd)
    qs = Swap(lambda peer: rot.at[q_rows(peer), :], lambda o: qkv_ref.at[:qw, seg(o, tokens)], qsems, me)
    kvs = Swap(lambda peer: rot.at[kv_rows(peer), :], lambda o: qkv_ref.at[qw:, seg(o, tokens)], ksems, me)
    qs.start()
    kvs.start()
    gw.start()
    keep_own(wo_ref, full_w, me)
    gain_row(g_scr, small_all, 1)
    qkv_ref[:qw, seg(me, tokens)] = rot[q_rows(me), :]
    qkv_ref[qw:, seg(me, tokens)] = rot[kv_rows(me), :]
    wgu_ref[:feat, seg(me)] = wg_t[seg(me, feat), :]
    wgu_ref[feat:, seg(me)] = wu_t[seg(me, feat), :]
    gates.start((CORE,))
    ups.start((CORE,))
    for swap in (qs, kvs):
        swap.wait_recv()
    heads = qkv_ref.shape[0] // hd - 2
    seq = qkv_ref.shape[1]
    scale = hd ** -0.5
    lanes = heads * QB
    key_rows(k_scr, qkv_ref, qw, hd)

    outs = Swap(lambda peer: o_send.at[seg(peer), :], lambda o: o_tok.at[:, seg(o)], osems, me)

    def q_block(qb):
        for at, r in ((2, 0), (4, 1), (5, 2), (6, 3), (7, 4)):
            @pl.when(qb == at)
            def _():
                gw.round(r)
        qs = seg(qb, QB)
        q2 = side_by_side(qkv_ref, heads, hd, qs)

        def scores(kb, top, diagonal):
            s = score_block(k_scr[seg(kb, KB), :], q2, scale, diagonal)
            s_scr[seg(kb, KB), :] = s
            return jnp.maximum(top, jnp.max(s, axis=0, keepdims=True))

        top = lax.fori_loop(0, qb, lambda kb, t: scores(kb, t, False), jnp.full((1, lanes), NEG_LARGE, F32))
        top = scores(qb, top, True)

        def expo(kb, tot):
            e = jnp.exp(s_scr[seg(kb, KB), :] - top)
            s_scr[seg(kb, KB), :] = e
            return tot + jnp.sum(e, axis=0, keepdims=True)

        inv = 1.0 / lax.fori_loop(0, qb + 1, expo, jnp.zeros((1, lanes), F32))

        def weigh(kb, acc):
            p = (s_scr[seg(kb, KB), :] * inv).astype(BF16)
            return acc + mm(qkv_ref[qw + hd:, seg(kb, KB)], p, NN)

        acc = lax.fori_loop(0, qb + 1, weigh, jnp.zeros((hd, lanes), F32))
        for h in range(heads):
            o_ref[h * hd:(h + 1) * hd, qs] = acc[:, h * QB:(h + 1) * QB].astype(BF16)
        stat_ref[qb, :1, :] = top
        stat_ref[qb, 1:, :] = inv
        o_send[qs, :] = o_ref[:, qs].T

    loop(seq // QB, q_block)
    outs.start()
    advance(3)
    o_tok[:, seg(me)] = o_send[seg(me), :]
    for r in (5, 6):
        gw.round(r)
    outs.wait_recv()
    for mask in CHIP_MASKS:
        gw.wait_pair(mask)

    def project(n):
        cs = seg(n, CHUNK)
        acc_o[:, cs] = mm(o_tok[...], full_w[:, :, cs].reshape(dim, CHUNK), NN)
    loop(dim // CHUNK, project)

    def residual(i):
        rs = seg(i, STRIP)
        h_ref[rs, :] = (x_ref[rs, :].astype(F32) + acc_o[rs, :]).astype(BF16)
    loop(tokens // STRIP, residual)
    norm_rows(h_ref, g_scr, m_ref)
    for swap in (gates, ups):
        swap.wait_recv()
    for mask in CHIP_MASKS:
        keep(mask).wait()
    outs.wait_send()
    for swap in (gates, ups):
        swap.wait_send((CORE,) + SETS[3])
    g.finish()
    gw.finish()
    for swap in (smalls, qs, kvs):
        swap.wait_send()


def dw_swaps(stage, gate_hbm, up_hbm, sems, me):
    feat = gate_hbm.shape[0] // N_DEV
    return [Swap(lambda peer, lo=lo: stage(peer).at[lo:lo + feat, seg(peer % 2)], lambda o, dst=dst: dst.at[seg(o, feat), :], sems[i:i + 2], me)
            for lo, dst, i in ((0, gate_hbm, 0), (feat, up_hbm, 2))]


def mlp(m_ref, dout_ref, wgu_hbm, down_hbm, u_ref, h_ref, small_all, wo_ref, o_ref,
        ucol_ref, m_out, dgu_out, ddown_out, y_ref, dh_ref, do_ref, dwo_ref, dg_ref, gate_hbm, up_hbm,
        wgu_ref, down_ref, glu_ref, dgu_ref, ddown_ref, isem, dsem, full_d, full_m, osem, stage, g_scr, dgu_t, glu_t, free, *scr):
    me = lax.axis_index('sp')
    feat, dim = down_ref.shape
    loads = fetch_all(isem, (wgu_hbm, wgu_ref), (down_hbm, down_ref))
    enter(me, OTHERS)
    sems = scr[4:]
    gd = row_gather(dout_ref, full_d, sems[:4], me, 0)
    gm = row_gather(m_ref, full_m, sems[4:8], me, 2)
    g = row_gather(dh_ref, full_d, sems[8:12], me, 1)
    ucols = Swap(lambda peer: u_ref.at[:, seg(peer)], lambda o: ucol_ref.at[seg(o), :], sems[12:14], me)
    gates, ups = dw_swaps(lambda peer: stage, gate_hbm, up_hbm, sems[14:18], me)
    gm.start()
    gd.start()
    ucol_ref[seg(me), :] = u_ref[:, seg(me)]
    keep_own(m_ref, full_m, me)
    keep_own(dout_ref, full_d, me)
    gain_row(g_scr, small_all, 1)
    dwo_ref[...] = jnp.zeros_like(dwo_ref)
    ddown_ref[...] = jnp.zeros_like(ddown_ref)

    def keep(mask):
        chip = flipped(me, mask) // 2
        ts = seg(chip, WIDE)
        ends = ((full_m.at[chip], m_out.at[chip]), (dgu_ref.at[:, ts], dgu_out.at[:, ts]))
        return [pltpu.make_async_copy(src, dst, osem.at[mask // 2, i]) for i, (src, dst) in enumerate(ends)]

    for load in loads:
        load.wait()

    def use(mask):
        gd.wait_pair(mask)
        gm.wait_pair(mask)
        chip = flipped(me, mask) // 2
        ts = seg(chip, WIDE)
        gu = mm(wgu_ref[...], full_m[chip], NT).astype(BF16).astype(F32)
        gate, up = gu[:feat], gu[feat:]
        d_glu = mm(down_ref[...], full_d[chip], NT).astype(BF16).astype(F32)
        sig = jax.nn.sigmoid(gate)
        act = gate * sig
        glu = (act * up).astype(BF16)
        glu_ref[:, ts] = glu
        dgu_ref[:feat, ts] = (d_glu * up * (sig * (1.0 + gate * (1.0 - sig)))).astype(BF16)
        dgu_ref[feat:, ts] = (d_glu * act).astype(BF16)

        def step(n):
            ddown_ref[:, seg(n, CHUNK)] += mm(glu, full_d[chip, :, seg(n, CHUNK)], NN)
        loop(dim // CHUNK, step)
        for copy in keep(mask):
            copy.start()

    for r in range(len(gm.ROUNDS)):
        gm.round(r)
        gd.round(r)
        if r == 3:
            ucols.start()
        for mask in gm.READY[r]:
            use(mask)
    far = seg(flipped(me, XYZ) // 2, WIDE)
    stage[...] = mm(dgu_ref[...], full_m[:, :, far].reshape(dgu_ref.shape[1], WIDE), NN)
    for swap in (gates, ups):
        swap.start(SETS[0])
    for gather in (gd, gm):
        gather.finish()
    leave = pltpu.make_async_copy(ddown_ref, ddown_out, dsem)
    leave.start()
    s = Scatter(*scr[:4], sems[18:], me)
    total = s.run(block_product(s, dgu_ref, wgu_ref, dgu_t))
    for mask in NEAR:
        pl.semaphore_signal(free, inc=1, device_id=(flipped(me, mask),), device_id_type=MESH)
    norm_back(total, h_ref, g_scr, dout_ref, dh_ref, dg_ref)
    g.start()
    keep_own(dh_ref, full_d, me)
    s.finish()
    pl.semaphore_wait(free, len(NEAR))

    def use_dh(mask):
        g.wait_pair(mask)
        chip = flipped(me, mask) // 2
        do_ref[:, seg(chip, WIDE)] = mm(wo_ref[...], full_d[chip], NT).astype(BF16)
        o = o_ref[:, seg(chip, WIDE)]

        def step(n):
            dwo_ref[:, seg(n, CHUNK)] += mm(o, full_d[chip, :, seg(n, CHUNK)], NN)
        loop(dim // CHUNK, step)

    def between(i):
        r = i if i < 3 else i - N_CHIP + 3
        if i < 3 or i >= N_CHIP:
            g.round(r)
            for mask in g.READY[r]:
                use_dh(mask)

    s = Scatter(*scr[:4], sems[18:], me)
    total = s.run(block_product(s, glu_ref, down_ref, glu_t), between)
    y_ref[...] = (h_ref[...].astype(F32) + total[...]).astype(BF16)
    s.finish()
    g.finish()
    for swap in (gates, ups):
        swap.wait_recv(SETS[0])
        swap.wait_send(SETS[0])
    ucols.wait_recv()
    ucols.wait_send()
    leave.wait()
    for mask in CHIP_MASKS:
        for copy in keep(mask):
            copy.wait()


def back(groups, hd, qkv_ref, do_ref, stat_ref, cos_all, sin_all, dgu_ref, m_hbm, ucol_ref, w_hbm, x_ref, small_all, dh_ref, dg2_ref, dg_in, du_in,
         dg_hbm, du_hbm, dwq_ref, dwkv_ref, dx_ref, gain_ref,
         p_scr, dp_scr, k_scr, v_scr, dk_acc, dv_acc, stage, dq_scr, dkv_scr, m_scr,
         full, w_scr, shares, dkv_own, full_kv, dqkv, dn, g_scr, dg1, gains, gains_in, wsem, lsem, msem, *sems):
    heads = qkv_ref.shape[0] // hd - 2
    seq = qkv_ref.shape[1]
    scale = hd ** -0.5
    lanes = heads * QB
    qw = heads * hd
    half = hd // 2
    me = lax.axis_index('sp')
    feat = dgu_ref.shape[0] // 2
    first = (X, Y + Z, Y, X + Z, Z, X + Y, 0)

    def fetch(mask):
        cols = seg(flipped(me, mask) // 2, WIDE)
        return pltpu.make_async_copy(m_hbm.at[:, :, cols], m_scr.at[:, :, cols], msem.at[mask // 2])
    for mask in first:
        fetch(mask).start()
    load = pltpu.make_async_copy(w_hbm, w_scr, wsem)
    load.start()
    enter(me, OTHERS)
    gain_row(g_scr, small_all, 0)

    gates, ups = dw_swaps(lambda peer: stage.at[peer // 2], dg_hbm, du_hbm, sems[:4], me)
    gq = row_gather(dq_scr, full, sems[6:10], me)
    own = [pltpu.make_async_copy(swap.src(me), swap.dst(me), lsem.at[i]) for i, swap in enumerate((gates, ups))]

    def make(mask):
        chip = flipped(me, mask) // 2
        fetch(mask).wait()
        cols = m_scr[:, :, seg(chip, WIDE)].reshape(seq, WIDE)
        stage[chip] = mm(dgu_ref[...], cols, NN)

    def advance(n):
        for swap in (gates, ups):
            if n > 1:
                swap.wait_send(SETS[n - 1])
            swap.start(SETS[n])

    for i, mask in enumerate(first):
        make(mask)
        if i == 1:
            advance(1)
    gates.start((CORE,))
    ups.start((CORE,))
    for copy in own:
        copy.start()

    dk_acc[...] = jnp.zeros_like(dk_acc)
    dv_acc[...] = jnp.zeros_like(dv_acc)
    key_rows(k_scr, qkv_ref, qw, hd)
    key_rows(v_scr, qkv_ref, qw + hd, hd)

    def q_block(qb):
        @pl.when(qb == 4)
        def _():
            advance(2)
        qs = seg(qb, QB)
        q2 = side_by_side(qkv_ref, heads, hd, qs)
        do2 = side_by_side(do_ref, heads, hd, qs)
        top = stat_ref[qb, :1, :]
        inv = stat_ref[qb, 1:, :]

        def probs(kb, rd, diagonal):
            ks = seg(kb, KB)
            s = score_block(k_scr[ks, :], q2, scale, diagonal)
            p = jnp.exp(s - top) * inv
            dp = mm(v_scr[ks, :], do2, NN).astype(BF16)
            p_scr[ks, :] = p
            dp_scr[ks, :] = dp
            dv_acc[ks, :] += mm(p.astype(BF16), do2, NT)
            return rd + jnp.sum(dp.astype(F32) * p, axis=0, keepdims=True)

        rd = lax.fori_loop(0, qb, lambda kb, r: probs(kb, r, False), jnp.zeros((1, lanes), F32))
        rd = probs(qb, rd, True)

        def d_scores(kb, acc):
            ks = seg(kb, KB)
            ds = (p_scr[ks, :] * (dp_scr[ks, :].astype(F32) - rd) * scale).astype(BF16)
            dk_acc[ks, :] += mm(ds, q2, NT)
            return acc + mm(qkv_ref[qw:qw + hd, ks], ds, NN)

        acc = lax.fori_loop(0, qb + 1, d_scores, jnp.zeros((hd, lanes), F32))
        cos, sin = cos_all[:, qs], sin_all[:, qs]
        for h in range(heads):
            dq = acc[:, h * QB:(h + 1) * QB].astype(BF16).astype(F32)
            p, q = dq[:half], dq[half:]
            dq_scr[h * hd:h * hd + half, qs] = (p * cos + q * sin).astype(BF16)
            dq_scr[h * hd + half:(h + 1) * hd, qs] = (q * cos - p * sin).astype(BF16)

    loop(seq // QB, q_block)

    def share(i):
        rs = seg(i, WIDE)
        dkv_scr[rs, :] = jnp.concatenate([dk_acc[rs, :], dv_acc[rs, :]], axis=1).astype(BF16)
    loop(seq // WIDE, share)
    tokens = ucol_ref.shape[1]
    per = N_DEV // groups
    q_all = dwq_ref.shape[0]
    sh = Swap(lambda peer: dkv_scr.at[seg(peer, tokens), :], lambda o: shares.at[o], sems[4:6], me)
    parts = thirds(dkv_own.shape[0], STRIP)
    gk = Gather(dkv_own, lambda o: full_kv.at[:, seg(o, tokens)], lambda view, c: [view.at[pl.ds(*parts[c]), :]], sems[10:14], me)
    gs = Swap(lambda peer: gains.at[:, seg(peer)], lambda o: gains_in.at[o], sems[14:], me)
    sh.start()
    gq.start()
    keep_own(dq_scr, full, me)
    shares[me] = dkv_scr[seg(me, tokens), :]
    sh.wait_recv()
    cos, sin = cos_all[:, seg(me)], sin_all[:, seg(me)]
    for k in range(groups):
        both = sum(shares[per * k + i].astype(F32) for i in range(per)).astype(BF16).astype(F32).T
        p, q = both[:half], both[half:hd]
        lo = 2 * hd * k
        dkv_own[lo:lo + half, :] = (p * cos + q * sin).astype(BF16)
        dkv_own[lo + half:lo + hd, :] = (q * cos - p * sin).astype(BF16)
        dkv_own[lo + hd:lo + 2 * hd, :] = both[hd:].astype(BF16)
    gk.start()
    full_kv[:, seg(me, tokens)] = dkv_own[...]
    for k in range(groups):
        dqkv[:, q_all + 2 * hd * k:q_all + 2 * hd * (k + 1)] = dkv_own[2 * hd * k:2 * hd * (k + 1), :].T

    def use(mask):
        gq.wait_pair(mask)
        chip = flipped(me, mask) // 2
        dwq_ref[seg(chip, WIDE), :] = mm(full[chip], ucol_ref[...], NN)
        dqkv[:, seg(chip, WIDE)] = full[chip, :, seg(me, tokens)].T

    for r in range(len(gq.ROUNDS)):
        gq.round(r)
        gk.round(r)
        if r == 3:
            advance(3)
        for mask in gq.READY[r]:
            use(mask)
    load.wait()

    def normed(i):
        dn[:, seg(i, WIDE)] = mm(dqkv[...], w_scr[i], NN)
    loop(N_CHIP, normed)
    norm_back(dn, x_ref, g_scr, dh_ref, dx_ref, dg1)
    gains[...] = jnp.concatenate([jnp.sum(dg1[...], axis=0, keepdims=True), jnp.sum(dg2_ref[...], axis=0, keepdims=True),
                                  jnp.zeros((N_CHIP - 2, dg1.shape[1]), F32)], axis=0)
    gs.start()
    gains_in[me] = gains[:, seg(me)]
    for mask in CHIP_MASKS:
        gk.wait_pair(mask)
    dwkv_ref[...] = mm(full_kv[...], ucol_ref[...], NN)
    gs.wait_recv()
    gain_ref[...] = sum(gains_in[o] for o in range(N_DEV))
    for swap in (gates, ups):
        swap.wait_recv((CORE,) + SETS[1] + SETS[2] + SETS[3])
        swap.wait_send((CORE,) + SETS[3])
    for copy in own:
        copy.wait()
    for c in (sh, gs):
        c.wait_send()
    for g in (gq, gk):
        g.finish()


def finish(dg_hbm, du_hbm, dkv_hbm, *refs):
    n = (len(refs) - 11) // 3
    srcs, (gate, up, dk, dv), dsts = refs[:n], refs[n:n + 4], refs[n + 4:2 * n + 4]
    (g_in, g_out, kv_in), holds, sems = refs[2 * n + 4:2 * n + 7], refs[2 * n + 7:3 * n + 7], refs[3 * n + 7:]
    t_in, t_out, p_in, p_out = sems
    step = LANE * 11
    cols = g_in.shape[1]
    hd = dk.shape[0] // (kv_in.shape[0] // LANE)
    starts = [(w, i) for i in range(cols // step) for w in range(2)]

    def fetch(w, i):
        rs = pl.ds(i * step, step)
        return pltpu.make_async_copy((dg_hbm, du_hbm)[w].at[rs, :], g_in.at[w, rs, :], t_in.at[w, i])

    def put(w, i):
        cs = pl.ds(i * step, step)
        return pltpu.make_async_copy(g_out.at[w, :, cs], (gate, up)[w].at[:, cs], t_out.at[w, i])
    moves = [(pltpu.make_async_copy(a, h, p_in.at[k]), pltpu.make_async_copy(h, b, p_out.at[k])) for k, (a, h, b) in enumerate(zip(srcs, holds, dsts))]
    kv = pltpu.make_async_copy(dkv_hbm, kv_in, p_in.at[n])
    for w, i in starts:
        fetch(w, i).start()
    kv.start()
    for load, _ in moves:
        load.start()
    for w, i in starts:
        fetch(w, i).wait()

        at = pl.ds(i * step, step)
        g_out[w, :, at] = g_in[w, at, :].T
        put(w, i).start()
    kv.wait()
    for k in range(dk.shape[0] // hd):
        for i, ref in enumerate((dk, dv)):
            ref[k * hd:(k + 1) * hd, :] = kv_in[(2 * k + i) * hd:(2 * k + i + 1) * hd, :]
    for load, store in moves:
        load.wait()
        store.start()
    for w, i in starts:
        put(w, i).wait()
    for _, store in moves:
        store.wait()


def solution(mesh):
    assert mesh.shape['sp'] == N_DEV

    def layer_step(x_in, positions, d_out, norm1_gain, norm2_gain, w_q, w_k, w_v, w_o, w_gate, w_up, w_down):
        tokens, dim = x_in.shape
        seq = tokens * N_DEV
        n_q, hd = w_q.shape[1:]
        n_kv = w_k.shape[1]
        qw = n_q // N_DEV * hd
        rows = w_q.shape[0]
        feat = w_down.shape[0]
        cols = (n_q + 2 * n_kv) * hd
        lanes = qw // hd * QB
        vm = pltpu.VMEM
        full = vm((N_CHIP, WIDE, dim), BF16)
        gain_scr = vm((N_CHIP, dim), F32)
        tok_shapes = 2 * (((tokens, dim), BF16),)
        dw_shapes = 2 * (((feat * N_DEV, rows), F32),)

        inv_freq = 1.0 / (ROPE_BASE ** (jnp.arange(hd // 2, dtype=F32) * (2.0 / hd)))
        freq = jnp.broadcast_to(inv_freq[:, None], (hd // 2, rows))
        row = lambda v: v.reshape(1, rows)
        by_head = lambda w: w.transpose(1, 2, 0).reshape(-1, rows)
        wo_own = w_o.reshape(qw, dim)

        args = (x_in, row(norm1_gain), row(norm2_gain), row(positions), by_head(w_q), by_head(w_k), by_head(w_v), freq, w_gate, w_up, wo_own)
        qkv, u, small_all, wqkv, attn_t, stat, wgu, hidden, mlp_in, cos_all, sin_all = call(
            functools.partial(head, n_kv, hd), 0, len(args),
            (((qw + 2 * hd, seq), BF16), tok_shapes[0], ((N_DEV, N_CHIP, rows), F32), ((N_CHIP, cols, WIDE), BF16),
             ((qw, seq), BF16), ((seq // QB, 2, lanes), F32), ((2 * feat, dim), BF16), *tok_shapes, *(2 * (((hd // 2, seq), F32),))),
            [full, vm((tokens, dim), F32), vm((tokens, dim), BF16), vm((seq, qw), BF16),
             vm((N_CHIP, rows), F32), vm((cols, rows), BF16), vm((N_CHIP, cols, WIDE), BF16), vm((cols, tokens), F32), vm((cols, tokens), BF16), gain_scr,
             vm((feat * N_DEV, rows), BF16), vm((feat * N_DEV, rows), BF16), vm((seq, lanes), F32), vm((seq, hd), BF16), dma(N_CHIP),
             *Gather.sems, *(6 * Swap.sems), *Gather.sems], 4 * qw * seq * seq, far_out=(3,))(*args)
        args = (mlp_in, d_out, wgu, w_down, u, hidden, small_all, wo_own, attn_t)
        u_col, m_full, dgu, d_down, y_out, d_hidden, d_attn, d_wo, d_g2, d_gate_t, d_up_t = call(
            mlp, 1, len(args),
            (((seq, rows), BF16), ((N_CHIP, WIDE, dim), BF16), ((2 * feat, seq), BF16), ((feat, dim), F32),
             *tok_shapes, ((qw, seq), BF16), ((qw, dim), F32), ((N_CHIP, dim), F32), *dw_shapes),
            [vm((2 * feat, dim), BF16), vm((feat, dim), BF16), vm((feat, seq), BF16), vm((2 * feat, seq), BF16), vm((feat, dim), F32), dma(2), dma(),
             full, full, dma(N_CHIP, 2), vm((2 * feat, WIDE), F32), gain_scr, vm((WIDE, 2 * feat), BF16), vm((WIDE, feat), BF16), pltpu.SemaphoreType.REGULAR,
             *Scatter.scratch(tokens, dim), *(3 * Gather.sems), *(3 * Swap.sems), *Scatter.sems], 12 * feat * seq * dim,
            far_in=(2, 3), far_out=(1, 2, 3, 9, 10))(*args)
        args = (qkv, d_attn, stat, cos_all, sin_all, dgu, m_full, u_col, wqkv, x_in, small_all, d_hidden, d_g2, d_gate_t, d_up_t)
        d_gate_t, d_up_t, d_wq, d_wkv, d_x, gains = call(
            functools.partial(back, n_kv, hd), 3, len(args),
            (*dw_shapes, ((n_q * hd, rows), F32), ((2 * n_kv * hd, rows), F32), tok_shapes[0], ((N_CHIP, rows), F32)),
            [vm((seq, lanes), F32), vm((seq, lanes), BF16), vm((seq, hd), BF16), vm((seq, hd), BF16), vm((seq, hd), F32), vm((seq, hd), F32),
             vm((N_CHIP, 2 * feat, WIDE), F32), vm((qw, seq), BF16), vm((seq, 2 * hd), BF16), full,
             full, vm((N_CHIP, cols, WIDE), BF16), vm((N_DEV, tokens, 2 * hd), BF16), vm((2 * n_kv * hd, tokens), BF16), vm((2 * n_kv * hd, seq), BF16),
             vm((tokens, cols), BF16), vm((tokens, dim), F32), gain_scr, gain_scr, gain_scr, vm((N_DEV, N_CHIP, rows), F32), dma(), dma(2), dma(N_CHIP),
             *(3 * Swap.sems), *(2 * Gather.sems), *Swap.sems], 10 * qw * seq * seq, far_in=(6, 8, 13, 14), far_out=(0, 1), aliases={13: 0, 14: 1})(*args)
        moved = (d_wq, d_wo, d_down, d_x, y_out, gains)
        half_kv = jax.ShapeDtypeStruct((n_kv * hd, rows), F32)
        wide = jax.ShapeDtypeStruct((rows, feat * N_DEV), F32)
        d_gate, d_up, d_wk, d_wv, d_wq, d_wo, d_down, d_x, y_out, gains = pl.pallas_call(
            finish,
            out_shape=[wide, wide, half_kv, half_kv] + [jax.ShapeDtypeStruct(v.shape, v.dtype) for v in moved],
            in_specs=[IN_HBM] * (3 + len(moved)), out_specs=[IN_HBM] * 2 + on_chip(2) + [IN_HBM] * len(moved),
            scratch_shapes=[vm((2, feat * N_DEV, rows), F32), vm((2, rows, feat * N_DEV), F32), vm(d_wkv.shape, F32)]
            + [vm(v.shape, v.dtype) for v in moved] + [dma(2, 4), dma(2, 4), dma(len(moved) + 1), dma(len(moved))],
            compiler_params=pltpu.CompilerParams(vmem_limit_bytes=VMEM_CAP), name='finish',
        )(d_gate_t, d_up_t, d_wkv, *moved)
        by_row = lambda g, heads: g.reshape(heads, hd, rows).transpose(2, 0, 1)
        return (y_out, d_x, gains[0], gains[1], by_row(d_wq, n_q), by_row(d_wk, n_kv), by_row(d_wv, n_kv),
                d_wo.reshape(w_o.shape), d_gate, d_up, d_down)

    all_rows = P('sp')
    return jax.shard_map(layer_step, mesh=mesh, in_specs=(all_rows,) * 12, out_specs=(all_rows,) * 11, check_vma=False)
```

```python
import functools
import jax
import jax.numpy as jnp
from jax import lax
from jax.experimental import pallas as pl
from jax.experimental.pallas import tpu as pltpu
from jax.sharding import PartitionSpec as P

ROPE_BASE = 10000.0
NORM_EPS = 1e-5
NEG_LARGE = -1e30
F32 = jnp.float32
BF16 = jnp.bfloat16
N_DEV, N_CHIP, LANE, WIDE, CHUNK, STRIP = 16, 8, 128, 256, 512, 16
NT = (((1,), (1,)), ((), ()))
TN = (((0,), (0,)), ((), ()))
NN = (((1,), (0,)), ((), ()))
MESH = pl.DeviceIdType.MESH
VMEM_CAP = 62 * 1024 * 1024

CORE, X, Y, Z = 1, 2, 4, 8
XYZ = X + Y + Z
ORDERS = ((X, Y, Z), (Y, Z, X), (Z, X, Y))
CHIP_MASKS = (0, X, Y, Z, X + Y, X + Z, Y + Z, XYZ)
NEAR = (CORE, X, Y, Z)
OTHERS = range(1, N_DEV)
SETS = tuple(tuple(m + c for m in masks for c in (0, CORE)) for masks in ((XYZ,), (X, Y + Z), (Y, X + Z), (Z, X + Y)))
N_COL = len(ORDERS)
COLOURS = range(N_COL)


def mm(a, b, dims):
    return lax.dot_general(a, b, dims, preferred_element_type=F32)


def seg(index, width=LANE):
    return pl.ds(pl.multiple_of(index * width, width), width)


def loop(count, body):
    lax.fori_loop(0, count, lambda i, c: (body(i), c)[1], 0)


def differing(index, mask):
    return sum(((index // bit + mask // bit) % 2) * bit for bit in NEAR)


def flipped(index, mask):
    out = index
    for bit in NEAR:
        if mask & bit:
            out = out + (1 - 2 * ((index // bit) % 2)) * bit
    return out


def thirds(total, unit):
    n = total // unit
    first = (n + 2) // 3
    second = (n - first + 1) // 2
    sizes = (first * unit, second * unit, (n - first - second) * unit)
    return ((0, sizes[0]), (sizes[0], sizes[1]), (sizes[0] + sizes[1], sizes[2]))


def pieces(rows, cols, unit):
    share = cols // LANE // N_COL * LANE
    strips = thirds(rows, unit)
    rest = cols - N_COL * share
    return [[(pl.ds(0, rows), pl.ds(c * share, share)), (pl.ds(*strips[c]), pl.ds(N_COL * share, rest))] for c in COLOURS]


def enter(me, masks):
    barrier = pltpu.get_barrier_semaphore()
    for mask in masks:
        pl.semaphore_signal(barrier, inc=1, device_id=(flipped(me, mask),), device_id_type=MESH)
    pl.semaphore_wait(barrier, len(masks))


def remote(src, dst, send, recv, peer):
    return pltpu.make_async_remote_copy(src_ref=src, dst_ref=dst, send_sem=send, recv_sem=recv, device_id=(peer,), device_id_type=MESH)


def dma(*shape):
    return pltpu.SemaphoreType.DMA(shape)


class Swap:
    sems = (dma(N_DEV), dma(N_DEV))

    def __init__(self, src, dst, sems, me):
        self.src, self.dst, (self.send, self.recv), self.me = src, dst, sems, me

    def copy(self, mask):
        peer = differing(self.me, mask)
        return remote(self.src(peer), self.dst(self.me), self.send.at[mask], self.recv.at[mask], peer)

    def arrival(self, mask):
        view = self.dst(differing(self.me, mask))
        return remote(view, view, self.send.at[mask], self.recv.at[mask], self.me)

    def each(self, masks, act):
        if masks is None:
            loop(N_DEV - 1, lambda i: act(i + 1))
        else:
            for mask in masks:
                act(mask)

    def start(self, masks=None):
        if masks is not None:
            return self.each(masks, lambda mask: self.copy(mask).start())

        def step(i):
            turn = (i // 2 + 5 + self.me % 2) % 6 + 1
            self.copy(2 * (2 * turn % 7) + i % 2).start()
        loop(12, step)
        self.each((XYZ, XYZ + CORE, CORE), lambda mask: self.copy(mask).start())

    def advance(self, n):
        if n:
            self.wait_send(SETS[n - 1])
        self.start(SETS[n])

    def wait_recv(self, masks=None):
        self.each(masks, lambda mask: self.arrival(mask).wait_recv())

    def wait_send(self, masks=None):
        self.each(masks, lambda mask: self.copy(mask).wait_send())


class Gather:
    ROUNDS = ((0,), (1,), (2,), (0, 1), (0, 2), (1, 2), (0, 1, 2))
    READY = ((0,), (), (), (X, Y), (Z,), (X + Y, X + Z), (Y + Z, XYZ))
    sems = (dma(N_COL, N_CHIP, 2), dma(N_COL, N_CHIP, 2), dma(N_CHIP), dma(N_CHIP))

    def __init__(self, own, block, cut, sems, me):
        self.own, self.block, self.cut, self.me = own, block, cut, me
        self.send, self.recv, self.pair_send, self.pair_recv = sems

    def source(self, mask):
        return self.block(flipped(self.me, mask)) if mask else self.own

    def unit(self, colour, mask, axis):
        ends = zip(self.cut(self.source(mask), colour), self.cut(self.block(flipped(self.me, mask)), colour))
        j = self.sends(colour).index((mask, axis))
        return [remote(src, dst, self.send.at[colour, j, i], self.recv.at[colour, (mask + axis) // 2, i],
                       flipped(self.me, axis)) for i, (src, dst) in enumerate(ends)]

    def sends(self, colour):
        return [(0, axis) for axis in ORDERS[colour]] + [step[1:] for step in self.onward(colour)]

    def start_unit(self, colour, mask, axis):
        for copy in self.unit(colour, mask, axis):
            copy.start()

    def pair(self, mask):
        return remote(self.source(mask), self.block(flipped(self.me, mask)), self.pair_send.at[mask // 2],
                      self.pair_recv.at[mask // 2], flipped(self.me, CORE))

    def wait_pair(self, mask):
        view = self.block(flipped(self.me, mask + CORE))
        remote(view, view, self.pair_send.at[mask // 2], self.pair_recv.at[mask // 2], self.me).wait_recv()

    def onward(self, colour):
        order = ORDERS[colour]
        for picks in self.ROUNDS:
            for axis in order[picks[-1] + 1:]:
                yield picks, sum(order[p] for p in picks), axis

    def start(self):
        for pos in COLOURS:
            for colour in COLOURS:
                self.start_unit(colour, 0, ORDERS[colour][pos])
        self.pair(0).start()

    def round(self, r):
        for colour in COLOURS:
            mask = sum(ORDERS[colour][p] for p in self.ROUNDS[r])
            for i, view in enumerate(self.cut(self.block(flipped(self.me, mask)), colour)):
                remote(view, view, self.send.at[colour, 0, i], self.recv.at[colour, mask // 2, i], self.me).wait_recv()
            for picks, at, axis in self.onward(colour):
                if picks == self.ROUNDS[r]:
                    self.start_unit(colour, at, axis)
        for mask in {2: (X, Y, Z), 5: (X + Y, X + Z, Y + Z), 6: (XYZ,)}.get(r, ()):
            self.pair(mask).start()

    def finish(self):
        for colour in COLOURS:
            for i, view in enumerate(self.cut(self.own, colour)):
                loop(len(self.sends(colour)), lambda j: remote(view, view, self.send.at[colour, j, i], self.recv.at[colour, j, i], self.me).wait_send())
        loop(N_CHIP, lambda j: remote(self.own, self.own, self.pair_send.at[j], self.pair_recv.at[j], self.me).wait_send())


def row_gather(own, full, sems, me, extra=None):
    rows, width = own.shape
    parts = pieces(rows, width, STRIP)
    if extra is not None:
        share = width // LANE // N_COL * LANE
        more = width - N_COL * share
        parts = [[(pl.ds(0, rows), pl.ds(c * share + more * (c > extra), share + more * (c == extra)))] for c in COLOURS]

    def block(o):
        return full.at[o // 2, seg(o % 2), :]

    return Gather(own, block, lambda view, c: [view.at[rs, cs] for rs, cs in parts[c]], sems, me)


def keep_own(own, full, me):
    def step(i):
        full[me // 2, pl.ds(pl.multiple_of((me % 2) * LANE + i * STRIP, STRIP), STRIP), :] = own[seg(i, STRIP), :]
    loop(LANE // STRIP, step)


class Scatter:
    ORDER = (XYZ, X + Y, Y + Z, X + Z, X, Y, Z, 0)
    sems = (dma(N_CHIP), dma(N_CHIP), dma(N_COL, N_CHIP, 2), dma(N_COL, N_CHIP, 2))

    @staticmethod
    def scratch(tokens, dim):
        return [pltpu.VMEM((n, tokens, dim), F32) for n in (N_CHIP, 2, N_CHIP, N_CHIP - 1)]

    def __init__(self, part, other, pair_in, link_in, sems, me):
        self.part, self.other, self.pair_in, self.link_in, self.me = part, other, pair_in, link_in, me
        self.pair_send, self.pair_recv, self.link_send, self.link_recv = sems
        self.tokens, self.dim = part.shape[1:]
        self.pieces = pieces(self.tokens, self.dim, STRIP // 2)
        self.ready, self.sent = set(), [0] * N_COL

    @staticmethod
    def first(colour, mask):
        return next((i for i, a in enumerate(ORDERS[colour]) if mask & a), 3)

    def slot(self, colour, mask, axis):
        slots = [(m, a) for m in self.ORDER for a in ORDERS[colour][:self.first(colour, m)]]
        return slots.index((mask, axis))

    def pair(self, i):
        return remote(self.other.at[i % 2], self.pair_in.at[i], self.pair_send.at[i], self.pair_recv.at[i], flipped(self.me, CORE))

    def link(self, colour, mask):
        axis = ORDERS[colour][self.first(colour, mask)]
        slot = self.slot(colour, mask - axis, axis)
        i = self.ORDER.index(mask)
        return [remote(self.part.at[i, rs, cs], self.link_in.at[slot, rs, cs], self.link_send.at[colour, i, k],
                       self.link_recv.at[colour, slot, k], flipped(self.me, axis)) for k, (rs, cs) in enumerate(self.pieces[colour])]

    def start_link(self, colour, mask):
        for copy in self.link(colour, mask):
            copy.start()

    def add(self, mask, ref, cs):
        i = self.ORDER.index(mask)

        def step(r):
            rs = seg(r, STRIP)
            self.part[i, rs, cs] += ref[rs, cs]
        loop(self.tokens // STRIP, step)

    def finish_pair(self, i):
        self.pair(i).wait_recv()
        self.add(self.ORDER[i], self.pair_in.at[i], pl.ds(0, self.dim))
        self.ready.add(self.ORDER[i])
        for colour in COLOURS:
            a, b, c = ORDERS[colour]
            todo = (XYZ, a + b, a + c, a)
            while self.sent[colour] < len(todo) and todo[self.sent[colour]] in self.ready:
                self.start_link(colour, todo[self.sent[colour]])
                self.sent[colour] += 1

    def take(self, colour, mask, axis):
        for copy in self.link(colour, mask + axis):
            copy.wait_recv()
        ref = self.link_in.at[self.slot(colour, mask, axis)]
        (_, wide), (rs, cs) = self.pieces[colour]
        self.add(mask, ref, wide)
        self.part[self.ORDER.index(mask), rs, cs] += ref[rs, cs]

    def run(self, product, between=lambda i: None):
        for i, mask in enumerate(self.ORDER):
            if i > 1:
                self.pair(i - 2).wait_send()
            product(i, flipped(self.me, mask) // 2)
            self.pair(i).start()
            if i:
                self.finish_pair(i - 1)
            between(i)
        self.finish_pair(N_CHIP - 1)
        for step in range(2):
            between(N_CHIP + step)
            for colour in COLOURS:
                a, b, c = ORDERS[colour]
                mask = (b + c, b)[step]
                self.take(colour, mask, a)
                self.start_link(colour, mask)
        between(N_CHIP + 2)
        for colour in COLOURS:
            a, b, c = ORDERS[colour]
            self.take(colour, c, a)
            self.take(colour, c, b)
            self.start_link(colour, c)
        between(N_CHIP + 3)
        for colour in COLOURS:
            for axis in ORDERS[colour]:
                self.take(colour, 0, axis)
        return self.part.at[N_CHIP - 1]

    def finish(self):
        for i in (N_CHIP - 2, N_CHIP - 1):
            self.pair(i).wait_send()
        for colour in COLOURS:
            for k, (rs, cs) in enumerate(self.pieces[colour]):
                view = self.part.at[0, rs, cs]
                loop(N_CHIP - 1, lambda i: remote(view, view, self.link_send.at[colour, i, k], self.link_recv.at[colour, i, k], self.me).wait_send())


def block_product(s, a_ref, w_ref, a_t):
    core = s.me % 2

    def product(i, chip):
        a_t[...] = a_ref[:, seg(chip, WIDE)].T

        def step(n):
            cs = seg(n, CHUNK)
            s.other[i % 2, :, cs] = mm(a_t[seg(1 - core), :], w_ref[:, cs], NN)
            s.part[i, :, cs] = mm(a_t[seg(core), :], w_ref[:, cs], NN)
        loop(s.dim // CHUNK, step)
    return product


def on_chip(n):
    return [pl.BlockSpec(memory_space=pltpu.VMEM)] * n


IN_HBM = pl.BlockSpec(memory_space=pl.ANY)


def call(kernel, ident, args, outs, scratch, flops, far_in=(), far_out=(), aliases={}):
    specs = [IN_HBM if i in far_in else on_chip(1)[0] for i in range(args)]
    out_specs = [IN_HBM if i in far_out else on_chip(1)[0] for i in range(len(outs))]
    return pl.pallas_call(
        kernel,
        out_shape=[jax.ShapeDtypeStruct(shape, dtype) for shape, dtype in outs],
        in_specs=specs, out_specs=out_specs, scratch_shapes=scratch, input_output_aliases=aliases,
        cost_estimate=pl.CostEstimate(flops=flops, bytes_accessed=flops // CHUNK, transcendentals=0),
        compiler_params=pltpu.CompilerParams(collective_id=ident, has_side_effects=True, vmem_limit_bytes=VMEM_CAP),
        name=kernel.func.__name__ if isinstance(kernel, functools.partial) else kernel.__name__,
    )


def fetch_all(sem, *pairs):
    copies = [pltpu.make_async_copy(src, dst, sem.at[i]) for i, (src, dst) in enumerate(pairs)]
    for copy in copies:
        copy.start()
    return copies


def gain_row(dst, small_all, which):
    for o in range(N_DEV):
        dst[:1, o * LANE:(o + 1) * LANE] = small_all[o, which:which + 1, :]


def norm_rows(src, gain, dst):
    def step(i):
        rs = seg(i, STRIP)
        t = src[rs, :].astype(F32)
        dst[rs, :] = (t * lax.rsqrt(jnp.mean(t * t, axis=-1, keepdims=True) + NORM_EPS) * gain[:1, :]).astype(BF16)
    loop(src.shape[0] // STRIP, step)


def norm_back(dy, src, gain, skip, dst, dgain):
    def step(i):
        rs = seg(i, STRIP)
        d = dy[rs, :].astype(BF16).astype(F32)
        t = src[rs, :].astype(F32)
        inv = lax.rsqrt(jnp.mean(t * t, axis=-1, keepdims=True) + NORM_EPS)
        gd = gain[:1, :] * d
        pull = jnp.mean(gd * t, axis=-1, keepdims=True)
        dst[rs, :] = (skip[rs, :].astype(F32) + (inv * gd - t * (inv * inv * inv * pull))).astype(BF16)
        g = d * (t * inv)
        dgain[...] += g[:N_CHIP] + g[N_CHIP:]
    dgain[...] = jnp.zeros_like(dgain)
    loop(src.shape[0] // STRIP, step)


QB = 256
KB = 256


def key_rows(dst, src, lo, hd):
    def step(i):
        dst[seg(i, KB), :] = src[lo:lo + hd, seg(i, KB)].T
    loop(src.shape[1] // KB, step)


def score_block(k, q2, scale, diagonal):
    s = mm(k, q2, NN) * scale
    if diagonal:
        key = lax.broadcasted_iota(jnp.int32, s.shape, 0)
        qry = lax.broadcasted_iota(jnp.int32, s.shape, 1) % QB
        s = jnp.where(qry >= key, s, NEG_LARGE)
    return s


def side_by_side(ref, heads, hd, qs):
    return jnp.concatenate([ref[h * hd:(h + 1) * hd, qs] for h in range(heads)], axis=1)


def head(groups, hd, x_ref, g1_ref, g2_ref, pos_ref, wq_ref, wk_ref, wv_ref, freq_ref, wg_hbm, wu_hbm, wo_hbm, qkv_out, u_out, small_all, w_out, o_ref, stat_ref, wgu_ref, h_ref, m_ref, cos_out, sin_out,
         wg_ref, wu_ref, wo_ref, qkv_ref, u_scr, cos_ref, sin_ref, isem, esem,
         full_w, acc_o, o_tok, o_send, small_ref, w_ref, full, acc, rot, g_scr, wg_t, wu_t, s_scr, k_scr, osem, *sems):
    me = lax.axis_index('sp')
    tokens, dim = x_ref.shape
    cols = w_ref.shape[0]
    small_ref[...] = jnp.concatenate([r[...].astype(F32) for r in (g1_ref, g2_ref, pos_ref)] + [jnp.zeros((N_CHIP - 3, LANE), F32)], axis=0)
    w_ref[:wq_ref.shape[0], :] = wq_ref[...]
    for k in range(groups):
        for i, ref in enumerate((wk_ref, wv_ref)):
            w_ref[pl.ds(wq_ref.shape[0] + (2 * k + i) * hd, hd), :] = ref[k * hd:(k + 1) * hd, :]
    qw = tokens
    q_all = N_DEV * qw
    gsems, ssems, qsems, ksems, gate_sems, up_sems, osems = sems[:4], *(sems[i:i + 2] for i in range(4, len(sems) - 4, 2))
    gw = row_gather(wo_ref, full_w, sems[-4:], me, 1)
    feat = wg_ref.shape[1] // N_DEV
    loads = fetch_all(isem, (wg_hbm, wg_ref), (wu_hbm, wu_ref), (wo_hbm, wo_ref))
    enter(me, OTHERS)
    smalls = Swap(lambda peer: small_ref, lambda o: small_all.at[o], ssems, me)
    smalls.start()
    parts = thirds(cols, STRIP)
    g = Gather(w_ref, lambda o: full.at[o // 2, :, seg(o % 2)], lambda view, c: [view.at[pl.ds(*parts[c]), :]], gsems, me)
    g.start()
    gates = Swap(lambda peer: wg_t.at[seg(peer, feat), :], lambda o: wgu_ref.at[:feat, seg(o)], gate_sems, me)
    ups = Swap(lambda peer: wu_t.at[seg(peer, feat), :], lambda o: wgu_ref.at[feat:, seg(o)], up_sems, me)

    def advance(n):
        gates.advance(n)
        ups.advance(n)

    def transpose(i):
        wg_t[seg(i, CHUNK), :] = wg_ref[:, seg(i, CHUNK)].T
        wu_t[seg(i, CHUNK), :] = wu_ref[:, seg(i, CHUNK)].T
    for load in loads:
        load.wait()
    loop(wg_ref.shape[1] // CHUNK, transpose)
    advance(0)

    def own_block(i):
        full[me // 2, seg(i, WIDE), seg(me % 2)] = w_ref[seg(i, WIDE), :]
    loop(cols // WIDE, own_block)
    acc[...] = jnp.zeros_like(acc)
    small_all[me] = small_ref[...]
    smalls.wait_recv()
    gain_row(g_scr, small_all, 0)
    norm_rows(x_ref, g_scr, u_scr)

    def keep(mask):
        chip = flipped(me, mask) // 2
        return pltpu.make_async_copy(full.at[chip], w_out.at[chip], osem.at[mask // 2])

    def use(mask):
        g.wait_pair(mask)
        keep(mask).start()
        chip = flipped(me, mask) // 2
        u = u_scr[:, seg(chip, WIDE)]

        def step(i):
            rs = seg(i, cols // 2)
            acc[rs, :] += mm(full[chip, rs, :], u, NT)
        loop(2, step)

    def tables(o):
        angles = freq_ref[...] * small_all[o, 2:3, :]
        cos_ref[:, seg(o)] = jnp.cos(angles)
        sin_ref[:, seg(o)] = jnp.sin(angles)

    for r in range(len(g.ROUNDS)):
        g.round(r)
        if r in (2, 4):
            advance(r // 2)
        if r == 1:
            loop(N_DEV, tables)
        for mask in g.READY[r]:
            use(mask)

    half = hd // 2
    cos, sin = cos_ref[:, seg(me)], sin_ref[:, seg(me)]

    def turn(h):
        first = seg(2 * h, half)
        second = seg(2 * h + 1, half)
        p = acc[first, :].astype(BF16).astype(F32)
        q = acc[second, :].astype(BF16).astype(F32)
        rot[first, :] = (p * cos - q * sin).astype(BF16)
        rot[second, :] = (q * cos + p * sin).astype(BF16)
    loop(q_all // hd, turn)
    for k in range(groups):
        turn(q_all // hd + 2 * k)
        vs = seg(q_all // hd + 2 * k + 1, hd)
        rot[vs, :] = acc[vs, :].astype(BF16)
    per = N_DEV // groups
    q_rows = lambda peer: seg(peer, qw)
    kv_rows = lambda peer: seg(q_all // (2 * hd) + peer // per, 2 * hd)
    qs = Swap(lambda peer: rot.at[q_rows(peer), :], lambda o: qkv_ref.at[:qw, seg(o, tokens)], qsems, me)
    kvs = Swap(lambda peer: rot.at[kv_rows(peer), :], lambda o: qkv_ref.at[qw:, seg(o, tokens)], ksems, me)
    qs.start()
    kvs.start()
    gw.start()
    keep_own(wo_ref, full_w, me)
    gain_row(g_scr, small_all, 1)
    qkv_ref[:qw, seg(me, tokens)] = rot[q_rows(me), :]
    qkv_ref[qw:, seg(me, tokens)] = rot[kv_rows(me), :]
    wgu_ref[:feat, seg(me)] = wg_t[seg(me, feat), :]
    wgu_ref[feat:, seg(me)] = wu_t[seg(me, feat), :]
    gates.start((CORE,))
    ups.start((CORE,))
    for swap in (qs, kvs):
        swap.wait_recv()
    stores = fetch_all(esem, (qkv_ref, qkv_out), (u_scr, u_out), (cos_ref, cos_out), (sin_ref, sin_out))
    heads = qkv_ref.shape[0] // hd - 2
    seq = qkv_ref.shape[1]
    scale = hd ** -0.5
    lanes = heads * QB
    key_rows(k_scr, qkv_ref, qw, hd)

    outs = Swap(lambda peer: o_send.at[seg(peer), :], lambda o: o_tok.at[:, seg(o)], osems, me)

    def q_block(qb):
        for at, r in ((2, 0), (4, 1), (5, 2), (6, 3), (7, 4)):
            @pl.when(qb == at)
            def _():
                gw.round(r)
        qs = seg(qb, QB)
        q2 = side_by_side(qkv_ref, heads, hd, qs)

        def scores(kb, top, diagonal):
            s = score_block(k_scr[seg(kb, KB), :], q2, scale, diagonal)
            s_scr[seg(kb, KB), :] = s
            return jnp.maximum(top, jnp.max(s, axis=0, keepdims=True))

        top = lax.fori_loop(0, qb, lambda kb, t: scores(kb, t, False), jnp.full((1, lanes), NEG_LARGE, F32))
        top = scores(qb, top, True)

        def expo(kb, tot):
            e = jnp.exp(s_scr[seg(kb, KB), :] - top)
            s_scr[seg(kb, KB), :] = e
            return tot + jnp.sum(e, axis=0, keepdims=True)

        inv = 1.0 / lax.fori_loop(0, qb + 1, expo, jnp.zeros((1, lanes), F32))

        def weigh(kb, acc):
            p = (s_scr[seg(kb, KB), :] * inv).astype(BF16)
            return acc + mm(qkv_ref[qw + hd:, seg(kb, KB)], p, NN)

        acc = lax.fori_loop(0, qb + 1, weigh, jnp.zeros((hd, lanes), F32))
        for h in range(heads):
            o_ref[h * hd:(h + 1) * hd, qs] = acc[:, h * QB:(h + 1) * QB].astype(BF16)
        stat_ref[qb, :1, :] = top
        stat_ref[qb, 1:, :] = inv
        o_send[qs, :] = o_ref[:, qs].T

    loop(seq // QB, q_block)
    outs.start()
    advance(3)
    o_tok[:, seg(me)] = o_send[seg(me), :]
    for r in (5, 6):
        gw.round(r)
    outs.wait_recv()
    for mask in CHIP_MASKS:
        gw.wait_pair(mask)

    def project(n):
        cs = seg(n, CHUNK)
        acc_o[:, cs] = mm(o_tok[...], full_w[:, :, cs].reshape(dim, CHUNK), NN)
    loop(dim // CHUNK, project)

    def residual(i):
        rs = seg(i, STRIP)
        h_ref[rs, :] = (x_ref[rs, :].astype(F32) + acc_o[rs, :]).astype(BF16)
    loop(tokens // STRIP, residual)
    norm_rows(h_ref, g_scr, m_ref)
    for swap in (gates, ups):
        swap.wait_recv()
    for mask in CHIP_MASKS:
        keep(mask).wait()
    outs.wait_send()
    for swap in (gates, ups):
        swap.wait_send((CORE,) + SETS[3])
    for store in stores:
        store.wait()
    g.finish()
    gw.finish()
    for swap in (smalls, qs, kvs):
        swap.wait_send()


def dw_swaps(stage, gate_hbm, up_hbm, sems, me):
    feat = gate_hbm.shape[0] // N_DEV
    return [Swap(lambda peer, lo=lo: stage(peer).at[lo:lo + feat, seg(peer % 2)], lambda o, dst=dst: dst.at[seg(o, feat), :], sems[i:i + 2], me)
            for lo, dst, i in ((0, gate_hbm, 0), (feat, up_hbm, 2))]


def mlp(m_ref, dout_ref, wgu_hbm, down_hbm, u_ref, h_ref, small_all, wo_ref, o_ref,
        ucol_ref, m_out, dgu_out, ddown_out, y_ref, dh_ref, do_ref, dwo_ref, dg_ref, gate_hbm, up_hbm,
        wgu_ref, down_ref, glu_ref, dgu_ref, ddown_ref, isem, dsem, full_d, full_m, osem, stage, g_scr, dgu_t, glu_t, free, *scr):
    me = lax.axis_index('sp')
    feat, dim = down_ref.shape
    loads = fetch_all(isem, (wgu_hbm, wgu_ref), (down_hbm, down_ref))
    enter(me, OTHERS)
    sems = scr[4:]
    gd = row_gather(dout_ref, full_d, sems[:4], me, 0)
    gm = row_gather(m_ref, full_m, sems[4:8], me, 2)
    g = row_gather(dh_ref, full_d, sems[8:12], me, 1)
    ucols = Swap(lambda peer: u_ref.at[:, seg(peer)], lambda o: ucol_ref.at[seg(o), :], sems[12:14], me)
    gates, ups = dw_swaps(lambda peer: stage, gate_hbm, up_hbm, sems[14:18], me)
    gm.start()
    gd.start()
    keep_own(m_ref, full_m, me)
    keep_own(dout_ref, full_d, me)
    gain_row(g_scr, small_all, 1)
    dwo_ref[...] = jnp.zeros_like(dwo_ref)
    ddown_ref[...] = jnp.zeros_like(ddown_ref)

    def keep(mask):
        chip = flipped(me, mask) // 2
        ts = seg(chip, WIDE)
        ends = ((full_m.at[chip], m_out.at[chip]), (dgu_ref.at[:, ts], dgu_out.at[:, ts]))
        return [pltpu.make_async_copy(src, dst, osem.at[mask // 2, i]) for i, (src, dst) in enumerate(ends)]

    for load in loads:
        load.wait()
    ucol_ref[seg(me), :] = u_ref[:, seg(me)]

    def use(mask):
        gd.wait_pair(mask)
        gm.wait_pair(mask)
        chip = flipped(me, mask) // 2
        ts = seg(chip, WIDE)
        gu = mm(wgu_ref[...], full_m[chip], NT).astype(BF16).astype(F32)
        gate, up = gu[:feat], gu[feat:]
        d_glu = mm(down_ref[...], full_d[chip], NT).astype(BF16).astype(F32)
        sig = jax.nn.sigmoid(gate)
        act = gate * sig
        glu = (act * up).astype(BF16)
        glu_ref[:, ts] = glu
        dgu_ref[:feat, ts] = (d_glu * up * (sig * (1.0 + gate * (1.0 - sig)))).astype(BF16)
        dgu_ref[feat:, ts] = (d_glu * act).astype(BF16)

        def step(n):
            ddown_ref[:, seg(n, CHUNK)] += mm(glu, full_d[chip, :, seg(n, CHUNK)], NN)
        loop(dim // CHUNK, step)
        for copy in keep(mask):
            copy.start()

    for r in range(len(gm.ROUNDS)):
        gm.round(r)
        gd.round(r)
        if r == 3:
            ucols.start()
        for mask in gm.READY[r]:
            use(mask)
    far = seg(flipped(me, XYZ) // 2, WIDE)
    stage[...] = mm(dgu_ref[...], full_m[:, :, far].reshape(dgu_ref.shape[1], WIDE), NN)
    for swap in (gates, ups):
        swap.start(SETS[0])
    for gather in (gd, gm):
        gather.finish()
    leave = pltpu.make_async_copy(ddown_ref, ddown_out, dsem)
    leave.start()
    s = Scatter(*scr[:4], sems[18:], me)
    total = s.run(block_product(s, dgu_ref, wgu_ref, dgu_t))
    for mask in NEAR:
        pl.semaphore_signal(free, inc=1, device_id=(flipped(me, mask),), device_id_type=MESH)
    norm_back(total, h_ref, g_scr, dout_ref, dh_ref, dg_ref)
    g.start()
    keep_own(dh_ref, full_d, me)
    s.finish()
    pl.semaphore_wait(free, len(NEAR))

    def use_dh(mask):
        g.wait_pair(mask)
        chip = flipped(me, mask) // 2
        do_ref[:, seg(chip, WIDE)] = mm(wo_ref[...], full_d[chip], NT).astype(BF16)
        o = o_ref[:, seg(chip, WIDE)]

        def step(n):
            dwo_ref[:, seg(n, CHUNK)] += mm(o, full_d[chip, :, seg(n, CHUNK)], NN)
        loop(dim // CHUNK, step)

    def between(i):
        r = i if i < 3 else i - N_CHIP + 3
        if i < 3 or i >= N_CHIP:
            g.round(r)
            for mask in g.READY[r]:
                use_dh(mask)

    s = Scatter(*scr[:4], sems[18:], me)
    total = s.run(block_product(s, glu_ref, down_ref, glu_t), between)
    y_ref[...] = (h_ref[...].astype(F32) + total[...]).astype(BF16)
    s.finish()
    g.finish()
    for swap in (gates, ups):
        swap.wait_recv(SETS[0])
        swap.wait_send(SETS[0])
    ucols.wait_recv()
    ucols.wait_send()
    leave.wait()
    ends = ((full_m.at[0], m_out.at[0]), (dgu_ref.at[:, seg(0, WIDE)], dgu_out.at[:, seg(0, WIDE)]))
    loop(N_CHIP, lambda j: [pltpu.make_async_copy(src, dst, osem.at[j, i]).wait() for i, (src, dst) in enumerate(ends)])


def back(groups, hd, qkv_hbm, do_hbm, stat_ref, cos_all, sin_all, dgu_hbm, m_hbm, ucol_ref, w_hbm, x_ref, small_all, dh_ref, dg2_ref, dg_in, du_in,
         dg_hbm, du_hbm, dwq_ref, dwkv_ref, dx_ref, gain_ref,
         dgu_ref, qkv_ref, do_ref, isem,
         p_scr, dp_scr, k_scr, v_scr, dk_acc, dv_acc, stage, dq_scr, dkv_scr, m_scr,
         full, w_scr, shares, dkv_own, full_kv, dqkv, dn, g_scr, dg1, gains, gains_in, wsem, lsem, msem, *sems):
    heads = qkv_ref.shape[0] // hd - 2
    seq = qkv_ref.shape[1]
    scale = hd ** -0.5
    lanes = heads * QB
    qw = heads * hd
    half = hd // 2
    me = lax.axis_index('sp')
    feat = dgu_ref.shape[0] // 2
    first = (X, Y + Z, Y, X + Z, Z, X + Y, 0)

    def fetch(mask):
        cols = seg(flipped(me, mask) // 2, WIDE)
        return pltpu.make_async_copy(m_hbm.at[:, :, cols], m_scr.at[:, :, cols], msem.at[mask // 2])
    for mask in first:
        fetch(mask).start()
    loads = fetch_all(isem, (dgu_hbm, dgu_ref), (qkv_hbm, qkv_ref), (do_hbm, do_ref))
    load = pltpu.make_async_copy(w_hbm, w_scr, wsem)
    load.start()
    enter(me, OTHERS)
    gain_row(g_scr, small_all, 0)

    gates, ups = dw_swaps(lambda peer: stage.at[peer // 2], dg_hbm, du_hbm, sems[:4], me)
    gq = row_gather(dq_scr, full, sems[6:10], me)
    own = [pltpu.make_async_copy(swap.src(me), swap.dst(me), lsem.at[i]) for i, swap in enumerate((gates, ups))]

    def make(mask):
        chip = flipped(me, mask) // 2
        fetch(mask).wait()
        cols = m_scr[:, :, seg(chip, WIDE)].reshape(seq, WIDE)
        stage[chip] = mm(dgu_ref[...], cols, NN)

    def advance(n):
        for swap in (gates, ups):
            if n > 1:
                swap.wait_send(SETS[n - 1])
            swap.start(SETS[n])

    for copy in loads:
        copy.wait()
    for i, mask in enumerate(first):
        make(mask)
        if i == 1:
            advance(1)
    gates.start((CORE,))
    ups.start((CORE,))
    for copy in own:
        copy.start()

    dk_acc[...] = jnp.zeros_like(dk_acc)
    dv_acc[...] = jnp.zeros_like(dv_acc)
    key_rows(k_scr, qkv_ref, qw, hd)
    key_rows(v_scr, qkv_ref, qw + hd, hd)

    def q_block(qb):
        @pl.when(qb == 4)
        def _():
            advance(2)
        qs = seg(qb, QB)
        q2 = side_by_side(qkv_ref, heads, hd, qs)
        do2 = side_by_side(do_ref, heads, hd, qs)
        top = stat_ref[qb, :1, :]
        inv = stat_ref[qb, 1:, :]

        def probs(kb, rd, diagonal):
            ks = seg(kb, KB)
            s = score_block(k_scr[ks, :], q2, scale, diagonal)
            p = jnp.exp(s - top) * inv
            dp = mm(v_scr[ks, :], do2, NN).astype(BF16)
            p_scr[ks, :] = p
            dp_scr[ks, :] = dp
            dv_acc[ks, :] += mm(p.astype(BF16), do2, NT)
            return rd + jnp.sum(dp.astype(F32) * p, axis=0, keepdims=True)

        rd = lax.fori_loop(0, qb, lambda kb, r: probs(kb, r, False), jnp.zeros((1, lanes), F32))
        rd = probs(qb, rd, True)

        def d_scores(kb, acc):
            ks = seg(kb, KB)
            ds = (p_scr[ks, :] * (dp_scr[ks, :].astype(F32) - rd) * scale).astype(BF16)
            dk_acc[ks, :] += mm(ds, q2, NT)
            return acc + mm(qkv_ref[qw:qw + hd, ks], ds, NN)

        acc = lax.fori_loop(0, qb + 1, d_scores, jnp.zeros((hd, lanes), F32))
        cos, sin = cos_all[:, qs], sin_all[:, qs]
        for h in range(heads):
            dq = acc[:, h * QB:(h + 1) * QB].astype(BF16).astype(F32)
            p, q = dq[:half], dq[half:]
            dq_scr[h * hd:h * hd + half, qs] = (p * cos + q * sin).astype(BF16)
            dq_scr[h * hd + half:(h + 1) * hd, qs] = (q * cos - p * sin).astype(BF16)

    loop(seq // QB, q_block)

    def share(i):
        rs = seg(i, WIDE)
        dkv_scr[rs, :] = jnp.concatenate([dk_acc[rs, :], dv_acc[rs, :]], axis=1).astype(BF16)
    loop(seq // WIDE, share)
    tokens = ucol_ref.shape[1]
    per = N_DEV // groups
    q_all = dwq_ref.shape[0]
    sh = Swap(lambda peer: dkv_scr.at[seg(peer, tokens), :], lambda o: shares.at[o], sems[4:6], me)
    parts = thirds(dkv_own.shape[0], STRIP)
    gk = Gather(dkv_own, lambda o: full_kv.at[:, seg(o, tokens)], lambda view, c: [view.at[pl.ds(*parts[c]), :]], sems[10:14], me)
    gs = Swap(lambda peer: gains.at[:, seg(peer)], lambda o: gains_in.at[o], sems[14:], me)
    sh.start()
    gq.start()
    keep_own(dq_scr, full, me)
    shares[me] = dkv_scr[seg(me, tokens), :]
    sh.wait_recv()
    cos, sin = cos_all[:, seg(me)], sin_all[:, seg(me)]
    for k in range(groups):
        both = sum(shares[per * k + i].astype(F32) for i in range(per)).astype(BF16).astype(F32).T
        p, q = both[:half], both[half:hd]
        lo = 2 * hd * k
        dkv_own[lo:lo + half, :] = (p * cos + q * sin).astype(BF16)
        dkv_own[lo + half:lo + hd, :] = (q * cos - p * sin).astype(BF16)
        dkv_own[lo + hd:lo + 2 * hd, :] = both[hd:].astype(BF16)
    gk.start()
    full_kv[:, seg(me, tokens)] = dkv_own[...]
    for k in range(groups):
        dqkv[:, q_all + 2 * hd * k:q_all + 2 * hd * (k + 1)] = dkv_own[2 * hd * k:2 * hd * (k + 1), :].T

    def use(mask):
        gq.wait_pair(mask)
        chip = flipped(me, mask) // 2
        dwq_ref[seg(chip, WIDE), :] = mm(full[chip], ucol_ref[...], NN)
        dqkv[:, seg(chip, WIDE)] = full[chip, :, seg(me, tokens)].T

    for r in range(len(gq.ROUNDS)):
        gq.round(r)
        gk.round(r)
        if r == 3:
            advance(3)
        for mask in gq.READY[r]:
            use(mask)
    load.wait()

    def normed(i):
        dn[:, seg(i, WIDE)] = mm(dqkv[...], w_scr[i], NN)
    loop(N_CHIP, normed)
    norm_back(dn, x_ref, g_scr, dh_ref, dx_ref, dg1)
    gains[...] = jnp.concatenate([jnp.sum(dg1[...], axis=0, keepdims=True), jnp.sum(dg2_ref[...], axis=0, keepdims=True),
                                  jnp.zeros((N_CHIP - 2, dg1.shape[1]), F32)], axis=0)
    gs.start()
    gains_in[me] = gains[:, seg(me)]
    for mask in CHIP_MASKS:
        gk.wait_pair(mask)
    dwkv_ref[...] = mm(full_kv[...], ucol_ref[...], NN)
    gs.wait_recv()
    gain_ref[...] = sum(gains_in[o] for o in range(N_DEV))
    for swap in (gates, ups):
        swap.wait_recv((CORE,) + SETS[1] + SETS[2] + SETS[3])
        swap.wait_send((CORE,) + SETS[3])
    for copy in own:
        copy.wait()
    for c in (sh, gs):
        c.wait_send()
    for g in (gq, gk):
        g.finish()


def finish(dg_hbm, du_hbm, dkv_hbm, *refs):
    n = (len(refs) - 14) // 3
    gains, refs = refs[0], refs[1:]
    srcs, (gate, up, dk, dv, dg1, dg2), refs = refs[:n], refs[n:n + 6], refs[n + 6:]
    dsts, (g_in, g_out, kv_in), holds, sems = refs[:n], refs[n:n + 3], refs[n + 3:2 * n + 3], refs[2 * n + 3:]
    dg1[...] = gains[:1, :]
    dg2[...] = gains[1:2, :]
    t_in, t_out, p_in, p_out = sems
    step = LANE * 11
    cols = g_in.shape[1]
    hd = dk.shape[0] // (kv_in.shape[0] // LANE)
    starts = [(w, i) for i in range(cols // step) for w in range(2)]

    def fetch(w, i):
        rs = pl.ds(i * step, step)
        return pltpu.make_async_copy((dg_hbm, du_hbm)[w].at[rs, :], g_in.at[w, rs, :], t_in.at[w, i])

    def put(w, i):
        cs = pl.ds(i * step, step)
        return pltpu.make_async_copy(g_out.at[w, :, cs], (gate, up)[w].at[:, cs], t_out.at[w, i])
    moves = [(pltpu.make_async_copy(a, h, p_in.at[k]), pltpu.make_async_copy(h, b, p_out.at[k])) for k, (a, h, b) in enumerate(zip(srcs, holds, dsts))]
    kv = pltpu.make_async_copy(dkv_hbm, kv_in, p_in.at[n])
    for w, i in starts:
        fetch(w, i).start()
    kv.start()
    for load, _ in moves:
        load.start()
    for w, i in starts:
        fetch(w, i).wait()

        at = pl.ds(i * step, step)
        g_out[w, :, at] = g_in[w, at, :].T
        put(w, i).start()
    kv.wait()
    for k in range(dk.shape[0] // hd):
        for i, ref in enumerate((dk, dv)):
            ref[k * hd:(k + 1) * hd, :] = kv_in[(2 * k + i) * hd:(2 * k + i + 1) * hd, :]
    for load, store in moves:
        load.wait()
        store.start()
    for w, i in starts:
        put(w, i).wait()
    for _, store in moves:
        store.wait()


def solution(mesh):
    assert mesh.shape['sp'] == N_DEV

    def layer_step(x_in, positions, d_out, norm1_gain, norm2_gain, w_q, w_k, w_v, w_o, w_gate, w_up, w_down):
        tokens, dim = x_in.shape
        seq = tokens * N_DEV
        n_q, hd = w_q.shape[1:]
        n_kv = w_k.shape[1]
        qw = n_q // N_DEV * hd
        rows = w_q.shape[0]
        feat = w_down.shape[0]
        cols = (n_q + 2 * n_kv) * hd
        lanes = qw // hd * QB
        vm = pltpu.VMEM
        full = vm((N_CHIP, WIDE, dim), BF16)
        gain_scr = vm((N_CHIP, dim), F32)
        tok_shapes = 2 * (((tokens, dim), BF16),)
        dw_shapes = 2 * (((feat * N_DEV, rows), F32),)

        inv_freq = 1.0 / (ROPE_BASE ** (jnp.arange(hd // 2, dtype=F32) * (2.0 / hd)))
        freq = jnp.broadcast_to(inv_freq[:, None], (hd // 2, rows))
        row = lambda v: v.reshape(1, rows)
        by_head = lambda w: w.transpose(1, 2, 0).reshape(-1, rows)
        wo_own = w_o.reshape(qw, dim)

        args = (x_in, row(norm1_gain), row(norm2_gain), row(positions), by_head(w_q), by_head(w_k), by_head(w_v), freq, w_gate, w_up, wo_own)
        qkv, u, small_all, wqkv, attn_t, stat, wgu, hidden, mlp_in, cos_all, sin_all = call(
            functools.partial(head, n_kv, hd), 0, len(args),
            (((qw + 2 * hd, seq), BF16), tok_shapes[0], ((N_DEV, N_CHIP, rows), F32), ((N_CHIP, cols, WIDE), BF16),
             ((qw, seq), BF16), ((seq // QB, 2, lanes), F32), ((2 * feat, dim), BF16), *tok_shapes, *(2 * (((hd // 2, seq), F32),))),
            [vm(w_gate.shape, BF16), vm(w_up.shape, BF16), vm((qw, dim), BF16), vm((qw + 2 * hd, seq), BF16), vm((tokens, dim), BF16),
             vm((hd // 2, seq), F32), vm((hd // 2, seq), F32), dma(3), dma(4),
             full, vm((tokens, dim), F32), vm((tokens, dim), BF16), vm((seq, qw), BF16),
             vm((N_CHIP, rows), F32), vm((cols, rows), BF16), vm((N_CHIP, cols, WIDE), BF16), vm((cols, tokens), F32), vm((cols, tokens), BF16), gain_scr,
             vm((feat * N_DEV, rows), BF16), vm((feat * N_DEV, rows), BF16), vm((seq, lanes), F32), vm((seq, hd), BF16), dma(N_CHIP),
             *Gather.sems, *(6 * Swap.sems), *Gather.sems], 4 * qw * seq * seq, far_in=(8, 9, 10), far_out=(0, 1, 3, 9, 10))(*args)
        args = (mlp_in, d_out, wgu, w_down, u, hidden, small_all, wo_own, attn_t)
        u_col, m_full, dgu, d_down, y_out, d_hidden, d_attn, d_wo, d_g2, d_gate_t, d_up_t = call(
            mlp, 1, len(args),
            (((seq, rows), BF16), ((N_CHIP, WIDE, dim), BF16), ((2 * feat, seq), BF16), ((feat, dim), F32),
             *tok_shapes, ((qw, seq), BF16), ((qw, dim), F32), ((N_CHIP, dim), F32), *dw_shapes),
            [vm((2 * feat, dim), BF16), vm((feat, dim), BF16),
             vm((feat, seq), BF16), vm((2 * feat, seq), BF16), vm((feat, dim), F32), dma(2), dma(),
             full, full, dma(N_CHIP, 2), vm((2 * feat, WIDE), F32), gain_scr, vm((WIDE, 2 * feat), BF16), vm((WIDE, feat), BF16), pltpu.SemaphoreType.REGULAR,
             *Scatter.scratch(tokens, dim), *(3 * Gather.sems), *(3 * Swap.sems), *Scatter.sems], 12 * feat * seq * dim,
            far_in=(2, 3), far_out=(1, 2, 3, 9, 10))(*args)
        args = (qkv, d_attn, stat, cos_all, sin_all, dgu, m_full, u_col, wqkv, x_in, small_all, d_hidden, d_g2, d_gate_t, d_up_t)
        d_gate_t, d_up_t, d_wq, d_wkv, d_x, gains = call(
            functools.partial(back, n_kv, hd), 3, len(args),
            (*dw_shapes, ((n_q * hd, rows), F32), ((2 * n_kv * hd, rows), F32), tok_shapes[0], ((N_CHIP, rows), F32)),
            [vm((2 * feat, seq), BF16), vm((qw + 2 * hd, seq), BF16), vm((qw, seq), BF16), dma(3),
             vm((seq, lanes), F32), vm((seq, lanes), BF16), vm((seq, hd), BF16), vm((seq, hd), BF16), vm((seq, hd), F32), vm((seq, hd), F32),
             vm((N_CHIP, 2 * feat, WIDE), F32), vm((qw, seq), BF16), vm((seq, 2 * hd), BF16), full,
             full, vm((N_CHIP, cols, WIDE), BF16), vm((N_DEV, tokens, 2 * hd), BF16), vm((2 * n_kv * hd, tokens), BF16), vm((2 * n_kv * hd, seq), BF16),
             vm((tokens, cols), BF16), vm((tokens, dim), F32), gain_scr, gain_scr, gain_scr, vm((N_DEV, N_CHIP, rows), F32), dma(), dma(2), dma(N_CHIP),
             *(3 * Swap.sems), *(2 * Gather.sems), *Swap.sems], 10 * qw * seq * seq, far_in=(0, 1, 5, 6, 8, 13, 14), far_out=(0, 1), aliases={13: 0, 14: 1})(*args)
        moved = (d_wq, d_wo, d_down, d_x, y_out)
        one_row = jax.ShapeDtypeStruct((1, rows), F32)
        half_kv = jax.ShapeDtypeStruct((n_kv * hd, rows), F32)
        wide = jax.ShapeDtypeStruct((rows, feat * N_DEV), F32)
        d_gate, d_up, d_wk, d_wv, d_g1, d_g2, d_wq, d_wo, d_down, d_x, y_out = pl.pallas_call(
            finish,
            out_shape=[wide, wide, half_kv, half_kv, one_row, one_row] + [jax.ShapeDtypeStruct(v.shape, v.dtype) for v in moved],
            in_specs=[IN_HBM] * 3 + on_chip(1) + [IN_HBM] * len(moved), out_specs=[IN_HBM] * 2 + on_chip(4) + [IN_HBM] * len(moved),
            scratch_shapes=[vm((2, feat * N_DEV, rows), F32), vm((2, rows, feat * N_DEV), F32), vm(d_wkv.shape, F32)]
            + [vm(v.shape, v.dtype) for v in moved] + [dma(2, 4), dma(2, 4), dma(len(moved) + 1), dma(len(moved))],
            compiler_params=pltpu.CompilerParams(vmem_limit_bytes=VMEM_CAP), name='finish',
        )(d_gate_t, d_up_t, d_wkv, gains, *moved)
        by_row = lambda g, heads: g.reshape(heads, hd, rows).transpose(2, 0, 1)
        return (y_out, d_x, d_g1.reshape(rows), d_g2.reshape(rows), by_row(d_wq, n_q), by_row(d_wk, n_kv), by_row(d_wv, n_kv),
                d_wo.reshape(w_o.shape), d_gate, d_up, d_down)

    all_rows = P('sp')
    return jax.shard_map(layer_step, mesh=mesh, in_specs=(all_rows,) * 12, out_specs=(all_rows,) * 11, check_vma=False)
```

```python
import functools
import jax
import jax.numpy as jnp
from jax import lax
from jax.experimental import pallas as pl
from jax.experimental.pallas import tpu as pltpu
from jax.sharding import PartitionSpec as P

ROPE_BASE = 10000.0
NORM_EPS = 1e-5
NEG_LARGE = -1e30
F32 = jnp.float32
BF16 = jnp.bfloat16
N_DEV, N_CHIP, LANE, WIDE, CHUNK, STRIP = 16, 8, 128, 256, 512, 16
NT = (((1,), (1,)), ((), ()))
TN = (((0,), (0,)), ((), ()))
NN = (((1,), (0,)), ((), ()))
MESH = pl.DeviceIdType.MESH
VMEM_CAP = 62 * 1024 * 1024

CORE, X, Y, Z = 1, 2, 4, 8
XYZ = X + Y + Z
ORDERS = ((X, Y, Z), (Y, Z, X), (Z, X, Y))
CHIP_MASKS = (0, X, Y, Z, X + Y, X + Z, Y + Z, XYZ)
NEAR = (CORE, X, Y, Z)
OTHERS = range(1, N_DEV)
SETS = tuple(tuple(m + c for m in masks for c in (0, CORE)) for masks in ((XYZ,), (X, Y + Z), (Y, X + Z), (Z, X + Y)))
N_COL = len(ORDERS)
COLOURS = range(N_COL)


def mm(a, b, dims):
    return lax.dot_general(a, b, dims, preferred_element_type=F32)


def seg(index, width=LANE):
    return pl.ds(pl.multiple_of(index * width, width), width)


def loop(count, body):
    lax.fori_loop(0, count, lambda i, c: (body(i), c)[1], 0)


def differing(index, mask):
    return sum(((index // bit + mask // bit) % 2) * bit for bit in NEAR)


def flipped(index, mask):
    out = index
    for bit in NEAR:
        if mask & bit:
            out = out + (1 - 2 * ((index // bit) % 2)) * bit
    return out


def thirds(total, unit):
    n = total // unit
    first = (n + 2) // 3
    second = (n - first + 1) // 2
    sizes = (first * unit, second * unit, (n - first - second) * unit)
    return ((0, sizes[0]), (sizes[0], sizes[1]), (sizes[0] + sizes[1], sizes[2]))


def pieces(rows, cols, unit):
    share = cols // LANE // N_COL * LANE
    strips = thirds(rows, unit)
    rest = cols - N_COL * share
    return [[(pl.ds(0, rows), pl.ds(c * share, share)), (pl.ds(*strips[c]), pl.ds(N_COL * share, rest))] for c in COLOURS]


def enter(me, masks):
    barrier = pltpu.get_barrier_semaphore()
    for mask in masks:
        pl.semaphore_signal(barrier, inc=1, device_id=(flipped(me, mask),), device_id_type=MESH)
    pl.semaphore_wait(barrier, len(masks))


def remote(src, dst, send, recv, peer):
    return pltpu.make_async_remote_copy(src_ref=src, dst_ref=dst, send_sem=send, recv_sem=recv, device_id=(peer,), device_id_type=MESH)


def dma(*shape):
    return pltpu.SemaphoreType.DMA(shape)


class Swap:
    sems = (dma(N_DEV), dma(N_DEV))

    def __init__(self, src, dst, sems, me):
        self.src, self.dst, (self.send, self.recv), self.me = src, dst, sems, me

    def copy(self, mask):
        peer = differing(self.me, mask)
        return remote(self.src(peer), self.dst(self.me), self.send.at[mask], self.recv.at[mask], peer)

    def arrival(self, mask):
        view = self.dst(differing(self.me, mask))
        return remote(view, view, self.send.at[mask], self.recv.at[mask], self.me)

    def each(self, masks, act):
        if masks is None:
            loop(N_DEV - 1, lambda i: act(i + 1))
        else:
            for mask in masks:
                act(mask)

    def start(self, masks=None):
        self.each(masks, lambda mask: self.copy(mask).start())

    def advance(self, n):
        if n:
            self.wait_send(SETS[n - 1])
        self.start(SETS[n])

    def wait_recv(self, masks=None):
        self.each(masks, lambda mask: self.arrival(mask).wait_recv())

    def wait_send(self, masks=None):
        self.each(masks, lambda mask: self.copy(mask).wait_send())


class Gather:
    ROUNDS = ((0,), (1,), (2,), (0, 1), (0, 2), (1, 2), (0, 1, 2))
    READY = ((0,), (), (), (X, Y), (Z,), (X + Y, X + Z), (Y + Z, XYZ))
    sems = (dma(N_COL, N_CHIP, 2), dma(N_COL, N_CHIP, 2), dma(N_CHIP), dma(N_CHIP))

    def __init__(self, own, block, cut, sems, me):
        self.own, self.block, self.cut, self.me = own, block, cut, me
        self.send, self.recv, self.pair_send, self.pair_recv = sems

    def source(self, mask):
        return self.block(flipped(self.me, mask)) if mask else self.own

    def unit(self, colour, mask, axis):
        ends = zip(self.cut(self.source(mask), colour), self.cut(self.block(flipped(self.me, mask)), colour))
        j = self.sends(colour).index((mask, axis))
        return [remote(src, dst, self.send.at[colour, j, i], self.recv.at[colour, (mask + axis) // 2, i],
                       flipped(self.me, axis)) for i, (src, dst) in enumerate(ends)]

    def sends(self, colour):
        return [(0, axis) for axis in ORDERS[colour]] + [step[1:] for step in self.onward(colour)]

    def start_unit(self, colour, mask, axis):
        for copy in self.unit(colour, mask, axis):
            copy.start()

    def pair(self, mask):
        return remote(self.source(mask), self.block(flipped(self.me, mask)), self.pair_send.at[mask // 2],
                      self.pair_recv.at[mask // 2], flipped(self.me, CORE))

    def wait_pair(self, mask):
        view = self.block(flipped(self.me, mask + CORE))
        remote(view, view, self.pair_send.at[mask // 2], self.pair_recv.at[mask // 2], self.me).wait_recv()

    def onward(self, colour):
        order = ORDERS[colour]
        for picks in self.ROUNDS:
            for axis in order[picks[-1] + 1:]:
                yield picks, sum(order[p] for p in picks), axis

    def start(self):
        for pos in COLOURS:
            for colour in COLOURS:
                self.start_unit(colour, 0, ORDERS[colour][pos])
        self.pair(0).start()

    def round(self, r):
        for colour in COLOURS:
            mask = sum(ORDERS[colour][p] for p in self.ROUNDS[r])
            for i, view in enumerate(self.cut(self.block(flipped(self.me, mask)), colour)):
                remote(view, view, self.send.at[colour, 0, i], self.recv.at[colour, mask // 2, i], self.me).wait_recv()
            for picks, at, axis in self.onward(colour):
                if picks == self.ROUNDS[r]:
                    self.start_unit(colour, at, axis)
        for mask in {2: (X, Y, Z), 5: (X + Y, X + Z, Y + Z), 6: (XYZ,)}.get(r, ()):
            self.pair(mask).start()

    def finish(self):
        for colour in COLOURS:
            for i, view in enumerate(self.cut(self.own, colour)):
                loop(len(self.sends(colour)), lambda j: remote(view, view, self.send.at[colour, j, i], self.recv.at[colour, j, i], self.me).wait_send())
        loop(N_CHIP, lambda j: remote(self.own, self.own, self.pair_send.at[j], self.pair_recv.at[j], self.me).wait_send())


def row_gather(own, full, sems, me, extra=None):
    rows, width = own.shape
    parts = pieces(rows, width, STRIP)
    if extra is not None:
        share = width // LANE // N_COL * LANE
        more = width - N_COL * share
        parts = [[(pl.ds(0, rows), pl.ds(c * share + more * (c > extra), share + more * (c == extra)))] for c in COLOURS]

    def block(o):
        return full.at[o // 2, seg(o % 2), :]

    return Gather(own, block, lambda view, c: [view.at[rs, cs] for rs, cs in parts[c]], sems, me)


def keep_own(own, full, me):
    def step(i):
        full[me // 2, pl.ds(pl.multiple_of((me % 2) * LANE + i * STRIP, STRIP), STRIP), :] = own[seg(i, STRIP), :]
    loop(LANE // STRIP, step)


class Scatter:
    ORDER = (XYZ, X + Y, Y + Z, X + Z, X, Y, Z, 0)
    sems = (dma(N_CHIP), dma(N_CHIP), dma(N_COL, N_CHIP, 2), dma(N_COL, N_CHIP, 2))

    @staticmethod
    def scratch(tokens, dim):
        return [pltpu.VMEM((n, tokens, dim), F32) for n in (N_CHIP, 2, N_CHIP, N_CHIP - 1)]

    def __init__(self, part, other, pair_in, link_in, sems, me):
        self.part, self.other, self.pair_in, self.link_in, self.me = part, other, pair_in, link_in, me
        self.pair_send, self.pair_recv, self.link_send, self.link_recv = sems
        self.tokens, self.dim = part.shape[1:]
        self.pieces = pieces(self.tokens, self.dim, STRIP // 2)
        self.ready, self.sent = set(), [0] * N_COL

    @staticmethod
    def first(colour, mask):
        return next((i for i, a in enumerate(ORDERS[colour]) if mask & a), 3)

    def slot(self, colour, mask, axis):
        slots = [(m, a) for m in self.ORDER for a in ORDERS[colour][:self.first(colour, m)]]
        return slots.index((mask, axis))

    def pair(self, i):
        return remote(self.other.at[i % 2], self.pair_in.at[i], self.pair_send.at[i], self.pair_recv.at[i], flipped(self.me, CORE))

    def link(self, colour, mask):
        axis = ORDERS[colour][self.first(colour, mask)]
        slot = self.slot(colour, mask - axis, axis)
        i = self.ORDER.index(mask)
        return [remote(self.part.at[i, rs, cs], self.link_in.at[slot, rs, cs], self.link_send.at[colour, i, k],
                       self.link_recv.at[colour, slot, k], flipped(self.me, axis)) for k, (rs, cs) in enumerate(self.pieces[colour])]

    def start_link(self, colour, mask):
        for copy in self.link(colour, mask):
            copy.start()

    def add(self, mask, ref, cs):
        i = self.ORDER.index(mask)

        def step(r):
            rs = seg(r, STRIP)
            self.part[i, rs, cs] += ref[rs, cs]
        loop(self.tokens // STRIP, step)

    def finish_pair(self, i):
        self.pair(i).wait_recv()
        self.add(self.ORDER[i], self.pair_in.at[i], pl.ds(0, self.dim))
        self.ready.add(self.ORDER[i])
        for colour in COLOURS:
            a, b, c = ORDERS[colour]
            todo = (XYZ, a + b, a + c, a)
            while self.sent[colour] < len(todo) and todo[self.sent[colour]] in self.ready:
                self.start_link(colour, todo[self.sent[colour]])
                self.sent[colour] += 1

    def take(self, colour, mask, axis):
        for copy in self.link(colour, mask + axis):
            copy.wait_recv()
        ref = self.link_in.at[self.slot(colour, mask, axis)]
        (_, wide), (rs, cs) = self.pieces[colour]
        self.add(mask, ref, wide)
        self.part[self.ORDER.index(mask), rs, cs] += ref[rs, cs]

    def run(self, product, between=lambda i: None):
        for i, mask in enumerate(self.ORDER):
            if i > 1:
                self.pair(i - 2).wait_send()
            product(i, flipped(self.me, mask) // 2)
            self.pair(i).start()
            if i:
                self.finish_pair(i - 1)
            between(i)
        self.finish_pair(N_CHIP - 1)
        for step in range(2):
            between(N_CHIP + step)
            for colour in COLOURS:
                a, b, c = ORDERS[colour]
                mask = (b + c, b)[step]
                self.take(colour, mask, a)
                self.start_link(colour, mask)
        between(N_CHIP + 2)
        for colour in COLOURS:
            a, b, c = ORDERS[colour]
            self.take(colour, c, a)
            self.take(colour, c, b)
            self.start_link(colour, c)
        between(N_CHIP + 3)
        for colour in COLOURS:
            for axis in ORDERS[colour]:
                self.take(colour, 0, axis)
        return self.part.at[N_CHIP - 1]

    def finish(self):
        for i in (N_CHIP - 2, N_CHIP - 1):
            self.pair(i).wait_send()
        for colour in COLOURS:
            for k, (rs, cs) in enumerate(self.pieces[colour]):
                view = self.part.at[0, rs, cs]
                loop(N_CHIP - 1, lambda i: remote(view, view, self.link_send.at[colour, i, k], self.link_recv.at[colour, i, k], self.me).wait_send())


def block_product(s, a_ref, w_ref, a_t):
    core = s.me % 2

    def product(i, chip):
        a_t[...] = a_ref[:, seg(chip, WIDE)].T

        def step(n):
            cs = seg(n, CHUNK)
            s.other[i % 2, :, cs] = mm(a_t[seg(1 - core), :], w_ref[:, cs], NN)
            s.part[i, :, cs] = mm(a_t[seg(core), :], w_ref[:, cs], NN)
        loop(s.dim // CHUNK, step)
    return product


def on_chip(n):
    return [pl.BlockSpec(memory_space=pltpu.VMEM)] * n


IN_HBM = pl.BlockSpec(memory_space=pl.ANY)


def call(kernel, ident, args, outs, scratch, flops, far_in=(), far_out=(), aliases={}):
    specs = [IN_HBM if i in far_in else on_chip(1)[0] for i in range(args)]
    out_specs = [IN_HBM if i in far_out else on_chip(1)[0] for i in range(len(outs))]
    return pl.pallas_call(
        kernel,
        out_shape=[jax.ShapeDtypeStruct(shape, dtype) for shape, dtype in outs],
        in_specs=specs, out_specs=out_specs, scratch_shapes=scratch, input_output_aliases=aliases,
        cost_estimate=pl.CostEstimate(flops=flops, bytes_accessed=flops // CHUNK, transcendentals=0),
        compiler_params=pltpu.CompilerParams(collective_id=ident, has_side_effects=True, vmem_limit_bytes=VMEM_CAP),
        name=kernel.func.__name__ if isinstance(kernel, functools.partial) else kernel.__name__,
    )


def fetch_all(sem, *pairs):
    copies = [pltpu.make_async_copy(src, dst, sem.at[i]) for i, (src, dst) in enumerate(pairs)]
    for copy in copies:
        copy.start()
    return copies


def gain_row(dst, small_all, which):
    for o in range(N_DEV):
        dst[:1, o * LANE:(o + 1) * LANE] = small_all[o, which:which + 1, :]


def norm_rows(src, gain, dst):
    def step(i):
        rs = seg(i, STRIP)
        t = src[rs, :].astype(F32)
        dst[rs, :] = (t * lax.rsqrt(jnp.mean(t * t, axis=-1, keepdims=True) + NORM_EPS) * gain[:1, :]).astype(BF16)
    loop(src.shape[0] // STRIP, step)


def norm_back(dy, src, gain, skip, dst, dgain):
    def step(i):
        rs = seg(i, STRIP)
        d = dy[rs, :].astype(BF16).astype(F32)
        t = src[rs, :].astype(F32)
        inv = lax.rsqrt(jnp.mean(t * t, axis=-1, keepdims=True) + NORM_EPS)
        gd = gain[:1, :] * d
        pull = jnp.mean(gd * t, axis=-1, keepdims=True)
        dst[rs, :] = (skip[rs, :].astype(F32) + (inv * gd - t * (inv * inv * inv * pull))).astype(BF16)
        g = d * (t * inv)
        dgain[...] += g[:N_CHIP] + g[N_CHIP:]
    dgain[...] = jnp.zeros_like(dgain)
    loop(src.shape[0] // STRIP, step)


QB = 256
KB = 256


def key_rows(dst, src, lo, hd):
    def step(i):
        dst[seg(i, KB), :] = src[lo:lo + hd, seg(i, KB)].T
    loop(src.shape[1] // KB, step)


def score_block(k, q2, scale, diagonal):
    s = mm(k, q2, NN) * scale
    if diagonal:
        key = lax.broadcasted_iota(jnp.int32, s.shape, 0)
        qry = lax.broadcasted_iota(jnp.int32, s.shape, 1) % QB
        s = jnp.where(qry >= key, s, NEG_LARGE)
    return s


def side_by_side(ref, heads, hd, qs):
    return jnp.concatenate([ref[h * hd:(h + 1) * hd, qs] for h in range(heads)], axis=1)


def head(groups, hd, x_ref, g1_ref, g2_ref, pos_ref, wq_ref, wk_ref, wv_ref, freq_ref, wg_hbm, wu_hbm, wo_hbm, qkv_out, u_out, small_all, w_out, o_ref, stat_ref, wgu_ref, h_ref, m_ref, cos_out, sin_out,
         wg_ref, wu_ref, wo_ref, qkv_ref, u_scr, cos_ref, sin_ref, isem, esem,
         full_w, acc_o, o_tok, o_send, small_ref, w_ref, full, acc, rot, g_scr, wg_t, wu_t, s_scr, k_scr, osem, *sems):
    me = lax.axis_index('sp')
    tokens, dim = x_ref.shape
    cols = w_ref.shape[0]
    small_ref[...] = jnp.concatenate([r[...].astype(F32) for r in (g1_ref, g2_ref, pos_ref)] + [jnp.zeros((N_CHIP - 3, LANE), F32)], axis=0)
    w_ref[:wq_ref.shape[0], :] = wq_ref[...]
    for k in range(groups):
        for i, ref in enumerate((wk_ref, wv_ref)):
            w_ref[pl.ds(wq_ref.shape[0] + (2 * k + i) * hd, hd), :] = ref[k * hd:(k + 1) * hd, :]
    qw = tokens
    q_all = N_DEV * qw
    gsems, ssems, qsems, ksems, gate_sems, up_sems, osems = sems[:4], *(sems[i:i + 2] for i in range(4, len(sems) - 4, 2))
    gw = row_gather(wo_ref, full_w, sems[-4:], me, 1)
    feat = wg_ref.shape[1] // N_DEV
    loads = fetch_all(isem, (wg_hbm, wg_ref), (wu_hbm, wu_ref), (wo_hbm, wo_ref))
    enter(me, OTHERS)
    smalls = Swap(lambda peer: small_ref, lambda o: small_all.at[o], ssems, me)
    smalls.start()
    parts = thirds(cols, STRIP)
    g = Gather(w_ref, lambda o: full.at[o // 2, :, seg(o % 2)], lambda view, c: [view.at[pl.ds(*parts[c]), :]], gsems, me)
    g.start()
    gates = Swap(lambda peer: wg_t.at[seg(peer, feat), :], lambda o: wgu_ref.at[:feat, seg(o)], gate_sems, me)
    ups = Swap(lambda peer: wu_t.at[seg(peer, feat), :], lambda o: wgu_ref.at[feat:, seg(o)], up_sems, me)

    def advance(n):
        gates.advance(n)
        ups.advance(n)

    def transpose(i):
        wg_t[seg(i, CHUNK), :] = wg_ref[:, seg(i, CHUNK)].T
        wu_t[seg(i, CHUNK), :] = wu_ref[:, seg(i, CHUNK)].T
    for load in loads:
        load.wait()
    loop(wg_ref.shape[1] // CHUNK, transpose)
    advance(0)

    def own_block(i):
        full[me // 2, seg(i, WIDE), seg(me % 2)] = w_ref[seg(i, WIDE), :]
    loop(cols // WIDE, own_block)
    acc[...] = jnp.zeros_like(acc)
    small_all[me] = small_ref[...]
    smalls.wait_recv()
    gain_row(g_scr, small_all, 0)
    norm_rows(x_ref, g_scr, u_scr)

    def keep(mask):
        chip = flipped(me, mask) // 2
        return pltpu.make_async_copy(full.at[chip], w_out.at[chip], osem.at[mask // 2])

    def use(mask):
        g.wait_pair(mask)
        keep(mask).start()
        chip = flipped(me, mask) // 2
        u = u_scr[:, seg(chip, WIDE)]

        def step(i):
            rs = seg(i, cols // 2)
            acc[rs, :] += mm(full[chip, rs, :], u, NT)
        loop(2, step)

    def tables(o):
        angles = freq_ref[...] * small_all[o, 2:3, :]
        cos_ref[:, seg(o)] = jnp.cos(angles)
        sin_ref[:, seg(o)] = jnp.sin(angles)

    for r in range(len(g.ROUNDS)):
        g.round(r)
        if r in (2, 5):
            advance(r // 2)
        if r == 1:
            loop(N_DEV, tables)
        for mask in g.READY[r]:
            use(mask)

    half = hd // 2
    cos, sin = cos_ref[:, seg(me)], sin_ref[:, seg(me)]

    def turn(h):
        first = seg(2 * h, half)
        second = seg(2 * h + 1, half)
        p = acc[first, :].astype(BF16).astype(F32)
        q = acc[second, :].astype(BF16).astype(F32)
        rot[first, :] = (p * cos - q * sin).astype(BF16)
        rot[second, :] = (q * cos + p * sin).astype(BF16)
    loop(q_all // hd, turn)
    for k in range(groups):
        turn(q_all // hd + 2 * k)
        vs = seg(q_all // hd + 2 * k + 1, hd)
        rot[vs, :] = acc[vs, :].astype(BF16)
    per = N_DEV // groups
    q_rows = lambda peer: seg(peer, qw)
    kv_rows = lambda peer: seg(q_all // (2 * hd) + peer // per, 2 * hd)
    qs = Swap(lambda peer: rot.at[q_rows(peer), :], lambda o: qkv_ref.at[:qw, seg(o, tokens)], qsems, me)
    kvs = Swap(lambda peer: rot.at[kv_rows(peer), :], lambda o: qkv_ref.at[qw:, seg(o, tokens)], ksems, me)
    qs.start()
    kvs.start()
    gw.start()
    keep_own(wo_ref, full_w, me)
    gain_row(g_scr, small_all, 1)
    qkv_ref[:qw, seg(me, tokens)] = rot[q_rows(me), :]
    qkv_ref[qw:, seg(me, tokens)] = rot[kv_rows(me), :]
    wgu_ref[:feat, seg(me)] = wg_t[seg(me, feat), :]
    wgu_ref[feat:, seg(me)] = wu_t[seg(me, feat), :]
    gates.start((CORE,))
    ups.start((CORE,))
    for swap in (qs, kvs):
        swap.wait_recv()
    stores = fetch_all(esem, (qkv_ref, qkv_out), (u_scr, u_out), (cos_ref, cos_out), (sin_ref, sin_out))
    heads = qkv_ref.shape[0] // hd - 2
    seq = qkv_ref.shape[1]
    scale = hd ** -0.5
    lanes = heads * QB
    key_rows(k_scr, qkv_ref, qw, hd)

    outs = Swap(lambda peer: o_send.at[seg(peer), :], lambda o: o_tok.at[:, seg(o)], osems, me)

    def q_block(qb):
        for at, r in ((2, 0), (4, 1), (5, 2), (6, 3), (7, 4)):
            @pl.when(qb == at)
            def _():
                gw.round(r)
        qs = seg(qb, QB)
        q2 = side_by_side(qkv_ref, heads, hd, qs)

        def scores(kb, top, diagonal):
            s = score_block(k_scr[seg(kb, KB), :], q2, scale, diagonal)
            s_scr[seg(kb, KB), :] = s
            return jnp.maximum(top, jnp.max(s, axis=0, keepdims=True))

        top = lax.fori_loop(0, qb, lambda kb, t: scores(kb, t, False), jnp.full((1, lanes), NEG_LARGE, F32))
        top = scores(qb, top, True)

        def expo(kb, tot):
            e = jnp.exp(s_scr[seg(kb, KB), :] - top)
            s_scr[seg(kb, KB), :] = e
            return tot + jnp.sum(e, axis=0, keepdims=True)

        inv = 1.0 / lax.fori_loop(0, qb + 1, expo, jnp.zeros((1, lanes), F32))

        def weigh(kb, acc):
            p = (s_scr[seg(kb, KB), :] * inv).astype(BF16)
            return acc + mm(qkv_ref[qw + hd:, seg(kb, KB)], p, NN)

        acc = lax.fori_loop(0, qb + 1, weigh, jnp.zeros((hd, lanes), F32))
        for h in range(heads):
            o_ref[h * hd:(h + 1) * hd, qs] = acc[:, h * QB:(h + 1) * QB].astype(BF16)
        stat_ref[qb, :1, :] = top
        stat_ref[qb, 1:, :] = inv
        o_send[qs, :] = o_ref[:, qs].T

    loop(seq // QB, q_block)
    outs.start()
    advance(3)
    o_tok[:, seg(me)] = o_send[seg(me), :]
    for r in (5, 6):
        gw.round(r)
    outs.wait_recv()
    for mask in CHIP_MASKS:
        gw.wait_pair(mask)

    def project(n):
        cs = seg(n, CHUNK)
        acc_o[:, cs] = mm(o_tok[...], full_w[:, :, cs].reshape(dim, CHUNK), NN)
    loop(dim // CHUNK, project)

    def residual(i):
        rs = seg(i, STRIP)
        h_ref[rs, :] = (x_ref[rs, :].astype(F32) + acc_o[rs, :]).astype(BF16)
    loop(tokens // STRIP, residual)
    norm_rows(h_ref, g_scr, m_ref)
    for swap in (gates, ups):
        swap.wait_recv()
    for mask in CHIP_MASKS:
        keep(mask).wait()
    outs.wait_send()
    for swap in (gates, ups):
        swap.wait_send((CORE,) + SETS[3])
    for store in stores:
        store.wait()
    g.finish()
    gw.finish()
    for swap in (smalls, qs, kvs):
        swap.wait_send()


def dw_swaps(stage, gate_hbm, up_hbm, sems, me):
    feat = gate_hbm.shape[0] // N_DEV
    return [Swap(lambda peer, lo=lo: stage(peer).at[lo:lo + feat, seg(peer % 2)], lambda o, dst=dst: dst.at[seg(o, feat), :], sems[i:i + 2], me)
            for lo, dst, i in ((0, gate_hbm, 0), (feat, up_hbm, 2))]


def mlp(m_ref, dout_ref, wgu_hbm, down_hbm, u_ref, h_ref, small_all, wo_ref, o_ref,
        ucol_ref, m_out, dgu_out, ddown_out, y_ref, dh_ref, do_ref, dwo_ref, dg_ref, gate_hbm, up_hbm,
        wgu_ref, down_ref, glu_ref, dgu_ref, ddown_ref, isem, dsem, full_d, full_m, osem, stage, g_scr, dgu_t, glu_t, free, *scr):
    me = lax.axis_index('sp')
    feat, dim = down_ref.shape
    loads = fetch_all(isem, (wgu_hbm, wgu_ref), (down_hbm, down_ref))
    enter(me, OTHERS)
    sems = scr[4:]
    gd = row_gather(dout_ref, full_d, sems[:4], me, 0)
    gm = row_gather(m_ref, full_m, sems[4:8], me, 2)
    g = row_gather(dh_ref, full_d, sems[8:12], me, 1)
    ucols = Swap(lambda peer: u_ref.at[:, seg(peer)], lambda o: ucol_ref.at[seg(o), :], sems[12:14], me)
    gates, ups = dw_swaps(lambda peer: stage, gate_hbm, up_hbm, sems[14:18], me)
    gm.start()
    gd.start()
    keep_own(m_ref, full_m, me)
    keep_own(dout_ref, full_d, me)
    gain_row(g_scr, small_all, 1)
    dwo_ref[...] = jnp.zeros_like(dwo_ref)
    ddown_ref[...] = jnp.zeros_like(ddown_ref)

    def keep(mask):
        chip = flipped(me, mask) // 2
        ts = seg(chip, WIDE)
        ends = ((full_m.at[chip], m_out.at[chip]), (dgu_ref.at[:, ts], dgu_out.at[:, ts]))
        return [pltpu.make_async_copy(src, dst, osem.at[mask // 2, i]) for i, (src, dst) in enumerate(ends)]

    for load in loads:
        load.wait()
    ucol_ref[seg(me), :] = u_ref[:, seg(me)]

    def use(mask):
        gd.wait_pair(mask)
        gm.wait_pair(mask)
        chip = flipped(me, mask) // 2
        ts = seg(chip, WIDE)
        gu = mm(wgu_ref[...], full_m[chip], NT).astype(BF16).astype(F32)
        gate, up = gu[:feat], gu[feat:]
        d_glu = mm(down_ref[...], full_d[chip], NT).astype(BF16).astype(F32)
        sig = jax.nn.sigmoid(gate)
        act = gate * sig
        glu = (act * up).astype(BF16)
        glu_ref[:, ts] = glu
        dgu_ref[:feat, ts] = (d_glu * up * (sig * (1.0 + gate * (1.0 - sig)))).astype(BF16)
        dgu_ref[feat:, ts] = (d_glu * act).astype(BF16)

        def step(n):
            ddown_ref[:, seg(n, CHUNK)] += mm(glu, full_d[chip, :, seg(n, CHUNK)], NN)
        loop(dim // CHUNK, step)
        for copy in keep(mask):
            copy.start()

    for r in range(len(gm.ROUNDS)):
        gm.round(r)
        gd.round(r)
        if r == 3:
            ucols.start()
        for mask in gm.READY[r]:
            use(mask)
    far = seg(flipped(me, XYZ) // 2, WIDE)
    stage[...] = mm(dgu_ref[...], full_m[:, :, far].reshape(dgu_ref.shape[1], WIDE), NN)
    for swap in (gates, ups):
        swap.start(SETS[0])
    for gather in (gd, gm):
        gather.finish()
    leave = pltpu.make_async_copy(ddown_ref, ddown_out, dsem)
    leave.start()
    s = Scatter(*scr[:4], sems[18:], me)
    total = s.run(block_product(s, dgu_ref, wgu_ref, dgu_t))
    for mask in NEAR:
        pl.semaphore_signal(free, inc=1, device_id=(flipped(me, mask),), device_id_type=MESH)
    norm_back(total, h_ref, g_scr, dout_ref, dh_ref, dg_ref)
    g.start()
    keep_own(dh_ref, full_d, me)
    s.finish()
    pl.semaphore_wait(free, len(NEAR))

    def use_dh(mask):
        g.wait_pair(mask)
        chip = flipped(me, mask) // 2
        do_ref[:, seg(chip, WIDE)] = mm(wo_ref[...], full_d[chip], NT).astype(BF16)
        o = o_ref[:, seg(chip, WIDE)]

        def step(n):
            dwo_ref[:, seg(n, CHUNK)] += mm(o, full_d[chip, :, seg(n, CHUNK)], NN)
        loop(dim // CHUNK, step)

    def between(i):
        r = i if i < 3 else i - N_CHIP + 3
        if i < 3 or i >= N_CHIP:
            g.round(r)
            for mask in g.READY[r]:
                use_dh(mask)

    s = Scatter(*scr[:4], sems[18:], me)
    total = s.run(block_product(s, glu_ref, down_ref, glu_t), between)
    y_ref[...] = (h_ref[...].astype(F32) + total[...]).astype(BF16)
    s.finish()
    g.finish()
    for swap in (gates, ups):
        swap.wait_recv(SETS[0])
        swap.wait_send(SETS[0])
    ucols.wait_recv()
    ucols.wait_send()
    leave.wait()
    ends = ((full_m.at[0], m_out.at[0]), (dgu_ref.at[:, seg(0, WIDE)], dgu_out.at[:, seg(0, WIDE)]))
    loop(N_CHIP, lambda j: [pltpu.make_async_copy(src, dst, osem.at[j, i]).wait() for i, (src, dst) in enumerate(ends)])


def back(groups, hd, qkv_hbm, do_hbm, stat_ref, cos_all, sin_all, dgu_hbm, m_hbm, ucol_ref, w_hbm, x_ref, small_all, dh_ref, dg2_ref, dg_in, du_in,
         dg_hbm, du_hbm, dwq_ref, dwkv_ref, dx_ref, gain_ref,
         dgu_ref, qkv_ref, do_ref, isem,
         p_scr, dp_scr, k_scr, v_scr, dk_acc, dv_acc, stage, dq_scr, dkv_scr, m_scr,
         full, w_scr, shares, dkv_own, full_kv, dqkv, dn, g_scr, dg1, gains, gains_in, wsem, lsem, msem, *sems):
    heads = qkv_ref.shape[0] // hd - 2
    seq = qkv_ref.shape[1]
    scale = hd ** -0.5
    lanes = heads * QB
    qw = heads * hd
    half = hd // 2
    me = lax.axis_index('sp')
    feat = dgu_ref.shape[0] // 2
    first = (X, Y + Z, Y, X + Z, Z, X + Y, 0)

    def fetch(mask):
        cols = seg(flipped(me, mask) // 2, WIDE)
        return pltpu.make_async_copy(m_hbm.at[:, :, cols], m_scr.at[:, :, cols], msem.at[mask // 2])
    for mask in first:
        fetch(mask).start()
    loads = fetch_all(isem, (dgu_hbm, dgu_ref), (qkv_hbm, qkv_ref), (do_hbm, do_ref))
    load = pltpu.make_async_copy(w_hbm, w_scr, wsem)
    load.start()
    enter(me, OTHERS)
    gain_row(g_scr, small_all, 0)

    gates, ups = dw_swaps(lambda peer: stage.at[peer // 2], dg_hbm, du_hbm, sems[:4], me)
    gq = row_gather(dq_scr, full, sems[6:10], me)
    own = [pltpu.make_async_copy(swap.src(me), swap.dst(me), lsem.at[i]) for i, swap in enumerate((gates, ups))]

    def make(mask):
        chip = flipped(me, mask) // 2
        fetch(mask).wait()
        cols = m_scr[:, :, seg(chip, WIDE)].reshape(seq, WIDE)
        stage[chip] = mm(dgu_ref[...], cols, NN)

    def advance(n):
        for swap in (gates, ups):
            if n > 1:
                swap.wait_send(SETS[n - 1])
            swap.start(SETS[n])

    for copy in loads:
        copy.wait()
    for i, mask in enumerate(first):
        make(mask)
        if i == 1:
            advance(1)
    gates.start((CORE,))
    ups.start((CORE,))
    for copy in own:
        copy.start()

    dk_acc[...] = jnp.zeros_like(dk_acc)
    dv_acc[...] = jnp.zeros_like(dv_acc)
    key_rows(k_scr, qkv_ref, qw, hd)
    key_rows(v_scr, qkv_ref, qw + hd, hd)

    def q_block(qb):
        @pl.when(qb == 4)
        def _():
            advance(2)
        qs = seg(qb, QB)
        q2 = side_by_side(qkv_ref, heads, hd, qs)
        do2 = side_by_side(do_ref, heads, hd, qs)
        top = stat_ref[qb, :1, :]
        inv = stat_ref[qb, 1:, :]

        def probs(kb, rd, diagonal):
            ks = seg(kb, KB)
            s = score_block(k_scr[ks, :], q2, scale, diagonal)
            p = jnp.exp(s - top) * inv
            dp = mm(v_scr[ks, :], do2, NN).astype(BF16)
            p_scr[ks, :] = p
            dp_scr[ks, :] = dp
            dv_acc[ks, :] += mm(p.astype(BF16), do2, NT)
            return rd + jnp.sum(dp.astype(F32) * p, axis=0, keepdims=True)

        rd = lax.fori_loop(0, qb, lambda kb, r: probs(kb, r, False), jnp.zeros((1, lanes), F32))
        rd = probs(qb, rd, True)

        def d_scores(kb, acc):
            ks = seg(kb, KB)
            ds = (p_scr[ks, :] * (dp_scr[ks, :].astype(F32) - rd) * scale).astype(BF16)
            dk_acc[ks, :] += mm(ds, q2, NT)
            return acc + mm(qkv_ref[qw:qw + hd, ks], ds, NN)

        acc = lax.fori_loop(0, qb + 1, d_scores, jnp.zeros((hd, lanes), F32))
        cos, sin = cos_all[:, qs], sin_all[:, qs]
        for h in range(heads):
            dq = acc[:, h * QB:(h + 1) * QB].astype(BF16).astype(F32)
            p, q = dq[:half], dq[half:]
            dq_scr[h * hd:h * hd + half, qs] = (p * cos + q * sin).astype(BF16)
            dq_scr[h * hd + half:(h + 1) * hd, qs] = (q * cos - p * sin).astype(BF16)

    loop(seq // QB, q_block)

    def share(i):
        rs = seg(i, WIDE)
        dkv_scr[rs, :] = jnp.concatenate([dk_acc[rs, :], dv_acc[rs, :]], axis=1).astype(BF16)
    loop(seq // WIDE, share)
    tokens = ucol_ref.shape[1]
    per = N_DEV // groups
    q_all = dwq_ref.shape[0]
    sh = Swap(lambda peer: dkv_scr.at[seg(peer, tokens), :], lambda o: shares.at[o], sems[4:6], me)
    parts = thirds(dkv_own.shape[0], STRIP)
    gk = Gather(dkv_own, lambda o: full_kv.at[:, seg(o, tokens)], lambda view, c: [view.at[pl.ds(*parts[c]), :]], sems[10:14], me)
    gs = Swap(lambda peer: gains.at[:, seg(peer)], lambda o: gains_in.at[o], sems[14:], me)
    sh.start()
    gq.start()
    keep_own(dq_scr, full, me)
    shares[me] = dkv_scr[seg(me, tokens), :]
    sh.wait_recv()
    cos, sin = cos_all[:, seg(me)], sin_all[:, seg(me)]
    for k in range(groups):
        both = sum(shares[per * k + i].astype(F32) for i in range(per)).astype(BF16).astype(F32).T
        p, q = both[:half], both[half:hd]
        lo = 2 * hd * k
        dkv_own[lo:lo + half, :] = (p * cos + q * sin).astype(BF16)
        dkv_own[lo + half:lo + hd, :] = (q * cos - p * sin).astype(BF16)
        dkv_own[lo + hd:lo + 2 * hd, :] = both[hd:].astype(BF16)
    gk.start()
    full_kv[:, seg(me, tokens)] = dkv_own[...]
    for k in range(groups):
        dqkv[:, q_all + 2 * hd * k:q_all + 2 * hd * (k + 1)] = dkv_own[2 * hd * k:2 * hd * (k + 1), :].T

    def use(mask):
        gq.wait_pair(mask)
        chip = flipped(me, mask) // 2
        dwq_ref[seg(chip, WIDE), :] = mm(full[chip], ucol_ref[...], NN)
        dqkv[:, seg(chip, WIDE)] = full[chip, :, seg(me, tokens)].T

    for r in range(len(gq.ROUNDS)):
        gq.round(r)
        gk.round(r)
        if r == 3:
            advance(3)
        for mask in gq.READY[r]:
            use(mask)
    load.wait()

    def normed(i):
        dn[:, seg(i, WIDE)] = mm(dqkv[...], w_scr[i], NN)
    loop(N_CHIP, normed)
    norm_back(dn, x_ref, g_scr, dh_ref, dx_ref, dg1)
    gains[...] = jnp.concatenate([jnp.sum(dg1[...], axis=0, keepdims=True), jnp.sum(dg2_ref[...], axis=0, keepdims=True),
                                  jnp.zeros((N_CHIP - 2, dg1.shape[1]), F32)], axis=0)
    gs.start()
    gains_in[me] = gains[:, seg(me)]
    for mask in CHIP_MASKS:
        gk.wait_pair(mask)
    dwkv_ref[...] = mm(full_kv[...], ucol_ref[...], NN)
    gs.wait_recv()
    gain_ref[...] = sum(gains_in[o] for o in range(N_DEV))
    for swap in (gates, ups):
        swap.wait_recv((CORE,) + SETS[1] + SETS[2] + SETS[3])
        swap.wait_send((CORE,) + SETS[3])
    for copy in own:
        copy.wait()
    for c in (sh, gs):
        c.wait_send()
    for g in (gq, gk):
        g.finish()


def finish(dg_hbm, du_hbm, dkv_hbm, *refs):
    n = (len(refs) - 14) // 3
    gains, refs = refs[0], refs[1:]
    srcs, (gate, up, dk, dv, dg1, dg2), refs = refs[:n], refs[n:n + 6], refs[n + 6:]
    dsts, (g_in, g_out, kv_in), holds, sems = refs[:n], refs[n:n + 3], refs[n + 3:2 * n + 3], refs[2 * n + 3:]
    dg1[...] = gains[:1, :]
    dg2[...] = gains[1:2, :]
    t_in, t_out, p_in, p_out = sems
    step = LANE * 11
    cols = g_in.shape[1]
    hd = dk.shape[0] // (kv_in.shape[0] // LANE)
    starts = [(w, i) for i in range(cols // step) for w in range(2)]

    def fetch(w, i):
        rs = pl.ds(i * step, step)
        return pltpu.make_async_copy((dg_hbm, du_hbm)[w].at[rs, :], g_in.at[w, rs, :], t_in.at[w, i])

    def put(w, i):
        cs = pl.ds(i * step, step)
        return pltpu.make_async_copy(g_out.at[w, :, cs], (gate, up)[w].at[:, cs], t_out.at[w, i])
    moves = [(pltpu.make_async_copy(a, h, p_in.at[k]), pltpu.make_async_copy(h, b, p_out.at[k])) for k, (a, h, b) in enumerate(zip(srcs, holds, dsts))]
    kv = pltpu.make_async_copy(dkv_hbm, kv_in, p_in.at[n])
    for w, i in starts:
        fetch(w, i).start()
    kv.start()
    for load, _ in moves:
        load.start()
    for w, i in starts:
        fetch(w, i).wait()

        at = pl.ds(i * step, step)
        g_out[w, :, at] = g_in[w, at, :].T
        put(w, i).start()
    kv.wait()
    for k in range(dk.shape[0] // hd):
        for i, ref in enumerate((dk, dv)):
            ref[k * hd:(k + 1) * hd, :] = kv_in[(2 * k + i) * hd:(2 * k + i + 1) * hd, :]
    for load, store in moves:
        load.wait()
        store.start()
    for w, i in starts:
        put(w, i).wait()
    for _, store in moves:
        store.wait()


def solution(mesh):
    assert mesh.shape['sp'] == N_DEV

    def layer_step(x_in, positions, d_out, norm1_gain, norm2_gain, w_q, w_k, w_v, w_o, w_gate, w_up, w_down):
        tokens, dim = x_in.shape
        seq = tokens * N_DEV
        n_q, hd = w_q.shape[1:]
        n_kv = w_k.shape[1]
        qw = n_q // N_DEV * hd
        rows = w_q.shape[0]
        feat = w_down.shape[0]
        cols = (n_q + 2 * n_kv) * hd
        lanes = qw // hd * QB
        vm = pltpu.VMEM
        full = vm((N_CHIP, WIDE, dim), BF16)
        gain_scr = vm((N_CHIP, dim), F32)
        tok_shapes = 2 * (((tokens, dim), BF16),)
        dw_shapes = 2 * (((feat * N_DEV, rows), F32),)

        inv_freq = 1.0 / (ROPE_BASE ** (jnp.arange(hd // 2, dtype=F32) * (2.0 / hd)))
        freq = jnp.broadcast_to(inv_freq[:, None], (hd // 2, rows))
        row = lambda v: v.reshape(1, rows)
        by_head = lambda w: w.transpose(1, 2, 0).reshape(-1, rows)
        wo_own = w_o.reshape(qw, dim)

        args = (x_in, row(norm1_gain), row(norm2_gain), row(positions), by_head(w_q), by_head(w_k), by_head(w_v), freq, w_gate, w_up, wo_own)
        qkv, u, small_all, wqkv, attn_t, stat, wgu, hidden, mlp_in, cos_all, sin_all = call(
            functools.partial(head, n_kv, hd), 0, len(args),
            (((qw + 2 * hd, seq), BF16), tok_shapes[0], ((N_DEV, N_CHIP, rows), F32), ((N_CHIP, cols, WIDE), BF16),
             ((qw, seq), BF16), ((seq // QB, 2, lanes), F32), ((2 * feat, dim), BF16), *tok_shapes, *(2 * (((hd // 2, seq), F32),))),
            [vm(w_gate.shape, BF16), vm(w_up.shape, BF16), vm((qw, dim), BF16), vm((qw + 2 * hd, seq), BF16), vm((tokens, dim), BF16),
             vm((hd // 2, seq), F32), vm((hd // 2, seq), F32), dma(3), dma(4),
             full, vm((tokens, dim), F32), vm((tokens, dim), BF16), vm((seq, qw), BF16),
             vm((N_CHIP, rows), F32), vm((cols, rows), BF16), vm((N_CHIP, cols, WIDE), BF16), vm((cols, tokens), F32), vm((cols, tokens), BF16), gain_scr,
             vm((feat * N_DEV, rows), BF16), vm((feat * N_DEV, rows), BF16), vm((seq, lanes), F32), vm((seq, hd), BF16), dma(N_CHIP),
             *Gather.sems, *(6 * Swap.sems), *Gather.sems], 4 * qw * seq * seq, far_in=(8, 9, 10), far_out=(0, 1, 3, 9, 10))(*args)
        args = (mlp_in, d_out, wgu, w_down, u, hidden, small_all, wo_own, attn_t)
        u_col, m_full, dgu, d_down, y_out, d_hidden, d_attn, d_wo, d_g2, d_gate_t, d_up_t = call(
            mlp, 1, len(args),
            (((seq, rows), BF16), ((N_CHIP, WIDE, dim), BF16), ((2 * feat, seq), BF16), ((feat, dim), F32),
             *tok_shapes, ((qw, seq), BF16), ((qw, dim), F32), ((N_CHIP, dim), F32), *dw_shapes),
            [vm((2 * feat, dim), BF16), vm((feat, dim), BF16),
             vm((feat, seq), BF16), vm((2 * feat, seq), BF16), vm((feat, dim), F32), dma(2), dma(),
             full, full, dma(N_CHIP, 2), vm((2 * feat, WIDE), F32), gain_scr, vm((WIDE, 2 * feat), BF16), vm((WIDE, feat), BF16), pltpu.SemaphoreType.REGULAR,
             *Scatter.scratch(tokens, dim), *(3 * Gather.sems), *(3 * Swap.sems), *Scatter.sems], 12 * feat * seq * dim,
            far_in=(2, 3), far_out=(1, 2, 3, 9, 10))(*args)
        args = (qkv, d_attn, stat, cos_all, sin_all, dgu, m_full, u_col, wqkv, x_in, small_all, d_hidden, d_g2, d_gate_t, d_up_t)
        d_gate_t, d_up_t, d_wq, d_wkv, d_x, gains = call(
            functools.partial(back, n_kv, hd), 3, len(args),
            (*dw_shapes, ((n_q * hd, rows), F32), ((2 * n_kv * hd, rows), F32), tok_shapes[0], ((N_CHIP, rows), F32)),
            [vm((2 * feat, seq), BF16), vm((qw + 2 * hd, seq), BF16), vm((qw, seq), BF16), dma(3),
             vm((seq, lanes), F32), vm((seq, lanes), BF16), vm((seq, hd), BF16), vm((seq, hd), BF16), vm((seq, hd), F32), vm((seq, hd), F32),
             vm((N_CHIP, 2 * feat, WIDE), F32), vm((qw, seq), BF16), vm((seq, 2 * hd), BF16), full,
             full, vm((N_CHIP, cols, WIDE), BF16), vm((N_DEV, tokens, 2 * hd), BF16), vm((2 * n_kv * hd, tokens), BF16), vm((2 * n_kv * hd, seq), BF16),
             vm((tokens, cols), BF16), vm((tokens, dim), F32), gain_scr, gain_scr, gain_scr, vm((N_DEV, N_CHIP, rows), F32), dma(), dma(2), dma(N_CHIP),
             *(3 * Swap.sems), *(2 * Gather.sems), *Swap.sems], 10 * qw * seq * seq, far_in=(0, 1, 5, 6, 8, 13, 14), far_out=(0, 1), aliases={13: 0, 14: 1})(*args)
        moved = (d_wq, d_wo, d_down, d_x, y_out)
        one_row = jax.ShapeDtypeStruct((1, rows), F32)
        half_kv = jax.ShapeDtypeStruct((n_kv * hd, rows), F32)
        wide = jax.ShapeDtypeStruct((rows, feat * N_DEV), F32)
        d_gate, d_up, d_wk, d_wv, d_g1, d_g2, d_wq, d_wo, d_down, d_x, y_out = pl.pallas_call(
            finish,
            out_shape=[wide, wide, half_kv, half_kv, one_row, one_row] + [jax.ShapeDtypeStruct(v.shape, v.dtype) for v in moved],
            in_specs=[IN_HBM] * 3 + on_chip(1) + [IN_HBM] * len(moved), out_specs=[IN_HBM] * 2 + on_chip(4) + [IN_HBM] * len(moved),
            scratch_shapes=[vm((2, feat * N_DEV, rows), F32), vm((2, rows, feat * N_DEV), F32), vm(d_wkv.shape, F32)]
            + [vm(v.shape, v.dtype) for v in moved] + [dma(2, 4), dma(2, 4), dma(len(moved) + 1), dma(len(moved))],
            compiler_params=pltpu.CompilerParams(vmem_limit_bytes=VMEM_CAP), name='finish',
        )(d_gate_t, d_up_t, d_wkv, gains, *moved)
        by_row = lambda g, heads: g.reshape(heads, hd, rows).transpose(2, 0, 1)
        return (y_out, d_x, d_g1.reshape(rows), d_g2.reshape(rows), by_row(d_wq, n_q), by_row(d_wk, n_kv), by_row(d_wv, n_kv),
                d_wo.reshape(w_o.shape), d_gate, d_up, d_down)

    all_rows = P('sp')
    return jax.shard_map(layer_step, mesh=mesh, in_specs=(all_rows,) * 12, out_specs=(all_rows,) * 11, check_vma=False)
```

```python
import functools
import jax
import jax.numpy as jnp
from jax import lax
from jax.experimental import pallas as pl
from jax.experimental.pallas import tpu as pltpu
from jax.sharding import PartitionSpec as P

ROPE_BASE = 10000.0
NORM_EPS = 1e-5
NEG_LARGE = -1e30
F32 = jnp.float32
BF16 = jnp.bfloat16
N_DEV, N_CHIP, LANE, WIDE, CHUNK, STRIP = 16, 8, 128, 256, 512, 16
NT = (((1,), (1,)), ((), ()))
TN = (((0,), (0,)), ((), ()))
NN = (((1,), (0,)), ((), ()))
MESH = pl.DeviceIdType.MESH
VMEM_CAP = 62 * 1024 * 1024

CORE, X, Y, Z = 1, 2, 4, 8
XYZ = X + Y + Z
ORDERS = ((X, Y, Z), (Y, Z, X), (Z, X, Y))
CHIP_MASKS = (0, X, Y, Z, X + Y, X + Z, Y + Z, XYZ)
NEAR = (CORE, X, Y, Z)
OTHERS = range(1, N_DEV)
SETS = tuple(tuple(m + c for m in masks for c in (0, CORE)) for masks in ((XYZ,), (X, Y + Z), (Y, X + Z), (Z, X + Y)))
N_COL = len(ORDERS)
COLOURS = range(N_COL)


def mm(a, b, dims):
    return lax.dot_general(a, b, dims, preferred_element_type=F32)


def seg(index, width=LANE):
    return pl.ds(pl.multiple_of(index * width, width), width)


def loop(count, body):
    lax.fori_loop(0, count, lambda i, c: (body(i), c)[1], 0)


def differing(index, mask):
    return sum(((index // bit + mask // bit) % 2) * bit for bit in NEAR)


def flipped(index, mask):
    out = index
    for bit in NEAR:
        if mask & bit:
            out = out + (1 - 2 * ((index // bit) % 2)) * bit
    return out


def thirds(total, unit):
    n = total // unit
    first = (n + 2) // 3
    second = (n - first + 1) // 2
    sizes = (first * unit, second * unit, (n - first - second) * unit)
    return ((0, sizes[0]), (sizes[0], sizes[1]), (sizes[0] + sizes[1], sizes[2]))


def pieces(rows, cols, unit):
    share = cols // LANE // N_COL * LANE
    strips = thirds(rows, unit)
    rest = cols - N_COL * share
    return [[(pl.ds(0, rows), pl.ds(c * share, share)), (pl.ds(*strips[c]), pl.ds(N_COL * share, rest))] for c in COLOURS]


def enter(me, masks):
    barrier = pltpu.get_barrier_semaphore()
    for mask in masks:
        pl.semaphore_signal(barrier, inc=1, device_id=(flipped(me, mask),), device_id_type=MESH)
    pl.semaphore_wait(barrier, len(masks))


def remote(src, dst, send, recv, peer):
    return pltpu.make_async_remote_copy(src_ref=src, dst_ref=dst, send_sem=send, recv_sem=recv, device_id=(peer,), device_id_type=MESH)


def dma(*shape):
    return pltpu.SemaphoreType.DMA(shape)


class Swap:
    sems = (dma(N_DEV), dma(N_DEV))

    def __init__(self, src, dst, sems, me):
        self.src, self.dst, (self.send, self.recv), self.me = src, dst, sems, me

    def copy(self, mask):
        peer = differing(self.me, mask)
        return remote(self.src(peer), self.dst(self.me), self.send.at[mask], self.recv.at[mask], peer)

    def arrival(self, mask):
        view = self.dst(differing(self.me, mask))
        return remote(view, view, self.send.at[mask], self.recv.at[mask], self.me)

    def each(self, masks, act):
        if masks is None:
            loop(N_DEV - 1, lambda i: act(i + 1))
        else:
            for mask in masks:
                act(mask)

    def start(self, masks=None):
        self.each(masks, lambda mask: self.copy(mask).start())

    def advance(self, n):
        if n:
            self.wait_send(SETS[n - 1])
        self.start(SETS[n])

    def wait_recv(self, masks=None):
        self.each(masks, lambda mask: self.arrival(mask).wait_recv())

    def wait_send(self, masks=None):
        self.each(masks, lambda mask: self.copy(mask).wait_send())


class Gather:
    ROUNDS = ((0,), (1,), (2,), (0, 1), (0, 2), (1, 2), (0, 1, 2))
    READY = ((0,), (), (), (X, Y), (Z,), (X + Y, X + Z), (Y + Z, XYZ))
    sems = (dma(N_COL, N_CHIP, 2), dma(N_COL, N_CHIP, 2), dma(N_CHIP), dma(N_CHIP))

    def __init__(self, own, block, cut, sems, me):
        self.own, self.block, self.cut, self.me = own, block, cut, me
        self.send, self.recv, self.pair_send, self.pair_recv = sems

    def source(self, mask):
        return self.block(flipped(self.me, mask)) if mask else self.own

    def unit(self, colour, mask, axis):
        ends = zip(self.cut(self.source(mask), colour), self.cut(self.block(flipped(self.me, mask)), colour))
        j = self.sends(colour).index((mask, axis))
        return [remote(src, dst, self.send.at[colour, j, i], self.recv.at[colour, (mask + axis) // 2, i],
                       flipped(self.me, axis)) for i, (src, dst) in enumerate(ends)]

    def sends(self, colour):
        return [(0, axis) for axis in ORDERS[colour]] + [step[1:] for step in self.onward(colour)]

    def start_unit(self, colour, mask, axis):
        for copy in self.unit(colour, mask, axis):
            copy.start()

    def pair(self, mask):
        return remote(self.source(mask), self.block(flipped(self.me, mask)), self.pair_send.at[mask // 2],
                      self.pair_recv.at[mask // 2], flipped(self.me, CORE))

    def wait_pair(self, mask):
        view = self.block(flipped(self.me, mask + CORE))
        remote(view, view, self.pair_send.at[mask // 2], self.pair_recv.at[mask // 2], self.me).wait_recv()

    def onward(self, colour):
        order = ORDERS[colour]
        for picks in self.ROUNDS:
            for axis in order[picks[-1] + 1:]:
                yield picks, sum(order[p] for p in picks), axis

    def start(self):
        for pos in COLOURS:
            for colour in COLOURS:
                self.start_unit(colour, 0, ORDERS[colour][pos])
        self.pair(0).start()

    def round(self, r):
        for colour in COLOURS:
            mask = sum(ORDERS[colour][p] for p in self.ROUNDS[r])
            for i, view in enumerate(self.cut(self.block(flipped(self.me, mask)), colour)):
                remote(view, view, self.send.at[colour, 0, i], self.recv.at[colour, mask // 2, i], self.me).wait_recv()
            for picks, at, axis in self.onward(colour):
                if picks == self.ROUNDS[r]:
                    self.start_unit(colour, at, axis)
        for mask in {2: (X, Y, Z), 5: (X + Y, X + Z, Y + Z), 6: (XYZ,)}.get(r, ()):
            self.pair(mask).start()

    def finish(self):
        for colour in COLOURS:
            for i, view in enumerate(self.cut(self.own, colour)):
                loop(len(self.sends(colour)), lambda j: remote(view, view, self.send.at[colour, j, i], self.recv.at[colour, j, i], self.me).wait_send())
        loop(N_CHIP, lambda j: remote(self.own, self.own, self.pair_send.at[j], self.pair_recv.at[j], self.me).wait_send())


def row_gather(own, full, sems, me, extra=None):
    rows, width = own.shape
    parts = pieces(rows, width, STRIP)
    if extra is not None:
        share = width // LANE // N_COL * LANE
        more = width - N_COL * share
        parts = [[(pl.ds(0, rows), pl.ds(c * share + more * (c > extra), share + more * (c == extra)))] for c in COLOURS]

    def block(o):
        return full.at[o // 2, seg(o % 2), :]

    return Gather(own, block, lambda view, c: [view.at[rs, cs] for rs, cs in parts[c]], sems, me)


def keep_own(own, full, me):
    def step(i):
        full[me // 2, pl.ds(pl.multiple_of((me % 2) * LANE + i * STRIP, STRIP), STRIP), :] = own[seg(i, STRIP), :]
    loop(LANE // STRIP, step)


class Scatter:
    ORDER = (XYZ, X + Y, Y + Z, X + Z, X, Y, Z, 0)
    sems = (dma(N_CHIP), dma(N_CHIP), dma(N_COL, N_CHIP, 2), dma(N_COL, N_CHIP, 2))

    @staticmethod
    def scratch(tokens, dim):
        return [pltpu.VMEM((n, tokens, dim), F32) for n in (N_CHIP, 2, N_CHIP, N_CHIP - 1)]

    def __init__(self, part, other, pair_in, link_in, sems, me):
        self.part, self.other, self.pair_in, self.link_in, self.me = part, other, pair_in, link_in, me
        self.pair_send, self.pair_recv, self.link_send, self.link_recv = sems
        self.tokens, self.dim = part.shape[1:]
        self.pieces = pieces(self.tokens, self.dim, STRIP // 2)
        self.ready, self.sent = set(), [0] * N_COL

    @staticmethod
    def first(colour, mask):
        return next((i for i, a in enumerate(ORDERS[colour]) if mask & a), 3)

    def slot(self, colour, mask, axis):
        slots = [(m, a) for m in self.ORDER for a in ORDERS[colour][:self.first(colour, m)]]
        return slots.index((mask, axis))

    def pair(self, i):
        return remote(self.other.at[i % 2], self.pair_in.at[i], self.pair_send.at[i], self.pair_recv.at[i], flipped(self.me, CORE))

    def link(self, colour, mask):
        axis = ORDERS[colour][self.first(colour, mask)]
        slot = self.slot(colour, mask - axis, axis)
        i = self.ORDER.index(mask)
        return [remote(self.part.at[i, rs, cs], self.link_in.at[slot, rs, cs], self.link_send.at[colour, i, k],
                       self.link_recv.at[colour, slot, k], flipped(self.me, axis)) for k, (rs, cs) in enumerate(self.pieces[colour])]

    def start_link(self, colour, mask):
        for copy in self.link(colour, mask):
            copy.start()

    def add(self, mask, ref, cs):
        i = self.ORDER.index(mask)

        def step(r):
            rs = seg(r, STRIP)
            self.part[i, rs, cs] += ref[rs, cs]
        loop(self.tokens // STRIP, step)

    def finish_pair(self, i):
        self.pair(i).wait_recv()
        self.add(self.ORDER[i], self.pair_in.at[i], pl.ds(0, self.dim))
        self.ready.add(self.ORDER[i])
        for colour in COLOURS:
            a, b, c = ORDERS[colour]
            todo = (XYZ, a + b, a + c, a)
            while self.sent[colour] < len(todo) and todo[self.sent[colour]] in self.ready:
                self.start_link(colour, todo[self.sent[colour]])
                self.sent[colour] += 1

    def take(self, colour, mask, axis):
        for copy in self.link(colour, mask + axis):
            copy.wait_recv()
        ref = self.link_in.at[self.slot(colour, mask, axis)]
        (_, wide), (rs, cs) = self.pieces[colour]
        self.add(mask, ref, wide)
        self.part[self.ORDER.index(mask), rs, cs] += ref[rs, cs]

    def run(self, product, between=lambda i: None):
        for i, mask in enumerate(self.ORDER):
            if i > 1:
                self.pair(i - 2).wait_send()
            product(i, flipped(self.me, mask) // 2)
            self.pair(i).start()
            if i:
                self.finish_pair(i - 1)
            between(i)
        self.finish_pair(N_CHIP - 1)
        for step in range(2):
            between(N_CHIP + step)
            for colour in COLOURS:
                a, b, c = ORDERS[colour]
                mask = (b + c, b)[step]
                self.take(colour, mask, a)
                self.start_link(colour, mask)
        between(N_CHIP + 2)
        for colour in COLOURS:
            a, b, c = ORDERS[colour]
            self.take(colour, c, a)
            self.take(colour, c, b)
            self.start_link(colour, c)
        between(N_CHIP + 3)
        for colour in COLOURS:
            for axis in ORDERS[colour]:
                self.take(colour, 0, axis)
        return self.part.at[N_CHIP - 1]

    def finish(self):
        for i in (N_CHIP - 2, N_CHIP - 1):
            self.pair(i).wait_send()
        for colour in COLOURS:
            for k, (rs, cs) in enumerate(self.pieces[colour]):
                view = self.part.at[0, rs, cs]
                loop(N_CHIP - 1, lambda i: remote(view, view, self.link_send.at[colour, i, k], self.link_recv.at[colour, i, k], self.me).wait_send())


def block_product(s, a_ref, w_ref, a_t):
    core = s.me % 2

    def product(i, chip):
        a_t[...] = a_ref[:, seg(chip, WIDE)].T

        def step(n):
            cs = seg(n, CHUNK)
            s.other[i % 2, :, cs] = mm(a_t[seg(1 - core), :], w_ref[:, cs], NN)
            s.part[i, :, cs] = mm(a_t[seg(core), :], w_ref[:, cs], NN)
        loop(s.dim // CHUNK, step)
    return product


def on_chip(n):
    return [pl.BlockSpec(memory_space=pltpu.VMEM)] * n


IN_HBM = pl.BlockSpec(memory_space=pl.ANY)


def call(kernel, ident, args, outs, scratch, flops, far_in=(), far_out=(), aliases={}):
    specs = [IN_HBM if i in far_in else on_chip(1)[0] for i in range(args)]
    out_specs = [IN_HBM if i in far_out else on_chip(1)[0] for i in range(len(outs))]
    return pl.pallas_call(
        kernel,
        out_shape=[jax.ShapeDtypeStruct(shape, dtype) for shape, dtype in outs],
        in_specs=specs, out_specs=out_specs, scratch_shapes=scratch, input_output_aliases=aliases,
        cost_estimate=pl.CostEstimate(flops=flops, bytes_accessed=flops // CHUNK, transcendentals=0),
        compiler_params=pltpu.CompilerParams(collective_id=ident, has_side_effects=True, vmem_limit_bytes=VMEM_CAP),
        name=kernel.func.__name__ if isinstance(kernel, functools.partial) else kernel.__name__,
    )


def fetch_all(sem, *pairs):
    copies = [pltpu.make_async_copy(src, dst, sem.at[i]) for i, (src, dst) in enumerate(pairs)]
    for copy in copies:
        copy.start()
    return copies


def gain_row(dst, small_all, which):
    for o in range(N_DEV):
        dst[:1, o * LANE:(o + 1) * LANE] = small_all[o, which:which + 1, :]


def norm_rows(src, gain, dst):
    def step(i):
        rs = seg(i, STRIP)
        t = src[rs, :].astype(F32)
        dst[rs, :] = (t * lax.rsqrt(jnp.mean(t * t, axis=-1, keepdims=True) + NORM_EPS) * gain[:1, :]).astype(BF16)
    loop(src.shape[0] // STRIP, step)


def norm_back(dy, src, gain, skip, dst, dgain):
    def step(i):
        rs = seg(i, STRIP)
        d = dy[rs, :].astype(BF16).astype(F32)
        t = src[rs, :].astype(F32)
        inv = lax.rsqrt(jnp.mean(t * t, axis=-1, keepdims=True) + NORM_EPS)
        gd = gain[:1, :] * d
        pull = jnp.mean(gd * t, axis=-1, keepdims=True)
        dst[rs, :] = (skip[rs, :].astype(F32) + (inv * gd - t * (inv * inv * inv * pull))).astype(BF16)
        g = d * (t * inv)
        dgain[...] += g[:N_CHIP] + g[N_CHIP:]
    dgain[...] = jnp.zeros_like(dgain)
    loop(src.shape[0] // STRIP, step)


QB = 256
KB = 256


def key_rows(dst, src, lo, hd):
    def step(i):
        dst[seg(i, KB), :] = src[lo:lo + hd, seg(i, KB)].T
    loop(src.shape[1] // KB, step)


def score_block(k, q2, scale, diagonal):
    s = mm(k, q2, NN) * scale
    if diagonal:
        key = lax.broadcasted_iota(jnp.int32, s.shape, 0)
        qry = lax.broadcasted_iota(jnp.int32, s.shape, 1) % QB
        s = jnp.where(qry >= key, s, NEG_LARGE)
    return s


def side_by_side(ref, heads, hd, qs):
    return jnp.concatenate([ref[h * hd:(h + 1) * hd, qs] for h in range(heads)], axis=1)


def head(groups, hd, x_ref, g1_ref, g2_ref, pos_ref, wq_ref, wk_ref, wv_ref, freq_ref, wg_hbm, wu_hbm, wo_hbm, qkv_out, u_out, small_all, w_out, o_ref, stat_ref, wgu_ref, h_ref, m_ref, cos_out, sin_out,
         wg_ref, wu_ref, wo_ref, qkv_ref, u_scr, cos_ref, sin_ref, isem, esem,
         full_w, acc_o, o_tok, o_send, small_ref, w_ref, full, acc, rot, g_scr, wg_t, wu_t, s_scr, k_scr, osem, *sems):
    me = lax.axis_index('sp')
    tokens, dim = x_ref.shape
    cols = w_ref.shape[0]
    small_ref[...] = jnp.concatenate([r[...].astype(F32) for r in (g1_ref, g2_ref, pos_ref)] + [jnp.zeros((N_CHIP - 3, LANE), F32)], axis=0)
    w_ref[:wq_ref.shape[0], :] = wq_ref[...]
    for k in range(groups):
        for i, ref in enumerate((wk_ref, wv_ref)):
            w_ref[pl.ds(wq_ref.shape[0] + (2 * k + i) * hd, hd), :] = ref[k * hd:(k + 1) * hd, :]
    qw = tokens
    q_all = N_DEV * qw
    gsems, ssems, qsems, ksems, gate_sems, up_sems, osems = sems[:4], *(sems[i:i + 2] for i in range(4, len(sems) - 4, 2))
    gw = row_gather(wo_ref, full_w, sems[-4:], me, 1)
    feat = wg_ref.shape[1] // N_DEV
    loads = fetch_all(isem, (wg_hbm, wg_ref), (wu_hbm, wu_ref), (wo_hbm, wo_ref))
    enter(me, OTHERS)
    smalls = Swap(lambda peer: small_ref, lambda o: small_all.at[o], ssems, me)
    smalls.start()
    parts = thirds(cols, STRIP)
    g = Gather(w_ref, lambda o: full.at[o // 2, :, seg(o % 2)], lambda view, c: [view.at[pl.ds(*parts[c]), :]], gsems, me)
    g.start()
    gates = Swap(lambda peer: wg_t.at[seg(peer, feat), :], lambda o: wgu_ref.at[:feat, seg(o)], gate_sems, me)
    ups = Swap(lambda peer: wu_t.at[seg(peer, feat), :], lambda o: wgu_ref.at[feat:, seg(o)], up_sems, me)

    def advance(n):
        gates.advance(n)
        ups.advance(n)

    def transpose(i):
        wg_t[seg(i, CHUNK), :] = wg_ref[:, seg(i, CHUNK)].T
        wu_t[seg(i, CHUNK), :] = wu_ref[:, seg(i, CHUNK)].T
    for load in loads:
        load.wait()
    loop(wg_ref.shape[1] // CHUNK, transpose)
    advance(0)

    def own_block(i):
        full[me // 2, seg(i, WIDE), seg(me % 2)] = w_ref[seg(i, WIDE), :]
    loop(cols // WIDE, own_block)
    acc[...] = jnp.zeros_like(acc)
    small_all[me] = small_ref[...]
    smalls.wait_recv()
    gain_row(g_scr, small_all, 0)
    norm_rows(x_ref, g_scr, u_scr)

    def keep(mask):
        chip = flipped(me, mask) // 2
        return pltpu.make_async_copy(full.at[chip], w_out.at[chip], osem.at[mask // 2])

    def use(mask):
        g.wait_pair(mask)
        keep(mask).start()
        chip = flipped(me, mask) // 2
        u = u_scr[:, seg(chip, WIDE)]

        def step(i):
            rs = seg(i, cols // 2)
            acc[rs, :] += mm(full[chip, rs, :], u, NT)
        loop(2, step)

    def tables(o):
        angles = freq_ref[...] * small_all[o, 2:3, :]
        cos_ref[:, seg(o)] = jnp.cos(angles)
        sin_ref[:, seg(o)] = jnp.sin(angles)

    for r in range(len(g.ROUNDS)):
        g.round(r)
        if r in (2, 5):
            advance(r // 2)
        if r == 1:
            loop(N_DEV, tables)
        for mask in g.READY[r]:
            use(mask)

    half = hd // 2
    cos, sin = cos_ref[:, seg(me)], sin_ref[:, seg(me)]

    def turn(h):
        first = seg(2 * h, half)
        second = seg(2 * h + 1, half)
        p = acc[first, :].astype(BF16).astype(F32)
        q = acc[second, :].astype(BF16).astype(F32)
        rot[first, :] = (p * cos - q * sin).astype(BF16)
        rot[second, :] = (q * cos + p * sin).astype(BF16)
    loop(q_all // hd, turn)
    for k in range(groups):
        turn(q_all // hd + 2 * k)
        vs = seg(q_all // hd + 2 * k + 1, hd)
        rot[vs, :] = acc[vs, :].astype(BF16)
    per = N_DEV // groups
    q_rows = lambda peer: seg(peer, qw)
    kv_rows = lambda peer: seg(q_all // (2 * hd) + peer // per, 2 * hd)
    qs = Swap(lambda peer: rot.at[q_rows(peer), :], lambda o: qkv_ref.at[:qw, seg(o, tokens)], qsems, me)
    kvs = Swap(lambda peer: rot.at[kv_rows(peer), :], lambda o: qkv_ref.at[qw:, seg(o, tokens)], ksems, me)
    qs.start()
    kvs.start()
    gw.start()
    keep_own(wo_ref, full_w, me)
    gain_row(g_scr, small_all, 1)
    qkv_ref[:qw, seg(me, tokens)] = rot[q_rows(me), :]
    qkv_ref[qw:, seg(me, tokens)] = rot[kv_rows(me), :]
    wgu_ref[:feat, seg(me)] = wg_t[seg(me, feat), :]
    wgu_ref[feat:, seg(me)] = wu_t[seg(me, feat), :]
    gates.start((CORE,))
    ups.start((CORE,))
    for swap in (qs, kvs):
        swap.wait_recv()
    stores = fetch_all(esem, (qkv_ref, qkv_out), (u_scr, u_out), (cos_ref, cos_out), (sin_ref, sin_out))
    heads = qkv_ref.shape[0] // hd - 2
    seq = qkv_ref.shape[1]
    scale = hd ** -0.5
    lanes = heads * QB
    key_rows(k_scr, qkv_ref, qw, hd)

    outs = Swap(lambda peer: o_send.at[seg(peer), :], lambda o: o_tok.at[:, seg(o)], osems, me)

    def q_block(qb):
        for at, r in ((2, 0), (4, 1), (5, 2), (6, 3), (7, 4)):
            @pl.when(qb == at)
            def _():
                gw.round(r)
        qs = seg(qb, QB)
        q2 = side_by_side(qkv_ref, heads, hd, qs)

        def scores(kb, top, diagonal):
            s = score_block(k_scr[seg(kb, KB), :], q2, scale, diagonal)
            s_scr[seg(kb, KB), :] = s
            return jnp.maximum(top, jnp.max(s, axis=0, keepdims=True))

        top = lax.fori_loop(0, qb, lambda kb, t: scores(kb, t, False), jnp.full((1, lanes), NEG_LARGE, F32))
        top = scores(qb, top, True)

        def expo(kb, tot):
            e = jnp.exp(s_scr[seg(kb, KB), :] - top)
            s_scr[seg(kb, KB), :] = e
            return tot + jnp.sum(e, axis=0, keepdims=True)

        inv = 1.0 / lax.fori_loop(0, qb + 1, expo, jnp.zeros((1, lanes), F32))

        def weigh(kb, acc):
            p = (s_scr[seg(kb, KB), :] * inv).astype(BF16)
            return acc + mm(qkv_ref[qw + hd:, seg(kb, KB)], p, NN)

        acc = lax.fori_loop(0, qb + 1, weigh, jnp.zeros((hd, lanes), F32))
        for h in range(heads):
            o_ref[h * hd:(h + 1) * hd, qs] = acc[:, h * QB:(h + 1) * QB].astype(BF16)
        stat_ref[qb, :1, :] = top
        stat_ref[qb, 1:, :] = inv
        o_send[qs, :] = o_ref[:, qs].T

    loop(seq // QB, q_block)
    outs.start()
    advance(3)
    o_tok[:, seg(me)] = o_send[seg(me), :]
    for r in (5, 6):
        gw.round(r)
    outs.wait_recv()
    for mask in CHIP_MASKS:
        gw.wait_pair(mask)

    def project(n):
        cs = seg(n, CHUNK)
        acc_o[:, cs] = mm(o_tok[...], full_w[:, :, cs].reshape(dim, CHUNK), NN)
    loop(dim // CHUNK, project)

    def residual(i):
        rs = seg(i, STRIP)
        h_ref[rs, :] = (x_ref[rs, :].astype(F32) + acc_o[rs, :]).astype(BF16)
    loop(tokens // STRIP, residual)
    norm_rows(h_ref, g_scr, m_ref)
    for swap in (gates, ups):
        swap.wait_recv()
    for mask in CHIP_MASKS:
        keep(mask).wait()
    outs.wait_send()
    for swap in (gates, ups):
        swap.wait_send((CORE,) + SETS[3])
    for store in stores:
        store.wait()
    g.finish()
    gw.finish()
    for swap in (smalls, qs, kvs):
        swap.wait_send()


def dw_swaps(stage, gate_hbm, up_hbm, sems, me):
    feat = gate_hbm.shape[0] // N_DEV
    return [Swap(lambda peer, lo=lo: stage(peer).at[lo:lo + feat, seg(peer % 2)], lambda o, dst=dst: dst.at[seg(o, feat), :], sems[i:i + 2], me)
            for lo, dst, i in ((0, gate_hbm, 0), (feat, up_hbm, 2))]


def mlp(m_ref, dout_ref, wgu_hbm, down_hbm, u_ref, h_ref, small_all, wo_ref, o_ref,
        ucol_ref, m_out, dgu_out, ddown_out, y_ref, dh_ref, do_ref, dwo_ref, dg_ref, gate_hbm, up_hbm,
        wgu_ref, down_ref, glu_ref, dgu_ref, ddown_ref, isem, dsem, full_d, full_m, osem, stage, g_scr, dgu_t, glu_t, free, *scr):
    me = lax.axis_index('sp')
    feat, dim = down_ref.shape
    loads = fetch_all(isem, (wgu_hbm, wgu_ref), (down_hbm, down_ref))
    enter(me, OTHERS)
    sems = scr[4:]
    gd = row_gather(dout_ref, full_d, sems[:4], me, 0)
    gm = row_gather(m_ref, full_m, sems[4:8], me, 2)
    g = row_gather(dh_ref, full_d, sems[8:12], me, 1)
    ucols = Swap(lambda peer: u_ref.at[:, seg(peer)], lambda o: ucol_ref.at[seg(o), :], sems[12:14], me)
    gates, ups = dw_swaps(lambda peer: stage, gate_hbm, up_hbm, sems[14:18], me)
    gm.start()
    gd.start()
    keep_own(m_ref, full_m, me)
    keep_own(dout_ref, full_d, me)
    gain_row(g_scr, small_all, 1)
    dwo_ref[...] = jnp.zeros_like(dwo_ref)
    ddown_ref[...] = jnp.zeros_like(ddown_ref)

    def keep(mask):
        chip = flipped(me, mask) // 2
        ts = seg(chip, WIDE)
        ends = ((full_m.at[chip], m_out.at[chip]), (dgu_ref.at[:, ts], dgu_out.at[:, ts]))
        return [pltpu.make_async_copy(src, dst, osem.at[mask // 2, i]) for i, (src, dst) in enumerate(ends)]

    for load in loads:
        load.wait()
    ucol_ref[seg(me), :] = u_ref[:, seg(me)]

    def use(mask):
        gd.wait_pair(mask)
        gm.wait_pair(mask)
        chip = flipped(me, mask) // 2
        ts = seg(chip, WIDE)
        gu = mm(wgu_ref[...], full_m[chip], NT).astype(BF16).astype(F32)
        gate, up = gu[:feat], gu[feat:]
        d_glu = mm(down_ref[...], full_d[chip], NT).astype(BF16).astype(F32)
        sig = jax.nn.sigmoid(gate)
        act = gate * sig
        glu = (act * up).astype(BF16)
        glu_ref[:, ts] = glu
        dgu_ref[:feat, ts] = (d_glu * up * (sig * (1.0 + gate * (1.0 - sig)))).astype(BF16)
        dgu_ref[feat:, ts] = (d_glu * act).astype(BF16)

        def step(n):
            ddown_ref[:, seg(n, CHUNK)] += mm(glu, full_d[chip, :, seg(n, CHUNK)], NN)
        loop(dim // CHUNK, step)
        for copy in keep(mask):
            copy.start()

    for r in range(len(gm.ROUNDS)):
        gm.round(r)
        gd.round(r)
        if r == 3:
            ucols.start()
        for mask in gm.READY[r]:
            use(mask)
    far = seg(flipped(me, XYZ) // 2, WIDE)
    stage[...] = mm(dgu_ref[...], full_m[:, :, far].reshape(dgu_ref.shape[1], WIDE), NN)
    for swap in (gates, ups):
        swap.start(SETS[0])
    for gather in (gd, gm):
        gather.finish()
    leave = pltpu.make_async_copy(ddown_ref, ddown_out, dsem)
    leave.start()
    s = Scatter(*scr[:4], sems[18:], me)
    total = s.run(block_product(s, dgu_ref, wgu_ref, dgu_t))
    for mask in NEAR:
        pl.semaphore_signal(free, inc=1, device_id=(flipped(me, mask),), device_id_type=MESH)
    norm_back(total, h_ref, g_scr, dout_ref, dh_ref, dg_ref)
    g.start()
    keep_own(dh_ref, full_d, me)
    s.finish()
    pl.semaphore_wait(free, len(NEAR))

    def use_dh(mask):
        g.wait_pair(mask)
        chip = flipped(me, mask) // 2
        do_ref[:, seg(chip, WIDE)] = mm(wo_ref[...], full_d[chip], NT).astype(BF16)
        o = o_ref[:, seg(chip, WIDE)]

        def step(n):
            dwo_ref[:, seg(n, CHUNK)] += mm(o, full_d[chip, :, seg(n, CHUNK)], NN)
        loop(dim // CHUNK, step)

    def between(i):
        r = i if i < 3 else i - N_CHIP + 3
        if i < 3 or i >= N_CHIP:
            g.round(r)
            for mask in g.READY[r]:
                use_dh(mask)

    s = Scatter(*scr[:4], sems[18:], me)
    total = s.run(block_product(s, glu_ref, down_ref, glu_t), between)
    y_ref[...] = (h_ref[...].astype(F32) + total[...]).astype(BF16)
    s.finish()
    g.finish()
    for swap in (gates, ups):
        swap.wait_recv(SETS[0])
        swap.wait_send(SETS[0])
    ucols.wait_recv()
    ucols.wait_send()
    leave.wait()
    ends = ((full_m.at[0], m_out.at[0]), (dgu_ref.at[:, seg(0, WIDE)], dgu_out.at[:, seg(0, WIDE)]))
    loop(N_CHIP, lambda j: [pltpu.make_async_copy(src, dst, osem.at[j, i]).wait() for i, (src, dst) in enumerate(ends)])


def back(groups, hd, qkv_hbm, do_hbm, stat_ref, cos_all, sin_all, dgu_hbm, m_hbm, ucol_ref, w_hbm, x_ref, small_all, dh_ref, dg2_ref, dg_in, du_in,
         dg_hbm, du_hbm, dwq_ref, dwkv_ref, dx_ref, gain_ref,
         dgu_ref, qkv_ref, do_ref, isem, qsem,
         p_scr, dp_scr, k_scr, v_scr, dk_acc, dv_acc, stage, dq_scr, dkv_scr, m_scr,
         full, w_scr, shares, dkv_own, full_kv, dqkv, dn, g_scr, dg1, gains, gains_in, wsem, lsem, msem, *sems):
    heads = qkv_ref.shape[0] // hd - 2
    seq = qkv_ref.shape[1]
    scale = hd ** -0.5
    lanes = heads * QB
    qw = heads * hd
    half = hd // 2
    me = lax.axis_index('sp')
    feat = dgu_ref.shape[0] // 2
    first = (X, Y + Z, Y, X + Z, Z, X + Y, 0)

    def fetch(mask):
        cols = seg(flipped(me, mask) // 2, WIDE)
        return pltpu.make_async_copy(m_hbm.at[:, :, cols], m_scr.at[:, :, cols], msem.at[mask // 2])
    needed, = fetch_all(isem, (dgu_hbm, dgu_ref))
    for mask in first[:2]:
        fetch(mask).start()
    load = pltpu.make_async_copy(w_hbm, w_scr, wsem)
    enter(me, OTHERS)
    for mask in first[2:]:
        fetch(mask).start()
    loads = fetch_all(qsem, (qkv_hbm, qkv_ref), (do_hbm, do_ref))
    gain_row(g_scr, small_all, 0)

    gates, ups = dw_swaps(lambda peer: stage.at[peer // 2], dg_hbm, du_hbm, sems[:4], me)
    gq = row_gather(dq_scr, full, sems[6:10], me)
    own = [pltpu.make_async_copy(swap.src(me), swap.dst(me), lsem.at[i]) for i, swap in enumerate((gates, ups))]

    def make(mask):
        chip = flipped(me, mask) // 2
        fetch(mask).wait()
        cols = m_scr[:, :, seg(chip, WIDE)].reshape(seq, WIDE)
        stage[chip] = mm(dgu_ref[...], cols, NN)

    def advance(n):
        for swap in (gates, ups):
            if n > 1:
                swap.wait_send(SETS[n - 1])
            swap.start(SETS[n])

    needed.wait()
    for i, mask in enumerate(first):
        make(mask)
        if i == 1:
            advance(1)
    load.start()
    for copy in loads:
        copy.wait()
    gates.start((CORE,))
    ups.start((CORE,))
    for copy in own:
        copy.start()

    dk_acc[...] = jnp.zeros_like(dk_acc)
    dv_acc[...] = jnp.zeros_like(dv_acc)
    key_rows(k_scr, qkv_ref, qw, hd)
    key_rows(v_scr, qkv_ref, qw + hd, hd)

    def q_block(qb):
        @pl.when(qb == 4)
        def _():
            advance(2)
        qs = seg(qb, QB)
        q2 = side_by_side(qkv_ref, heads, hd, qs)
        do2 = side_by_side(do_ref, heads, hd, qs)
        top = stat_ref[qb, :1, :]
        inv = stat_ref[qb, 1:, :]

        def probs(kb, rd, diagonal):
            ks = seg(kb, KB)
            s = score_block(k_scr[ks, :], q2, scale, diagonal)
            p = jnp.exp(s - top) * inv
            dp = mm(v_scr[ks, :], do2, NN).astype(BF16)
            p_scr[ks, :] = p
            dp_scr[ks, :] = dp
            dv_acc[ks, :] += mm(p.astype(BF16), do2, NT)
            return rd + jnp.sum(dp.astype(F32) * p, axis=0, keepdims=True)

        rd = lax.fori_loop(0, qb, lambda kb, r: probs(kb, r, False), jnp.zeros((1, lanes), F32))
        rd = probs(qb, rd, True)

        def d_scores(kb, acc):
            ks = seg(kb, KB)
            ds = (p_scr[ks, :] * (dp_scr[ks, :].astype(F32) - rd) * scale).astype(BF16)
            dk_acc[ks, :] += mm(ds, q2, NT)
            return acc + mm(qkv_ref[qw:qw + hd, ks], ds, NN)

        acc = lax.fori_loop(0, qb + 1, d_scores, jnp.zeros((hd, lanes), F32))
        cos, sin = cos_all[:, qs], sin_all[:, qs]
        for h in range(heads):
            dq = acc[:, h * QB:(h + 1) * QB].astype(BF16).astype(F32)
            p, q = dq[:half], dq[half:]
            dq_scr[h * hd:h * hd + half, qs] = (p * cos + q * sin).astype(BF16)
            dq_scr[h * hd + half:(h + 1) * hd, qs] = (q * cos - p * sin).astype(BF16)

    loop(seq // QB, q_block)

    def share(i):
        rs = seg(i, WIDE)
        dkv_scr[rs, :] = jnp.concatenate([dk_acc[rs, :], dv_acc[rs, :]], axis=1).astype(BF16)
    loop(seq // WIDE, share)
    tokens = ucol_ref.shape[1]
    per = N_DEV // groups
    q_all = dwq_ref.shape[0]
    sh = Swap(lambda peer: dkv_scr.at[seg(peer, tokens), :], lambda o: shares.at[o], sems[4:6], me)
    parts = thirds(dkv_own.shape[0], STRIP)
    gk = Gather(dkv_own, lambda o: full_kv.at[:, seg(o, tokens)], lambda view, c: [view.at[pl.ds(*parts[c]), :]], sems[10:14], me)
    gs = Swap(lambda peer: gains.at[:, seg(peer)], lambda o: gains_in.at[o], sems[14:], me)
    sh.start()
    gq.start()
    keep_own(dq_scr, full, me)
    shares[me] = dkv_scr[seg(me, tokens), :]
    sh.wait_recv()
    cos, sin = cos_all[:, seg(me)], sin_all[:, seg(me)]
    for k in range(groups):
        both = sum(shares[per * k + i].astype(F32) for i in range(per)).astype(BF16).astype(F32).T
        p, q = both[:half], both[half:hd]
        lo = 2 * hd * k
        dkv_own[lo:lo + half, :] = (p * cos + q * sin).astype(BF16)
        dkv_own[lo + half:lo + hd, :] = (q * cos - p * sin).astype(BF16)
        dkv_own[lo + hd:lo + 2 * hd, :] = both[hd:].astype(BF16)
    gk.start()
    full_kv[:, seg(me, tokens)] = dkv_own[...]
    for k in range(groups):
        dqkv[:, q_all + 2 * hd * k:q_all + 2 * hd * (k + 1)] = dkv_own[2 * hd * k:2 * hd * (k + 1), :].T

    def use(mask):
        gq.wait_pair(mask)
        chip = flipped(me, mask) // 2
        dwq_ref[seg(chip, WIDE), :] = mm(full[chip], ucol_ref[...], NN)
        dqkv[:, seg(chip, WIDE)] = full[chip, :, seg(me, tokens)].T

    for r in range(len(gq.ROUNDS)):
        gq.round(r)
        gk.round(r)
        if r == 3:
            advance(3)
        for mask in gq.READY[r]:
            use(mask)
    load.wait()

    def normed(i):
        dn[:, seg(i, WIDE)] = mm(dqkv[...], w_scr[i], NN)
    loop(N_CHIP, normed)
    norm_back(dn, x_ref, g_scr, dh_ref, dx_ref, dg1)
    gains[...] = jnp.concatenate([jnp.sum(dg1[...], axis=0, keepdims=True), jnp.sum(dg2_ref[...], axis=0, keepdims=True),
                                  jnp.zeros((N_CHIP - 2, dg1.shape[1]), F32)], axis=0)
    gs.start()
    gains_in[me] = gains[:, seg(me)]
    for mask in CHIP_MASKS:
        gk.wait_pair(mask)
    dwkv_ref[...] = mm(full_kv[...], ucol_ref[...], NN)
    gs.wait_recv()
    gain_ref[...] = sum(gains_in[o] for o in range(N_DEV))
    for swap in (gates, ups):
        swap.wait_recv((CORE,) + SETS[1] + SETS[2] + SETS[3])
        swap.wait_send((CORE,) + SETS[3])
    for copy in own:
        copy.wait()
    for c in (sh, gs):
        c.wait_send()
    for g in (gq, gk):
        g.finish()


def finish(dg_hbm, du_hbm, dkv_hbm, *refs):
    n = (len(refs) - 14) // 3
    gains, refs = refs[0], refs[1:]
    srcs, (gate, up, dk, dv, dg1, dg2), refs = refs[:n], refs[n:n + 6], refs[n + 6:]
    dsts, (g_in, g_out, kv_in), holds, sems = refs[:n], refs[n:n + 3], refs[n + 3:2 * n + 3], refs[2 * n + 3:]
    dg1[...] = gains[:1, :]
    dg2[...] = gains[1:2, :]
    t_in, t_out, p_in, p_out = sems
    step = LANE * 11
    cols = g_in.shape[1]
    hd = dk.shape[0] // (kv_in.shape[0] // LANE)
    starts = [(w, i) for i in range(cols // step) for w in range(2)]

    def fetch(w, i):
        rs = pl.ds(i * step, step)
        return pltpu.make_async_copy((dg_hbm, du_hbm)[w].at[rs, :], g_in.at[w, rs, :], t_in.at[w, i])

    def put(w, i):
        cs = pl.ds(i * step, step)
        return pltpu.make_async_copy(g_out.at[w, :, cs], (gate, up)[w].at[:, cs], t_out.at[w, i])
    moves = [(pltpu.make_async_copy(a, h, p_in.at[k]), pltpu.make_async_copy(h, b, p_out.at[k])) for k, (a, h, b) in enumerate(zip(srcs, holds, dsts))]
    kv = pltpu.make_async_copy(dkv_hbm, kv_in, p_in.at[n])
    for w, i in starts:
        fetch(w, i).start()
    kv.start()
    for load, _ in moves:
        load.start()
    for w, i in starts:
        fetch(w, i).wait()

        at = pl.ds(i * step, step)
        g_out[w, :, at] = g_in[w, at, :].T
        put(w, i).start()
    kv.wait()
    for k in range(dk.shape[0] // hd):
        for i, ref in enumerate((dk, dv)):
            ref[k * hd:(k + 1) * hd, :] = kv_in[(2 * k + i) * hd:(2 * k + i + 1) * hd, :]
    for load, store in moves:
        load.wait()
        store.start()
    for w, i in starts:
        put(w, i).wait()
    for _, store in moves:
        store.wait()


def solution(mesh):
    assert mesh.shape['sp'] == N_DEV

    def layer_step(x_in, positions, d_out, norm1_gain, norm2_gain, w_q, w_k, w_v, w_o, w_gate, w_up, w_down):
        tokens, dim = x_in.shape
        seq = tokens * N_DEV
        n_q, hd = w_q.shape[1:]
        n_kv = w_k.shape[1]
        qw = n_q // N_DEV * hd
        rows = w_q.shape[0]
        feat = w_down.shape[0]
        cols = (n_q + 2 * n_kv) * hd
        lanes = qw // hd * QB
        vm = pltpu.VMEM
        full = vm((N_CHIP, WIDE, dim), BF16)
        gain_scr = vm((N_CHIP, dim), F32)
        tok_shapes = 2 * (((tokens, dim), BF16),)
        dw_shapes = 2 * (((feat * N_DEV, rows), F32),)

        inv_freq = 1.0 / (ROPE_BASE ** (jnp.arange(hd // 2, dtype=F32) * (2.0 / hd)))
        freq = jnp.broadcast_to(inv_freq[:, None], (hd // 2, rows))
        row = lambda v: v.reshape(1, rows)
        by_head = lambda w: w.transpose(1, 2, 0).reshape(-1, rows)
        wo_own = w_o.reshape(qw, dim)

        args = (x_in, row(norm1_gain), row(norm2_gain), row(positions), by_head(w_q), by_head(w_k), by_head(w_v), freq, w_gate, w_up, wo_own)
        qkv, u, small_all, wqkv, attn_t, stat, wgu, hidden, mlp_in, cos_all, sin_all = call(
            functools.partial(head, n_kv, hd), 0, len(args),
            (((qw + 2 * hd, seq), BF16), tok_shapes[0], ((N_DEV, N_CHIP, rows), F32), ((N_CHIP, cols, WIDE), BF16),
             ((qw, seq), BF16), ((seq // QB, 2, lanes), F32), ((2 * feat, dim), BF16), *tok_shapes, *(2 * (((hd // 2, seq), F32),))),
            [vm(w_gate.shape, BF16), vm(w_up.shape, BF16), vm((qw, dim), BF16), vm((qw + 2 * hd, seq), BF16), vm((tokens, dim), BF16),
             vm((hd // 2, seq), F32), vm((hd // 2, seq), F32), dma(3), dma(4),
             full, vm((tokens, dim), F32), vm((tokens, dim), BF16), vm((seq, qw), BF16),
             vm((N_CHIP, rows), F32), vm((cols, rows), BF16), vm((N_CHIP, cols, WIDE), BF16), vm((cols, tokens), F32), vm((cols, tokens), BF16), gain_scr,
             vm((feat * N_DEV, rows), BF16), vm((feat * N_DEV, rows), BF16), vm((seq, lanes), F32), vm((seq, hd), BF16), dma(N_CHIP),
             *Gather.sems, *(6 * Swap.sems), *Gather.sems], 4 * qw * seq * seq, far_in=(8, 9, 10), far_out=(0, 1, 3, 9, 10))(*args)
        args = (mlp_in, d_out, wgu, w_down, u, hidden, small_all, wo_own, attn_t)
        u_col, m_full, dgu, d_down, y_out, d_hidden, d_attn, d_wo, d_g2, d_gate_t, d_up_t = call(
            mlp, 1, len(args),
            (((seq, rows), BF16), ((N_CHIP, WIDE, dim), BF16), ((2 * feat, seq), BF16), ((feat, dim), F32),
             *tok_shapes, ((qw, seq), BF16), ((qw, dim), F32), ((N_CHIP, dim), F32), *dw_shapes),
            [vm((2 * feat, dim), BF16), vm((feat, dim), BF16),
             vm((feat, seq), BF16), vm((2 * feat, seq), BF16), vm((feat, dim), F32), dma(2), dma(),
             full, full, dma(N_CHIP, 2), vm((2 * feat, WIDE), F32), gain_scr, vm((WIDE, 2 * feat), BF16), vm((WIDE, feat), BF16), pltpu.SemaphoreType.REGULAR,
             *Scatter.scratch(tokens, dim), *(3 * Gather.sems), *(3 * Swap.sems), *Scatter.sems], 12 * feat * seq * dim,
            far_in=(2, 3), far_out=(1, 2, 3, 9, 10))(*args)
        args = (qkv, d_attn, stat, cos_all, sin_all, dgu, m_full, u_col, wqkv, x_in, small_all, d_hidden, d_g2, d_gate_t, d_up_t)
        d_gate_t, d_up_t, d_wq, d_wkv, d_x, gains = call(
            functools.partial(back, n_kv, hd), 3, len(args),
            (*dw_shapes, ((n_q * hd, rows), F32), ((2 * n_kv * hd, rows), F32), tok_shapes[0], ((N_CHIP, rows), F32)),
            [vm((2 * feat, seq), BF16), vm((qw + 2 * hd, seq), BF16), vm((qw, seq), BF16), dma(1), dma(2),
             vm((seq, lanes), F32), vm((seq, lanes), BF16), vm((seq, hd), BF16), vm((seq, hd), BF16), vm((seq, hd), F32), vm((seq, hd), F32),
             vm((N_CHIP, 2 * feat, WIDE), F32), vm((qw, seq), BF16), vm((seq, 2 * hd), BF16), full,
             full, vm((N_CHIP, cols, WIDE), BF16), vm((N_DEV, tokens, 2 * hd), BF16), vm((2 * n_kv * hd, tokens), BF16), vm((2 * n_kv * hd, seq), BF16),
             vm((tokens, cols), BF16), vm((tokens, dim), F32), gain_scr, gain_scr, gain_scr, vm((N_DEV, N_CHIP, rows), F32), dma(), dma(2), dma(N_CHIP),
             *(3 * Swap.sems), *(2 * Gather.sems), *Swap.sems], 10 * qw * seq * seq, far_in=(0, 1, 5, 6, 8, 13, 14), far_out=(0, 1), aliases={13: 0, 14: 1})(*args)
        moved = (d_wq, d_wo, d_down, d_x, y_out)
        one_row = jax.ShapeDtypeStruct((1, rows), F32)
        half_kv = jax.ShapeDtypeStruct((n_kv * hd, rows), F32)
        wide = jax.ShapeDtypeStruct((rows, feat * N_DEV), F32)
        d_gate, d_up, d_wk, d_wv, d_g1, d_g2, d_wq, d_wo, d_down, d_x, y_out = pl.pallas_call(
            finish,
            out_shape=[wide, wide, half_kv, half_kv, one_row, one_row] + [jax.ShapeDtypeStruct(v.shape, v.dtype) for v in moved],
            in_specs=[IN_HBM] * 3 + on_chip(1) + [IN_HBM] * len(moved), out_specs=[IN_HBM] * 2 + on_chip(4) + [IN_HBM] * len(moved),
            scratch_shapes=[vm((2, feat * N_DEV, rows), F32), vm((2, rows, feat * N_DEV), F32), vm(d_wkv.shape, F32)]
            + [vm(v.shape, v.dtype) for v in moved] + [dma(2, 4), dma(2, 4), dma(len(moved) + 1), dma(len(moved))],
            compiler_params=pltpu.CompilerParams(vmem_limit_bytes=VMEM_CAP), name='finish',
        )(d_gate_t, d_up_t, d_wkv, gains, *moved)
        by_row = lambda g, heads: g.reshape(heads, hd, rows).transpose(2, 0, 1)
        return (y_out, d_x, d_g1.reshape(rows), d_g2.reshape(rows), by_row(d_wq, n_q), by_row(d_wk, n_kv), by_row(d_wv, n_kv),
                d_wo.reshape(w_o.shape), d_gate, d_up, d_down)

    all_rows = P('sp')
    return jax.shard_map(layer_step, mesh=mesh, in_specs=(all_rows,) * 12, out_specs=(all_rows,) * 11, check_vma=False)
```

```python
import functools
import jax
import jax.numpy as jnp
from jax import lax
from jax.experimental import pallas as pl
from jax.experimental.pallas import tpu as pltpu
from jax.sharding import PartitionSpec as P

ROPE_BASE = 10000.0
NORM_EPS = 1e-5
NEG_LARGE = -1e30
F32 = jnp.float32
BF16 = jnp.bfloat16
N_DEV, N_CHIP, LANE, WIDE, CHUNK, STRIP = 16, 8, 128, 256, 512, 16
NT = (((1,), (1,)), ((), ()))
TN = (((0,), (0,)), ((), ()))
NN = (((1,), (0,)), ((), ()))
MESH = pl.DeviceIdType.MESH
VMEM_CAP = 67043328

CORE, X, Y, Z = 1, 2, 4, 8
XYZ = X + Y + Z
ORDERS = ((X, Y, Z), (Y, Z, X), (Z, X, Y))
CHIP_MASKS = (0, X, Y, Z, X + Y, X + Z, Y + Z, XYZ)
NEAR = (CORE, X, Y, Z)
OTHERS = range(1, N_DEV)
SETS = tuple(tuple(m + c for m in masks for c in (0, CORE)) for masks in ((XYZ,), (X, Y + Z), (Y, X + Z), (Z, X + Y)))
N_COL = len(ORDERS)
COLOURS = range(N_COL)


def mm(a, b, dims):
    return lax.dot_general(a, b, dims, preferred_element_type=F32)


def seg(index, width=LANE):
    return pl.ds(pl.multiple_of(index * width, width), width)


def loop(count, body):
    lax.fori_loop(0, count, lambda i, c: (body(i), c)[1], 0)


def differing(index, mask):
    return sum(((index // bit + mask // bit) % 2) * bit for bit in NEAR)


def flipped(index, mask):
    if not isinstance(mask, int):
        return differing(index, mask)
    out = index
    for bit in NEAR:
        if mask & bit:
            out = out + (1 - 2 * ((index // bit) % 2)) * bit
    return out


def run_ready(masks, use):
    if len(masks) == 2:
        loop(2, lambda j: use(masks[0] + (masks[1] - masks[0]) * j))
    else:
        for mask in masks:
            use(mask)


def thirds(total, unit):
    n = total // unit
    first = (n + 2) // 3
    second = (n - first + 1) // 2
    sizes = (first * unit, second * unit, (n - first - second) * unit)
    return ((0, sizes[0]), (sizes[0], sizes[1]), (sizes[0] + sizes[1], sizes[2]))


def pieces(rows, cols, unit):
    share = cols // LANE // N_COL * LANE
    strips = thirds(rows, unit)
    rest = cols - N_COL * share
    return [[(pl.ds(0, rows), pl.ds(c * share, share)), (pl.ds(*strips[c]), pl.ds(N_COL * share, rest))] for c in COLOURS]


def enter(me, masks):
    barrier = pltpu.get_barrier_semaphore()
    for mask in masks:
        pl.semaphore_signal(barrier, inc=1, device_id=(flipped(me, mask),), device_id_type=MESH)
    pl.semaphore_wait(barrier, len(masks))


def remote(src, dst, send, recv, peer):
    return pltpu.make_async_remote_copy(src_ref=src, dst_ref=dst, send_sem=send, recv_sem=recv, device_id=(peer,), device_id_type=MESH)


def dma(*shape):
    return pltpu.SemaphoreType.DMA(shape)


class Swap:
    sems = (dma(N_DEV), dma(N_DEV))

    def __init__(self, src, dst, sems, me):
        self.src, self.dst, (self.send, self.recv), self.me = src, dst, sems, me

    def copy(self, mask):
        peer = differing(self.me, mask)
        return remote(self.src(peer), self.dst(self.me), self.send.at[mask], self.recv.at[mask], peer)

    def arrival(self, mask):
        view = self.dst(differing(self.me, mask))
        return remote(view, view, self.send.at[mask], self.recv.at[mask], self.me)

    def each(self, masks, act):
        if masks is None:
            loop(N_DEV - 1, lambda i: act(i + 1))
        else:
            for mask in masks:
                act(mask)

    def start(self, masks=None):
        self.each(masks, lambda mask: self.copy(mask).start())

    def advance(self, n):
        if n:
            self.wait_send(SETS[n - 1])
        self.start(SETS[n])

    def wait_recv(self, masks=None):
        self.each(masks, lambda mask: self.arrival(mask).wait_recv())

    def wait_send(self, masks=None):
        self.each(masks, lambda mask: self.copy(mask).wait_send())


class Gather:
    ROUNDS = ((0,), (1,), (2,), (0, 1), (0, 2), (1, 2), (0, 1, 2))
    READY = ((0,), (), (), (X, Y), (Z,), (X + Y, X + Z), (Y + Z, XYZ))
    sems = (dma(N_COL, N_CHIP, 2), dma(N_COL, N_CHIP, 2), dma(N_CHIP), dma(N_CHIP))

    def __init__(self, own, block, cut, sems, me):
        self.own, self.block, self.cut, self.me = own, block, cut, me
        self.send, self.recv, self.pair_send, self.pair_recv = sems

    def source(self, mask):
        return self.block(flipped(self.me, mask)) if mask else self.own

    def unit(self, colour, mask, axis):
        ends = zip(self.cut(self.source(mask), colour), self.cut(self.block(flipped(self.me, mask)), colour))
        j = self.sends(colour).index((mask, axis))
        return [remote(src, dst, self.send.at[colour, j, i], self.recv.at[colour, (mask + axis) // 2, i],
                       flipped(self.me, axis)) for i, (src, dst) in enumerate(ends)]

    def sends(self, colour):
        return [(0, axis) for axis in ORDERS[colour]] + [step[1:] for step in self.onward(colour)]

    def start_unit(self, colour, mask, axis):
        for copy in self.unit(colour, mask, axis):
            copy.start()

    def pair(self, mask):
        return remote(self.source(mask), self.block(flipped(self.me, mask)), self.pair_send.at[mask // 2],
                      self.pair_recv.at[mask // 2], flipped(self.me, CORE))

    def wait_pair(self, mask):
        view = self.block(flipped(self.me, mask + CORE))
        remote(view, view, self.pair_send.at[mask // 2], self.pair_recv.at[mask // 2], self.me).wait_recv()

    def onward(self, colour):
        order = ORDERS[colour]
        for picks in self.ROUNDS:
            for axis in order[picks[-1] + 1:]:
                yield picks, sum(order[p] for p in picks), axis

    def start(self):
        for pos in COLOURS:
            for colour in COLOURS:
                self.start_unit(colour, 0, ORDERS[colour][pos])
        self.pair(0).start()

    def round(self, r):
        for colour in COLOURS:
            mask = sum(ORDERS[colour][p] for p in self.ROUNDS[r])
            for i, view in enumerate(self.cut(self.block(flipped(self.me, mask)), colour)):
                remote(view, view, self.send.at[colour, 0, i], self.recv.at[colour, mask // 2, i], self.me).wait_recv()
            for picks, at, axis in self.onward(colour):
                if picks == self.ROUNDS[r]:
                    self.start_unit(colour, at, axis)
        for mask in {2: (X, Y, Z), 5: (X + Y, X + Z, Y + Z), 6: (XYZ,)}.get(r, ()):
            self.pair(mask).start()

    def finish(self):
        for colour in COLOURS:
            for i, view in enumerate(self.cut(self.own, colour)):
                loop(len(self.sends(colour)), lambda j: remote(view, view, self.send.at[colour, j, i], self.recv.at[colour, j, i], self.me).wait_send())
        loop(N_CHIP, lambda j: remote(self.own, self.own, self.pair_send.at[j], self.pair_recv.at[j], self.me).wait_send())


def row_gather(own, full, sems, me, extra=None):
    rows, width = own.shape
    parts = pieces(rows, width, STRIP)
    if extra is not None:
        share = width // LANE // N_COL * LANE
        more = width - N_COL * share
        parts = [[(pl.ds(0, rows), pl.ds(c * share + more * (c > extra), share + more * (c == extra)))] for c in COLOURS]

    def block(o):
        return full.at[o // 2, seg(o % 2), :]

    return Gather(own, block, lambda view, c: [view.at[rs, cs] for rs, cs in parts[c]], sems, me)


def keep_own(own, full, me):
    def step(i):
        full[me // 2, pl.ds(pl.multiple_of((me % 2) * LANE + i * STRIP, STRIP), STRIP), :] = own[seg(i, STRIP), :]
    loop(LANE // STRIP, step)


class Scatter:
    ORDER = (XYZ, X + Y, Y + Z, X + Z, X, Y, Z, 0)
    sems = (dma(N_CHIP), dma(N_CHIP), dma(N_COL, N_CHIP, 2), dma(N_COL, N_CHIP, 2))

    @staticmethod
    def scratch(tokens, dim):
        return [pltpu.VMEM((n, tokens, dim), F32) for n in (N_CHIP, 2, N_CHIP, N_CHIP - 1)]

    def __init__(self, part, other, pair_in, link_in, sems, me):
        self.part, self.other, self.pair_in, self.link_in, self.me = part, other, pair_in, link_in, me
        self.pair_send, self.pair_recv, self.link_send, self.link_recv = sems
        self.tokens, self.dim = part.shape[1:]
        self.pieces = pieces(self.tokens, self.dim, STRIP // 2)
        self.ready, self.sent = set(), [0] * N_COL

    @staticmethod
    def first(colour, mask):
        return next((i for i, a in enumerate(ORDERS[colour]) if mask & a), 3)

    def slot(self, colour, mask, axis):
        slots = [(m, a) for m in self.ORDER for a in ORDERS[colour][:self.first(colour, m)]]
        return slots.index((mask, axis))

    def pair(self, i):
        return remote(self.other.at[i % 2], self.pair_in.at[i], self.pair_send.at[i], self.pair_recv.at[i], flipped(self.me, CORE))

    def link(self, colour, mask):
        axis = ORDERS[colour][self.first(colour, mask)]
        slot = self.slot(colour, mask - axis, axis)
        i = self.ORDER.index(mask)
        return [remote(self.part.at[i, rs, cs], self.link_in.at[slot, rs, cs], self.link_send.at[colour, i, k],
                       self.link_recv.at[colour, slot, k], flipped(self.me, axis)) for k, (rs, cs) in enumerate(self.pieces[colour])]

    def start_link(self, colour, mask):
        for copy in self.link(colour, mask):
            copy.start()

    def add(self, mask, ref, cs):
        i = self.ORDER.index(mask)

        def step(r):
            rs = seg(r, STRIP)
            self.part[i, rs, cs] += ref[rs, cs]
        loop(self.tokens // STRIP, step)

    def finish_pair(self, i):
        self.pair(i).wait_recv()
        self.add(self.ORDER[i], self.pair_in.at[i], pl.ds(0, self.dim))
        self.ready.add(self.ORDER[i])
        for colour in COLOURS:
            a, b, c = ORDERS[colour]
            todo = (XYZ, a + b, a + c, a)
            while self.sent[colour] < len(todo) and todo[self.sent[colour]] in self.ready:
                self.start_link(colour, todo[self.sent[colour]])
                self.sent[colour] += 1

    def take(self, colour, mask, axis):
        for copy in self.link(colour, mask + axis):
            copy.wait_recv()
        ref = self.link_in.at[self.slot(colour, mask, axis)]
        (_, wide), (rs, cs) = self.pieces[colour]
        self.add(mask, ref, wide)
        self.part[self.ORDER.index(mask), rs, cs] += ref[rs, cs]

    def run(self, product, between=lambda i: None):
        for i, mask in enumerate(self.ORDER):
            if i > 1:
                self.pair(i - 2).wait_send()
            product(i, flipped(self.me, mask) // 2)
            self.pair(i).start()
            if i:
                self.finish_pair(i - 1)
            between(i)
        self.finish_pair(N_CHIP - 1)
        for step in range(2):
            between(N_CHIP + step)
            for colour in COLOURS:
                a, b, c = ORDERS[colour]
                mask = (b + c, b)[step]
                self.take(colour, mask, a)
                self.start_link(colour, mask)
        between(N_CHIP + 2)
        for colour in COLOURS:
            a, b, c = ORDERS[colour]
            self.take(colour, c, a)
            self.take(colour, c, b)
            self.start_link(colour, c)
        between(N_CHIP + 3)
        for colour in COLOURS:
            for axis in ORDERS[colour]:
                self.take(colour, 0, axis)
        return self.part.at[N_CHIP - 1]

    def finish(self):
        for i in (N_CHIP - 2, N_CHIP - 1):
            self.pair(i).wait_send()
        for colour in COLOURS:
            for k, (rs, cs) in enumerate(self.pieces[colour]):
                view = self.part.at[0, rs, cs]
                loop(N_CHIP - 1, lambda i: remote(view, view, self.link_send.at[colour, i, k], self.link_recv.at[colour, i, k], self.me).wait_send())


def block_product(s, a_ref, w_ref, a_t):
    core = s.me % 2

    def product(i, chip):
        a_t[...] = a_ref[:, seg(chip, WIDE)].T

        def step(n):
            cs = seg(n, CHUNK)
            s.other[i % 2, :, cs] = mm(a_t[seg(1 - core), :], w_ref[:, cs], NN)
            s.part[i, :, cs] = mm(a_t[seg(core), :], w_ref[:, cs], NN)
        loop(s.dim // CHUNK, step)
    return product


def on_chip(n):
    return [pl.BlockSpec(memory_space=pltpu.VMEM)] * n


IN_HBM = pl.BlockSpec(memory_space=pl.ANY)


def call(kernel, ident, args, outs, scratch, flops, far_in=(), far_out=(), aliases={}):
    specs = [IN_HBM if i in far_in else on_chip(1)[0] for i in range(args)]
    out_specs = [IN_HBM if i in far_out else on_chip(1)[0] for i in range(len(outs))]
    return pl.pallas_call(
        kernel,
        out_shape=[jax.ShapeDtypeStruct(shape, dtype) for shape, dtype in outs],
        in_specs=specs, out_specs=out_specs, scratch_shapes=scratch, input_output_aliases=aliases,
        cost_estimate=pl.CostEstimate(flops=flops, bytes_accessed=flops // CHUNK, transcendentals=0),
        compiler_params=pltpu.CompilerParams(collective_id=ident, has_side_effects=True, vmem_limit_bytes=VMEM_CAP),
        name=kernel.func.__name__ if isinstance(kernel, functools.partial) else kernel.__name__,
    )


def fetch_all(sem, *pairs):
    copies = [pltpu.make_async_copy(src, dst, sem.at[i]) for i, (src, dst) in enumerate(pairs)]
    for copy in copies:
        copy.start()
    return copies


def gain_row(dst, small_all, which):
    for o in range(N_DEV):
        dst[:1, o * LANE:(o + 1) * LANE] = small_all[o, which:which + 1, :]


def norm_rows(src, gain, dst):
    def step(i):
        rs = seg(i, STRIP)
        t = src[rs, :].astype(F32)
        dst[rs, :] = (t * lax.rsqrt(jnp.mean(t * t, axis=-1, keepdims=True) + NORM_EPS) * gain[:1, :]).astype(BF16)
    loop(src.shape[0] // STRIP, step)


def norm_back(dy, src, gain, skip, dst, dgain):
    def step(i):
        rs = seg(i, STRIP)
        d = dy[rs, :].astype(BF16).astype(F32)
        t = src[rs, :].astype(F32)
        inv = lax.rsqrt(jnp.mean(t * t, axis=-1, keepdims=True) + NORM_EPS)
        gd = gain[:1, :] * d
        pull = jnp.mean(gd * t, axis=-1, keepdims=True)
        dst[rs, :] = (skip[rs, :].astype(F32) + (inv * gd - t * (inv * inv * inv * pull))).astype(BF16)
        g = d * (t * inv)
        dgain[...] += g[:N_CHIP] + g[N_CHIP:]
    dgain[...] = jnp.zeros_like(dgain)
    loop(src.shape[0] // STRIP, step)


QB = 256
KB = 256


def key_rows(dst, src, lo, hd):
    def step(i):
        dst[seg(i, KB), :] = src[lo:lo + hd, seg(i, KB)].T
    loop(src.shape[1] // KB, step)


def score_block(k, q2, scale, diagonal):
    s = mm(k, q2, NN) * scale
    if diagonal:
        key = lax.broadcasted_iota(jnp.int32, s.shape, 0)
        qry = lax.broadcasted_iota(jnp.int32, s.shape, 1) % QB
        s = jnp.where(qry >= key, s, NEG_LARGE)
    return s


def side_by_side(ref, heads, hd, qs):
    return jnp.concatenate([ref[h * hd:(h + 1) * hd, qs] for h in range(heads)], axis=1)


def head(groups, hd, x_ref, g1_ref, g2_ref, pos_ref, wq_ref, wk_ref, wv_ref, freq_ref, wg_hbm, wu_hbm, wo_hbm, qkv_out, u_out, small_all, w_out, o_ref, stat_ref, wgu_ref, h_ref, m_ref, cos_out, sin_out,
         wg_ref, wu_ref, wo_ref, qkv_ref, u_scr, cos_ref, sin_ref, isem, esem,
         full_w, acc_o, o_tok, o_send, small_ref, w_ref, full, acc, rot, g_scr, wg_t, wu_t, s_scr, k_scr, osem, *sems):
    me = lax.axis_index('sp')
    tokens, dim = x_ref.shape
    cols = w_ref.shape[0]
    small_ref[...] = jnp.concatenate([r[...].astype(F32) for r in (g1_ref, g2_ref, pos_ref)] + [jnp.zeros((N_CHIP - 3, LANE), F32)], axis=0)
    w_ref[:wq_ref.shape[0], :] = wq_ref[...]
    for k in range(groups):
        for i, ref in enumerate((wk_ref, wv_ref)):
            w_ref[pl.ds(wq_ref.shape[0] + (2 * k + i) * hd, hd), :] = ref[k * hd:(k + 1) * hd, :]
    qw = tokens
    q_all = N_DEV * qw
    gsems, ssems, qsems, ksems, gate_sems, up_sems, osems = sems[:4], *(sems[i:i + 2] for i in range(4, len(sems) - 4, 2))
    gw = row_gather(wo_ref, full_w, sems[-4:], me, 1)
    feat = wg_ref.shape[1] // N_DEV
    loads = fetch_all(isem, (wg_hbm, wg_ref), (wu_hbm, wu_ref), (wo_hbm, wo_ref))
    enter(me, OTHERS)
    smalls = Swap(lambda peer: small_ref, lambda o: small_all.at[o], ssems, me)
    smalls.start()
    parts = thirds(cols, STRIP)
    g = Gather(w_ref, lambda o: full.at[o // 2, :, seg(o % 2)], lambda view, c: [view.at[pl.ds(*parts[c]), :]], gsems, me)
    g.start()
    gates = Swap(lambda peer: wg_t.at[seg(peer, feat), :], lambda o: wgu_ref.at[:feat, seg(o)], gate_sems, me)
    ups = Swap(lambda peer: wu_t.at[seg(peer, feat), :], lambda o: wgu_ref.at[feat:, seg(o)], up_sems, me)

    def advance(n):
        gates.advance(n)
        ups.advance(n)

    def transpose(i):
        wg_t[seg(i, CHUNK), :] = wg_ref[:, seg(i, CHUNK)].T
        wu_t[seg(i, CHUNK), :] = wu_ref[:, seg(i, CHUNK)].T
    for load in loads:
        load.wait()
    loop(wg_ref.shape[1] // CHUNK, transpose)
    advance(0)

    def own_block(i):
        full[me // 2, seg(i, WIDE), seg(me % 2)] = w_ref[seg(i, WIDE), :]
    loop(cols // WIDE, own_block)
    acc[...] = jnp.zeros_like(acc)
    small_all[me] = small_ref[...]
    smalls.wait_recv()
    gain_row(g_scr, small_all, 0)
    norm_rows(x_ref, g_scr, u_scr)

    def keep(mask):
        chip = flipped(me, mask) // 2
        return pltpu.make_async_copy(full.at[chip], w_out.at[chip], osem.at[mask // 2])

    def use(mask):
        g.wait_pair(mask)
        keep(mask).start()
        chip = flipped(me, mask) // 2
        u = u_scr[:, seg(chip, WIDE)]

        def step(i):
            rs = seg(i, cols // 2)
            acc[rs, :] += mm(full[chip, rs, :], u, NT)
        loop(2, step)

    def tables(o):
        angles = freq_ref[...] * small_all[o, 2:3, :]
        cos_ref[:, seg(o)] = jnp.cos(angles)
        sin_ref[:, seg(o)] = jnp.sin(angles)

    for r in range(len(g.ROUNDS)):
        g.round(r)
        if r in (2, 5):
            advance(r // 2)
        if r == 1:
            loop(N_DEV, tables)
        run_ready(g.READY[r], use)

    half = hd // 2
    cos, sin = cos_ref[:, seg(me)], sin_ref[:, seg(me)]

    def turn(h):
        first = seg(2 * h, half)
        second = seg(2 * h + 1, half)
        p = acc[first, :].astype(BF16).astype(F32)
        q = acc[second, :].astype(BF16).astype(F32)
        rot[first, :] = (p * cos - q * sin).astype(BF16)
        rot[second, :] = (q * cos + p * sin).astype(BF16)
    loop(q_all // hd, turn)
    for k in range(groups):
        turn(q_all // hd + 2 * k)
        vs = seg(q_all // hd + 2 * k + 1, hd)
        rot[vs, :] = acc[vs, :].astype(BF16)
    per = N_DEV // groups
    q_rows = lambda peer: seg(peer, qw)
    kv_rows = lambda peer: seg(q_all // (2 * hd) + peer // per, 2 * hd)
    qs = Swap(lambda peer: rot.at[q_rows(peer), :], lambda o: qkv_ref.at[:qw, seg(o, tokens)], qsems, me)
    kvs = Swap(lambda peer: rot.at[kv_rows(peer), :], lambda o: qkv_ref.at[qw:, seg(o, tokens)], ksems, me)
    qs.start()
    kvs.start()
    gw.start()
    keep_own(wo_ref, full_w, me)
    gain_row(g_scr, small_all, 1)
    qkv_ref[:qw, seg(me, tokens)] = rot[q_rows(me), :]
    qkv_ref[qw:, seg(me, tokens)] = rot[kv_rows(me), :]
    wgu_ref[:feat, seg(me)] = wg_t[seg(me, feat), :]
    wgu_ref[feat:, seg(me)] = wu_t[seg(me, feat), :]
    gates.start((CORE,))
    ups.start((CORE,))
    for swap in (qs, kvs):
        swap.wait_recv()
    stores = fetch_all(esem, (qkv_ref, qkv_out), (u_scr, u_out), (cos_ref, cos_out), (sin_ref, sin_out))
    heads = qkv_ref.shape[0] // hd - 2
    seq = qkv_ref.shape[1]
    scale = hd ** -0.5
    lanes = heads * QB
    key_rows(k_scr, qkv_ref, qw, hd)

    outs = Swap(lambda peer: o_send.at[seg(peer), :], lambda o: o_tok.at[:, seg(o)], osems, me)

    def q_block(qb):
        for at, r in ((2, 0), (4, 1), (5, 2), (6, 3), (7, 4)):
            @pl.when(qb == at)
            def _():
                gw.round(r)
        qs = seg(qb, QB)
        q2 = side_by_side(qkv_ref, heads, hd, qs)

        def scores(kb, top, diagonal):
            s = score_block(k_scr[seg(kb, KB), :], q2, scale, diagonal)
            s_scr[seg(kb, KB), :] = s
            return jnp.maximum(top, jnp.max(s, axis=0, keepdims=True))

        top = lax.fori_loop(0, qb, lambda kb, t: scores(kb, t, False), jnp.full((1, lanes), NEG_LARGE, F32))
        top = scores(qb, top, True)

        def expo(kb, tot):
            e = jnp.exp(s_scr[seg(kb, KB), :] - top)
            s_scr[seg(kb, KB), :] = e
            return tot + jnp.sum(e, axis=0, keepdims=True)

        inv = 1.0 / lax.fori_loop(0, qb + 1, expo, jnp.zeros((1, lanes), F32))

        def weigh(kb, acc):
            p = (s_scr[seg(kb, KB), :] * inv).astype(BF16)
            return acc + mm(qkv_ref[qw + hd:, seg(kb, KB)], p, NN)

        acc = lax.fori_loop(0, qb + 1, weigh, jnp.zeros((hd, lanes), F32))
        for h in range(heads):
            o_ref[h * hd:(h + 1) * hd, qs] = acc[:, h * QB:(h + 1) * QB].astype(BF16)
        stat_ref[qb, :1, :] = top
        stat_ref[qb, 1:, :] = inv
        o_send[qs, :] = o_ref[:, qs].T

    loop(seq // QB, q_block)
    outs.start()
    advance(3)
    o_tok[:, seg(me)] = o_send[seg(me), :]
    for r in (5, 6):
        gw.round(r)
    outs.wait_recv()
    for mask in CHIP_MASKS:
        gw.wait_pair(mask)

    def project(n):
        cs = seg(n, CHUNK)
        acc_o[:, cs] = mm(o_tok[...], full_w[:, :, cs].reshape(dim, CHUNK), NN)
    loop(dim // CHUNK, project)

    def residual(i):
        rs = seg(i, STRIP)
        h_ref[rs, :] = (x_ref[rs, :].astype(F32) + acc_o[rs, :]).astype(BF16)
    loop(tokens // STRIP, residual)
    norm_rows(h_ref, g_scr, m_ref)
    for swap in (gates, ups):
        swap.wait_recv()
    for mask in CHIP_MASKS:
        keep(mask).wait()
    outs.wait_send()
    for swap in (gates, ups):
        swap.wait_send((CORE,) + SETS[3])
    for store in stores:
        store.wait()
    g.finish()
    gw.finish()
    for swap in (smalls, qs, kvs):
        swap.wait_send()


def dw_swaps(stage, gate_hbm, up_hbm, sems, me):
    feat = gate_hbm.shape[0] // N_DEV
    return [Swap(lambda peer, lo=lo: stage(peer).at[lo:lo + feat, seg(peer % 2)], lambda o, dst=dst: dst.at[seg(o, feat), :], sems[i:i + 2], me)
            for lo, dst, i in ((0, gate_hbm, 0), (feat, up_hbm, 2))]


def mlp(m_ref, dout_ref, wgu_hbm, down_hbm, u_ref, h_ref, small_all, wo_ref, o_ref,
        ucol_ref, m_out, dgu_out, ddown_out, y_ref, dh_ref, do_ref, dwo_ref, dg_ref, gate_hbm, up_hbm,
        wgu_ref, down_ref, glu_ref, dgu_ref, ddown_ref, isem, dsem, full_d, full_m, osem, stage, g_scr, dgu_t, glu_t, free, *scr):
    me = lax.axis_index('sp')
    feat, dim = down_ref.shape
    loads = fetch_all(isem, (wgu_hbm, wgu_ref), (down_hbm, down_ref))
    enter(me, OTHERS)
    sems = scr[4:]
    gd = row_gather(dout_ref, full_d, sems[:4], me, 0)
    gm = row_gather(m_ref, full_m, sems[4:8], me, 2)
    g = row_gather(dh_ref, full_d, sems[8:12], me, 1)
    ucols = Swap(lambda peer: u_ref.at[:, seg(peer)], lambda o: ucol_ref.at[seg(o), :], sems[12:14], me)
    gates, ups = dw_swaps(lambda peer: stage, gate_hbm, up_hbm, sems[14:18], me)
    gm.start()
    gd.start()
    keep_own(m_ref, full_m, me)
    keep_own(dout_ref, full_d, me)
    gain_row(g_scr, small_all, 1)
    dwo_ref[...] = jnp.zeros_like(dwo_ref)
    ddown_ref[...] = jnp.zeros_like(ddown_ref)

    def keep(mask):
        chip = flipped(me, mask) // 2
        ts = seg(chip, WIDE)
        ends = ((full_m.at[chip], m_out.at[chip]), (dgu_ref.at[:, ts], dgu_out.at[:, ts]))
        return [pltpu.make_async_copy(src, dst, osem.at[mask // 2, i]) for i, (src, dst) in enumerate(ends)]

    for load in loads:
        load.wait()
    ucol_ref[seg(me), :] = u_ref[:, seg(me)]

    def use(mask):
        gd.wait_pair(mask)
        gm.wait_pair(mask)
        chip = flipped(me, mask) // 2
        ts = seg(chip, WIDE)
        gu = mm(wgu_ref[...], full_m[chip], NT).astype(BF16).astype(F32)
        gate, up = gu[:feat], gu[feat:]
        d_glu = mm(down_ref[...], full_d[chip], NT).astype(BF16).astype(F32)
        sig = jax.nn.sigmoid(gate)
        act = gate * sig
        glu = (act * up).astype(BF16)
        glu_ref[:, ts] = glu
        dgu_ref[:feat, ts] = (d_glu * up * (sig * (1.0 + gate * (1.0 - sig)))).astype(BF16)
        dgu_ref[feat:, ts] = (d_glu * act).astype(BF16)

        def step(n):
            ddown_ref[:, seg(n, CHUNK)] += mm(glu, full_d[chip, :, seg(n, CHUNK)], NN)
        loop(dim // CHUNK, step)
        for copy in keep(mask):
            copy.start()

    for r in range(len(gm.ROUNDS)):
        gm.round(r)
        gd.round(r)
        if r == 3:
            ucols.start()
        run_ready(gm.READY[r], use)
    far = seg(flipped(me, XYZ) // 2, WIDE)
    stage[...] = mm(dgu_ref[...], full_m[:, :, far].reshape(dgu_ref.shape[1], WIDE), NN)
    for swap in (gates, ups):
        swap.start(SETS[0])
    for gather in (gd, gm):
        gather.finish()
    leave = pltpu.make_async_copy(ddown_ref, ddown_out, dsem)
    leave.start()
    s = Scatter(*scr[:4], sems[18:], me)
    total = s.run(block_product(s, dgu_ref, wgu_ref, dgu_t))
    for mask in NEAR:
        pl.semaphore_signal(free, inc=1, device_id=(flipped(me, mask),), device_id_type=MESH)
    norm_back(total, h_ref, g_scr, dout_ref, dh_ref, dg_ref)
    g.start()
    keep_own(dh_ref, full_d, me)
    s.finish()
    pl.semaphore_wait(free, len(NEAR))

    def use_dh(mask):
        g.wait_pair(mask)
        chip = flipped(me, mask) // 2
        do_ref[:, seg(chip, WIDE)] = mm(wo_ref[...], full_d[chip], NT).astype(BF16)
        o = o_ref[:, seg(chip, WIDE)]

        def step(n):
            dwo_ref[:, seg(n, CHUNK)] += mm(o, full_d[chip, :, seg(n, CHUNK)], NN)
        loop(dim // CHUNK, step)

    def between(i):
        r = i if i < 3 else i - N_CHIP + 3
        if i < 3 or i >= N_CHIP:
            g.round(r)
            run_ready(g.READY[r], use_dh)

    s = Scatter(*scr[:4], sems[18:], me)
    total = s.run(block_product(s, glu_ref, down_ref, glu_t), between)
    y_ref[...] = (h_ref[...].astype(F32) + total[...]).astype(BF16)
    s.finish()
    g.finish()
    for swap in (gates, ups):
        swap.wait_recv(SETS[0])
        swap.wait_send(SETS[0])
    ucols.wait_recv()
    ucols.wait_send()
    leave.wait()
    ends = ((full_m.at[0], m_out.at[0]), (dgu_ref.at[:, seg(0, WIDE)], dgu_out.at[:, seg(0, WIDE)]))
    loop(N_CHIP, lambda j: [pltpu.make_async_copy(src, dst, osem.at[j, i]).wait() for i, (src, dst) in enumerate(ends)])


def back(groups, hd, qkv_hbm, do_hbm, stat_ref, cos_all, sin_all, dgu_hbm, m_hbm, ucol_ref, w_hbm, x_ref, small_all, dh_ref, dg2_ref, dg_in, du_in,
         dg_hbm, du_hbm, dwq_ref, dwkv_ref, dx_ref, gain_ref,
         dgu_ref, qkv_ref, do_ref, isem, qsem,
         p_scr, dp_scr, k_scr, v_scr, dk_acc, dv_acc, stage, dq_scr, dkv_scr, m_scr,
         full, w_scr, shares, dkv_own, full_kv, dqkv, dn, g_scr, dg1, gains, gains_in, wsem, lsem, msem, *sems):
    heads = qkv_ref.shape[0] // hd - 2
    seq = qkv_ref.shape[1]
    scale = hd ** -0.5
    lanes = heads * QB
    qw = heads * hd
    half = hd // 2
    me = lax.axis_index('sp')
    feat = dgu_ref.shape[0] // 2
    first = (X, Y + Z, Y, X + Z, Z, X + Y, 0)

    def fetch(mask):
        cols = seg(flipped(me, mask) // 2, WIDE)
        return pltpu.make_async_copy(m_hbm.at[:, :, cols], m_scr.at[:, :, cols], msem.at[mask // 2])
    needed, = fetch_all(isem, (dgu_hbm, dgu_ref))
    for mask in first[:2]:
        fetch(mask).start()
    load = pltpu.make_async_copy(w_hbm, w_scr, wsem)
    enter(me, OTHERS)
    for mask in first[2:]:
        fetch(mask).start()
    loads = fetch_all(qsem, (qkv_hbm, qkv_ref), (do_hbm, do_ref))
    gain_row(g_scr, small_all, 0)

    gates, ups = dw_swaps(lambda peer: stage.at[peer // 2], dg_hbm, du_hbm, sems[:4], me)
    gq = row_gather(dq_scr, full, sems[6:10], me)
    own = [pltpu.make_async_copy(swap.src(me), swap.dst(me), lsem.at[i]) for i, swap in enumerate((gates, ups))]

    def make(mask):
        chip = flipped(me, mask) // 2
        fetch(mask).wait()
        cols = m_scr[:, :, seg(chip, WIDE)].reshape(seq, WIDE)
        stage[chip] = mm(dgu_ref[...], cols, NN)

    def advance(n):
        for swap in (gates, ups):
            if n > 1:
                swap.wait_send(SETS[n - 1])
            swap.start(SETS[n])

    needed.wait()
    for mask in first[:2]:
        make(mask)
    advance(1)
    loop(5, lambda j: make(2 * ((j + 2) % 6)))
    load.start()
    for copy in loads:
        copy.wait()
    gates.start((CORE,))
    ups.start((CORE,))
    for copy in own:
        copy.start()

    dk_acc[...] = jnp.zeros_like(dk_acc)
    dv_acc[...] = jnp.zeros_like(dv_acc)
    key_rows(k_scr, qkv_ref, qw, hd)
    key_rows(v_scr, qkv_ref, qw + hd, hd)

    def q_block(qb):
        @pl.when(qb == 4)
        def _():
            advance(2)
        qs = seg(qb, QB)
        q2 = side_by_side(qkv_ref, heads, hd, qs)
        do2 = side_by_side(do_ref, heads, hd, qs)
        top = stat_ref[qb, :1, :]
        inv = stat_ref[qb, 1:, :]

        def probs(kb, rd, diagonal):
            ks = seg(kb, KB)
            s = score_block(k_scr[ks, :], q2, scale, diagonal)
            p = jnp.exp(s - top) * inv
            dp = mm(v_scr[ks, :], do2, NN).astype(BF16)
            p_scr[ks, :] = p
            dp_scr[ks, :] = dp
            dv_acc[ks, :] += mm(p.astype(BF16), do2, NT)
            return rd + jnp.sum(dp.astype(F32) * p, axis=0, keepdims=True)

        rd = lax.fori_loop(0, qb, lambda kb, r: probs(kb, r, False), jnp.zeros((1, lanes), F32))
        rd = probs(qb, rd, True)

        def d_scores(kb, acc):
            ks = seg(kb, KB)
            ds = (p_scr[ks, :] * (dp_scr[ks, :].astype(F32) - rd) * scale).astype(BF16)
            dk_acc[ks, :] += mm(ds, q2, NT)
            return acc + mm(qkv_ref[qw:qw + hd, ks], ds, NN)

        acc = lax.fori_loop(0, qb + 1, d_scores, jnp.zeros((hd, lanes), F32))
        cos, sin = cos_all[:, qs], sin_all[:, qs]
        for h in range(heads):
            dq = acc[:, h * QB:(h + 1) * QB].astype(BF16).astype(F32)
            p, q = dq[:half], dq[half:]
            dq_scr[h * hd:h * hd + half, qs] = (p * cos + q * sin).astype(BF16)
            dq_scr[h * hd + half:(h + 1) * hd, qs] = (q * cos - p * sin).astype(BF16)

    loop(seq // QB, q_block)

    def share(i):
        rs = seg(i, WIDE)
        dkv_scr[rs, :] = jnp.concatenate([dk_acc[rs, :], dv_acc[rs, :]], axis=1).astype(BF16)
    loop(seq // WIDE, share)
    tokens = ucol_ref.shape[1]
    per = N_DEV // groups
    q_all = dwq_ref.shape[0]
    sh = Swap(lambda peer: dkv_scr.at[seg(peer, tokens), :], lambda o: shares.at[o], sems[4:6], me)
    parts = thirds(dkv_own.shape[0], STRIP)
    gk = Gather(dkv_own, lambda o: full_kv.at[:, seg(o, tokens)], lambda view, c: [view.at[pl.ds(*parts[c]), :]], sems[10:14], me)
    gs = Swap(lambda peer: gains.at[:, seg(peer)], lambda o: gains_in.at[o], sems[14:], me)
    sh.start()
    gq.start()
    keep_own(dq_scr, full, me)
    shares[me] = dkv_scr[seg(me, tokens), :]
    sh.wait_recv()
    cos, sin = cos_all[:, seg(me)], sin_all[:, seg(me)]
    for k in range(groups):
        both = sum(shares[per * k + i].astype(F32) for i in range(per)).astype(BF16).astype(F32).T
        p, q = both[:half], both[half:hd]
        lo = 2 * hd * k
        dkv_own[lo:lo + half, :] = (p * cos + q * sin).astype(BF16)
        dkv_own[lo + half:lo + hd, :] = (q * cos - p * sin).astype(BF16)
        dkv_own[lo + hd:lo + 2 * hd, :] = both[hd:].astype(BF16)
    gk.start()
    full_kv[:, seg(me, tokens)] = dkv_own[...]
    for k in range(groups):
        dqkv[:, q_all + 2 * hd * k:q_all + 2 * hd * (k + 1)] = dkv_own[2 * hd * k:2 * hd * (k + 1), :].T

    def use(mask):
        gq.wait_pair(mask)
        chip = flipped(me, mask) // 2
        dwq_ref[seg(chip, WIDE), :] = mm(full[chip], ucol_ref[...], NN)
        dqkv[:, seg(chip, WIDE)] = full[chip, :, seg(me, tokens)].T

    for r in range(len(gq.ROUNDS)):
        gq.round(r)
        gk.round(r)
        if r == 3:
            advance(3)
        run_ready(gq.READY[r], use)
    load.wait()

    def normed(i):
        dn[:, seg(i, WIDE)] = mm(dqkv[...], w_scr[i], NN)
    loop(N_CHIP, normed)
    norm_back(dn, x_ref, g_scr, dh_ref, dx_ref, dg1)
    gains[...] = jnp.concatenate([jnp.sum(dg1[...], axis=0, keepdims=True), jnp.sum(dg2_ref[...], axis=0, keepdims=True),
                                  jnp.zeros((N_CHIP - 2, dg1.shape[1]), F32)], axis=0)
    gs.start()
    gains_in[me] = gains[:, seg(me)]
    for mask in CHIP_MASKS:
        gk.wait_pair(mask)
    dwkv_ref[...] = mm(full_kv[...], ucol_ref[...], NN)
    gs.wait_recv()
    gain_ref[...] = sum(gains_in[o] for o in range(N_DEV))
    for swap in (gates, ups):
        swap.wait_recv((CORE,) + SETS[1] + SETS[2] + SETS[3])
        swap.wait_send((CORE,) + SETS[3])
    for copy in own:
        copy.wait()
    for c in (sh, gs):
        c.wait_send()
    for g in (gq, gk):
        g.finish()


def finish(dg_hbm, du_hbm, dkv_hbm, *refs):
    n = (len(refs) - 14) // 3
    gains, refs = refs[0], refs[1:]
    srcs, (gate, up, dk, dv, dg1, dg2), refs = refs[:n], refs[n:n + 6], refs[n + 6:]
    dsts, (g_in, g_out, kv_in), holds, sems = refs[:n], refs[n:n + 3], refs[n + 3:2 * n + 3], refs[2 * n + 3:]
    dg1[...] = gains[:1, :]
    dg2[...] = gains[1:2, :]
    t_in, t_out, p_in, p_out = sems
    step = LANE * 11
    cols = g_in.shape[1]
    hd = dk.shape[0] // (kv_in.shape[0] // LANE)
    starts = [(w, i) for i in range(cols // step) for w in range(2)]

    def fetch(w, i):
        rs = pl.ds(i * step, step)
        return pltpu.make_async_copy((dg_hbm, du_hbm)[w].at[rs, :], g_in.at[w, rs, :], t_in.at[w, i])

    def put(w, i):
        cs = pl.ds(i * step, step)
        return pltpu.make_async_copy(g_out.at[w, :, cs], (gate, up)[w].at[:, cs], t_out.at[w, i])
    moves = [(pltpu.make_async_copy(a, h, p_in.at[k]), pltpu.make_async_copy(h, b, p_out.at[k])) for k, (a, h, b) in enumerate(zip(srcs, holds, dsts))]
    kv = pltpu.make_async_copy(dkv_hbm, kv_in, p_in.at[n])
    for w, i in starts:
        fetch(w, i).start()
    kv.start()
    for load, _ in moves:
        load.start()
    for w, i in starts:
        fetch(w, i).wait()

        at = pl.ds(i * step, step)
        g_out[w, :, at] = g_in[w, at, :].T
        put(w, i).start()
    kv.wait()
    for k in range(dk.shape[0] // hd):
        for i, ref in enumerate((dk, dv)):
            ref[k * hd:(k + 1) * hd, :] = kv_in[(2 * k + i) * hd:(2 * k + i + 1) * hd, :]
    for load, store in moves:
        load.wait()
        store.start()
    for w, i in starts:
        put(w, i).wait()
    for _, store in moves:
        store.wait()


def solution(mesh):
    assert mesh.shape['sp'] == N_DEV

    def layer_step(x_in, positions, d_out, norm1_gain, norm2_gain, w_q, w_k, w_v, w_o, w_gate, w_up, w_down):
        tokens, dim = x_in.shape
        seq = tokens * N_DEV
        n_q, hd = w_q.shape[1:]
        n_kv = w_k.shape[1]
        qw = n_q // N_DEV * hd
        rows = w_q.shape[0]
        feat = w_down.shape[0]
        cols = (n_q + 2 * n_kv) * hd
        lanes = qw // hd * QB
        vm = pltpu.VMEM
        full = vm((N_CHIP, WIDE, dim), BF16)
        gain_scr = vm((N_CHIP, dim), F32)
        tok_shapes = 2 * (((tokens, dim), BF16),)
        dw_shapes = 2 * (((feat * N_DEV, rows), F32),)

        inv_freq = 1.0 / (ROPE_BASE ** (jnp.arange(hd // 2, dtype=F32) * (2.0 / hd)))
        freq = jnp.broadcast_to(inv_freq[:, None], (hd // 2, rows))
        row = lambda v: v.reshape(1, rows)
        by_head = lambda w: w.transpose(1, 2, 0).reshape(-1, rows)
        wo_own = w_o.reshape(qw, dim)

        args = (x_in, row(norm1_gain), row(norm2_gain), row(positions), by_head(w_q), by_head(w_k), by_head(w_v), freq, w_gate, w_up, wo_own)
        qkv, u, small_all, wqkv, attn_t, stat, wgu, hidden, mlp_in, cos_all, sin_all = call(
            functools.partial(head, n_kv, hd), 0, len(args),
            (((qw + 2 * hd, seq), BF16), tok_shapes[0], ((N_DEV, N_CHIP, rows), F32), ((N_CHIP, cols, WIDE), BF16),
             ((qw, seq), BF16), ((seq // QB, 2, lanes), F32), ((2 * feat, dim), BF16), *tok_shapes, *(2 * (((hd // 2, seq), F32),))),
            [vm(w_gate.shape, BF16), vm(w_up.shape, BF16), vm((qw, dim), BF16), vm((qw + 2 * hd, seq), BF16), vm((tokens, dim), BF16),
             vm((hd // 2, seq), F32), vm((hd // 2, seq), F32), dma(3), dma(4),
             full, vm((tokens, dim), F32), vm((tokens, dim), BF16), vm((seq, qw), BF16),
             vm((N_CHIP, rows), F32), vm((cols, rows), BF16), vm((N_CHIP, cols, WIDE), BF16), vm((cols, tokens), F32), vm((cols, tokens), BF16), gain_scr,
             vm((feat * N_DEV, rows), BF16), vm((feat * N_DEV, rows), BF16), vm((seq, lanes), F32), vm((seq, hd), BF16), dma(N_CHIP),
             *Gather.sems, *(6 * Swap.sems), *Gather.sems], 4 * qw * seq * seq, far_in=(8, 9, 10), far_out=(0, 1, 3, 9, 10))(*args)
        args = (mlp_in, d_out, wgu, w_down, u, hidden, small_all, wo_own, attn_t)
        u_col, m_full, dgu, d_down, y_out, d_hidden, d_attn, d_wo, d_g2, d_gate_t, d_up_t = call(
            mlp, 1, len(args),
            (((seq, rows), BF16), ((N_CHIP, WIDE, dim), BF16), ((2 * feat, seq), BF16), ((feat, dim), F32),
             *tok_shapes, ((qw, seq), BF16), ((qw, dim), F32), ((N_CHIP, dim), F32), *dw_shapes),
            [vm((2 * feat, dim), BF16), vm((feat, dim), BF16),
             vm((feat, seq), BF16), vm((2 * feat, seq), BF16), vm((feat, dim), F32), dma(2), dma(),
             full, full, dma(N_CHIP, 2), vm((2 * feat, WIDE), F32), gain_scr, vm((WIDE, 2 * feat), BF16), vm((WIDE, feat), BF16), pltpu.SemaphoreType.REGULAR,
             *Scatter.scratch(tokens, dim), *(3 * Gather.sems), *(3 * Swap.sems), *Scatter.sems], 12 * feat * seq * dim,
            far_in=(2, 3), far_out=(1, 2, 3, 9, 10))(*args)
        args = (qkv, d_attn, stat, cos_all, sin_all, dgu, m_full, u_col, wqkv, x_in, small_all, d_hidden, d_g2, d_gate_t, d_up_t)
        d_gate_t, d_up_t, d_wq, d_wkv, d_x, gains = call(
            functools.partial(back, n_kv, hd), 3, len(args),
            (*dw_shapes, ((n_q * hd, rows), F32), ((2 * n_kv * hd, rows), F32), tok_shapes[0], ((N_CHIP, rows), F32)),
            [vm((2 * feat, seq), BF16), vm((qw + 2 * hd, seq), BF16), vm((qw, seq), BF16), dma(1), dma(2),
             vm((seq, lanes), F32), vm((seq, lanes), BF16), vm((seq, hd), BF16), vm((seq, hd), BF16), vm((seq, hd), F32), vm((seq, hd), F32),
             vm((N_CHIP, 2 * feat, WIDE), F32), vm((qw, seq), BF16), vm((seq, 2 * hd), BF16), full,
             full, vm((N_CHIP, cols, WIDE), BF16), vm((N_DEV, tokens, 2 * hd), BF16), vm((2 * n_kv * hd, tokens), BF16), vm((2 * n_kv * hd, seq), BF16),
             vm((tokens, cols), BF16), vm((tokens, dim), F32), gain_scr, gain_scr, gain_scr, vm((N_DEV, N_CHIP, rows), F32), dma(), dma(2), dma(N_CHIP),
             *(3 * Swap.sems), *(2 * Gather.sems), *Swap.sems], 10 * qw * seq * seq, far_in=(0, 1, 5, 6, 8, 13, 14), far_out=(0, 1), aliases={13: 0, 14: 1})(*args)
        moved = (d_wq, d_wo, d_down, d_x, y_out)
        one_row = jax.ShapeDtypeStruct((1, rows), F32)
        half_kv = jax.ShapeDtypeStruct((n_kv * hd, rows), F32)
        wide = jax.ShapeDtypeStruct((rows, feat * N_DEV), F32)
        d_gate, d_up, d_wk, d_wv, d_g1, d_g2, d_wq, d_wo, d_down, d_x, y_out = pl.pallas_call(
            finish,
            out_shape=[wide, wide, half_kv, half_kv, one_row, one_row] + [jax.ShapeDtypeStruct(v.shape, v.dtype) for v in moved],
            in_specs=[IN_HBM] * 3 + on_chip(1) + [IN_HBM] * len(moved), out_specs=[IN_HBM] * 2 + on_chip(4) + [IN_HBM] * len(moved),
            scratch_shapes=[vm((2, feat * N_DEV, rows), F32), vm((2, rows, feat * N_DEV), F32), vm(d_wkv.shape, F32)]
            + [vm(v.shape, v.dtype) for v in moved] + [dma(2, 4), dma(2, 4), dma(len(moved) + 1), dma(len(moved))],
            compiler_params=pltpu.CompilerParams(vmem_limit_bytes=VMEM_CAP), name='finish',
        )(d_gate_t, d_up_t, d_wkv, gains, *moved)
        by_row = lambda g, heads: g.reshape(heads, hd, rows).transpose(2, 0, 1)
        return (y_out, d_x, d_g1.reshape(rows), d_g2.reshape(rows), by_row(d_wq, n_q), by_row(d_wk, n_kv), by_row(d_wv, n_kv),
                d_wo.reshape(w_o.shape), d_gate, d_up, d_down)

    all_rows = P('sp')
    return jax.shard_map(layer_step, mesh=mesh, in_specs=(all_rows,) * 12, out_specs=(all_rows,) * 11, check_vma=False)
```

```python
import functools
import jax
import jax.numpy as jnp
from jax import lax
from jax.experimental import pallas as pl
from jax.experimental.pallas import tpu as pltpu
from jax.sharding import PartitionSpec as P

ROPE_BASE = 10000.0
NORM_EPS = 1e-5
NEG_LARGE = -1e30
F32 = jnp.float32
BF16 = jnp.bfloat16
N_DEV, N_CHIP, LANE, WIDE, CHUNK, STRIP = 16, 8, 128, 256, 512, 16
NT = (((1,), (1,)), ((), ()))
TN = (((0,), (0,)), ((), ()))
NN = (((1,), (0,)), ((), ()))
MESH = pl.DeviceIdType.MESH
VMEM_CAP = 67043328

CORE, X, Y, Z = 1, 2, 4, 8
XYZ = X + Y + Z
ORDERS = ((X, Y, Z), (Y, Z, X), (Z, X, Y))
CHIP_MASKS = (0, X, Y, Z, X + Y, X + Z, Y + Z, XYZ)
NEAR = (CORE, X, Y, Z)
OTHERS = range(1, N_DEV)
SETS = tuple(tuple(m + c for m in masks for c in (0, CORE)) for masks in ((XYZ,), (X, Y + Z), (Y, X + Z), (Z, X + Y)))
N_COL = len(ORDERS)
COLOURS = range(N_COL)


def mm(a, b, dims):
    return lax.dot_general(a, b, dims, preferred_element_type=F32)


def seg(index, width=LANE):
    return pl.ds(pl.multiple_of(index * width, width), width)


def loop(count, body):
    lax.fori_loop(0, count, lambda i, c: (body(i), c)[1], 0)


def differing(index, mask):
    return sum(((index // bit + mask // bit) % 2) * bit for bit in NEAR)


def flipped(index, mask):
    if not isinstance(mask, int):
        return differing(index, mask)
    out = index
    for bit in NEAR:
        if mask & bit:
            out = out + (1 - 2 * ((index // bit) % 2)) * bit
    return out


def run_ready(masks, use):
    if len(masks) == 2:
        loop(2, lambda j: use(masks[0] + (masks[1] - masks[0]) * j))
    else:
        for mask in masks:
            use(mask)


def thirds(total, unit):
    n = total // unit
    first = (n + 2) // 3
    second = (n - first + 1) // 2
    sizes = (first * unit, second * unit, (n - first - second) * unit)
    return ((0, sizes[0]), (sizes[0], sizes[1]), (sizes[0] + sizes[1], sizes[2]))


def pieces(rows, cols, unit):
    share = cols // LANE // N_COL * LANE
    strips = thirds(rows, unit)
    rest = cols - N_COL * share
    return [[(pl.ds(0, rows), pl.ds(c * share, share)), (pl.ds(*strips[c]), pl.ds(N_COL * share, rest))] for c in COLOURS]


def enter(me, masks):
    barrier = pltpu.get_barrier_semaphore()
    for mask in masks:
        pl.semaphore_signal(barrier, inc=1, device_id=(flipped(me, mask),), device_id_type=MESH)
    pl.semaphore_wait(barrier, len(masks))


def remote(src, dst, send, recv, peer):
    return pltpu.make_async_remote_copy(src_ref=src, dst_ref=dst, send_sem=send, recv_sem=recv, device_id=(peer,), device_id_type=MESH)


def dma(*shape):
    return pltpu.SemaphoreType.DMA(shape)


class Swap:
    sems = (dma(N_DEV), dma(N_DEV))

    def __init__(self, src, dst, sems, me):
        self.src, self.dst, (self.send, self.recv), self.me = src, dst, sems, me

    def copy(self, mask):
        peer = differing(self.me, mask)
        return remote(self.src(peer), self.dst(self.me), self.send.at[mask], self.recv.at[mask], peer)

    def arrival(self, mask):
        view = self.dst(differing(self.me, mask))
        return remote(view, view, self.send.at[mask], self.recv.at[mask], self.me)

    def each(self, masks, act):
        if masks is None:
            loop(N_DEV - 1, lambda i: act(i + 1))
        else:
            for mask in masks:
                act(mask)

    def start(self, masks=None):
        self.each(masks, lambda mask: self.copy(mask).start())

    def advance(self, n):
        if n:
            self.wait_send(SETS[n - 1])
        self.start(SETS[n])

    def wait_recv(self, masks=None):
        self.each(masks, lambda mask: self.arrival(mask).wait_recv())

    def wait_send(self, masks=None):
        self.each(masks, lambda mask: self.copy(mask).wait_send())


class Gather:
    ROUNDS = ((0,), (1,), (2,), (0, 1), (0, 2), (1, 2), (0, 1, 2))
    READY = ((0,), (), (), (X, Y), (Z,), (X + Y, X + Z), (Y + Z, XYZ))
    sems = (dma(N_COL, N_CHIP, 2), dma(N_COL, N_CHIP, 2), dma(N_CHIP), dma(N_CHIP))

    def __init__(self, own, block, cut, sems, me):
        self.own, self.block, self.cut, self.me = own, block, cut, me
        self.send, self.recv, self.pair_send, self.pair_recv = sems

    def source(self, mask):
        return self.block(flipped(self.me, mask)) if mask else self.own

    def unit(self, colour, mask, axis):
        ends = zip(self.cut(self.source(mask), colour), self.cut(self.block(flipped(self.me, mask)), colour))
        j = self.sends(colour).index((mask, axis))
        return [remote(src, dst, self.send.at[colour, j, i], self.recv.at[colour, (mask + axis) // 2, i],
                       flipped(self.me, axis)) for i, (src, dst) in enumerate(ends)]

    def sends(self, colour):
        return [(0, axis) for axis in ORDERS[colour]] + [step[1:] for step in self.onward(colour)]

    def start_unit(self, colour, mask, axis):
        for copy in self.unit(colour, mask, axis):
            copy.start()

    def pair(self, mask):
        return remote(self.source(mask), self.block(flipped(self.me, mask)), self.pair_send.at[mask // 2],
                      self.pair_recv.at[mask // 2], flipped(self.me, CORE))

    def wait_pair(self, mask):
        view = self.block(flipped(self.me, mask + CORE))
        remote(view, view, self.pair_send.at[mask // 2], self.pair_recv.at[mask // 2], self.me).wait_recv()

    def onward(self, colour):
        order = ORDERS[colour]
        for picks in self.ROUNDS:
            for axis in order[picks[-1] + 1:]:
                yield picks, sum(order[p] for p in picks), axis

    def start(self):
        for pos in COLOURS:
            for colour in COLOURS:
                self.start_unit(colour, 0, ORDERS[colour][pos])
        self.pair(0).start()

    def round(self, r):
        for colour in COLOURS:
            mask = sum(ORDERS[colour][p] for p in self.ROUNDS[r])
            for i, view in enumerate(self.cut(self.block(flipped(self.me, mask)), colour)):
                remote(view, view, self.send.at[colour, 0, i], self.recv.at[colour, mask // 2, i], self.me).wait_recv()
            for picks, at, axis in self.onward(colour):
                if picks == self.ROUNDS[r]:
                    self.start_unit(colour, at, axis)
        for mask in {2: (X, Y, Z), 5: (X + Y, X + Z, Y + Z), 6: (XYZ,)}.get(r, ()):
            self.pair(mask).start()

    def finish(self):
        for colour in COLOURS:
            for i, view in enumerate(self.cut(self.own, colour)):
                loop(len(self.sends(colour)), lambda j: remote(view, view, self.send.at[colour, j, i], self.recv.at[colour, j, i], self.me).wait_send())
        loop(N_CHIP, lambda j: remote(self.own, self.own, self.pair_send.at[j], self.pair_recv.at[j], self.me).wait_send())


def row_gather(own, full, sems, me, extra=None):
    rows, width = own.shape
    parts = pieces(rows, width, STRIP)
    if extra is not None:
        share = width // LANE // N_COL * LANE
        more = width - N_COL * share
        parts = [[(pl.ds(0, rows), pl.ds(c * share + more * (c > extra), share + more * (c == extra)))] for c in COLOURS]

    def block(o):
        return full.at[o // 2, seg(o % 2), :]

    return Gather(own, block, lambda view, c: [view.at[rs, cs] for rs, cs in parts[c]], sems, me)


def keep_own(own, full, me):
    def step(i):
        full[me // 2, pl.ds(pl.multiple_of((me % 2) * LANE + i * STRIP, STRIP), STRIP), :] = own[seg(i, STRIP), :]
    loop(LANE // STRIP, step)


class Scatter:
    ORDER = (XYZ, X + Y, Y + Z, X + Z, X, Y, Z, 0)
    sems = (dma(N_CHIP), dma(N_CHIP), dma(N_COL, N_CHIP, 2), dma(N_COL, N_CHIP, 2))

    @staticmethod
    def scratch(tokens, dim):
        return [pltpu.VMEM((n, tokens, dim), F32) for n in (N_CHIP, 2, N_CHIP, N_CHIP - 1)]

    def __init__(self, part, other, pair_in, link_in, sems, me):
        self.part, self.other, self.pair_in, self.link_in, self.me = part, other, pair_in, link_in, me
        self.pair_send, self.pair_recv, self.link_send, self.link_recv = sems
        self.tokens, self.dim = part.shape[1:]
        self.pieces = pieces(self.tokens, self.dim, STRIP // 2)
        self.ready, self.sent = set(), [0] * N_COL

    @staticmethod
    def first(colour, mask):
        return next((i for i, a in enumerate(ORDERS[colour]) if mask & a), 3)

    def slot(self, colour, mask, axis):
        slots = [(m, a) for m in self.ORDER for a in ORDERS[colour][:self.first(colour, m)]]
        return slots.index((mask, axis))

    def pair(self, i):
        return remote(self.other.at[i % 2], self.pair_in.at[i], self.pair_send.at[i], self.pair_recv.at[i], flipped(self.me, CORE))

    def link(self, colour, mask):
        axis = ORDERS[colour][self.first(colour, mask)]
        slot = self.slot(colour, mask - axis, axis)
        i = self.ORDER.index(mask)
        return [remote(self.part.at[i, rs, cs], self.link_in.at[slot, rs, cs], self.link_send.at[colour, i, k],
                       self.link_recv.at[colour, slot, k], flipped(self.me, axis)) for k, (rs, cs) in enumerate(self.pieces[colour])]

    def start_link(self, colour, mask):
        for copy in self.link(colour, mask):
            copy.start()

    def add(self, mask, ref, cs):
        i = self.ORDER.index(mask)

        def step(r):
            rs = seg(r, STRIP)
            self.part[i, rs, cs] += ref[rs, cs]
        loop(self.tokens // STRIP, step)

    def finish_pair(self, i):
        self.pair(i).wait_recv()
        self.add(self.ORDER[i], self.pair_in.at[i], pl.ds(0, self.dim))
        self.ready.add(self.ORDER[i])
        for colour in COLOURS:
            a, b, c = ORDERS[colour]
            todo = (XYZ, a + b, a + c, a)
            while self.sent[colour] < len(todo) and todo[self.sent[colour]] in self.ready:
                self.start_link(colour, todo[self.sent[colour]])
                self.sent[colour] += 1

    def take(self, colour, mask, axis):
        for copy in self.link(colour, mask + axis):
            copy.wait_recv()
        ref = self.link_in.at[self.slot(colour, mask, axis)]
        (_, wide), (rs, cs) = self.pieces[colour]
        self.add(mask, ref, wide)
        self.part[self.ORDER.index(mask), rs, cs] += ref[rs, cs]

    def run(self, product, between=lambda i: None):
        for i, mask in enumerate(self.ORDER):
            if i > 1:
                self.pair(i - 2).wait_send()
            product(i, flipped(self.me, mask) // 2)
            self.pair(i).start()
            if i:
                self.finish_pair(i - 1)
            between(i)
        self.finish_pair(N_CHIP - 1)
        for step in range(2):
            between(N_CHIP + step)
            for colour in COLOURS:
                a, b, c = ORDERS[colour]
                mask = (b + c, b)[step]
                self.take(colour, mask, a)
                self.start_link(colour, mask)
        between(N_CHIP + 2)
        for colour in COLOURS:
            a, b, c = ORDERS[colour]
            self.take(colour, c, a)
            self.take(colour, c, b)
            self.start_link(colour, c)
        between(N_CHIP + 3)
        for colour in COLOURS:
            for axis in ORDERS[colour]:
                self.take(colour, 0, axis)
        return self.part.at[N_CHIP - 1]

    def finish(self):
        for i in (N_CHIP - 2, N_CHIP - 1):
            self.pair(i).wait_send()
        for colour in COLOURS:
            for k, (rs, cs) in enumerate(self.pieces[colour]):
                view = self.part.at[0, rs, cs]
                loop(N_CHIP - 1, lambda i: remote(view, view, self.link_send.at[colour, i, k], self.link_recv.at[colour, i, k], self.me).wait_send())


def block_product(s, a_ref, w_ref, a_t):
    core = s.me % 2

    def product(i, chip):
        a_t[...] = a_ref[:, seg(chip, WIDE)].T

        def step(n):
            cs = seg(n, CHUNK)
            s.other[i % 2, :, cs] = mm(a_t[seg(1 - core), :], w_ref[:, cs], NN)
            s.part[i, :, cs] = mm(a_t[seg(core), :], w_ref[:, cs], NN)
        loop(s.dim // CHUNK, step)
    return product


def on_chip(n):
    return [pl.BlockSpec(memory_space=pltpu.VMEM)] * n


IN_HBM = pl.BlockSpec(memory_space=pl.ANY)


def call(kernel, ident, args, outs, scratch, flops, far_in=(), far_out=(), aliases={}):
    specs = [IN_HBM if i in far_in else on_chip(1)[0] for i in range(args)]
    out_specs = [IN_HBM if i in far_out else on_chip(1)[0] for i in range(len(outs))]
    return pl.pallas_call(
        kernel,
        out_shape=[jax.ShapeDtypeStruct(shape, dtype) for shape, dtype in outs],
        in_specs=specs, out_specs=out_specs, scratch_shapes=scratch, input_output_aliases=aliases,
        cost_estimate=pl.CostEstimate(flops=flops, bytes_accessed=flops // CHUNK, transcendentals=0),
        compiler_params=pltpu.CompilerParams(collective_id=ident, has_side_effects=True, vmem_limit_bytes=VMEM_CAP),
        name=kernel.func.__name__ if isinstance(kernel, functools.partial) else kernel.__name__,
    )


def fetch_all(sem, *pairs):
    copies = [pltpu.make_async_copy(src, dst, sem.at[i]) for i, (src, dst) in enumerate(pairs)]
    for copy in copies:
        copy.start()
    return copies


def gain_row(dst, small_all, which):
    for o in range(N_DEV):
        dst[:1, o * LANE:(o + 1) * LANE] = small_all[o, which:which + 1, :]


def norm_rows(src, gain, dst):
    def step(i):
        rs = seg(i, STRIP)
        t = src[rs, :].astype(F32)
        dst[rs, :] = (t * lax.rsqrt(jnp.mean(t * t, axis=-1, keepdims=True) + NORM_EPS) * gain[:1, :]).astype(BF16)
    loop(src.shape[0] // STRIP, step)


def norm_back(dy, src, gain, skip, dst, dgain):
    def step(i):
        rs = seg(i, STRIP)
        d = dy[rs, :].astype(BF16).astype(F32)
        t = src[rs, :].astype(F32)
        inv = lax.rsqrt(jnp.mean(t * t, axis=-1, keepdims=True) + NORM_EPS)
        gd = gain[:1, :] * d
        pull = jnp.mean(gd * t, axis=-1, keepdims=True)
        dst[rs, :] = (skip[rs, :].astype(F32) + (inv * gd - t * (inv * inv * inv * pull))).astype(BF16)
        g = d * (t * inv)
        dgain[...] += g[:N_CHIP] + g[N_CHIP:]
    dgain[...] = jnp.zeros_like(dgain)
    loop(src.shape[0] // STRIP, step)


QB = 256
KB = 256


def key_rows(dst, src, lo, hd):
    def step(i):
        dst[seg(i, KB), :] = src[lo:lo + hd, seg(i, KB)].T
    loop(src.shape[1] // KB, step)


def score_block(k, q2, scale, diagonal):
    s = mm(k, q2, NN) * scale
    if diagonal:
        key = lax.broadcasted_iota(jnp.int32, s.shape, 0)
        qry = lax.broadcasted_iota(jnp.int32, s.shape, 1) % QB
        s = jnp.where(qry >= key, s, NEG_LARGE)
    return s


def side_by_side(ref, heads, hd, qs):
    return jnp.concatenate([ref[h * hd:(h + 1) * hd, qs] for h in range(heads)], axis=1)


def head(groups, hd, x_ref, g1_ref, g2_ref, pos_ref, wq_ref, wk_ref, wv_ref, freq_ref, wg_hbm, wu_hbm, wo_hbm, qkv_out, u_out, small_all, w_out, o_ref, stat_ref, wgu_ref, h_ref, m_ref, cos_out, sin_out,
         wg_ref, wu_ref, wo_ref, qkv_ref, u_scr, cos_ref, sin_ref, isem, esem,
         full_w, acc_o, o_tok, o_send, small_ref, w_ref, full, acc, rot, g_scr, wg_t, wu_t, s_scr, k_scr, osem, *sems):
    me = lax.axis_index('sp')
    tokens, dim = x_ref.shape
    cols = w_ref.shape[0]
    small_ref[...] = jnp.concatenate([r[...].astype(F32) for r in (g1_ref, g2_ref, pos_ref)] + [jnp.zeros((N_CHIP - 3, LANE), F32)], axis=0)
    w_ref[:wq_ref.shape[0], :] = wq_ref[...]
    for k in range(groups):
        for i, ref in enumerate((wk_ref, wv_ref)):
            w_ref[pl.ds(wq_ref.shape[0] + (2 * k + i) * hd, hd), :] = ref[k * hd:(k + 1) * hd, :]
    qw = tokens
    q_all = N_DEV * qw
    gsems, ssems, qsems, ksems, gate_sems, up_sems, osems = sems[:4], *(sems[i:i + 2] for i in range(4, len(sems) - 4, 2))
    gw = row_gather(wo_ref, full_w, sems[-4:], me, 1)
    feat = wg_ref.shape[1] // N_DEV
    loads = fetch_all(isem, (wg_hbm, wg_ref), (wu_hbm, wu_ref), (wo_hbm, wo_ref))
    enter(me, OTHERS)
    smalls = Swap(lambda peer: small_ref, lambda o: small_all.at[o], ssems, me)
    smalls.start()
    parts = thirds(cols, STRIP)
    g = Gather(w_ref, lambda o: full.at[o // 2, :, seg(o % 2)], lambda view, c: [view.at[pl.ds(*parts[c]), :]], gsems, me)
    g.start()
    gates = Swap(lambda peer: wg_t.at[seg(peer, feat), :], lambda o: wgu_ref.at[:feat, seg(o)], gate_sems, me)
    ups = Swap(lambda peer: wu_t.at[seg(peer, feat), :], lambda o: wgu_ref.at[feat:, seg(o)], up_sems, me)

    def advance(n):
        gates.advance(n)
        ups.advance(n)

    def transpose(i):
        wg_t[seg(i, CHUNK), :] = wg_ref[:, seg(i, CHUNK)].T
        wu_t[seg(i, CHUNK), :] = wu_ref[:, seg(i, CHUNK)].T
    for load in loads:
        load.wait()
    loop(wg_ref.shape[1] // CHUNK, transpose)
    advance(0)

    def own_block(i):
        full[me // 2, seg(i, WIDE), seg(me % 2)] = w_ref[seg(i, WIDE), :]
    loop(cols // WIDE, own_block)
    acc[...] = jnp.zeros_like(acc)
    small_all[me] = small_ref[...]
    smalls.wait_recv()
    gain_row(g_scr, small_all, 0)
    norm_rows(x_ref, g_scr, u_scr)

    def keep(mask):
        chip = flipped(me, mask) // 2
        return pltpu.make_async_copy(full.at[chip], w_out.at[chip], osem.at[mask // 2])

    def use(mask):
        g.wait_pair(mask)
        keep(mask).start()
        chip = flipped(me, mask) // 2
        u = u_scr[:, seg(chip, WIDE)]

        def step(i):
            rs = seg(i, cols // 2)
            acc[rs, :] += mm(full[chip, rs, :], u, NT)
        loop(2, step)

    def tables(o):
        angles = freq_ref[...] * small_all[o, 2:3, :]
        cos_ref[:, seg(o)] = jnp.cos(angles)
        sin_ref[:, seg(o)] = jnp.sin(angles)

    for r in range(len(g.ROUNDS)):
        g.round(r)
        if r in (2, 5):
            advance(r // 2)
        if r == 1:
            loop(N_DEV, tables)
        run_ready(g.READY[r], use)

    half = hd // 2
    cos, sin = cos_ref[:, seg(me)], sin_ref[:, seg(me)]

    def turn(h):
        first = seg(2 * h, half)
        second = seg(2 * h + 1, half)
        p = acc[first, :].astype(BF16).astype(F32)
        q = acc[second, :].astype(BF16).astype(F32)
        rot[first, :] = (p * cos - q * sin).astype(BF16)
        rot[second, :] = (q * cos + p * sin).astype(BF16)
    loop(q_all // hd, turn)
    for k in range(groups):
        turn(q_all // hd + 2 * k)
        vs = seg(q_all // hd + 2 * k + 1, hd)
        rot[vs, :] = acc[vs, :].astype(BF16)
    per = N_DEV // groups
    q_rows = lambda peer: seg(peer, qw)
    kv_rows = lambda peer: seg(q_all // (2 * hd) + peer // per, 2 * hd)
    qs = Swap(lambda peer: rot.at[q_rows(peer), :], lambda o: qkv_ref.at[:qw, seg(o, tokens)], qsems, me)
    kvs = Swap(lambda peer: rot.at[kv_rows(peer), :], lambda o: qkv_ref.at[qw:, seg(o, tokens)], ksems, me)
    qs.start()
    kvs.start()
    gw.start()
    keep_own(wo_ref, full_w, me)
    gain_row(g_scr, small_all, 1)
    qkv_ref[:qw, seg(me, tokens)] = rot[q_rows(me), :]
    qkv_ref[qw:, seg(me, tokens)] = rot[kv_rows(me), :]
    wgu_ref[:feat, seg(me)] = wg_t[seg(me, feat), :]
    wgu_ref[feat:, seg(me)] = wu_t[seg(me, feat), :]
    gates.start((CORE,))
    ups.start((CORE,))
    for swap in (qs, kvs):
        swap.wait_recv()
    stores = fetch_all(esem, (qkv_ref, qkv_out), (u_scr, u_out), (cos_ref, cos_out), (sin_ref, sin_out))
    heads = qkv_ref.shape[0] // hd - 2
    seq = qkv_ref.shape[1]
    scale = hd ** -0.5
    lanes = heads * QB
    key_rows(k_scr, qkv_ref, qw, hd)

    outs = Swap(lambda peer: o_send.at[seg(peer), :], lambda o: o_tok.at[:, seg(o)], osems, me)

    def q_block(qb):
        for at, r in ((2, 0), (4, 1), (5, 2), (6, 3), (7, 4)):
            @pl.when(qb == at)
            def _():
                gw.round(r)
        qs = seg(qb, QB)
        q2 = side_by_side(qkv_ref, heads, hd, qs)

        def scores(kb, top, diagonal):
            s = score_block(k_scr[seg(kb, KB), :], q2, scale, diagonal)
            s_scr[seg(kb, KB), :] = s
            return jnp.maximum(top, jnp.max(s, axis=0, keepdims=True))

        top = lax.fori_loop(0, qb, lambda kb, t: scores(kb, t, False), jnp.full((1, lanes), NEG_LARGE, F32))
        top = scores(qb, top, True)

        def expo(kb, tot):
            e = jnp.exp(s_scr[seg(kb, KB), :] - top)
            s_scr[seg(kb, KB), :] = e
            return tot + jnp.sum(e, axis=0, keepdims=True)

        inv = 1.0 / lax.fori_loop(0, qb + 1, expo, jnp.zeros((1, lanes), F32))

        def weigh(kb, acc):
            p = (s_scr[seg(kb, KB), :] * inv).astype(BF16)
            return acc + mm(qkv_ref[qw + hd:, seg(kb, KB)], p, NN)

        acc = lax.fori_loop(0, qb + 1, weigh, jnp.zeros((hd, lanes), F32))
        for h in range(heads):
            o_ref[h * hd:(h + 1) * hd, qs] = acc[:, h * QB:(h + 1) * QB].astype(BF16)
        stat_ref[qb, :1, :] = top
        stat_ref[qb, 1:, :] = inv
        o_send[qs, :] = o_ref[:, qs].T

    loop(seq // QB, q_block)
    outs.start()
    advance(3)
    o_tok[:, seg(me)] = o_send[seg(me), :]
    for r in (5, 6):
        gw.round(r)
    outs.wait_recv()
    for mask in CHIP_MASKS:
        gw.wait_pair(mask)

    def project(n):
        cs = seg(n, CHUNK)
        acc_o[:, cs] = mm(o_tok[...], full_w[:, :, cs].reshape(dim, CHUNK), NN)
    loop(dim // CHUNK, project)

    def residual(i):
        rs = seg(i, STRIP)
        h_ref[rs, :] = (x_ref[rs, :].astype(F32) + acc_o[rs, :]).astype(BF16)
    loop(tokens // STRIP, residual)
    norm_rows(h_ref, g_scr, m_ref)
    for swap in (gates, ups):
        swap.wait_recv()
    for mask in CHIP_MASKS:
        keep(mask).wait()
    outs.wait_send()
    for swap in (gates, ups):
        swap.wait_send((CORE,) + SETS[3])
    for store in stores:
        store.wait()
    g.finish()
    gw.finish()
    for swap in (smalls, qs, kvs):
        swap.wait_send()


def dw_swaps(stage, gate_hbm, up_hbm, sems, me):
    feat = gate_hbm.shape[0] // N_DEV
    return [Swap(lambda peer, lo=lo: stage(peer).at[lo:lo + feat, seg(peer % 2)], lambda o, dst=dst: dst.at[seg(o, feat), :], sems[i:i + 2], me)
            for lo, dst, i in ((0, gate_hbm, 0), (feat, up_hbm, 2))]


def mlp(m_ref, dout_ref, wgu_hbm, down_hbm, u_ref, h_ref, small_all, wo_ref, o_ref,
        ucol_ref, m_out, dgu_out, ddown_out, y_ref, dh_ref, do_ref, dwo_ref, dg_ref, gate_hbm, up_hbm,
        wgu_ref, down_ref, glu_ref, dgu_ref, ddown_ref, isem, dsem, full_d, full_m, osem, stage, g_scr, dgu_t, glu_t, free, *scr):
    me = lax.axis_index('sp')
    feat, dim = down_ref.shape
    loads = fetch_all(isem, (wgu_hbm, wgu_ref), (down_hbm, down_ref))
    enter(me, OTHERS)
    sems = scr[4:]
    gd = row_gather(dout_ref, full_d, sems[:4], me, 0)
    gm = row_gather(m_ref, full_m, sems[4:8], me, 2)
    g = row_gather(dh_ref, full_d, sems[8:12], me, 1)
    ucols = Swap(lambda peer: u_ref.at[:, seg(peer)], lambda o: ucol_ref.at[seg(o), :], sems[12:14], me)
    gates, ups = dw_swaps(lambda peer: stage, gate_hbm, up_hbm, sems[14:18], me)
    gm.start()
    gd.start()
    keep_own(m_ref, full_m, me)
    keep_own(dout_ref, full_d, me)
    gain_row(g_scr, small_all, 1)
    dwo_ref[...] = jnp.zeros_like(dwo_ref)
    ddown_ref[...] = jnp.zeros_like(ddown_ref)

    def keep(mask):
        chip = flipped(me, mask) // 2
        ts = seg(chip, WIDE)
        ends = ((full_m.at[chip], m_out.at[chip]), (dgu_ref.at[:, ts], dgu_out.at[:, ts]))
        return [pltpu.make_async_copy(src, dst, osem.at[mask // 2, i]) for i, (src, dst) in enumerate(ends)]

    for load in loads:
        load.wait()
    ucol_ref[seg(me), :] = u_ref[:, seg(me)]

    def use(mask):
        gd.wait_pair(mask)
        gm.wait_pair(mask)
        chip = flipped(me, mask) // 2
        ts = seg(chip, WIDE)
        gu = mm(wgu_ref[...], full_m[chip], NT).astype(BF16).astype(F32)
        gate, up = gu[:feat], gu[feat:]
        d_glu = mm(down_ref[...], full_d[chip], NT).astype(BF16).astype(F32)
        sig = jax.nn.sigmoid(gate)
        act = gate * sig
        glu = (act * up).astype(BF16)
        glu_ref[:, ts] = glu
        dgu_ref[:feat, ts] = (d_glu * up * (sig * (1.0 + gate * (1.0 - sig)))).astype(BF16)
        dgu_ref[feat:, ts] = (d_glu * act).astype(BF16)

        def step(n):
            ddown_ref[:, seg(n, CHUNK)] += mm(glu, full_d[chip, :, seg(n, CHUNK)], NN)
        loop(dim // CHUNK, step)
        for copy in keep(mask):
            copy.start()

    for r in range(len(gm.ROUNDS)):
        gm.round(r)
        gd.round(r)
        if r == 3:
            ucols.start()
        run_ready(gm.READY[r], use)
    far = seg(flipped(me, XYZ) // 2, WIDE)
    stage[...] = mm(dgu_ref[...], full_m[:, :, far].reshape(dgu_ref.shape[1], WIDE), NN)
    for swap in (gates, ups):
        swap.start(SETS[0])
    for gather in (gd, gm):
        gather.finish()
    leave = pltpu.make_async_copy(ddown_ref, ddown_out, dsem)
    leave.start()
    s = Scatter(*scr[:4], sems[18:], me)
    total = s.run(block_product(s, dgu_ref, wgu_ref, dgu_t))
    for mask in NEAR:
        pl.semaphore_signal(free, inc=1, device_id=(flipped(me, mask),), device_id_type=MESH)
    norm_back(total, h_ref, g_scr, dout_ref, dh_ref, dg_ref)
    g.start()
    keep_own(dh_ref, full_d, me)
    s.finish()
    pl.semaphore_wait(free, len(NEAR))

    def use_dh(mask):
        g.wait_pair(mask)
        chip = flipped(me, mask) // 2
        do_ref[:, seg(chip, WIDE)] = mm(wo_ref[...], full_d[chip], NT).astype(BF16)
        o = o_ref[:, seg(chip, WIDE)]

        def step(n):
            dwo_ref[:, seg(n, CHUNK)] += mm(o, full_d[chip, :, seg(n, CHUNK)], NN)
        loop(dim // CHUNK, step)

    def between(i):
        r = i if i < 3 else i - N_CHIP + 3
        if i < 3 or i >= N_CHIP:
            g.round(r)
            run_ready(g.READY[r], use_dh)

    s = Scatter(*scr[:4], sems[18:], me)
    total = s.run(block_product(s, glu_ref, down_ref, glu_t), between)
    y_ref[...] = (h_ref[...].astype(F32) + total[...]).astype(BF16)
    s.finish()
    g.finish()
    for swap in (gates, ups):
        swap.wait_recv(SETS[0])
        swap.wait_send(SETS[0])
    ucols.wait_recv()
    ucols.wait_send()
    leave.wait()
    ends = ((full_m.at[0], m_out.at[0]), (dgu_ref.at[:, seg(0, WIDE)], dgu_out.at[:, seg(0, WIDE)]))
    loop(N_CHIP, lambda j: [pltpu.make_async_copy(src, dst, osem.at[j, i]).wait() for i, (src, dst) in enumerate(ends)])


def back(groups, hd, qkv_hbm, do_hbm, stat_ref, cos_all, sin_all, dgu_hbm, m_hbm, ucol_ref, w_hbm, x_ref, small_all, dh_ref, dg2_ref, dg_in, du_in,
         dg_hbm, du_hbm, dwq_ref, dwkv_ref, dx_ref, gain_ref,
         dgu_ref, qkv_ref, do_ref, isem, qsem,
         p_scr, dp_scr, k_scr, v_scr, dk_acc, dv_acc, stage, dq_scr, dkv_scr, m_scr,
         full, w_scr, shares, dkv_own, full_kv, dqkv, dn, g_scr, dg1, gains, gains_in, wsem, lsem, msem, *sems):
    heads = qkv_ref.shape[0] // hd - 2
    seq = qkv_ref.shape[1]
    scale = hd ** -0.5
    lanes = heads * QB
    qw = heads * hd
    half = hd // 2
    me = lax.axis_index('sp')
    feat = dgu_ref.shape[0] // 2
    first = (X, Y + Z, Y, X + Z, Z, X + Y, 0)

    def fetch(mask):
        cols = seg(flipped(me, mask) // 2, WIDE)
        return pltpu.make_async_copy(m_hbm.at[:, :, cols], m_scr.at[:, :, cols], msem.at[mask // 2])
    needed, = fetch_all(isem, (dgu_hbm, dgu_ref))
    for mask in first[:2]:
        fetch(mask).start()
    load = pltpu.make_async_copy(w_hbm, w_scr, wsem)
    enter(me, OTHERS)
    for mask in first[2:]:
        fetch(mask).start()
    loads = fetch_all(qsem, (qkv_hbm, qkv_ref), (do_hbm, do_ref))
    gain_row(g_scr, small_all, 0)

    gates, ups = dw_swaps(lambda peer: stage.at[peer // 2], dg_hbm, du_hbm, sems[:4], me)
    gq = row_gather(dq_scr, full, sems[6:10], me)
    own = [pltpu.make_async_copy(swap.src(me), swap.dst(me), lsem.at[i]) for i, swap in enumerate((gates, ups))]

    def make(mask):
        chip = flipped(me, mask) // 2
        fetch(mask).wait()
        cols = m_scr[:, :, seg(chip, WIDE)].reshape(seq, WIDE)
        stage[chip] = mm(dgu_ref[...], cols, NN)

    def advance(n):
        for swap in (gates, ups):
            if n > 1:
                swap.wait_send(SETS[n - 1])
            swap.start(SETS[n])

    needed.wait()
    for i, mask in enumerate(first):
        make(mask)
        if i == 1:
            advance(1)
    load.start()
    for copy in loads:
        copy.wait()
    gates.start((CORE,))
    ups.start((CORE,))
    for copy in own:
        copy.start()

    dk_acc[...] = jnp.zeros_like(dk_acc)
    dv_acc[...] = jnp.zeros_like(dv_acc)
    key_rows(k_scr, qkv_ref, qw, hd)
    key_rows(v_scr, qkv_ref, qw + hd, hd)

    def q_block(qb):
        @pl.when(qb == 4)
        def _():
            advance(2)
        qs = seg(qb, QB)
        q2 = side_by_side(qkv_ref, heads, hd, qs)
        do2 = side_by_side(do_ref, heads, hd, qs)
        top = stat_ref[qb, :1, :]
        inv = stat_ref[qb, 1:, :]

        def probs(kb, rd, diagonal):
            ks = seg(kb, KB)
            s = score_block(k_scr[ks, :], q2, scale, diagonal)
            p = jnp.exp(s - top) * inv
            dp = mm(v_scr[ks, :], do2, NN).astype(BF16)
            p_scr[ks, :] = p
            dp_scr[ks, :] = dp
            dv_acc[ks, :] += mm(p.astype(BF16), do2, NT)
            return rd + jnp.sum(dp.astype(F32) * p, axis=0, keepdims=True)

        rd = lax.fori_loop(0, qb, lambda kb, r: probs(kb, r, False), jnp.zeros((1, lanes), F32))
        rd = probs(qb, rd, True)

        def d_scores(kb, acc):
            ks = seg(kb, KB)
            ds = (p_scr[ks, :] * (dp_scr[ks, :].astype(F32) - rd) * scale).astype(BF16)
            dk_acc[ks, :] += mm(ds, q2, NT)
            return acc + mm(qkv_ref[qw:qw + hd, ks], ds, NN)

        acc = lax.fori_loop(0, qb + 1, d_scores, jnp.zeros((hd, lanes), F32))
        cos, sin = cos_all[:, qs], sin_all[:, qs]
        for h in range(heads):
            dq = acc[:, h * QB:(h + 1) * QB].astype(BF16).astype(F32)
            p, q = dq[:half], dq[half:]
            dq_scr[h * hd:h * hd + half, qs] = (p * cos + q * sin).astype(BF16)
            dq_scr[h * hd + half:(h + 1) * hd, qs] = (q * cos - p * sin).astype(BF16)

    loop(seq // QB, q_block)

    def share(i):
        rs = seg(i, WIDE)
        dkv_scr[rs, :] = jnp.concatenate([dk_acc[rs, :], dv_acc[rs, :]], axis=1).astype(BF16)
    loop(seq // WIDE, share)
    tokens = ucol_ref.shape[1]
    per = N_DEV // groups
    q_all = dwq_ref.shape[0]
    sh = Swap(lambda peer: dkv_scr.at[seg(peer, tokens), :], lambda o: shares.at[o], sems[4:6], me)
    parts = thirds(dkv_own.shape[0], STRIP)
    gk = Gather(dkv_own, lambda o: full_kv.at[:, seg(o, tokens)], lambda view, c: [view.at[pl.ds(*parts[c]), :]], sems[10:14], me)
    gs = Swap(lambda peer: gains.at[:, seg(peer)], lambda o: gains_in.at[o], sems[14:], me)
    sh.start()
    gq.start()
    keep_own(dq_scr, full, me)
    shares[me] = dkv_scr[seg(me, tokens), :]
    sh.wait_recv()
    cos, sin = cos_all[:, seg(me)], sin_all[:, seg(me)]
    for k in range(groups):
        both = sum(shares[per * k + i].astype(F32) for i in range(per)).astype(BF16).astype(F32).T
        p, q = both[:half], both[half:hd]
        lo = 2 * hd * k
        dkv_own[lo:lo + half, :] = (p * cos + q * sin).astype(BF16)
        dkv_own[lo + half:lo + hd, :] = (q * cos - p * sin).astype(BF16)
        dkv_own[lo + hd:lo + 2 * hd, :] = both[hd:].astype(BF16)
    gk.start()
    full_kv[:, seg(me, tokens)] = dkv_own[...]
    for k in range(groups):
        dqkv[:, q_all + 2 * hd * k:q_all + 2 * hd * (k + 1)] = dkv_own[2 * hd * k:2 * hd * (k + 1), :].T

    def use(mask):
        gq.wait_pair(mask)
        chip = flipped(me, mask) // 2
        dwq_ref[seg(chip, WIDE), :] = mm(full[chip], ucol_ref[...], NN)
        dqkv[:, seg(chip, WIDE)] = full[chip, :, seg(me, tokens)].T

    for r in range(len(gq.ROUNDS)):
        gq.round(r)
        gk.round(r)
        if r == 3:
            advance(3)
        run_ready(gq.READY[r], use)
    load.wait()

    def normed(i):
        dn[:, seg(i, WIDE)] = mm(dqkv[...], w_scr[i], NN)
    loop(N_CHIP, normed)
    norm_back(dn, x_ref, g_scr, dh_ref, dx_ref, dg1)
    gains[...] = jnp.concatenate([jnp.sum(dg1[...], axis=0, keepdims=True), jnp.sum(dg2_ref[...], axis=0, keepdims=True),
                                  jnp.zeros((N_CHIP - 2, dg1.shape[1]), F32)], axis=0)
    gs.start()
    gains_in[me] = gains[:, seg(me)]
    for mask in CHIP_MASKS:
        gk.wait_pair(mask)
    dwkv_ref[...] = mm(full_kv[...], ucol_ref[...], NN)
    gs.wait_recv()
    gain_ref[...] = sum(gains_in[o] for o in range(N_DEV))
    for swap in (gates, ups):
        swap.wait_recv((CORE,) + SETS[1] + SETS[2] + SETS[3])
        swap.wait_send((CORE,) + SETS[3])
    for copy in own:
        copy.wait()
    for c in (sh, gs):
        c.wait_send()
    for g in (gq, gk):
        g.finish()


def finish(dg_hbm, du_hbm, dkv_hbm, *refs):
    n = (len(refs) - 14) // 3
    gains, refs = refs[0], refs[1:]
    srcs, (gate, up, dk, dv, dg1, dg2), refs = refs[:n], refs[n:n + 6], refs[n + 6:]
    dsts, (g_in, g_out, kv_in), holds, sems = refs[:n], refs[n:n + 3], refs[n + 3:2 * n + 3], refs[2 * n + 3:]
    dg1[...] = gains[:1, :]
    dg2[...] = gains[1:2, :]
    t_in, t_out, p_in, p_out = sems
    step = LANE * 11
    cols = g_in.shape[1]
    hd = dk.shape[0] // (kv_in.shape[0] // LANE)
    starts = [(w, i) for i in range(cols // step) for w in range(2)]

    def fetch(w, i):
        rs = pl.ds(i * step, step)
        return pltpu.make_async_copy((dg_hbm, du_hbm)[w].at[rs, :], g_in.at[w, rs, :], t_in.at[w, i])

    def put(w, i):
        cs = pl.ds(i * step, step)
        return pltpu.make_async_copy(g_out.at[w, :, cs], (gate, up)[w].at[:, cs], t_out.at[w, i])
    moves = [(pltpu.make_async_copy(a, h, p_in.at[k]), pltpu.make_async_copy(h, b, p_out.at[k])) for k, (a, h, b) in enumerate(zip(srcs, holds, dsts))]
    kv = pltpu.make_async_copy(dkv_hbm, kv_in, p_in.at[n])
    for w, i in starts:
        fetch(w, i).start()
    kv.start()
    for load, _ in moves:
        load.start()
    for w, i in starts:
        fetch(w, i).wait()

        at = pl.ds(i * step, step)
        g_out[w, :, at] = g_in[w, at, :].T
        put(w, i).start()
    kv.wait()
    for k in range(dk.shape[0] // hd):
        for i, ref in enumerate((dk, dv)):
            ref[k * hd:(k + 1) * hd, :] = kv_in[(2 * k + i) * hd:(2 * k + i + 1) * hd, :]
    for load, store in moves:
        load.wait()
        store.start()
    for w, i in starts:
        put(w, i).wait()
    for _, store in moves:
        store.wait()


def solution(mesh):
    assert mesh.shape['sp'] == N_DEV

    def layer_step(x_in, positions, d_out, norm1_gain, norm2_gain, w_q, w_k, w_v, w_o, w_gate, w_up, w_down):
        tokens, dim = x_in.shape
        seq = tokens * N_DEV
        n_q, hd = w_q.shape[1:]
        n_kv = w_k.shape[1]
        qw = n_q // N_DEV * hd
        rows = w_q.shape[0]
        feat = w_down.shape[0]
        cols = (n_q + 2 * n_kv) * hd
        lanes = qw // hd * QB
        vm = pltpu.VMEM
        full = vm((N_CHIP, WIDE, dim), BF16)
        gain_scr = vm((N_CHIP, dim), F32)
        tok_shapes = 2 * (((tokens, dim), BF16),)
        dw_shapes = 2 * (((feat * N_DEV, rows), F32),)

        inv_freq = 1.0 / (ROPE_BASE ** (jnp.arange(hd // 2, dtype=F32) * (2.0 / hd)))
        freq = jnp.broadcast_to(inv_freq[:, None], (hd // 2, rows))
        row = lambda v: v.reshape(1, rows)
        by_head = lambda w: w.transpose(1, 2, 0).reshape(-1, rows)
        wo_own = w_o.reshape(qw, dim)

        args = (x_in, row(norm1_gain), row(norm2_gain), row(positions), by_head(w_q), by_head(w_k), by_head(w_v), freq, w_gate, w_up, wo_own)
        qkv, u, small_all, wqkv, attn_t, stat, wgu, hidden, mlp_in, cos_all, sin_all = call(
            functools.partial(head, n_kv, hd), 0, len(args),
            (((qw + 2 * hd, seq), BF16), tok_shapes[0], ((N_DEV, N_CHIP, rows), F32), ((N_CHIP, cols, WIDE), BF16),
             ((qw, seq), BF16), ((seq // QB, 2, lanes), F32), ((2 * feat, dim), BF16), *tok_shapes, *(2 * (((hd // 2, seq), F32),))),
            [vm(w_gate.shape, BF16), vm(w_up.shape, BF16), vm((qw, dim), BF16), vm((qw + 2 * hd, seq), BF16), vm((tokens, dim), BF16),
             vm((hd // 2, seq), F32), vm((hd // 2, seq), F32), dma(3), dma(4),
             full, vm((tokens, dim), F32), vm((tokens, dim), BF16), vm((seq, qw), BF16),
             vm((N_CHIP, rows), F32), vm((cols, rows), BF16), vm((N_CHIP, cols, WIDE), BF16), vm((cols, tokens), F32), vm((cols, tokens), BF16), gain_scr,
             vm((feat * N_DEV, rows), BF16), vm((feat * N_DEV, rows), BF16), vm((seq, lanes), F32), vm((seq, hd), BF16), dma(N_CHIP),
             *Gather.sems, *(6 * Swap.sems), *Gather.sems], 4 * qw * seq * seq, far_in=(8, 9, 10), far_out=(0, 1, 3, 9, 10))(*args)
        args = (mlp_in, d_out, wgu, w_down, u, hidden, small_all, wo_own, attn_t)
        u_col, m_full, dgu, d_down, y_out, d_hidden, d_attn, d_wo, d_g2, d_gate_t, d_up_t = call(
            mlp, 1, len(args),
            (((seq, rows), BF16), ((N_CHIP, WIDE, dim), BF16), ((2 * feat, seq), BF16), ((feat, dim), F32),
             *tok_shapes, ((qw, seq), BF16), ((qw, dim), F32), ((N_CHIP, dim), F32), *dw_shapes),
            [vm((2 * feat, dim), BF16), vm((feat, dim), BF16),
             vm((feat, seq), BF16), vm((2 * feat, seq), BF16), vm((feat, dim), F32), dma(2), dma(),
             full, full, dma(N_CHIP, 2), vm((2 * feat, WIDE), F32), gain_scr, vm((WIDE, 2 * feat), BF16), vm((WIDE, feat), BF16), pltpu.SemaphoreType.REGULAR,
             *Scatter.scratch(tokens, dim), *(3 * Gather.sems), *(3 * Swap.sems), *Scatter.sems], 12 * feat * seq * dim,
            far_in=(2, 3), far_out=(1, 2, 3, 9, 10))(*args)
        args = (qkv, d_attn, stat, cos_all, sin_all, dgu, m_full, u_col, wqkv, x_in, small_all, d_hidden, d_g2, d_gate_t, d_up_t)
        d_gate_t, d_up_t, d_wq, d_wkv, d_x, gains = call(
            functools.partial(back, n_kv, hd), 3, len(args),
            (*dw_shapes, ((n_q * hd, rows), F32), ((2 * n_kv * hd, rows), F32), tok_shapes[0], ((N_CHIP, rows), F32)),
            [vm((2 * feat, seq), BF16), vm((qw + 2 * hd, seq), BF16), vm((qw, seq), BF16), dma(1), dma(2),
             vm((seq, lanes), F32), vm((seq, lanes), BF16), vm((seq, hd), BF16), vm((seq, hd), BF16), vm((seq, hd), F32), vm((seq, hd), F32),
             vm((N_CHIP, 2 * feat, WIDE), F32), vm((qw, seq), BF16), vm((seq, 2 * hd), BF16), full,
             full, vm((N_CHIP, cols, WIDE), BF16), vm((N_DEV, tokens, 2 * hd), BF16), vm((2 * n_kv * hd, tokens), BF16), vm((2 * n_kv * hd, seq), BF16),
             vm((tokens, cols), BF16), vm((tokens, dim), F32), gain_scr, gain_scr, gain_scr, vm((N_DEV, N_CHIP, rows), F32), dma(), dma(2), dma(N_CHIP),
             *(3 * Swap.sems), *(2 * Gather.sems), *Swap.sems], 10 * qw * seq * seq, far_in=(0, 1, 5, 6, 8, 13, 14), far_out=(0, 1), aliases={13: 0, 14: 1})(*args)
        moved = (d_wq, d_wo, d_down, d_x, y_out)
        one_row = jax.ShapeDtypeStruct((1, rows), F32)
        half_kv = jax.ShapeDtypeStruct((n_kv * hd, rows), F32)
        wide = jax.ShapeDtypeStruct((rows, feat * N_DEV), F32)
        d_gate, d_up, d_wk, d_wv, d_g1, d_g2, d_wq, d_wo, d_down, d_x, y_out = pl.pallas_call(
            finish,
            out_shape=[wide, wide, half_kv, half_kv, one_row, one_row] + [jax.ShapeDtypeStruct(v.shape, v.dtype) for v in moved],
            in_specs=[IN_HBM] * 3 + on_chip(1) + [IN_HBM] * len(moved), out_specs=[IN_HBM] * 2 + on_chip(4) + [IN_HBM] * len(moved),
            scratch_shapes=[vm((2, feat * N_DEV, rows), F32), vm((2, rows, feat * N_DEV), F32), vm(d_wkv.shape, F32)]
            + [vm(v.shape, v.dtype) for v in moved] + [dma(2, 4), dma(2, 4), dma(len(moved) + 1), dma(len(moved))],
            compiler_params=pltpu.CompilerParams(vmem_limit_bytes=VMEM_CAP), name='finish',
        )(d_gate_t, d_up_t, d_wkv, gains, *moved)
        by_row = lambda g, heads: g.reshape(heads, hd, rows).transpose(2, 0, 1)
        return (y_out, d_x, d_g1.reshape(rows), d_g2.reshape(rows), by_row(d_wq, n_q), by_row(d_wk, n_kv), by_row(d_wv, n_kv),
                d_wo.reshape(w_o.shape), d_gate, d_up, d_down)

    all_rows = P('sp')
    return jax.shard_map(layer_step, mesh=mesh, in_specs=(all_rows,) * 12, out_specs=(all_rows,) * 11, check_vma=False)
```

```python
import functools
import jax
import jax.numpy as jnp
from jax import lax
from jax.experimental import pallas as pl
from jax.experimental.pallas import tpu as pltpu
from jax.sharding import PartitionSpec as P

ROPE_BASE = 10000.0
NORM_EPS = 1e-5
NEG_LARGE = -1e30
F32 = jnp.float32
BF16 = jnp.bfloat16
N_DEV, N_CHIP, LANE, WIDE, CHUNK, STRIP = 16, 8, 128, 256, 512, 16
NT = (((1,), (1,)), ((), ()))
TN = (((0,), (0,)), ((), ()))
NN = (((1,), (0,)), ((), ()))
MESH = pl.DeviceIdType.MESH
VMEM_CAP = 67043328

CORE, X, Y, Z = 1, 2, 4, 8
XYZ = X + Y + Z
ORDERS = ((X, Y, Z), (Y, Z, X), (Z, X, Y))
CHIP_MASKS = (0, X, Y, Z, X + Y, X + Z, Y + Z, XYZ)
NEAR = (CORE, X, Y, Z)
OTHERS = range(1, N_DEV)
SETS = tuple(tuple(m + c for m in masks for c in (0, CORE)) for masks in ((XYZ,), (X, Y + Z), (Y, X + Z), (Z, X + Y)))
N_COL = len(ORDERS)
COLOURS = range(N_COL)


def mm(a, b, dims):
    return lax.dot_general(a, b, dims, preferred_element_type=F32)


def seg(index, width=LANE):
    return pl.ds(pl.multiple_of(index * width, width), width)


def loop(count, body):
    lax.fori_loop(0, count, lambda i, c: (body(i), c)[1], 0)


def differing(index, mask):
    return sum(((index // bit + mask // bit) % 2) * bit for bit in NEAR)


def flipped(index, mask):
    if not isinstance(mask, int):
        return differing(index, mask)
    out = index
    for bit in NEAR:
        if mask & bit:
            out = out + (1 - 2 * ((index // bit) % 2)) * bit
    return out


def run_ready(masks, use):
    if len(masks) == 2:
        loop(2, lambda j: use(masks[0] + (masks[1] - masks[0]) * j))
    else:
        for mask in masks:
            use(mask)


def thirds(total, unit):
    n = total // unit
    first = (n + 2) // 3
    second = (n - first + 1) // 2
    sizes = (first * unit, second * unit, (n - first - second) * unit)
    return ((0, sizes[0]), (sizes[0], sizes[1]), (sizes[0] + sizes[1], sizes[2]))


def pieces(rows, cols, unit):
    share = cols // LANE // N_COL * LANE
    strips = thirds(rows, unit)
    rest = cols - N_COL * share
    return [[(pl.ds(0, rows), pl.ds(c * share, share)), (pl.ds(*strips[c]), pl.ds(N_COL * share, rest))] for c in COLOURS]


def enter(me, masks):
    barrier = pltpu.get_barrier_semaphore()
    for mask in masks:
        pl.semaphore_signal(barrier, inc=1, device_id=(flipped(me, mask),), device_id_type=MESH)
    pl.semaphore_wait(barrier, len(masks))


def remote(src, dst, send, recv, peer):
    return pltpu.make_async_remote_copy(src_ref=src, dst_ref=dst, send_sem=send, recv_sem=recv, device_id=(peer,), device_id_type=MESH)


def dma(*shape):
    return pltpu.SemaphoreType.DMA(shape)


class Swap:
    sems = (dma(N_DEV), dma(N_DEV))

    def __init__(self, src, dst, sems, me):
        self.src, self.dst, (self.send, self.recv), self.me = src, dst, sems, me

    def copy(self, mask):
        peer = differing(self.me, mask)
        return remote(self.src(peer), self.dst(self.me), self.send.at[mask], self.recv.at[mask], peer)

    def arrival(self, mask):
        view = self.dst(differing(self.me, mask))
        return remote(view, view, self.send.at[mask], self.recv.at[mask], self.me)

    def each(self, masks, act):
        if masks is None:
            loop(N_DEV - 1, lambda i: act(i + 1))
        else:
            for mask in masks:
                act(mask)

    def start(self, masks=None):
        self.each(masks, lambda mask: self.copy(mask).start())

    def advance(self, n):
        if n:
            self.wait_send(SETS[n - 1])
        self.start(SETS[n])

    def wait_recv(self, masks=None):
        self.each(masks, lambda mask: self.arrival(mask).wait_recv())

    def wait_send(self, masks=None):
        self.each(masks, lambda mask: self.copy(mask).wait_send())


class Gather:
    ROUNDS = ((0,), (1,), (2,), (0, 1), (0, 2), (1, 2), (0, 1, 2))
    READY = ((0,), (), (), (X, Y), (Z,), (X + Y, X + Z), (Y + Z, XYZ))
    sems = (dma(N_COL, N_CHIP, 2), dma(N_COL, N_CHIP, 2), dma(N_CHIP), dma(N_CHIP))

    def __init__(self, own, block, cut, sems, me):
        self.own, self.block, self.cut, self.me = own, block, cut, me
        self.send, self.recv, self.pair_send, self.pair_recv = sems

    def source(self, mask):
        return self.block(flipped(self.me, mask)) if mask else self.own

    def unit(self, colour, mask, axis):
        ends = zip(self.cut(self.source(mask), colour), self.cut(self.block(flipped(self.me, mask)), colour))
        j = self.sends(colour).index((mask, axis))
        return [remote(src, dst, self.send.at[colour, j, i], self.recv.at[colour, (mask + axis) // 2, i],
                       flipped(self.me, axis)) for i, (src, dst) in enumerate(ends)]

    def sends(self, colour):
        return [(0, axis) for axis in ORDERS[colour]] + [step[1:] for step in self.onward(colour)]

    def start_unit(self, colour, mask, axis):
        for copy in self.unit(colour, mask, axis):
            copy.start()

    def pair(self, mask):
        return remote(self.source(mask), self.block(flipped(self.me, mask)), self.pair_send.at[mask // 2],
                      self.pair_recv.at[mask // 2], flipped(self.me, CORE))

    def wait_pair(self, mask):
        view = self.block(flipped(self.me, mask + CORE))
        remote(view, view, self.pair_send.at[mask // 2], self.pair_recv.at[mask // 2], self.me).wait_recv()

    def onward(self, colour):
        order = ORDERS[colour]
        for picks in self.ROUNDS:
            for axis in order[picks[-1] + 1:]:
                yield picks, sum(order[p] for p in picks), axis

    def start(self):
        for pos in COLOURS:
            for colour in COLOURS:
                self.start_unit(colour, 0, ORDERS[colour][pos])
        self.pair(0).start()

    def round(self, r):
        for colour in COLOURS:
            mask = sum(ORDERS[colour][p] for p in self.ROUNDS[r])
            for i, view in enumerate(self.cut(self.block(flipped(self.me, mask)), colour)):
                remote(view, view, self.send.at[colour, 0, i], self.recv.at[colour, mask // 2, i], self.me).wait_recv()
            for picks, at, axis in self.onward(colour):
                if picks == self.ROUNDS[r]:
                    self.start_unit(colour, at, axis)
        for mask in {2: (X, Y, Z), 5: (X + Y, X + Z, Y + Z), 6: (XYZ,)}.get(r, ()):
            self.pair(mask).start()

    def finish(self):
        for colour in COLOURS:
            for i, view in enumerate(self.cut(self.own, colour)):
                loop(len(self.sends(colour)), lambda j: remote(view, view, self.send.at[colour, j, i], self.recv.at[colour, j, i], self.me).wait_send())
        loop(N_CHIP, lambda j: remote(self.own, self.own, self.pair_send.at[j], self.pair_recv.at[j], self.me).wait_send())


def row_gather(own, full, sems, me, extra=None):
    rows, width = own.shape
    parts = pieces(rows, width, STRIP)
    if extra is not None:
        share = width // LANE // N_COL * LANE
        more = width - N_COL * share
        parts = [[(pl.ds(0, rows), pl.ds(c * share + more * (c > extra), share + more * (c == extra)))] for c in COLOURS]

    def block(o):
        return full.at[o // 2, seg(o % 2), :]

    return Gather(own, block, lambda view, c: [view.at[rs, cs] for rs, cs in parts[c]], sems, me)


def keep_own(own, full, me):
    def step(i):
        full[me // 2, pl.ds(pl.multiple_of((me % 2) * LANE + i * STRIP, STRIP), STRIP), :] = own[seg(i, STRIP), :]
    loop(LANE // STRIP, step)


class Scatter:
    ORDER = (XYZ, X + Y, Y + Z, X + Z, X, Y, Z, 0)
    sems = (dma(N_CHIP), dma(N_CHIP), dma(N_COL, N_CHIP, 2), dma(N_COL, N_CHIP, 2))

    @staticmethod
    def scratch(tokens, dim):
        return [pltpu.VMEM((n, tokens, dim), F32) for n in (N_CHIP, 2, N_CHIP, N_CHIP - 1)]

    def __init__(self, part, other, pair_in, link_in, sems, me):
        self.part, self.other, self.pair_in, self.link_in, self.me = part, other, pair_in, link_in, me
        self.pair_send, self.pair_recv, self.link_send, self.link_recv = sems
        self.tokens, self.dim = part.shape[1:]
        self.pieces = pieces(self.tokens, self.dim, STRIP // 2)
        self.ready, self.sent = set(), [0] * N_COL

    @staticmethod
    def first(colour, mask):
        return next((i for i, a in enumerate(ORDERS[colour]) if mask & a), 3)

    def slot(self, colour, mask, axis):
        slots = [(m, a) for m in self.ORDER for a in ORDERS[colour][:self.first(colour, m)]]
        return slots.index((mask, axis))

    def pair(self, i):
        return remote(self.other.at[i % 2], self.pair_in.at[i], self.pair_send.at[i], self.pair_recv.at[i], flipped(self.me, CORE))

    def link(self, colour, mask):
        axis = ORDERS[colour][self.first(colour, mask)]
        slot = self.slot(colour, mask - axis, axis)
        i = self.ORDER.index(mask)
        return [remote(self.part.at[i, rs, cs], self.link_in.at[slot, rs, cs], self.link_send.at[colour, i, k],
                       self.link_recv.at[colour, slot, k], flipped(self.me, axis)) for k, (rs, cs) in enumerate(self.pieces[colour])]

    def start_link(self, colour, mask):
        for copy in self.link(colour, mask):
            copy.start()

    def add(self, mask, ref, cs):
        i = self.ORDER.index(mask)

        def step(r):
            rs = seg(r, STRIP)
            self.part[i, rs, cs] += ref[rs, cs]
        loop(self.tokens // STRIP, step)

    def finish_pair(self, i):
        self.pair(i).wait_recv()
        self.add(self.ORDER[i], self.pair_in.at[i], pl.ds(0, self.dim))
        self.ready.add(self.ORDER[i])
        for colour in COLOURS:
            a, b, c = ORDERS[colour]
            todo = (XYZ, a + b, a + c, a)
            while self.sent[colour] < len(todo) and todo[self.sent[colour]] in self.ready:
                self.start_link(colour, todo[self.sent[colour]])
                self.sent[colour] += 1

    def take(self, colour, mask, axis):
        for copy in self.link(colour, mask + axis):
            copy.wait_recv()
        ref = self.link_in.at[self.slot(colour, mask, axis)]
        (_, wide), (rs, cs) = self.pieces[colour]
        self.add(mask, ref, wide)
        self.part[self.ORDER.index(mask), rs, cs] += ref[rs, cs]

    def run(self, product, between=lambda i: None):
        for i, mask in enumerate(self.ORDER):
            if i > 1:
                self.pair(i - 2).wait_send()
            product(i, flipped(self.me, mask) // 2)
            self.pair(i).start()
            if i:
                self.finish_pair(i - 1)
            between(i)
        self.finish_pair(N_CHIP - 1)
        for step in range(2):
            between(N_CHIP + step)
            for colour in COLOURS:
                a, b, c = ORDERS[colour]
                mask = (b + c, b)[step]
                self.take(colour, mask, a)
                self.start_link(colour, mask)
        between(N_CHIP + 2)
        for colour in COLOURS:
            a, b, c = ORDERS[colour]
            self.take(colour, c, a)
            self.take(colour, c, b)
            self.start_link(colour, c)
        between(N_CHIP + 3)
        for colour in COLOURS:
            for axis in ORDERS[colour]:
                self.take(colour, 0, axis)
        return self.part.at[N_CHIP - 1]

    def finish(self):
        for i in (N_CHIP - 2, N_CHIP - 1):
            self.pair(i).wait_send()
        for colour in COLOURS:
            for k, (rs, cs) in enumerate(self.pieces[colour]):
                view = self.part.at[0, rs, cs]
                loop(N_CHIP - 1, lambda i: remote(view, view, self.link_send.at[colour, i, k], self.link_recv.at[colour, i, k], self.me).wait_send())


def block_product(s, a_ref, w_ref, a_t):
    core = s.me % 2

    def product(i, chip):
        a_t[...] = a_ref[:, seg(chip, WIDE)].T

        def step(n):
            cs = seg(n, CHUNK)
            s.other[i % 2, :, cs] = mm(a_t[seg(1 - core), :], w_ref[:, cs], NN)
            s.part[i, :, cs] = mm(a_t[seg(core), :], w_ref[:, cs], NN)
        loop(s.dim // CHUNK, step)
    return product


def on_chip(n):
    return [pl.BlockSpec(memory_space=pltpu.VMEM)] * n


IN_HBM = pl.BlockSpec(memory_space=pl.ANY)


def call(kernel, ident, args, outs, scratch, flops, far_in=(), far_out=(), aliases={}):
    specs = [IN_HBM if i in far_in else on_chip(1)[0] for i in range(args)]
    out_specs = [IN_HBM if i in far_out else on_chip(1)[0] for i in range(len(outs))]
    return pl.pallas_call(
        kernel,
        out_shape=[jax.ShapeDtypeStruct(shape, dtype) for shape, dtype in outs],
        in_specs=specs, out_specs=out_specs, scratch_shapes=scratch, input_output_aliases=aliases,
        cost_estimate=pl.CostEstimate(flops=flops, bytes_accessed=flops // CHUNK, transcendentals=0),
        compiler_params=pltpu.CompilerParams(collective_id=ident, has_side_effects=True, vmem_limit_bytes=VMEM_CAP),
        name=kernel.func.__name__ if isinstance(kernel, functools.partial) else kernel.__name__,
    )


def fetch_all(sem, *pairs):
    copies = [pltpu.make_async_copy(src, dst, sem.at[i]) for i, (src, dst) in enumerate(pairs)]
    for copy in copies:
        copy.start()
    return copies


def gain_row(dst, small_all, which):
    for o in range(N_DEV):
        dst[:1, o * LANE:(o + 1) * LANE] = small_all[o, which:which + 1, :]


def norm_rows(src, gain, dst):
    def step(i):
        rs = seg(i, STRIP)
        t = src[rs, :].astype(F32)
        dst[rs, :] = (t * lax.rsqrt(jnp.mean(t * t, axis=-1, keepdims=True) + NORM_EPS) * gain[:1, :]).astype(BF16)
    loop(src.shape[0] // STRIP, step)


def norm_back(dy, src, gain, skip, dst, dgain):
    def step(i):
        rs = seg(i, STRIP)
        d = dy[rs, :].astype(BF16).astype(F32)
        t = src[rs, :].astype(F32)
        inv = lax.rsqrt(jnp.mean(t * t, axis=-1, keepdims=True) + NORM_EPS)
        gd = gain[:1, :] * d
        pull = jnp.mean(gd * t, axis=-1, keepdims=True)
        dst[rs, :] = (skip[rs, :].astype(F32) + (inv * gd - t * (inv * inv * inv * pull))).astype(BF16)
        g = d * (t * inv)
        dgain[...] += g[:N_CHIP] + g[N_CHIP:]
    dgain[...] = jnp.zeros_like(dgain)
    loop(src.shape[0] // STRIP, step)


QB = 256
KB = 256


def key_rows(dst, src, lo, hd):
    def step(i):
        dst[seg(i, KB), :] = src[lo:lo + hd, seg(i, KB)].T
    loop(src.shape[1] // KB, step)


def score_block(k, q2, scale, diagonal):
    s = mm(k, q2, NN) * scale
    if diagonal:
        key = lax.broadcasted_iota(jnp.int32, s.shape, 0)
        qry = lax.broadcasted_iota(jnp.int32, s.shape, 1) % QB
        s = jnp.where(qry >= key, s, NEG_LARGE)
    return s


def side_by_side(ref, heads, hd, qs):
    return jnp.concatenate([ref[h * hd:(h + 1) * hd, qs] for h in range(heads)], axis=1)


def head(groups, hd, x_ref, g1_ref, g2_ref, pos_ref, wq_ref, wk_ref, wv_ref, freq_ref, wg_hbm, wu_hbm, wo_hbm, qkv_out, u_out, small_all, w_out, o_ref, stat_ref, wgu_ref, h_ref, m_ref, cos_out, sin_out,
         wg_ref, wu_ref, wo_ref, qkv_ref, u_scr, cos_ref, sin_ref, isem, esem,
         full_w, acc_o, o_tok, o_send, small_ref, w_ref, full, acc, rot, g_scr, wg_t, wu_t, s_scr, k_scr, osem, *sems):
    me = lax.axis_index('sp')
    tokens, dim = x_ref.shape
    cols = w_ref.shape[0]
    small_ref[...] = jnp.concatenate([r[...].astype(F32) for r in (g1_ref, g2_ref, pos_ref)] + [jnp.zeros((N_CHIP - 3, LANE), F32)], axis=0)
    w_ref[:wq_ref.shape[0], :] = wq_ref[...]
    for k in range(groups):
        for i, ref in enumerate((wk_ref, wv_ref)):
            w_ref[pl.ds(wq_ref.shape[0] + (2 * k + i) * hd, hd), :] = ref[k * hd:(k + 1) * hd, :]
    qw = tokens
    q_all = N_DEV * qw
    gsems, ssems, qsems, ksems, gate_sems, up_sems, osems = sems[:4], *(sems[i:i + 2] for i in range(4, len(sems) - 4, 2))
    gw = row_gather(wo_ref, full_w, sems[-4:], me, 1)
    feat = wg_ref.shape[1] // N_DEV
    loads = fetch_all(isem, (wg_hbm, wg_ref), (wu_hbm, wu_ref), (wo_hbm, wo_ref))
    enter(me, OTHERS)
    smalls = Swap(lambda peer: small_ref, lambda o: small_all.at[o], ssems, me)
    smalls.start()
    parts = thirds(cols, STRIP)
    g = Gather(w_ref, lambda o: full.at[o // 2, :, seg(o % 2)], lambda view, c: [view.at[pl.ds(*parts[c]), :]], gsems, me)
    g.start()
    gates = Swap(lambda peer: wg_t.at[seg(peer, feat), :], lambda o: wgu_ref.at[:feat, seg(o)], gate_sems, me)
    ups = Swap(lambda peer: wu_t.at[seg(peer, feat), :], lambda o: wgu_ref.at[feat:, seg(o)], up_sems, me)

    def advance(n):
        gates.advance(n)
        ups.advance(n)

    def transpose(i):
        wg_t[seg(i, CHUNK), :] = wg_ref[:, seg(i, CHUNK)].T
        wu_t[seg(i, CHUNK), :] = wu_ref[:, seg(i, CHUNK)].T
    for load in loads:
        load.wait()
    loop(wg_ref.shape[1] // CHUNK, transpose)
    advance(0)

    def own_block(i):
        full[me // 2, seg(i, WIDE), seg(me % 2)] = w_ref[seg(i, WIDE), :]
    loop(cols // WIDE, own_block)
    acc[...] = jnp.zeros_like(acc)
    small_all[me] = small_ref[...]
    smalls.wait_recv()
    gain_row(g_scr, small_all, 0)
    norm_rows(x_ref, g_scr, u_scr)

    def keep(mask):
        chip = flipped(me, mask) // 2
        return pltpu.make_async_copy(full.at[chip], w_out.at[chip], osem.at[mask // 2])

    def use(mask):
        g.wait_pair(mask)
        keep(mask).start()
        chip = flipped(me, mask) // 2
        u = u_scr[:, seg(chip, WIDE)]

        def step(i):
            rs = seg(i, cols // 2)
            acc[rs, :] += mm(full[chip, rs, :], u, NT)
        loop(2, step)

    def tables(o):
        angles = freq_ref[...] * small_all[o, 2:3, :]
        cos_ref[:, seg(o)] = jnp.cos(angles)
        sin_ref[:, seg(o)] = jnp.sin(angles)

    for r in range(len(g.ROUNDS)):
        g.round(r)
        if r in (2, 5):
            advance(r // 2)
        if r == 1:
            loop(N_DEV, tables)
        run_ready(g.READY[r], use)

    half = hd // 2
    cos, sin = cos_ref[:, seg(me)], sin_ref[:, seg(me)]

    def turn(h):
        first = seg(2 * h, half)
        second = seg(2 * h + 1, half)
        p = acc[first, :].astype(BF16).astype(F32)
        q = acc[second, :].astype(BF16).astype(F32)
        rot[first, :] = (p * cos - q * sin).astype(BF16)
        rot[second, :] = (q * cos + p * sin).astype(BF16)
    loop(q_all // hd, turn)
    for k in range(groups):
        turn(q_all // hd + 2 * k)
        vs = seg(q_all // hd + 2 * k + 1, hd)
        rot[vs, :] = acc[vs, :].astype(BF16)
    per = N_DEV // groups
    q_rows = lambda peer: seg(peer, qw)
    kv_rows = lambda peer: seg(q_all // (2 * hd) + peer // per, 2 * hd)
    qs = Swap(lambda peer: rot.at[q_rows(peer), :], lambda o: qkv_ref.at[:qw, seg(o, tokens)], qsems, me)
    kvs = Swap(lambda peer: rot.at[kv_rows(peer), :], lambda o: qkv_ref.at[qw:, seg(o, tokens)], ksems, me)
    qs.start()
    kvs.start()
    gw.start()
    keep_own(wo_ref, full_w, me)
    gain_row(g_scr, small_all, 1)
    qkv_ref[:qw, seg(me, tokens)] = rot[q_rows(me), :]
    qkv_ref[qw:, seg(me, tokens)] = rot[kv_rows(me), :]
    wgu_ref[:feat, seg(me)] = wg_t[seg(me, feat), :]
    wgu_ref[feat:, seg(me)] = wu_t[seg(me, feat), :]
    gates.start((CORE,))
    ups.start((CORE,))
    for swap in (qs, kvs):
        swap.wait_recv()
    stores = fetch_all(esem, (qkv_ref, qkv_out), (u_scr, u_out), (cos_ref, cos_out), (sin_ref, sin_out))
    heads = qkv_ref.shape[0] // hd - 2
    seq = qkv_ref.shape[1]
    scale = hd ** -0.5
    lanes = heads * QB
    key_rows(k_scr, qkv_ref, qw, hd)

    outs = Swap(lambda peer: o_send.at[seg(peer), :], lambda o: o_tok.at[:, seg(o)], osems, me)

    def q_block(qb):
        for at, r in ((2, 0), (4, 1), (5, 2), (6, 3), (7, 4)):
            @pl.when(qb == at)
            def _():
                gw.round(r)
        qs = seg(qb, QB)
        q2 = side_by_side(qkv_ref, heads, hd, qs)

        def scores(kb, top, diagonal):
            s = score_block(k_scr[seg(kb, KB), :], q2, scale, diagonal)
            s_scr[seg(kb, KB), :] = s
            return jnp.maximum(top, jnp.max(s, axis=0, keepdims=True))

        top = lax.fori_loop(0, qb, lambda kb, t: scores(kb, t, False), jnp.full((1, lanes), NEG_LARGE, F32))
        top = scores(qb, top, True)

        def expo(kb, tot):
            e = jnp.exp(s_scr[seg(kb, KB), :] - top)
            s_scr[seg(kb, KB), :] = e
            return tot + jnp.sum(e, axis=0, keepdims=True)

        inv = 1.0 / lax.fori_loop(0, qb + 1, expo, jnp.zeros((1, lanes), F32))

        def weigh(kb, acc):
            p = (s_scr[seg(kb, KB), :] * inv).astype(BF16)
            return acc + mm(qkv_ref[qw + hd:, seg(kb, KB)], p, NN)

        acc = lax.fori_loop(0, qb + 1, weigh, jnp.zeros((hd, lanes), F32))
        for h in range(heads):
            o_ref[h * hd:(h + 1) * hd, qs] = acc[:, h * QB:(h + 1) * QB].astype(BF16)
        stat_ref[qb, :1, :] = top
        stat_ref[qb, 1:, :] = inv
        o_send[qs, :] = o_ref[:, qs].T

    loop(seq // QB, q_block)
    outs.start()
    advance(3)
    o_tok[:, seg(me)] = o_send[seg(me), :]
    for r in (5, 6):
        gw.round(r)
    outs.wait_recv()
    for mask in CHIP_MASKS:
        gw.wait_pair(mask)

    def project(n):
        cs = seg(n, CHUNK)
        acc_o[:, cs] = mm(o_tok[...], full_w[:, :, cs].reshape(dim, CHUNK), NN)
    loop(dim // CHUNK, project)

    def residual(i):
        rs = seg(i, STRIP)
        h_ref[rs, :] = (x_ref[rs, :].astype(F32) + acc_o[rs, :]).astype(BF16)
    loop(tokens // STRIP, residual)
    norm_rows(h_ref, g_scr, m_ref)
    for swap in (gates, ups):
        swap.wait_recv()
    for mask in CHIP_MASKS:
        keep(mask).wait()
    outs.wait_send()
    for swap in (gates, ups):
        swap.wait_send((CORE,) + SETS[3])
    for store in stores:
        store.wait()
    g.finish()
    gw.finish()
    for swap in (smalls, qs, kvs):
        swap.wait_send()


def dw_swaps(stage, gate_hbm, up_hbm, sems, me):
    feat = gate_hbm.shape[0] // N_DEV
    return [Swap(lambda peer, lo=lo: stage(peer).at[lo:lo + feat, seg(peer % 2)], lambda o, dst=dst: dst.at[seg(o, feat), :], sems[i:i + 2], me)
            for lo, dst, i in ((0, gate_hbm, 0), (feat, up_hbm, 2))]


def mlp(m_ref, dout_ref, wgu_hbm, down_hbm, u_ref, h_ref, small_all, wo_ref, o_ref,
        ucol_ref, m_out, dgu_out, ddown_out, y_ref, dh_ref, do_ref, dwo_ref, dg_ref, gate_hbm, up_hbm,
        wgu_ref, down_ref, glu_ref, dgu_ref, ddown_ref, isem, dsem, full_d, full_m, osem, stage, g_scr, dgu_t, glu_t, free, *scr):
    me = lax.axis_index('sp')
    feat, dim = down_ref.shape
    loads = fetch_all(isem, (wgu_hbm, wgu_ref), (down_hbm, down_ref))
    enter(me, OTHERS)
    sems = scr[4:]
    gd = row_gather(dout_ref, full_d, sems[:4], me, 0)
    gm = row_gather(m_ref, full_m, sems[4:8], me, 2)
    g = row_gather(dh_ref, full_d, sems[8:12], me, 1)
    ucols = Swap(lambda peer: u_ref.at[:, seg(peer)], lambda o: ucol_ref.at[seg(o), :], sems[12:14], me)
    gates, ups = dw_swaps(lambda peer: stage, gate_hbm, up_hbm, sems[14:18], me)
    gm.start()
    gd.start()
    keep_own(m_ref, full_m, me)
    keep_own(dout_ref, full_d, me)
    gain_row(g_scr, small_all, 1)
    dwo_ref[...] = jnp.zeros_like(dwo_ref)
    ddown_ref[...] = jnp.zeros_like(ddown_ref)

    def keep(mask):
        chip = flipped(me, mask) // 2
        ts = seg(chip, WIDE)
        ends = ((full_m.at[chip], m_out.at[chip]), (dgu_ref.at[:, ts], dgu_out.at[:, ts]))
        return [pltpu.make_async_copy(src, dst, osem.at[mask // 2, i]) for i, (src, dst) in enumerate(ends)]

    for load in loads:
        load.wait()
    ucol_ref[seg(me), :] = u_ref[:, seg(me)]

    def use(mask):
        gd.wait_pair(mask)
        gm.wait_pair(mask)
        chip = flipped(me, mask) // 2
        ts = seg(chip, WIDE)
        gu = mm(wgu_ref[...], full_m[chip], NT).astype(BF16).astype(F32)
        gate, up = gu[:feat], gu[feat:]
        d_glu = mm(down_ref[...], full_d[chip], NT).astype(BF16).astype(F32)
        sig = jax.nn.sigmoid(gate)
        act = gate * sig
        glu = (act * up).astype(BF16)
        glu_ref[:, ts] = glu
        dgu_ref[:feat, ts] = (d_glu * up * (sig * (1.0 + gate * (1.0 - sig)))).astype(BF16)
        dgu_ref[feat:, ts] = (d_glu * act).astype(BF16)

        def step(n):
            ddown_ref[:, seg(n, CHUNK)] += mm(glu, full_d[chip, :, seg(n, CHUNK)], NN)
        loop(dim // CHUNK, step)
        for copy in keep(mask):
            copy.start()

    for r in range(len(gm.ROUNDS)):
        gm.round(r)
        gd.round(r)
        if r == 3:
            ucols.start()
        run_ready(gm.READY[r], use)
    far = seg(flipped(me, XYZ) // 2, WIDE)
    stage[...] = mm(dgu_ref[...], full_m[:, :, far].reshape(dgu_ref.shape[1], WIDE), NN)
    for swap in (gates, ups):
        swap.start(SETS[0])
    for gather in (gd, gm):
        gather.finish()
    leave = pltpu.make_async_copy(ddown_ref, ddown_out, dsem)
    leave.start()
    s = Scatter(*scr[:4], sems[18:], me)
    total = s.run(block_product(s, dgu_ref, wgu_ref, dgu_t))
    for mask in NEAR:
        pl.semaphore_signal(free, inc=1, device_id=(flipped(me, mask),), device_id_type=MESH)
    norm_back(total, h_ref, g_scr, dout_ref, dh_ref, dg_ref)
    g.start()
    keep_own(dh_ref, full_d, me)
    s.finish()
    pl.semaphore_wait(free, len(NEAR))

    def use_dh(mask):
        g.wait_pair(mask)
        chip = flipped(me, mask) // 2
        do_ref[:, seg(chip, WIDE)] = mm(wo_ref[...], full_d[chip], NT).astype(BF16)
        o = o_ref[:, seg(chip, WIDE)]

        def step(n):
            dwo_ref[:, seg(n, CHUNK)] += mm(o, full_d[chip, :, seg(n, CHUNK)], NN)
        loop(dim // CHUNK, step)

    def between(i):
        r = i if i < 3 else i - N_CHIP + 3
        if i < 3 or i >= N_CHIP:
            g.round(r)
            run_ready(g.READY[r], use_dh)

    s = Scatter(*scr[:4], sems[18:], me)
    total = s.run(block_product(s, glu_ref, down_ref, glu_t), between)
    y_ref[...] = (h_ref[...].astype(F32) + total[...]).astype(BF16)
    s.finish()
    g.finish()
    for swap in (gates, ups):
        swap.wait_recv(SETS[0])
        swap.wait_send(SETS[0])
    ucols.wait_recv()
    ucols.wait_send()
    leave.wait()
    ends = ((full_m.at[0], m_out.at[0]), (dgu_ref.at[:, seg(0, WIDE)], dgu_out.at[:, seg(0, WIDE)]))
    loop(N_CHIP, lambda j: [pltpu.make_async_copy(src, dst, osem.at[j, i]).wait() for i, (src, dst) in enumerate(ends)])


def back(groups, hd, qkv_hbm, do_hbm, stat_ref, cos_all, sin_all, dgu_hbm, m_hbm, ucol_ref, w_hbm, x_ref, small_all, dh_ref, dg2_ref, dg_in, du_in,
         dg_hbm, du_hbm, dwq_ref, dwkv_ref, dx_ref, gain_ref,
         dgu_ref, qkv_ref, do_ref, isem, qsem,
         p_scr, dp_scr, k_scr, v_scr, dk_acc, dv_acc, stage, dq_scr, dkv_scr, m_scr,
         full, w_scr, shares, dkv_own, full_kv, dqkv, dn, g_scr, dg1, gains, gains_in, wsem, lsem, msem, *sems):
    heads = qkv_ref.shape[0] // hd - 2
    seq = qkv_ref.shape[1]
    scale = hd ** -0.5
    lanes = heads * QB
    qw = heads * hd
    half = hd // 2
    me = lax.axis_index('sp')
    feat = dgu_ref.shape[0] // 2
    first = (X, Y + Z, Y, X + Z, Z, X + Y, 0)

    def fetch(mask):
        cols = seg(flipped(me, mask) // 2, WIDE)
        return pltpu.make_async_copy(m_hbm.at[:, :, cols], m_scr.at[:, :, cols], msem.at[mask // 2])
    needed, = fetch_all(isem, (dgu_hbm, dgu_ref))
    for mask in first[:2]:
        fetch(mask).start()
    load = pltpu.make_async_copy(w_hbm, w_scr, wsem)
    enter(me, OTHERS)
    for mask in first[2:]:
        fetch(mask).start()
    loads = fetch_all(qsem, (qkv_hbm, qkv_ref), (do_hbm, do_ref))
    gain_row(g_scr, small_all, 0)

    gates, ups = dw_swaps(lambda peer: stage.at[peer // 2], dg_hbm, du_hbm, sems[:4], me)
    gq = row_gather(dq_scr, full, sems[6:10], me)
    own = [pltpu.make_async_copy(swap.src(me), swap.dst(me), lsem.at[i]) for i, swap in enumerate((gates, ups))]

    def make(mask):
        chip = flipped(me, mask) // 2
        fetch(mask).wait()
        cols = m_scr[:, :, seg(chip, WIDE)].reshape(seq, WIDE)
        stage[chip] = mm(dgu_ref[...], cols, NN)

    def advance(n):
        for swap in (gates, ups):
            if n > 1:
                swap.wait_send(SETS[n - 1])
            swap.start(SETS[n])

    needed.wait()
    for i, mask in enumerate(first):
        make(mask)
        if i == 1:
            advance(1)
    load.start()
    for copy in loads:
        copy.wait()
    gates.start((CORE,))
    ups.start((CORE,))
    for copy in own:
        copy.start()

    dk_acc[...] = jnp.zeros_like(dk_acc)
    dv_acc[...] = jnp.zeros_like(dv_acc)
    key_rows(k_scr, qkv_ref, qw, hd)
    key_rows(v_scr, qkv_ref, qw + hd, hd)

    def q_block(qb):
        @pl.when(qb == 5)
        def _():
            advance(2)
        qs = seg(qb, QB)
        q2 = side_by_side(qkv_ref, heads, hd, qs)
        do2 = side_by_side(do_ref, heads, hd, qs)
        top = stat_ref[qb, :1, :]
        inv = stat_ref[qb, 1:, :]

        def probs(kb, rd, diagonal):
            ks = seg(kb, KB)
            s = score_block(k_scr[ks, :], q2, scale, diagonal)
            p = jnp.exp(s - top) * inv
            dp = mm(v_scr[ks, :], do2, NN).astype(BF16)
            p_scr[ks, :] = p
            dp_scr[ks, :] = dp
            dv_acc[ks, :] += mm(p.astype(BF16), do2, NT)
            return rd + jnp.sum(dp.astype(F32) * p, axis=0, keepdims=True)

        rd = lax.fori_loop(0, qb, lambda kb, r: probs(kb, r, False), jnp.zeros((1, lanes), F32))
        rd = probs(qb, rd, True)

        def d_scores(kb, acc):
            ks = seg(kb, KB)
            ds = (p_scr[ks, :] * (dp_scr[ks, :].astype(F32) - rd) * scale).astype(BF16)
            dk_acc[ks, :] += mm(ds, q2, NT)
            return acc + mm(qkv_ref[qw:qw + hd, ks], ds, NN)

        acc = lax.fori_loop(0, qb + 1, d_scores, jnp.zeros((hd, lanes), F32))
        cos, sin = cos_all[:, qs], sin_all[:, qs]
        for h in range(heads):
            dq = acc[:, h * QB:(h + 1) * QB].astype(BF16).astype(F32)
            p, q = dq[:half], dq[half:]
            dq_scr[h * hd:h * hd + half, qs] = (p * cos + q * sin).astype(BF16)
            dq_scr[h * hd + half:(h + 1) * hd, qs] = (q * cos - p * sin).astype(BF16)

    loop(seq // QB, q_block)

    def share(i):
        rs = seg(i, WIDE)
        dkv_scr[rs, :] = jnp.concatenate([dk_acc[rs, :], dv_acc[rs, :]], axis=1).astype(BF16)
    loop(seq // WIDE, share)
    tokens = ucol_ref.shape[1]
    per = N_DEV // groups
    q_all = dwq_ref.shape[0]
    sh = Swap(lambda peer: dkv_scr.at[seg(peer, tokens), :], lambda o: shares.at[o], sems[4:6], me)
    parts = thirds(dkv_own.shape[0], STRIP)
    gk = Gather(dkv_own, lambda o: full_kv.at[:, seg(o, tokens)], lambda view, c: [view.at[pl.ds(*parts[c]), :]], sems[10:14], me)
    gs = Swap(lambda peer: gains.at[:, seg(peer)], lambda o: gains_in.at[o], sems[14:], me)
    sh.start()
    gq.start()
    keep_own(dq_scr, full, me)
    shares[me] = dkv_scr[seg(me, tokens), :]
    sh.wait_recv()
    cos, sin = cos_all[:, seg(me)], sin_all[:, seg(me)]
    for k in range(groups):
        both = sum(shares[per * k + i].astype(F32) for i in range(per)).astype(BF16).astype(F32).T
        p, q = both[:half], both[half:hd]
        lo = 2 * hd * k
        dkv_own[lo:lo + half, :] = (p * cos + q * sin).astype(BF16)
        dkv_own[lo + half:lo + hd, :] = (q * cos - p * sin).astype(BF16)
        dkv_own[lo + hd:lo + 2 * hd, :] = both[hd:].astype(BF16)
    gk.start()
    full_kv[:, seg(me, tokens)] = dkv_own[...]
    for k in range(groups):
        dqkv[:, q_all + 2 * hd * k:q_all + 2 * hd * (k + 1)] = dkv_own[2 * hd * k:2 * hd * (k + 1), :].T

    def use(mask):
        gq.wait_pair(mask)
        chip = flipped(me, mask) // 2
        dwq_ref[seg(chip, WIDE), :] = mm(full[chip], ucol_ref[...], NN)
        dqkv[:, seg(chip, WIDE)] = full[chip, :, seg(me, tokens)].T

    for r in range(len(gq.ROUNDS)):
        gq.round(r)
        gk.round(r)
        if r == 3:
            advance(3)
        run_ready(gq.READY[r], use)
    load.wait()

    def normed(i):
        dn[:, seg(i, WIDE)] = mm(dqkv[...], w_scr[i], NN)
    loop(N_CHIP, normed)
    norm_back(dn, x_ref, g_scr, dh_ref, dx_ref, dg1)
    gains[...] = jnp.concatenate([jnp.sum(dg1[...], axis=0, keepdims=True), jnp.sum(dg2_ref[...], axis=0, keepdims=True),
                                  jnp.zeros((N_CHIP - 2, dg1.shape[1]), F32)], axis=0)
    gs.start()
    gains_in[me] = gains[:, seg(me)]
    for mask in CHIP_MASKS:
        gk.wait_pair(mask)
    dwkv_ref[...] = mm(full_kv[...], ucol_ref[...], NN)
    gs.wait_recv()
    gain_ref[...] = sum(gains_in[o] for o in range(N_DEV))
    for swap in (gates, ups):
        swap.wait_recv((CORE,) + SETS[1] + SETS[2] + SETS[3])
        swap.wait_send((CORE,) + SETS[3])
    for copy in own:
        copy.wait()
    for c in (sh, gs):
        c.wait_send()
    for g in (gq, gk):
        g.finish()


def finish(dg_hbm, du_hbm, dkv_hbm, *refs):
    n = (len(refs) - 14) // 3
    gains, refs = refs[0], refs[1:]
    srcs, (gate, up, dk, dv, dg1, dg2), refs = refs[:n], refs[n:n + 6], refs[n + 6:]
    dsts, (g_in, g_out, kv_in), holds, sems = refs[:n], refs[n:n + 3], refs[n + 3:2 * n + 3], refs[2 * n + 3:]
    dg1[...] = gains[:1, :]
    dg2[...] = gains[1:2, :]
    t_in, t_out, p_in, p_out = sems
    step = LANE * 11
    cols = g_in.shape[1]
    hd = dk.shape[0] // (kv_in.shape[0] // LANE)
    starts = [(w, i) for i in range(cols // step) for w in range(2)]

    def fetch(w, i):
        rs = pl.ds(i * step, step)
        return pltpu.make_async_copy((dg_hbm, du_hbm)[w].at[rs, :], g_in.at[w, rs, :], t_in.at[w, i])

    def put(w, i):
        cs = pl.ds(i * step, step)
        return pltpu.make_async_copy(g_out.at[w, :, cs], (gate, up)[w].at[:, cs], t_out.at[w, i])
    moves = [(pltpu.make_async_copy(a, h, p_in.at[k]), pltpu.make_async_copy(h, b, p_out.at[k])) for k, (a, h, b) in enumerate(zip(srcs, holds, dsts))]
    kv = pltpu.make_async_copy(dkv_hbm, kv_in, p_in.at[n])
    for w, i in starts:
        fetch(w, i).start()
    kv.start()
    for load, _ in moves:
        load.start()
    for w, i in starts:
        fetch(w, i).wait()

        at = pl.ds(i * step, step)
        g_out[w, :, at] = g_in[w, at, :].T
        put(w, i).start()
    kv.wait()
    for k in range(dk.shape[0] // hd):
        for i, ref in enumerate((dk, dv)):
            ref[k * hd:(k + 1) * hd, :] = kv_in[(2 * k + i) * hd:(2 * k + i + 1) * hd, :]
    for load, store in moves:
        load.wait()
        store.start()
    for w, i in starts:
        put(w, i).wait()
    for _, store in moves:
        store.wait()


def solution(mesh):
    assert mesh.shape['sp'] == N_DEV

    def layer_step(x_in, positions, d_out, norm1_gain, norm2_gain, w_q, w_k, w_v, w_o, w_gate, w_up, w_down):
        tokens, dim = x_in.shape
        seq = tokens * N_DEV
        n_q, hd = w_q.shape[1:]
        n_kv = w_k.shape[1]
        qw = n_q // N_DEV * hd
        rows = w_q.shape[0]
        feat = w_down.shape[0]
        cols = (n_q + 2 * n_kv) * hd
        lanes = qw // hd * QB
        vm = pltpu.VMEM
        full = vm((N_CHIP, WIDE, dim), BF16)
        gain_scr = vm((N_CHIP, dim), F32)
        tok_shapes = 2 * (((tokens, dim), BF16),)
        dw_shapes = 2 * (((feat * N_DEV, rows), F32),)

        inv_freq = 1.0 / (ROPE_BASE ** (jnp.arange(hd // 2, dtype=F32) * (2.0 / hd)))
        freq = jnp.broadcast_to(inv_freq[:, None], (hd // 2, rows))
        row = lambda v: v.reshape(1, rows)
        by_head = lambda w: w.transpose(1, 2, 0).reshape(-1, rows)
        wo_own = w_o.reshape(qw, dim)

        args = (x_in, row(norm1_gain), row(norm2_gain), row(positions), by_head(w_q), by_head(w_k), by_head(w_v), freq, w_gate, w_up, wo_own)
        qkv, u, small_all, wqkv, attn_t, stat, wgu, hidden, mlp_in, cos_all, sin_all = call(
            functools.partial(head, n_kv, hd), 0, len(args),
            (((qw + 2 * hd, seq), BF16), tok_shapes[0], ((N_DEV, N_CHIP, rows), F32), ((N_CHIP, cols, WIDE), BF16),
             ((qw, seq), BF16), ((seq // QB, 2, lanes), F32), ((2 * feat, dim), BF16), *tok_shapes, *(2 * (((hd // 2, seq), F32),))),
            [vm(w_gate.shape, BF16), vm(w_up.shape, BF16), vm((qw, dim), BF16), vm((qw + 2 * hd, seq), BF16), vm((tokens, dim), BF16),
             vm((hd // 2, seq), F32), vm((hd // 2, seq), F32), dma(3), dma(4),
             full, vm((tokens, dim), F32), vm((tokens, dim), BF16), vm((seq, qw), BF16),
             vm((N_CHIP, rows), F32), vm((cols, rows), BF16), vm((N_CHIP, cols, WIDE), BF16), vm((cols, tokens), F32), vm((cols, tokens), BF16), gain_scr,
             vm((feat * N_DEV, rows), BF16), vm((feat * N_DEV, rows), BF16), vm((seq, lanes), F32), vm((seq, hd), BF16), dma(N_CHIP),
             *Gather.sems, *(6 * Swap.sems), *Gather.sems], 4 * qw * seq * seq, far_in=(8, 9, 10), far_out=(0, 1, 3, 9, 10))(*args)
        args = (mlp_in, d_out, wgu, w_down, u, hidden, small_all, wo_own, attn_t)
        u_col, m_full, dgu, d_down, y_out, d_hidden, d_attn, d_wo, d_g2, d_gate_t, d_up_t = call(
            mlp, 1, len(args),
            (((seq, rows), BF16), ((N_CHIP, WIDE, dim), BF16), ((2 * feat, seq), BF16), ((feat, dim), F32),
             *tok_shapes, ((qw, seq), BF16), ((qw, dim), F32), ((N_CHIP, dim), F32), *dw_shapes),
            [vm((2 * feat, dim), BF16), vm((feat, dim), BF16),
             vm((feat, seq), BF16), vm((2 * feat, seq), BF16), vm((feat, dim), F32), dma(2), dma(),
             full, full, dma(N_CHIP, 2), vm((2 * feat, WIDE), F32), gain_scr, vm((WIDE, 2 * feat), BF16), vm((WIDE, feat), BF16), pltpu.SemaphoreType.REGULAR,
             *Scatter.scratch(tokens, dim), *(3 * Gather.sems), *(3 * Swap.sems), *Scatter.sems], 12 * feat * seq * dim,
            far_in=(2, 3), far_out=(1, 2, 3, 9, 10))(*args)
        args = (qkv, d_attn, stat, cos_all, sin_all, dgu, m_full, u_col, wqkv, x_in, small_all, d_hidden, d_g2, d_gate_t, d_up_t)
        d_gate_t, d_up_t, d_wq, d_wkv, d_x, gains = call(
            functools.partial(back, n_kv, hd), 3, len(args),
            (*dw_shapes, ((n_q * hd, rows), F32), ((2 * n_kv * hd, rows), F32), tok_shapes[0], ((N_CHIP, rows), F32)),
            [vm((2 * feat, seq), BF16), vm((qw + 2 * hd, seq), BF16), vm((qw, seq), BF16), dma(1), dma(2),
             vm((seq, lanes), F32), vm((seq, lanes), BF16), vm((seq, hd), BF16), vm((seq, hd), BF16), vm((seq, hd), F32), vm((seq, hd), F32),
             vm((N_CHIP, 2 * feat, WIDE), F32), vm((qw, seq), BF16), vm((seq, 2 * hd), BF16), full,
             full, vm((N_CHIP, cols, WIDE), BF16), vm((N_DEV, tokens, 2 * hd), BF16), vm((2 * n_kv * hd, tokens), BF16), vm((2 * n_kv * hd, seq), BF16),
             vm((tokens, cols), BF16), vm((tokens, dim), F32), gain_scr, gain_scr, gain_scr, vm((N_DEV, N_CHIP, rows), F32), dma(), dma(2), dma(N_CHIP),
             *(3 * Swap.sems), *(2 * Gather.sems), *Swap.sems], 10 * qw * seq * seq, far_in=(0, 1, 5, 6, 8, 13, 14), far_out=(0, 1), aliases={13: 0, 14: 1})(*args)
        moved = (d_wq, d_wo, d_down, d_x, y_out)
        one_row = jax.ShapeDtypeStruct((1, rows), F32)
        half_kv = jax.ShapeDtypeStruct((n_kv * hd, rows), F32)
        wide = jax.ShapeDtypeStruct((rows, feat * N_DEV), F32)
        d_gate, d_up, d_wk, d_wv, d_g1, d_g2, d_wq, d_wo, d_down, d_x, y_out = pl.pallas_call(
            finish,
            out_shape=[wide, wide, half_kv, half_kv, one_row, one_row] + [jax.ShapeDtypeStruct(v.shape, v.dtype) for v in moved],
            in_specs=[IN_HBM] * 3 + on_chip(1) + [IN_HBM] * len(moved), out_specs=[IN_HBM] * 2 + on_chip(4) + [IN_HBM] * len(moved),
            scratch_shapes=[vm((2, feat * N_DEV, rows), F32), vm((2, rows, feat * N_DEV), F32), vm(d_wkv.shape, F32)]
            + [vm(v.shape, v.dtype) for v in moved] + [dma(2, 4), dma(2, 4), dma(len(moved) + 1), dma(len(moved))],
            compiler_params=pltpu.CompilerParams(vmem_limit_bytes=VMEM_CAP), name='finish',
        )(d_gate_t, d_up_t, d_wkv, gains, *moved)
        by_row = lambda g, heads: g.reshape(heads, hd, rows).transpose(2, 0, 1)
        return (y_out, d_x, d_g1.reshape(rows), d_g2.reshape(rows), by_row(d_wq, n_q), by_row(d_wk, n_kv), by_row(d_wv, n_kv),
                d_wo.reshape(w_o.shape), d_gate, d_up, d_down)

    all_rows = P('sp')
    return jax.shard_map(layer_step, mesh=mesh, in_specs=(all_rows,) * 12, out_specs=(all_rows,) * 11, check_vma=False)
```
